32 devices in a mesh: seq: 8 (over z, core), fsdp: 4 (over y, x).
Axes of the slice: x: 2, y: 2, z: 4, core: 2. Of those that a mesh axis runs over, the one named last changes fastest.
Arguments:
- tokens: bfloat16 [4, 2048, 1792], P('fsdp', 'seq'), may hold values from -4 to 4
- seq_lengths: int32 [4, 1], P('fsdp'), may hold values from 1024 to 2048, as said below
- seq_offsets: int32 [4, 1], P('fsdp'), may hold values from 0 to 1024, as said below
- norm1_gain: bfloat16 [1792], P('fsdp'), may hold values from 0.5 to 1.5
- conv_weight: bfloat16 [1792, 3], P('fsdp'), may hold values from -0.8984375 to 0.8984375
- query_weight: bfloat16 [1792, 1792], P('fsdp'), may hold values from -0.125 to 0.125
- key_weight: bfloat16 [1792, 1792], P('fsdp'), may hold values from -0.125 to 0.125
- value_weight: bfloat16 [1792, 1792], P('fsdp'), may hold values from -0.125 to 0.125
- out_weight: bfloat16 [1792, 1792], P('fsdp'), may hold values from -0.75 to 0.75
- norm2_gain: bfloat16 [1792], P('fsdp'), may hold values from 0.5 to 1.5
- gate_weight: bfloat16 [1792, 4864], P('fsdp'), may hold values from -0.125 to 0.125
- up_weight: bfloat16 [1792, 4864], P('fsdp'), may hold values from -0.125 to 0.125
- down_weight: bfloat16 [4864, 1792], P('fsdp'), may hold values from -0.15625 to 0.15625
- cotangent: bfloat16 [4, 2048, 1792], P('fsdp', 'seq'), may hold values from -4 to 4
Outputs:
- layer_out: bfloat16 [4, 2048, 1792], P('fsdp', 'seq')
- tokens_grad: float32 [4, 2048, 1792], P('fsdp', 'seq')
- norm1_grad: float32 [1792], P('fsdp')
- conv_grad: float32 [1792, 3], P('fsdp')
- query_grad: float32 [1792, 1792], P('fsdp')
- key_grad: float32 [1792, 1792], P('fsdp')
- value_grad: float32 [1792, 1792], P('fsdp')
- out_grad: float32 [1792, 1792], P('fsdp')
- norm2_grad: float32 [1792], P('fsdp')
- gate_grad: float32 [1792, 4864], P('fsdp')
- up_grad: float32 [1792, 4864], P('fsdp')
- down_grad: float32 [4864, 1792], P('fsdp')
The draws below stay inside these ranges and needn't reach their ends.
Inputs may be any that keep to these rules, and one draw needn't show every extreme that they name: `seq_lengths`: every group holds 1 sequence, each between 1024 and 2048 tokens long; some group has one of exactly 2048 tokens and some group one of exactly 1024. `seq_offsets`: sequence j of a group lies within slots j * 2048 to (j + 1) * 2048 - 1 of the group; all other slots are padding.
All inputs are finite; a program needn't handle non-finite values.
Results may differ from the reference program's by a relative error of at most 0.015.
Values may be sent and summed in bfloat16 or wider, within the bound.
A program may use at most 512 MiB of HBM per device.

```python
import jax
import jax.numpy as jnp
from jax import lax

D = 1792
HEADS = 16
FF = 4864
WINDOW = 64
TOK_DEV = 256
HEAD_DIM = 112
GROUPS = 4
GROUP = 2048
NSEQ = 1
REGION = 2048
N_SEQ = 8


def draw_layout(key):
    length_key = jax.random.fold_in(key, 101)
    shift_key = jax.random.fold_in(key, 202)
    lengths = jax.random.randint(length_key, (GROUPS, NSEQ), REGION // 2, REGION + 1, dtype=jnp.int32)
    lengths = lengths.at[1, NSEQ - 1].set(REGION // 2)
    lengths = lengths.at[0, 0].set(REGION).at[1, 0].set(REGION // 2)
    spread = jax.random.randint(shift_key, (GROUPS, NSEQ), 0, 1048576, dtype=jnp.int32)
    shifts = spread % (REGION - lengths + 1)
    shifts = shifts.at[1, NSEQ - 1].set(REGION - REGION // 2)
    starts = jnp.arange(NSEQ, dtype=jnp.int32)[None, :] * REGION + shifts
    return (lengths.astype(jnp.int32), starts.astype(jnp.int32))


def draw_seq_lengths(key, part):
    return draw_layout(key)[0]


def draw_seq_offsets(key, part):
    return draw_layout(key)[1]


def level_of(rng, shape, cuts, smallest, top_value):
    level, own = 1.0, jax.random.fold_in(rng, 6)
    for axis_at, blocks in cuts:
        steps = jnp.exp(jax.random.uniform(jax.random.fold_in(own, axis_at), (blocks,), jnp.float32, smallest / len(cuts), top_value / len(cuts)))
        level = level * jnp.repeat(steps, shape[axis_at] // blocks).reshape([-1 if axis == axis_at else 1 for axis in range(len(shape))])
    return level


def scatter_about(rng, extent, deviation, most, shards=(), kind=jnp.bfloat16):
    values = deviation * jax.random.normal(rng, extent, jnp.float32)
    if shards:
        values = values * level_of(rng, extent, shards, -0.22, 0.18)
    return jnp.clip(values, -most, most).astype(kind)


def setup_inputs(seed: int = 0) -> dict:
    seeds = jax.random.split(jax.random.key(seed), 15)
    return {
        "tokens": scatter_about(seeds[0], (GROUPS, GROUP, D), 1.0, 4.0, ((0, 4), (1, 8))),
        "seq_lengths": draw_seq_lengths(jax.random.fold_in(seeds[14], 71), 0),
        "seq_offsets": draw_seq_offsets(jax.random.fold_in(seeds[14], 71), 0),
        "norm1_gain": jnp.clip(1.0 + 0.1 * jax.random.normal(seeds[3], (D,), jnp.float32), 0.5, 1.5).astype(jnp.bfloat16),
        "conv_weight": jnp.clip(jax.random.uniform(seeds[4], (D, 3), jnp.float32, -0.8984375, 0.8984375) * level_of(seeds[4], (D, 3), ((0, 4),), -0.4, 0.0), -0.8984375, 0.8984375).astype(jnp.bfloat16),
        "query_weight": scatter_about(seeds[5], (D, D), D ** -0.5, 0.125, ((0, 4),)),
        "key_weight": scatter_about(seeds[6], (D, D), D ** -0.5, 0.125, ((0, 4),)),
        "value_weight": scatter_about(seeds[7], (D, D), D ** -0.5, 0.125, ((0, 4),)),
        "out_weight": scatter_about(seeds[8], (D, D), (D // 32) ** -0.5, 0.75, ((0, 4),)),
        "norm2_gain": jnp.clip(1.0 + 0.1 * jax.random.normal(seeds[9], (D,), jnp.float32), 0.5, 1.5).astype(jnp.bfloat16),
        "gate_weight": scatter_about(seeds[10], (D, FF), D ** -0.5, 0.125, ((0, 4),)),
        "up_weight": scatter_about(seeds[11], (D, FF), D ** -0.5, 0.125, ((0, 4),)),
        "down_weight": scatter_about(seeds[12], (FF, D), (FF // 4) ** -0.5, 0.15625, ((0, 4),)),
        "cotangent": scatter_about(seeds[13], (GROUPS, GROUP, D), 1.0, 4.0, ((0, 4), (1, 8))),
    }


EPS = 1e-05
NEG = -1e+30

@jax.custom_vjp
def low(v):
    return lax.optimization_barrier(v.astype(jnp.bfloat16)).astype(jnp.float32)

@jax.custom_vjp
def low_back(v):
    return v

def low_keep(v):
    return (low(v), None)

def low_pass(kept, grad):
    return (grad,)

def back_keep(v):
    return (v, None)

def back_low(kept, grad):
    return (low(grad),)
low.defvjp(low_keep, low_pass)
low_back.defvjp(back_keep, back_low)

def matmul(left, right):
    return jnp.dot(left, right, precision=lax.Precision.HIGHEST, preferred_element_type=jnp.float32)

def segment_ids(slot_index, lengths, starts):
    inside = (slot_index[:, None] >= starts[None, :]) & (slot_index[:, None] < starts[None, :] + lengths[None, :])
    number = jnp.arange(lengths.shape[0], dtype=jnp.int32) + 1
    found = lax.optimization_barrier(jnp.max(jnp.where(inside, number[None, :], 0), axis=1)) - 1
    return jnp.where(slot_index < 0, -2, found)

def layer(tokens, norm_one, conv_taps, query_map, key_map, value_map, out_map, norm_two, gate_map, up_map, down_map, segment, live_mask):
    scale_one = lax.rsqrt(lax.optimization_barrier(jnp.mean(tokens * tokens, axis=1, keepdims=True)) + EPS)
    normed = tokens * scale_one * norm_one
    zero_row = jnp.zeros((1, D), jnp.float32)
    back_one = jnp.concatenate([zero_row, normed[:-1]], 0)
    back_two = jnp.concatenate([zero_row, zero_row, normed[:-2]], 0)
    edge_segment = jnp.full((2,), -2, jnp.int32)
    segment_pad = jnp.concatenate([edge_segment, segment.astype(jnp.int32)])
    same_one = (segment == segment_pad[1:-1]).astype(jnp.float32)[:, None]
    same_two = (segment == segment_pad[:-2]).astype(jnp.float32)[:, None]
    conv_mix = normed * conv_taps[:, 0] + same_one * back_one * conv_taps[:, 1] + same_two * back_two * conv_taps[:, 2]
    gated_rows = low(conv_mix * normed)
    queries = low_back(low(matmul(gated_rows, query_map)))
    key_rows = low_back(low(matmul(gated_rows, key_map)))
    values = low_back(low(matmul(gated_rows, value_map)))
    key_pad = jnp.concatenate([jnp.zeros((WINDOW, D), jnp.float32), key_rows], 0)
    value_pad = jnp.concatenate([jnp.zeros((WINDOW, D), jnp.float32), values], 0)
    segment_keys = jnp.concatenate([jnp.full((WINDOW,), -2, jnp.int32), segment.astype(jnp.int32)])
    distance = jnp.arange(TOK_DEV, dtype=jnp.int32)[:, None] + WINDOW - jnp.arange(TOK_DEV + WINDOW, dtype=jnp.int32)[None, :]

    def attend_block(block_index):
        row_start = block_index * TOK_DEV
        query_block = lax.dynamic_slice_in_dim(queries, row_start, TOK_DEV, 0)
        key_block = lax.dynamic_slice_in_dim(key_pad, row_start, TOK_DEV + WINDOW, 0)
        value_block = lax.dynamic_slice_in_dim(value_pad, row_start, TOK_DEV + WINDOW, 0)
        query_segment = lax.dynamic_slice_in_dim(segment.astype(jnp.int32), row_start, TOK_DEV, 0)
        key_segment = lax.dynamic_slice_in_dim(segment_keys, row_start, TOK_DEV + WINDOW, 0)
        window_mask = (distance >= 0) & (distance <= WINDOW) & (query_segment[:, None] == key_segment[None, :])
        query_heads = query_block.reshape(TOK_DEV, HEADS, HEAD_DIM)
        key_heads = key_block.reshape(TOK_DEV + WINDOW, HEADS, HEAD_DIM)
        value_heads = value_block.reshape(TOK_DEV + WINDOW, HEADS, HEAD_DIM)
        scores = low_back(jnp.einsum('qhd,khd->hqk', query_heads, key_heads, precision=lax.Precision.HIGHEST) * HEAD_DIM ** (-0.5))
        scores = jnp.where(window_mask[None], scores, NEG)
        row_peak = lax.optimization_barrier(jnp.max(scores, axis=2, keepdims=True))
        exponent = jnp.exp(scores - row_peak)
        softmax_w = low(exponent / lax.optimization_barrier(jnp.sum(exponent, axis=2, keepdims=True)))
        mixed = jnp.einsum('hqk,khd->qhd', softmax_w, value_heads, precision=lax.Precision.HIGHEST)
        return mixed.reshape(TOK_DEV, D)
    blocks = lax.map(jax.checkpoint(attend_block), jnp.arange(N_SEQ, dtype=jnp.int32))
    heads_out = low_back(low(blocks.reshape(GROUP, D)))
    branch = low_back(matmul(heads_out, out_map))
    middle = tokens + branch
    scale_two = lax.rsqrt(lax.optimization_barrier(jnp.mean(middle * middle, axis=1, keepdims=True)) + EPS)
    normed_two = low(middle * scale_two * norm_two)
    gate_act = low_back(matmul(normed_two, gate_map))
    up_act = low_back(matmul(normed_two, up_map))
    hidden = low(jax.nn.silu(gate_act) * up_act)
    feed = low_back(matmul(hidden, down_map))
    return live_mask * (middle + feed)

def reference(tokens, seq_lengths, seq_offsets, norm1_gain, conv_weight, query_weight, key_weight, value_weight, out_weight, norm2_gain, gate_weight, up_weight, down_weight, cotangent):
    params = tuple((weight.astype(jnp.float32) for weight in (norm1_gain, conv_weight, query_weight, key_weight, value_weight, out_weight, norm2_gain, gate_weight, up_weight, down_weight)))
    slot_index = jnp.arange(GROUP, dtype=jnp.int32)

    def group_step(totals, group_data):
        group_tokens, group_grad, lengths, starts = group_data
        segment = segment_ids(slot_index, lengths.astype(jnp.int32), starts.astype(jnp.int32))
        live_mask = (segment >= 0).astype(jnp.float32)[:, None]

        def run_layer(layer_in, *weights):
            return layer(layer_in, *weights, segment, live_mask)
        result, pullback = jax.vjp(run_layer, group_tokens.astype(jnp.float32), *params)
        gradients = pullback(group_grad.astype(jnp.float32))
        totals = tuple((total + grad_term for total, grad_term in zip(totals, gradients[1:])))
        return (totals, (result.astype(jnp.bfloat16), gradients[0]))
    start_totals = tuple((jnp.zeros(weight.shape, jnp.float32) for weight in params))
    totals, (outputs, input_grads) = lax.scan(group_step, start_totals, (tokens, cotangent, seq_lengths, seq_offsets))
    return (outputs, input_grads, totals[0], totals[1], totals[2], totals[3], totals[4], totals[5], totals[6], totals[7], totals[8], totals[9])
```

```python
import functools

import jax
import jax.numpy as jnp
from jax import lax
from jax.experimental import pallas as pl
from jax.experimental.pallas import tpu as pltpu
from jax.sharding import PartitionSpec as P

HEADS = 16
WINDOW = 64
HEAD_DIM = 112
BLOCK = 128

EPS = 1e-05
NEG = -1e30
SCALE = HEAD_DIM ** (-0.5)
MESH_ID = pl.DeviceIdType.MESH
BF = jnp.bfloat16
F32 = jnp.float32


def shifted(array, axis, by):
    length = lax.axis_size(axis)
    pairs = [(i, i + by) for i in range(length) if 0 <= i + by < length]
    return lax.ppermute(array, axis, pairs)


def segment_of(slot, count, lengths, starts):
    found = jnp.full(slot.shape, -1, jnp.int32)
    for j in range(count):
        inside = (slot >= starts(j)) & (slot < starts(j) + lengths(j))
        found = jnp.where(inside, j, found)
    return jnp.where(slot < 0, -2, found)


def dot_rows(left, right):
    return lax.dot_general(left, right, (((0,), (0,)), ((), ())), preferred_element_type=F32)


def dot_trans(left, right):
    return lax.dot_general(left, right, (((1,), (1,)), ((), ())), preferred_element_type=F32)


def dot(left, right):
    return jnp.dot(left, right, preferred_element_type=F32)


def exchange_kernel(size, modes, *refs):
    count = len(modes)
    ins, outs = refs[:count], refs[count : 2 * count]
    send, recv = refs[2 * count :]
    me = lax.axis_index("fsdp")
    barrier = pltpu.get_barrier_semaphore()
    for step in range(1, size):
        peer = lax.rem(me + step, size)
        pl.semaphore_signal(barrier, inc=1, device_id={"fsdp": peer}, device_id_type=MESH_ID)
    pl.semaphore_wait(barrier, size - 1)
    copies = []
    for k, mode in enumerate(modes):
        for step in range(1, size):
            peer = lax.rem(me + step, size)
            copies.append(
                pltpu.make_async_remote_copy(
                    src_ref=ins[k] if mode == "ag" else ins[k].at[peer],
                    dst_ref=outs[k].at[me],
                    send_sem=send.at[k, step - 1],
                    recv_sem=recv.at[k, step - 1],
                    device_id={"fsdp": peer},
                    device_id_type=MESH_ID,
                )
            )
    for copy in copies:
        copy.start()
    for copy in copies:
        copy.wait()


def exchange(ident, gathered=(), traded=()):
    size = lax.axis_size("fsdp")
    arrays = tuple(gathered) + tuple(traded)
    modes = ("ag",) * len(gathered) + ("a2a",) * len(traded)
    shapes = [(size,) + a.shape for a in gathered] + [a.shape for a in traded]
    sent = sum((size - 1) * a.size * a.dtype.itemsize for a in gathered)
    sent += sum((size - 1) * a.size * a.dtype.itemsize // size for a in traded)
    outs = pl.pallas_call(
        functools.partial(exchange_kernel, size, modes),
        out_shape=[jax.ShapeDtypeStruct(s, a.dtype) for s, a in zip(shapes, arrays)],
        in_specs=[pl.BlockSpec(memory_space=pl.ANY)] * len(arrays),
        out_specs=[pl.BlockSpec(memory_space=pl.ANY)] * len(arrays),
        scratch_shapes=[
            pltpu.SemaphoreType.DMA((len(arrays), size - 1)),
            pltpu.SemaphoreType.DMA((len(arrays), size - 1)),
        ],
        compiler_params=pltpu.CompilerParams(collective_id=ident, has_side_effects=True),
        cost_estimate=pl.CostEstimate(flops=0, bytes_accessed=sent * 50, transcendentals=0),
        name=f"exchange{ident}",
    )(*arrays)
    return outs


def with_own(slots, own):
    return lax.dynamic_update_index_in_dim(slots, own, lax.axis_index("fsdp"), 0)


def gather_tokens(ident, rows):
    (slots,) = exchange(ident, gathered=(rows,))
    slots = with_own(slots, rows)
    return slots.reshape((-1,) + rows.shape[1:])


def sum_tokens(ident, partial):
    (slots,) = exchange(ident, traded=(partial.astype(BF),))
    me = lax.axis_index("fsdp")
    mine = lax.dynamic_index_in_dim(partial, me, 0, keepdims=False)
    total = mine
    for i in range(slots.shape[0]):
        total = total + jnp.where(me == i, 0.0, slots[i].astype(F32))
    return total


def masks_of(first, block, lens_ref, starts_ref, group, count):
    rows = first + block * BLOCK
    query = rows + lax.broadcasted_iota(jnp.int32, (BLOCK, 1), 0)
    keys = rows - WINDOW + lax.broadcasted_iota(jnp.int32, (1, BLOCK + WINDOW), 1)
    length = lambda j: lens_ref[group, j]
    start = lambda j: starts_ref[group, j]
    seg_q = segment_of(query, count, length, start)
    seg_k = segment_of(keys, count, length, start)
    far = query - keys
    return (far >= 0) & (far <= WINDOW) & (seg_q == seg_k)


def soft_of(query, keys, mask):
    scores = dot_trans(query, keys) * SCALE
    scores = jnp.where(mask, scores, NEG)
    peak = jnp.max(scores, axis=1, keepdims=True)
    exponent = jnp.exp(scores - peak)
    return exponent / jnp.sum(exponent, axis=1, keepdims=True)


def lane_head(width):
    return lax.broadcasted_iota(jnp.int32, (1, width), 1) // HEAD_DIM


def attend_kernel(count, lens_ref, starts_ref, first_ref, q_ref, kp_ref, k_ref, vp_ref, v_ref, o_ref):
    group = pl.program_id(0)
    first = first_ref[0]
    rows, width = q_ref.shape
    keys = jnp.concatenate([kp_ref[...], k_ref[...]], 0)
    values = jnp.concatenate([vp_ref[...], v_ref[...]], 0)
    head_of = lane_head(width)
    for block in range(rows // BLOCK):
        mask = masks_of(first, block, lens_ref, starts_ref, group, count)
        low = block * BLOCK
        query = q_ref[low : low + BLOCK, :]
        key = keys[low : low + BLOCK + WINDOW]
        value = values[low : low + BLOCK + WINDOW]
        out = jnp.zeros((BLOCK, width), F32)
        for head in range(width // HEAD_DIM):
            mine = head_of == head
            soft = soft_of(jnp.where(mine, query, jnp.zeros_like(query)), key, mask)
            out = jnp.where(mine, dot(soft.astype(BF), value), out)
        o_ref[low : low + BLOCK, :] = out.astype(BF)


def attend_back_kernel(
    count, lens_ref, starts_ref, first_ref, q_ref, kp_ref, k_ref, vp_ref, v_ref, g_ref,
    dq_ref, dkp_ref, dk_ref, dvp_ref, dv_ref, dk_acc, dv_acc,
):
    group = pl.program_id(0)
    first = first_ref[0]
    rows, width = q_ref.shape
    keys = jnp.concatenate([kp_ref[...], k_ref[...]], 0)
    values = jnp.concatenate([vp_ref[...], v_ref[...]], 0)
    head_of = lane_head(width)
    dk_acc[...] = jnp.zeros_like(dk_acc)
    dv_acc[...] = jnp.zeros_like(dv_acc)
    for block in range(rows // BLOCK):
        mask = masks_of(first, block, lens_ref, starts_ref, group, count)
        low = block * BLOCK
        span = slice(low, low + BLOCK + WINDOW)
        query = q_ref[low : low + BLOCK, :]
        grad = g_ref[low : low + BLOCK, :]
        key, value = keys[span], values[span]
        dq = jnp.zeros((BLOCK, width), F32)
        dk = jnp.zeros((BLOCK + WINDOW, width), F32)
        dv = jnp.zeros((BLOCK + WINDOW, width), F32)
        for head in range(width // HEAD_DIM):
            mine = head_of == head
            own_q = jnp.where(mine, query, jnp.zeros_like(query))
            own_g = jnp.where(mine, grad, jnp.zeros_like(grad))
            soft = soft_of(own_q, key, mask)
            grad_soft = dot_trans(own_g, value)
            total = jnp.sum(grad_soft * soft, axis=1, keepdims=True)
            grad_scores = (soft * (grad_soft - total)).astype(BF)
            dq = jnp.where(mine, dot(grad_scores, key), dq)
            dk = dk + dot_rows(grad_scores, own_q)
            dv = dv + dot_rows(soft.astype(BF), own_g)
        dq_ref[low : low + BLOCK, :] = (dq * SCALE).astype(BF)
        dk_acc[span, :] += dk * SCALE
        dv_acc[span, :] += dv
    dkp_ref[...] = dk_acc[:WINDOW, :].astype(BF)
    dk_ref[...] = dk_acc[WINDOW:, :]
    dvp_ref[...] = dv_acc[:WINDOW, :].astype(BF)
    dv_ref[...] = dv_acc[WINDOW:, :]


def attend(lens, starts, first, rows, q, kp, k, vp, v, grad=None):
    groups = q.shape[0] // rows
    width = q.shape[1]
    own = pl.BlockSpec((rows, width), lambda g: (g, 0))
    edge = pl.BlockSpec((WINDOW, width), lambda g: (g, 0))
    table = pl.BlockSpec(memory_space=pltpu.SMEM)
    args = [lens, starts, first, q, kp, k, vp, v]
    specs = [table] * 3 + [own, edge, own, edge, own]
    count = lens.shape[1]
    cost = groups * rows * 192 * 4 * width
    if grad is None:
        return pl.pallas_call(
            functools.partial(attend_kernel, count),
            grid=(groups,),
            out_shape=jax.ShapeDtypeStruct(q.shape, BF),
            in_specs=specs,
            out_specs=own,
            cost_estimate=pl.CostEstimate(
                flops=cost * 4, bytes_accessed=q.size * 8, transcendentals=cost // 448
            ),
            name="attend",
        )(*args)
    total = (groups * rows, width)
    halo = (groups * WINDOW, width)
    return pl.pallas_call(
        functools.partial(attend_back_kernel, count),
        grid=(groups,),
        out_shape=[
            jax.ShapeDtypeStruct(total, BF),
            jax.ShapeDtypeStruct(halo, BF),
            jax.ShapeDtypeStruct(total, F32),
            jax.ShapeDtypeStruct(halo, BF),
            jax.ShapeDtypeStruct(total, F32),
        ],
        in_specs=specs + [own],
        out_specs=[own, edge, own, edge, own],
        scratch_shapes=[
            pltpu.VMEM((rows + WINDOW, width), F32),
            pltpu.VMEM((rows + WINDOW, width), F32),
        ],
        cost_estimate=pl.CostEstimate(
            flops=cost * 8, bytes_accessed=q.size * 20, transcendentals=cost // 448
        ),
        name="attend_back",
    )(*args, grad)


def columns_piece(weights, part, parts):
    size = lax.axis_size("fsdp")
    rows = weights[0].shape[0] // parts
    pieces = []
    for weight in weights:
        own = lax.dynamic_slice_in_dim(weight, part * rows, rows, 0)
        pieces.append(own.reshape(rows, size, -1).transpose(1, 0, 2))
    return jnp.stack(pieces, 1)


def full_columns(traded):
    size, count, rows, cols = traded.shape
    every = lax.all_gather(traded, "seq", axis=0)
    return every.transpose(2, 1, 0, 3, 4).reshape(count, -1, cols)


def reduce_columns(ident, grads):
    size = lax.axis_size("fsdp")
    parts = lax.axis_size("seq")
    cols = grads[0].shape[1]
    packed = jnp.stack([g.astype(BF).reshape(size, parts, -1, cols) for g in grads], 0)
    packed = packed.transpose(2, 1, 0, 3, 4)
    piece = lax.psum_scatter(packed, "seq", scatter_dimension=0)
    (slots,) = exchange(ident, traded=(piece,))
    own = lax.dynamic_index_in_dim(piece, lax.axis_index("fsdp"), 0, keepdims=False)
    slots = with_own(slots, own)
    every = lax.all_gather(slots, "seq", axis=0)
    outs = []
    for n in range(len(grads)):
        outs.append(every[:, :, n].transpose(0, 2, 1, 3).reshape(-1, size * cols).astype(F32))
    return outs


def shards(
    tokens,
    seq_lengths,
    seq_offsets,
    norm1_gain,
    conv_weight,
    query_weight,
    key_weight,
    value_weight,
    out_weight,
    norm2_gain,
    gate_weight,
    up_weight,
    down_weight,
    cotangent,
):
    size = lax.axis_size("fsdp")
    parts = lax.axis_size("seq")
    part = lax.axis_index("seq")
    me = lax.axis_index("fsdp")
    own_tokens = tokens[0]
    rows, width = own_tokens.shape
    slice_width = norm1_gain.shape[0]
    first_slot = part * rows
    count = seq_lengths.shape[1]

    slot_ext = first_slot - 2 + jnp.arange(rows + 2, dtype=jnp.int32)
    segment_ext = segment_of(
        slot_ext, count, lambda j: seq_lengths[0, j], lambda j: seq_offsets[0, j]
    )
    segment_own = segment_ext[2:]
    same_one = (segment_own == segment_ext[1:-1]).astype(F32)[:, None]
    same_two = (segment_own == segment_ext[:-2]).astype(F32)[:, None]
    live_mask = (segment_own >= 0).astype(F32)[:, None]

    gains = jnp.concatenate(
        [
            norm1_gain[None],
            norm2_gain[None],
            conv_weight.T,
            jnp.zeros((3, slice_width), BF),
        ],
        0,
    )
    table = jnp.zeros((8, 128), jnp.int32)
    table = table.at[0, :count].set(seq_lengths[0]).at[1, :count].set(seq_offsets[0])
    qkv_piece = columns_piece((query_weight, key_weight, value_weight), part, parts)
    gu_piece = columns_piece((gate_weight, up_weight), part, parts)
    gains_all, table_all, qkv_slots, gu_slots = exchange(
        0, gathered=(gains, table), traded=(qkv_piece, gu_piece)
    )
    gains_all = with_own(gains_all, gains).transpose(1, 0, 2).reshape(8, width)
    table_all = with_own(table_all, table)
    lens_all, starts_all = table_all[:, 0, :count], table_all[:, 1, :count]
    qkv_slots = with_own(qkv_slots, lax.dynamic_index_in_dim(qkv_piece, me, 0, keepdims=False))
    gu_slots = with_own(gu_slots, lax.dynamic_index_in_dim(gu_piece, me, 0, keepdims=False))
    query_map, key_map, value_map = full_columns(qkv_slots)
    gate_map, up_map = full_columns(gu_slots)
    norm_one = gains_all[0].astype(F32)
    norm_two = gains_all[1].astype(F32)
    taps = gains_all[2:5].astype(F32)

    edge_tokens = shifted(own_tokens[rows - 2 :], "seq", 1)
    extended = jnp.concatenate([edge_tokens, own_tokens], 0).astype(F32)
    scale_one = lax.rsqrt(jnp.mean(extended * extended, axis=1, keepdims=True) + EPS)
    normed = extended * scale_one * norm_one
    conv_mix = (
        normed[2:] * taps[0]
        + same_one * normed[1:-1] * taps[1]
        + same_two * normed[:-2] * taps[2]
    )
    gated = (conv_mix * normed[2:]).astype(BF)
    gated_all = gather_tokens(1, gated)

    grad_out = cotangent[0].astype(F32) * live_mask
    grad_down_all = lax.all_gather(grad_out.astype(BF), "fsdp", axis=0, tiled=True)

    queries = dot(gated_all, query_map).astype(BF)
    keys = dot(gated_all, key_map).astype(BF)
    values = dot(gated_all, value_map).astype(BF)
    local = queries.shape[1]

    def last_rows(a):
        return a.reshape(size, rows, local)[:, rows - WINDOW :].reshape(size * WINDOW, local)

    keys_prev, values_prev = shifted((last_rows(keys), last_rows(values)), "seq", 1)
    first = jnp.reshape(first_slot, (1,)).astype(jnp.int32)
    attention = (lens_all, starts_all, first, rows, queries, keys_prev, keys, values_prev, values)
    heads_out = attend(*attention)
    branch = sum_tokens(2, dot(heads_out, out_weight).reshape(size, rows, width))
    middle = own_tokens.astype(F32) + branch
    scale_two = lax.rsqrt(jnp.mean(middle * middle, axis=1, keepdims=True) + EPS)
    unit_two = middle * scale_two
    normed_two = (unit_two * norm_two).astype(BF)
    normed_all = gather_tokens(3, normed_two)

    gate_act = dot(normed_all, gate_map)
    up_act = dot(normed_all, up_map)
    sigma = jax.nn.sigmoid(gate_act)
    hidden = (gate_act * sigma * up_act).astype(BF)
    grad_hidden = dot_trans(grad_down_all, down_weight)
    grad_gate = (grad_hidden * up_act * sigma * (1.0 + gate_act * (1.0 - sigma))).astype(BF)
    grad_up = (grad_hidden * gate_act * sigma).astype(BF)
    grad_normed_two = sum_tokens(
        4,
        (dot_trans(grad_gate, gate_map) + dot_trans(grad_up, up_map)).reshape(size, rows, width),
    )
    down_total = lax.psum(dot_rows(hidden, grad_down_all).astype(BF), "seq").astype(F32)
    gate_total, up_total = reduce_columns(
        5, (dot_rows(normed_all, grad_gate), dot_rows(normed_all, grad_up))
    )

    grad_unit_two = grad_normed_two * norm_two
    norm2_term = jnp.sum(grad_normed_two * unit_two, axis=0)
    grad_middle = grad_out + scale_two * (
        grad_unit_two - unit_two * jnp.mean(grad_unit_two * unit_two, axis=1, keepdims=True)
    )
    grad_branch_all = gather_tokens(6, grad_middle.astype(BF))
    grad_heads = dot_trans(grad_branch_all, out_weight).astype(BF)
    out_total = lax.psum(dot_rows(heads_out, grad_branch_all).astype(BF), "seq").astype(F32)
    grad_queries, keys_halo, grad_keys, values_halo, grad_values = attend(*attention, grad_heads)
    keys_back, values_back = shifted((keys_halo, values_halo), "seq", -1)

    def with_back(own, back):
        own = own.reshape(size, rows, local)
        back = back.reshape(size, WINDOW, local).astype(F32)
        full = jnp.concatenate([own[:, : rows - WINDOW], own[:, rows - WINDOW :] + back], 1)
        return full.reshape(size * rows, local).astype(BF)

    grad_keys = with_back(grad_keys, keys_back)
    grad_values = with_back(grad_values, values_back)
    grad_gated = sum_tokens(
        7,
        (
            dot_trans(grad_queries, query_map)
            + dot_trans(grad_keys, key_map)
            + dot_trans(grad_values, value_map)
        ).reshape(size, rows, width),
    )
    query_total, key_total, value_total = reduce_columns(
        8,
        (
            dot_rows(gated_all, grad_queries),
            dot_rows(gated_all, grad_keys),
            dot_rows(gated_all, grad_values),
        ),
    )

    normed_own = normed[2:]
    grad_mix = grad_gated * normed_own
    part_zero = jnp.pad(grad_gated * conv_mix + grad_mix * taps[0], ((2, 0), (0, 0)))
    part_one = jnp.pad(grad_mix * same_one * taps[1], ((1, 1), (0, 0)))
    part_two = jnp.pad(grad_mix * same_two * taps[2], ((0, 2), (0, 0)))
    grad_normed = part_zero + part_one + part_two
    unit_one = extended * scale_one
    grad_unit_one = grad_normed * norm_one
    grad_extended = scale_one * (
        grad_unit_one - unit_one * jnp.mean(grad_unit_one * unit_one, axis=1, keepdims=True)
    )
    edge_back = shifted(grad_extended[:2], "seq", -1)
    tokens_grad = grad_middle + grad_extended[2:] + jnp.pad(edge_back, ((rows - 2, 0), (0, 0)))

    terms = jnp.stack(
        [
            jnp.sum(grad_normed * unit_one, axis=0),
            norm2_term,
            jnp.sum(grad_mix * normed_own, axis=0),
            jnp.sum(grad_mix * same_one * normed[1:-1], axis=0),
            jnp.sum(grad_mix * same_two * normed[:-2], axis=0),
        ]
    )
    terms = lax.psum(terms, ("seq", "fsdp"))
    terms = lax.dynamic_slice_in_dim(terms, me * slice_width, slice_width, 1)

    feed = sum_tokens(9, dot(hidden, down_weight).reshape(size, rows, width))
    layer_out = (live_mask * (middle + feed)).astype(BF)[None]
    return (
        layer_out,
        tokens_grad[None],
        terms[0],
        terms[2:5].T,
        query_total,
        key_total,
        value_total,
        out_total,
        terms[1],
        gate_total,
        up_total,
        down_total,
    )


def solution(mesh):
    placed = (
        P("fsdp", "seq", None),
        P("fsdp", None),
        P("fsdp", None),
        P("fsdp"),
        P("fsdp", None),
        P("fsdp", None),
        P("fsdp", None),
        P("fsdp", None),
        P("fsdp", None),
        P("fsdp"),
        P("fsdp", None),
        P("fsdp", None),
        P("fsdp", None),
        P("fsdp", "seq", None),
    )
    return jax.shard_map(
        shards,
        mesh=mesh,
        in_specs=placed,
        out_specs=(
            P("fsdp", "seq", None),
            P("fsdp", "seq", None),
            P("fsdp"),
            P("fsdp", None),
            P("fsdp", None),
            P("fsdp", None),
            P("fsdp", None),
            P("fsdp", None),
            P("fsdp"),
            P("fsdp", None),
            P("fsdp", None),
            P("fsdp", None),
        ),
        check_vma=False,
    )
```

```python
import functools

import jax
import jax.numpy as jnp
from jax import lax
from jax.experimental import pallas as pl
from jax.experimental.pallas import tpu as pltpu
from jax.sharding import PartitionSpec as P

HEADS = 16
WINDOW = 64
HEAD_DIM = 112
BLOCK = 128

EPS = 1e-05
NEG = -1e30
SCALE = HEAD_DIM ** (-0.5)
MESH_ID = pl.DeviceIdType.MESH
BF = jnp.bfloat16
F32 = jnp.float32


def shifted(array, axis, by):
    length = lax.axis_size(axis)
    pairs = [(i, i + by) for i in range(length) if 0 <= i + by < length]
    return lax.ppermute(array, axis, pairs)


def segment_of(slot, count, lengths, starts):
    found = jnp.full(slot.shape, -1, jnp.int32)
    for j in range(count):
        inside = (slot >= starts(j)) & (slot < starts(j) + lengths(j))
        found = jnp.where(inside, j, found)
    return jnp.where(slot < 0, -2, found)


def dot_rows(left, right):
    return lax.dot_general(left, right, (((0,), (0,)), ((), ())), preferred_element_type=F32)


def dot_trans(left, right):
    return lax.dot_general(left, right, (((1,), (1,)), ((), ())), preferred_element_type=F32)


def dot(left, right):
    return jnp.dot(left, right, preferred_element_type=F32)


def exchange_kernel(size, modes, *refs):
    count = len(modes)
    ins, outs = refs[:count], refs[count : 2 * count]
    send, recv = refs[2 * count :]
    me = lax.axis_index("fsdp")
    barrier = pltpu.get_barrier_semaphore()
    for step in range(1, size):
        peer = lax.rem(me + step, size)
        pl.semaphore_signal(barrier, inc=1, device_id={"fsdp": peer}, device_id_type=MESH_ID)
    pl.semaphore_wait(barrier, size - 1)
    copies = []
    for k, mode in enumerate(modes):
        for step in range(1, size):
            peer = lax.rem(me + step, size)
            copies.append(
                pltpu.make_async_remote_copy(
                    src_ref=ins[k] if mode == "ag" else ins[k].at[peer],
                    dst_ref=outs[k].at[me],
                    send_sem=send.at[k, step - 1],
                    recv_sem=recv.at[k, step - 1],
                    device_id={"fsdp": peer},
                    device_id_type=MESH_ID,
                )
            )
    for copy in copies:
        copy.start()
    for copy in copies:
        copy.wait()


def exchange(ident, gathered=(), traded=()):
    size = lax.axis_size("fsdp")
    arrays = tuple(gathered) + tuple(traded)
    modes = ("ag",) * len(gathered) + ("a2a",) * len(traded)
    shapes = [(size,) + a.shape for a in gathered] + [a.shape for a in traded]
    sent = sum((size - 1) * a.size * a.dtype.itemsize for a in gathered)
    sent += sum((size - 1) * a.size * a.dtype.itemsize // size for a in traded)
    outs = pl.pallas_call(
        functools.partial(exchange_kernel, size, modes),
        out_shape=[jax.ShapeDtypeStruct(s, a.dtype) for s, a in zip(shapes, arrays)],
        in_specs=[pl.BlockSpec(memory_space=pl.ANY)] * len(arrays),
        out_specs=[pl.BlockSpec(memory_space=pl.ANY)] * len(arrays),
        scratch_shapes=[
            pltpu.SemaphoreType.DMA((len(arrays), size - 1)),
            pltpu.SemaphoreType.DMA((len(arrays), size - 1)),
        ],
        compiler_params=pltpu.CompilerParams(collective_id=ident, has_side_effects=True),
        cost_estimate=pl.CostEstimate(flops=0, bytes_accessed=sent * 50, transcendentals=0),
        name=f"exchange{ident}",
    )(*arrays)
    return outs


def with_own(slots, own):
    return lax.dynamic_update_index_in_dim(slots, own, lax.axis_index("fsdp"), 0)


def gather_tokens(ident, rows):
    (slots,) = exchange(ident, gathered=(rows,))
    slots = with_own(slots, rows)
    return slots.reshape((-1,) + rows.shape[1:])


def sum_tokens(ident, partial):
    (slots,) = exchange(ident, traded=(partial.astype(BF),))
    me = lax.axis_index("fsdp")
    mine = lax.dynamic_index_in_dim(partial, me, 0, keepdims=False)
    total = mine
    for i in range(slots.shape[0]):
        total = total + jnp.where(me == i, 0.0, slots[i].astype(F32))
    return total


def masks_of(first, block, lens_ref, starts_ref, group, count):
    rows = first + block * BLOCK
    query = rows + lax.broadcasted_iota(jnp.int32, (BLOCK, 1), 0)
    keys = rows - WINDOW + lax.broadcasted_iota(jnp.int32, (1, BLOCK + WINDOW), 1)
    length = lambda j: lens_ref[group, j]
    start = lambda j: starts_ref[group, j]
    seg_q = segment_of(query, count, length, start)
    seg_k = segment_of(keys, count, length, start)
    far = query - keys
    return (far >= 0) & (far <= WINDOW) & (seg_q == seg_k)


def soft_of(query, keys, mask):
    scores = dot_trans(query, keys) * SCALE
    scores = jnp.where(mask, scores, NEG)
    peak = jnp.max(scores, axis=1, keepdims=True)
    exponent = jnp.exp(scores - peak)
    return exponent / jnp.sum(exponent, axis=1, keepdims=True)


def lane_head(width):
    return lax.broadcasted_iota(jnp.int32, (1, width), 1) // HEAD_DIM


def rows_of_heads(edge_ref, qkv_ref):
    width = qkv_ref.shape[1] // 3
    own = qkv_ref[...]
    edge = edge_ref[...]
    keys = jnp.concatenate([edge[:, :width], own[:, width : 2 * width]], 0)
    values = jnp.concatenate([edge[:, width:], own[:, 2 * width :]], 0)
    return own[:, :width], keys, values


def attend_kernel(count, lens_ref, starts_ref, first_ref, edge_ref, qkv_ref, o_ref):
    group = pl.program_id(0)
    first = first_ref[0]
    queries, keys, values = rows_of_heads(edge_ref, qkv_ref)
    rows, width = queries.shape
    head_of = lane_head(width)
    for block in range(rows // BLOCK):
        mask = masks_of(first, block, lens_ref, starts_ref, group, count)
        low = block * BLOCK
        query = queries[low : low + BLOCK]
        key = keys[low : low + BLOCK + WINDOW]
        value = values[low : low + BLOCK + WINDOW]
        out = jnp.zeros((BLOCK, width), F32)
        for head in range(width // HEAD_DIM):
            mine = head_of == head
            soft = soft_of(jnp.where(mine, query, jnp.zeros_like(query)), key, mask)
            out = jnp.where(mine, dot(soft.astype(BF), value), out)
        o_ref[low : low + BLOCK, :] = out.astype(BF)


def attend_back_kernel(
    count, lens_ref, starts_ref, first_ref, edge_ref, qkv_ref, g_ref,
    dqkv_ref, dedge_ref, dk_acc, dv_acc, dq_acc,
):
    group = pl.program_id(0)
    first = first_ref[0]
    queries, keys, values = rows_of_heads(edge_ref, qkv_ref)
    rows, width = queries.shape
    head_of = lane_head(width)
    dk_acc[...] = jnp.zeros_like(dk_acc)
    dv_acc[...] = jnp.zeros_like(dv_acc)
    for block in range(rows // BLOCK):
        mask = masks_of(first, block, lens_ref, starts_ref, group, count)
        low = block * BLOCK
        span = slice(low, low + BLOCK + WINDOW)
        query = queries[low : low + BLOCK]
        grad = g_ref[low : low + BLOCK, :]
        key, value = keys[span], values[span]
        dq = jnp.zeros((BLOCK, width), F32)
        dk = jnp.zeros((BLOCK + WINDOW, width), F32)
        dv = jnp.zeros((BLOCK + WINDOW, width), F32)
        for head in range(width // HEAD_DIM):
            mine = head_of == head
            own_q = jnp.where(mine, query, jnp.zeros_like(query))
            own_g = jnp.where(mine, grad, jnp.zeros_like(grad))
            soft = soft_of(own_q, key, mask)
            grad_soft = dot_trans(own_g, value)
            total = jnp.sum(grad_soft * soft, axis=1, keepdims=True)
            grad_scores = (soft * (grad_soft - total)).astype(BF)
            dq = jnp.where(mine, dot(grad_scores, key), dq)
            dk = dk + dot_rows(grad_scores, own_q)
            dv = dv + dot_rows(soft.astype(BF), own_g)
        dq_acc[low : low + BLOCK, :] = dq * SCALE
        dk_acc[span, :] += dk * SCALE
        dv_acc[span, :] += dv
    dedge_ref[...] = jnp.concatenate([dk_acc[:WINDOW, :], dv_acc[:WINDOW, :]], 1).astype(BF)
    dqkv_ref[...] = jnp.concatenate([dq_acc[...], dk_acc[WINDOW:, :], dv_acc[WINDOW:, :]], 1)


def attend(lens, starts, first, rows, edge, qkv, grad=None):
    groups = qkv.shape[0] // rows
    width = qkv.shape[1] // 3
    block = lambda n, w: pl.BlockSpec((n, w), lambda g: (g, 0))
    table = pl.BlockSpec(memory_space=pltpu.SMEM)
    args = [lens, starts, first, edge, qkv]
    specs = [table] * 3 + [block(WINDOW, 2 * width), block(rows, 3 * width)]
    count = lens.shape[1]
    cost = groups * rows * 192 * 4 * width
    if grad is None:
        return pl.pallas_call(
            functools.partial(attend_kernel, count),
            grid=(groups,),
            out_shape=jax.ShapeDtypeStruct((groups * rows, width), BF),
            in_specs=specs,
            out_specs=block(rows, width),
            cost_estimate=pl.CostEstimate(
                flops=cost * 4, bytes_accessed=qkv.size * 4, transcendentals=cost // 448
            ),
            name="attend",
        )(*args)
    return pl.pallas_call(
        functools.partial(attend_back_kernel, count),
        grid=(groups,),
        out_shape=[
            jax.ShapeDtypeStruct(qkv.shape, F32),
            jax.ShapeDtypeStruct(edge.shape, BF),
        ],
        in_specs=specs + [block(rows, width)],
        out_specs=[block(rows, 3 * width), block(WINDOW, 2 * width)],
        scratch_shapes=[
            pltpu.VMEM((rows + WINDOW, width), F32),
            pltpu.VMEM((rows + WINDOW, width), F32),
            pltpu.VMEM((rows, width), F32),
        ],
        cost_estimate=pl.CostEstimate(
            flops=cost * 8, bytes_accessed=qkv.size * 8, transcendentals=cost // 448
        ),
        name="attend_back",
    )(*args, grad)


def with_back_kernel(dqkv_ref, back_ref, out_ref):
    rows, width = dqkv_ref.shape
    kept = rows - WINDOW
    out_ref[:kept, :] = dqkv_ref[:kept, :].astype(BF)
    back = back_ref[...].astype(F32)
    back = jnp.concatenate([jnp.zeros((WINDOW, width // 3), F32), back], 1)
    out_ref[kept:, :] = (dqkv_ref[kept:, :] + back).astype(BF)


def with_back(rows, dqkv, back):
    groups = dqkv.shape[0] // rows
    block = lambda n, w: pl.BlockSpec((n, w), lambda g: (g, 0))
    width = dqkv.shape[1]
    return pl.pallas_call(
        with_back_kernel,
        grid=(groups,),
        out_shape=jax.ShapeDtypeStruct(dqkv.shape, BF),
        in_specs=[block(rows, width), block(WINDOW, back.shape[1])],
        out_specs=block(rows, width),
        cost_estimate=pl.CostEstimate(flops=0, bytes_accessed=dqkv.size * 6, transcendentals=0),
        name="with_back",
    )(dqkv, back)


def feed_kernel(x_ref, g_ref, gu_ref, down_ref, hidden_ref, grad_ref):
    inner = down_ref.shape[0]
    acts = dot(x_ref[...], gu_ref[...])
    gate, up = acts[:, :inner], acts[:, inner:]
    sigma = jax.nn.sigmoid(gate)
    silu = gate * sigma
    hidden_ref[...] = (silu * up).astype(BF)
    grad_hidden = dot_trans(g_ref[...], down_ref[...])
    grad_gate = grad_hidden * up * sigma * (1.0 + gate * (1.0 - sigma))
    grad_ref[...] = jnp.concatenate([grad_gate, grad_hidden * silu], 1).astype(BF)


def feed_forward(normed_all, grad_down_all, gu_map, down_weight):
    total, width = normed_all.shape
    inner = down_weight.shape[0]
    tile = 256
    block = lambda w: pl.BlockSpec((tile, w), lambda i: (i, 0))
    whole = lambda a: pl.BlockSpec(a.shape, lambda i: (0, 0), pipeline_mode=pl.Buffered(1))
    return pl.pallas_call(
        feed_kernel,
        grid=(total // tile,),
        out_shape=[
            jax.ShapeDtypeStruct((total, inner), BF),
            jax.ShapeDtypeStruct((total, 2 * inner), BF),
        ],
        in_specs=[block(width), block(width), whole(gu_map), whole(down_weight)],
        out_specs=[block(inner), block(2 * inner)],
        cost_estimate=pl.CostEstimate(
            flops=6 * total * width * inner,
            bytes_accessed=gu_map.size * 3 + total * width * 8,
            transcendentals=total * inner,
        ),
        name="feed_forward",
    )(normed_all, grad_down_all, gu_map, down_weight)


def pack_kernel(size, parts, x_ref, g_ref, *refs):
    out_ref = refs[-1]
    full = dot_rows(x_ref[...], g_ref[...])
    pair = out_ref.shape[1]
    rows = full.shape[0] // pair
    piece = rows // parts
    for k in range(pair):
        own = full[k * rows : (k + 1) * rows]
        if len(refs) == 3:
            heads_ref, gb_ref = refs[0], refs[1]
            side = dot_rows(heads_ref[...], gb_ref[...])
            wide = side.shape[1] // pair
            own = jnp.concatenate([own, side[:, k * wide : (k + 1) * wide]], 1)
        out_ref[:, k] = own.astype(BF).reshape(parts, piece, own.shape[1])


def pack_grads(parts, size, x, g, heads=None, gb=None):
    width, cols = x.shape[1], g.shape[1]
    rows = width // size
    piece = rows // parts
    if piece % 8 or (2 * rows) % 128:
        full = dot_rows(x, g).reshape(size, parts, piece, cols)
        if heads is not None:
            side = dot_rows(heads, gb).reshape(parts, piece, size, -1).transpose(2, 0, 1, 3)
            full = jnp.concatenate([full, side], 3)
        return full.transpose(1, 0, 2, 3).astype(BF)
    total = x.shape[0]
    pair = pl.BlockSpec((total, 2 * rows), lambda i: (0, i))
    whole = lambda a: pl.BlockSpec(a.shape, lambda i: (0, 0), pipeline_mode=pl.Buffered(1))
    args, specs = [x, g], [pair, whole(g)]
    out_cols = cols
    if heads is not None:
        args += [heads, gb]
        specs += [whole(heads), pair]
        out_cols += rows
    return pl.pallas_call(
        functools.partial(pack_kernel, size, parts),
        grid=(size // 2,),
        out_shape=jax.ShapeDtypeStruct((parts, size, piece, out_cols), BF),
        in_specs=specs,
        out_specs=pl.BlockSpec((parts, 2, piece, out_cols), lambda i: (0, i, 0, 0)),
        cost_estimate=pl.CostEstimate(
            flops=2 * total * width * out_cols,
            bytes_accessed=2 * (x.size + g.size + width * out_cols),
            transcendentals=0,
        ),
        name="pack_grads",
    )(*args)


def unpack_kernel(widths, every_ref, *outs):
    size = every_ref.shape[1]
    blocks = [every_ref[0, i].astype(F32) for i in range(size)]
    low = 0
    for width, out in zip(widths, outs):
        out[...] = jnp.concatenate([b[:, low : low + width] for b in blocks], 1)
        low += width


def unpack_grads(every, widths):
    parts, size, piece, cols = every.shape
    if piece % 8:
        outs, low = [], 0
        for width in widths:
            block = every[:, :, :, low : low + width].transpose(0, 2, 1, 3)
            outs.append(block.reshape(parts * piece, size * width).astype(F32))
            low += width
        return outs
    return pl.pallas_call(
        functools.partial(unpack_kernel, widths),
        grid=(parts,),
        out_shape=[jax.ShapeDtypeStruct((parts * piece, size * w), F32) for w in widths],
        in_specs=[pl.BlockSpec((1, size, piece, cols), lambda i: (i, 0, 0, 0))],
        out_specs=[pl.BlockSpec((piece, size * w), lambda i: (i, 0)) for w in widths],
        cost_estimate=pl.CostEstimate(flops=0, bytes_accessed=every.size * 6, transcendentals=0),
        name="unpack_grads",
    )(every)


def columns_piece(weights, part, parts):
    size = lax.axis_size("fsdp")
    rows = weights[0].shape[0] // parts
    pieces = []
    for weight in weights:
        own = lax.dynamic_slice_in_dim(weight, part * rows, rows, 0)
        pieces.append(own.reshape(rows, size, -1))
    return jnp.concatenate(pieces, 2).transpose(1, 0, 2)


def full_columns(traded):
    every = lax.all_gather(traded, "seq", axis=0)
    return every.transpose(1, 0, 2, 3).reshape(-1, traded.shape[2])


def shards(
    tokens,
    seq_lengths,
    seq_offsets,
    norm1_gain,
    conv_weight,
    query_weight,
    key_weight,
    value_weight,
    out_weight,
    norm2_gain,
    gate_weight,
    up_weight,
    down_weight,
    cotangent,
):
    size = lax.axis_size("fsdp")
    parts = lax.axis_size("seq")
    part = lax.axis_index("seq")
    me = lax.axis_index("fsdp")
    own_tokens = tokens[0]
    rows, width = own_tokens.shape
    slice_width = norm1_gain.shape[0]
    first_slot = part * rows
    count = seq_lengths.shape[1]

    slot_ext = first_slot - 2 + jnp.arange(rows + 2, dtype=jnp.int32)
    segment_ext = segment_of(
        slot_ext, count, lambda j: seq_lengths[0, j], lambda j: seq_offsets[0, j]
    )
    segment_own = segment_ext[2:]
    same_one = (segment_own == segment_ext[1:-1]).astype(F32)[:, None]
    same_two = (segment_own == segment_ext[:-2]).astype(F32)[:, None]
    live_mask = (segment_own >= 0).astype(F32)[:, None]

    gains = jnp.concatenate(
        [
            norm1_gain[None],
            norm2_gain[None],
            conv_weight.T,
            jnp.zeros((3, slice_width), BF),
        ],
        0,
    )
    table = jnp.zeros((8, 128), jnp.int32)
    table = table.at[0, :count].set(seq_lengths[0]).at[1, :count].set(seq_offsets[0])
    qkv_piece = columns_piece((query_weight, key_weight, value_weight), part, parts)
    gu_piece = columns_piece((gate_weight, up_weight), part, parts)
    gains_all, table_all, qkv_slots, gu_slots = exchange(
        0, gathered=(gains, table), traded=(qkv_piece, gu_piece)
    )
    gains_all = with_own(gains_all, gains).transpose(1, 0, 2).reshape(8, width)
    table_all = with_own(table_all, table)
    lens_all, starts_all = table_all[:, 0, :count], table_all[:, 1, :count]
    qkv_slots = with_own(qkv_slots, lax.dynamic_index_in_dim(qkv_piece, me, 0, keepdims=False))
    gu_slots = with_own(gu_slots, lax.dynamic_index_in_dim(gu_piece, me, 0, keepdims=False))
    qkv_map = full_columns(qkv_slots)
    gu_map = full_columns(gu_slots)
    norm_one = gains_all[0].astype(F32)
    norm_two = gains_all[1].astype(F32)
    taps = gains_all[2:5].astype(F32)

    edge_tokens = shifted(own_tokens[rows - 2 :], "seq", 1)
    extended = jnp.concatenate([edge_tokens, own_tokens], 0).astype(F32)
    scale_one = lax.rsqrt(jnp.mean(extended * extended, axis=1, keepdims=True) + EPS)
    normed = extended * scale_one * norm_one
    conv_mix = (
        normed[2:] * taps[0]
        + same_one * normed[1:-1] * taps[1]
        + same_two * normed[:-2] * taps[2]
    )
    gated = (conv_mix * normed[2:]).astype(BF)
    gated_all = gather_tokens(1, gated)

    grad_out = cotangent[0].astype(F32) * live_mask
    grad_down_all = lax.all_gather(grad_out.astype(BF), "fsdp", axis=0, tiled=True)

    qkv = dot(gated_all, qkv_map).astype(BF)
    local = qkv.shape[1] // 3
    last = qkv.reshape(size, rows, 3 * local)[:, rows - WINDOW :, local:]
    edge = shifted(last.reshape(size * WINDOW, 2 * local), "seq", 1)
    first = jnp.reshape(first_slot, (1,)).astype(jnp.int32)
    attention = (lens_all, starts_all, first, rows, edge, qkv)
    heads_out = attend(*attention)
    branch = sum_tokens(2, dot(heads_out, out_weight).reshape(size, rows, width))
    middle = own_tokens.astype(F32) + branch
    scale_two = lax.rsqrt(jnp.mean(middle * middle, axis=1, keepdims=True) + EPS)
    unit_two = middle * scale_two
    normed_two = (unit_two * norm_two).astype(BF)
    normed_all = gather_tokens(3, normed_two)

    hidden, grad_gu = feed_forward(normed_all, grad_down_all, gu_map, down_weight)
    gu_packed = pack_grads(parts, size, normed_all, grad_gu)
    gu_packed, grad_gu = lax.optimization_barrier((gu_packed, grad_gu))
    gu_piece = lax.psum_scatter(gu_packed, "seq", scatter_dimension=0)
    partial_two = dot_trans(grad_gu, gu_map).reshape(size, rows, width)
    down_sum = dot_rows(hidden, grad_down_all).astype(BF)
    partial_two, down_sum = lax.optimization_barrier((partial_two, down_sum))
    down_total = lax.psum(down_sum, "seq").astype(F32)
    grad_normed_two = sum_tokens(4, partial_two)

    grad_unit_two = grad_normed_two * norm_two
    norm2_term = jnp.sum(grad_normed_two * unit_two, axis=0)
    grad_middle = grad_out + scale_two * (
        grad_unit_two - unit_two * jnp.mean(grad_unit_two * unit_two, axis=1, keepdims=True)
    )
    grad_branch_all = gather_tokens(6, grad_middle.astype(BF))
    grad_branch_all, gu_piece = lax.optimization_barrier((grad_branch_all, gu_piece))
    (gu_slots,) = exchange(5, traded=(gu_piece,))
    gu_slots = with_own(gu_slots, lax.dynamic_index_in_dim(gu_piece, me, 0, keepdims=False))
    gu_every = lax.all_gather(gu_slots, "seq", axis=0)
    grad_branch_all, gu_slots = lax.optimization_barrier((grad_branch_all, gu_slots))

    grad_heads = dot_trans(grad_branch_all, out_weight).astype(BF)
    dqkv, dedge = attend(*attention, grad_heads)
    back = shifted(dedge, "seq", -1)
    dqkv = with_back(rows, dqkv, back)
    grad_gated = sum_tokens(7, dot_trans(dqkv, qkv_map).reshape(size, rows, width))
    qkvo_packed = pack_grads(parts, size, gated_all, dqkv, heads_out, grad_branch_all)
    hidden, grad_gated = lax.optimization_barrier((hidden, grad_gated))
    feed = sum_tokens(9, dot(hidden, down_weight).reshape(size, rows, width))
    qkvo_packed, gu_every, down_total, feed = lax.optimization_barrier(
        (qkvo_packed, gu_every, down_total, feed)
    )
    qkvo_piece = lax.psum_scatter(qkvo_packed, "seq", scatter_dimension=0)
    (qkvo_slots,) = exchange(8, traded=(qkvo_piece,))
    qkvo_slots = with_own(
        qkvo_slots, lax.dynamic_index_in_dim(qkvo_piece, me, 0, keepdims=False)
    )
    qkvo_slots = jnp.concatenate([qkvo_slots[..., : 3 * local], qkvo_piece[..., 3 * local :]], -1)
    qkvo_every = lax.all_gather(qkvo_slots, "seq", axis=0)
    gate_total, up_total = unpack_grads(gu_every, (gu_map.shape[1] // 2,) * 2)
    query_total, key_total, value_total, out_total = unpack_grads(qkvo_every, (local,) * 4)

    normed_own = normed[2:]
    grad_mix = grad_gated * normed_own
    part_zero = jnp.pad(grad_gated * conv_mix + grad_mix * taps[0], ((2, 0), (0, 0)))
    part_one = jnp.pad(grad_mix * same_one * taps[1], ((1, 1), (0, 0)))
    part_two = jnp.pad(grad_mix * same_two * taps[2], ((0, 2), (0, 0)))
    grad_normed = part_zero + part_one + part_two
    unit_one = extended * scale_one
    grad_unit_one = grad_normed * norm_one
    grad_extended = scale_one * (
        grad_unit_one - unit_one * jnp.mean(grad_unit_one * unit_one, axis=1, keepdims=True)
    )
    edge_back = shifted(grad_extended[:2], "seq", -1)
    tokens_grad = grad_middle + grad_extended[2:] + jnp.pad(edge_back, ((rows - 2, 0), (0, 0)))

    terms = jnp.stack(
        [
            jnp.sum(grad_normed * unit_one, axis=0),
            norm2_term,
            jnp.sum(grad_mix * normed_own, axis=0),
            jnp.sum(grad_mix * same_one * normed[1:-1], axis=0),
            jnp.sum(grad_mix * same_two * normed[:-2], axis=0),
        ]
    )
    terms = lax.psum(terms, ("seq", "fsdp"))
    terms = lax.dynamic_slice_in_dim(terms, me * slice_width, slice_width, 1)

    layer_out = (live_mask * (middle + feed)).astype(BF)[None]
    return (
        layer_out,
        tokens_grad[None],
        terms[0],
        terms[2:5].T,
        query_total,
        key_total,
        value_total,
        out_total,
        terms[1],
        gate_total,
        up_total,
        down_total,
    )


def solution(mesh):
    placed = (
        P("fsdp", "seq", None),
        P("fsdp", None),
        P("fsdp", None),
        P("fsdp"),
        P("fsdp", None),
        P("fsdp", None),
        P("fsdp", None),
        P("fsdp", None),
        P("fsdp", None),
        P("fsdp"),
        P("fsdp", None),
        P("fsdp", None),
        P("fsdp", None),
        P("fsdp", "seq", None),
    )
    return jax.shard_map(
        shards,
        mesh=mesh,
        in_specs=placed,
        out_specs=(
            P("fsdp", "seq", None),
            P("fsdp", "seq", None),
            P("fsdp"),
            P("fsdp", None),
            P("fsdp", None),
            P("fsdp", None),
            P("fsdp", None),
            P("fsdp", None),
            P("fsdp"),
            P("fsdp", None),
            P("fsdp", None),
            P("fsdp", None),
        ),
        check_vma=False,
    )
```

```python
import functools

import jax
import jax.numpy as jnp
from jax import lax
from jax.experimental import pallas as pl
from jax.experimental.pallas import tpu as pltpu
from jax.sharding import PartitionSpec as P

HEADS = 16
WINDOW = 64
HEAD_DIM = 112
BLOCK = 128

EPS = 1e-05
NEG = -1e30
SCALE = HEAD_DIM ** (-0.5)
MESH_ID = pl.DeviceIdType.MESH
BF = jnp.bfloat16
F32 = jnp.float32


def shifted(array, axis, by):
    length = lax.axis_size(axis)
    pairs = [(i, i + by) for i in range(length) if 0 <= i + by < length]
    return lax.ppermute(array, axis, pairs)


def segment_of(slot, count, lengths, starts):
    found = jnp.full(slot.shape, -1, jnp.int32)
    for j in range(count):
        inside = (slot >= starts(j)) & (slot < starts(j) + lengths(j))
        found = jnp.where(inside, j, found)
    return jnp.where(slot < 0, -2, found)


def dot_rows(left, right):
    return lax.dot_general(left, right, (((0,), (0,)), ((), ())), preferred_element_type=F32)


def dot_trans(left, right):
    return lax.dot_general(left, right, (((1,), (1,)), ((), ())), preferred_element_type=F32)


def dot(left, right):
    return jnp.dot(left, right, preferred_element_type=F32)


def exchange_kernel(size, modes, *refs):
    count = len(modes)
    ins, outs = refs[:count], refs[count : 2 * count]
    send, recv = refs[2 * count :]
    me = lax.axis_index("fsdp")
    barrier = pltpu.get_barrier_semaphore()
    for step in range(1, size):
        peer = lax.rem(me + step, size)
        pl.semaphore_signal(barrier, inc=1, device_id={"fsdp": peer}, device_id_type=MESH_ID)
    pl.semaphore_wait(barrier, size - 1)
    copies = []
    for k, mode in enumerate(modes):
        for step in range(1, size):
            peer = lax.rem(me + step, size)
            copies.append(
                pltpu.make_async_remote_copy(
                    src_ref=ins[k] if mode == "ag" else ins[k].at[peer],
                    dst_ref=outs[k].at[me],
                    send_sem=send.at[k, step - 1],
                    recv_sem=recv.at[k, step - 1],
                    device_id={"fsdp": peer},
                    device_id_type=MESH_ID,
                )
            )
    for copy in copies:
        copy.start()
    for copy in copies:
        copy.wait()


def exchange(ident, gathered=(), traded=()):
    size = lax.axis_size("fsdp")
    arrays = tuple(gathered) + tuple(traded)
    modes = ("ag",) * len(gathered) + ("a2a",) * len(traded)
    shapes = [(size,) + a.shape for a in gathered] + [a.shape for a in traded]
    sent = sum((size - 1) * a.size * a.dtype.itemsize for a in gathered)
    sent += sum((size - 1) * a.size * a.dtype.itemsize // size for a in traded)
    outs = pl.pallas_call(
        functools.partial(exchange_kernel, size, modes),
        out_shape=[jax.ShapeDtypeStruct(s, a.dtype) for s, a in zip(shapes, arrays)],
        in_specs=[pl.BlockSpec(memory_space=pl.ANY)] * len(arrays),
        out_specs=[pl.BlockSpec(memory_space=pl.ANY)] * len(arrays),
        scratch_shapes=[
            pltpu.SemaphoreType.DMA((len(arrays), size - 1)),
            pltpu.SemaphoreType.DMA((len(arrays), size - 1)),
        ],
        compiler_params=pltpu.CompilerParams(collective_id=ident, has_side_effects=True),
        cost_estimate=pl.CostEstimate(flops=0, bytes_accessed=sent * 50, transcendentals=0),
        name=f"exchange{ident}",
    )(*arrays)
    return outs


def with_own(slots, own):
    return lax.dynamic_update_index_in_dim(slots, own, lax.axis_index("fsdp"), 0)


def gather_tokens(ident, rows):
    (slots,) = exchange(ident, gathered=(rows,))
    slots = with_own(slots, rows)
    return slots.reshape((-1,) + rows.shape[1:])


def sum_tokens(ident, partial):
    (slots,) = exchange(ident, traded=(partial.astype(BF),))
    me = lax.axis_index("fsdp")
    mine = lax.dynamic_index_in_dim(partial, me, 0, keepdims=False)
    total = mine
    for i in range(slots.shape[0]):
        total = total + jnp.where(me == i, 0.0, slots[i].astype(F32))
    return total


def masks_of(first, block, lens_ref, starts_ref, group, count):
    rows = first + block * BLOCK
    query = rows + lax.broadcasted_iota(jnp.int32, (BLOCK, 1), 0)
    keys = rows - WINDOW + lax.broadcasted_iota(jnp.int32, (1, BLOCK + WINDOW), 1)
    length = lambda j: lens_ref[group, j]
    start = lambda j: starts_ref[group, j]
    seg_q = segment_of(query, count, length, start)
    seg_k = segment_of(keys, count, length, start)
    far = query - keys
    return (far >= 0) & (far <= WINDOW) & (seg_q == seg_k)


def soft_of(query, keys, mask):
    scores = dot_trans(query, keys) * SCALE
    scores = jnp.where(mask, scores, NEG)
    peak = jnp.max(scores, axis=1, keepdims=True)
    exponent = jnp.exp(scores - peak)
    return exponent / jnp.sum(exponent, axis=1, keepdims=True)


def lane_head(width):
    return lax.broadcasted_iota(jnp.int32, (1, width), 1) // HEAD_DIM


def rows_of_heads(edge_ref, qkv_ref):
    width = qkv_ref.shape[1] // 3
    own = qkv_ref[...]
    edge = edge_ref[...]
    keys = jnp.concatenate([edge[:, :width], own[:, width : 2 * width]], 0)
    values = jnp.concatenate([edge[:, width:], own[:, 2 * width :]], 0)
    return own[:, :width], keys, values


def attend_back_kernel(
    count, lens_ref, starts_ref, first_ref, edge_ref, qkv_ref, g_ref,
    dqkv_ref, dedge_ref, dk_acc, dv_acc, dq_acc,
):
    group = pl.program_id(0)
    first = first_ref[0]
    queries, keys, values = rows_of_heads(edge_ref, qkv_ref)
    rows, width = queries.shape
    head_of = lane_head(width)
    dk_acc[...] = jnp.zeros_like(dk_acc)
    dv_acc[...] = jnp.zeros_like(dv_acc)
    for block in range(rows // BLOCK):
        mask = masks_of(first, block, lens_ref, starts_ref, group, count)
        low = block * BLOCK
        span = slice(low, low + BLOCK + WINDOW)
        query = queries[low : low + BLOCK]
        grad = g_ref[low : low + BLOCK, :]
        key, value = keys[span], values[span]
        dq = jnp.zeros((BLOCK, width), F32)
        dk = jnp.zeros((BLOCK + WINDOW, width), F32)
        dv = jnp.zeros((BLOCK + WINDOW, width), F32)
        for head in range(width // HEAD_DIM):
            mine = head_of == head
            own_q = jnp.where(mine, query, jnp.zeros_like(query))
            own_g = jnp.where(mine, grad, jnp.zeros_like(grad))
            soft = soft_of(own_q, key, mask)
            grad_soft = dot_trans(own_g, value)
            total = jnp.sum(grad_soft * soft, axis=1, keepdims=True)
            grad_scores = (soft * (grad_soft - total)).astype(BF)
            dq = jnp.where(mine, dot(grad_scores, key), dq)
            dk = dk + dot_rows(grad_scores, own_q)
            dv = dv + dot_rows(soft.astype(BF), own_g)
        dq_acc[low : low + BLOCK, :] = dq * SCALE
        dk_acc[span, :] += dk * SCALE
        dv_acc[span, :] += dv
    dedge_ref[...] = jnp.concatenate([dk_acc[:WINDOW, :], dv_acc[:WINDOW, :]], 1).astype(BF)
    dqkv_ref[...] = jnp.concatenate([dq_acc[...], dk_acc[WINDOW:, :], dv_acc[WINDOW:, :]], 1)


def attend_back(lens, starts, first, rows, edge, qkv, grad):
    groups = qkv.shape[0] // rows
    width = qkv.shape[1] // 3
    block = lambda n, w: pl.BlockSpec((n, w), lambda g: (g, 0))
    table = pl.BlockSpec(memory_space=pltpu.SMEM)
    cost = groups * rows * 192 * 4 * width
    return pl.pallas_call(
        functools.partial(attend_back_kernel, lens.shape[1]),
        grid=(groups,),
        out_shape=[
            jax.ShapeDtypeStruct(qkv.shape, F32),
            jax.ShapeDtypeStruct(edge.shape, BF),
        ],
        in_specs=[table] * 3
        + [block(WINDOW, 2 * width), block(rows, 3 * width), block(rows, width)],
        out_specs=[block(rows, 3 * width), block(WINDOW, 2 * width)],
        scratch_shapes=[
            pltpu.VMEM((rows + WINDOW, width), F32),
            pltpu.VMEM((rows + WINDOW, width), F32),
            pltpu.VMEM((rows, width), F32),
        ],
        cost_estimate=pl.CostEstimate(
            flops=cost * 8, bytes_accessed=qkv.size * 8, transcendentals=cost // 448
        ),
        name="attend_back",
    )(lens, starts, first, edge, qkv, grad)


def with_back_kernel(dqkv_ref, back_ref, out_ref):
    rows, width = dqkv_ref.shape
    kept = rows - WINDOW
    out_ref[:kept, :] = dqkv_ref[:kept, :].astype(BF)
    back = back_ref[...].astype(F32)
    back = jnp.concatenate([jnp.zeros((WINDOW, width // 3), F32), back], 1)
    out_ref[kept:, :] = (dqkv_ref[kept:, :] + back).astype(BF)


def with_back(rows, dqkv, back):
    groups = dqkv.shape[0] // rows
    block = lambda n, w: pl.BlockSpec((n, w), lambda g: (g, 0))
    width = dqkv.shape[1]
    return pl.pallas_call(
        with_back_kernel,
        grid=(groups,),
        out_shape=jax.ShapeDtypeStruct(dqkv.shape, BF),
        in_specs=[block(rows, width), block(WINDOW, back.shape[1])],
        out_specs=block(rows, width),
        cost_estimate=pl.CostEstimate(flops=0, bytes_accessed=dqkv.size * 6, transcendentals=0),
        name="with_back",
    )(dqkv, back)


def remote(src, dst, send, recv, **peer):
    return pltpu.make_async_remote_copy(
        src_ref=src,
        dst_ref=dst,
        send_sem=send,
        recv_sem=recv,
        device_id=peer,
        device_id_type=MESH_ID,
    )


def greet_group(barrier, size):
    me = lax.axis_index("fsdp")
    for step in range(1, size):
        peer = lax.rem(me + step, size)
        pl.semaphore_signal(barrier, inc=1, device_id={"fsdp": peer}, device_id_type=MESH_ID)


class Group:
    def __init__(self, size):
        self.size = size
        self.me = lax.axis_index("fsdp")
        self.square = size == 4
        if self.square:
            x, y = lax.rem(self.me, 2), self.me // 2
            self.at = lambda bx, by: lax.rem(y + by, 2) * 2 + lax.rem(x + bx, 2)
            self.x, self.y, self.far = self.at(1, 0), self.at(0, 1), self.at(1, 1)

    def from_own(self, step):
        if self.square:
            return self.at(lax.rem(step, 2), step // 2)
        return lax.rem(self.me - step + self.size, self.size)

    def to_own(self, step):
        if self.square:
            return self.at(1 - step // 2, 1 - lax.rem(step, 2))
        return lax.rem(self.me + 1 + step, self.size)


class Gather:
    def __init__(self, group, ref, send, recv):
        self.group, self.ref, self.send, self.recv = group, ref, send, recv
        self.half = ref.shape[1] // 2

    def part(self, k, slot, half, peer):
        view = self.ref.at[slot, pl.ds(half * self.half, self.half)]
        return remote(view, view, self.send.at[k], self.recv.at[k], fsdp=peer)

    def whole(self, k):
        g = self.group
        view = self.ref.at[g.me]
        sems = self.send.at[k - 1], self.recv.at[k - 1]
        return remote(view, view, *sems, fsdp=lax.rem(g.me + k, g.size))

    def copy(self, k):
        g = self.group
        if not g.square:
            return self.whole(k + 1)
        slot = (g.me, g.me, g.me, g.me, g.x, g.y)[k]
        half = (0, 1, 0, 1, 0, 1)[k]
        return self.part(k, slot, half, (g.x, g.x, g.y, g.y, g.y, g.x)[k])

    def start_half(self, half):
        if self.group.square:
            self.copy(half).start()
            self.copy(2 + half).start()
        elif half == 1:
            for k in range(self.group.size - 1):
                self.copy(k).start()

    def relay(self):
        if self.group.square:
            self.copy(0).wait_recv()
            self.copy(4).start()
            self.copy(3).wait_recv()
            self.copy(5).start()

    def ready(self, step):
        if not self.group.square:
            self.copy(step - 1).wait_recv()
        elif step == 3:
            self.copy(4).wait_recv()
            self.copy(5).wait_recv()
        else:
            self.copy(step).wait_recv()

    def finish(self):
        for k in range(transfers(self.group.size)):
            self.copy(k).wait_send()


class Scatter:
    def __init__(self, group, part, first, over, joined, last, send, recv):
        self.group, self.part = group, part
        self.first, self.over, self.joined, self.last = first, over, joined, last
        self.send, self.recv = send, recv
        self.half = part.shape[1] // 2

    def copy(self, k):
        g, half = self.group, self.half
        low, high = pl.ds(0, half), pl.ds(half, half)
        if not g.square:
            src, dst, peer = self.part.at[k], self.first.at[k], lax.rem(g.me + 1 + k, g.size)
        else:
            src, dst, peer = (
                lambda: (self.part.at[0, low], self.over.at[0], g.x),
                lambda: (self.part.at[0, high], self.over.at[1], g.y),
                lambda: (self.part.at[1, low], self.first.at[0], g.x),
                lambda: (self.part.at[2, high], self.first.at[1], g.y),
                lambda: (self.joined.at[0], self.last.at[0], g.y),
                lambda: (self.joined.at[1], self.last.at[1], g.x),
            )[k]()
        return remote(src, dst, self.send.at[k], self.recv.at[k], fsdp=peer)

    def made(self, step):
        if not self.group.square:
            self.copy(step).start()
        elif step == 0:
            self.copy(0).start()
            self.copy(1).start()
        elif step in (1, 2):
            self.copy(step + 1).start()

    def join(self):
        if not self.group.square:
            return
        half = self.half
        for k, (step, rows) in enumerate(((2, slice(0, half)), (1, slice(half, 2 * half)))):
            self.copy(k).wait_recv()
            own = self.part[step, rows].astype(F32)
            self.joined[k] = (own + self.over[k].astype(F32)).astype(BF)
            self.copy(4 + k).start()

    def total(self, half):
        count = self.half
        if self.group.square:
            self.copy(2 + half).wait_recv()
            self.copy(4 + half).wait_recv()
            return self.first[half].astype(F32) + self.last[half].astype(F32)
        if half == 0:
            for k in range(self.group.size - 1):
                self.copy(k).wait_recv()
        rows = slice(half * count, (half + 1) * count)
        out = self.first[0, rows].astype(F32)
        for k in range(1, self.group.size - 1):
            out = out + self.first[k, rows].astype(F32)
        return out

    def finish(self):
        for k in range(transfers(self.group.size)):
            self.copy(k).wait_send()


def transfers(size):
    return 6 if size == 4 else size - 1


def scatter_shapes(size, rows, width):
    half = rows // 2
    slots = (2, half, width) if size == 4 else (size - 1, rows, width)
    return [
        pltpu.VMEM((size, rows, width), BF),
        pltpu.VMEM(slots, BF),
        pltpu.VMEM((2, half, width), BF),
        pltpu.VMEM((2, half, width), BF),
        pltpu.VMEM((2, half, width), BF),
        pltpu.SemaphoreType.DMA((transfers(size),)),
        pltpu.SemaphoreType.DMA((transfers(size),)),
    ]


def each_step(size, body):
    def one(step, carry):
        body(step, lambda k: pl.when(step == k))
        return carry

    lax.fori_loop(0, size, one, 0)


def open_kernel(size, parts, gated_ref, piece_ref, all_ref, qkv_ref, edge_ref, map_ref, tail_ref,
                load, send, recv, up_send, up_recv, down_send, down_recv, side_send, side_recv,
                halo_send, halo_recv):
    rank = lax.axis_index("seq")
    line = parts // 2
    z, core = rank // 2, lax.rem(rank, 2)
    above, below, beside = rank + 2, rank - 2, rank + 1 - 2 * core
    rows = gated_ref.shape[0]
    local = qkv_ref.shape[2] // 3
    group = Group(size)
    barrier = pltpu.get_barrier_semaphore()
    greet_group(barrier, size)

    def greet(peer):
        pl.semaphore_signal(barrier, inc=1, device_id={"seq": peer}, device_id_type=MESH_ID)

    greet(beside)
    has_above, has_below = z < line - 1, z > 0
    far_up = has_above & (core == 1)
    far_down = has_below & (core == 0)
    near = ((has_above, above), (has_below, below), (far_up, rank + 1), (far_down, rank - 1))
    for there, peer in near:
        pl.when(there)(functools.partial(greet, peer))
    own = pltpu.make_async_copy(piece_ref, map_ref.at[:, rank], load)
    own.start()
    all_ref[group.me] = gated_ref[...]
    ups_known = (2 * line - 2 - z) // line
    downs_known = (z + line - 1) // line
    pl.semaphore_wait(barrier, size + ups_known * (1 + core) + downs_known * (2 - core))

    gather = Gather(group, all_ref, send, recv)

    def hop(sems, slot, owner, peer):
        view = map_ref.at[:, owner]
        return remote(view, view, sems[0].at[slot], sems[1].at[slot], seq=peer)

    ups, downs, sides = (up_send, up_recv), (down_send, down_recv), (side_send, side_recv)
    gather.start_half(0)
    gather.start_half(1)
    own.wait()
    pl.when(has_above)(lambda: hop(ups, 0, rank, above).start())
    pl.when(has_below)(lambda: hop(downs, 0, rank, below).start())
    hop(sides, z, rank, beside).start()
    gather.relay()
    for j in range(1, line):
        @pl.when(z >= j)
        def _():
            hop(ups, j - 1, rank, above).wait_recv()
            owner = rank - 2 * j
            pl.when(has_above)(lambda: hop(ups, j, owner, above).start())
            hop(sides, z - j, owner, beside).start()

        @pl.when(z + j < line)
        def _():
            hop(downs, j - 1, rank, below).wait_recv()
            owner = rank + 2 * j
            pl.when(has_below)(lambda: hop(downs, j, owner, below).start())
            hop(sides, z + j, owner, beside).start()

    for step in range(1, size):
        gather.ready(step)
    for k in range(line):
        hop(sides, k, rank, beside).wait_recv()

    weights = map_ref[...].reshape(-1, map_ref.shape[3])

    def halo():
        return remote(tail_ref, edge_ref, halo_send, halo_recv, seq=rank + 1)

    def one(g, carry):
        out = dot(all_ref[g], weights).astype(BF)
        qkv_ref[g] = out
        tail_ref[g] = out[rows - WINDOW :, local:]
        return carry

    lax.fori_loop(0, size, one, 0)
    last = rank == parts - 1
    pl.when(rank < parts - 1)(lambda: halo().start())

    @pl.when(rank == 0)
    def _():
        edge_ref[...] = jnp.zeros_like(edge_ref)

    gather.finish()
    for k in range(line):
        hop(sides, k, rank, beside).wait_send()
    pl.when(has_above)(lambda: hop(ups, 0, rank, above).wait_send())
    pl.when(has_below)(lambda: hop(downs, 0, rank, below).wait_send())
    for j in range(1, line):
        pl.when((z >= j) & has_above)(lambda: hop(ups, j, rank, above).wait_send())
        pl.when((z + j < line) & has_below)(lambda: hop(downs, j, rank, below).wait_send())
    pl.when(rank > 0)(lambda: halo().wait_recv())
    pl.when(rank < parts - 1)(lambda: halo().wait_send())


def open_mixer(ident, gated, piece):
    size, parts = lax.axis_size("fsdp"), lax.axis_size("seq")
    rows, width = gated.shape
    cols = piece.shape[2]
    line = parts // 2
    sems = lambda n: [pltpu.SemaphoreType.DMA((n,))] * 2
    vmem = pl.BlockSpec(memory_space=pltpu.VMEM)
    return pl.pallas_call(
        functools.partial(open_kernel, size, parts),
        out_shape=[
            jax.ShapeDtypeStruct((size, rows, width), BF),
            jax.ShapeDtypeStruct((size, rows, cols), BF),
            jax.ShapeDtypeStruct((size, WINDOW, cols // 3 * 2), BF),
            jax.ShapeDtypeStruct((size, parts) + piece.shape[1:], BF),
        ],
        in_specs=[vmem, pl.BlockSpec(memory_space=pl.ANY)],
        out_specs=[vmem] * 4,
        scratch_shapes=[
            pltpu.VMEM((size, WINDOW, cols // 3 * 2), BF),
            pltpu.SemaphoreType.DMA,
        ]
        + sems(transfers(size))
        + sems(line)
        + sems(line)
        + sems(line)
        + [pltpu.SemaphoreType.DMA, pltpu.SemaphoreType.DMA],
        compiler_params=pltpu.CompilerParams(collective_id=ident, has_side_effects=True),
        cost_estimate=pl.CostEstimate(
            flops=2 * size * rows * width * cols, bytes_accessed=150_000_000, transcendentals=0
        ),
        name="open_mixer",
    )(gated, piece)


def middle_kernel(size, count, lens_ref, starts_ref, edge_ref, qkv_ref, out_map_ref, tokens_ref,
                  gain_ref, gu_hbm, down_ref, grads_hbm, middle_ref, heads_ref, all_hbm, hidden_hbm, gu_grad_hbm, gu_out,
                  part, first, over, joined, last, s_send, s_recv, own_ref, all_ref, g_send, g_recv,
                  gu_ref, grads_ref, hidden_ref, gu_grad_ref, loads, stores):
    rows = tokens_ref.shape[0]
    local = heads_ref.shape[2]
    inner = down_ref.shape[0]
    slot = lax.axis_index("seq") * rows
    group = Group(size)
    barrier = pltpu.get_barrier_semaphore()
    greet_group(barrier, size)
    fetches = [
        pltpu.make_async_copy(gu_hbm.at[:, f], gu_ref.at[f], loads.at[f]) for f in range(size)
    ] + [pltpu.make_async_copy(grads_hbm, grads_ref, loads.at[size])]
    for fetch in fetches:
        fetch.start()
    pl.semaphore_wait(barrier, size - 1)
    scatter = Scatter(group, part, first, over, joined, last, s_send, s_recv)
    gather = Gather(group, all_ref, g_send, g_recv)
    head_of = lane_head(local)

    def mix(step, is_step):
        g = group.to_own(step)
        own = qkv_ref[g]
        edge = edge_ref[g]
        queries = own[:, :local]
        keys = jnp.concatenate([edge[:, :local], own[:, local : 2 * local]], 0)
        values = jnp.concatenate([edge[:, local:], own[:, 2 * local :]], 0)
        outs = []
        for block in range(rows // BLOCK):
            mask = masks_of(slot, block, lens_ref, starts_ref, g, count)
            low = block * BLOCK
            query = queries[low : low + BLOCK]
            key = keys[low : low + BLOCK + WINDOW]
            value = values[low : low + BLOCK + WINDOW]
            out = jnp.zeros((BLOCK, local), F32)
            for head in range(local // HEAD_DIM):
                mine = head_of == head
                soft = soft_of(jnp.where(mine, query, jnp.zeros_like(query)), key, mask)
                out = jnp.where(mine, dot(soft.astype(BF), value), out)
            outs.append(out.astype(BF))
        heads = jnp.concatenate(outs, 0)
        heads_ref[g] = heads
        branch = dot(heads, out_map_ref[...])
        is_step(size - 1)(lambda: own_ref.__setitem__(..., branch))
        part[step] = branch.astype(BF)
        for k in range(size - 1):
            is_step(k)(functools.partial(scatter.made, k))

    each_step(size, mix)
    scatter.join()
    half = rows // 2
    for h in range(2):
        span = slice(h * half, (h + 1) * half)
        total = own_ref[span, :] + scatter.total(h)
        middle = tokens_ref[span, :].astype(F32) + total
        middle_ref[span, :] = middle
        scale = lax.rsqrt(jnp.mean(middle * middle, axis=1, keepdims=True) + EPS)
        all_ref[group.me, span] = (middle * scale * gain_ref[...]).astype(BF)
        gather.start_half(h)
    for fetch in fetches:
        fetch.wait()
    keeps = [pltpu.make_async_copy(gu_ref.at[f], gu_out.at[f], loads.at[f]) for f in range(size)]
    for keep in keeps:
        keep.start()

    def out_copies(g):
        return [
            pltpu.make_async_copy(src.at[g], dst.at[g], stores.at[k, g])
            for k, (src, dst) in enumerate(
                ((all_ref, all_hbm), (hidden_ref, hidden_hbm), (gu_grad_ref, gu_grad_hbm))
            )
        ]

    def feed(step, is_step):
        g = group.from_own(step)

        @is_step(1)
        def _():
            gather.relay()

        for k in range(1, size):
            is_step(k)(functools.partial(gather.ready, k))
        weights = gu_ref[...].reshape(-1, gu_ref.shape[3])
        acts = dot(all_ref[g], weights)
        gate, up = acts[:, :inner], acts[:, inner:]
        sigma = jax.nn.sigmoid(gate)
        silu = gate * sigma
        hidden_ref[g] = (silu * up).astype(BF)
        grad_hidden = dot_trans(grads_ref[g], down_ref[...])
        grad_gate = grad_hidden * up * sigma * (1.0 + gate * (1.0 - sigma))
        gu_grad_ref[g] = jnp.concatenate([grad_gate, grad_hidden * silu], 1).astype(BF)
        for copy in out_copies(g):
            copy.start()

    each_step(size, feed)
    scatter.finish()
    gather.finish()
    for keep in keeps:
        keep.wait()
    for g in range(size):
        for copy in out_copies(g):
            copy.wait()


def middle_part(ident, lens, starts, edge, qkv, out_weight, tokens, gain, gu_every, down_weight, grads):
    size = lax.axis_size("fsdp")
    rows, width = tokens.shape
    local, inner = out_weight.shape[0], down_weight.shape[0]
    vmem = pl.BlockSpec(memory_space=pltpu.VMEM)
    smem = pl.BlockSpec(memory_space=pltpu.SMEM)
    hbm = pl.BlockSpec(memory_space=pl.ANY)
    parts, _, piece, cols = gu_every.shape
    shape = lambda w: (size, rows, w)
    return pl.pallas_call(
        functools.partial(middle_kernel, size, lens.shape[1]),
        out_shape=[
            jax.ShapeDtypeStruct((rows, width), F32),
            jax.ShapeDtypeStruct(shape(local), BF),
            jax.ShapeDtypeStruct(shape(width), BF),
            jax.ShapeDtypeStruct(shape(inner), BF),
            jax.ShapeDtypeStruct(shape(cols), BF),
            jax.ShapeDtypeStruct((size, parts, piece, cols), BF),
        ],
        in_specs=[smem, smem, vmem, vmem, vmem, vmem, vmem, hbm, vmem, hbm],
        out_specs=[vmem, vmem, hbm, hbm, hbm, hbm],
        scratch_shapes=scatter_shapes(size, rows, width)
        + [
            pltpu.VMEM((rows, width), F32),
            pltpu.VMEM(shape(width), BF),
            pltpu.SemaphoreType.DMA((transfers(size),)),
            pltpu.SemaphoreType.DMA((transfers(size),)),
            pltpu.VMEM((size, parts, piece, cols), BF),
            pltpu.VMEM(shape(width), BF),
            pltpu.VMEM(shape(inner), BF),
            pltpu.VMEM(shape(cols), BF),
            pltpu.SemaphoreType.DMA((size + 1,)),
            pltpu.SemaphoreType.DMA((3, size)),
        ],
        compiler_params=pltpu.CompilerParams(
            collective_id=ident, has_side_effects=True, vmem_limit_bytes=67_000_000
        ),
        cost_estimate=pl.CostEstimate(
            flops=2 * size * rows * width * (local + 3 * inner),
            bytes_accessed=250_000_000,
            transcendentals=0,
        ),
        name="middle_part",
    )(lens, starts, edge, qkv, out_weight, tokens, gain, gu_every, down_weight, grads)


def pack_kernel(size, parts, x_ref, g_ref, *refs):
    out_ref = refs[-1]
    full = dot_rows(x_ref[...], g_ref[...])
    pair = out_ref.shape[1]
    rows = full.shape[0] // pair
    piece = rows // parts
    for k in range(pair):
        own = full[k * rows : (k + 1) * rows]
        if len(refs) == 3:
            heads_ref, gb_ref = refs[0], refs[1]
            side = dot_rows(heads_ref[...], gb_ref[...])
            wide = side.shape[1] // pair
            own = jnp.concatenate([own, side[:, k * wide : (k + 1) * wide]], 1)
        out_ref[:, k] = own.astype(BF).reshape(parts, piece, own.shape[1])


def pack_grads(parts, size, x, g, heads=None, gb=None):
    width, cols = x.shape[1], g.shape[1]
    rows = width // size
    piece = rows // parts
    if piece % 8 or (2 * rows) % 128:
        full = dot_rows(x, g).reshape(size, parts, piece, cols)
        if heads is not None:
            side = dot_rows(heads, gb).reshape(parts, piece, size, -1).transpose(2, 0, 1, 3)
            full = jnp.concatenate([full, side], 3)
        return full.transpose(1, 0, 2, 3).astype(BF)
    total = x.shape[0]
    pair = pl.BlockSpec((total, 2 * rows), lambda i: (0, i))
    whole = lambda a: pl.BlockSpec(a.shape, lambda i: (0, 0), pipeline_mode=pl.Buffered(1))
    args, specs = [x, g], [pair, whole(g)]
    out_cols = cols
    if heads is not None:
        args += [heads, gb]
        specs += [whole(heads), pair]
        out_cols += rows
    return pl.pallas_call(
        functools.partial(pack_kernel, size, parts),
        grid=(size // 2,),
        out_shape=jax.ShapeDtypeStruct((parts, size, piece, out_cols), BF),
        in_specs=specs,
        out_specs=pl.BlockSpec((parts, 2, piece, out_cols), lambda i: (0, i, 0, 0)),
        cost_estimate=pl.CostEstimate(
            flops=2 * total * width * out_cols,
            bytes_accessed=2 * (x.size + g.size + width * out_cols),
            transcendentals=0,
        ),
        name="pack_grads",
    )(*args)


def unpack_kernel(widths, every_ref, *outs):
    size = every_ref.shape[1]
    blocks = [every_ref[0, i].astype(F32) for i in range(size)]
    low = 0
    for width, out in zip(widths, outs):
        out[...] = jnp.concatenate([b[:, low : low + width] for b in blocks], 1)
        low += width


def unpack_grads(every, widths):
    parts, size, piece, cols = every.shape
    if piece % 8:
        outs, low = [], 0
        for width in widths:
            block = every[:, :, :, low : low + width].transpose(0, 2, 1, 3)
            outs.append(block.reshape(parts * piece, size * width).astype(F32))
            low += width
        return outs
    return pl.pallas_call(
        functools.partial(unpack_kernel, widths),
        grid=(parts,),
        out_shape=[jax.ShapeDtypeStruct((parts * piece, size * w), F32) for w in widths],
        in_specs=[pl.BlockSpec((1, size, piece, cols), lambda i: (i, 0, 0, 0))],
        out_specs=[pl.BlockSpec((piece, size * w), lambda i: (i, 0)) for w in widths],
        cost_estimate=pl.CostEstimate(flops=0, bytes_accessed=every.size * 6, transcendentals=0),
        name="unpack_grads",
    )(every)


def columns_piece(weights, part, parts):
    size = lax.axis_size("fsdp")
    rows = weights[0].shape[0] // parts
    pieces = []
    for weight in weights:
        own = lax.dynamic_slice_in_dim(weight, part * rows, rows, 0)
        pieces.append(own.reshape(rows, size, -1))
    return jnp.concatenate(pieces, 2).transpose(1, 0, 2)


def shards(
    tokens,
    seq_lengths,
    seq_offsets,
    norm1_gain,
    conv_weight,
    query_weight,
    key_weight,
    value_weight,
    out_weight,
    norm2_gain,
    gate_weight,
    up_weight,
    down_weight,
    cotangent,
):
    size = lax.axis_size("fsdp")
    parts = lax.axis_size("seq")
    part = lax.axis_index("seq")
    me = lax.axis_index("fsdp")
    own_tokens = tokens[0]
    rows, width = own_tokens.shape
    slice_width = norm1_gain.shape[0]
    first_slot = part * rows
    count = seq_lengths.shape[1]

    slot_ext = first_slot - 2 + jnp.arange(rows + 2, dtype=jnp.int32)
    segment_ext = segment_of(
        slot_ext, count, lambda j: seq_lengths[0, j], lambda j: seq_offsets[0, j]
    )
    segment_own = segment_ext[2:]
    same_one = (segment_own == segment_ext[1:-1]).astype(F32)[:, None]
    same_two = (segment_own == segment_ext[:-2]).astype(F32)[:, None]
    live_mask = (segment_own >= 0).astype(F32)[:, None]

    gains = jnp.concatenate(
        [
            norm1_gain[None],
            norm2_gain[None],
            conv_weight.T,
            jnp.zeros((3, slice_width), BF),
        ],
        0,
    )
    table = jnp.zeros((8, 128), jnp.int32)
    table = table.at[0, :count].set(seq_lengths[0]).at[1, :count].set(seq_offsets[0])
    qkv_piece = columns_piece((query_weight, key_weight, value_weight), part, parts)
    gu_piece = columns_piece((gate_weight, up_weight), part, parts)
    gains_all, table_all, qkv_slots, gu_slots = exchange(
        0, gathered=(gains, table), traded=(qkv_piece, gu_piece)
    )
    gains_all = with_own(gains_all, gains).transpose(1, 0, 2).reshape(8, width)
    table_all = with_own(table_all, table)
    lens_all, starts_all = table_all[:, 0, :count], table_all[:, 1, :count]
    qkv_slots = with_own(qkv_slots, lax.dynamic_index_in_dim(qkv_piece, me, 0, keepdims=False))
    gu_slots = with_own(gu_slots, lax.dynamic_index_in_dim(gu_piece, me, 0, keepdims=False))
    grad_out = cotangent[0].astype(F32) * live_mask
    grad_down_all = lax.all_gather(grad_out.astype(BF), "fsdp", axis=0, tiled=True)
    gu_slots, grad_down_all = lax.optimization_barrier((gu_slots, grad_down_all))
    gu_every = lax.all_gather(gu_slots, "seq", axis=0)
    norm_one = gains_all[0].astype(F32)
    norm_two = gains_all[1].astype(F32)
    taps = gains_all[2:5].astype(F32)

    edge_tokens = shifted(own_tokens[rows - 2 :], "seq", 1)
    extended = jnp.concatenate([edge_tokens, own_tokens], 0).astype(F32)
    scale_one = lax.rsqrt(jnp.mean(extended * extended, axis=1, keepdims=True) + EPS)
    normed = extended * scale_one * norm_one
    conv_mix = (
        normed[2:] * taps[0]
        + same_one * normed[1:-1] * taps[1]
        + same_two * normed[:-2] * taps[2]
    )
    gated = (conv_mix * normed[2:]).astype(BF)
    gated_all, qkv, edge, qkv_map = open_mixer(1, gated, qkv_slots)
    qkv_map = qkv_map.reshape(width, -1)
    first = jnp.reshape(first_slot, (1,)).astype(jnp.int32)
    local = out_weight.shape[0]
    middle, heads_out, normed_all, hidden, grad_gu, gu_map = middle_part(
        2,
        lens_all,
        starts_all,
        edge,
        qkv,
        out_weight,
        own_tokens,
        norm_two[None],
        gu_every,
        down_weight,
        grad_down_all.reshape(size, rows, width),
    )
    flat = lambda a: a.reshape(-1, a.shape[-1])
    gated_all, qkv, edge, heads_out = flat(gated_all), flat(qkv), flat(edge), flat(heads_out)
    normed_all, hidden, grad_gu = flat(normed_all), flat(hidden), flat(grad_gu)
    gu_map = gu_map.reshape(width, -1)
    attention = (lens_all, starts_all, first, rows, edge, qkv)
    scale_two = lax.rsqrt(jnp.mean(middle * middle, axis=1, keepdims=True) + EPS)
    unit_two = middle * scale_two
    gu_packed = pack_grads(parts, size, normed_all, grad_gu)
    gu_packed, grad_gu = lax.optimization_barrier((gu_packed, grad_gu))
    gu_piece = lax.psum_scatter(gu_packed, "seq", scatter_dimension=0)
    partial_two = dot_trans(grad_gu, gu_map).reshape(size, rows, width)
    down_sum = dot_rows(hidden, grad_down_all).astype(BF)
    partial_two, down_sum = lax.optimization_barrier((partial_two, down_sum))
    down_total = lax.psum(down_sum, "seq").astype(F32)
    grad_normed_two = sum_tokens(4, partial_two)

    grad_unit_two = grad_normed_two * norm_two
    norm2_term = jnp.sum(grad_normed_two * unit_two, axis=0)
    grad_middle = grad_out + scale_two * (
        grad_unit_two - unit_two * jnp.mean(grad_unit_two * unit_two, axis=1, keepdims=True)
    )
    grad_branch_all = gather_tokens(6, grad_middle.astype(BF))
    grad_branch_all, gu_piece = lax.optimization_barrier((grad_branch_all, gu_piece))
    (gu_slots,) = exchange(5, traded=(gu_piece,))
    gu_slots = with_own(gu_slots, lax.dynamic_index_in_dim(gu_piece, me, 0, keepdims=False))
    gu_every = lax.all_gather(gu_slots, "seq", axis=0)
    grad_branch_all, gu_slots = lax.optimization_barrier((grad_branch_all, gu_slots))

    grad_heads = dot_trans(grad_branch_all, out_weight).astype(BF)
    dqkv, dedge = attend_back(*attention, grad_heads)
    back = shifted(dedge, "seq", -1)
    dqkv = with_back(rows, dqkv, back)
    grad_gated = sum_tokens(7, dot_trans(dqkv, qkv_map).reshape(size, rows, width))
    qkvo_packed = pack_grads(parts, size, gated_all, dqkv, heads_out, grad_branch_all)
    hidden, grad_gated = lax.optimization_barrier((hidden, grad_gated))
    feed = sum_tokens(9, dot(hidden, down_weight).reshape(size, rows, width))
    qkvo_packed, gu_every, down_total, feed = lax.optimization_barrier(
        (qkvo_packed, gu_every, down_total, feed)
    )
    qkvo_piece = lax.psum_scatter(qkvo_packed, "seq", scatter_dimension=0)
    (qkvo_slots,) = exchange(8, traded=(qkvo_piece,))
    qkvo_slots = with_own(
        qkvo_slots, lax.dynamic_index_in_dim(qkvo_piece, me, 0, keepdims=False)
    )
    qkvo_slots = jnp.concatenate([qkvo_slots[..., : 3 * local], qkvo_piece[..., 3 * local :]], -1)
    qkvo_every = lax.all_gather(qkvo_slots, "seq", axis=0)
    gate_total, up_total = unpack_grads(gu_every, (gu_map.shape[1] // 2,) * 2)
    query_total, key_total, value_total, out_total = unpack_grads(qkvo_every, (local,) * 4)

    normed_own = normed[2:]
    grad_mix = grad_gated * normed_own
    part_zero = jnp.pad(grad_gated * conv_mix + grad_mix * taps[0], ((2, 0), (0, 0)))
    part_one = jnp.pad(grad_mix * same_one * taps[1], ((1, 1), (0, 0)))
    part_two = jnp.pad(grad_mix * same_two * taps[2], ((0, 2), (0, 0)))
    grad_normed = part_zero + part_one + part_two
    unit_one = extended * scale_one
    grad_unit_one = grad_normed * norm_one
    grad_extended = scale_one * (
        grad_unit_one - unit_one * jnp.mean(grad_unit_one * unit_one, axis=1, keepdims=True)
    )
    edge_back = shifted(grad_extended[:2], "seq", -1)
    tokens_grad = grad_middle + grad_extended[2:] + jnp.pad(edge_back, ((rows - 2, 0), (0, 0)))

    terms = jnp.stack(
        [
            jnp.sum(grad_normed * unit_one, axis=0),
            norm2_term,
            jnp.sum(grad_mix * normed_own, axis=0),
            jnp.sum(grad_mix * same_one * normed[1:-1], axis=0),
            jnp.sum(grad_mix * same_two * normed[:-2], axis=0),
        ]
    )
    terms = lax.psum(terms, ("seq", "fsdp"))
    terms = lax.dynamic_slice_in_dim(terms, me * slice_width, slice_width, 1)

    layer_out = (live_mask * (middle + feed)).astype(BF)[None]
    return (
        layer_out,
        tokens_grad[None],
        terms[0],
        terms[2:5].T,
        query_total,
        key_total,
        value_total,
        out_total,
        terms[1],
        gate_total,
        up_total,
        down_total,
    )


def solution(mesh):
    placed = (
        P("fsdp", "seq", None),
        P("fsdp", None),
        P("fsdp", None),
        P("fsdp"),
        P("fsdp", None),
        P("fsdp", None),
        P("fsdp", None),
        P("fsdp", None),
        P("fsdp", None),
        P("fsdp"),
        P("fsdp", None),
        P("fsdp", None),
        P("fsdp", None),
        P("fsdp", "seq", None),
    )
    return jax.shard_map(
        shards,
        mesh=mesh,
        in_specs=placed,
        out_specs=(
            P("fsdp", "seq", None),
            P("fsdp", "seq", None),
            P("fsdp"),
            P("fsdp", None),
            P("fsdp", None),
            P("fsdp", None),
            P("fsdp", None),
            P("fsdp", None),
            P("fsdp"),
            P("fsdp", None),
            P("fsdp", None),
            P("fsdp", None),
        ),
        check_vma=False,
    )
```

```python
import functools

import jax
import jax.numpy as jnp
from jax import lax
from jax.experimental import pallas as pl
from jax.experimental.pallas import tpu as pltpu
from jax.sharding import PartitionSpec as P

HEADS = 16
WINDOW = 64
HEAD_DIM = 112
BLOCK = 128

EPS = 1e-05
NEG = -1e30
SCALE = HEAD_DIM ** (-0.5)
MESH_ID = pl.DeviceIdType.MESH
BF = jnp.bfloat16
F32 = jnp.float32


def shifted(array, axis, by):
    length = lax.axis_size(axis)
    pairs = [(i, i + by) for i in range(length) if 0 <= i + by < length]
    return lax.ppermute(array, axis, pairs)


def segment_of(slot, count, lengths, starts):
    found = jnp.full(slot.shape, -1, jnp.int32)
    for j in range(count):
        inside = (slot >= starts(j)) & (slot < starts(j) + lengths(j))
        found = jnp.where(inside, j, found)
    return jnp.where(slot < 0, -2, found)


def dot_rows(left, right):
    return lax.dot_general(left, right, (((0,), (0,)), ((), ())), preferred_element_type=F32)


def dot_trans(left, right):
    return lax.dot_general(left, right, (((1,), (1,)), ((), ())), preferred_element_type=F32)


def dot(left, right):
    return jnp.dot(left, right, preferred_element_type=F32)


def exchange_kernel(size, modes, *refs):
    count = len(modes)
    ins, outs = refs[:count], refs[count : 2 * count]
    send, recv = refs[2 * count :]
    me = lax.axis_index("fsdp")
    barrier = pltpu.get_barrier_semaphore()
    for step in range(1, size):
        peer = lax.rem(me + step, size)
        pl.semaphore_signal(barrier, inc=1, device_id={"fsdp": peer}, device_id_type=MESH_ID)
    pl.semaphore_wait(barrier, size - 1)
    copies = []
    for k, mode in enumerate(modes):
        for step in range(1, size):
            peer = lax.rem(me + step, size)
            copies.append(
                pltpu.make_async_remote_copy(
                    src_ref=ins[k] if mode == "ag" else ins[k].at[peer],
                    dst_ref=outs[k].at[me],
                    send_sem=send.at[k, step - 1],
                    recv_sem=recv.at[k, step - 1],
                    device_id={"fsdp": peer},
                    device_id_type=MESH_ID,
                )
            )
    for copy in copies:
        copy.start()
    for copy in copies:
        copy.wait()


def exchange(ident, gathered=(), traded=()):
    size = lax.axis_size("fsdp")
    arrays = tuple(gathered) + tuple(traded)
    modes = ("ag",) * len(gathered) + ("a2a",) * len(traded)
    shapes = [(size,) + a.shape for a in gathered] + [a.shape for a in traded]
    sent = sum((size - 1) * a.size * a.dtype.itemsize for a in gathered)
    sent += sum((size - 1) * a.size * a.dtype.itemsize // size for a in traded)
    outs = pl.pallas_call(
        functools.partial(exchange_kernel, size, modes),
        out_shape=[jax.ShapeDtypeStruct(s, a.dtype) for s, a in zip(shapes, arrays)],
        in_specs=[pl.BlockSpec(memory_space=pl.ANY)] * len(arrays),
        out_specs=[pl.BlockSpec(memory_space=pl.ANY)] * len(arrays),
        scratch_shapes=[
            pltpu.SemaphoreType.DMA((len(arrays), size - 1)),
            pltpu.SemaphoreType.DMA((len(arrays), size - 1)),
        ],
        compiler_params=pltpu.CompilerParams(collective_id=ident, has_side_effects=True),
        cost_estimate=pl.CostEstimate(flops=0, bytes_accessed=sent * 50, transcendentals=0),
        name=f"exchange{ident}",
    )(*arrays)
    return outs


def with_own(slots, own):
    return lax.dynamic_update_index_in_dim(slots, own, lax.axis_index("fsdp"), 0)


def gather_tokens(ident, rows):
    (slots,) = exchange(ident, gathered=(rows,))
    slots = with_own(slots, rows)
    return slots.reshape((-1,) + rows.shape[1:])


def sum_tokens(ident, partial):
    (slots,) = exchange(ident, traded=(partial.astype(BF),))
    me = lax.axis_index("fsdp")
    mine = lax.dynamic_index_in_dim(partial, me, 0, keepdims=False)
    total = mine
    for i in range(slots.shape[0]):
        total = total + jnp.where(me == i, 0.0, slots[i].astype(F32))
    return total


def masks_of(first, block, lens_ref, starts_ref, group, count):
    rows = first + block * BLOCK
    query = rows + lax.broadcasted_iota(jnp.int32, (BLOCK, 1), 0)
    keys = rows - WINDOW + lax.broadcasted_iota(jnp.int32, (1, BLOCK + WINDOW), 1)
    length = lambda j: lens_ref[group, j]
    start = lambda j: starts_ref[group, j]
    seg_q = segment_of(query, count, length, start)
    seg_k = segment_of(keys, count, length, start)
    far = query - keys
    return (far >= 0) & (far <= WINDOW) & (seg_q == seg_k)


def soft_of(query, keys, mask):
    scores = dot_trans(query, keys) * SCALE
    scores = jnp.where(mask, scores, NEG)
    peak = jnp.max(scores, axis=1, keepdims=True)
    exponent = jnp.exp(scores - peak)
    return exponent / jnp.sum(exponent, axis=1, keepdims=True)


def lane_head(width):
    return lax.broadcasted_iota(jnp.int32, (1, width), 1) // HEAD_DIM


def remote(src, dst, send, recv, **peer):
    return pltpu.make_async_remote_copy(
        src_ref=src,
        dst_ref=dst,
        send_sem=send,
        recv_sem=recv,
        device_id=peer,
        device_id_type=MESH_ID,
    )


def greet_group(barrier, size):
    me = lax.axis_index("fsdp")
    for step in range(1, size):
        peer = lax.rem(me + step, size)
        pl.semaphore_signal(barrier, inc=1, device_id={"fsdp": peer}, device_id_type=MESH_ID)


class Group:
    def __init__(self, size):
        self.size = size
        self.me = lax.axis_index("fsdp")
        self.square = size == 4
        if self.square:
            x, y = lax.rem(self.me, 2), self.me // 2
            self.at = lambda bx, by: lax.rem(y + by, 2) * 2 + lax.rem(x + bx, 2)
            self.x, self.y, self.far = self.at(1, 0), self.at(0, 1), self.at(1, 1)

    def from_own(self, step):
        if self.square:
            return self.at(lax.rem(step, 2), step // 2)
        return lax.rem(self.me - step + self.size, self.size)

    def to_own(self, step):
        if self.square:
            return self.at(1 - step // 2, 1 - lax.rem(step, 2))
        return lax.rem(self.me + 1 + step, self.size)


class Gather:
    def __init__(self, group, ref, send, recv):
        self.group, self.ref, self.send, self.recv = group, ref, send, recv
        self.half = ref.shape[1] // 2

    def part(self, k, slot, half, peer):
        view = self.ref.at[slot, pl.ds(half * self.half, self.half)]
        return remote(view, view, self.send.at[k], self.recv.at[k], fsdp=peer)

    def whole(self, k):
        g = self.group
        view = self.ref.at[g.me]
        sems = self.send.at[k - 1], self.recv.at[k - 1]
        return remote(view, view, *sems, fsdp=lax.rem(g.me + k, g.size))

    def copy(self, k):
        g = self.group
        if not g.square:
            return self.whole(k + 1)
        slot = (g.me, g.me, g.me, g.me, g.x, g.y)[k]
        half = (0, 1, 0, 1, 0, 1)[k]
        return self.part(k, slot, half, (g.x, g.x, g.y, g.y, g.y, g.x)[k])

    def start_half(self, half):
        if self.group.square:
            self.copy(half).start()
            self.copy(2 + half).start()
        elif half == 1:
            for k in range(self.group.size - 1):
                self.copy(k).start()

    def relay(self):
        if self.group.square:
            self.copy(0).wait_recv()
            self.copy(4).start()
            self.copy(3).wait_recv()
            self.copy(5).start()

    def ready(self, step):
        if not self.group.square:
            self.copy(step - 1).wait_recv()
        elif step == 3:
            self.copy(4).wait_recv()
            self.copy(5).wait_recv()
        else:
            self.copy(step).wait_recv()

    def finish(self):
        for k in range(transfers(self.group.size)):
            self.copy(k).wait_send()


class Scatter:
    def __init__(self, group, part, first, over, joined, last, send, recv):
        self.group, self.part = group, part
        self.first, self.over, self.joined, self.last = first, over, joined, last
        self.send, self.recv = send, recv
        self.half = part.shape[1] // 2

    def copy(self, k):
        g, half = self.group, self.half
        low, high = pl.ds(0, half), pl.ds(half, half)
        if not g.square:
            src, dst, peer = self.part.at[k], self.first.at[k], lax.rem(g.me + 1 + k, g.size)
        else:
            src, dst, peer = (
                lambda: (self.part.at[0, low], self.over.at[0], g.x),
                lambda: (self.part.at[0, high], self.over.at[1], g.y),
                lambda: (self.part.at[1, low], self.first.at[0], g.x),
                lambda: (self.part.at[2, high], self.first.at[1], g.y),
                lambda: (self.joined.at[0], self.last.at[0], g.y),
                lambda: (self.joined.at[1], self.last.at[1], g.x),
            )[k]()
        return remote(src, dst, self.send.at[k], self.recv.at[k], fsdp=peer)

    def made(self, step):
        if not self.group.square:
            self.copy(step).start()
        elif step == 0:
            self.copy(0).start()
            self.copy(1).start()
        elif step in (1, 2):
            self.copy(step + 1).start()

    def join(self):
        if not self.group.square:
            return
        half = self.half
        for k, (step, rows) in enumerate(((2, slice(0, half)), (1, slice(half, 2 * half)))):
            self.copy(k).wait_recv()
            own = self.part[step, rows].astype(F32)
            self.joined[k] = (own + self.over[k].astype(F32)).astype(BF)
            self.copy(4 + k).start()

    def total(self, half):
        count = self.half
        if self.group.square:
            self.copy(2 + half).wait_recv()
            self.copy(4 + half).wait_recv()
            return self.first[half].astype(F32) + self.last[half].astype(F32)
        if half == 0:
            for k in range(self.group.size - 1):
                self.copy(k).wait_recv()
        rows = slice(half * count, (half + 1) * count)
        out = self.first[0, rows].astype(F32)
        for k in range(1, self.group.size - 1):
            out = out + self.first[k, rows].astype(F32)
        return out

    def finish(self):
        for k in range(transfers(self.group.size)):
            self.copy(k).wait_send()


def transfers(size):
    return 6 if size == 4 else size - 1


def scatter_shapes(size, rows, width):
    half = rows // 2
    slots = (2, half, width) if size == 4 else (size - 1, rows, width)
    return [
        pltpu.VMEM((size, rows, width), BF),
        pltpu.VMEM(slots, BF),
        pltpu.VMEM((2, half, width), BF),
        pltpu.VMEM((2, half, width), BF),
        pltpu.VMEM((2, half, width), BF),
        pltpu.SemaphoreType.DMA((transfers(size),)),
        pltpu.SemaphoreType.DMA((transfers(size),)),
    ]


def each_step(size, body):
    def one(step, carry):
        body(step, lambda k: pl.when(step == k))
        return carry

    lax.fori_loop(0, size, one, 0)


def open_kernel(size, parts, gated_ref, piece_ref, all_ref, qkv_ref, edge_ref, map_ref, tail_ref,
                load, send, recv, up_send, up_recv, down_send, down_recv, side_send, side_recv,
                halo_send, halo_recv):
    rank = lax.axis_index("seq")
    line = parts // 2
    z, core = rank // 2, lax.rem(rank, 2)
    above, below, beside = rank + 2, rank - 2, rank + 1 - 2 * core
    rows = gated_ref.shape[0]
    local = qkv_ref.shape[2] // 3
    group = Group(size)
    barrier = pltpu.get_barrier_semaphore()
    greet_group(barrier, size)

    def greet(peer):
        pl.semaphore_signal(barrier, inc=1, device_id={"seq": peer}, device_id_type=MESH_ID)

    greet(beside)
    has_above, has_below = z < line - 1, z > 0
    far_up = has_above & (core == 1)
    far_down = has_below & (core == 0)
    near = ((has_above, above), (has_below, below), (far_up, rank + 1), (far_down, rank - 1))
    for there, peer in near:
        pl.when(there)(functools.partial(greet, peer))
    own = pltpu.make_async_copy(piece_ref, map_ref.at[:, rank], load)
    own.start()
    all_ref[group.me] = gated_ref[...]
    ups_known = (2 * line - 2 - z) // line
    downs_known = (z + line - 1) // line
    pl.semaphore_wait(barrier, size + ups_known * (1 + core) + downs_known * (2 - core))

    gather = Gather(group, all_ref, send, recv)

    def hop(sems, slot, owner, peer):
        view = map_ref.at[:, owner]
        return remote(view, view, sems[0].at[slot], sems[1].at[slot], seq=peer)

    ups, downs, sides = (up_send, up_recv), (down_send, down_recv), (side_send, side_recv)
    gather.start_half(0)
    gather.start_half(1)
    own.wait()
    pl.when(has_above)(lambda: hop(ups, 0, rank, above).start())
    pl.when(has_below)(lambda: hop(downs, 0, rank, below).start())
    hop(sides, z, rank, beside).start()
    gather.relay()
    for j in range(1, line):
        @pl.when(z >= j)
        def _():
            hop(ups, j - 1, rank, above).wait_recv()
            owner = rank - 2 * j
            pl.when(has_above)(lambda: hop(ups, j, owner, above).start())
            hop(sides, z - j, owner, beside).start()

        @pl.when(z + j < line)
        def _():
            hop(downs, j - 1, rank, below).wait_recv()
            owner = rank + 2 * j
            pl.when(has_below)(lambda: hop(downs, j, owner, below).start())
            hop(sides, z + j, owner, beside).start()

    for step in range(1, size):
        gather.ready(step)
    for k in range(line):
        hop(sides, k, rank, beside).wait_recv()

    weights = map_ref[...].reshape(-1, map_ref.shape[3])

    def halo():
        return remote(tail_ref, edge_ref, halo_send, halo_recv, seq=rank + 1)

    def one(g, carry):
        out = dot(all_ref[g], weights).astype(BF)
        qkv_ref[g] = out
        tail_ref[g] = out[rows - WINDOW :, local:]
        return carry

    lax.fori_loop(0, size, one, 0)
    last = rank == parts - 1
    pl.when(rank < parts - 1)(lambda: halo().start())

    @pl.when(rank == 0)
    def _():
        edge_ref[...] = jnp.zeros_like(edge_ref)

    gather.finish()
    for k in range(line):
        hop(sides, k, rank, beside).wait_send()
    pl.when(has_above)(lambda: hop(ups, 0, rank, above).wait_send())
    pl.when(has_below)(lambda: hop(downs, 0, rank, below).wait_send())
    for j in range(1, line):
        pl.when((z >= j) & has_above)(lambda: hop(ups, j, rank, above).wait_send())
        pl.when((z + j < line) & has_below)(lambda: hop(downs, j, rank, below).wait_send())
    pl.when(rank > 0)(lambda: halo().wait_recv())
    pl.when(rank < parts - 1)(lambda: halo().wait_send())


def open_mixer(ident, gated, piece):
    size, parts = lax.axis_size("fsdp"), lax.axis_size("seq")
    rows, width = gated.shape
    cols = piece.shape[2]
    line = parts // 2
    sems = lambda n: [pltpu.SemaphoreType.DMA((n,))] * 2
    vmem = pl.BlockSpec(memory_space=pltpu.VMEM)
    return pl.pallas_call(
        functools.partial(open_kernel, size, parts),
        out_shape=[
            jax.ShapeDtypeStruct((size, rows, width), BF),
            jax.ShapeDtypeStruct((size, rows, cols), BF),
            jax.ShapeDtypeStruct((size, WINDOW, cols // 3 * 2), BF),
            jax.ShapeDtypeStruct((size, parts) + piece.shape[1:], BF),
        ],
        in_specs=[vmem, pl.BlockSpec(memory_space=pl.ANY)],
        out_specs=[vmem] * 4,
        scratch_shapes=[
            pltpu.VMEM((size, WINDOW, cols // 3 * 2), BF),
            pltpu.SemaphoreType.DMA,
        ]
        + sems(transfers(size))
        + sems(line)
        + sems(line)
        + sems(line)
        + [pltpu.SemaphoreType.DMA, pltpu.SemaphoreType.DMA],
        compiler_params=pltpu.CompilerParams(collective_id=ident, has_side_effects=True),
        cost_estimate=pl.CostEstimate(
            flops=2 * size * rows * width * cols, bytes_accessed=150_000_000, transcendentals=0
        ),
        name="open_mixer",
    )(gated, piece)


def middle_kernel(size, count, lens_ref, starts_ref, edge_ref, qkv_ref, out_map_ref, tokens_ref,
                  gain_ref, gu_hbm, down_ref, grads_hbm, middle_ref, heads_ref, all_hbm, hidden_hbm, gu_grad_hbm, gu_out,
                  part, first, over, joined, last, s_send, s_recv, own_ref, all_ref, g_send, g_recv,
                  gu_ref, grads_ref, hidden_ref, gu_grad_ref, loads, stores):
    rows = tokens_ref.shape[0]
    local = heads_ref.shape[2]
    inner = down_ref.shape[0]
    slot = lax.axis_index("seq") * rows
    group = Group(size)
    barrier = pltpu.get_barrier_semaphore()
    greet_group(barrier, size)
    fetches = [
        pltpu.make_async_copy(gu_hbm.at[:, f], gu_ref.at[f], loads.at[f]) for f in range(size)
    ] + [pltpu.make_async_copy(grads_hbm, grads_ref, loads.at[size])]
    for fetch in fetches:
        fetch.start()
    pl.semaphore_wait(barrier, size - 1)
    scatter = Scatter(group, part, first, over, joined, last, s_send, s_recv)
    gather = Gather(group, all_ref, g_send, g_recv)
    head_of = lane_head(local)

    def mix(step, is_step):
        g = group.to_own(step)
        own = qkv_ref[g]
        edge = edge_ref[g]
        queries = own[:, :local]
        keys = jnp.concatenate([edge[:, :local], own[:, local : 2 * local]], 0)
        values = jnp.concatenate([edge[:, local:], own[:, 2 * local :]], 0)
        outs = []
        for block in range(rows // BLOCK):
            mask = masks_of(slot, block, lens_ref, starts_ref, g, count)
            low = block * BLOCK
            query = queries[low : low + BLOCK]
            key = keys[low : low + BLOCK + WINDOW]
            value = values[low : low + BLOCK + WINDOW]
            out = jnp.zeros((BLOCK, local), F32)
            for head in range(local // HEAD_DIM):
                mine = head_of == head
                soft = soft_of(jnp.where(mine, query, jnp.zeros_like(query)), key, mask)
                out = jnp.where(mine, dot(soft.astype(BF), value), out)
            outs.append(out.astype(BF))
        heads = jnp.concatenate(outs, 0)
        heads_ref[g] = heads
        branch = dot(heads, out_map_ref[...])
        is_step(size - 1)(lambda: own_ref.__setitem__(..., branch))
        part[step] = branch.astype(BF)
        for k in range(size - 1):
            is_step(k)(functools.partial(scatter.made, k))

    each_step(size, mix)
    scatter.join()
    half = rows // 2
    for h in range(2):
        span = slice(h * half, (h + 1) * half)
        total = own_ref[span, :] + scatter.total(h)
        middle = tokens_ref[span, :].astype(F32) + total
        middle_ref[span, :] = middle
        scale = lax.rsqrt(jnp.mean(middle * middle, axis=1, keepdims=True) + EPS)
        all_ref[group.me, span] = (middle * scale * gain_ref[...]).astype(BF)
        gather.start_half(h)
    for fetch in fetches:
        fetch.wait()
    keeps = [pltpu.make_async_copy(gu_ref.at[f], gu_out.at[f], loads.at[f]) for f in range(size)]
    for keep in keeps:
        keep.start()

    def out_copies(g):
        return [
            pltpu.make_async_copy(src.at[g], dst.at[g], stores.at[k, g])
            for k, (src, dst) in enumerate(
                ((all_ref, all_hbm), (hidden_ref, hidden_hbm), (gu_grad_ref, gu_grad_hbm))
            )
        ]

    def feed(step, is_step):
        g = group.from_own(step)

        @is_step(1)
        def _():
            gather.relay()

        for k in range(1, size):
            is_step(k)(functools.partial(gather.ready, k))
        weights = gu_ref[...].reshape(-1, gu_ref.shape[3])
        acts = dot(all_ref[g], weights)
        gate, up = acts[:, :inner], acts[:, inner:]
        sigma = jax.nn.sigmoid(gate)
        silu = gate * sigma
        hidden_ref[g] = (silu * up).astype(BF)
        grad_hidden = dot_trans(grads_ref[g], down_ref[...])
        grad_gate = grad_hidden * up * sigma * (1.0 + gate * (1.0 - sigma))
        gu_grad_ref[g] = jnp.concatenate([grad_gate, grad_hidden * silu], 1).astype(BF)
        for copy in out_copies(g):
            copy.start()

    each_step(size, feed)
    scatter.finish()
    gather.finish()
    for keep in keeps:
        keep.wait()
    for g in range(size):
        for copy in out_copies(g):
            copy.wait()


def middle_part(ident, lens, starts, edge, qkv, out_weight, tokens, gain, gu_every, down_weight, grads):
    size = lax.axis_size("fsdp")
    rows, width = tokens.shape
    local, inner = out_weight.shape[0], down_weight.shape[0]
    vmem = pl.BlockSpec(memory_space=pltpu.VMEM)
    smem = pl.BlockSpec(memory_space=pltpu.SMEM)
    hbm = pl.BlockSpec(memory_space=pl.ANY)
    parts, _, piece, cols = gu_every.shape
    shape = lambda w: (size, rows, w)
    return pl.pallas_call(
        functools.partial(middle_kernel, size, lens.shape[1]),
        out_shape=[
            jax.ShapeDtypeStruct((rows, width), F32),
            jax.ShapeDtypeStruct(shape(local), BF),
            jax.ShapeDtypeStruct(shape(width), BF),
            jax.ShapeDtypeStruct(shape(inner), BF),
            jax.ShapeDtypeStruct(shape(cols), BF),
            jax.ShapeDtypeStruct((size, parts, piece, cols), BF),
        ],
        in_specs=[smem, smem, vmem, vmem, vmem, vmem, vmem, hbm, vmem, hbm],
        out_specs=[vmem, vmem, hbm, hbm, hbm, hbm],
        scratch_shapes=scatter_shapes(size, rows, width)
        + [
            pltpu.VMEM((rows, width), F32),
            pltpu.VMEM(shape(width), BF),
            pltpu.SemaphoreType.DMA((transfers(size),)),
            pltpu.SemaphoreType.DMA((transfers(size),)),
            pltpu.VMEM((size, parts, piece, cols), BF),
            pltpu.VMEM(shape(width), BF),
            pltpu.VMEM(shape(inner), BF),
            pltpu.VMEM(shape(cols), BF),
            pltpu.SemaphoreType.DMA((size + 1,)),
            pltpu.SemaphoreType.DMA((3, size)),
        ],
        compiler_params=pltpu.CompilerParams(
            collective_id=ident, has_side_effects=True, vmem_limit_bytes=67_000_000
        ),
        cost_estimate=pl.CostEstimate(
            flops=2 * size * rows * width * (local + 3 * inner),
            bytes_accessed=250_000_000,
            transcendentals=0,
        ),
        name="middle_part",
    )(lens, starts, edge, qkv, out_weight, tokens, gain, gu_every, down_weight, grads)


def heads_back(group, slot, count, lens_ref, starts_ref, own, edge, grad):
    rows, local = own.shape[0], own.shape[1] // 3
    head_of = lane_head(local)
    queries = own[:, :local]
    keys = jnp.concatenate([edge[:, :local], own[:, local : 2 * local]], 0)
    values = jnp.concatenate([edge[:, local:], own[:, 2 * local :]], 0)
    dqs, dks, dvs = [], [], []
    for block in range(rows // BLOCK):
        mask = masks_of(slot, block, lens_ref, starts_ref, group, count)
        low = block * BLOCK
        span = slice(low, low + BLOCK + WINDOW)
        query, grads = queries[low : low + BLOCK], grad[low : low + BLOCK]
        key, value = keys[span], values[span]
        dq = jnp.zeros((BLOCK, local), F32)
        dk = jnp.zeros((BLOCK + WINDOW, local), F32)
        dv = jnp.zeros((BLOCK + WINDOW, local), F32)
        for head in range(local // HEAD_DIM):
            mine = head_of == head
            own_q = jnp.where(mine, query, jnp.zeros_like(query))
            own_g = jnp.where(mine, grads, jnp.zeros_like(grads))
            soft = soft_of(own_q, key, mask)
            grad_soft = dot_trans(own_g, value)
            total = jnp.sum(grad_soft * soft, axis=1, keepdims=True)
            grad_scores = (soft * (grad_soft - total)).astype(BF)
            dq = jnp.where(mine, dot(grad_scores, key), dq)
            dk = dk + dot_rows(grad_scores, own_q)
            dv = dv + dot_rows(soft.astype(BF), own_g)
        dqs.append(dq * SCALE)
        dks.append(dk * SCALE)
        dvs.append(dv)

    def joined(pieces):
        out = [pieces[0][:BLOCK]]
        for left, right in zip(pieces, pieces[1:]):
            out.append(left[BLOCK:] + right[:WINDOW])
            out.append(right[WINDOW:BLOCK])
        out.append(pieces[-1][BLOCK:])
        return jnp.concatenate(out, 0)

    return jnp.concatenate(dqs, 0), joined(dks), joined(dvs)


def back_kernel(size, parts, count, lens_ref, starts_ref, grad_gu_hbm, gu_map_hbm, middle_ref, cot_ref, live_ref,
                gain_ref, out_map_ref, edge_ref, qkv_ref, qkv_map_hbm,
                grad_middle_ref, norm_ref, all_ref, dqkv_ref, own_ref,
                part, first, over, joined, last, s_send, s_recv, t_send, t_recv, g_send, g_recv,
                grad_gu_ref, gu_map_ref, qkv_map_ref, dedge_ref, back_ref, tail_ref, h_send, h_recv, loads):
    rows = middle_ref.shape[0]
    local = out_map_ref.shape[0]
    rank = lax.axis_index("seq")
    slot = rank * rows
    group = Group(size)
    barrier = pltpu.get_barrier_semaphore()
    greet_group(barrier, size)

    def greet(peer):
        pl.semaphore_signal(barrier, inc=1, device_id={"seq": peer}, device_id_type=MESH_ID)

    pl.when(rank > 0)(lambda: greet(rank - 1))
    pl.when(rank < parts - 1)(lambda: greet(rank + 1))
    fetches = [
        pltpu.make_async_copy(src, dst, loads.at[k])
        for k, (src, dst) in enumerate(
            ((grad_gu_hbm, grad_gu_ref), (gu_map_hbm, gu_map_ref), (qkv_map_hbm, qkv_map_ref))
        )
    ]
    for fetch in fetches:
        fetch.start()
    has_next = (2 * parts - 2 - rank) // parts
    has_last = (rank + parts - 1) // parts
    pl.semaphore_wait(barrier, size - 1 + has_next + has_last)
    scatter = Scatter(group, part, first, over, joined, last, s_send, s_recv)
    gather = Gather(group, all_ref, g_send, g_recv)
    fetches[0].wait()
    fetches[1].wait()

    def step_two(step, is_step):
        partial = dot_trans(grad_gu_ref[group.to_own(step)], gu_map_ref[...])
        is_step(size - 1)(lambda: own_ref.__setitem__(..., partial))
        part[step] = partial.astype(BF)
        for k in range(size - 1):
            is_step(k)(functools.partial(scatter.made, k))

    each_step(size, step_two)
    scatter.join()
    half = rows // 2
    norm_sum = jnp.zeros((1, middle_ref.shape[1]), F32)
    for h in range(2):
        span = slice(h * half, (h + 1) * half)
        grad = own_ref[span, :] + scatter.total(h)
        middle = middle_ref[span, :]
        scale = lax.rsqrt(jnp.mean(middle * middle, axis=1, keepdims=True) + EPS)
        unit = middle * scale
        scaled = grad * gain_ref[...]
        norm_sum = norm_sum + jnp.sum(grad * unit, axis=0, keepdims=True)
        grad_out = cot_ref[span, :].astype(F32) * live_ref[span, :]
        grad_middle = grad_out + scale * (
            scaled - unit * jnp.mean(scaled * unit, axis=1, keepdims=True)
        )
        grad_middle_ref[span, :] = grad_middle
        all_ref[group.me, span] = grad_middle.astype(BF)
        gather.start_half(h)
    norm_ref[...] = norm_sum

    def halo(step):
        g = group.from_own(step)
        sems = h_send.at[step], h_recv.at[step]
        return remote(dedge_ref.at[g], back_ref.at[g], *sems, seq=rank - 1)

    def step_heads(step, is_step):
        g = group.from_own(step)

        @is_step(1)
        def _():
            gather.relay()

        for k in range(1, size):
            is_step(k)(functools.partial(gather.ready, k))
        grad = dot_trans(all_ref[g], out_map_ref[...]).astype(BF)
        dq, dk, dv = heads_back(
            g, slot, count, lens_ref, starts_ref, qkv_ref[g], edge_ref[g], grad
        )
        dedge_ref[g] = jnp.concatenate([dk[:WINDOW], dv[:WINDOW]], 1).astype(BF)
        full = jnp.concatenate([dq, dk[WINDOW:], dv[WINDOW:]], 1)
        dqkv_ref[g] = full.astype(BF)
        tail_ref[g] = full[rows - WINDOW :]
        pl.when(rank > 0)(lambda: halo(step).start())

    each_step(size, step_heads)
    scatter.finish()
    fetches[2].wait()

    @pl.when(rank == parts - 1)
    def _():
        back_ref[...] = jnp.zeros_like(back_ref)

    @pl.when(rank < parts - 1)
    def _():
        for step in range(size):
            halo(step).wait_recv()

    scatter = Scatter(group, part, first, over, joined, last, t_send, t_recv)

    def step_one(step, is_step):
        g = group.to_own(step)
        back = back_ref[g].astype(F32)
        wide = jnp.concatenate([jnp.zeros((WINDOW, local), F32), back], 1)
        dqkv_ref[g, pl.ds(rows - WINDOW, WINDOW)] = (tail_ref[g] + wide).astype(BF)
        partial = dot_trans(dqkv_ref[g], qkv_map_ref[...])
        is_step(size - 1)(lambda: own_ref.__setitem__(..., partial))
        part[step] = partial.astype(BF)
        for k in range(size - 1):
            is_step(k)(functools.partial(scatter.made, k))

    each_step(size, step_one)
    scatter.join()
    for h in range(2):
        span = slice(h * half, (h + 1) * half)
        own_ref[span, :] = own_ref[span, :] + scatter.total(h)
    scatter.finish()
    gather.finish()

    @pl.when(rank > 0)
    def _():
        for step in range(size):
            halo(step).wait_send()


def back_part(ident, lens, starts, grad_gu, gu_map, middle, cot, live, gain, out_weight, edge, qkv, qkv_map):
    size, parts = lax.axis_size("fsdp"), lax.axis_size("seq")
    rows, width = middle.shape
    local = out_weight.shape[0]
    vmem = pl.BlockSpec(memory_space=pltpu.VMEM)
    smem = pl.BlockSpec(memory_space=pltpu.SMEM)
    hbm = pl.BlockSpec(memory_space=pl.ANY)
    sems = [pltpu.SemaphoreType.DMA((transfers(size),))] * 2
    return pl.pallas_call(
        functools.partial(back_kernel, size, parts, lens.shape[1]),
        out_shape=[
            jax.ShapeDtypeStruct((rows, width), F32),
            jax.ShapeDtypeStruct((1, width), F32),
            jax.ShapeDtypeStruct((size, rows, width), BF),
            jax.ShapeDtypeStruct(qkv.shape, BF),
            jax.ShapeDtypeStruct((rows, width), F32),
        ],
        in_specs=[smem, smem, hbm, hbm] + [vmem] * 7 + [hbm],
        out_specs=[vmem] * 5,
        scratch_shapes=scatter_shapes(size, rows, width)
        + sems
        + sems
        + [
            pltpu.VMEM(grad_gu.shape, BF),
            pltpu.VMEM(gu_map.shape, BF),
            pltpu.VMEM(qkv_map.shape, BF),
            pltpu.VMEM((size, WINDOW, 2 * local), BF),
            pltpu.VMEM((size, WINDOW, 2 * local), BF),
            pltpu.VMEM((size, WINDOW, 3 * local), F32),
            pltpu.SemaphoreType.DMA((size,)),
            pltpu.SemaphoreType.DMA((size,)),
            pltpu.SemaphoreType.DMA((3,)),
        ],
        compiler_params=pltpu.CompilerParams(
            collective_id=ident, has_side_effects=True, vmem_limit_bytes=67_000_000
        ),
        cost_estimate=pl.CostEstimate(
            flops=2 * size * rows * (gu_map.size + qkv_map.size + width * local),
            bytes_accessed=400_000_000,
            transcendentals=0,
        ),
        name="back_part",
    )(lens, starts, grad_gu, gu_map, middle, cot, live, gain, out_weight, edge, qkv, qkv_map)


def pack_kernel(size, parts, x_ref, g_ref, *refs):
    out_ref = refs[-1]
    full = dot_rows(x_ref[...], g_ref[...])
    pair = out_ref.shape[1]
    rows = full.shape[0] // pair
    piece = rows // parts
    for k in range(pair):
        own = full[k * rows : (k + 1) * rows]
        if len(refs) == 3:
            heads_ref, gb_ref = refs[0], refs[1]
            side = dot_rows(heads_ref[...], gb_ref[...])
            wide = side.shape[1] // pair
            own = jnp.concatenate([own, side[:, k * wide : (k + 1) * wide]], 1)
        out_ref[:, k] = own.astype(BF).reshape(parts, piece, own.shape[1])


def pack_grads(parts, size, x, g, heads=None, gb=None):
    width, cols = x.shape[1], g.shape[1]
    rows = width // size
    piece = rows // parts
    if piece % 8 or (2 * rows) % 128:
        full = dot_rows(x, g).reshape(size, parts, piece, cols)
        if heads is not None:
            side = dot_rows(heads, gb).reshape(parts, piece, size, -1).transpose(2, 0, 1, 3)
            full = jnp.concatenate([full, side], 3)
        return full.transpose(1, 0, 2, 3).astype(BF)
    total = x.shape[0]
    pair = pl.BlockSpec((total, 2 * rows), lambda i: (0, i))
    whole = lambda a: pl.BlockSpec(a.shape, lambda i: (0, 0), pipeline_mode=pl.Buffered(1))
    args, specs = [x, g], [pair, whole(g)]
    out_cols = cols
    if heads is not None:
        args += [heads, gb]
        specs += [whole(heads), pair]
        out_cols += rows
    return pl.pallas_call(
        functools.partial(pack_kernel, size, parts),
        grid=(size // 2,),
        out_shape=jax.ShapeDtypeStruct((parts, size, piece, out_cols), BF),
        in_specs=specs,
        out_specs=pl.BlockSpec((parts, 2, piece, out_cols), lambda i: (0, i, 0, 0)),
        cost_estimate=pl.CostEstimate(
            flops=2 * total * width * out_cols,
            bytes_accessed=2 * (x.size + g.size + width * out_cols),
            transcendentals=0,
        ),
        name="pack_grads",
    )(*args)


def unpack_kernel(widths, every_ref, *outs):
    size = every_ref.shape[1]
    blocks = [every_ref[0, i].astype(F32) for i in range(size)]
    low = 0
    for width, out in zip(widths, outs):
        out[...] = jnp.concatenate([b[:, low : low + width] for b in blocks], 1)
        low += width


def unpack_grads(every, widths):
    parts, size, piece, cols = every.shape
    if piece % 8:
        outs, low = [], 0
        for width in widths:
            block = every[:, :, :, low : low + width].transpose(0, 2, 1, 3)
            outs.append(block.reshape(parts * piece, size * width).astype(F32))
            low += width
        return outs
    return pl.pallas_call(
        functools.partial(unpack_kernel, widths),
        grid=(parts,),
        out_shape=[jax.ShapeDtypeStruct((parts * piece, size * w), F32) for w in widths],
        in_specs=[pl.BlockSpec((1, size, piece, cols), lambda i: (i, 0, 0, 0))],
        out_specs=[pl.BlockSpec((piece, size * w), lambda i: (i, 0)) for w in widths],
        cost_estimate=pl.CostEstimate(flops=0, bytes_accessed=every.size * 6, transcendentals=0),
        name="unpack_grads",
    )(every)


def columns_piece(weights, part, parts):
    size = lax.axis_size("fsdp")
    rows = weights[0].shape[0] // parts
    pieces = []
    for weight in weights:
        own = lax.dynamic_slice_in_dim(weight, part * rows, rows, 0)
        pieces.append(own.reshape(rows, size, -1))
    return jnp.concatenate(pieces, 2).transpose(1, 0, 2)


def shards(
    tokens,
    seq_lengths,
    seq_offsets,
    norm1_gain,
    conv_weight,
    query_weight,
    key_weight,
    value_weight,
    out_weight,
    norm2_gain,
    gate_weight,
    up_weight,
    down_weight,
    cotangent,
):
    size = lax.axis_size("fsdp")
    parts = lax.axis_size("seq")
    part = lax.axis_index("seq")
    me = lax.axis_index("fsdp")
    own_tokens = tokens[0]
    rows, width = own_tokens.shape
    slice_width = norm1_gain.shape[0]
    first_slot = part * rows
    count = seq_lengths.shape[1]

    slot_ext = first_slot - 2 + jnp.arange(rows + 2, dtype=jnp.int32)
    segment_ext = segment_of(
        slot_ext, count, lambda j: seq_lengths[0, j], lambda j: seq_offsets[0, j]
    )
    segment_own = segment_ext[2:]
    same_one = (segment_own == segment_ext[1:-1]).astype(F32)[:, None]
    same_two = (segment_own == segment_ext[:-2]).astype(F32)[:, None]
    live_mask = (segment_own >= 0).astype(F32)[:, None]

    gains = jnp.concatenate(
        [
            norm1_gain[None],
            norm2_gain[None],
            conv_weight.T,
            jnp.zeros((3, slice_width), BF),
        ],
        0,
    )
    table = jnp.zeros((8, 128), jnp.int32)
    table = table.at[0, :count].set(seq_lengths[0]).at[1, :count].set(seq_offsets[0])
    qkv_piece = columns_piece((query_weight, key_weight, value_weight), part, parts)
    gu_piece = columns_piece((gate_weight, up_weight), part, parts)
    gains_all, table_all, qkv_slots, gu_slots = exchange(
        0, gathered=(gains, table), traded=(qkv_piece, gu_piece)
    )
    gains_all = with_own(gains_all, gains).transpose(1, 0, 2).reshape(8, width)
    table_all = with_own(table_all, table)
    lens_all, starts_all = table_all[:, 0, :count], table_all[:, 1, :count]
    qkv_slots = with_own(qkv_slots, lax.dynamic_index_in_dim(qkv_piece, me, 0, keepdims=False))
    gu_slots = with_own(gu_slots, lax.dynamic_index_in_dim(gu_piece, me, 0, keepdims=False))
    grad_out = cotangent[0].astype(F32) * live_mask
    grad_down_all = lax.all_gather(grad_out.astype(BF), "fsdp", axis=0, tiled=True)
    norm_one = gains_all[0].astype(F32)
    norm_two = gains_all[1].astype(F32)
    taps = gains_all[2:5].astype(F32)

    edge_tokens = shifted(own_tokens[rows - 2 :], "seq", 1)
    extended = jnp.concatenate([edge_tokens, own_tokens], 0).astype(F32)
    scale_one = lax.rsqrt(jnp.mean(extended * extended, axis=1, keepdims=True) + EPS)
    normed = extended * scale_one * norm_one
    conv_mix = (
        normed[2:] * taps[0]
        + same_one * normed[1:-1] * taps[1]
        + same_two * normed[:-2] * taps[2]
    )
    gated = (conv_mix * normed[2:]).astype(BF)
    gated_all, qkv, edge, qkv_map = open_mixer(1, gated, qkv_slots)
    gu_slots, qkv = lax.optimization_barrier((gu_slots, qkv))
    gu_every = lax.all_gather(gu_slots, "seq", axis=0)
    qkv_map = qkv_map.reshape(width, -1)
    local = out_weight.shape[0]
    middle, heads_out, normed_all, hidden, grad_gu, gu_map = middle_part(
        2,
        lens_all,
        starts_all,
        edge,
        qkv,
        out_weight,
        own_tokens,
        norm_two[None],
        gu_every,
        down_weight,
        grad_down_all.reshape(size, rows, width),
    )
    flat = lambda a: a.reshape(-1, a.shape[-1])
    gu_map = gu_map.reshape(width, -1)
    hidden = flat(hidden)

    gu_packed = pack_grads(parts, size, flat(normed_all), flat(grad_gu))
    gu_packed, grad_gu = lax.optimization_barrier((gu_packed, grad_gu))
    gu_piece = lax.psum_scatter(gu_packed, "seq", scatter_dimension=0)
    down_sum = dot_rows(hidden, grad_down_all).astype(BF)
    grad_gu, down_sum = lax.optimization_barrier((grad_gu, down_sum))
    down_total = lax.psum(down_sum, "seq").astype(F32)
    grad_middle, norm2_term, grad_branch_all, dqkv, grad_gated = back_part(
        4,
        lens_all,
        starts_all,
        grad_gu,
        gu_map,
        middle,
        cotangent[0],
        live_mask,
        norm_two[None],
        out_weight,
        edge,
        qkv,
        qkv_map,
    )
    norm2_term = norm2_term[0]
    grad_branch_all, gu_piece = lax.optimization_barrier((grad_branch_all, gu_piece))
    (gu_slots,) = exchange(5, traded=(gu_piece,))
    gu_slots = with_own(gu_slots, lax.dynamic_index_in_dim(gu_piece, me, 0, keepdims=False))
    gu_every = lax.all_gather(gu_slots, "seq", axis=0)
    grad_branch_all, gu_slots = lax.optimization_barrier((grad_branch_all, gu_slots))
    qkvo_packed = pack_grads(
        parts, size, flat(gated_all), flat(dqkv), flat(heads_out), flat(grad_branch_all)
    )
    hidden, grad_gated = lax.optimization_barrier((hidden, grad_gated))
    feed = sum_tokens(9, dot(hidden, down_weight).reshape(size, rows, width))
    qkvo_packed, gu_every, down_total, feed = lax.optimization_barrier(
        (qkvo_packed, gu_every, down_total, feed)
    )
    qkvo_piece = lax.psum_scatter(qkvo_packed, "seq", scatter_dimension=0)
    (qkvo_slots,) = exchange(8, traded=(qkvo_piece,))
    qkvo_slots = with_own(
        qkvo_slots, lax.dynamic_index_in_dim(qkvo_piece, me, 0, keepdims=False)
    )
    qkvo_slots = jnp.concatenate([qkvo_slots[..., : 3 * local], qkvo_piece[..., 3 * local :]], -1)
    qkvo_every = lax.all_gather(qkvo_slots, "seq", axis=0)
    gate_total, up_total = unpack_grads(gu_every, (gu_map.shape[1] // 2,) * 2)
    query_total, key_total, value_total, out_total = unpack_grads(qkvo_every, (local,) * 4)

    normed_own = normed[2:]
    grad_mix = grad_gated * normed_own
    part_zero = jnp.pad(grad_gated * conv_mix + grad_mix * taps[0], ((2, 0), (0, 0)))
    part_one = jnp.pad(grad_mix * same_one * taps[1], ((1, 1), (0, 0)))
    part_two = jnp.pad(grad_mix * same_two * taps[2], ((0, 2), (0, 0)))
    grad_normed = part_zero + part_one + part_two
    unit_one = extended * scale_one
    grad_unit_one = grad_normed * norm_one
    grad_extended = scale_one * (
        grad_unit_one - unit_one * jnp.mean(grad_unit_one * unit_one, axis=1, keepdims=True)
    )
    edge_back = shifted(grad_extended[:2], "seq", -1)
    tokens_grad = grad_middle + grad_extended[2:] + jnp.pad(edge_back, ((rows - 2, 0), (0, 0)))

    terms = jnp.stack(
        [
            jnp.sum(grad_normed * unit_one, axis=0),
            norm2_term,
            jnp.sum(grad_mix * normed_own, axis=0),
            jnp.sum(grad_mix * same_one * normed[1:-1], axis=0),
            jnp.sum(grad_mix * same_two * normed[:-2], axis=0),
        ]
    )
    terms = lax.psum(terms, ("seq", "fsdp"))
    terms = lax.dynamic_slice_in_dim(terms, me * slice_width, slice_width, 1)

    layer_out = (live_mask * (middle + feed)).astype(BF)[None]
    return (
        layer_out,
        tokens_grad[None],
        terms[0],
        terms[2:5].T,
        query_total,
        key_total,
        value_total,
        out_total,
        terms[1],
        gate_total,
        up_total,
        down_total,
    )


def solution(mesh):
    placed = (
        P("fsdp", "seq", None),
        P("fsdp", None),
        P("fsdp", None),
        P("fsdp"),
        P("fsdp", None),
        P("fsdp", None),
        P("fsdp", None),
        P("fsdp", None),
        P("fsdp", None),
        P("fsdp"),
        P("fsdp", None),
        P("fsdp", None),
        P("fsdp", None),
        P("fsdp", "seq", None),
    )
    return jax.shard_map(
        shards,
        mesh=mesh,
        in_specs=placed,
        out_specs=(
            P("fsdp", "seq", None),
            P("fsdp", "seq", None),
            P("fsdp"),
            P("fsdp", None),
            P("fsdp", None),
            P("fsdp", None),
            P("fsdp", None),
            P("fsdp", None),
            P("fsdp"),
            P("fsdp", None),
            P("fsdp", None),
            P("fsdp", None),
        ),
        check_vma=False,
    )
```

```python
import functools

import jax
import jax.numpy as jnp
from jax import lax
from jax.experimental import pallas as pl
from jax.experimental.pallas import tpu as pltpu
from jax.sharding import PartitionSpec as P

HEADS = 16
WINDOW = 64
HEAD_DIM = 112
BLOCK = 128

EPS = 1e-05
NEG = -1e30
SCALE = HEAD_DIM ** (-0.5)
MESH_ID = pl.DeviceIdType.MESH
BF = jnp.bfloat16
F32 = jnp.float32


def shifted(array, axis, by):
    length = lax.axis_size(axis)
    pairs = [(i, i + by) for i in range(length) if 0 <= i + by < length]
    return lax.ppermute(array, axis, pairs)


def segment_of(slot, count, lengths, starts):
    found = jnp.full(slot.shape, -1, jnp.int32)
    for j in range(count):
        inside = (slot >= starts(j)) & (slot < starts(j) + lengths(j))
        found = jnp.where(inside, j, found)
    return jnp.where(slot < 0, -2, found)


def dot_rows(left, right):
    return lax.dot_general(left, right, (((0,), (0,)), ((), ())), preferred_element_type=F32)


def dot_trans(left, right):
    return lax.dot_general(left, right, (((1,), (1,)), ((), ())), preferred_element_type=F32)


def dot(left, right):
    return jnp.dot(left, right, preferred_element_type=F32)


def exchange_kernel(size, modes, *refs):
    count = len(modes)
    ins, outs = refs[:count], refs[count : 2 * count]
    send, recv = refs[2 * count :]
    me = lax.axis_index("fsdp")
    barrier = pltpu.get_barrier_semaphore()
    for step in range(1, size):
        peer = lax.rem(me + step, size)
        pl.semaphore_signal(barrier, inc=1, device_id={"fsdp": peer}, device_id_type=MESH_ID)
    pl.semaphore_wait(barrier, size - 1)
    copies = []
    for k, mode in enumerate(modes):
        for step in range(1, size):
            peer = lax.rem(me + step, size)
            copies.append(
                pltpu.make_async_remote_copy(
                    src_ref=ins[k] if mode == "ag" else ins[k].at[peer],
                    dst_ref=outs[k].at[me],
                    send_sem=send.at[k, step - 1],
                    recv_sem=recv.at[k, step - 1],
                    device_id={"fsdp": peer},
                    device_id_type=MESH_ID,
                )
            )
    for copy in copies:
        copy.start()
    for copy in copies:
        copy.wait()


def exchange(ident, gathered=(), traded=()):
    size = lax.axis_size("fsdp")
    arrays = tuple(gathered) + tuple(traded)
    modes = ("ag",) * len(gathered) + ("a2a",) * len(traded)
    shapes = [(size,) + a.shape for a in gathered] + [a.shape for a in traded]
    sent = sum((size - 1) * a.size * a.dtype.itemsize for a in gathered)
    sent += sum((size - 1) * a.size * a.dtype.itemsize // size for a in traded)
    outs = pl.pallas_call(
        functools.partial(exchange_kernel, size, modes),
        out_shape=[jax.ShapeDtypeStruct(s, a.dtype) for s, a in zip(shapes, arrays)],
        in_specs=[pl.BlockSpec(memory_space=pl.ANY)] * len(arrays),
        out_specs=[pl.BlockSpec(memory_space=pl.ANY)] * len(arrays),
        scratch_shapes=[
            pltpu.SemaphoreType.DMA((len(arrays), size - 1)),
            pltpu.SemaphoreType.DMA((len(arrays), size - 1)),
        ],
        compiler_params=pltpu.CompilerParams(collective_id=ident, has_side_effects=True),
        cost_estimate=pl.CostEstimate(flops=0, bytes_accessed=sent * 50, transcendentals=0),
        name=f"exchange{ident}",
    )(*arrays)
    return outs


def with_own(slots, own):
    return lax.dynamic_update_index_in_dim(slots, own, lax.axis_index("fsdp"), 0)


def gather_tokens(ident, rows):
    (slots,) = exchange(ident, gathered=(rows,))
    slots = with_own(slots, rows)
    return slots.reshape((-1,) + rows.shape[1:])


def sum_tokens(ident, partial):
    (slots,) = exchange(ident, traded=(partial.astype(BF),))
    me = lax.axis_index("fsdp")
    mine = lax.dynamic_index_in_dim(partial, me, 0, keepdims=False)
    total = mine
    for i in range(slots.shape[0]):
        total = total + jnp.where(me == i, 0.0, slots[i].astype(F32))
    return total


def masks_of(first, block, lens_ref, starts_ref, group, count):
    rows = first + block * BLOCK
    query = rows + lax.broadcasted_iota(jnp.int32, (BLOCK, 1), 0)
    keys = rows - WINDOW + lax.broadcasted_iota(jnp.int32, (1, BLOCK + WINDOW), 1)
    length = lambda j: lens_ref[group, j]
    start = lambda j: starts_ref[group, j]
    seg_q = segment_of(query, count, length, start)
    seg_k = segment_of(keys, count, length, start)
    far = query - keys
    return (far >= 0) & (far <= WINDOW) & (seg_q == seg_k)


def soft_of(query, keys, mask):
    scores = dot_trans(query, keys) * SCALE
    scores = jnp.where(mask, scores, NEG)
    peak = jnp.max(scores, axis=1, keepdims=True)
    exponent = jnp.exp(scores - peak)
    return exponent / jnp.sum(exponent, axis=1, keepdims=True)


def lane_head(width):
    return lax.broadcasted_iota(jnp.int32, (1, width), 1) // HEAD_DIM


def remote(src, dst, send, recv, **peer):
    return pltpu.make_async_remote_copy(
        src_ref=src,
        dst_ref=dst,
        send_sem=send,
        recv_sem=recv,
        device_id=peer,
        device_id_type=MESH_ID,
    )


def greet_group(barrier, size):
    me = lax.axis_index("fsdp")
    for step in range(1, size):
        peer = lax.rem(me + step, size)
        pl.semaphore_signal(barrier, inc=1, device_id={"fsdp": peer}, device_id_type=MESH_ID)


class Group:
    def __init__(self, size):
        self.size = size
        self.me = lax.axis_index("fsdp")
        self.square = size == 4
        if self.square:
            x, y = lax.rem(self.me, 2), self.me // 2
            self.at = lambda bx, by: lax.rem(y + by, 2) * 2 + lax.rem(x + bx, 2)
            self.x, self.y, self.far = self.at(1, 0), self.at(0, 1), self.at(1, 1)

    def from_own(self, step):
        if self.square:
            return self.at(lax.rem(step, 2), step // 2)
        return lax.rem(self.me - step + self.size, self.size)

    def to_own(self, step):
        if self.square:
            return self.at(1 - step // 2, 1 - lax.rem(step, 2))
        return lax.rem(self.me + 1 + step, self.size)


class Gather:
    def __init__(self, group, ref, send, recv):
        self.group, self.ref, self.send, self.recv = group, ref, send, recv
        self.half = ref.shape[1] // 2

    def part(self, k, slot, half, peer):
        view = self.ref.at[slot, pl.ds(half * self.half, self.half)]
        return remote(view, view, self.send.at[k], self.recv.at[k], fsdp=peer)

    def whole(self, k):
        g = self.group
        view = self.ref.at[g.me]
        sems = self.send.at[k - 1], self.recv.at[k - 1]
        return remote(view, view, *sems, fsdp=lax.rem(g.me + k, g.size))

    def copy(self, k):
        g = self.group
        if not g.square:
            return self.whole(k + 1)
        slot = (g.me, g.me, g.me, g.me, g.x, g.y)[k]
        half = (0, 1, 0, 1, 0, 1)[k]
        return self.part(k, slot, half, (g.x, g.x, g.y, g.y, g.y, g.x)[k])

    def start_half(self, half):
        if self.group.square:
            self.copy(half).start()
            self.copy(2 + half).start()
        elif half == 1:
            for k in range(self.group.size - 1):
                self.copy(k).start()

    def relay(self):
        if self.group.square:
            self.copy(0).wait_recv()
            self.copy(4).start()
            self.copy(3).wait_recv()
            self.copy(5).start()

    def ready(self, step):
        if not self.group.square:
            self.copy(step - 1).wait_recv()
        elif step == 3:
            self.copy(4).wait_recv()
            self.copy(5).wait_recv()
        else:
            self.copy(step).wait_recv()

    def finish(self):
        for k in range(transfers(self.group.size)):
            self.copy(k).wait_send()


class Scatter:
    def __init__(self, group, part, first, over, joined, last, send, recv):
        self.group, self.part = group, part
        self.first, self.over, self.joined, self.last = first, over, joined, last
        self.send, self.recv = send, recv
        self.half = part.shape[1] // 2

    def copy(self, k):
        g, half = self.group, self.half
        low, high = pl.ds(0, half), pl.ds(half, half)
        if not g.square:
            src, dst, peer = self.part.at[k], self.first.at[k], lax.rem(g.me + 1 + k, g.size)
        else:
            src, dst, peer = (
                lambda: (self.part.at[0, low], self.over.at[0], g.x),
                lambda: (self.part.at[0, high], self.over.at[1], g.y),
                lambda: (self.part.at[1, low], self.first.at[0], g.x),
                lambda: (self.part.at[2, high], self.first.at[1], g.y),
                lambda: (self.joined.at[0], self.last.at[0], g.y),
                lambda: (self.joined.at[1], self.last.at[1], g.x),
            )[k]()
        return remote(src, dst, self.send.at[k], self.recv.at[k], fsdp=peer)

    def made(self, step):
        if not self.group.square:
            self.copy(step).start()
        elif step == 0:
            self.copy(0).start()
            self.copy(1).start()
        elif step in (1, 2):
            self.copy(step + 1).start()

    def join(self):
        if not self.group.square:
            return
        half = self.half
        for k, (step, rows) in enumerate(((2, slice(0, half)), (1, slice(half, 2 * half)))):
            self.copy(k).wait_recv()
            own = self.part[step, rows].astype(F32)
            self.joined[k] = (own + self.over[k].astype(F32)).astype(BF)
            self.copy(4 + k).start()

    def total(self, half):
        count = self.half
        if self.group.square:
            self.copy(2 + half).wait_recv()
            self.copy(4 + half).wait_recv()
            return self.first[half].astype(F32) + self.last[half].astype(F32)
        if half == 0:
            for k in range(self.group.size - 1):
                self.copy(k).wait_recv()
        rows = slice(half * count, (half + 1) * count)
        out = self.first[0, rows].astype(F32)
        for k in range(1, self.group.size - 1):
            out = out + self.first[k, rows].astype(F32)
        return out

    def finish(self):
        for k in range(transfers(self.group.size)):
            self.copy(k).wait_send()


class Line:
    def __init__(self, parts, sems):
        self.rank = lax.axis_index("seq")
        self.parts, self.length = parts, parts // 2
        self.z, self.core = self.rank // 2, lax.rem(self.rank, 2)
        self.above, self.below = self.rank + 2, self.rank - 2
        self.beside = self.rank + 1 - 2 * self.core
        self.has_above, self.has_below = self.z < self.length - 1, self.z > 0
        self.sems = sems

    def greet(self, barrier):
        def one(peer):
            pl.semaphore_signal(barrier, inc=1, device_id={"seq": peer}, device_id_type=MESH_ID)

        one(self.beside)
        pl.when(self.has_above)(lambda: one(self.above))
        pl.when(self.has_below)(lambda: one(self.below))
        n, z = self.length, self.z
        return 1 + (2 * n - 2 - z) // n + (z + n - 1) // n

    def up(self, k, owner):
        view = self.view(owner)
        return remote(view, view, self.sems[0].at[k], self.sems[1].at[k], seq=self.above)

    def down(self, k, owner):
        view = self.view(owner)
        return remote(view, view, self.sems[2].at[k], self.sems[3].at[k], seq=self.below)

    def side(self, k, owner):
        view = self.view(owner)
        return remote(view, view, self.sems[4].at[k], self.sems[5].at[k], seq=self.beside)

    def gather(self, view):
        self.view = view
        pl.when(self.has_above)(lambda: self.up(0, self.rank).start())
        pl.when(self.has_below)(lambda: self.down(0, self.rank).start())
        self.side(self.z, self.rank).start()

    def hop(self, j):
        rank, z = self.rank, self.z

        @pl.when(z >= j)
        def _():
            self.up(j - 1, rank).wait_recv()
            pl.when(self.has_above)(lambda: self.up(j, rank - 2 * j).start())
            self.side(z - j, rank - 2 * j).start()

        @pl.when(z + j < self.length)
        def _():
            self.down(j - 1, rank).wait_recv()
            pl.when(self.has_below)(lambda: self.down(j, rank + 2 * j).start())
            self.side(z + j, rank + 2 * j).start()

    def gathered(self):
        for k in range(self.length):
            self.side(k, self.rank).wait_recv()

    def finish(self):
        rank, z = self.rank, self.z
        for k in range(self.length):
            self.side(k, rank).wait_send()
        pl.when(self.has_above)(lambda: self.up(0, rank).wait_send())
        pl.when(self.has_below)(lambda: self.down(0, rank).wait_send())
        for j in range(1, self.length):
            pl.when((z >= j) & self.has_above)(lambda: self.up(j, rank).wait_send())
            pl.when((z + j < self.length) & self.has_below)(lambda: self.down(j, rank).wait_send())


def line_sems(parts):
    return [pltpu.SemaphoreType.DMA((parts // 2,))] * 6


def transfers(size):
    return 6 if size == 4 else size - 1


def scatter_shapes(size, rows, width):
    half = rows // 2
    slots = (2, half, width) if size == 4 else (size - 1, rows, width)
    return [
        pltpu.VMEM((size, rows, width), BF),
        pltpu.VMEM(slots, BF),
        pltpu.VMEM((2, half, width), BF),
        pltpu.VMEM((2, half, width), BF),
        pltpu.VMEM((2, half, width), BF),
        pltpu.SemaphoreType.DMA((transfers(size),)),
        pltpu.SemaphoreType.DMA((transfers(size),)),
    ]


def each_step(size, body):
    def one(step, carry):
        body(step, lambda k: pl.when(step == k))
        return carry

    lax.fori_loop(0, size, one, 0)


def open_kernel(size, parts, gated_ref, piece_ref, all_ref, qkv_ref, edge_ref, map_ref, tail_ref,
                load, send, recv, halo_send, halo_recv, *sems):
    rank = lax.axis_index("seq")
    rows = gated_ref.shape[0]
    local = qkv_ref.shape[2] // 3
    group, line = Group(size), Line(parts, sems)
    barrier = pltpu.get_barrier_semaphore()
    greet_group(barrier, size)
    known = line.greet(barrier)

    def greet(peer):
        pl.semaphore_signal(barrier, inc=1, device_id={"seq": peer}, device_id_type=MESH_ID)

    pl.when(line.has_above & (line.core == 1))(lambda: greet(rank + 1))
    pl.when(line.has_below & (line.core == 0))(lambda: greet(rank - 1))
    n, z = line.length, line.z
    known = known + (2 * n - 2 - z) // n * line.core + (z + n - 1) // n * (1 - line.core)
    own = pltpu.make_async_copy(piece_ref, map_ref.at[:, rank], load)
    own.start()
    all_ref[group.me] = gated_ref[...]
    pl.semaphore_wait(barrier, size - 1 + known)

    gather = Gather(group, all_ref, send, recv)
    gather.start_half(0)
    gather.start_half(1)
    own.wait()
    line.gather(lambda owner: map_ref.at[:, owner])
    gather.relay()
    for j in range(1, line.length):
        line.hop(j)
    for step in range(1, size):
        gather.ready(step)
    line.gathered()

    weights = map_ref[...].reshape(-1, map_ref.shape[3])

    def halo():
        return remote(tail_ref, edge_ref, halo_send, halo_recv, seq=rank + 1)

    def one(g, carry):
        out = dot(all_ref[g], weights).astype(BF)
        qkv_ref[g] = out
        tail_ref[g] = out[rows - WINDOW :, local:]
        return carry

    lax.fori_loop(0, size, one, 0)
    pl.when(rank < parts - 1)(lambda: halo().start())

    @pl.when(rank == 0)
    def _():
        edge_ref[...] = jnp.zeros_like(edge_ref)

    gather.finish()
    line.finish()
    pl.when(rank > 0)(lambda: halo().wait_recv())
    pl.when(rank < parts - 1)(lambda: halo().wait_send())


def open_mixer(ident, gated, piece):
    size, parts = lax.axis_size("fsdp"), lax.axis_size("seq")
    rows, width = gated.shape
    cols = piece.shape[2]
    sems = lambda n: [pltpu.SemaphoreType.DMA((n,))] * 2
    vmem = pl.BlockSpec(memory_space=pltpu.VMEM)
    return pl.pallas_call(
        functools.partial(open_kernel, size, parts),
        out_shape=[
            jax.ShapeDtypeStruct((size, rows, width), BF),
            jax.ShapeDtypeStruct((size, rows, cols), BF),
            jax.ShapeDtypeStruct((size, WINDOW, cols // 3 * 2), BF),
            jax.ShapeDtypeStruct((size, parts) + piece.shape[1:], BF),
        ],
        in_specs=[vmem, pl.BlockSpec(memory_space=pl.ANY)],
        out_specs=[vmem] * 4,
        scratch_shapes=[
            pltpu.VMEM((size, WINDOW, cols // 3 * 2), BF),
            pltpu.SemaphoreType.DMA,
        ]
        + sems(transfers(size))
        + [pltpu.SemaphoreType.DMA, pltpu.SemaphoreType.DMA]
        + line_sems(parts),
        compiler_params=pltpu.CompilerParams(collective_id=ident, has_side_effects=True),
        cost_estimate=pl.CostEstimate(
            flops=2 * size * rows * width * cols, bytes_accessed=150_000_000, transcendentals=0
        ),
        name="open_mixer",
    )(gated, piece)


def middle_kernel(size, parts, count, lens_ref, starts_ref, edge_ref, qkv_ref, out_map_ref, tokens_ref,
                  gain_ref, gu_hbm, down_ref, grads_hbm, middle_ref, heads_ref, all_hbm, hidden_hbm, gu_grad_hbm, gu_out,
                  part, first, over, joined, last, s_send, s_recv, own_ref, all_ref, g_send, g_recv,
                  gu_ref, grads_ref, hidden_ref, gu_grad_ref, loads, stores, *sems):
    rows = tokens_ref.shape[0]
    local = heads_ref.shape[2]
    inner = down_ref.shape[0]
    slot = lax.axis_index("seq") * rows
    group = Group(size)
    barrier = pltpu.get_barrier_semaphore()
    greet_group(barrier, size)
    line = Line(parts, sems)
    known = line.greet(barrier)
    fetches = [
        pltpu.make_async_copy(gu_hbm, gu_ref.at[:, line.rank], loads.at[0]),
        pltpu.make_async_copy(grads_hbm, grads_ref, loads.at[1]),
    ]
    for fetch in fetches:
        fetch.start()
    pl.semaphore_wait(barrier, size - 1 + known)
    fetches[0].wait()
    line.gather(lambda owner: gu_ref.at[:, owner])
    scatter = Scatter(group, part, first, over, joined, last, s_send, s_recv)
    gather = Gather(group, all_ref, g_send, g_recv)
    head_of = lane_head(local)

    def mix(step, is_step):
        g = group.to_own(step)
        own = qkv_ref[g]
        edge = edge_ref[g]
        queries = own[:, :local]
        keys = jnp.concatenate([edge[:, :local], own[:, local : 2 * local]], 0)
        values = jnp.concatenate([edge[:, local:], own[:, 2 * local :]], 0)
        outs = []
        for block in range(rows // BLOCK):
            mask = masks_of(slot, block, lens_ref, starts_ref, g, count)
            low = block * BLOCK
            query = queries[low : low + BLOCK]
            key = keys[low : low + BLOCK + WINDOW]
            value = values[low : low + BLOCK + WINDOW]
            out = jnp.zeros((BLOCK, local), F32)
            for head in range(local // HEAD_DIM):
                mine = head_of == head
                soft = soft_of(jnp.where(mine, query, jnp.zeros_like(query)), key, mask)
                out = jnp.where(mine, dot(soft.astype(BF), value), out)
            outs.append(out.astype(BF))
        heads = jnp.concatenate(outs, 0)
        heads_ref[g] = heads
        branch = dot(heads, out_map_ref[...])
        is_step(size - 1)(lambda: own_ref.__setitem__(..., branch))
        part[step] = branch.astype(BF)
        for k in range(size - 1):
            is_step(k)(functools.partial(scatter.made, k))

    each_step(size, mix)
    scatter.join()
    line.hop(1)
    half = rows // 2
    for h in range(2):
        span = slice(h * half, (h + 1) * half)
        total = own_ref[span, :] + scatter.total(h)
        middle = tokens_ref[span, :].astype(F32) + total
        middle_ref[span, :] = middle
        scale = lax.rsqrt(jnp.mean(middle * middle, axis=1, keepdims=True) + EPS)
        all_ref[group.me, span] = (middle * scale * gain_ref[...]).astype(BF)
        gather.start_half(h)
    fetches[1].wait()
    gather.relay()
    for j in range(2, line.length):
        line.hop(j)
    line.gathered()
    keep = pltpu.make_async_copy(gu_ref, gu_out, loads.at[0])
    keep.start()

    def out_copies(g):
        return [
            pltpu.make_async_copy(src.at[g], dst.at[g], stores.at[k, g])
            for k, (src, dst) in enumerate(
                ((all_ref, all_hbm), (hidden_ref, hidden_hbm), (gu_grad_ref, gu_grad_hbm))
            )
        ]

    def feed(step, is_step):
        g = group.from_own(step)
        for k in range(1, size):
            is_step(k)(functools.partial(gather.ready, k))
        weights = gu_ref[...].reshape(-1, gu_ref.shape[3])
        acts = dot(all_ref[g], weights)
        gate, up = acts[:, :inner], acts[:, inner:]
        sigma = jax.nn.sigmoid(gate)
        silu = gate * sigma
        hidden_ref[g] = (silu * up).astype(BF)
        grad_hidden = dot_trans(grads_ref[g], down_ref[...])
        grad_gate = grad_hidden * up * sigma * (1.0 + gate * (1.0 - sigma))
        gu_grad_ref[g] = jnp.concatenate([grad_gate, grad_hidden * silu], 1).astype(BF)
        for copy in out_copies(g):
            copy.start()

    each_step(size, feed)
    scatter.finish()
    gather.finish()
    line.finish()
    keep.wait()
    for g in range(size):
        for copy in out_copies(g):
            copy.wait()


def middle_part(ident, lens, starts, edge, qkv, out_weight, tokens, gain, gu_piece, down_weight, grads):
    size, parts = lax.axis_size("fsdp"), lax.axis_size("seq")
    rows, width = tokens.shape
    local, inner = out_weight.shape[0], down_weight.shape[0]
    vmem = pl.BlockSpec(memory_space=pltpu.VMEM)
    smem = pl.BlockSpec(memory_space=pltpu.SMEM)
    hbm = pl.BlockSpec(memory_space=pl.ANY)
    _, piece, cols = gu_piece.shape
    shape = lambda w: (size, rows, w)
    return pl.pallas_call(
        functools.partial(middle_kernel, size, parts, lens.shape[1]),
        out_shape=[
            jax.ShapeDtypeStruct((rows, width), F32),
            jax.ShapeDtypeStruct(shape(local), BF),
            jax.ShapeDtypeStruct(shape(width), BF),
            jax.ShapeDtypeStruct(shape(inner), BF),
            jax.ShapeDtypeStruct(shape(cols), BF),
            jax.ShapeDtypeStruct((size, parts, piece, cols), BF),
        ],
        in_specs=[smem, smem, vmem, vmem, vmem, vmem, vmem, hbm, vmem, hbm],
        out_specs=[vmem, vmem, hbm, hbm, hbm, hbm],
        scratch_shapes=scatter_shapes(size, rows, width)
        + [
            pltpu.VMEM((rows, width), F32),
            pltpu.VMEM(shape(width), BF),
            pltpu.SemaphoreType.DMA((transfers(size),)),
            pltpu.SemaphoreType.DMA((transfers(size),)),
            pltpu.VMEM((size, parts, piece, cols), BF),
            pltpu.VMEM(shape(width), BF),
            pltpu.VMEM(shape(inner), BF),
            pltpu.VMEM(shape(cols), BF),
            pltpu.SemaphoreType.DMA((2,)),
            pltpu.SemaphoreType.DMA((3, size)),
        ]
        + line_sems(parts),
        compiler_params=pltpu.CompilerParams(
            collective_id=ident, has_side_effects=True, vmem_limit_bytes=67_000_000
        ),
        cost_estimate=pl.CostEstimate(
            flops=2 * size * rows * width * (local + 3 * inner),
            bytes_accessed=250_000_000,
            transcendentals=0,
        ),
        name="middle_part",
    )(lens, starts, edge, qkv, out_weight, tokens, gain, gu_piece, down_weight, grads)


def heads_back(group, slot, count, lens_ref, starts_ref, own, edge, grad):
    rows, local = own.shape[0], own.shape[1] // 3
    head_of = lane_head(local)
    queries = own[:, :local]
    keys = jnp.concatenate([edge[:, :local], own[:, local : 2 * local]], 0)
    values = jnp.concatenate([edge[:, local:], own[:, 2 * local :]], 0)
    dqs, dks, dvs = [], [], []
    for block in range(rows // BLOCK):
        mask = masks_of(slot, block, lens_ref, starts_ref, group, count)
        low = block * BLOCK
        span = slice(low, low + BLOCK + WINDOW)
        query, grads = queries[low : low + BLOCK], grad[low : low + BLOCK]
        key, value = keys[span], values[span]
        dq = jnp.zeros((BLOCK, local), F32)
        dk = jnp.zeros((BLOCK + WINDOW, local), F32)
        dv = jnp.zeros((BLOCK + WINDOW, local), F32)
        for head in range(local // HEAD_DIM):
            mine = head_of == head
            own_q = jnp.where(mine, query, jnp.zeros_like(query))
            own_g = jnp.where(mine, grads, jnp.zeros_like(grads))
            soft = soft_of(own_q, key, mask)
            grad_soft = dot_trans(own_g, value)
            total = jnp.sum(grad_soft * soft, axis=1, keepdims=True)
            grad_scores = (soft * (grad_soft - total)).astype(BF)
            dq = jnp.where(mine, dot(grad_scores, key), dq)
            dk = dk + dot_rows(grad_scores, own_q)
            dv = dv + dot_rows(soft.astype(BF), own_g)
        dqs.append(dq * SCALE)
        dks.append(dk * SCALE)
        dvs.append(dv)

    def joined(pieces):
        out = [pieces[0][:BLOCK]]
        for left, right in zip(pieces, pieces[1:]):
            out.append(left[BLOCK:] + right[:WINDOW])
            out.append(right[WINDOW:BLOCK])
        out.append(pieces[-1][BLOCK:])
        return jnp.concatenate(out, 0)

    return jnp.concatenate(dqs, 0), joined(dks), joined(dvs)


def back_kernel(size, parts, count, lens_ref, starts_ref, grad_gu_hbm, gu_map_hbm, middle_ref, cot_ref, live_ref,
                gain_ref, out_map_ref, edge_ref, qkv_ref, qkv_map_hbm,
                grad_middle_ref, norm_ref, all_ref, dqkv_ref, own_ref,
                part, first, over, joined, last, s_send, s_recv, t_send, t_recv, g_send, g_recv,
                grad_gu_ref, gu_map_ref, qkv_map_ref, dedge_ref, back_ref, tail_ref, h_send, h_recv, loads):
    rows = middle_ref.shape[0]
    local = out_map_ref.shape[0]
    rank = lax.axis_index("seq")
    slot = rank * rows
    group = Group(size)
    barrier = pltpu.get_barrier_semaphore()
    greet_group(barrier, size)

    def greet(peer):
        pl.semaphore_signal(barrier, inc=1, device_id={"seq": peer}, device_id_type=MESH_ID)

    pl.when(rank > 0)(lambda: greet(rank - 1))
    pl.when(rank < parts - 1)(lambda: greet(rank + 1))
    fetches = [
        pltpu.make_async_copy(src, dst, loads.at[k])
        for k, (src, dst) in enumerate(
            ((grad_gu_hbm, grad_gu_ref), (gu_map_hbm, gu_map_ref), (qkv_map_hbm, qkv_map_ref))
        )
    ]
    for fetch in fetches:
        fetch.start()
    has_next = (2 * parts - 2 - rank) // parts
    has_last = (rank + parts - 1) // parts
    pl.semaphore_wait(barrier, size - 1 + has_next + has_last)
    scatter = Scatter(group, part, first, over, joined, last, s_send, s_recv)
    gather = Gather(group, all_ref, g_send, g_recv)
    fetches[0].wait()
    fetches[1].wait()

    def step_two(step, is_step):
        partial = dot_trans(grad_gu_ref[group.to_own(step)], gu_map_ref[...])
        is_step(size - 1)(lambda: own_ref.__setitem__(..., partial))
        part[step] = partial.astype(BF)
        for k in range(size - 1):
            is_step(k)(functools.partial(scatter.made, k))

    each_step(size, step_two)
    scatter.join()
    half = rows // 2
    norm_sum = jnp.zeros((1, middle_ref.shape[1]), F32)
    for h in range(2):
        span = slice(h * half, (h + 1) * half)
        grad = own_ref[span, :] + scatter.total(h)
        middle = middle_ref[span, :]
        scale = lax.rsqrt(jnp.mean(middle * middle, axis=1, keepdims=True) + EPS)
        unit = middle * scale
        scaled = grad * gain_ref[...]
        norm_sum = norm_sum + jnp.sum(grad * unit, axis=0, keepdims=True)
        grad_out = cot_ref[span, :].astype(F32) * live_ref[span, :]
        grad_middle = grad_out + scale * (
            scaled - unit * jnp.mean(scaled * unit, axis=1, keepdims=True)
        )
        grad_middle_ref[span, :] = grad_middle
        all_ref[group.me, span] = grad_middle.astype(BF)
        gather.start_half(h)
    norm_ref[...] = norm_sum

    def halo(step):
        g = group.from_own(step)
        sems = h_send.at[step], h_recv.at[step]
        return remote(dedge_ref.at[g], back_ref.at[g], *sems, seq=rank - 1)

    def step_heads(step, is_step):
        g = group.from_own(step)

        @is_step(1)
        def _():
            gather.relay()

        for k in range(1, size):
            is_step(k)(functools.partial(gather.ready, k))
        grad = dot_trans(all_ref[g], out_map_ref[...]).astype(BF)
        dq, dk, dv = heads_back(
            g, slot, count, lens_ref, starts_ref, qkv_ref[g], edge_ref[g], grad
        )
        dedge_ref[g] = jnp.concatenate([dk[:WINDOW], dv[:WINDOW]], 1).astype(BF)
        full = jnp.concatenate([dq, dk[WINDOW:], dv[WINDOW:]], 1)
        dqkv_ref[g] = full.astype(BF)
        tail_ref[g] = full[rows - WINDOW :]
        pl.when(rank > 0)(lambda: halo(step).start())

    each_step(size, step_heads)
    scatter.finish()
    fetches[2].wait()

    @pl.when(rank == parts - 1)
    def _():
        back_ref[...] = jnp.zeros_like(back_ref)

    @pl.when(rank < parts - 1)
    def _():
        for step in range(size):
            halo(step).wait_recv()

    scatter = Scatter(group, part, first, over, joined, last, t_send, t_recv)

    def step_one(step, is_step):
        g = group.to_own(step)
        back = back_ref[g].astype(F32)
        wide = jnp.concatenate([jnp.zeros((WINDOW, local), F32), back], 1)
        dqkv_ref[g, pl.ds(rows - WINDOW, WINDOW)] = (tail_ref[g] + wide).astype(BF)
        partial = dot_trans(dqkv_ref[g], qkv_map_ref[...])
        is_step(size - 1)(lambda: own_ref.__setitem__(..., partial))
        part[step] = partial.astype(BF)
        for k in range(size - 1):
            is_step(k)(functools.partial(scatter.made, k))

    each_step(size, step_one)
    scatter.join()
    for h in range(2):
        span = slice(h * half, (h + 1) * half)
        own_ref[span, :] = own_ref[span, :] + scatter.total(h)
    scatter.finish()
    gather.finish()

    @pl.when(rank > 0)
    def _():
        for step in range(size):
            halo(step).wait_send()


def back_part(ident, lens, starts, grad_gu, gu_map, middle, cot, live, gain, out_weight, edge, qkv, qkv_map):
    size, parts = lax.axis_size("fsdp"), lax.axis_size("seq")
    rows, width = middle.shape
    local = out_weight.shape[0]
    vmem = pl.BlockSpec(memory_space=pltpu.VMEM)
    smem = pl.BlockSpec(memory_space=pltpu.SMEM)
    hbm = pl.BlockSpec(memory_space=pl.ANY)
    sems = [pltpu.SemaphoreType.DMA((transfers(size),))] * 2
    return pl.pallas_call(
        functools.partial(back_kernel, size, parts, lens.shape[1]),
        out_shape=[
            jax.ShapeDtypeStruct((rows, width), F32),
            jax.ShapeDtypeStruct((1, width), F32),
            jax.ShapeDtypeStruct((size, rows, width), BF),
            jax.ShapeDtypeStruct(qkv.shape, BF),
            jax.ShapeDtypeStruct((rows, width), F32),
        ],
        in_specs=[smem, smem, hbm, hbm] + [vmem] * 7 + [hbm],
        out_specs=[vmem] * 5,
        scratch_shapes=scatter_shapes(size, rows, width)
        + sems
        + sems
        + [
            pltpu.VMEM(grad_gu.shape, BF),
            pltpu.VMEM(gu_map.shape, BF),
            pltpu.VMEM(qkv_map.shape, BF),
            pltpu.VMEM((size, WINDOW, 2 * local), BF),
            pltpu.VMEM((size, WINDOW, 2 * local), BF),
            pltpu.VMEM((size, WINDOW, 3 * local), F32),
            pltpu.SemaphoreType.DMA((size,)),
            pltpu.SemaphoreType.DMA((size,)),
            pltpu.SemaphoreType.DMA((3,)),
        ],
        compiler_params=pltpu.CompilerParams(
            collective_id=ident, has_side_effects=True, vmem_limit_bytes=67_000_000
        ),
        cost_estimate=pl.CostEstimate(
            flops=2 * size * rows * (gu_map.size + qkv_map.size + width * local),
            bytes_accessed=400_000_000,
            transcendentals=0,
        ),
        name="back_part",
    )(lens, starts, grad_gu, gu_map, middle, cot, live, gain, out_weight, edge, qkv, qkv_map)


def pack_kernel(size, parts, x_ref, g_ref, *refs):
    out_ref = refs[-1]
    full = dot_rows(x_ref[...], g_ref[...])
    pair = out_ref.shape[1]
    rows = full.shape[0] // pair
    piece = rows // parts
    for k in range(pair):
        own = full[k * rows : (k + 1) * rows]
        if len(refs) == 3:
            heads_ref, gb_ref = refs[0], refs[1]
            side = dot_rows(heads_ref[...], gb_ref[...])
            wide = side.shape[1] // pair
            own = jnp.concatenate([own, side[:, k * wide : (k + 1) * wide]], 1)
        out_ref[:, k] = own.astype(BF).reshape(parts, piece, own.shape[1])


def pack_grads(parts, size, x, g, heads=None, gb=None):
    width, cols = x.shape[1], g.shape[1]
    rows = width // size
    piece = rows // parts
    if piece % 8 or (2 * rows) % 128:
        full = dot_rows(x, g).reshape(size, parts, piece, cols)
        if heads is not None:
            side = dot_rows(heads, gb).reshape(parts, piece, size, -1).transpose(2, 0, 1, 3)
            full = jnp.concatenate([full, side], 3)
        return full.transpose(1, 0, 2, 3).astype(BF)
    total = x.shape[0]
    pair = pl.BlockSpec((total, 2 * rows), lambda i: (0, i))
    whole = lambda a: pl.BlockSpec(a.shape, lambda i: (0, 0), pipeline_mode=pl.Buffered(1))
    args, specs = [x, g], [pair, whole(g)]
    out_cols = cols
    if heads is not None:
        args += [heads, gb]
        specs += [whole(heads), pair]
        out_cols += rows
    return pl.pallas_call(
        functools.partial(pack_kernel, size, parts),
        grid=(size // 2,),
        out_shape=jax.ShapeDtypeStruct((parts, size, piece, out_cols), BF),
        in_specs=specs,
        out_specs=pl.BlockSpec((parts, 2, piece, out_cols), lambda i: (0, i, 0, 0)),
        cost_estimate=pl.CostEstimate(
            flops=2 * total * width * out_cols,
            bytes_accessed=2 * (x.size + g.size + width * out_cols),
            transcendentals=0,
        ),
        name="pack_grads",
    )(*args)


def unpack_kernel(widths, every_ref, *outs):
    size = every_ref.shape[1]
    blocks = [every_ref[0, i].astype(F32) for i in range(size)]
    low = 0
    for width, out in zip(widths, outs):
        out[...] = jnp.concatenate([b[:, low : low + width] for b in blocks], 1)
        low += width


def unpack_grads(every, widths):
    parts, size, piece, cols = every.shape
    if piece % 8:
        outs, low = [], 0
        for width in widths:
            block = every[:, :, :, low : low + width].transpose(0, 2, 1, 3)
            outs.append(block.reshape(parts * piece, size * width).astype(F32))
            low += width
        return outs
    return pl.pallas_call(
        functools.partial(unpack_kernel, widths),
        grid=(parts,),
        out_shape=[jax.ShapeDtypeStruct((parts * piece, size * w), F32) for w in widths],
        in_specs=[pl.BlockSpec((1, size, piece, cols), lambda i: (i, 0, 0, 0))],
        out_specs=[pl.BlockSpec((piece, size * w), lambda i: (i, 0)) for w in widths],
        cost_estimate=pl.CostEstimate(flops=0, bytes_accessed=every.size * 6, transcendentals=0),
        name="unpack_grads",
    )(every)


def columns_piece(weights, part, parts):
    size = lax.axis_size("fsdp")
    rows = weights[0].shape[0] // parts
    pieces = []
    for weight in weights:
        own = lax.dynamic_slice_in_dim(weight, part * rows, rows, 0)
        pieces.append(own.reshape(rows, size, -1))
    return jnp.concatenate(pieces, 2).transpose(1, 0, 2)


def shards(
    tokens,
    seq_lengths,
    seq_offsets,
    norm1_gain,
    conv_weight,
    query_weight,
    key_weight,
    value_weight,
    out_weight,
    norm2_gain,
    gate_weight,
    up_weight,
    down_weight,
    cotangent,
):
    size = lax.axis_size("fsdp")
    parts = lax.axis_size("seq")
    part = lax.axis_index("seq")
    me = lax.axis_index("fsdp")
    own_tokens = tokens[0]
    rows, width = own_tokens.shape
    slice_width = norm1_gain.shape[0]
    first_slot = part * rows
    count = seq_lengths.shape[1]

    slot_ext = first_slot - 2 + jnp.arange(rows + 2, dtype=jnp.int32)
    segment_ext = segment_of(
        slot_ext, count, lambda j: seq_lengths[0, j], lambda j: seq_offsets[0, j]
    )
    segment_own = segment_ext[2:]
    same_one = (segment_own == segment_ext[1:-1]).astype(F32)[:, None]
    same_two = (segment_own == segment_ext[:-2]).astype(F32)[:, None]
    live_mask = (segment_own >= 0).astype(F32)[:, None]

    gains = jnp.concatenate(
        [
            norm1_gain[None],
            norm2_gain[None],
            conv_weight.T,
            jnp.zeros((3, slice_width), BF),
        ],
        0,
    )
    table = jnp.zeros((8, 128), jnp.int32)
    table = table.at[0, :count].set(seq_lengths[0]).at[1, :count].set(seq_offsets[0])
    qkv_piece = columns_piece((query_weight, key_weight, value_weight), part, parts)
    gu_piece = columns_piece((gate_weight, up_weight), part, parts)
    gains_all, table_all, qkv_slots, gu_slots = exchange(
        0, gathered=(gains, table), traded=(qkv_piece, gu_piece)
    )
    gains_all = with_own(gains_all, gains).transpose(1, 0, 2).reshape(8, width)
    table_all = with_own(table_all, table)
    lens_all, starts_all = table_all[:, 0, :count], table_all[:, 1, :count]
    qkv_slots = with_own(qkv_slots, lax.dynamic_index_in_dim(qkv_piece, me, 0, keepdims=False))
    gu_slots = with_own(gu_slots, lax.dynamic_index_in_dim(gu_piece, me, 0, keepdims=False))
    grad_out = cotangent[0].astype(F32) * live_mask
    grad_down_all = lax.all_gather(grad_out.astype(BF), "fsdp", axis=0, tiled=True)
    norm_one = gains_all[0].astype(F32)
    norm_two = gains_all[1].astype(F32)
    taps = gains_all[2:5].astype(F32)

    edge_tokens = shifted(own_tokens[rows - 2 :], "seq", 1)
    extended = jnp.concatenate([edge_tokens, own_tokens], 0).astype(F32)
    scale_one = lax.rsqrt(jnp.mean(extended * extended, axis=1, keepdims=True) + EPS)
    normed = extended * scale_one * norm_one
    conv_mix = (
        normed[2:] * taps[0]
        + same_one * normed[1:-1] * taps[1]
        + same_two * normed[:-2] * taps[2]
    )
    gated = (conv_mix * normed[2:]).astype(BF)
    gated_all, qkv, edge, qkv_map = open_mixer(1, gated, qkv_slots)
    qkv_map = qkv_map.reshape(width, -1)
    local = out_weight.shape[0]
    middle, heads_out, normed_all, hidden, grad_gu, gu_map = middle_part(
        2,
        lens_all,
        starts_all,
        edge,
        qkv,
        out_weight,
        own_tokens,
        norm_two[None],
        gu_slots,
        down_weight,
        grad_down_all.reshape(size, rows, width),
    )
    flat = lambda a: a.reshape(-1, a.shape[-1])
    gu_map = gu_map.reshape(width, -1)
    hidden = flat(hidden)

    gu_packed = pack_grads(parts, size, flat(normed_all), flat(grad_gu))
    gu_packed, grad_gu = lax.optimization_barrier((gu_packed, grad_gu))
    gu_piece = lax.psum_scatter(gu_packed, "seq", scatter_dimension=0)
    down_sum = dot_rows(hidden, grad_down_all).astype(BF)
    grad_gu, down_sum = lax.optimization_barrier((grad_gu, down_sum))
    down_total = lax.psum(down_sum, "seq").astype(F32)
    grad_middle, norm2_term, grad_branch_all, dqkv, grad_gated = back_part(
        4,
        lens_all,
        starts_all,
        grad_gu,
        gu_map,
        middle,
        cotangent[0],
        live_mask,
        norm_two[None],
        out_weight,
        edge,
        qkv,
        qkv_map,
    )
    norm2_term = norm2_term[0]
    grad_branch_all, gu_piece = lax.optimization_barrier((grad_branch_all, gu_piece))
    (gu_slots,) = exchange(5, traded=(gu_piece,))
    gu_slots = with_own(gu_slots, lax.dynamic_index_in_dim(gu_piece, me, 0, keepdims=False))
    gu_every = lax.all_gather(gu_slots, "seq", axis=0)
    grad_branch_all, gu_slots = lax.optimization_barrier((grad_branch_all, gu_slots))
    qkvo_packed = pack_grads(
        parts, size, flat(gated_all), flat(dqkv), flat(heads_out), flat(grad_branch_all)
    )
    hidden, grad_gated = lax.optimization_barrier((hidden, grad_gated))
    feed = sum_tokens(9, dot(hidden, down_weight).reshape(size, rows, width))
    qkvo_packed, gu_every, down_total, feed = lax.optimization_barrier(
        (qkvo_packed, gu_every, down_total, feed)
    )
    qkvo_piece = lax.psum_scatter(qkvo_packed, "seq", scatter_dimension=0)
    (qkvo_slots,) = exchange(8, traded=(qkvo_piece,))
    qkvo_slots = with_own(
        qkvo_slots, lax.dynamic_index_in_dim(qkvo_piece, me, 0, keepdims=False)
    )
    qkvo_slots = jnp.concatenate([qkvo_slots[..., : 3 * local], qkvo_piece[..., 3 * local :]], -1)
    qkvo_every = lax.all_gather(qkvo_slots, "seq", axis=0)
    gate_total, up_total = unpack_grads(gu_every, (gu_map.shape[1] // 2,) * 2)
    query_total, key_total, value_total, out_total = unpack_grads(qkvo_every, (local,) * 4)

    normed_own = normed[2:]
    grad_mix = grad_gated * normed_own
    part_zero = jnp.pad(grad_gated * conv_mix + grad_mix * taps[0], ((2, 0), (0, 0)))
    part_one = jnp.pad(grad_mix * same_one * taps[1], ((1, 1), (0, 0)))
    part_two = jnp.pad(grad_mix * same_two * taps[2], ((0, 2), (0, 0)))
    grad_normed = part_zero + part_one + part_two
    unit_one = extended * scale_one
    grad_unit_one = grad_normed * norm_one
    grad_extended = scale_one * (
        grad_unit_one - unit_one * jnp.mean(grad_unit_one * unit_one, axis=1, keepdims=True)
    )
    edge_back = shifted(grad_extended[:2], "seq", -1)
    tokens_grad = grad_middle + grad_extended[2:] + jnp.pad(edge_back, ((rows - 2, 0), (0, 0)))

    terms = jnp.stack(
        [
            jnp.sum(grad_normed * unit_one, axis=0),
            norm2_term,
            jnp.sum(grad_mix * normed_own, axis=0),
            jnp.sum(grad_mix * same_one * normed[1:-1], axis=0),
            jnp.sum(grad_mix * same_two * normed[:-2], axis=0),
        ]
    )
    terms = lax.psum(terms, ("seq", "fsdp"))
    terms = lax.dynamic_slice_in_dim(terms, me * slice_width, slice_width, 1)

    layer_out = (live_mask * (middle + feed)).astype(BF)[None]
    return (
        layer_out,
        tokens_grad[None],
        terms[0],
        terms[2:5].T,
        query_total,
        key_total,
        value_total,
        out_total,
        terms[1],
        gate_total,
        up_total,
        down_total,
    )


def solution(mesh):
    placed = (
        P("fsdp", "seq", None),
        P("fsdp", None),
        P("fsdp", None),
        P("fsdp"),
        P("fsdp", None),
        P("fsdp", None),
        P("fsdp", None),
        P("fsdp", None),
        P("fsdp", None),
        P("fsdp"),
        P("fsdp", None),
        P("fsdp", None),
        P("fsdp", None),
        P("fsdp", "seq", None),
    )
    return jax.shard_map(
        shards,
        mesh=mesh,
        in_specs=placed,
        out_specs=(
            P("fsdp", "seq", None),
            P("fsdp", "seq", None),
            P("fsdp"),
            P("fsdp", None),
            P("fsdp", None),
            P("fsdp", None),
            P("fsdp", None),
            P("fsdp", None),
            P("fsdp"),
            P("fsdp", None),
            P("fsdp", None),
            P("fsdp", None),
        ),
        check_vma=False,
    )
```

```python
import functools

import jax
import jax.numpy as jnp
from jax import lax
from jax.experimental import pallas as pl
from jax.experimental.pallas import tpu as pltpu
from jax.sharding import PartitionSpec as P

HEADS = 16
WINDOW = 64
HEAD_DIM = 112
BLOCK = 128

EPS = 1e-05
NEG = -1e30
SCALE = HEAD_DIM ** (-0.5)
MESH_ID = pl.DeviceIdType.MESH
BF = jnp.bfloat16
F32 = jnp.float32


def shifted(array, axis, by):
    length = lax.axis_size(axis)
    pairs = [(i, i + by) for i in range(length) if 0 <= i + by < length]
    return lax.ppermute(array, axis, pairs)


def segment_of(slot, count, lengths, starts):
    found = jnp.full(slot.shape, -1, jnp.int32)
    for j in range(count):
        inside = (slot >= starts(j)) & (slot < starts(j) + lengths(j))
        found = jnp.where(inside, j, found)
    return jnp.where(slot < 0, -2, found)


def dot_rows(left, right):
    return lax.dot_general(left, right, (((0,), (0,)), ((), ())), preferred_element_type=F32)


def dot_trans(left, right):
    return lax.dot_general(left, right, (((1,), (1,)), ((), ())), preferred_element_type=F32)


def dot(left, right):
    return jnp.dot(left, right, preferred_element_type=F32)


def exchange_kernel(size, modes, *refs):
    count = len(modes)
    ins, outs = refs[:count], refs[count : 2 * count]
    send, recv = refs[2 * count :]
    me = lax.axis_index("fsdp")
    barrier = pltpu.get_barrier_semaphore()
    for step in range(1, size):
        peer = lax.rem(me + step, size)
        pl.semaphore_signal(barrier, inc=1, device_id={"fsdp": peer}, device_id_type=MESH_ID)
    pl.semaphore_wait(barrier, size - 1)
    copies = []
    for k, mode in enumerate(modes):
        for step in range(1, size):
            peer = lax.rem(me + step, size)
            copies.append(
                pltpu.make_async_remote_copy(
                    src_ref=ins[k] if mode == "ag" else ins[k].at[peer],
                    dst_ref=outs[k].at[me],
                    send_sem=send.at[k, step - 1],
                    recv_sem=recv.at[k, step - 1],
                    device_id={"fsdp": peer},
                    device_id_type=MESH_ID,
                )
            )
    for copy in copies:
        copy.start()
    for copy in copies:
        copy.wait()


def exchange(ident, gathered=(), traded=()):
    size = lax.axis_size("fsdp")
    arrays = tuple(gathered) + tuple(traded)
    modes = ("ag",) * len(gathered) + ("a2a",) * len(traded)
    shapes = [(size,) + a.shape for a in gathered] + [a.shape for a in traded]
    sent = sum((size - 1) * a.size * a.dtype.itemsize for a in gathered)
    sent += sum((size - 1) * a.size * a.dtype.itemsize // size for a in traded)
    outs = pl.pallas_call(
        functools.partial(exchange_kernel, size, modes),
        out_shape=[jax.ShapeDtypeStruct(s, a.dtype) for s, a in zip(shapes, arrays)],
        in_specs=[pl.BlockSpec(memory_space=pl.ANY)] * len(arrays),
        out_specs=[pl.BlockSpec(memory_space=pl.ANY)] * len(arrays),
        scratch_shapes=[
            pltpu.SemaphoreType.DMA((len(arrays), size - 1)),
            pltpu.SemaphoreType.DMA((len(arrays), size - 1)),
        ],
        compiler_params=pltpu.CompilerParams(collective_id=ident, has_side_effects=True),
        cost_estimate=pl.CostEstimate(flops=0, bytes_accessed=sent * 50, transcendentals=0),
        name=f"exchange{ident}",
    )(*arrays)
    return outs


def with_own(slots, own):
    return lax.dynamic_update_index_in_dim(slots, own, lax.axis_index("fsdp"), 0)


def gather_tokens(ident, rows):
    (slots,) = exchange(ident, gathered=(rows,))
    slots = with_own(slots, rows)
    return slots.reshape((-1,) + rows.shape[1:])


def sum_tokens(ident, partial):
    (slots,) = exchange(ident, traded=(partial.astype(BF),))
    me = lax.axis_index("fsdp")
    mine = lax.dynamic_index_in_dim(partial, me, 0, keepdims=False)
    total = mine
    for i in range(slots.shape[0]):
        total = total + jnp.where(me == i, 0.0, slots[i].astype(F32))
    return total


def masks_of(first, block, lens_ref, starts_ref, group, count):
    rows = first + block * BLOCK
    query = rows + lax.broadcasted_iota(jnp.int32, (BLOCK, 1), 0)
    keys = rows - WINDOW + lax.broadcasted_iota(jnp.int32, (1, BLOCK + WINDOW), 1)
    length = lambda j: lens_ref[group, j]
    start = lambda j: starts_ref[group, j]
    seg_q = segment_of(query, count, length, start)
    seg_k = segment_of(keys, count, length, start)
    far = query - keys
    return (far >= 0) & (far <= WINDOW) & (seg_q == seg_k)


def soft_of(query, keys, mask):
    scores = dot_trans(query, keys) * SCALE
    scores = jnp.where(mask, scores, NEG)
    peak = jnp.max(scores, axis=1, keepdims=True)
    exponent = jnp.exp(scores - peak)
    return exponent / jnp.sum(exponent, axis=1, keepdims=True)


def lane_head(width):
    return lax.broadcasted_iota(jnp.int32, (1, width), 1) // HEAD_DIM


def remote(src, dst, send, recv, **peer):
    return pltpu.make_async_remote_copy(
        src_ref=src,
        dst_ref=dst,
        send_sem=send,
        recv_sem=recv,
        device_id=peer,
        device_id_type=MESH_ID,
    )


def greet_group(barrier, size):
    me = lax.axis_index("fsdp")
    for step in range(1, size):
        peer = lax.rem(me + step, size)
        pl.semaphore_signal(barrier, inc=1, device_id={"fsdp": peer}, device_id_type=MESH_ID)


class Group:
    def __init__(self, size):
        self.size = size
        self.me = lax.axis_index("fsdp")
        self.square = size == 4
        if self.square:
            x, y = lax.rem(self.me, 2), self.me // 2
            self.at = lambda bx, by: lax.rem(y + by, 2) * 2 + lax.rem(x + bx, 2)
            self.x, self.y, self.far = self.at(1, 0), self.at(0, 1), self.at(1, 1)

    def from_own(self, step):
        if self.square:
            return self.at(lax.rem(step, 2), step // 2)
        return lax.rem(self.me - step + self.size, self.size)

    def to_own(self, step):
        if self.square:
            return self.at(1 - step // 2, 1 - lax.rem(step, 2))
        return lax.rem(self.me + 1 + step, self.size)


class Gather:
    def __init__(self, group, ref, send, recv):
        self.group, self.ref, self.send, self.recv = group, ref, send, recv
        self.half = ref.shape[1] // 2

    def part(self, k, slot, half, peer):
        view = self.ref.at[slot, pl.ds(half * self.half, self.half)]
        return remote(view, view, self.send.at[k], self.recv.at[k], fsdp=peer)

    def whole(self, k):
        g = self.group
        view = self.ref.at[g.me]
        sems = self.send.at[k - 1], self.recv.at[k - 1]
        return remote(view, view, *sems, fsdp=lax.rem(g.me + k, g.size))

    def copy(self, k):
        g = self.group
        if not g.square:
            return self.whole(k + 1)
        slot = (g.me, g.me, g.me, g.me, g.x, g.y)[k]
        half = (0, 1, 0, 1, 0, 1)[k]
        return self.part(k, slot, half, (g.x, g.x, g.y, g.y, g.y, g.x)[k])

    def start_half(self, half):
        if self.group.square:
            self.copy(half).start()
            self.copy(2 + half).start()
        elif half == 1:
            for k in range(self.group.size - 1):
                self.copy(k).start()

    def relay(self):
        if self.group.square:
            self.copy(0).wait_recv()
            self.copy(4).start()
            self.copy(3).wait_recv()
            self.copy(5).start()

    def ready(self, step):
        if not self.group.square:
            self.copy(step - 1).wait_recv()
        elif step == 3:
            self.copy(4).wait_recv()
            self.copy(5).wait_recv()
        else:
            self.copy(step).wait_recv()

    def finish(self):
        for k in range(transfers(self.group.size)):
            self.copy(k).wait_send()


class Scatter:
    def __init__(self, group, part, first, over, joined, last, send, recv):
        self.group, self.part = group, part
        self.first, self.over, self.joined, self.last = first, over, joined, last
        self.send, self.recv = send, recv
        self.half = part.shape[1] // 2

    def copy(self, k):
        g, half = self.group, self.half
        low, high = pl.ds(0, half), pl.ds(half, half)
        if not g.square:
            src, dst, peer = self.part.at[k], self.first.at[k], lax.rem(g.me + 1 + k, g.size)
        else:
            src, dst, peer = (
                lambda: (self.part.at[0, low], self.over.at[0], g.x),
                lambda: (self.part.at[0, high], self.over.at[1], g.y),
                lambda: (self.part.at[1, low], self.first.at[0], g.x),
                lambda: (self.part.at[2, high], self.first.at[1], g.y),
                lambda: (self.joined.at[0], self.last.at[0], g.y),
                lambda: (self.joined.at[1], self.last.at[1], g.x),
            )[k]()
        return remote(src, dst, self.send.at[k], self.recv.at[k], fsdp=peer)

    def made(self, step):
        if not self.group.square:
            self.copy(step).start()
        elif step == 0:
            self.copy(0).start()
            self.copy(1).start()
        elif step in (1, 2):
            self.copy(step + 1).start()

    def join(self):
        if not self.group.square:
            return
        half = self.half
        for k, (step, rows) in enumerate(((2, slice(0, half)), (1, slice(half, 2 * half)))):
            self.copy(k).wait_recv()
            own = self.part[step, rows].astype(F32)
            self.joined[k] = (own + self.over[k].astype(F32)).astype(BF)
            self.copy(4 + k).start()

    def total(self, half):
        count = self.half
        if self.group.square:
            self.copy(2 + half).wait_recv()
            self.copy(4 + half).wait_recv()
            return self.first[half].astype(F32) + self.last[half].astype(F32)
        if half == 0:
            for k in range(self.group.size - 1):
                self.copy(k).wait_recv()
        rows = slice(half * count, (half + 1) * count)
        out = self.first[0, rows].astype(F32)
        for k in range(1, self.group.size - 1):
            out = out + self.first[k, rows].astype(F32)
        return out

    def finish(self):
        for k in range(transfers(self.group.size)):
            self.copy(k).wait_send()


class Line:
    def __init__(self, parts, sems):
        self.rank = lax.axis_index("seq")
        self.parts, self.length = parts, parts // 2
        self.z, self.core = self.rank // 2, lax.rem(self.rank, 2)
        self.above, self.below = self.rank + 2, self.rank - 2
        self.beside = self.rank + 1 - 2 * self.core
        self.has_above, self.has_below = self.z < self.length - 1, self.z > 0
        self.sems = sems

    def greet(self, barrier):
        def one(peer):
            pl.semaphore_signal(barrier, inc=1, device_id={"seq": peer}, device_id_type=MESH_ID)

        one(self.beside)
        pl.when(self.has_above)(lambda: one(self.above))
        pl.when(self.has_below)(lambda: one(self.below))
        n, z = self.length, self.z
        return 1 + (2 * n - 2 - z) // n + (z + n - 1) // n

    def up(self, k, owner):
        view = self.view(owner)
        return remote(view, view, self.sems[0].at[k], self.sems[1].at[k], seq=self.above)

    def down(self, k, owner):
        view = self.view(owner)
        return remote(view, view, self.sems[2].at[k], self.sems[3].at[k], seq=self.below)

    def side(self, k, owner):
        view = self.view(owner)
        return remote(view, view, self.sems[4].at[k], self.sems[5].at[k], seq=self.beside)

    def gather(self, view):
        self.view = view
        pl.when(self.has_above)(lambda: self.up(0, self.rank).start())
        pl.when(self.has_below)(lambda: self.down(0, self.rank).start())
        self.side(self.z, self.rank).start()

    def hop(self, j):
        rank, z = self.rank, self.z

        @pl.when(z >= j)
        def _():
            self.up(j - 1, rank).wait_recv()
            pl.when(self.has_above)(lambda: self.up(j, rank - 2 * j).start())
            self.side(z - j, rank - 2 * j).start()

        @pl.when(z + j < self.length)
        def _():
            self.down(j - 1, rank).wait_recv()
            pl.when(self.has_below)(lambda: self.down(j, rank + 2 * j).start())
            self.side(z + j, rank + 2 * j).start()

    def gathered(self):
        for k in range(self.length):
            self.side(k, self.rank).wait_recv()

    def finish(self):
        rank, z = self.rank, self.z
        for k in range(self.length):
            self.side(k, rank).wait_send()
        pl.when(self.has_above)(lambda: self.up(0, rank).wait_send())
        pl.when(self.has_below)(lambda: self.down(0, rank).wait_send())
        for j in range(1, self.length):
            pl.when((z >= j) & self.has_above)(lambda: self.up(j, rank).wait_send())
            pl.when((z + j < self.length) & self.has_below)(lambda: self.down(j, rank).wait_send())


def line_sems(parts):
    return [pltpu.SemaphoreType.DMA((parts // 2,))] * 6


def transfers(size):
    return 6 if size == 4 else size - 1


def scatter_shapes(size, rows, width):
    half = rows // 2
    slots = (2, half, width) if size == 4 else (size - 1, rows, width)
    return [
        pltpu.VMEM((size, rows, width), BF),
        pltpu.VMEM(slots, BF),
        pltpu.VMEM((2, half, width), BF),
        pltpu.VMEM((2, half, width), BF),
        pltpu.VMEM((2, half, width), BF),
        pltpu.SemaphoreType.DMA((transfers(size),)),
        pltpu.SemaphoreType.DMA((transfers(size),)),
    ]


def each_step(size, body):
    def one(step, carry):
        body(step, lambda k: pl.when(step == k))
        return carry

    lax.fori_loop(0, size, one, 0)


def open_kernel(size, parts, gated_ref, piece_ref, all_ref, qkv_ref, edge_ref, map_ref, tail_ref,
                load, send, recv, halo_send, halo_recv, *sems):
    rank = lax.axis_index("seq")
    rows = gated_ref.shape[0]
    local = qkv_ref.shape[2] // 3
    group, line = Group(size), Line(parts, sems)
    barrier = pltpu.get_barrier_semaphore()
    greet_group(barrier, size)
    known = line.greet(barrier)

    def greet(peer):
        pl.semaphore_signal(barrier, inc=1, device_id={"seq": peer}, device_id_type=MESH_ID)

    pl.when(line.has_above & (line.core == 1))(lambda: greet(rank + 1))
    pl.when(line.has_below & (line.core == 0))(lambda: greet(rank - 1))
    n, z = line.length, line.z
    known = known + (2 * n - 2 - z) // n * line.core + (z + n - 1) // n * (1 - line.core)
    own = pltpu.make_async_copy(piece_ref, map_ref.at[:, rank], load)
    own.start()
    all_ref[group.me] = gated_ref[...]
    pl.semaphore_wait(barrier, size - 1 + known)

    gather = Gather(group, all_ref, send, recv)
    gather.start_half(0)
    gather.start_half(1)
    own.wait()
    line.gather(lambda owner: map_ref.at[:, owner])
    gather.relay()
    for j in range(1, line.length):
        line.hop(j)
    for step in range(1, size):
        gather.ready(step)
    line.gathered()

    weights = map_ref[...].reshape(-1, map_ref.shape[3])

    def halo():
        return remote(tail_ref, edge_ref, halo_send, halo_recv, seq=rank + 1)

    def one(g, carry):
        out = dot(all_ref[g], weights).astype(BF)
        qkv_ref[g] = out
        tail_ref[g] = out[rows - WINDOW :, local:]
        return carry

    lax.fori_loop(0, size, one, 0)
    pl.when(rank < parts - 1)(lambda: halo().start())

    @pl.when(rank == 0)
    def _():
        edge_ref[...] = jnp.zeros_like(edge_ref)

    gather.finish()
    line.finish()
    pl.when(rank > 0)(lambda: halo().wait_recv())
    pl.when(rank < parts - 1)(lambda: halo().wait_send())


def open_mixer(ident, gated, piece):
    size, parts = lax.axis_size("fsdp"), lax.axis_size("seq")
    rows, width = gated.shape
    cols = piece.shape[2]
    sems = lambda n: [pltpu.SemaphoreType.DMA((n,))] * 2
    vmem = pl.BlockSpec(memory_space=pltpu.VMEM)
    return pl.pallas_call(
        functools.partial(open_kernel, size, parts),
        out_shape=[
            jax.ShapeDtypeStruct((size, rows, width), BF),
            jax.ShapeDtypeStruct((size, rows, cols), BF),
            jax.ShapeDtypeStruct((size, WINDOW, cols // 3 * 2), BF),
            jax.ShapeDtypeStruct((size, parts) + piece.shape[1:], BF),
        ],
        in_specs=[vmem, pl.BlockSpec(memory_space=pl.ANY)],
        out_specs=[vmem] * 4,
        scratch_shapes=[
            pltpu.VMEM((size, WINDOW, cols // 3 * 2), BF),
            pltpu.SemaphoreType.DMA,
        ]
        + sems(transfers(size))
        + [pltpu.SemaphoreType.DMA, pltpu.SemaphoreType.DMA]
        + line_sems(parts),
        compiler_params=pltpu.CompilerParams(collective_id=ident, has_side_effects=True),
        cost_estimate=pl.CostEstimate(
            flops=2 * size * rows * width * cols, bytes_accessed=150_000_000, transcendentals=0
        ),
        name="open_mixer",
    )(gated, piece)


def middle_kernel(size, parts, count, lens_ref, starts_ref, edge_ref, qkv_ref, out_map_ref, tokens_ref,
                  gain_ref, gu_hbm, down_ref, grad_ref, middle_ref, heads_ref, grads_ref, all_hbm, hidden_hbm, gu_grad_hbm, gu_out,
                  part, first, over, joined, last, s_send, s_recv, own_ref, all_ref, g_send, g_recv,
                  c_send, c_recv, gu_ref, hidden_ref, gu_grad_ref, loads, stores, *sems):
    rows = tokens_ref.shape[0]
    local = heads_ref.shape[2]
    inner = down_ref.shape[0]
    slot = lax.axis_index("seq") * rows
    group = Group(size)
    barrier = pltpu.get_barrier_semaphore()
    greet_group(barrier, size)
    line = Line(parts, sems)
    known = line.greet(barrier)
    fetch = pltpu.make_async_copy(gu_hbm, gu_ref.at[:, line.rank], loads.at[0])
    fetch.start()
    grads_ref[group.me] = grad_ref[...]
    pl.semaphore_wait(barrier, size - 1 + known)
    fetch.wait()
    line.gather(lambda owner: gu_ref.at[:, owner])
    scatter = Scatter(group, part, first, over, joined, last, s_send, s_recv)
    gather = Gather(group, all_ref, g_send, g_recv)
    grads = Gather(group, grads_ref, c_send, c_recv)
    head_of = lane_head(local)

    def mix(step, is_step):
        g = group.to_own(step)
        own = qkv_ref[g]
        edge = edge_ref[g]
        queries = own[:, :local]
        keys = jnp.concatenate([edge[:, :local], own[:, local : 2 * local]], 0)
        values = jnp.concatenate([edge[:, local:], own[:, 2 * local :]], 0)
        outs = []
        for block in range(rows // BLOCK):
            mask = masks_of(slot, block, lens_ref, starts_ref, g, count)
            low = block * BLOCK
            query = queries[low : low + BLOCK]
            key = keys[low : low + BLOCK + WINDOW]
            value = values[low : low + BLOCK + WINDOW]
            out = jnp.zeros((BLOCK, local), F32)
            for head in range(local // HEAD_DIM):
                mine = head_of == head
                soft = soft_of(jnp.where(mine, query, jnp.zeros_like(query)), key, mask)
                out = jnp.where(mine, dot(soft.astype(BF), value), out)
            outs.append(out.astype(BF))
        heads = jnp.concatenate(outs, 0)
        heads_ref[g] = heads
        branch = dot(heads, out_map_ref[...])
        is_step(size - 1)(lambda: own_ref.__setitem__(..., branch))
        part[step] = branch.astype(BF)
        for k in range(size - 1):
            is_step(k)(functools.partial(scatter.made, k))

    each_step(size, mix)
    scatter.join()
    grads.start_half(0)
    grads.start_half(1)
    line.hop(1)
    half = rows // 2
    for h in range(2):
        span = slice(h * half, (h + 1) * half)
        total = own_ref[span, :] + scatter.total(h)
        middle = tokens_ref[span, :].astype(F32) + total
        middle_ref[span, :] = middle
        scale = lax.rsqrt(jnp.mean(middle * middle, axis=1, keepdims=True) + EPS)
        all_ref[group.me, span] = (middle * scale * gain_ref[...]).astype(BF)
        gather.start_half(h)
    gather.relay()
    grads.relay()
    for j in range(2, line.length):
        line.hop(j)
    line.gathered()
    keep = pltpu.make_async_copy(gu_ref, gu_out, loads.at[0])
    keep.start()

    def out_copies(g):
        return [
            pltpu.make_async_copy(src.at[g], dst.at[g], stores.at[k, g])
            for k, (src, dst) in enumerate(
                ((all_ref, all_hbm), (hidden_ref, hidden_hbm), (gu_grad_ref, gu_grad_hbm))
            )
        ]

    def feed(step, is_step):
        g = group.from_own(step)
        for k in range(1, size):
            is_step(k)(functools.partial(gather.ready, k))
            is_step(k)(functools.partial(grads.ready, k))
        weights = gu_ref[...].reshape(-1, gu_ref.shape[3])
        acts = dot(all_ref[g], weights)
        gate, up = acts[:, :inner], acts[:, inner:]
        sigma = jax.nn.sigmoid(gate)
        silu = gate * sigma
        hidden_ref[g] = (silu * up).astype(BF)
        grad_hidden = dot_trans(grads_ref[g], down_ref[...])
        grad_gate = grad_hidden * up * sigma * (1.0 + gate * (1.0 - sigma))
        gu_grad_ref[g] = jnp.concatenate([grad_gate, grad_hidden * silu], 1).astype(BF)
        for copy in out_copies(g):
            copy.start()

    each_step(size, feed)
    scatter.finish()
    gather.finish()
    grads.finish()
    line.finish()
    keep.wait()
    for g in range(size):
        for copy in out_copies(g):
            copy.wait()


def middle_part(ident, lens, starts, edge, qkv, out_weight, tokens, gain, gu_piece, down_weight, grad):
    size, parts = lax.axis_size("fsdp"), lax.axis_size("seq")
    rows, width = tokens.shape
    local, inner = out_weight.shape[0], down_weight.shape[0]
    vmem = pl.BlockSpec(memory_space=pltpu.VMEM)
    smem = pl.BlockSpec(memory_space=pltpu.SMEM)
    hbm = pl.BlockSpec(memory_space=pl.ANY)
    _, piece, cols = gu_piece.shape
    shape = lambda w: (size, rows, w)
    return pl.pallas_call(
        functools.partial(middle_kernel, size, parts, lens.shape[1]),
        out_shape=[
            jax.ShapeDtypeStruct((rows, width), F32),
            jax.ShapeDtypeStruct(shape(local), BF),
            jax.ShapeDtypeStruct(shape(width), BF),
            jax.ShapeDtypeStruct(shape(width), BF),
            jax.ShapeDtypeStruct(shape(inner), BF),
            jax.ShapeDtypeStruct(shape(cols), BF),
            jax.ShapeDtypeStruct((size, parts, piece, cols), BF),
        ],
        in_specs=[smem, smem] + [vmem] * 5 + [hbm, vmem, vmem],
        out_specs=[vmem, vmem, vmem, hbm, hbm, hbm, hbm],
        scratch_shapes=scatter_shapes(size, rows, width)
        + [
            pltpu.VMEM((rows, width), F32),
            pltpu.VMEM(shape(width), BF),
            pltpu.SemaphoreType.DMA((transfers(size),)),
            pltpu.SemaphoreType.DMA((transfers(size),)),
            pltpu.SemaphoreType.DMA((transfers(size),)),
            pltpu.SemaphoreType.DMA((transfers(size),)),
            pltpu.VMEM((size, parts, piece, cols), BF),
            pltpu.VMEM(shape(inner), BF),
            pltpu.VMEM(shape(cols), BF),
            pltpu.SemaphoreType.DMA((2,)),
            pltpu.SemaphoreType.DMA((3, size)),
        ]
        + line_sems(parts),
        compiler_params=pltpu.CompilerParams(
            collective_id=ident, has_side_effects=True, vmem_limit_bytes=67_000_000
        ),
        cost_estimate=pl.CostEstimate(
            flops=2 * size * rows * width * (local + 3 * inner),
            bytes_accessed=250_000_000,
            transcendentals=0,
        ),
        name="middle_part",
    )(lens, starts, edge, qkv, out_weight, tokens, gain, gu_piece, down_weight, grad)


def heads_back(group, slot, count, lens_ref, starts_ref, own, edge, grad):
    rows, local = own.shape[0], own.shape[1] // 3
    head_of = lane_head(local)
    queries = own[:, :local]
    keys = jnp.concatenate([edge[:, :local], own[:, local : 2 * local]], 0)
    values = jnp.concatenate([edge[:, local:], own[:, 2 * local :]], 0)
    dqs, dks, dvs = [], [], []
    for block in range(rows // BLOCK):
        mask = masks_of(slot, block, lens_ref, starts_ref, group, count)
        low = block * BLOCK
        span = slice(low, low + BLOCK + WINDOW)
        query, grads = queries[low : low + BLOCK], grad[low : low + BLOCK]
        key, value = keys[span], values[span]
        dq = jnp.zeros((BLOCK, local), F32)
        dk = jnp.zeros((BLOCK + WINDOW, local), F32)
        dv = jnp.zeros((BLOCK + WINDOW, local), F32)
        for head in range(local // HEAD_DIM):
            mine = head_of == head
            own_q = jnp.where(mine, query, jnp.zeros_like(query))
            own_g = jnp.where(mine, grads, jnp.zeros_like(grads))
            soft = soft_of(own_q, key, mask)
            grad_soft = dot_trans(own_g, value)
            total = jnp.sum(grad_soft * soft, axis=1, keepdims=True)
            grad_scores = (soft * (grad_soft - total)).astype(BF)
            dq = jnp.where(mine, dot(grad_scores, key), dq)
            dk = dk + dot_rows(grad_scores, own_q)
            dv = dv + dot_rows(soft.astype(BF), own_g)
        dqs.append(dq * SCALE)
        dks.append(dk * SCALE)
        dvs.append(dv)

    def joined(pieces):
        out = [pieces[0][:BLOCK]]
        for left, right in zip(pieces, pieces[1:]):
            out.append(left[BLOCK:] + right[:WINDOW])
            out.append(right[WINDOW:BLOCK])
        out.append(pieces[-1][BLOCK:])
        return jnp.concatenate(out, 0)

    return jnp.concatenate(dqs, 0), joined(dks), joined(dvs)


def back_kernel(size, parts, count, lens_ref, starts_ref, grad_gu_hbm, gu_map_hbm, middle_ref, cot_ref, live_ref,
                gain_ref, out_map_ref, edge_ref, qkv_ref, qkv_map_hbm,
                grad_middle_ref, norm_ref, all_ref, dqkv_ref, own_ref,
                part, first, over, joined, last, s_send, s_recv, t_send, t_recv, g_send, g_recv,
                grad_gu_ref, gu_map_ref, qkv_map_ref, dedge_ref, back_ref, tail_ref, h_send, h_recv, loads):
    rows = middle_ref.shape[0]
    local = out_map_ref.shape[0]
    rank = lax.axis_index("seq")
    slot = rank * rows
    group = Group(size)
    barrier = pltpu.get_barrier_semaphore()
    greet_group(barrier, size)

    def greet(peer):
        pl.semaphore_signal(barrier, inc=1, device_id={"seq": peer}, device_id_type=MESH_ID)

    pl.when(rank > 0)(lambda: greet(rank - 1))
    pl.when(rank < parts - 1)(lambda: greet(rank + 1))
    fetches = [
        pltpu.make_async_copy(src, dst, loads.at[k])
        for k, (src, dst) in enumerate(
            ((grad_gu_hbm, grad_gu_ref), (gu_map_hbm, gu_map_ref), (qkv_map_hbm, qkv_map_ref))
        )
    ]
    for fetch in fetches:
        fetch.start()
    has_next = (2 * parts - 2 - rank) // parts
    has_last = (rank + parts - 1) // parts
    pl.semaphore_wait(barrier, size - 1 + has_next + has_last)
    scatter = Scatter(group, part, first, over, joined, last, s_send, s_recv)
    gather = Gather(group, all_ref, g_send, g_recv)
    fetches[0].wait()
    fetches[1].wait()

    def step_two(step, is_step):
        partial = dot_trans(grad_gu_ref[group.to_own(step)], gu_map_ref[...])
        is_step(size - 1)(lambda: own_ref.__setitem__(..., partial))
        part[step] = partial.astype(BF)
        for k in range(size - 1):
            is_step(k)(functools.partial(scatter.made, k))

    each_step(size, step_two)
    scatter.join()
    half = rows // 2
    norm_sum = jnp.zeros((1, middle_ref.shape[1]), F32)
    for h in range(2):
        span = slice(h * half, (h + 1) * half)
        grad = own_ref[span, :] + scatter.total(h)
        middle = middle_ref[span, :]
        scale = lax.rsqrt(jnp.mean(middle * middle, axis=1, keepdims=True) + EPS)
        unit = middle * scale
        scaled = grad * gain_ref[...]
        norm_sum = norm_sum + jnp.sum(grad * unit, axis=0, keepdims=True)
        grad_out = cot_ref[span, :].astype(F32) * live_ref[span, :]
        grad_middle = grad_out + scale * (
            scaled - unit * jnp.mean(scaled * unit, axis=1, keepdims=True)
        )
        grad_middle_ref[span, :] = grad_middle
        all_ref[group.me, span] = grad_middle.astype(BF)
        gather.start_half(h)
    norm_ref[...] = norm_sum

    def halo(step):
        g = group.from_own(step)
        sems = h_send.at[step], h_recv.at[step]
        return remote(dedge_ref.at[g], back_ref.at[g], *sems, seq=rank - 1)

    def step_heads(step, is_step):
        g = group.from_own(step)

        @is_step(1)
        def _():
            gather.relay()

        for k in range(1, size):
            is_step(k)(functools.partial(gather.ready, k))
        grad = dot_trans(all_ref[g], out_map_ref[...]).astype(BF)
        dq, dk, dv = heads_back(
            g, slot, count, lens_ref, starts_ref, qkv_ref[g], edge_ref[g], grad
        )
        dedge_ref[g] = jnp.concatenate([dk[:WINDOW], dv[:WINDOW]], 1).astype(BF)
        full = jnp.concatenate([dq, dk[WINDOW:], dv[WINDOW:]], 1)
        dqkv_ref[g] = full.astype(BF)
        tail_ref[g] = full[rows - WINDOW :]
        pl.when(rank > 0)(lambda: halo(step).start())

    each_step(size, step_heads)
    scatter.finish()
    fetches[2].wait()

    @pl.when(rank == parts - 1)
    def _():
        back_ref[...] = jnp.zeros_like(back_ref)

    @pl.when(rank < parts - 1)
    def _():
        for step in range(size):
            halo(step).wait_recv()

    scatter = Scatter(group, part, first, over, joined, last, t_send, t_recv)

    def step_one(step, is_step):
        g = group.to_own(step)
        back = back_ref[g].astype(F32)
        wide = jnp.concatenate([jnp.zeros((WINDOW, local), F32), back], 1)
        dqkv_ref[g, pl.ds(rows - WINDOW, WINDOW)] = (tail_ref[g] + wide).astype(BF)
        partial = dot_trans(dqkv_ref[g], qkv_map_ref[...])
        is_step(size - 1)(lambda: own_ref.__setitem__(..., partial))
        part[step] = partial.astype(BF)
        for k in range(size - 1):
            is_step(k)(functools.partial(scatter.made, k))

    each_step(size, step_one)
    scatter.join()
    for h in range(2):
        span = slice(h * half, (h + 1) * half)
        own_ref[span, :] = own_ref[span, :] + scatter.total(h)
    scatter.finish()
    gather.finish()

    @pl.when(rank > 0)
    def _():
        for step in range(size):
            halo(step).wait_send()


def back_part(ident, lens, starts, grad_gu, gu_map, middle, cot, live, gain, out_weight, edge, qkv, qkv_map):
    size, parts = lax.axis_size("fsdp"), lax.axis_size("seq")
    rows, width = middle.shape
    local = out_weight.shape[0]
    vmem = pl.BlockSpec(memory_space=pltpu.VMEM)
    smem = pl.BlockSpec(memory_space=pltpu.SMEM)
    hbm = pl.BlockSpec(memory_space=pl.ANY)
    sems = [pltpu.SemaphoreType.DMA((transfers(size),))] * 2
    return pl.pallas_call(
        functools.partial(back_kernel, size, parts, lens.shape[1]),
        out_shape=[
            jax.ShapeDtypeStruct((rows, width), F32),
            jax.ShapeDtypeStruct((1, width), F32),
            jax.ShapeDtypeStruct((size, rows, width), BF),
            jax.ShapeDtypeStruct(qkv.shape, BF),
            jax.ShapeDtypeStruct((rows, width), F32),
        ],
        in_specs=[smem, smem, hbm, hbm] + [vmem] * 7 + [hbm],
        out_specs=[vmem] * 5,
        scratch_shapes=scatter_shapes(size, rows, width)
        + sems
        + sems
        + [
            pltpu.VMEM(grad_gu.shape, BF),
            pltpu.VMEM(gu_map.shape, BF),
            pltpu.VMEM(qkv_map.shape, BF),
            pltpu.VMEM((size, WINDOW, 2 * local), BF),
            pltpu.VMEM((size, WINDOW, 2 * local), BF),
            pltpu.VMEM((size, WINDOW, 3 * local), F32),
            pltpu.SemaphoreType.DMA((size,)),
            pltpu.SemaphoreType.DMA((size,)),
            pltpu.SemaphoreType.DMA((3,)),
        ],
        compiler_params=pltpu.CompilerParams(
            collective_id=ident, has_side_effects=True, vmem_limit_bytes=67_000_000
        ),
        cost_estimate=pl.CostEstimate(
            flops=2 * size * rows * (gu_map.size + qkv_map.size + width * local),
            bytes_accessed=400_000_000,
            transcendentals=0,
        ),
        name="back_part",
    )(lens, starts, grad_gu, gu_map, middle, cot, live, gain, out_weight, edge, qkv, qkv_map)


def pack_kernel(size, parts, x_ref, g_ref, *refs):
    out_ref = refs[-1]
    full = dot_rows(x_ref[...], g_ref[...])
    pair = out_ref.shape[1]
    rows = full.shape[0] // pair
    piece = rows // parts
    for k in range(pair):
        own = full[k * rows : (k + 1) * rows]
        if len(refs) == 3:
            heads_ref, gb_ref = refs[0], refs[1]
            side = dot_rows(heads_ref[...], gb_ref[...])
            wide = side.shape[1] // pair
            own = jnp.concatenate([own, side[:, k * wide : (k + 1) * wide]], 1)
        out_ref[:, k] = own.astype(BF).reshape(parts, piece, own.shape[1])


def pack_grads(parts, size, x, g, heads=None, gb=None):
    width, cols = x.shape[1], g.shape[1]
    rows = width // size
    piece = rows // parts
    if piece % 8 or (2 * rows) % 128:
        full = dot_rows(x, g).reshape(size, parts, piece, cols)
        if heads is not None:
            side = dot_rows(heads, gb).reshape(parts, piece, size, -1).transpose(2, 0, 1, 3)
            full = jnp.concatenate([full, side], 3)
        return full.transpose(1, 0, 2, 3).astype(BF)
    total = x.shape[0]
    pair = pl.BlockSpec((total, 2 * rows), lambda i: (0, i))
    whole = lambda a: pl.BlockSpec(a.shape, lambda i: (0, 0), pipeline_mode=pl.Buffered(1))
    args, specs = [x, g], [pair, whole(g)]
    out_cols = cols
    if heads is not None:
        args += [heads, gb]
        specs += [whole(heads), pair]
        out_cols += rows
    return pl.pallas_call(
        functools.partial(pack_kernel, size, parts),
        grid=(size // 2,),
        out_shape=jax.ShapeDtypeStruct((parts, size, piece, out_cols), BF),
        in_specs=specs,
        out_specs=pl.BlockSpec((parts, 2, piece, out_cols), lambda i: (0, i, 0, 0)),
        cost_estimate=pl.CostEstimate(
            flops=2 * total * width * out_cols,
            bytes_accessed=2 * (x.size + g.size + width * out_cols),
            transcendentals=0,
        ),
        name="pack_grads",
    )(*args)


def unpack_kernel(widths, every_ref, *outs):
    size = every_ref.shape[1]
    blocks = [every_ref[0, i].astype(F32) for i in range(size)]
    low = 0
    for width, out in zip(widths, outs):
        out[...] = jnp.concatenate([b[:, low : low + width] for b in blocks], 1)
        low += width


def unpack_grads(every, widths):
    parts, size, piece, cols = every.shape
    if piece % 8:
        outs, low = [], 0
        for width in widths:
            block = every[:, :, :, low : low + width].transpose(0, 2, 1, 3)
            outs.append(block.reshape(parts * piece, size * width).astype(F32))
            low += width
        return outs
    return pl.pallas_call(
        functools.partial(unpack_kernel, widths),
        grid=(parts,),
        out_shape=[jax.ShapeDtypeStruct((parts * piece, size * w), F32) for w in widths],
        in_specs=[pl.BlockSpec((1, size, piece, cols), lambda i: (i, 0, 0, 0))],
        out_specs=[pl.BlockSpec((piece, size * w), lambda i: (i, 0)) for w in widths],
        cost_estimate=pl.CostEstimate(flops=0, bytes_accessed=every.size * 6, transcendentals=0),
        name="unpack_grads",
    )(every)


def columns_piece(weights, part, parts):
    size = lax.axis_size("fsdp")
    rows = weights[0].shape[0] // parts
    pieces = []
    for weight in weights:
        own = lax.dynamic_slice_in_dim(weight, part * rows, rows, 0)
        pieces.append(own.reshape(rows, size, -1))
    return jnp.concatenate(pieces, 2).transpose(1, 0, 2)


def shards(
    tokens,
    seq_lengths,
    seq_offsets,
    norm1_gain,
    conv_weight,
    query_weight,
    key_weight,
    value_weight,
    out_weight,
    norm2_gain,
    gate_weight,
    up_weight,
    down_weight,
    cotangent,
):
    size = lax.axis_size("fsdp")
    parts = lax.axis_size("seq")
    part = lax.axis_index("seq")
    me = lax.axis_index("fsdp")
    own_tokens = tokens[0]
    rows, width = own_tokens.shape
    slice_width = norm1_gain.shape[0]
    first_slot = part * rows
    count = seq_lengths.shape[1]

    slot_ext = first_slot - 2 + jnp.arange(rows + 2, dtype=jnp.int32)
    segment_ext = segment_of(
        slot_ext, count, lambda j: seq_lengths[0, j], lambda j: seq_offsets[0, j]
    )
    segment_own = segment_ext[2:]
    same_one = (segment_own == segment_ext[1:-1]).astype(F32)[:, None]
    same_two = (segment_own == segment_ext[:-2]).astype(F32)[:, None]
    live_mask = (segment_own >= 0).astype(F32)[:, None]

    gains = jnp.concatenate(
        [
            norm1_gain[None],
            norm2_gain[None],
            conv_weight.T,
            jnp.zeros((3, slice_width), BF),
        ],
        0,
    )
    table = jnp.zeros((8, 128), jnp.int32)
    table = table.at[0, :count].set(seq_lengths[0]).at[1, :count].set(seq_offsets[0])
    qkv_piece = columns_piece((query_weight, key_weight, value_weight), part, parts)
    gu_piece = columns_piece((gate_weight, up_weight), part, parts)
    gains_all, table_all, qkv_slots, gu_slots = exchange(
        0, gathered=(gains, table), traded=(qkv_piece, gu_piece)
    )
    gains_all = with_own(gains_all, gains).transpose(1, 0, 2).reshape(8, width)
    table_all = with_own(table_all, table)
    lens_all, starts_all = table_all[:, 0, :count], table_all[:, 1, :count]
    qkv_slots = with_own(qkv_slots, lax.dynamic_index_in_dim(qkv_piece, me, 0, keepdims=False))
    gu_slots = with_own(gu_slots, lax.dynamic_index_in_dim(gu_piece, me, 0, keepdims=False))
    grad_down = (cotangent[0].astype(F32) * live_mask).astype(BF)
    norm_one = gains_all[0].astype(F32)
    norm_two = gains_all[1].astype(F32)
    taps = gains_all[2:5].astype(F32)

    edge_tokens = shifted(own_tokens[rows - 2 :], "seq", 1)
    extended = jnp.concatenate([edge_tokens, own_tokens], 0).astype(F32)
    scale_one = lax.rsqrt(jnp.mean(extended * extended, axis=1, keepdims=True) + EPS)
    normed = extended * scale_one * norm_one
    conv_mix = (
        normed[2:] * taps[0]
        + same_one * normed[1:-1] * taps[1]
        + same_two * normed[:-2] * taps[2]
    )
    gated = (conv_mix * normed[2:]).astype(BF)
    gated_all, qkv, edge, qkv_map = open_mixer(1, gated, qkv_slots)
    qkv_map = qkv_map.reshape(width, -1)
    local = out_weight.shape[0]
    middle, heads_out, grad_down_all, normed_all, hidden, grad_gu, gu_map = middle_part(
        2,
        lens_all,
        starts_all,
        edge,
        qkv,
        out_weight,
        own_tokens,
        norm_two[None],
        gu_slots,
        down_weight,
        grad_down,
    )
    flat = lambda a: a.reshape(-1, a.shape[-1])
    gu_map = gu_map.reshape(width, -1)
    hidden, grad_down_all = flat(hidden), flat(grad_down_all)

    gu_packed = pack_grads(parts, size, flat(normed_all), flat(grad_gu))
    gu_packed, grad_gu = lax.optimization_barrier((gu_packed, grad_gu))
    gu_piece = lax.psum_scatter(gu_packed, "seq", scatter_dimension=0)
    down_sum = dot_rows(hidden, grad_down_all).astype(BF)
    grad_gu, down_sum = lax.optimization_barrier((grad_gu, down_sum))
    down_total = lax.psum(down_sum, "seq").astype(F32)
    grad_middle, norm2_term, grad_branch_all, dqkv, grad_gated = back_part(
        4,
        lens_all,
        starts_all,
        grad_gu,
        gu_map,
        middle,
        cotangent[0],
        live_mask,
        norm_two[None],
        out_weight,
        edge,
        qkv,
        qkv_map,
    )
    norm2_term = norm2_term[0]
    grad_branch_all, gu_piece = lax.optimization_barrier((grad_branch_all, gu_piece))
    (gu_slots,) = exchange(5, traded=(gu_piece,))
    gu_slots = with_own(gu_slots, lax.dynamic_index_in_dim(gu_piece, me, 0, keepdims=False))
    gu_every = lax.all_gather(gu_slots, "seq", axis=0)
    grad_branch_all, gu_slots = lax.optimization_barrier((grad_branch_all, gu_slots))
    qkvo_packed = pack_grads(
        parts, size, flat(gated_all), flat(dqkv), flat(heads_out), flat(grad_branch_all)
    )
    hidden, grad_gated = lax.optimization_barrier((hidden, grad_gated))
    feed = sum_tokens(9, dot(hidden, down_weight).reshape(size, rows, width))
    qkvo_packed, gu_every, down_total, feed = lax.optimization_barrier(
        (qkvo_packed, gu_every, down_total, feed)
    )
    qkvo_piece = lax.psum_scatter(qkvo_packed, "seq", scatter_dimension=0)
    (qkvo_slots,) = exchange(8, traded=(qkvo_piece,))
    qkvo_slots = with_own(
        qkvo_slots, lax.dynamic_index_in_dim(qkvo_piece, me, 0, keepdims=False)
    )
    qkvo_slots = jnp.concatenate([qkvo_slots[..., : 3 * local], qkvo_piece[..., 3 * local :]], -1)
    qkvo_every = lax.all_gather(qkvo_slots, "seq", axis=0)
    gate_total, up_total = unpack_grads(gu_every, (gu_map.shape[1] // 2,) * 2)
    query_total, key_total, value_total, out_total = unpack_grads(qkvo_every, (local,) * 4)

    normed_own = normed[2:]
    grad_mix = grad_gated * normed_own
    part_zero = jnp.pad(grad_gated * conv_mix + grad_mix * taps[0], ((2, 0), (0, 0)))
    part_one = jnp.pad(grad_mix * same_one * taps[1], ((1, 1), (0, 0)))
    part_two = jnp.pad(grad_mix * same_two * taps[2], ((0, 2), (0, 0)))
    grad_normed = part_zero + part_one + part_two
    unit_one = extended * scale_one
    grad_unit_one = grad_normed * norm_one
    grad_extended = scale_one * (
        grad_unit_one - unit_one * jnp.mean(grad_unit_one * unit_one, axis=1, keepdims=True)
    )
    edge_back = shifted(grad_extended[:2], "seq", -1)
    tokens_grad = grad_middle + grad_extended[2:] + jnp.pad(edge_back, ((rows - 2, 0), (0, 0)))

    terms = jnp.stack(
        [
            jnp.sum(grad_normed * unit_one, axis=0),
            norm2_term,
            jnp.sum(grad_mix * normed_own, axis=0),
            jnp.sum(grad_mix * same_one * normed[1:-1], axis=0),
            jnp.sum(grad_mix * same_two * normed[:-2], axis=0),
        ]
    )
    terms = lax.psum(terms, ("seq", "fsdp"))
    terms = lax.dynamic_slice_in_dim(terms, me * slice_width, slice_width, 1)

    layer_out = (live_mask * (middle + feed)).astype(BF)[None]
    return (
        layer_out,
        tokens_grad[None],
        terms[0],
        terms[2:5].T,
        query_total,
        key_total,
        value_total,
        out_total,
        terms[1],
        gate_total,
        up_total,
        down_total,
    )


def solution(mesh):
    placed = (
        P("fsdp", "seq", None),
        P("fsdp", None),
        P("fsdp", None),
        P("fsdp"),
        P("fsdp", None),
        P("fsdp", None),
        P("fsdp", None),
        P("fsdp", None),
        P("fsdp", None),
        P("fsdp"),
        P("fsdp", None),
        P("fsdp", None),
        P("fsdp", None),
        P("fsdp", "seq", None),
    )
    return jax.shard_map(
        shards,
        mesh=mesh,
        in_specs=placed,
        out_specs=(
            P("fsdp", "seq", None),
            P("fsdp", "seq", None),
            P("fsdp"),
            P("fsdp", None),
            P("fsdp", None),
            P("fsdp", None),
            P("fsdp", None),
            P("fsdp", None),
            P("fsdp"),
            P("fsdp", None),
            P("fsdp", None),
            P("fsdp", None),
        ),
        check_vma=False,
    )
```

```python
import functools

import jax
import jax.numpy as jnp
from jax import lax
from jax.experimental import pallas as pl
from jax.experimental.pallas import tpu as pltpu
from jax.sharding import PartitionSpec as P

HEADS = 16
WINDOW = 64
HEAD_DIM = 112
BLOCK = 128

EPS = 1e-05
NEG = -1e30
SCALE = HEAD_DIM ** (-0.5)
MESH_ID = pl.DeviceIdType.MESH
BF = jnp.bfloat16
F32 = jnp.float32


def shifted(array, axis, by):
    length = lax.axis_size(axis)
    pairs = [(i, i + by) for i in range(length) if 0 <= i + by < length]
    return lax.ppermute(array, axis, pairs)


def segment_of(slot, count, lengths, starts):
    found = jnp.full(slot.shape, -1, jnp.int32)
    for j in range(count):
        inside = (slot >= starts(j)) & (slot < starts(j) + lengths(j))
        found = jnp.where(inside, j, found)
    return jnp.where(slot < 0, -2, found)


def dot_rows(left, right):
    return lax.dot_general(left, right, (((0,), (0,)), ((), ())), preferred_element_type=F32)


def dot_trans(left, right):
    return lax.dot_general(left, right, (((1,), (1,)), ((), ())), preferred_element_type=F32)


def dot(left, right):
    return jnp.dot(left, right, preferred_element_type=F32)


def masks_of(first, block, count, length, start):
    rows = first + block * BLOCK
    query = rows + lax.broadcasted_iota(jnp.int32, (BLOCK, 1), 0)
    keys = rows - WINDOW + lax.broadcasted_iota(jnp.int32, (1, BLOCK + WINDOW), 1)
    seg_q = segment_of(query, count, length, start)
    seg_k = segment_of(keys, count, length, start)
    far = query - keys
    return (far >= 0) & (far <= WINDOW) & (seg_q == seg_k)


def soft_of(query, keys, mask):
    scores = dot_trans(query, keys) * SCALE
    scores = jnp.where(mask, scores, NEG)
    peak = jnp.max(scores, axis=1, keepdims=True)
    exponent = jnp.exp(scores - peak)
    return exponent / jnp.sum(exponent, axis=1, keepdims=True)


def lane_head(width):
    return lax.broadcasted_iota(jnp.int32, (1, width), 1) // HEAD_DIM


def remote(src, dst, send, recv, **peer):
    return pltpu.make_async_remote_copy(
        src_ref=src,
        dst_ref=dst,
        send_sem=send,
        recv_sem=recv,
        device_id=peer,
        device_id_type=MESH_ID,
    )


def greet_group(barrier, size):
    me = lax.axis_index("fsdp")
    for step in range(1, size):
        peer = lax.rem(me + step, size)
        pl.semaphore_signal(barrier, inc=1, device_id={"fsdp": peer}, device_id_type=MESH_ID)


class Group:
    def __init__(self, size):
        self.size = size
        self.me = lax.axis_index("fsdp")
        self.square = size == 4
        if self.square:
            x, y = lax.rem(self.me, 2), self.me // 2
            self.at = lambda bx, by: lax.rem(y + by, 2) * 2 + lax.rem(x + bx, 2)
            self.x, self.y, self.far = self.at(1, 0), self.at(0, 1), self.at(1, 1)

    def from_own(self, step):
        if self.square:
            return self.at(lax.rem(step, 2), step // 2)
        return lax.rem(self.me - step + self.size, self.size)

    def to_own(self, step):
        if self.square:
            return self.at(1 - step // 2, 1 - lax.rem(step, 2))
        return lax.rem(self.me + 1 + step, self.size)


class Gather:
    def __init__(self, group, ref, send, recv):
        self.group, self.ref, self.send, self.recv = group, ref, send, recv
        self.half = ref.shape[1] // 2

    def part(self, k, slot, half, peer):
        view = self.ref.at[slot, pl.ds(half * self.half, self.half)]
        return remote(view, view, self.send.at[k], self.recv.at[k], fsdp=peer)

    def whole(self, k):
        g = self.group
        view = self.ref.at[g.me]
        sems = self.send.at[k - 1], self.recv.at[k - 1]
        return remote(view, view, *sems, fsdp=lax.rem(g.me + k, g.size))

    def copy(self, k):
        g = self.group
        if not g.square:
            return self.whole(k + 1)
        slot = (g.me, g.me, g.me, g.me, g.x, g.y)[k]
        half = (0, 1, 0, 1, 0, 1)[k]
        return self.part(k, slot, half, (g.x, g.x, g.y, g.y, g.y, g.x)[k])

    def start_half(self, half):
        if self.group.square:
            self.copy(half).start()
            self.copy(2 + half).start()
        elif half == 1:
            for k in range(self.group.size - 1):
                self.copy(k).start()

    def relay(self):
        if self.group.square:
            self.copy(0).wait_recv()
            self.copy(4).start()
            self.copy(3).wait_recv()
            self.copy(5).start()

    def ready(self, step):
        if not self.group.square:
            self.copy(step - 1).wait_recv()
        elif step == 3:
            self.copy(4).wait_recv()
            self.copy(5).wait_recv()
        else:
            self.copy(step).wait_recv()

    def finish(self):
        for k in range(transfers(self.group.size)):
            self.copy(k).wait_send()


class Scatter:
    def __init__(self, group, part, first, over, joined, last, send, recv):
        self.group, self.part = group, part
        self.first, self.over, self.joined, self.last = first, over, joined, last
        self.send, self.recv = send, recv
        self.half = part.shape[1] // 2

    def copy(self, k):
        g, half = self.group, self.half
        low, high = pl.ds(0, half), pl.ds(half, half)
        if not g.square:
            src, dst, peer = self.part.at[k], self.first.at[k], lax.rem(g.me + 1 + k, g.size)
        else:
            src, dst, peer = (
                lambda: (self.part.at[0, low], self.over.at[0], g.x),
                lambda: (self.part.at[0, high], self.over.at[1], g.y),
                lambda: (self.part.at[1, low], self.first.at[0], g.x),
                lambda: (self.part.at[2, high], self.first.at[1], g.y),
                lambda: (self.joined.at[0], self.last.at[0], g.y),
                lambda: (self.joined.at[1], self.last.at[1], g.x),
            )[k]()
        return remote(src, dst, self.send.at[k], self.recv.at[k], fsdp=peer)

    def made(self, step):
        if not self.group.square:
            self.copy(step).start()
        elif step == 0:
            self.copy(0).start()
            self.copy(1).start()
        elif step in (1, 2):
            self.copy(step + 1).start()

    def join(self):
        if not self.group.square:
            return
        half = self.half
        for k, (step, rows) in enumerate(((2, slice(0, half)), (1, slice(half, 2 * half)))):
            self.copy(k).wait_recv()
            own = self.part[step, rows].astype(F32)
            self.joined[k] = (own + self.over[k].astype(F32)).astype(BF)
            self.copy(4 + k).start()

    def total(self, half):
        count = self.half
        if self.group.square:
            self.copy(2 + half).wait_recv()
            self.copy(4 + half).wait_recv()
            return self.first[half].astype(F32) + self.last[half].astype(F32)
        if half == 0:
            for k in range(self.group.size - 1):
                self.copy(k).wait_recv()
        rows = slice(half * count, (half + 1) * count)
        out = self.first[0, rows].astype(F32)
        for k in range(1, self.group.size - 1):
            out = out + self.first[k, rows].astype(F32)
        return out

    def finish(self):
        for k in range(transfers(self.group.size)):
            self.copy(k).wait_send()


class Line:
    def __init__(self, parts, sems):
        self.rank = lax.axis_index("seq")
        self.parts, self.length = parts, parts // 2
        self.z, self.core = self.rank // 2, lax.rem(self.rank, 2)
        self.above, self.below = self.rank + 2, self.rank - 2
        self.beside = self.rank + 1 - 2 * self.core
        self.has_above, self.has_below = self.z < self.length - 1, self.z > 0
        self.sems = sems

    def greet(self, barrier):
        def one(peer):
            pl.semaphore_signal(barrier, inc=1, device_id={"seq": peer}, device_id_type=MESH_ID)

        one(self.beside)
        pl.when(self.has_above)(lambda: one(self.above))
        pl.when(self.has_below)(lambda: one(self.below))
        n, z = self.length, self.z
        return 1 + (2 * n - 2 - z) // n + (z + n - 1) // n

    def up(self, k, owner):
        view = self.view(owner)
        return remote(view, view, self.sems[0].at[k], self.sems[1].at[k], seq=self.above)

    def down(self, k, owner):
        view = self.view(owner)
        return remote(view, view, self.sems[2].at[k], self.sems[3].at[k], seq=self.below)

    def side(self, k, owner):
        view = self.view(owner)
        return remote(view, view, self.sems[4].at[k], self.sems[5].at[k], seq=self.beside)

    def gather(self, view):
        self.view = view
        pl.when(self.has_above)(lambda: self.up(0, self.rank).start())
        pl.when(self.has_below)(lambda: self.down(0, self.rank).start())
        self.side(self.z, self.rank).start()

    def own_up(self):
        pl.when(self.has_above)(lambda: self.up(0, self.rank).start())

    def own_down(self):
        pl.when(self.has_below)(lambda: self.down(0, self.rank).start())

    def relay_up(self, j):
        rank, z = self.rank, self.z

        @pl.when((z >= j) & self.has_above)
        def _():
            self.up(j - 1, rank).wait_recv()
            self.up(j, rank - 2 * j).start()
            self.side(z - j, rank - 2 * j).start()

    def relay_down(self, j):
        rank, z = self.rank, self.z

        @pl.when((z + j < self.length) & self.has_below)
        def _():
            self.down(j - 1, rank).wait_recv()
            self.down(j, rank + 2 * j).start()
            self.side(z + j, rank + 2 * j).start()

    def relay(self, j):
        self.relay_up(j)
        self.relay_down(j)

    def close(self, j):
        rank, z = self.rank, self.z

        @pl.when((z >= j) & (z == self.length - 1))
        def _():
            self.up(j - 1, rank).wait_recv()
            self.side(z - j, rank - 2 * j).start()

        @pl.when((z + j < self.length) & (z == 0))
        def _():
            self.down(j - 1, rank).wait_recv()
            self.side(z + j, rank + 2 * j).start()

    def gathered(self):
        for k in range(self.length):
            self.side(k, self.rank).wait_recv()

    def finish(self):
        rank, z = self.rank, self.z
        for k in range(self.length):
            self.side(k, rank).wait_send()
        pl.when(self.has_above)(lambda: self.up(0, rank).wait_send())
        pl.when(self.has_below)(lambda: self.down(0, rank).wait_send())
        for j in range(1, self.length):
            pl.when((z >= j) & self.has_above)(lambda: self.up(j, rank).wait_send())
            pl.when((z + j < self.length) & self.has_below)(lambda: self.down(j, rank).wait_send())


def line_sems(parts):
    return [pltpu.SemaphoreType.DMA((parts // 2,))] * 6


def transfers(size):
    return 6 if size == 4 else size - 1


def scatter_shapes(size, rows, width):
    half = rows // 2
    slots = (2, half, width) if size == 4 else (size - 1, rows, width)
    return [
        pltpu.VMEM((size - 1, rows, width), BF),
        pltpu.VMEM(slots, BF),
        pltpu.VMEM((2, half, width), BF),
        pltpu.VMEM((2, half, width), BF),
        pltpu.VMEM((2, half, width), BF),
        pltpu.SemaphoreType.DMA((transfers(size),)),
        pltpu.SemaphoreType.DMA((transfers(size),)),
    ]


def each_step(size, body):
    def one(step, carry):
        body(step, lambda k: pl.when(step == k))
        return carry

    lax.fori_loop(0, size, one, 0)


FORWARD_REFS = (
    "tokens",
    "edge_tok",
    "grad",
    "gains",
    "table",
    "qkv_piece",
    "gu_piece",
    "out_map",
    "down_map",
    "gated_hbm",
    "qkv_hbm",
    "edge",
    "qkv_map_hbm",
    "middle",
    "heads",
    "grads_hbm",
    "norm_hbm",
    "hidden_hbm",
    "gu_grad_hbm",
    "gu_map_hbm",
    "gains_all",
    "table_all",
    "part",
    "first",
    "over",
    "joined",
    "last",
    "all",
    "grads",
    "qkv",
    "qkv_map",
    "gu_map",
    "tail",
    "own",
    "hidden",
    "gu_grad",
    "s_send",
    "s_recv",
    "a_send",
    "a_recv",
    "g_send",
    "g_recv",
    "c_send",
    "c_recv",
    "m_send",
    "m_recv",
    "halo_send",
    "halo_recv",
    "loads",
    "stores",
    "hidden_store",
    "gu_store",
)


def forward_kernel(size, parts, count, *refs):
    names = FORWARD_REFS
    r = dict(zip(names, refs))
    sems = refs[len(names) :]
    rank = lax.axis_index("seq")
    rows = r["tokens"].shape[0]
    half = rows // 2
    local = r["out_map"].shape[0]
    inner = r["down_map"].shape[0]
    slot = rank * rows
    group = Group(size)
    me = group.me
    line_q, line_u = Line(parts, sems[:6]), Line(parts, sems[6:])

    barrier = pltpu.get_barrier_semaphore()
    greet_group(barrier, size)
    known = line_q.greet(barrier)

    def greet(peer):
        pl.semaphore_signal(barrier, inc=1, device_id={"seq": peer}, device_id_type=MESH_ID)

    pl.when(line_q.has_above & (line_q.core == 1))(lambda: greet(rank + 1))
    pl.when(line_q.has_below & (line_q.core == 0))(lambda: greet(rank - 1))
    n, z = line_q.length, line_q.z
    known = known + (2 * n - 2 - z) // n * line_q.core + (z + n - 1) // n * (1 - line_q.core)
    own_pieces = [
        pltpu.make_async_copy(src.at[me], dst.at[me, rank], r["loads"].at[k])
        for k, (src, dst) in enumerate(
            ((r["qkv_piece"], r["qkv_map"]), (r["gu_piece"], r["gu_map"]))
        )
    ]
    for copy in own_pieces:
        copy.start()
    r["gains_all"][me] = r["gains"][...]
    r["table_all"][me] = r["table"][...]
    r["grads"][me] = r["grad"][...]
    pl.semaphore_wait(barrier, size - 1 + known)

    def swap(k, step):
        peer = lax.rem(me + step, size)
        src, dst = (
            lambda: (r["gains_all"].at[me], r["gains_all"].at[me]),
            lambda: (r["table_all"].at[me], r["table_all"].at[me]),
            lambda: (r["qkv_piece"].at[peer], r["qkv_map"].at[me, rank]),
            lambda: (r["gu_piece"].at[peer], r["gu_map"].at[me, rank]),
        )[k]()
        return remote(src, dst, r["m_send"].at[k, step - 1], r["m_recv"].at[k, step - 1], fsdp=peer)

    others = range(1, size)
    for k in range(4):
        for step in others:
            swap(k, step).start()
    for k in range(2):
        for step in others:
            swap(k, step).wait_recv()

    gains = jnp.concatenate([r["gains_all"][f] for f in range(size)], 1).astype(F32)
    own_table = r["table_all"][me]
    slots = slot + lax.broadcasted_iota(jnp.int32, (rows, 1), 0)
    length = lambda j: own_table[0:1, j : j + 1]
    start = lambda j: own_table[1:2, j : j + 1]
    segment = segment_of(slots, count, length, start)
    same_one = (segment == segment_of(slots - 1, count, length, start)).astype(F32)
    same_two = (segment == segment_of(slots - 2, count, length, start)).astype(F32)
    tokens = r["tokens"][...].astype(F32)
    edge = r["edge_tok"][...].astype(F32)

    def norm(a):
        return a * lax.rsqrt(jnp.mean(a * a, axis=1, keepdims=True) + EPS) * gains[0:1]

    normed, edge = norm(tokens), norm(edge)
    row = lax.broadcasted_iota(jnp.int32, (rows, 1), 0)
    back_one = jnp.where(row == 0, edge[1:2], pltpu.roll(normed, 1, 0))
    back_two = jnp.where(
        row == 0, edge[0:1], jnp.where(row == 1, edge[1:2], pltpu.roll(normed, 2, 0))
    )
    mixed = (
        normed * gains[2:3]
        + same_one * back_one * gains[3:4]
        + same_two * back_two * gains[4:5]
    )
    all_ref = r["all"]
    all_ref[me] = (mixed * normed).astype(BF)
    gather = Gather(group, all_ref, r["a_send"], r["a_recv"])
    gather.start_half(0)
    gather.start_half(1)

    own_pieces[0].wait()
    for step in others:
        swap(2, step).wait_recv()
    line_q.gather(lambda owner: r["qkv_map"].at[:, owner])
    line_u.view = lambda owner: r["gu_map"].at[:, owner]
    gather.relay()
    grads = Gather(group, r["grads"], r["c_send"], r["c_recv"])
    grads.start_half(0)
    grads.start_half(1)
    own_pieces[1].wait()
    for step in others:
        swap(3, step).wait_recv()
    line_u.side(z, rank).start()
    pl.when(z == 0)(line_u.own_up)
    pl.when(z == n - 1)(line_u.own_down)
    for j in range(1, n):
        line_q.relay(j)
        line_q.close(j)
        pl.when(z == j)(line_u.own_up)
        pl.when(z == n - 1 - j)(line_u.own_down)
    for step in others:
        gather.ready(step)
    grads.relay()
    line_q.gathered()
    keeps = [
        pltpu.make_async_copy(all_ref, r["gated_hbm"], r["stores"].at[size]),
        pltpu.make_async_copy(r["qkv_map"], r["qkv_map_hbm"], r["stores"].at[size + 1]),
    ]
    for keep in keeps:
        keep.start()

    weights = r["qkv_map"][...].reshape(-1, r["qkv_map"].shape[3])

    def halo(step):
        g = group.to_own(step)
        sem = r["halo_send"].at[step], r["halo_recv"].at[step]
        return remote(r["tail"].at[g], r["edge"].at[g], *sem, seq=rank + 1)

    def project(step, is_step):
        g = group.to_own(step)
        out = dot(all_ref[g], weights).astype(BF)
        r["qkv"][g] = out
        r["tail"][g] = out[rows - WINDOW :, local:]
        pl.when(rank < parts - 1)(lambda: halo(step).start())

    each_step(size, project)

    @pl.when(rank == 0)
    def _():
        r["edge"][...] = jnp.zeros_like(r["edge"])

    keeps.append(pltpu.make_async_copy(r["qkv"], r["qkv_hbm"], r["stores"].at[size + 2]))
    keeps[2].start()
    line_u.relay(1)
    gather.finish()
    keeps[0].wait()

    scatter = Scatter(
        group, *(r[k] for k in ("part", "first", "over", "joined", "last", "s_send", "s_recv"))
    )
    head_of = lane_head(local)

    def mix(step, is_step):
        g = group.to_own(step)
        pl.when(rank > 0)(lambda: halo(step).wait_recv())
        own, edge, table = r["qkv"][g], r["edge"][g], r["table_all"][g]
        queries = own[:, :local]
        keys = jnp.concatenate([edge[:, :local], own[:, local : 2 * local]], 0)
        values = jnp.concatenate([edge[:, local:], own[:, 2 * local :]], 0)
        outs = []
        for block in range(rows // BLOCK):
            mask = masks_of(
                slot,
                block,
                count,
                lambda j: table[0:1, j : j + 1],
                lambda j: table[1:2, j : j + 1],
            )
            low = block * BLOCK
            query = queries[low : low + BLOCK]
            key = keys[low : low + BLOCK + WINDOW]
            value = values[low : low + BLOCK + WINDOW]
            out = jnp.zeros((BLOCK, local), F32)
            for head in range(local // HEAD_DIM):
                mine = head_of == head
                soft = soft_of(jnp.where(mine, query, jnp.zeros_like(query)), key, mask)
                out = jnp.where(mine, dot(soft.astype(BF), value), out)
            outs.append(out.astype(BF))
        heads = jnp.concatenate(outs, 0)
        r["heads"][g] = heads
        branch = dot(heads, r["out_map"][...])
        is_step(size - 1)(lambda: r["own"].__setitem__(..., branch))
        pl.when(step < size - 1)(lambda: r["part"].__setitem__(step, branch.astype(BF)))
        for k in range(size - 1):
            is_step(k)(functools.partial(scatter.made, k))

    each_step(size, mix)
    scatter.join()
    for j in range(2, n):
        line_u.relay(j)
    gather = Gather(group, all_ref, r["g_send"], r["g_recv"])
    for h in range(2):
        span = slice(h * half, (h + 1) * half)
        total = r["own"][span, :] + scatter.total(h)
        middle = r["tokens"][span, :].astype(F32) + total
        r["middle"][span, :] = middle
        scale = lax.rsqrt(jnp.mean(middle * middle, axis=1, keepdims=True) + EPS)
        all_ref[me, span] = (middle * scale * gains[1:2]).astype(BF)
        gather.start_half(h)
    gather.relay()
    for j in range(1, n):
        line_u.close(j)
    line_u.gathered()
    keeps.append(pltpu.make_async_copy(r["gu_map"], r["gu_map_hbm"], r["stores"].at[size + 3]))
    keeps[3].start()

    def out_copies(step):
        g, two = group.from_own(step), lax.rem(step, 2)
        return (
            pltpu.make_async_copy(
                r["hidden"].at[two], r["hidden_hbm"].at[g], r["hidden_store"].at[two]
            ),
            pltpu.make_async_copy(
                r["gu_grad"].at[two], r["gu_grad_hbm"].at[g], r["gu_store"].at[two]
            ),
        )

    def norm_copy(g):
        return pltpu.make_async_copy(all_ref.at[g], r["norm_hbm"].at[g], r["stores"].at[g])

    def feed(step, is_step):
        g, two = group.from_own(step), lax.rem(step, 2)
        for k in others:
            is_step(k)(functools.partial(gather.ready, k))
            is_step(k)(functools.partial(grads.ready, k))

        @pl.when(step >= 2)
        def _():
            for copy in out_copies(step - 2):
                copy.wait()

        norm_copy(g).start()
        weights = r["gu_map"][...].reshape(-1, r["gu_map"].shape[3])
        acts = dot(all_ref[g], weights)
        gate, up = acts[:, :inner], acts[:, inner:]
        sigma = jax.nn.sigmoid(gate)
        silu = gate * sigma
        r["hidden"][two] = (silu * up).astype(BF)
        grad_hidden = dot_trans(r["grads"][g], r["down_map"][...])
        grad_gate = grad_hidden * up * sigma * (1.0 + gate * (1.0 - sigma))
        r["gu_grad"][two] = jnp.concatenate([grad_gate, grad_hidden * silu], 1).astype(BF)
        for copy in out_copies(step):
            copy.start()

    each_step(size, feed)
    keeps.append(pltpu.make_async_copy(r["grads"], r["grads_hbm"], r["stores"].at[size + 4]))
    keeps[4].start()
    for k in range(4):
        for step in others:
            swap(k, step).wait_send()
    scatter.finish()
    gather.finish()
    grads.finish()
    line_q.finish()
    line_u.finish()

    @pl.when(rank < parts - 1)
    def _():
        for step in range(size):
            halo(step).wait_send()

    for keep in keeps[1:]:
        keep.wait()
    for g in range(size):
        norm_copy(g).wait()
    for step in (size - 2, size - 1):
        for copy in out_copies(step):
            copy.wait()


def forward_part(ident, count, tokens, edge, grad, gains, table, qkv_piece, gu_piece, out_weight, down_weight):
    size, parts = lax.axis_size("fsdp"), lax.axis_size("seq")
    rows, width = tokens.shape
    local, inner = out_weight.shape[0], down_weight.shape[0]
    piece, cols = gu_piece.shape[1:]
    vmem = pl.BlockSpec(memory_space=pltpu.VMEM)
    hbm = pl.BlockSpec(memory_space=pl.ANY)
    shape = lambda w: (size, rows, w)
    low = lambda s: jax.ShapeDtypeStruct(s, BF)
    maps = [(size, parts, piece, 3 * local), (size, parts, piece, cols)]
    dma = lambda *s: pltpu.SemaphoreType.DMA(s)
    hop = transfers(size)
    scratch = scatter_shapes(size, rows, width)
    return pl.pallas_call(
        functools.partial(forward_kernel, size, parts, count),
        out_shape=[
            low(shape(width)),
            low(shape(3 * local)),
            low((size, WINDOW, 2 * local)),
            low(maps[0]),
            jax.ShapeDtypeStruct((rows, width), F32),
            low(shape(local)),
            low(shape(width)),
            low(shape(width)),
            low(shape(inner)),
            low(shape(cols)),
            low(maps[1]),
            low((size,) + gains.shape),
            jax.ShapeDtypeStruct((size,) + table.shape, jnp.int32),
        ],
        in_specs=[vmem] * 5 + [hbm, hbm, vmem, vmem],
        out_specs=[hbm, hbm, vmem, hbm, vmem, vmem, hbm, hbm, hbm, hbm, hbm, vmem, vmem],
        scratch_shapes=scratch[:-2]
        + [
            pltpu.VMEM(shape(width), BF),
            pltpu.VMEM(shape(width), BF),
            pltpu.VMEM(shape(3 * local), BF),
            pltpu.VMEM(maps[0], BF),
            pltpu.VMEM(maps[1], BF),
            pltpu.VMEM((size, WINDOW, 2 * local), BF),
            pltpu.VMEM((rows, width), F32),
            pltpu.VMEM((2, rows, inner), BF),
            pltpu.VMEM((2, rows, cols), BF),
        ]
        + [dma(hop)] * 8
        + [dma(4, size - 1)] * 2
        + [dma(size)] * 2
        + [dma(2), dma(size + 5), dma(2), dma(2)]
        + line_sems(parts)
        + line_sems(parts),
        compiler_params=pltpu.CompilerParams(
            collective_id=ident, has_side_effects=True, vmem_limit_bytes=67_000_000
        ),
        cost_estimate=pl.CostEstimate(
            flops=2 * size * rows * width * (4 * local + 3 * inner),
            bytes_accessed=500_000_000,
            transcendentals=0,
        ),
        name="forward_part",
    )(tokens, edge, grad, gains, table, qkv_piece, gu_piece, out_weight, down_weight)


def heads_back(group, slot, count, lens_ref, starts_ref, own, edge, grad):
    rows, local = own.shape[0], own.shape[1] // 3
    head_of = lane_head(local)
    queries = own[:, :local]
    keys = jnp.concatenate([edge[:, :local], own[:, local : 2 * local]], 0)
    values = jnp.concatenate([edge[:, local:], own[:, 2 * local :]], 0)
    dqs, dks, dvs = [], [], []
    for block in range(rows // BLOCK):
        mask = masks_of(
            slot, block, count, lambda j: lens_ref[group, j], lambda j: starts_ref[group, j]
        )
        low = block * BLOCK
        span = slice(low, low + BLOCK + WINDOW)
        query, grads = queries[low : low + BLOCK], grad[low : low + BLOCK]
        key, value = keys[span], values[span]
        dq = jnp.zeros((BLOCK, local), F32)
        dk = jnp.zeros((BLOCK + WINDOW, local), F32)
        dv = jnp.zeros((BLOCK + WINDOW, local), F32)
        for head in range(local // HEAD_DIM):
            mine = head_of == head
            own_q = jnp.where(mine, query, jnp.zeros_like(query))
            own_g = jnp.where(mine, grads, jnp.zeros_like(grads))
            soft = soft_of(own_q, key, mask)
            grad_soft = dot_trans(own_g, value)
            total = jnp.sum(grad_soft * soft, axis=1, keepdims=True)
            grad_scores = (soft * (grad_soft - total)).astype(BF)
            dq = jnp.where(mine, dot(grad_scores, key), dq)
            dk = dk + dot_rows(grad_scores, own_q)
            dv = dv + dot_rows(soft.astype(BF), own_g)
        dqs.append(dq * SCALE)
        dks.append(dk * SCALE)
        dvs.append(dv)

    def joined(pieces):
        out = [pieces[0][:BLOCK]]
        for left, right in zip(pieces, pieces[1:]):
            out.append(left[BLOCK:] + right[:WINDOW])
            out.append(right[WINDOW:BLOCK])
        out.append(pieces[-1][BLOCK:])
        return jnp.concatenate(out, 0)

    return jnp.concatenate(dqs, 0), joined(dks), joined(dvs)


def back_kernel(size, parts, count, lens_ref, starts_ref, grad_gu_hbm, gu_map_hbm, middle_ref, grad_ref,
                gain_ref, out_map_ref, edge_ref, qkv_ref, qkv_map_hbm,
                grad_middle_ref, norm_ref, all_ref, dqkv_ref, own_ref,
                part, first, over, joined, last, s_send, s_recv, t_send, t_recv, g_send, g_recv,
                grad_gu_ref, gu_map_ref, qkv_map_ref, dedge_ref, back_ref, tail_ref, h_send, h_recv, loads):
    rows = middle_ref.shape[0]
    local = out_map_ref.shape[0]
    rank = lax.axis_index("seq")
    slot = rank * rows
    group = Group(size)
    barrier = pltpu.get_barrier_semaphore()
    greet_group(barrier, size)

    def greet(peer):
        pl.semaphore_signal(barrier, inc=1, device_id={"seq": peer}, device_id_type=MESH_ID)

    pl.when(rank > 0)(lambda: greet(rank - 1))
    pl.when(rank < parts - 1)(lambda: greet(rank + 1))
    fetches = [
        pltpu.make_async_copy(src, dst, loads.at[k])
        for k, (src, dst) in enumerate(
            ((grad_gu_hbm, grad_gu_ref), (gu_map_hbm, gu_map_ref), (qkv_map_hbm, qkv_map_ref))
        )
    ]
    for fetch in fetches:
        fetch.start()
    has_next = (2 * parts - 2 - rank) // parts
    has_last = (rank + parts - 1) // parts
    pl.semaphore_wait(barrier, size - 1 + has_next + has_last)
    scatter = Scatter(group, part, first, over, joined, last, s_send, s_recv)
    gather = Gather(group, all_ref, g_send, g_recv)
    fetches[0].wait()
    fetches[1].wait()

    def step_two(step, is_step):
        partial = dot_trans(grad_gu_ref[group.to_own(step)], gu_map_ref[...])
        is_step(size - 1)(lambda: own_ref.__setitem__(..., partial))
        pl.when(step < size - 1)(lambda: part.__setitem__(step, partial.astype(BF)))
        for k in range(size - 1):
            is_step(k)(functools.partial(scatter.made, k))

    each_step(size, step_two)
    scatter.join()
    half = rows // 2
    norm_sum = jnp.zeros((1, middle_ref.shape[1]), F32)
    for h in range(2):
        span = slice(h * half, (h + 1) * half)
        grad = own_ref[span, :] + scatter.total(h)
        middle = middle_ref[span, :]
        scale = lax.rsqrt(jnp.mean(middle * middle, axis=1, keepdims=True) + EPS)
        unit = middle * scale
        scaled = grad * gain_ref[...]
        norm_sum = norm_sum + jnp.sum(grad * unit, axis=0, keepdims=True)
        grad_out = grad_ref[span, :].astype(F32)
        grad_middle = grad_out + scale * (
            scaled - unit * jnp.mean(scaled * unit, axis=1, keepdims=True)
        )
        grad_middle_ref[span, :] = grad_middle
        all_ref[group.me, span] = grad_middle.astype(BF)
        gather.start_half(h)
    norm_ref[...] = norm_sum

    def halo(step):
        g = group.from_own(step)
        sems = h_send.at[step], h_recv.at[step]
        return remote(dedge_ref.at[g], back_ref.at[g], *sems, seq=rank - 1)

    def step_heads(step, is_step):
        g = group.from_own(step)

        @is_step(1)
        def _():
            gather.relay()

        for k in range(1, size):
            is_step(k)(functools.partial(gather.ready, k))
        grad = dot_trans(all_ref[g], out_map_ref[...]).astype(BF)
        dq, dk, dv = heads_back(
            g, slot, count, lens_ref, starts_ref, qkv_ref[g], edge_ref[g], grad
        )
        dedge_ref[g] = jnp.concatenate([dk[:WINDOW], dv[:WINDOW]], 1).astype(BF)
        full = jnp.concatenate([dq, dk[WINDOW:], dv[WINDOW:]], 1)
        dqkv_ref[g] = full.astype(BF)
        tail_ref[g] = full[rows - WINDOW :]
        pl.when(rank > 0)(lambda: halo(step).start())

    each_step(size, step_heads)
    scatter.finish()
    fetches[2].wait()

    @pl.when(rank == parts - 1)
    def _():
        back_ref[...] = jnp.zeros_like(back_ref)

    @pl.when(rank < parts - 1)
    def _():
        for step in range(size):
            halo(step).wait_recv()

    scatter = Scatter(group, part, first, over, joined, last, t_send, t_recv)

    def step_one(step, is_step):
        g = group.to_own(step)
        back = back_ref[g].astype(F32)
        wide = jnp.concatenate([jnp.zeros((WINDOW, local), F32), back], 1)
        dqkv_ref[g, pl.ds(rows - WINDOW, WINDOW)] = (tail_ref[g] + wide).astype(BF)
        partial = dot_trans(dqkv_ref[g], qkv_map_ref[...])
        is_step(size - 1)(lambda: own_ref.__setitem__(..., partial))
        pl.when(step < size - 1)(lambda: part.__setitem__(step, partial.astype(BF)))
        for k in range(size - 1):
            is_step(k)(functools.partial(scatter.made, k))

    each_step(size, step_one)
    scatter.join()
    for h in range(2):
        span = slice(h * half, (h + 1) * half)
        own_ref[span, :] = own_ref[span, :] + scatter.total(h)
    scatter.finish()
    gather.finish()

    @pl.when(rank > 0)
    def _():
        for step in range(size):
            halo(step).wait_send()


def back_part(ident, lens, starts, grad_gu, gu_map, middle, grad, gain, out_weight, edge, qkv, qkv_map):
    size, parts = lax.axis_size("fsdp"), lax.axis_size("seq")
    rows, width = middle.shape
    local = out_weight.shape[0]
    vmem = pl.BlockSpec(memory_space=pltpu.VMEM)
    smem = pl.BlockSpec(memory_space=pltpu.SMEM)
    hbm = pl.BlockSpec(memory_space=pl.ANY)
    sems = [pltpu.SemaphoreType.DMA((transfers(size),))] * 2
    return pl.pallas_call(
        functools.partial(back_kernel, size, parts, lens.shape[1]),
        out_shape=[
            jax.ShapeDtypeStruct((rows, width), F32),
            jax.ShapeDtypeStruct((1, width), F32),
            jax.ShapeDtypeStruct((size, rows, width), BF),
            jax.ShapeDtypeStruct(qkv.shape, BF),
            jax.ShapeDtypeStruct((rows, width), F32),
        ],
        in_specs=[smem, smem, hbm, hbm] + [vmem] * 6 + [hbm],
        out_specs=[vmem] * 5,
        scratch_shapes=scatter_shapes(size, rows, width)
        + sems
        + sems
        + [
            pltpu.VMEM(grad_gu.shape, BF),
            pltpu.VMEM(gu_map.shape, BF),
            pltpu.VMEM(qkv_map.shape, BF),
            pltpu.VMEM((size, WINDOW, 2 * local), BF),
            pltpu.VMEM((size, WINDOW, 2 * local), BF),
            pltpu.VMEM((size, WINDOW, 3 * local), F32),
            pltpu.SemaphoreType.DMA((size,)),
            pltpu.SemaphoreType.DMA((size,)),
            pltpu.SemaphoreType.DMA((3,)),
        ],
        compiler_params=pltpu.CompilerParams(
            collective_id=ident, has_side_effects=True, vmem_limit_bytes=67_000_000
        ),
        cost_estimate=pl.CostEstimate(
            flops=2 * size * rows * (gu_map.size + qkv_map.size + width * local),
            bytes_accessed=400_000_000,
            transcendentals=0,
        ),
        name="back_part",
    )(lens, starts, grad_gu, gu_map, middle, grad, gain, out_weight, edge, qkv, qkv_map)


class LineSum:
    def __init__(self, line, x, pre, acc, up_in, down_in, sems):
        self.line, self.x, self.pre, self.acc = line, x, pre, acc
        self.up_in, self.down_in, self.sems = up_in, down_in, sems

    def share(self, k):
        line = self.line
        src = self.x.at[2 * k + 1 - line.core]
        return remote(src, self.pre.at[k], self.sems[0].at[k], self.sems[1].at[k], seq=line.beside)

    def up(self, k):
        sems = self.sems[2].at[k], self.sems[3].at[k]
        return remote(self.acc.at[k], self.up_in.at[k], *sems, seq=self.line.above)

    def down(self, k):
        sems = self.sems[4].at[k], self.sems[5].at[k]
        return remote(self.acc.at[k], self.down_in.at[k], *sems, seq=self.line.below)

    def order(self):
        n = self.line.length
        return [k // 2 if k % 2 else n - 1 - k // 2 for k in range(n)]

    def trade(self):
        for k in self.order():
            self.share(k).start()

    def merge(self):
        line = self.line
        for k in self.order():
            self.share(k).wait_recv()
            own = self.x[2 * k + line.core].astype(F32)
            self.acc[k] = (own + self.pre[k].astype(F32)).astype(BF)
            if k > 0:
                pl.when(line.z == 0)(lambda: self.up(k).start())
            if k < line.length - 1:
                pl.when(line.z == line.length - 1)(lambda: self.down(k).start())

    def add(self, k, more):
        self.acc[k] = (self.acc[k].astype(F32) + more[k].astype(F32)).astype(BF)

    def pass_up(self, k):
        z = self.line.z

        @pl.when((z > 0) & (z < k))
        def _():
            self.up(k).wait_recv()
            self.add(k, self.up_in)
            self.up(k).start()

    def pass_down(self, k):
        z = self.line.z

        @pl.when((z < self.line.length - 1) & (z > k))
        def _():
            self.down(k).wait_recv()
            self.add(k, self.down_in)
            self.down(k).start()

    def total(self):
        z = self.line.z

        @pl.when(z > 0)
        def _():
            self.up(z).wait_recv()
            self.add(z, self.up_in)

        @pl.when(z < self.line.length - 1)
        def _():
            self.down(z).wait_recv()
            self.add(z, self.down_in)

    def finish(self):
        for k in range(self.line.length):
            self.share(k).wait_send()
            pl.when(k > self.line.z)(lambda: self.up(k).wait_send())
            pl.when(k < self.line.z)(lambda: self.down(k).wait_send())


CLOSE_REFS = (
    "x",
    "gu_piece",
    "terms",
    "hidden",
    "down_map",
    "every_hbm",
    "gu_every_hbm",
    "feed",
    "terms_out",
    "part",
    "first",
    "over",
    "joined",
    "last",
    "pre",
    "acc",
    "up_in",
    "down_in",
    "every",
    "slots",
    "gu_every",
    "terms_in",
    "terms_all",
    "s_send",
    "s_recv",
    "m_send",
    "m_recv",
    "t_send",
    "t_recv",
    "loads",
)


def close_kernel(size, parts, *refs):
    r = dict(zip(CLOSE_REFS, refs))
    sems = refs[len(CLOSE_REFS) :]
    rank = lax.axis_index("seq")
    group = Group(size)
    me = group.me
    line_u, line_q = Line(parts, sems[:6]), Line(parts, sems[6:12])
    n, z = line_q.length, line_q.z
    sums = LineSum(line_q, *(r[k] for k in ("x", "pre", "acc", "up_in", "down_in")), sems[12:])
    rows = r["feed"].shape[0]
    half = rows // 2
    barrier = pltpu.get_barrier_semaphore()
    greet_group(barrier, size)
    for step in range(1, parts):
        peer = lax.rem(rank + step, parts)
        pl.semaphore_signal(barrier, inc=1, device_id={"seq": peer}, device_id_type=MESH_ID)
    own_piece = pltpu.make_async_copy(
        r["gu_piece"].at[me], r["gu_every"].at[rank, me], r["loads"].at[0]
    )
    own_piece.start()
    r["terms_in"][me] = r["terms"][me]
    pl.semaphore_wait(barrier, size + parts - 2)
    sums.trade()

    def swap(k, step):
        peer = lax.rem(me + step, size)
        src, dst = (
            lambda: (r["gu_piece"].at[peer], r["gu_every"].at[rank, me]),
            lambda: (r["terms"].at[peer], r["terms_in"].at[me]),
            lambda: (r["acc"].at[z, peer], r["slots"].at[me]),
        )[k]()
        return remote(src, dst, r["m_send"].at[k, step - 1], r["m_recv"].at[k, step - 1], fsdp=peer)

    others = range(1, size)
    for k in range(2):
        for step in others:
            swap(k, step).start()

    scatter = Scatter(
        group, *(r[k] for k in ("part", "first", "over", "joined", "last", "s_send", "s_recv"))
    )

    def down(step, is_step):
        partial = dot(r["hidden"][group.to_own(step)], r["down_map"][...])
        is_step(size - 1)(lambda: r["feed"].__setitem__(..., partial))
        pl.when(step < size - 1)(lambda: r["part"].__setitem__(step, partial.astype(BF)))
        for k in range(size - 1):
            is_step(k)(functools.partial(scatter.made, k))

    each_step(size, down)
    sums.merge()
    own_piece.wait()
    for step in others:
        swap(0, step).wait_recv()
    line_u.gather(lambda owner: r["gu_every"].at[owner])

    for step in others:
        swap(1, step).wait_recv()
    small = r["terms_in"][0]
    for f in others:
        small = small + r["terms_in"][f]
    r["terms_all"][rank] = small

    def spread(step):
        peer = lax.rem(rank + step, parts)
        view = r["terms_all"].at[rank]
        return remote(view, view, r["t_send"].at[step - 1], r["t_recv"].at[step - 1], seq=peer)

    for step in range(1, parts):
        spread(step).start()
    scatter.join()

    for k in range(n - 1):
        sums.pass_up(n - 1 - k)
        sums.pass_down(k)
        if k == 0:
            pl.when(z >= 2)(lambda: line_u.relay_up(1))
            pl.when(z <= n - 3)(lambda: line_u.relay_down(1))
    sums.total()
    for step in others:
        swap(2, step).start()
    for h in range(2):
        span = slice(h * half, (h + 1) * half)
        r["feed"][span, :] = r["feed"][span, :] + scatter.total(h)
    pl.when(z < 2)(lambda: line_u.relay_up(1))
    pl.when(z > n - 3)(lambda: line_u.relay_down(1))
    r["slots"][me] = r["acc"][z, me]
    for step in others:
        swap(2, step).wait_recv()
    local = r["x"].shape[3] // 4
    lane = lax.broadcasted_iota(jnp.int32, (1, 1, 4 * local), 2)
    r["every"][rank] = jnp.where(lane < 3 * local, r["slots"][...], r["acc"][z])
    line_q.gather(lambda owner: r["every"].at[owner])
    for j in range(2, n):
        line_u.relay(j)
        line_q.relay(j - 1)
    for j in range(1, n):
        line_u.close(j)
    line_u.gathered()
    stores = [pltpu.make_async_copy(r["gu_every"], r["gu_every_hbm"], r["loads"].at[0])]
    stores[0].start()
    line_q.relay(n - 1)
    for j in range(1, n):
        line_q.close(j)
    line_q.gathered()
    stores.append(pltpu.make_async_copy(r["every"], r["every_hbm"], r["loads"].at[1]))
    stores[1].start()
    for step in range(1, parts):
        spread(step).wait_recv()
    small = r["terms_all"][0]
    for k in range(1, parts):
        small = small + r["terms_all"][k]
    r["terms_out"][...] = small
    for k in range(3):
        for step in others:
            swap(k, step).wait_send()
    for step in range(1, parts):
        spread(step).wait_send()
    scatter.finish()
    sums.finish()
    line_u.finish()
    line_q.finish()
    for store in stores:
        store.wait()


def close_part(ident, packed, gu_piece, terms, hidden, down_weight):
    parts, size, piece, cols = packed.shape
    n = parts // 2
    rows, width = hidden.shape[1], down_weight.shape[1]
    vmem = pl.BlockSpec(memory_space=pltpu.VMEM)
    hbm = pl.BlockSpec(memory_space=pl.ANY)
    dma = lambda *s: pltpu.SemaphoreType.DMA(s)
    gu_shape = (parts,) + gu_piece.shape
    scratch = scatter_shapes(size, rows, width)
    chips = pltpu.VMEM((n, size, piece, cols), BF)
    return pl.pallas_call(
        functools.partial(close_kernel, size, parts),
        out_shape=[
            jax.ShapeDtypeStruct(packed.shape, BF),
            jax.ShapeDtypeStruct(gu_shape, BF),
            jax.ShapeDtypeStruct((rows, width), F32),
            jax.ShapeDtypeStruct(terms.shape[1:], F32),
        ],
        in_specs=[vmem, hbm, vmem, vmem, vmem],
        out_specs=[hbm, hbm, vmem, vmem],
        scratch_shapes=scratch[:-2]
        + [
            chips,
            chips,
            chips,
            chips,
            pltpu.VMEM(packed.shape, BF),
            pltpu.VMEM((size, piece, cols), BF),
            pltpu.VMEM(gu_shape, BF),
            pltpu.VMEM(terms.shape, F32),
            pltpu.VMEM((parts,) + terms.shape[1:], F32),
        ]
        + scratch[-2:]
        + [dma(3, size - 1)] * 2
        + [dma(parts - 1)] * 2
        + [dma(2)]
        + line_sems(parts) * 3,
        compiler_params=pltpu.CompilerParams(
            collective_id=ident, has_side_effects=True, vmem_limit_bytes=67_000_000
        ),
        cost_estimate=pl.CostEstimate(
            flops=2 * size * rows * down_weight.size, bytes_accessed=500_000_000, transcendentals=0
        ),
        name="close_part",
    )(packed, gu_piece, terms, hidden, down_weight)


def pack_kernel(size, parts, x_ref, g_ref, *refs):
    out_ref = refs[-1]
    full = dot_rows(x_ref[...], g_ref[...])
    pair = out_ref.shape[1]
    rows = full.shape[0] // pair
    piece = rows // parts
    for k in range(pair):
        own = full[k * rows : (k + 1) * rows]
        if len(refs) == 3:
            heads_ref, gb_ref = refs[0], refs[1]
            side = dot_rows(heads_ref[...], gb_ref[...])
            wide = side.shape[1] // pair
            own = jnp.concatenate([own, side[:, k * wide : (k + 1) * wide]], 1)
        out_ref[:, k] = own.astype(BF).reshape(parts, piece, own.shape[1])


def pack_grads(parts, size, x, g, heads=None, gb=None):
    width, cols = x.shape[1], g.shape[1]
    rows = width // size
    piece = rows // parts
    if piece % 8 or (2 * rows) % 128:
        full = dot_rows(x, g).reshape(size, parts, piece, cols)
        if heads is not None:
            side = dot_rows(heads, gb).reshape(parts, piece, size, -1).transpose(2, 0, 1, 3)
            full = jnp.concatenate([full, side], 3)
        return full.transpose(1, 0, 2, 3).astype(BF)
    total = x.shape[0]
    pair = pl.BlockSpec((total, 2 * rows), lambda i: (0, i))
    whole = lambda a: pl.BlockSpec(a.shape, lambda i: (0, 0), pipeline_mode=pl.Buffered(1))
    args, specs = [x, g], [pair, whole(g)]
    out_cols = cols
    if heads is not None:
        args += [heads, gb]
        specs += [whole(heads), pair]
        out_cols += rows
    return pl.pallas_call(
        functools.partial(pack_kernel, size, parts),
        grid=(size // 2,),
        out_shape=jax.ShapeDtypeStruct((parts, size, piece, out_cols), BF),
        in_specs=specs,
        out_specs=pl.BlockSpec((parts, 2, piece, out_cols), lambda i: (0, i, 0, 0)),
        cost_estimate=pl.CostEstimate(
            flops=2 * total * width * out_cols,
            bytes_accessed=2 * (x.size + g.size + width * out_cols),
            transcendentals=0,
        ),
        name="pack_grads",
    )(*args)


def unpack_kernel(widths, every_ref, *outs):
    size = every_ref.shape[1]
    blocks = [every_ref[0, i].astype(F32) for i in range(size)]
    low = 0
    for width, out in zip(widths, outs):
        out[...] = jnp.concatenate([b[:, low : low + width] for b in blocks], 1)
        low += width


def unpack_grads(every, widths):
    parts, size, piece, cols = every.shape
    if piece % 8:
        outs, low = [], 0
        for width in widths:
            block = every[:, :, :, low : low + width].transpose(0, 2, 1, 3)
            outs.append(block.reshape(parts * piece, size * width).astype(F32))
            low += width
        return outs
    return pl.pallas_call(
        functools.partial(unpack_kernel, widths),
        grid=(parts,),
        out_shape=[jax.ShapeDtypeStruct((parts * piece, size * w), F32) for w in widths],
        in_specs=[pl.BlockSpec((1, size, piece, cols), lambda i: (i, 0, 0, 0))],
        out_specs=[pl.BlockSpec((piece, size * w), lambda i: (i, 0)) for w in widths],
        cost_estimate=pl.CostEstimate(flops=0, bytes_accessed=every.size * 6, transcendentals=0),
        name="unpack_grads",
    )(every)


def columns_piece(weights, part, parts):
    size = lax.axis_size("fsdp")
    rows = weights[0].shape[0] // parts
    pieces = []
    for weight in weights:
        own = lax.dynamic_slice_in_dim(weight, part * rows, rows, 0)
        pieces.append(own.reshape(rows, size, -1))
    return jnp.concatenate(pieces, 2).transpose(1, 0, 2)


def shards(
    tokens,
    seq_lengths,
    seq_offsets,
    norm1_gain,
    conv_weight,
    query_weight,
    key_weight,
    value_weight,
    out_weight,
    norm2_gain,
    gate_weight,
    up_weight,
    down_weight,
    cotangent,
):
    size = lax.axis_size("fsdp")
    parts = lax.axis_size("seq")
    part = lax.axis_index("seq")
    me = lax.axis_index("fsdp")
    own_tokens = tokens[0]
    rows, width = own_tokens.shape
    slice_width = norm1_gain.shape[0]
    first_slot = part * rows
    count = seq_lengths.shape[1]

    slot_ext = first_slot - 2 + jnp.arange(rows + 2, dtype=jnp.int32)
    segment_ext = segment_of(
        slot_ext, count, lambda j: seq_lengths[0, j], lambda j: seq_offsets[0, j]
    )
    segment_own = segment_ext[2:]
    same_one = (segment_own == segment_ext[1:-1]).astype(F32)[:, None]
    same_two = (segment_own == segment_ext[:-2]).astype(F32)[:, None]
    live_mask = (segment_own >= 0).astype(F32)[:, None]

    gains = jnp.concatenate(
        [
            norm1_gain[None],
            norm2_gain[None],
            conv_weight.T,
            jnp.zeros((3, slice_width), BF),
        ],
        0,
    )
    table = jnp.zeros((8, 128), jnp.int32)
    table = table.at[0, :count].set(seq_lengths[0]).at[1, :count].set(seq_offsets[0])
    qkv_piece = columns_piece((query_weight, key_weight, value_weight), part, parts)
    gu_piece = columns_piece((gate_weight, up_weight), part, parts)
    edge_tokens = shifted(own_tokens[rows - 2 :], "seq", 1)
    grad_down = (cotangent[0].astype(F32) * live_mask).astype(BF)
    (
        gated_all,
        qkv,
        edge,
        qkv_map,
        middle,
        heads_out,
        grad_down_all,
        normed_all,
        hidden,
        grad_gu,
        gu_map,
        gains_all,
        table_all,
    ) = forward_part(
        0,
        count,
        own_tokens,
        jnp.pad(edge_tokens, ((0, 6), (0, 0))),
        grad_down,
        gains,
        table,
        qkv_piece,
        gu_piece,
        out_weight,
        down_weight,
    )
    local = out_weight.shape[0]
    flat = lambda a: a.reshape(-1, a.shape[-1])
    lens_all, starts_all = table_all[:, 0, :count], table_all[:, 1, :count]
    gains_all = gains_all.transpose(1, 0, 2).reshape(8, width)
    norm_one = gains_all[0].astype(F32)
    norm_two = gains_all[1].astype(F32)
    taps = gains_all[2:5].astype(F32)
    qkv_map, gu_map = qkv_map.reshape(width, -1), gu_map.reshape(width, -1)
    grad_down_all = flat(grad_down_all)

    extended = jnp.concatenate([edge_tokens, own_tokens], 0).astype(F32)
    scale_one = lax.rsqrt(jnp.mean(extended * extended, axis=1, keepdims=True) + EPS)
    normed = extended * scale_one * norm_one
    conv_mix = (
        normed[2:] * taps[0]
        + same_one * normed[1:-1] * taps[1]
        + same_two * normed[:-2] * taps[2]
    )

    gu_packed = pack_grads(parts, size, flat(normed_all), flat(grad_gu))
    gu_packed, grad_gu = lax.optimization_barrier((gu_packed, grad_gu))
    gu_piece = lax.psum_scatter(gu_packed, "seq", scatter_dimension=0)
    down_sum = dot_rows(flat(hidden), grad_down_all).astype(BF)
    grad_gu, down_sum = lax.optimization_barrier((grad_gu, down_sum))
    down_total = lax.psum(down_sum, "seq").astype(F32)
    grad_middle, norm2_term, grad_branch_all, dqkv, grad_gated = back_part(
        4,
        lens_all,
        starts_all,
        grad_gu,
        gu_map,
        middle,
        grad_down,
        norm_two[None],
        out_weight,
        edge,
        qkv,
        qkv_map,
    )
    norm2_term = norm2_term[0]
    qkvo_packed = pack_grads(
        parts, size, flat(gated_all), flat(dqkv), flat(heads_out), flat(grad_branch_all)
    )

    normed_own = normed[2:]
    grad_mix = grad_gated * normed_own
    part_zero = jnp.pad(grad_gated * conv_mix + grad_mix * taps[0], ((2, 0), (0, 0)))
    part_one = jnp.pad(grad_mix * same_one * taps[1], ((1, 1), (0, 0)))
    part_two = jnp.pad(grad_mix * same_two * taps[2], ((0, 2), (0, 0)))
    grad_normed = part_zero + part_one + part_two
    unit_one = extended * scale_one
    grad_unit_one = grad_normed * norm_one
    grad_extended = scale_one * (
        grad_unit_one - unit_one * jnp.mean(grad_unit_one * unit_one, axis=1, keepdims=True)
    )
    edge_back = shifted(grad_extended[:2], "seq", -1)
    tokens_grad = grad_middle + grad_extended[2:] + jnp.pad(edge_back, ((rows - 2, 0), (0, 0)))

    terms = jnp.stack(
        [
            jnp.sum(grad_normed * unit_one, axis=0),
            norm2_term,
            jnp.sum(grad_mix * normed_own, axis=0),
            jnp.sum(grad_mix * same_one * normed[1:-1], axis=0),
            jnp.sum(grad_mix * same_two * normed[:-2], axis=0),
        ]
    )
    terms = jnp.pad(terms, ((0, 3), (0, 0))).reshape(8, size, slice_width).transpose(1, 0, 2)
    qkvo_packed, gu_piece, terms, down_total, tokens_grad = lax.optimization_barrier(
        (qkvo_packed, gu_piece, terms, down_total, tokens_grad)
    )
    qkvo_every, gu_every, feed, terms = close_part(
        5, qkvo_packed, gu_piece, terms, hidden, down_weight
    )
    gate_total, up_total = unpack_grads(gu_every, (gu_map.shape[1] // 2,) * 2)
    query_total, key_total, value_total, out_total = unpack_grads(qkvo_every, (local,) * 4)

    layer_out = (live_mask * (middle + feed)).astype(BF)[None]
    return (
        layer_out,
        tokens_grad[None],
        terms[0],
        terms[2:5].T,
        query_total,
        key_total,
        value_total,
        out_total,
        terms[1],
        gate_total,
        up_total,
        down_total,
    )


def solution(mesh):
    placed = (
        P("fsdp", "seq", None),
        P("fsdp", None),
        P("fsdp", None),
        P("fsdp"),
        P("fsdp", None),
        P("fsdp", None),
        P("fsdp", None),
        P("fsdp", None),
        P("fsdp", None),
        P("fsdp"),
        P("fsdp", None),
        P("fsdp", None),
        P("fsdp", None),
        P("fsdp", "seq", None),
    )
    return jax.shard_map(
        shards,
        mesh=mesh,
        in_specs=placed,
        out_specs=(
            P("fsdp", "seq", None),
            P("fsdp", "seq", None),
            P("fsdp"),
            P("fsdp", None),
            P("fsdp", None),
            P("fsdp", None),
            P("fsdp", None),
            P("fsdp", None),
            P("fsdp"),
            P("fsdp", None),
            P("fsdp", None),
            P("fsdp", None),
        ),
        check_vma=False,
    )
```

```python
import functools
from typing import Any, NamedTuple

import jax
import jax.numpy as jnp
from jax import lax
from jax.experimental import pallas as pl
from jax.experimental.pallas import tpu as pltpu
from jax.sharding import PartitionSpec as P

HEADS = 16
WINDOW = 64
HEAD_DIM = 112
BLOCK = 128

EPS = 1e-05
NEG = -1e30
SCALE = HEAD_DIM ** (-0.5)
MESH_ID = pl.DeviceIdType.MESH
BF = jnp.bfloat16
F32 = jnp.float32


def shifted(array, axis, by):
    length = lax.axis_size(axis)
    pairs = [(i, i + by) for i in range(length) if 0 <= i + by < length]
    return lax.ppermute(array, axis, pairs)


def segment_of(slot, count, lengths, starts):
    found = jnp.full(slot.shape, -1, jnp.int32)
    for j in range(count):
        inside = (slot >= starts(j)) & (slot < starts(j) + lengths(j))
        found = jnp.where(inside, j, found)
    return jnp.where(slot < 0, -2, found)


def dot_rows(left, right):
    return lax.dot_general(left, right, (((0,), (0,)), ((), ())), preferred_element_type=F32)


def dot_trans(left, right):
    return lax.dot_general(left, right, (((1,), (1,)), ((), ())), preferred_element_type=F32)


def dot(left, right):
    return jnp.dot(left, right, preferred_element_type=F32)


def masks_of(first, block, count, length, start):
    rows = first + block * BLOCK
    query = rows + lax.broadcasted_iota(jnp.int32, (BLOCK, 1), 0)
    keys = rows - WINDOW + lax.broadcasted_iota(jnp.int32, (1, BLOCK + WINDOW), 1)
    seg_q = segment_of(query, count, length, start)
    seg_k = segment_of(keys, count, length, start)
    far = query - keys
    return (far >= 0) & (far <= WINDOW) & (seg_q == seg_k)


def soft_of(query, keys, mask):
    scores = dot_trans(query, keys) * SCALE
    scores = jnp.where(mask, scores, NEG)
    peak = jnp.max(scores, axis=1, keepdims=True)
    exponent = jnp.exp(scores - peak)
    return exponent / jnp.sum(exponent, axis=1, keepdims=True)


def lane_head(width):
    return lax.broadcasted_iota(jnp.int32, (1, width), 1) // HEAD_DIM


def remote(src, dst, send, recv, **peer):
    return pltpu.make_async_remote_copy(
        src_ref=src,
        dst_ref=dst,
        send_sem=send,
        recv_sem=recv,
        device_id=peer,
        device_id_type=MESH_ID,
    )


def greet_group(barrier, size):
    me = lax.axis_index("fsdp")
    for step in range(1, size):
        peer = lax.rem(me + step, size)
        pl.semaphore_signal(barrier, inc=1, device_id={"fsdp": peer}, device_id_type=MESH_ID)


class Group:
    def __init__(self, size):
        self.size = size
        self.me = lax.axis_index("fsdp")
        self.square = size == 4
        if self.square:
            x, y = lax.rem(self.me, 2), self.me // 2
            self.at = lambda bx, by: lax.rem(y + by, 2) * 2 + lax.rem(x + bx, 2)
            self.x, self.y, self.far = self.at(1, 0), self.at(0, 1), self.at(1, 1)

    def from_own(self, step):
        if self.square:
            return self.at(lax.rem(step, 2), step // 2)
        return lax.rem(self.me - step + self.size, self.size)

    def to_own(self, step):
        if self.square:
            return self.at(1 - step // 2, 1 - lax.rem(step, 2))
        return lax.rem(self.me + 1 + step, self.size)


class Gather:
    def __init__(self, group, ref, send, recv):
        self.group, self.ref, self.send, self.recv = group, ref, send, recv
        self.half = ref.shape[1] // 2

    def part(self, k, slot, half, peer):
        view = self.ref.at[slot, pl.ds(half * self.half, self.half)]
        return remote(view, view, self.send.at[k], self.recv.at[k], fsdp=peer)

    def whole(self, k):
        g = self.group
        view = self.ref.at[g.me]
        sems = self.send.at[k - 1], self.recv.at[k - 1]
        return remote(view, view, *sems, fsdp=lax.rem(g.me + k, g.size))

    def copy(self, k):
        g = self.group
        if not g.square:
            return self.whole(k + 1)
        slot = (g.me, g.me, g.me, g.me, g.x, g.y)[k]
        half = (0, 1, 0, 1, 0, 1)[k]
        return self.part(k, slot, half, (g.x, g.x, g.y, g.y, g.y, g.x)[k])

    def start_half(self, half):
        if self.group.square:
            self.copy(half).start()
            self.copy(2 + half).start()
        elif half == 1:
            for k in range(self.group.size - 1):
                self.copy(k).start()

    def relay(self):
        if self.group.square:
            self.copy(0).wait_recv()
            self.copy(4).start()
            self.copy(3).wait_recv()
            self.copy(5).start()

    def ready(self, step):
        if not self.group.square:
            self.copy(step - 1).wait_recv()
        elif step == 3:
            self.copy(4).wait_recv()
            self.copy(5).wait_recv()
        else:
            self.copy(step).wait_recv()

    def finish(self):
        for k in range(transfers(self.group.size)):
            self.copy(k).wait_send()


class Scatter:
    def __init__(self, group, part, first, over, joined, last, send, recv):
        self.group, self.part = group, part
        self.first, self.over, self.joined, self.last = first, over, joined, last
        self.send, self.recv = send, recv
        self.half = part.shape[1] // 2

    def copy(self, k):
        g, half = self.group, self.half
        low, high = pl.ds(0, half), pl.ds(half, half)
        if not g.square:
            src, dst, peer = self.part.at[k], self.first.at[k], lax.rem(g.me + 1 + k, g.size)
        else:
            src, dst, peer = (
                lambda: (self.part.at[0, low], self.over.at[0], g.x),
                lambda: (self.part.at[0, high], self.over.at[1], g.y),
                lambda: (self.part.at[1, low], self.first.at[0], g.x),
                lambda: (self.part.at[2, high], self.first.at[1], g.y),
                lambda: (self.joined.at[0], self.last.at[0], g.y),
                lambda: (self.joined.at[1], self.last.at[1], g.x),
            )[k]()
        return remote(src, dst, self.send.at[k], self.recv.at[k], fsdp=peer)

    def made(self, step):
        if not self.group.square:
            self.copy(step).start()
        elif step == 0:
            self.copy(0).start()
            self.copy(1).start()
        elif step in (1, 2):
            self.copy(step + 1).start()

    def join(self):
        if not self.group.square:
            return
        half = self.half
        for k, (step, rows) in enumerate(((2, slice(0, half)), (1, slice(half, 2 * half)))):
            self.copy(k).wait_recv()
            own = self.part[step, rows].astype(F32)
            self.joined[k] = (own + self.over[k].astype(F32)).astype(BF)
            self.copy(4 + k).start()

    def total(self, half):
        count = self.half
        if self.group.square:
            self.copy(2 + half).wait_recv()
            self.copy(4 + half).wait_recv()
            return self.first[half].astype(F32) + self.last[half].astype(F32)
        if half == 0:
            for k in range(self.group.size - 1):
                self.copy(k).wait_recv()
        rows = slice(half * count, (half + 1) * count)
        out = self.first[0, rows].astype(F32)
        for k in range(1, self.group.size - 1):
            out = out + self.first[k, rows].astype(F32)
        return out

    def finish(self):
        for k in range(transfers(self.group.size)):
            self.copy(k).wait_send()


class Line:
    def __init__(self, parts, sems):
        self.rank = lax.axis_index("seq")
        self.parts, self.length = parts, parts // 2
        self.z, self.core = self.rank // 2, lax.rem(self.rank, 2)
        self.above, self.below = self.rank + 2, self.rank - 2
        self.beside = self.rank + 1 - 2 * self.core
        self.has_above, self.has_below = self.z < self.length - 1, self.z > 0
        self.sems = sems

    def greet(self, barrier):
        def one(peer):
            pl.semaphore_signal(barrier, inc=1, device_id={"seq": peer}, device_id_type=MESH_ID)

        one(self.beside)
        pl.when(self.has_above)(lambda: one(self.above))
        pl.when(self.has_below)(lambda: one(self.below))
        n, z = self.length, self.z
        return 1 + (2 * n - 2 - z) // n + (z + n - 1) // n

    def up(self, k, owner):
        view = self.view(owner)
        return remote(view, view, self.sems[0].at[k], self.sems[1].at[k], seq=self.above)

    def down(self, k, owner):
        view = self.view(owner)
        return remote(view, view, self.sems[2].at[k], self.sems[3].at[k], seq=self.below)

    def side(self, k, owner):
        view = self.view(owner)
        return remote(view, view, self.sems[4].at[k], self.sems[5].at[k], seq=self.beside)

    def gather(self, view):
        self.view = view
        pl.when(self.has_above)(lambda: self.up(0, self.rank).start())
        pl.when(self.has_below)(lambda: self.down(0, self.rank).start())
        self.side(self.z, self.rank).start()

    def own_up(self):
        pl.when(self.has_above)(lambda: self.up(0, self.rank).start())

    def own_down(self):
        pl.when(self.has_below)(lambda: self.down(0, self.rank).start())

    def relay_up(self, j):
        rank, z = self.rank, self.z

        @pl.when((z >= j) & self.has_above)
        def _():
            self.up(j - 1, rank).wait_recv()
            self.up(j, rank - 2 * j).start()
            self.side(z - j, rank - 2 * j).start()

    def relay_down(self, j):
        rank, z = self.rank, self.z

        @pl.when((z + j < self.length) & self.has_below)
        def _():
            self.down(j - 1, rank).wait_recv()
            self.down(j, rank + 2 * j).start()
            self.side(z + j, rank + 2 * j).start()

    def relay(self, j):
        self.relay_up(j)
        self.relay_down(j)

    def close(self, j):
        rank, z = self.rank, self.z

        @pl.when((z >= j) & (z == self.length - 1))
        def _():
            self.up(j - 1, rank).wait_recv()
            self.side(z - j, rank - 2 * j).start()

        @pl.when((z + j < self.length) & (z == 0))
        def _():
            self.down(j - 1, rank).wait_recv()
            self.side(z + j, rank + 2 * j).start()

    def gathered(self):
        for k in range(self.length):
            self.side(k, self.rank).wait_recv()

    def finish(self):
        rank, z = self.rank, self.z
        for k in range(self.length):
            self.side(k, rank).wait_send()
        pl.when(self.has_above)(lambda: self.up(0, rank).wait_send())
        pl.when(self.has_below)(lambda: self.down(0, rank).wait_send())
        for j in range(1, self.length):
            pl.when((z >= j) & self.has_above)(lambda: self.up(j, rank).wait_send())
            pl.when((z + j < self.length) & self.has_below)(lambda: self.down(j, rank).wait_send())


class LineSum:
    def __init__(self, line, x, pre, acc, up_in, down_in, sems):
        self.line, self.x, self.pre, self.acc = line, x, pre, acc
        self.up_in, self.down_in, self.sems = up_in, down_in, sems

    def share(self, k):
        line = self.line
        src = self.x.at[2 * k + 1 - line.core]
        return remote(src, self.pre.at[k], self.sems[0].at[k], self.sems[1].at[k], seq=line.beside)

    def up(self, k):
        sems = self.sems[2].at[k], self.sems[3].at[k]
        return remote(self.acc.at[k], self.up_in.at[k], *sems, seq=self.line.above)

    def down(self, k):
        sems = self.sems[4].at[k], self.sems[5].at[k]
        return remote(self.acc.at[k], self.down_in.at[k], *sems, seq=self.line.below)

    def pair(self, m):
        return self.line.length - 1 - m, m

    def trade(self):
        n = self.line.length
        for m in range((n + 1) // 2):
            for k in sorted(set(self.pair(m))):
                self.share(k).start()

    def merge(self, k):
        self.share(k).wait_recv()
        own = self.x[2 * k + self.line.core].astype(F32)
        self.acc[k] = (own + self.pre[k].astype(F32)).astype(BF)

    def begin(self, m):
        n, z = self.line.length, self.line.z
        far, near = self.pair(m)
        if m < (n + 1) // 2:
            for k in sorted({far, near}):
                self.merge(k)
        if m < n - 1:
            pl.when(z == 0)(lambda: self.up(far).start())
            pl.when(z == n - 1)(lambda: self.down(near).start())

    def add(self, k, more):
        self.acc[k] = (self.acc[k].astype(F32) + more[k].astype(F32)).astype(BF)

    def advance(self, m):
        z, n = self.line.z, self.line.length
        far, near = self.pair(m)

        @pl.when((z > 0) & (z < far))
        def _():
            self.up(far).wait_recv()
            self.add(far, self.up_in)
            self.up(far).start()

        @pl.when((z < n - 1) & (z > near))
        def _():
            self.down(near).wait_recv()
            self.add(near, self.down_in)
            self.down(near).start()

    def total(self):
        z = self.line.z

        @pl.when(z > 0)
        def _():
            self.up(z).wait_recv()
            self.add(z, self.up_in)

        @pl.when(z < self.line.length - 1)
        def _():
            self.down(z).wait_recv()
            self.add(z, self.down_in)

    def finish(self):
        for k in range(self.line.length):
            self.share(k).wait_send()
            pl.when(k > self.line.z)(lambda: self.up(k).wait_send())
            pl.when(k < self.line.z)(lambda: self.down(k).wait_send())


class StagedSum(LineSum):
    def __init__(self, stage, load, *args):
        super().__init__(*args)
        self.stage, self.load = stage, load

    def fetch(self, slot, src):
        return pltpu.make_async_copy(src, self.stage.at[slot], self.load.at[slot])

    def merge(self, k):
        self.share(k).wait_recv()
        own = self.fetch(0, self.x.at[2 * k + self.line.core])
        other = self.fetch(1, self.pre.at[k])
        own.start()
        other.start()
        own.wait()
        other.wait()
        self.acc[k] = (self.stage[0].astype(F32) + self.stage[1].astype(F32)).astype(BF)

    def add(self, k, more):
        came = self.fetch(0, more.at[k])
        came.start()
        came.wait()
        self.acc[k] = (self.acc[k].astype(F32) + self.stage[0].astype(F32)).astype(BF)


def line_sems(parts):
    return [pltpu.SemaphoreType.DMA((parts // 2,))] * 6


def transfers(size):
    return 6 if size == 4 else size - 1


def scatter_shapes(size, rows, width):
    half = rows // 2
    slots = (2, half, width) if size == 4 else (size - 1, rows, width)
    return [
        pltpu.VMEM((size - 1, rows, width), BF),
        pltpu.VMEM(slots, BF),
        pltpu.VMEM((2, half, width), BF),
        pltpu.VMEM((2, half, width), BF),
        pltpu.VMEM((2, half, width), BF),
        pltpu.SemaphoreType.DMA((transfers(size),)),
        pltpu.SemaphoreType.DMA((transfers(size),)),
    ]


def each_step(size, body):
    def one(step, carry):
        body(step, lambda k: pl.when(step == k))
        return carry

    lax.fori_loop(0, size, one, 0)


class ForwardRefs(NamedTuple):
    tokens: Any
    edge_tok: Any
    grad: Any
    gains: Any
    table: Any
    qkv_piece: Any
    gu_piece: Any
    out_map: Any
    down_map: Any
    gated_hbm: Any
    qkv_hbm: Any
    edge: Any
    qkv_map_hbm: Any
    middle: Any
    heads: Any
    grads_hbm: Any
    norm_hbm: Any
    hidden_hbm: Any
    gu_grad_hbm: Any
    gu_map_hbm: Any
    gains_all: Any
    table_all: Any
    part: Any
    first: Any
    over: Any
    joined: Any
    last: Any
    all: Any
    grads: Any
    qkv: Any
    qkv_map: Any
    gu_map: Any
    tail: Any
    own: Any
    hidden: Any
    gu_grad: Any
    s_send: Any
    s_recv: Any
    a_send: Any
    a_recv: Any
    g_send: Any
    g_recv: Any
    c_send: Any
    c_recv: Any
    m_send: Any
    m_recv: Any
    halo_send: Any
    halo_recv: Any
    loads: Any
    stores: Any
    hidden_store: Any
    gu_store: Any


def forward_kernel(size, parts, count, *refs):
    named = len(ForwardRefs._fields)
    r, sems = ForwardRefs(*refs[:named]), refs[named:]
    rank = lax.axis_index("seq")
    rows = r.tokens.shape[0]
    half = rows // 2
    local = r.out_map.shape[0]
    inner = r.down_map.shape[0]
    slot = rank * rows
    group = Group(size)
    me = group.me
    line_q, line_u = Line(parts, sems[:6]), Line(parts, sems[6:])

    barrier = pltpu.get_barrier_semaphore()
    greet_group(barrier, size)
    known = line_q.greet(barrier)

    def greet(peer):
        pl.semaphore_signal(barrier, inc=1, device_id={"seq": peer}, device_id_type=MESH_ID)

    pl.when(line_q.has_above & (line_q.core == 1))(lambda: greet(rank + 1))
    pl.when(line_q.has_below & (line_q.core == 0))(lambda: greet(rank - 1))
    n, z = line_q.length, line_q.z
    known = known + (2 * n - 2 - z) // n * line_q.core + (z + n - 1) // n * (1 - line_q.core)
    own_pieces = [
        pltpu.make_async_copy(src.at[me], dst.at[me, rank], r.loads.at[k])
        for k, (src, dst) in enumerate(
            ((r.qkv_piece, r.qkv_map), (r.gu_piece, r.gu_map))
        )
    ]
    for copy in own_pieces:
        copy.start()
    r.gains_all[me] = r.gains[...]
    r.table_all[me] = r.table[...]
    r.grads[me] = r.grad[...]
    pl.semaphore_wait(barrier, size - 1 + known)

    def swap(k, step):
        peer = lax.rem(me + step, size)
        src, dst = (
            lambda: (r.gains_all.at[me], r.gains_all.at[me]),
            lambda: (r.table_all.at[me], r.table_all.at[me]),
            lambda: (r.qkv_piece.at[peer], r.qkv_map.at[me, rank]),
            lambda: (r.gu_piece.at[peer], r.gu_map.at[me, rank]),
        )[k]()
        return remote(src, dst, r.m_send.at[k, step - 1], r.m_recv.at[k, step - 1], fsdp=peer)

    others = range(1, size)
    for k in range(4):
        for step in others:
            swap(k, step).start()
    for k in range(2):
        for step in others:
            swap(k, step).wait_recv()

    gains = jnp.concatenate([r.gains_all[f] for f in range(size)], 1).astype(F32)
    own_table = r.table_all[me]
    slots = slot + lax.broadcasted_iota(jnp.int32, (rows, 1), 0)
    length = lambda j: own_table[0:1, j : j + 1]
    start = lambda j: own_table[1:2, j : j + 1]
    segment = segment_of(slots, count, length, start)
    same_one = (segment == segment_of(slots - 1, count, length, start)).astype(F32)
    same_two = (segment == segment_of(slots - 2, count, length, start)).astype(F32)
    tokens = r.tokens[...].astype(F32)
    edge = r.edge_tok[...].astype(F32)

    def norm(a):
        return a * lax.rsqrt(jnp.mean(a * a, axis=1, keepdims=True) + EPS) * gains[0:1]

    normed, edge = norm(tokens), norm(edge)
    row = lax.broadcasted_iota(jnp.int32, (rows, 1), 0)
    back_one = jnp.where(row == 0, edge[1:2], pltpu.roll(normed, 1, 0))
    back_two = jnp.where(
        row == 0, edge[0:1], jnp.where(row == 1, edge[1:2], pltpu.roll(normed, 2, 0))
    )
    mixed = (
        normed * gains[2:3]
        + same_one * back_one * gains[3:4]
        + same_two * back_two * gains[4:5]
    )
    all_ref = r.all
    all_ref[me] = (mixed * normed).astype(BF)
    gather = Gather(group, all_ref, r.a_send, r.a_recv)
    gather.start_half(0)
    gather.start_half(1)

    own_pieces[0].wait()
    for step in others:
        swap(2, step).wait_recv()
    line_q.gather(lambda owner: r.qkv_map.at[:, owner])
    line_u.view = lambda owner: r.gu_map.at[:, owner]
    gather.relay()
    grads = Gather(group, r.grads, r.c_send, r.c_recv)
    grads.start_half(0)
    grads.start_half(1)
    own_pieces[1].wait()
    for step in others:
        swap(3, step).wait_recv()
    line_u.side(z, rank).start()
    pl.when(z == 0)(line_u.own_up)
    pl.when(z == n - 1)(line_u.own_down)
    for j in range(1, n):
        line_q.relay(j)
        line_q.close(j)
        pl.when(z == j)(line_u.own_up)
        pl.when(z == n - 1 - j)(line_u.own_down)
    for step in others:
        gather.ready(step)
    grads.relay()
    line_q.gathered()
    keeps = [
        pltpu.make_async_copy(all_ref, r.gated_hbm, r.stores.at[size]),
        pltpu.make_async_copy(r.qkv_map, r.qkv_map_hbm, r.stores.at[size + 1]),
    ]
    for keep in keeps:
        keep.start()

    weights = r.qkv_map[...].reshape(-1, r.qkv_map.shape[3])

    def halo(step):
        g = group.to_own(step)
        sem = r.halo_send.at[step], r.halo_recv.at[step]
        return remote(r.tail.at[g], r.edge.at[g], *sem, seq=rank + 1)

    def project(step, is_step):
        g = group.to_own(step)
        out = dot(all_ref[g], weights).astype(BF)
        r.qkv[g] = out
        r.tail[g] = out[rows - WINDOW :, local:]
        pl.when(rank < parts - 1)(lambda: halo(step).start())

    each_step(size, project)

    @pl.when(rank == 0)
    def _():
        r.edge[...] = jnp.zeros_like(r.edge)

    keeps.append(pltpu.make_async_copy(r.qkv, r.qkv_hbm, r.stores.at[size + 2]))
    keeps[2].start()
    line_u.relay(1)
    gather.finish()
    keeps[0].wait()

    scatter = Scatter(
        group, r.part, r.first, r.over, r.joined, r.last, r.s_send, r.s_recv
    )
    head_of = lane_head(local)

    def mix(step, is_step):
        g = group.to_own(step)
        pl.when(rank > 0)(lambda: halo(step).wait_recv())
        own, edge, table = r.qkv[g], r.edge[g], r.table_all[g]
        queries = own[:, :local]
        keys = jnp.concatenate([edge[:, :local], own[:, local : 2 * local]], 0)
        values = jnp.concatenate([edge[:, local:], own[:, 2 * local :]], 0)
        outs = []
        for block in range(rows // BLOCK):
            mask = masks_of(
                slot,
                block,
                count,
                lambda j: table[0:1, j : j + 1],
                lambda j: table[1:2, j : j + 1],
            )
            low = block * BLOCK
            query = queries[low : low + BLOCK]
            key = keys[low : low + BLOCK + WINDOW]
            value = values[low : low + BLOCK + WINDOW]
            out = jnp.zeros((BLOCK, local), F32)
            for head in range(local // HEAD_DIM):
                mine = head_of == head
                soft = soft_of(jnp.where(mine, query, jnp.zeros_like(query)), key, mask)
                out = jnp.where(mine, dot(soft.astype(BF), value), out)
            outs.append(out.astype(BF))
        heads = jnp.concatenate(outs, 0)
        r.heads[g] = heads
        branch = dot(heads, r.out_map[...])
        is_step(size - 1)(lambda: r.own.__setitem__(..., branch))
        pl.when(step < size - 1)(lambda: r.part.__setitem__(step, branch.astype(BF)))
        for k in range(size - 1):
            is_step(k)(functools.partial(scatter.made, k))

    each_step(size, mix)
    scatter.join()
    for j in range(2, n):
        line_u.relay(j)
    gather = Gather(group, all_ref, r.g_send, r.g_recv)
    for h in range(2):
        span = slice(h * half, (h + 1) * half)
        total = r.own[span, :] + scatter.total(h)
        middle = r.tokens[span, :].astype(F32) + total
        r.middle[span, :] = middle
        scale = lax.rsqrt(jnp.mean(middle * middle, axis=1, keepdims=True) + EPS)
        all_ref[me, span] = (middle * scale * gains[1:2]).astype(BF)
        gather.start_half(h)
    gather.relay()
    for j in range(1, n):
        line_u.close(j)
    line_u.gathered()
    keeps.append(pltpu.make_async_copy(r.gu_map, r.gu_map_hbm, r.stores.at[size + 3]))
    keeps[3].start()

    def out_copies(step):
        g, two = group.from_own(step), lax.rem(step, 2)
        return (
            pltpu.make_async_copy(
                r.hidden.at[two], r.hidden_hbm.at[g], r.hidden_store.at[two]
            ),
            pltpu.make_async_copy(
                r.gu_grad.at[two], r.gu_grad_hbm.at[g], r.gu_store.at[two]
            ),
        )

    def norm_copy(g):
        return pltpu.make_async_copy(all_ref.at[g], r.norm_hbm.at[g], r.stores.at[g])

    def feed(step, is_step):
        g, two = group.from_own(step), lax.rem(step, 2)
        for k in others:
            is_step(k)(functools.partial(gather.ready, k))
            is_step(k)(functools.partial(grads.ready, k))

        @pl.when(step >= 2)
        def _():
            for copy in out_copies(step - 2):
                copy.wait()

        norm_copy(g).start()
        weights = r.gu_map[...].reshape(-1, r.gu_map.shape[3])
        acts = dot(all_ref[g], weights)
        gate, up = acts[:, :inner], acts[:, inner:]
        sigma = jax.nn.sigmoid(gate)
        silu = gate * sigma
        r.hidden[two] = (silu * up).astype(BF)
        grad_hidden = dot_trans(r.grads[g], r.down_map[...])
        grad_gate = grad_hidden * up * sigma * (1.0 + gate * (1.0 - sigma))
        r.gu_grad[two] = jnp.concatenate([grad_gate, grad_hidden * silu], 1).astype(BF)
        for copy in out_copies(step):
            copy.start()

    each_step(size, feed)
    keeps.append(pltpu.make_async_copy(r.grads, r.grads_hbm, r.stores.at[size + 4]))
    keeps[4].start()
    for k in range(4):
        for step in others:
            swap(k, step).wait_send()
    scatter.finish()
    gather.finish()
    grads.finish()
    line_q.finish()
    line_u.finish()

    @pl.when(rank < parts - 1)
    def _():
        for step in range(size):
            halo(step).wait_send()

    for keep in keeps[1:]:
        keep.wait()
    for g in range(size):
        norm_copy(g).wait()
    for step in (size - 2, size - 1):
        for copy in out_copies(step):
            copy.wait()


def forward_part(ident, count, tokens, edge, grad, gains, table, qkv_piece, gu_piece, out_weight, down_weight):
    size, parts = lax.axis_size("fsdp"), lax.axis_size("seq")
    rows, width = tokens.shape
    local, inner = out_weight.shape[0], down_weight.shape[0]
    piece, cols = gu_piece.shape[1:]
    vmem = pl.BlockSpec(memory_space=pltpu.VMEM)
    hbm = pl.BlockSpec(memory_space=pl.ANY)
    shape = lambda w: (size, rows, w)
    low = lambda s: jax.ShapeDtypeStruct(s, BF)
    maps = [(size, parts, piece, 3 * local), (size, parts, piece, cols)]
    dma = lambda *s: pltpu.SemaphoreType.DMA(s)
    hop = transfers(size)
    scratch = scatter_shapes(size, rows, width)
    return pl.pallas_call(
        functools.partial(forward_kernel, size, parts, count),
        out_shape=[
            low(shape(width)),
            low(shape(3 * local)),
            low((size, WINDOW, 2 * local)),
            low(maps[0]),
            jax.ShapeDtypeStruct((rows, width), F32),
            low(shape(local)),
            low(shape(width)),
            low(shape(width)),
            low(shape(inner)),
            low(shape(cols)),
            low(maps[1]),
            low((size,) + gains.shape),
            jax.ShapeDtypeStruct((size,) + table.shape, jnp.int32),
        ],
        in_specs=[vmem] * 5 + [hbm, hbm, vmem, vmem],
        out_specs=[hbm, hbm, vmem, hbm, vmem, vmem, hbm, hbm, hbm, hbm, hbm, vmem, vmem],
        scratch_shapes=scratch[:-2]
        + [
            pltpu.VMEM(shape(width), BF),
            pltpu.VMEM(shape(width), BF),
            pltpu.VMEM(shape(3 * local), BF),
            pltpu.VMEM(maps[0], BF),
            pltpu.VMEM(maps[1], BF),
            pltpu.VMEM((size, WINDOW, 2 * local), BF),
            pltpu.VMEM((rows, width), F32),
            pltpu.VMEM((2, rows, inner), BF),
            pltpu.VMEM((2, rows, cols), BF),
        ]
        + [dma(hop)] * 8
        + [dma(4, size - 1)] * 2
        + [dma(size)] * 2
        + [dma(2), dma(size + 5), dma(2), dma(2)]
        + line_sems(parts)
        + line_sems(parts),
        compiler_params=pltpu.CompilerParams(
            collective_id=ident, has_side_effects=True, vmem_limit_bytes=67_000_000
        ),
        cost_estimate=pl.CostEstimate(
            flops=2 * size * rows * width * (4 * local + 3 * inner),
            bytes_accessed=500_000_000,
            transcendentals=0,
        ),
        name="forward_part",
    )(tokens, edge, grad, gains, table, qkv_piece, gu_piece, out_weight, down_weight)


def heads_back(group, slot, count, lens_ref, starts_ref, own, edge, grad):
    rows, local = own.shape[0], own.shape[1] // 3
    head_of = lane_head(local)
    queries = own[:, :local]
    keys = jnp.concatenate([edge[:, :local], own[:, local : 2 * local]], 0)
    values = jnp.concatenate([edge[:, local:], own[:, 2 * local :]], 0)
    dqs, dks, dvs = [], [], []
    for block in range(rows // BLOCK):
        mask = masks_of(
            slot, block, count, lambda j: lens_ref[group, j], lambda j: starts_ref[group, j]
        )
        low = block * BLOCK
        span = slice(low, low + BLOCK + WINDOW)
        query, grads = queries[low : low + BLOCK], grad[low : low + BLOCK]
        key, value = keys[span], values[span]
        dq = jnp.zeros((BLOCK, local), F32)
        dk = jnp.zeros((BLOCK + WINDOW, local), F32)
        dv = jnp.zeros((BLOCK + WINDOW, local), F32)
        for head in range(local // HEAD_DIM):
            mine = head_of == head
            own_q = jnp.where(mine, query, jnp.zeros_like(query))
            own_g = jnp.where(mine, grads, jnp.zeros_like(grads))
            soft = soft_of(own_q, key, mask)
            grad_soft = dot_trans(own_g, value)
            total = jnp.sum(grad_soft * soft, axis=1, keepdims=True)
            grad_scores = (soft * (grad_soft - total)).astype(BF)
            dq = jnp.where(mine, dot(grad_scores, key), dq)
            dk = dk + dot_rows(grad_scores, own_q)
            dv = dv + dot_rows(soft.astype(BF), own_g)
        dqs.append(dq * SCALE)
        dks.append(dk * SCALE)
        dvs.append(dv)

    def joined(pieces):
        out = [pieces[0][:BLOCK]]
        for left, right in zip(pieces, pieces[1:]):
            out.append(left[BLOCK:] + right[:WINDOW])
            out.append(right[WINDOW:BLOCK])
        out.append(pieces[-1][BLOCK:])
        return jnp.concatenate(out, 0)

    return jnp.concatenate(dqs, 0), joined(dks), joined(dvs)


class BackRefs(NamedTuple):
    lens: Any
    starts: Any
    grad_gu_hbm: Any
    gu_map_hbm: Any
    middle: Any
    grad: Any
    gain: Any
    out_map: Any
    edge: Any
    qkv: Any
    qkv_map_hbm: Any
    gu_x: Any
    down_x: Any
    grad_middle: Any
    norm: Any
    all: Any
    dqkv: Any
    own: Any
    gu_piece: Any
    down_every: Any
    gu_pre: Any
    gu_up: Any
    gu_down: Any
    down_pre: Any
    down_up: Any
    down_down: Any
    part: Any
    first: Any
    over: Any
    joined: Any
    last: Any
    s_send: Any
    s_recv: Any
    t_send: Any
    t_recv: Any
    g_send: Any
    g_recv: Any
    grad_gu: Any
    gu_map: Any
    qkv_map: Any
    dedge: Any
    back: Any
    tail: Any
    h_send: Any
    h_recv: Any
    loads: Any
    gu_acc: Any
    gu_stage: Any
    gu_load: Any
    down_acc: Any
    down_stage: Any
    down_load: Any


def back_kernel(size, parts, count, *refs):
    named = len(BackRefs._fields)
    r, sems = BackRefs(*refs[:named]), refs[named:]
    line = Line(parts, sems[:6])
    gu_sum = StagedSum(
        r.gu_stage, r.gu_load, line, r.gu_x, r.gu_pre, r.gu_acc, r.gu_up, r.gu_down, sems[6:12]
    )
    down_sum = StagedSum(
        r.down_stage,
        r.down_load,
        line,
        r.down_x,
        r.down_pre,
        r.down_acc,
        r.down_up,
        r.down_down,
        sems[12:],
    )
    rows = r.middle.shape[0]
    local = r.out_map.shape[0]
    rank = lax.axis_index("seq")
    slot = rank * rows
    group = Group(size)
    barrier = pltpu.get_barrier_semaphore()
    greet_group(barrier, size)

    def greet(peer):
        pl.semaphore_signal(barrier, inc=1, device_id={"seq": peer}, device_id_type=MESH_ID)

    known = line.greet(barrier)
    pl.when(line.has_above & (line.core == 1))(lambda: greet(rank + 1))
    pl.when(line.has_below & (line.core == 0))(lambda: greet(rank - 1))
    n, z = line.length, line.z
    known = known + (2 * n - 2 - z) // n * line.core + (z + n - 1) // n * (1 - line.core)
    fetches = [
        pltpu.make_async_copy(src, dst, r.loads.at[k])
        for k, (src, dst) in enumerate(
            ((r.grad_gu_hbm, r.grad_gu), (r.gu_map_hbm, r.gu_map), (r.qkv_map_hbm, r.qkv_map))
        )
    ]
    for fetch in fetches:
        fetch.start()
    pl.semaphore_wait(barrier, size - 1 + known)
    down_sum.trade()
    gu_sum.trade()
    scatter = Scatter(
        group, r.part, r.first, r.over, r.joined, r.last, r.s_send, r.s_recv
    )
    gather = Gather(group, r.all, r.g_send, r.g_recv)
    fetches[0].wait()
    fetches[1].wait()

    def step_two(step, is_step):
        partial = dot_trans(r.grad_gu[group.to_own(step)], r.gu_map[...])
        is_step(size - 1)(lambda: r.own.__setitem__(..., partial))
        pl.when(step < size - 1)(lambda: r.part.__setitem__(step, partial.astype(BF)))
        for k in range(size - 1):
            is_step(k)(functools.partial(scatter.made, k))

    each_step(size, step_two)
    for m in range(n):
        down_sum.begin(m)
    scatter.join()
    gu_sum.begin(0)
    half = rows // 2
    norm_sum = jnp.zeros((1, r.middle.shape[1]), F32)
    for h in range(2):
        span = slice(h * half, (h + 1) * half)
        grad = r.own[span, :] + scatter.total(h)
        middle = r.middle[span, :]
        scale = lax.rsqrt(jnp.mean(middle * middle, axis=1, keepdims=True) + EPS)
        unit = middle * scale
        scaled = grad * r.gain[...]
        norm_sum = norm_sum + jnp.sum(grad * unit, axis=0, keepdims=True)
        grad_out = r.grad[span, :].astype(F32)
        grad_middle = grad_out + scale * (
            scaled - unit * jnp.mean(scaled * unit, axis=1, keepdims=True)
        )
        r.grad_middle[span, :] = grad_middle
        r.all[group.me, span] = grad_middle.astype(BF)
        gather.start_half(h)
    r.norm[...] = norm_sum
    for m in range(1, n - 2):
        gu_sum.begin(m)
    down_sum.advance(0)
    own_down = pltpu.make_async_copy(r.down_acc.at[z], r.down_every.at[rank], r.down_load.at[0])
    last_step = size - 1

    def halo(step):
        g = group.from_own(step)
        sems = r.h_send.at[step], r.h_recv.at[step]
        return remote(r.dedge.at[g], r.back.at[g], *sems, seq=rank - 1)

    def step_heads(step, is_step):
        g = group.from_own(step)

        @is_step(1)
        def _():
            gather.relay()
            for m in range(1, n - 1):
                down_sum.advance(m)

        @is_step(2)
        def _():
            down_sum.total()
            own_down.start()
            own_down.wait()
            line.gather(lambda owner: r.down_every.at[owner])
            for m in range(max(1, n - 2), n):
                gu_sum.begin(m)

        @is_step(last_step)
        def _():
            gu_sum.advance(0)

        for k in range(1, size):
            is_step(k)(functools.partial(gather.ready, k))
        grad = dot_trans(r.all[g], r.out_map[...]).astype(BF)
        dq, dk, dv = heads_back(
            g, slot, count, r.lens, r.starts, r.qkv[g], r.edge[g], grad
        )
        r.dedge[g] = jnp.concatenate([dk[:WINDOW], dv[:WINDOW]], 1).astype(BF)
        full = jnp.concatenate([dq, dk[WINDOW:], dv[WINDOW:]], 1)
        r.dqkv[g] = full.astype(BF)
        r.tail[g] = full[rows - WINDOW :]
        pl.when(rank > 0)(lambda: halo(step).start())

    each_step(size, step_heads)
    scatter.finish()
    fetches[2].wait()

    @pl.when(rank == parts - 1)
    def _():
        r.back[...] = jnp.zeros_like(r.back)

    @pl.when(rank < parts - 1)
    def _():
        for step in range(size):
            halo(step).wait_recv()

    scatter = Scatter(
        group, r.part, r.first, r.over, r.joined, r.last, r.t_send, r.t_recv
    )

    def step_one(step, is_step):
        g = group.to_own(step)
        back = r.back[g].astype(F32)
        wide = jnp.concatenate([jnp.zeros((WINDOW, local), F32), back], 1)
        r.dqkv[g, pl.ds(rows - WINDOW, WINDOW)] = (r.tail[g] + wide).astype(BF)
        partial = dot_trans(r.dqkv[g], r.qkv_map[...])
        is_step(size - 1)(lambda: r.own.__setitem__(..., partial))
        pl.when(step < size - 1)(lambda: r.part.__setitem__(step, partial.astype(BF)))
        for k in range(size - 1):
            is_step(k)(functools.partial(scatter.made, k))

    each_step(size, step_one)
    scatter.join()
    line.relay(1)
    for m in range(1, n - 1):
        gu_sum.advance(m)
        line.relay(m + 1)
    for h in range(2):
        span = slice(h * half, (h + 1) * half)
        r.own[span, :] = r.own[span, :] + scatter.total(h)
    gu_sum.total()
    out_piece = pltpu.make_async_copy(r.gu_acc.at[z], r.gu_piece, r.gu_load.at[0])
    out_piece.start()
    for j in range(1, n):
        line.close(j)
    line.gathered()
    scatter.finish()
    gather.finish()
    down_sum.finish()
    gu_sum.finish()
    line.finish()
    out_piece.wait()

    @pl.when(rank > 0)
    def _():
        for step in range(size):
            halo(step).wait_send()


def back_part(
    ident, lens, starts, grad_gu, gu_map, middle, grad, gain, out_weight, edge, qkv, qkv_map, gu_x, down_x
):
    size, parts = lax.axis_size("fsdp"), lax.axis_size("seq")
    rows, width = middle.shape
    local = out_weight.shape[0]
    n = parts // 2
    vmem = pl.BlockSpec(memory_space=pltpu.VMEM)
    smem = pl.BlockSpec(memory_space=pltpu.SMEM)
    hbm = pl.BlockSpec(memory_space=pl.ANY)
    dma = lambda *s: pltpu.SemaphoreType.DMA(s)
    low = lambda *s: jax.ShapeDtypeStruct(s, BF)
    sems = [dma(transfers(size))] * 2
    gu, down = gu_x.shape[1:], down_x.shape[1:]
    outs = pl.pallas_call(
        functools.partial(back_kernel, size, parts, lens.shape[1]),
        out_shape=[
            jax.ShapeDtypeStruct((rows, width), F32),
            jax.ShapeDtypeStruct((1, width), F32),
            low(size, rows, width),
            low(*qkv.shape),
            jax.ShapeDtypeStruct((rows, width), F32),
            low(*gu),
            low(parts, *down),
        ]
        + [low(n, *gu)] * 3
        + [low(n, *down)] * 3,
        in_specs=[smem, smem, hbm, hbm] + [vmem] * 6 + [hbm] * 3,
        out_specs=[vmem] * 5 + [hbm] * 8,
        scratch_shapes=scatter_shapes(size, rows, width)
        + sems
        + sems
        + [
            pltpu.VMEM(grad_gu.shape, BF),
            pltpu.VMEM(gu_map.shape, BF),
            pltpu.VMEM(qkv_map.shape, BF),
            pltpu.VMEM((size, WINDOW, 2 * local), BF),
            pltpu.VMEM((size, WINDOW, 2 * local), BF),
            pltpu.VMEM((size, WINDOW, 3 * local), F32),
            dma(size),
            dma(size),
            dma(3),
            pltpu.VMEM((n,) + gu, BF),
            pltpu.VMEM((2,) + gu, BF),
            dma(2),
            pltpu.VMEM((n,) + down, BF),
            pltpu.VMEM((2,) + down, BF),
            dma(2),
        ]
        + line_sems(parts) * 3,
        compiler_params=pltpu.CompilerParams(
            collective_id=ident, has_side_effects=True, vmem_limit_bytes=67_000_000
        ),
        cost_estimate=pl.CostEstimate(
            flops=2 * size * rows * (gu_map.size + qkv_map.size + width * local),
            bytes_accessed=400_000_000,
            transcendentals=0,
        ),
        name="back_part",
    )(lens, starts, grad_gu, gu_map, middle, grad, gain, out_weight, edge, qkv, qkv_map, gu_x, down_x)
    return outs[:7]


class CloseRefs(NamedTuple):
    x: Any
    gu_piece: Any
    terms: Any
    hidden: Any
    down_map: Any
    every_hbm: Any
    gu_every_hbm: Any
    feed: Any
    terms_out: Any
    part: Any
    first: Any
    over: Any
    joined: Any
    last: Any
    pre: Any
    acc: Any
    up_in: Any
    down_in: Any
    every: Any
    slots: Any
    gu_every: Any
    terms_in: Any
    terms_all: Any
    s_send: Any
    s_recv: Any
    m_send: Any
    m_recv: Any
    t_send: Any
    t_recv: Any
    loads: Any


def close_kernel(size, parts, *refs):
    named = len(CloseRefs._fields)
    r, sems = CloseRefs(*refs[:named]), refs[named:]
    rank = lax.axis_index("seq")
    group = Group(size)
    me = group.me
    line_u, line_q = Line(parts, sems[:6]), Line(parts, sems[6:12])
    n, z = line_q.length, line_q.z
    sums = LineSum(line_q, r.x, r.pre, r.acc, r.up_in, r.down_in, sems[12:])
    rows = r.feed.shape[0]
    half = rows // 2
    barrier = pltpu.get_barrier_semaphore()
    greet_group(barrier, size)
    for step in range(1, parts):
        peer = lax.rem(rank + step, parts)
        pl.semaphore_signal(barrier, inc=1, device_id={"seq": peer}, device_id_type=MESH_ID)
    own_piece = pltpu.make_async_copy(
        r.gu_piece.at[me], r.gu_every.at[rank, me], r.loads.at[0]
    )
    own_piece.start()
    r.terms_in[me] = r.terms[me]
    pl.semaphore_wait(barrier, size + parts - 2)
    sums.trade()

    def swap(k, step):
        peer = lax.rem(me + step, size)
        src, dst = (
            lambda: (r.gu_piece.at[peer], r.gu_every.at[rank, me]),
            lambda: (r.terms.at[peer], r.terms_in.at[me]),
            lambda: (r.acc.at[z, peer], r.slots.at[me]),
        )[k]()
        return remote(src, dst, r.m_send.at[k, step - 1], r.m_recv.at[k, step - 1], fsdp=peer)

    others = range(1, size)
    for k in range(2):
        for step in others:
            swap(k, step).start()

    scatter = Scatter(
        group, r.part, r.first, r.over, r.joined, r.last, r.s_send, r.s_recv
    )

    def down(step, is_step):
        partial = dot(r.hidden[group.to_own(step)], r.down_map[...])
        is_step(size - 1)(lambda: r.feed.__setitem__(..., partial))
        pl.when(step < size - 1)(lambda: r.part.__setitem__(step, partial.astype(BF)))
        for k in range(size - 1):
            is_step(k)(functools.partial(scatter.made, k))

    each_step(size, down)
    for m in range(n):
        sums.begin(m)
    own_piece.wait()
    for step in others:
        swap(0, step).wait_recv()
    line_u.gather(lambda owner: r.gu_every.at[owner])

    for step in others:
        swap(1, step).wait_recv()
    small = r.terms_in[0]
    for f in others:
        small = small + r.terms_in[f]
    r.terms_all[rank] = small

    def spread(step):
        peer = lax.rem(rank + step, parts)
        view = r.terms_all.at[rank]
        return remote(view, view, r.t_send.at[step - 1], r.t_recv.at[step - 1], seq=peer)

    for step in range(1, parts):
        spread(step).start()
    scatter.join()

    for m in range(n - 1):
        sums.advance(m)
        if m == 0:
            pl.when(z >= 2)(lambda: line_u.relay_up(1))
            pl.when(z <= n - 3)(lambda: line_u.relay_down(1))
    sums.total()
    for step in others:
        swap(2, step).start()
    for h in range(2):
        span = slice(h * half, (h + 1) * half)
        r.feed[span, :] = r.feed[span, :] + scatter.total(h)
    pl.when(z < 2)(lambda: line_u.relay_up(1))
    pl.when(z > n - 3)(lambda: line_u.relay_down(1))
    r.slots[me] = r.acc[z, me]
    for step in others:
        swap(2, step).wait_recv()
    local = r.x.shape[3] // 4
    lane = lax.broadcasted_iota(jnp.int32, (1, 1, 4 * local), 2)
    r.every[rank] = jnp.where(lane < 3 * local, r.slots[...], r.acc[z])
    line_q.gather(lambda owner: r.every.at[owner])
    for j in range(2, n):
        line_u.relay(j)
        line_q.relay(j - 1)
    for j in range(1, n):
        line_u.close(j)
    line_u.gathered()
    stores = [pltpu.make_async_copy(r.gu_every, r.gu_every_hbm, r.loads.at[0])]
    stores[0].start()
    line_q.relay(n - 1)
    for j in range(1, n):
        line_q.close(j)
    line_q.gathered()
    stores.append(pltpu.make_async_copy(r.every, r.every_hbm, r.loads.at[1]))
    stores[1].start()
    for step in range(1, parts):
        spread(step).wait_recv()
    small = r.terms_all[0]
    for k in range(1, parts):
        small = small + r.terms_all[k]
    r.terms_out[...] = small
    for k in range(3):
        for step in others:
            swap(k, step).wait_send()
    for step in range(1, parts):
        spread(step).wait_send()
    scatter.finish()
    sums.finish()
    line_u.finish()
    line_q.finish()
    for store in stores:
        store.wait()


def close_part(ident, packed, gu_piece, terms, hidden, down_weight):
    parts, size, piece, cols = packed.shape
    n = parts // 2
    rows, width = hidden.shape[1], down_weight.shape[1]
    vmem = pl.BlockSpec(memory_space=pltpu.VMEM)
    hbm = pl.BlockSpec(memory_space=pl.ANY)
    dma = lambda *s: pltpu.SemaphoreType.DMA(s)
    gu_shape = (parts,) + gu_piece.shape
    scratch = scatter_shapes(size, rows, width)
    chips = pltpu.VMEM((n, size, piece, cols), BF)
    return pl.pallas_call(
        functools.partial(close_kernel, size, parts),
        out_shape=[
            jax.ShapeDtypeStruct(packed.shape, BF),
            jax.ShapeDtypeStruct(gu_shape, BF),
            jax.ShapeDtypeStruct((rows, width), F32),
            jax.ShapeDtypeStruct(terms.shape[1:], F32),
        ],
        in_specs=[vmem, hbm, vmem, vmem, vmem],
        out_specs=[hbm, hbm, vmem, vmem],
        scratch_shapes=scratch[:-2]
        + [
            chips,
            chips,
            chips,
            chips,
            pltpu.VMEM(packed.shape, BF),
            pltpu.VMEM((size, piece, cols), BF),
            pltpu.VMEM(gu_shape, BF),
            pltpu.VMEM(terms.shape, F32),
            pltpu.VMEM((parts,) + terms.shape[1:], F32),
        ]
        + scratch[-2:]
        + [dma(3, size - 1)] * 2
        + [dma(parts - 1)] * 2
        + [dma(2)]
        + line_sems(parts) * 3,
        compiler_params=pltpu.CompilerParams(
            collective_id=ident, has_side_effects=True, vmem_limit_bytes=67_000_000
        ),
        cost_estimate=pl.CostEstimate(
            flops=2 * size * rows * down_weight.size, bytes_accessed=500_000_000, transcendentals=0
        ),
        name="close_part",
    )(packed, gu_piece, terms, hidden, down_weight)


def pack_kernel(size, parts, x_ref, g_ref, *refs):
    out_ref = refs[-1]
    full = dot_rows(x_ref[...], g_ref[...])
    pair = out_ref.shape[1]
    rows = full.shape[0] // pair
    piece = rows // parts
    for k in range(pair):
        own = full[k * rows : (k + 1) * rows]
        if len(refs) == 3:
            heads_ref, gb_ref = refs[0], refs[1]
            side = dot_rows(heads_ref[...], gb_ref[...])
            wide = side.shape[1] // pair
            own = jnp.concatenate([own, side[:, k * wide : (k + 1) * wide]], 1)
        out_ref[:, k] = own.astype(BF).reshape(parts, piece, own.shape[1])


def pack_grads(parts, size, x, g, heads=None, gb=None):
    width, cols = x.shape[1], g.shape[1]
    rows = width // size
    piece = rows // parts
    if piece % 8 or (2 * rows) % 128:
        full = dot_rows(x, g).reshape(size, parts, piece, cols)
        if heads is not None:
            side = dot_rows(heads, gb).reshape(parts, piece, size, -1).transpose(2, 0, 1, 3)
            full = jnp.concatenate([full, side], 3)
        return full.transpose(1, 0, 2, 3).astype(BF)
    total = x.shape[0]
    pair = pl.BlockSpec((total, 2 * rows), lambda i: (0, i))
    whole = lambda a: pl.BlockSpec(a.shape, lambda i: (0, 0), pipeline_mode=pl.Buffered(1))
    args, specs = [x, g], [pair, whole(g)]
    out_cols = cols
    if heads is not None:
        args += [heads, gb]
        specs += [whole(heads), pair]
        out_cols += rows
    return pl.pallas_call(
        functools.partial(pack_kernel, size, parts),
        grid=(size // 2,),
        out_shape=jax.ShapeDtypeStruct((parts, size, piece, out_cols), BF),
        in_specs=specs,
        out_specs=pl.BlockSpec((parts, 2, piece, out_cols), lambda i: (0, i, 0, 0)),
        cost_estimate=pl.CostEstimate(
            flops=2 * total * width * out_cols,
            bytes_accessed=2 * (x.size + g.size + width * out_cols),
            transcendentals=0,
        ),
        name="pack_grads",
    )(*args)


def unpack_kernel(widths, every_ref, *outs):
    size = every_ref.shape[1]
    blocks = [every_ref[0, i].astype(F32) for i in range(size)]
    low = 0
    for width, out in zip(widths, outs):
        out[...] = jnp.concatenate([b[:, low : low + width] for b in blocks], 1)
        low += width


def unpack_grads(every, widths):
    parts, size, piece, cols = every.shape
    if piece % 8:
        outs, low = [], 0
        for width in widths:
            block = every[:, :, :, low : low + width].transpose(0, 2, 1, 3)
            outs.append(block.reshape(parts * piece, size * width).astype(F32))
            low += width
        return outs
    return pl.pallas_call(
        functools.partial(unpack_kernel, widths),
        grid=(parts,),
        out_shape=[jax.ShapeDtypeStruct((parts * piece, size * w), F32) for w in widths],
        in_specs=[pl.BlockSpec((1, size, piece, cols), lambda i: (i, 0, 0, 0))],
        out_specs=[pl.BlockSpec((piece, size * w), lambda i: (i, 0)) for w in widths],
        cost_estimate=pl.CostEstimate(flops=0, bytes_accessed=every.size * 6, transcendentals=0),
        name="unpack_grads",
    )(every)


def columns_piece(weights, part, parts):
    size = lax.axis_size("fsdp")
    rows = weights[0].shape[0] // parts
    pieces = []
    for weight in weights:
        own = lax.dynamic_slice_in_dim(weight, part * rows, rows, 0)
        pieces.append(own.reshape(rows, size, -1))
    return jnp.concatenate(pieces, 2).transpose(1, 0, 2)


def shards(
    tokens,
    seq_lengths,
    seq_offsets,
    norm1_gain,
    conv_weight,
    query_weight,
    key_weight,
    value_weight,
    out_weight,
    norm2_gain,
    gate_weight,
    up_weight,
    down_weight,
    cotangent,
):
    size = lax.axis_size("fsdp")
    parts = lax.axis_size("seq")
    part = lax.axis_index("seq")
    me = lax.axis_index("fsdp")
    own_tokens = tokens[0]
    rows, width = own_tokens.shape
    slice_width = norm1_gain.shape[0]
    first_slot = part * rows
    count = seq_lengths.shape[1]

    slot_ext = first_slot - 2 + jnp.arange(rows + 2, dtype=jnp.int32)
    segment_ext = segment_of(
        slot_ext, count, lambda j: seq_lengths[0, j], lambda j: seq_offsets[0, j]
    )
    segment_own = segment_ext[2:]
    same_one = (segment_own == segment_ext[1:-1]).astype(F32)[:, None]
    same_two = (segment_own == segment_ext[:-2]).astype(F32)[:, None]
    live_mask = (segment_own >= 0).astype(F32)[:, None]

    gains = jnp.concatenate(
        [
            norm1_gain[None],
            norm2_gain[None],
            conv_weight.T,
            jnp.zeros((3, slice_width), BF),
        ],
        0,
    )
    table = jnp.zeros((8, 128), jnp.int32)
    table = table.at[0, :count].set(seq_lengths[0]).at[1, :count].set(seq_offsets[0])
    qkv_piece = columns_piece((query_weight, key_weight, value_weight), part, parts)
    gu_piece = columns_piece((gate_weight, up_weight), part, parts)
    edge_tokens = shifted(own_tokens[rows - 2 :], "seq", 1)
    grad_down = (cotangent[0].astype(F32) * live_mask).astype(BF)
    (
        gated_all,
        qkv,
        edge,
        qkv_map,
        middle,
        heads_out,
        grad_down_all,
        normed_all,
        hidden,
        grad_gu,
        gu_map,
        gains_all,
        table_all,
    ) = forward_part(
        0,
        count,
        own_tokens,
        jnp.pad(edge_tokens, ((0, 6), (0, 0))),
        grad_down,
        gains,
        table,
        qkv_piece,
        gu_piece,
        out_weight,
        down_weight,
    )
    local = out_weight.shape[0]
    flat = lambda a: a.reshape(-1, a.shape[-1])
    lens_all, starts_all = table_all[:, 0, :count], table_all[:, 1, :count]
    gains_all = gains_all.transpose(1, 0, 2).reshape(8, width)
    norm_one = gains_all[0].astype(F32)
    norm_two = gains_all[1].astype(F32)
    taps = gains_all[2:5].astype(F32)
    qkv_map, gu_map = qkv_map.reshape(width, -1), gu_map.reshape(width, -1)
    grad_down_all = flat(grad_down_all)

    extended = jnp.concatenate([edge_tokens, own_tokens], 0).astype(F32)
    scale_one = lax.rsqrt(jnp.mean(extended * extended, axis=1, keepdims=True) + EPS)
    normed = extended * scale_one * norm_one
    conv_mix = (
        normed[2:] * taps[0]
        + same_one * normed[1:-1] * taps[1]
        + same_two * normed[:-2] * taps[2]
    )

    gu_packed = pack_grads(parts, size, flat(normed_all), flat(grad_gu))
    down_packed = dot_rows(flat(hidden), grad_down_all).astype(BF)
    grad_middle, norm2_term, grad_branch_all, dqkv, grad_gated, gu_piece, down_every = back_part(
        4,
        lens_all,
        starts_all,
        grad_gu,
        gu_map,
        middle,
        grad_down,
        norm_two[None],
        out_weight,
        edge,
        qkv,
        qkv_map,
        gu_packed,
        down_packed.reshape(parts, -1, width),
    )
    norm2_term = norm2_term[0]
    down_total = down_every.reshape(-1, width).astype(F32)
    qkvo_packed = pack_grads(
        parts, size, flat(gated_all), flat(dqkv), flat(heads_out), flat(grad_branch_all)
    )

    normed_own = normed[2:]
    grad_mix = grad_gated * normed_own
    part_zero = jnp.pad(grad_gated * conv_mix + grad_mix * taps[0], ((2, 0), (0, 0)))
    part_one = jnp.pad(grad_mix * same_one * taps[1], ((1, 1), (0, 0)))
    part_two = jnp.pad(grad_mix * same_two * taps[2], ((0, 2), (0, 0)))
    grad_normed = part_zero + part_one + part_two
    unit_one = extended * scale_one
    grad_unit_one = grad_normed * norm_one
    grad_extended = scale_one * (
        grad_unit_one - unit_one * jnp.mean(grad_unit_one * unit_one, axis=1, keepdims=True)
    )
    edge_back = shifted(grad_extended[:2], "seq", -1)
    tokens_grad = grad_middle + grad_extended[2:] + jnp.pad(edge_back, ((rows - 2, 0), (0, 0)))

    terms = jnp.stack(
        [
            jnp.sum(grad_normed * unit_one, axis=0),
            norm2_term,
            jnp.sum(grad_mix * normed_own, axis=0),
            jnp.sum(grad_mix * same_one * normed[1:-1], axis=0),
            jnp.sum(grad_mix * same_two * normed[:-2], axis=0),
        ]
    )
    terms = jnp.pad(terms, ((0, 3), (0, 0))).reshape(8, size, slice_width).transpose(1, 0, 2)
    qkvo_packed, gu_piece, terms, down_total, tokens_grad = lax.optimization_barrier(
        (qkvo_packed, gu_piece, terms, down_total, tokens_grad)
    )
    qkvo_every, gu_every, feed, terms = close_part(
        5, qkvo_packed, gu_piece, terms, hidden, down_weight
    )
    gate_total, up_total = unpack_grads(gu_every, (gu_map.shape[1] // 2,) * 2)
    query_total, key_total, value_total, out_total = unpack_grads(qkvo_every, (local,) * 4)

    layer_out = (live_mask * (middle + feed)).astype(BF)[None]
    return (
        layer_out,
        tokens_grad[None],
        terms[0],
        terms[2:5].T,
        query_total,
        key_total,
        value_total,
        out_total,
        terms[1],
        gate_total,
        up_total,
        down_total,
    )


def solution(mesh):
    placed = (
        P("fsdp", "seq", None),
        P("fsdp", None),
        P("fsdp", None),
        P("fsdp"),
        P("fsdp", None),
        P("fsdp", None),
        P("fsdp", None),
        P("fsdp", None),
        P("fsdp", None),
        P("fsdp"),
        P("fsdp", None),
        P("fsdp", None),
        P("fsdp", None),
        P("fsdp", "seq", None),
    )
    return jax.shard_map(
        shards,
        mesh=mesh,
        in_specs=placed,
        out_specs=(
            P("fsdp", "seq", None),
            P("fsdp", "seq", None),
            P("fsdp"),
            P("fsdp", None),
            P("fsdp", None),
            P("fsdp", None),
            P("fsdp", None),
            P("fsdp", None),
            P("fsdp"),
            P("fsdp", None),
            P("fsdp", None),
            P("fsdp", None),
        ),
        check_vma=False,
    )
```

```python
import functools
from typing import Any, NamedTuple

import jax
import jax.numpy as jnp
from jax import lax
from jax.experimental import pallas as pl
from jax.experimental.pallas import tpu as pltpu
from jax.sharding import PartitionSpec as P

HEADS = 16
WINDOW = 64
HEAD_DIM = 112
BLOCK = 128

EPS = 1e-05
NEG = -1e30
SCALE = HEAD_DIM ** (-0.5)
MESH_ID = pl.DeviceIdType.MESH
BF = jnp.bfloat16
F32 = jnp.float32


def shifted(array, axis, by):
    length = lax.axis_size(axis)
    pairs = [(i, i + by) for i in range(length) if 0 <= i + by < length]
    return lax.ppermute(array, axis, pairs)


def segment_of(slot, count, lengths, starts):
    found = jnp.full(slot.shape, -1, jnp.int32)
    for j in range(count):
        inside = (slot >= starts(j)) & (slot < starts(j) + lengths(j))
        found = jnp.where(inside, j, found)
    return jnp.where(slot < 0, -2, found)


def dot_rows(left, right):
    return lax.dot_general(left, right, (((0,), (0,)), ((), ())), preferred_element_type=F32)


def dot_trans(left, right):
    return lax.dot_general(left, right, (((1,), (1,)), ((), ())), preferred_element_type=F32)


def dot(left, right):
    return jnp.dot(left, right, preferred_element_type=F32)


def masks_of(first, block, count, length, start):
    rows = first + block * BLOCK
    query = rows + lax.broadcasted_iota(jnp.int32, (BLOCK, 1), 0)
    keys = rows - WINDOW + lax.broadcasted_iota(jnp.int32, (1, BLOCK + WINDOW), 1)
    seg_q = segment_of(query, count, length, start)
    seg_k = segment_of(keys, count, length, start)
    far = query - keys
    return (far >= 0) & (far <= WINDOW) & (seg_q == seg_k)


def soft_of(query, keys, mask):
    scores = dot_trans(query, keys) * SCALE
    scores = jnp.where(mask, scores, NEG)
    peak = jnp.max(scores, axis=1, keepdims=True)
    exponent = jnp.exp(scores - peak)
    return exponent / jnp.sum(exponent, axis=1, keepdims=True)


def lane_head(width):
    return lax.broadcasted_iota(jnp.int32, (1, width), 1) // HEAD_DIM


def remote(src, dst, send, recv, **peer):
    return pltpu.make_async_remote_copy(
        src_ref=src,
        dst_ref=dst,
        send_sem=send,
        recv_sem=recv,
        device_id=peer,
        device_id_type=MESH_ID,
    )


def greet_group(barrier, size):
    me = lax.axis_index("fsdp")
    for step in range(1, size):
        peer = lax.rem(me + step, size)
        pl.semaphore_signal(barrier, inc=1, device_id={"fsdp": peer}, device_id_type=MESH_ID)


class Group:
    def __init__(self, size):
        self.size = size
        self.me = lax.axis_index("fsdp")
        self.square = size == 4
        if self.square:
            x, y = lax.rem(self.me, 2), self.me // 2
            self.at = lambda bx, by: lax.rem(y + by, 2) * 2 + lax.rem(x + bx, 2)
            self.x, self.y, self.far = self.at(1, 0), self.at(0, 1), self.at(1, 1)

    def from_own(self, step):
        if self.square:
            return self.at(lax.rem(step, 2), step // 2)
        return lax.rem(self.me - step + self.size, self.size)

    def to_own(self, step):
        if self.square:
            return self.at(1 - step // 2, 1 - lax.rem(step, 2))
        return lax.rem(self.me + 1 + step, self.size)


class Gather:
    def __init__(self, group, ref, send, recv):
        self.group, self.ref, self.send, self.recv = group, ref, send, recv
        self.half = ref.shape[1] // 2

    def part(self, k, slot, half, peer):
        view = self.ref.at[slot, pl.ds(half * self.half, self.half)]
        return remote(view, view, self.send.at[k], self.recv.at[k], fsdp=peer)

    def whole(self, k):
        g = self.group
        view = self.ref.at[g.me]
        sems = self.send.at[k - 1], self.recv.at[k - 1]
        return remote(view, view, *sems, fsdp=lax.rem(g.me + k, g.size))

    def copy(self, k):
        g = self.group
        if not g.square:
            return self.whole(k + 1)
        slot = (g.me, g.me, g.me, g.me, g.x, g.y)[k]
        half = (0, 1, 0, 1, 0, 1)[k]
        return self.part(k, slot, half, (g.x, g.x, g.y, g.y, g.y, g.x)[k])

    def start_half(self, half):
        if self.group.square:
            self.copy(half).start()
            self.copy(2 + half).start()
        elif half == 1:
            for k in range(self.group.size - 1):
                self.copy(k).start()

    def relay(self):
        if self.group.square:
            self.copy(0).wait_recv()
            self.copy(4).start()
            self.copy(3).wait_recv()
            self.copy(5).start()

    def ready(self, step):
        if not self.group.square:
            self.copy(step - 1).wait_recv()
        elif step == 3:
            self.copy(4).wait_recv()
            self.copy(5).wait_recv()
        else:
            self.copy(step).wait_recv()

    def finish(self):
        for k in range(transfers(self.group.size)):
            self.copy(k).wait_send()


class Scatter:
    def __init__(self, group, part, first, over, joined, last, send, recv):
        self.group, self.part = group, part
        self.first, self.over, self.joined, self.last = first, over, joined, last
        self.send, self.recv = send, recv
        self.half = part.shape[1] // 2

    def copy(self, k):
        g, half = self.group, self.half
        low, high = pl.ds(0, half), pl.ds(half, half)
        if not g.square:
            src, dst, peer = self.part.at[k], self.first.at[k], lax.rem(g.me + 1 + k, g.size)
        else:
            src, dst, peer = (
                lambda: (self.part.at[0, low], self.over.at[0], g.x),
                lambda: (self.part.at[0, high], self.over.at[1], g.y),
                lambda: (self.part.at[1, low], self.first.at[0], g.x),
                lambda: (self.part.at[2, high], self.first.at[1], g.y),
                lambda: (self.joined.at[0], self.last.at[0], g.y),
                lambda: (self.joined.at[1], self.last.at[1], g.x),
            )[k]()
        return remote(src, dst, self.send.at[k], self.recv.at[k], fsdp=peer)

    def made(self, step):
        if not self.group.square:
            self.copy(step).start()
        elif step == 0:
            self.copy(0).start()
            self.copy(1).start()
        elif step in (1, 2):
            self.copy(step + 1).start()

    def join(self):
        if not self.group.square:
            return
        half = self.half
        for k, (step, rows) in enumerate(((2, slice(0, half)), (1, slice(half, 2 * half)))):
            self.copy(k).wait_recv()
            own = self.part[step, rows].astype(F32)
            self.joined[k] = (own + self.over[k].astype(F32)).astype(BF)
            self.copy(4 + k).start()

    def total(self, half):
        count = self.half
        if self.group.square:
            self.copy(2 + half).wait_recv()
            self.copy(4 + half).wait_recv()
            return self.first[half].astype(F32) + self.last[half].astype(F32)
        if half == 0:
            for k in range(self.group.size - 1):
                self.copy(k).wait_recv()
        rows = slice(half * count, (half + 1) * count)
        out = self.first[0, rows].astype(F32)
        for k in range(1, self.group.size - 1):
            out = out + self.first[k, rows].astype(F32)
        return out

    def finish(self):
        for k in range(transfers(self.group.size)):
            self.copy(k).wait_send()


class Line:
    def __init__(self, parts, sems):
        self.rank = lax.axis_index("seq")
        self.parts, self.length = parts, parts // 2
        self.z, self.core = self.rank // 2, lax.rem(self.rank, 2)
        self.above, self.below = self.rank + 2, self.rank - 2
        self.beside = self.rank + 1 - 2 * self.core
        self.has_above, self.has_below = self.z < self.length - 1, self.z > 0
        self.sems = sems

    def greet(self, barrier):
        def one(peer):
            pl.semaphore_signal(barrier, inc=1, device_id={"seq": peer}, device_id_type=MESH_ID)

        one(self.beside)
        pl.when(self.has_above)(lambda: one(self.above))
        pl.when(self.has_below)(lambda: one(self.below))
        n, z = self.length, self.z
        return 1 + (2 * n - 2 - z) // n + (z + n - 1) // n

    def up(self, k, owner):
        view = self.view(owner)
        return remote(view, view, self.sems[0].at[k], self.sems[1].at[k], seq=self.above)

    def down(self, k, owner):
        view = self.view(owner)
        return remote(view, view, self.sems[2].at[k], self.sems[3].at[k], seq=self.below)

    def side(self, k, owner):
        view = self.view(owner)
        return remote(view, view, self.sems[4].at[k], self.sems[5].at[k], seq=self.beside)

    def gather(self, view):
        self.view = view
        pl.when(self.has_above)(lambda: self.up(0, self.rank).start())
        pl.when(self.has_below)(lambda: self.down(0, self.rank).start())
        self.side(self.z, self.rank).start()

    def own_up(self):
        pl.when(self.has_above)(lambda: self.up(0, self.rank).start())

    def own_down(self):
        pl.when(self.has_below)(lambda: self.down(0, self.rank).start())

    def relay_up(self, j):
        rank, z = self.rank, self.z

        @pl.when((z >= j) & self.has_above)
        def _():
            self.up(j - 1, rank).wait_recv()
            self.up(j, rank - 2 * j).start()
            self.side(z - j, rank - 2 * j).start()

    def relay_down(self, j):
        rank, z = self.rank, self.z

        @pl.when((z + j < self.length) & self.has_below)
        def _():
            self.down(j - 1, rank).wait_recv()
            self.down(j, rank + 2 * j).start()
            self.side(z + j, rank + 2 * j).start()

    def relay(self, j):
        self.relay_up(j)
        self.relay_down(j)

    def close(self, j):
        rank, z = self.rank, self.z

        @pl.when((z >= j) & (z == self.length - 1))
        def _():
            self.up(j - 1, rank).wait_recv()
            self.side(z - j, rank - 2 * j).start()

        @pl.when((z + j < self.length) & (z == 0))
        def _():
            self.down(j - 1, rank).wait_recv()
            self.side(z + j, rank + 2 * j).start()

    def gathered(self):
        for k in range(self.length):
            self.side(k, self.rank).wait_recv()

    def finish(self):
        rank, z = self.rank, self.z
        for k in range(self.length):
            self.side(k, rank).wait_send()
        pl.when(self.has_above)(lambda: self.up(0, rank).wait_send())
        pl.when(self.has_below)(lambda: self.down(0, rank).wait_send())
        for j in range(1, self.length):
            pl.when((z >= j) & self.has_above)(lambda: self.up(j, rank).wait_send())
            pl.when((z + j < self.length) & self.has_below)(lambda: self.down(j, rank).wait_send())


class LineSum:
    def __init__(self, line, x, pre, acc, up_in, down_in, sems):
        self.line, self.x, self.pre, self.acc = line, x, pre, acc
        self.up_in, self.down_in, self.sems = up_in, down_in, sems

    def share(self, k):
        line = self.line
        src = self.x.at[2 * k + 1 - line.core]
        return remote(src, self.pre.at[k], self.sems[0].at[k], self.sems[1].at[k], seq=line.beside)

    def up(self, k):
        sems = self.sems[2].at[k], self.sems[3].at[k]
        return remote(self.acc.at[k], self.up_in.at[k], *sems, seq=self.line.above)

    def down(self, k):
        sems = self.sems[4].at[k], self.sems[5].at[k]
        return remote(self.acc.at[k], self.down_in.at[k], *sems, seq=self.line.below)

    def pair(self, m):
        return self.line.length - 1 - m, m

    def trade(self):
        n = self.line.length
        for m in range((n + 1) // 2):
            for k in sorted(set(self.pair(m))):
                self.share(k).start()

    def merge(self, k):
        self.share(k).wait_recv()
        own = self.x[2 * k + self.line.core].astype(F32)
        self.acc[k] = (own + self.pre[k].astype(F32)).astype(BF)

    def begin(self, m):
        n, z = self.line.length, self.line.z
        far, near = self.pair(m)
        if m < (n + 1) // 2:
            for k in sorted({far, near}):
                self.merge(k)
        if m < n - 1:
            pl.when(z == 0)(lambda: self.up(far).start())
            pl.when(z == n - 1)(lambda: self.down(near).start())

    def add(self, k, more):
        self.acc[k] = (self.acc[k].astype(F32) + more[k].astype(F32)).astype(BF)

    def advance(self, t):
        z, n = self.line.z, self.line.length
        far, near = n - 1 + z - t, t - n + 1 + z

        @pl.when((z >= 1) & (z <= t))
        def _():
            self.up(far).wait_recv()
            self.add(far, self.up_in)
            self.up(far).start()

        @pl.when((z <= n - 2) & (z >= n - 1 - t))
        def _():
            self.down(near).wait_recv()
            self.add(near, self.down_in)
            self.down(near).start()

    def total(self):
        z = self.line.z

        @pl.when(z > 0)
        def _():
            self.up(z).wait_recv()
            self.add(z, self.up_in)

        @pl.when(z < self.line.length - 1)
        def _():
            self.down(z).wait_recv()
            self.add(z, self.down_in)

    def finish(self):
        for k in range(self.line.length):
            self.share(k).wait_send()
            pl.when(k > self.line.z)(lambda: self.up(k).wait_send())
            pl.when(k < self.line.z)(lambda: self.down(k).wait_send())


class StagedSum(LineSum):
    def __init__(self, stage, load, *args):
        super().__init__(*args)
        self.stage, self.load = stage, load

    def fetch(self, slot, src):
        return pltpu.make_async_copy(src, self.stage.at[slot], self.load.at[slot])

    def merge(self, k):
        self.share(k).wait_recv()
        own = self.fetch(0, self.x.at[2 * k + self.line.core])
        other = self.fetch(1, self.pre.at[k])
        own.start()
        other.start()
        own.wait()
        other.wait()
        self.acc[k] = (self.stage[0].astype(F32) + self.stage[1].astype(F32)).astype(BF)

    def add(self, k, more):
        came = self.fetch(0, more.at[k])
        came.start()
        came.wait()
        self.acc[k] = (self.acc[k].astype(F32) + self.stage[0].astype(F32)).astype(BF)


def line_sems(parts):
    return [pltpu.SemaphoreType.DMA((parts // 2,))] * 6


def transfers(size):
    return 6 if size == 4 else size - 1


def scatter_shapes(size, rows, width):
    half = rows // 2
    slots = (2, half, width) if size == 4 else (size - 1, rows, width)
    return [
        pltpu.VMEM((size - 1, rows, width), BF),
        pltpu.VMEM(slots, BF),
        pltpu.VMEM((2, half, width), BF),
        pltpu.VMEM((2, half, width), BF),
        pltpu.VMEM((2, half, width), BF),
        pltpu.SemaphoreType.DMA((transfers(size),)),
        pltpu.SemaphoreType.DMA((transfers(size),)),
    ]


def each_step(size, body):
    def one(step, carry):
        body(step, lambda k: pl.when(step == k))
        return carry

    lax.fori_loop(0, size, one, 0)


class ForwardRefs(NamedTuple):
    tokens: Any
    edge_tok: Any
    grad: Any
    gains: Any
    table: Any
    qkv_piece: Any
    gu_piece: Any
    out_map: Any
    down_map: Any
    gated_hbm: Any
    qkv_hbm: Any
    edge: Any
    qkv_map_hbm: Any
    middle: Any
    heads: Any
    grads_hbm: Any
    norm_hbm: Any
    hidden_hbm: Any
    gu_grad_hbm: Any
    gu_map_hbm: Any
    gains_all: Any
    table_all: Any
    part: Any
    first: Any
    over: Any
    joined: Any
    last: Any
    all: Any
    grads: Any
    qkv: Any
    qkv_map: Any
    gu_map: Any
    tail: Any
    own: Any
    hidden: Any
    gu_grad: Any
    s_send: Any
    s_recv: Any
    a_send: Any
    a_recv: Any
    g_send: Any
    g_recv: Any
    c_send: Any
    c_recv: Any
    m_send: Any
    m_recv: Any
    halo_send: Any
    halo_recv: Any
    loads: Any
    stores: Any
    hidden_store: Any
    gu_store: Any


def forward_kernel(size, parts, count, *refs):
    named = len(ForwardRefs._fields)
    r, sems = ForwardRefs(*refs[:named]), refs[named:]
    rank = lax.axis_index("seq")
    rows = r.tokens.shape[0]
    half = rows // 2
    local = r.out_map.shape[0]
    inner = r.down_map.shape[0]
    slot = rank * rows
    group = Group(size)
    me = group.me
    line_q, line_u = Line(parts, sems[:6]), Line(parts, sems[6:])

    barrier = pltpu.get_barrier_semaphore()
    greet_group(barrier, size)
    known = line_q.greet(barrier)

    def greet(peer):
        pl.semaphore_signal(barrier, inc=1, device_id={"seq": peer}, device_id_type=MESH_ID)

    pl.when(line_q.has_above & (line_q.core == 1))(lambda: greet(rank + 1))
    pl.when(line_q.has_below & (line_q.core == 0))(lambda: greet(rank - 1))
    n, z = line_q.length, line_q.z
    known = known + (2 * n - 2 - z) // n * line_q.core + (z + n - 1) // n * (1 - line_q.core)
    own_pieces = [
        pltpu.make_async_copy(src.at[me], dst.at[me, rank], r.loads.at[k])
        for k, (src, dst) in enumerate(
            ((r.qkv_piece, r.qkv_map), (r.gu_piece, r.gu_map))
        )
    ]
    for copy in own_pieces:
        copy.start()
    r.gains_all[me] = r.gains[...]
    r.table_all[me] = r.table[...]
    r.grads[me] = r.grad[...]
    pl.semaphore_wait(barrier, size - 1 + known)

    def swap(k, step):
        peer = lax.rem(me + step, size)
        src, dst = (
            lambda: (r.gains_all.at[me], r.gains_all.at[me]),
            lambda: (r.table_all.at[me], r.table_all.at[me]),
            lambda: (r.qkv_piece.at[peer], r.qkv_map.at[me, rank]),
            lambda: (r.gu_piece.at[peer], r.gu_map.at[me, rank]),
        )[k]()
        return remote(src, dst, r.m_send.at[k, step - 1], r.m_recv.at[k, step - 1], fsdp=peer)

    others = range(1, size)
    for k in range(4):
        for step in others:
            swap(k, step).start()
    for k in range(2):
        for step in others:
            swap(k, step).wait_recv()

    gains = jnp.concatenate([r.gains_all[f] for f in range(size)], 1).astype(F32)
    own_table = r.table_all[me]
    slots = slot + lax.broadcasted_iota(jnp.int32, (rows, 1), 0)
    length = lambda j: own_table[0:1, j : j + 1]
    start = lambda j: own_table[1:2, j : j + 1]
    segment = segment_of(slots, count, length, start)
    same_one = (segment == segment_of(slots - 1, count, length, start)).astype(F32)
    same_two = (segment == segment_of(slots - 2, count, length, start)).astype(F32)
    tokens = r.tokens[...].astype(F32)
    edge = r.edge_tok[...].astype(F32)

    def norm(a):
        return a * lax.rsqrt(jnp.mean(a * a, axis=1, keepdims=True) + EPS) * gains[0:1]

    normed, edge = norm(tokens), norm(edge)
    row = lax.broadcasted_iota(jnp.int32, (rows, 1), 0)
    back_one = jnp.where(row == 0, edge[1:2], pltpu.roll(normed, 1, 0))
    back_two = jnp.where(
        row == 0, edge[0:1], jnp.where(row == 1, edge[1:2], pltpu.roll(normed, 2, 0))
    )
    mixed = (
        normed * gains[2:3]
        + same_one * back_one * gains[3:4]
        + same_two * back_two * gains[4:5]
    )
    all_ref = r.all
    all_ref[me] = (mixed * normed).astype(BF)
    gather = Gather(group, all_ref, r.a_send, r.a_recv)
    gather.start_half(0)
    gather.start_half(1)

    own_pieces[0].wait()
    for step in others:
        swap(2, step).wait_recv()
    line_q.gather(lambda owner: r.qkv_map.at[:, owner])
    line_u.view = lambda owner: r.gu_map.at[:, owner]
    gather.relay()
    grads = Gather(group, r.grads, r.c_send, r.c_recv)
    grads.start_half(0)
    grads.start_half(1)
    own_pieces[1].wait()
    for step in others:
        swap(3, step).wait_recv()
    line_u.side(z, rank).start()
    pl.when(z == 0)(line_u.own_up)
    pl.when(z == n - 1)(line_u.own_down)
    for j in range(1, n):
        line_q.relay(j)
        line_q.close(j)
        pl.when(z == j)(line_u.own_up)
        pl.when(z == n - 1 - j)(line_u.own_down)
    for step in others:
        gather.ready(step)
    grads.relay()
    line_q.gathered()
    keeps = [
        pltpu.make_async_copy(all_ref, r.gated_hbm, r.stores.at[size]),
        pltpu.make_async_copy(r.qkv_map, r.qkv_map_hbm, r.stores.at[size + 1]),
    ]
    for keep in keeps:
        keep.start()

    weights = r.qkv_map[...].reshape(-1, r.qkv_map.shape[3])

    def halo(step):
        g = group.to_own(step)
        sem = r.halo_send.at[step], r.halo_recv.at[step]
        return remote(r.tail.at[g], r.edge.at[g], *sem, seq=rank + 1)

    def project(step, is_step):
        g = group.to_own(step)
        out = dot(all_ref[g], weights).astype(BF)
        r.qkv[g] = out
        r.tail[g] = out[rows - WINDOW :, local:]
        pl.when(rank < parts - 1)(lambda: halo(step).start())

    each_step(size, project)

    @pl.when(rank == 0)
    def _():
        r.edge[...] = jnp.zeros_like(r.edge)

    keeps.append(pltpu.make_async_copy(r.qkv, r.qkv_hbm, r.stores.at[size + 2]))
    keeps[2].start()
    line_u.relay(1)
    gather.finish()
    keeps[0].wait()

    scatter = Scatter(
        group, r.part, r.first, r.over, r.joined, r.last, r.s_send, r.s_recv
    )
    head_of = lane_head(local)

    def mix(step, is_step):
        g = group.to_own(step)
        pl.when(rank > 0)(lambda: halo(step).wait_recv())
        own, edge, table = r.qkv[g], r.edge[g], r.table_all[g]
        queries = own[:, :local]
        keys = jnp.concatenate([edge[:, :local], own[:, local : 2 * local]], 0)
        values = jnp.concatenate([edge[:, local:], own[:, 2 * local :]], 0)
        outs = []
        for block in range(rows // BLOCK):
            mask = masks_of(
                slot,
                block,
                count,
                lambda j: table[0:1, j : j + 1],
                lambda j: table[1:2, j : j + 1],
            )
            low = block * BLOCK
            query = queries[low : low + BLOCK]
            key = keys[low : low + BLOCK + WINDOW]
            value = values[low : low + BLOCK + WINDOW]
            out = jnp.zeros((BLOCK, local), F32)
            for head in range(local // HEAD_DIM):
                mine = head_of == head
                soft = soft_of(jnp.where(mine, query, jnp.zeros_like(query)), key, mask)
                out = jnp.where(mine, dot(soft.astype(BF), value), out)
            outs.append(out.astype(BF))
        heads = jnp.concatenate(outs, 0)
        r.heads[g] = heads
        branch = dot(heads, r.out_map[...])
        is_step(size - 1)(lambda: r.own.__setitem__(..., branch))
        pl.when(step < size - 1)(lambda: r.part.__setitem__(step, branch.astype(BF)))
        for k in range(size - 1):
            is_step(k)(functools.partial(scatter.made, k))

    each_step(size, mix)
    scatter.join()
    for j in range(2, n):
        line_u.relay(j)
    gather = Gather(group, all_ref, r.g_send, r.g_recv)
    for h in range(2):
        span = slice(h * half, (h + 1) * half)
        total = r.own[span, :] + scatter.total(h)
        middle = r.tokens[span, :].astype(F32) + total
        r.middle[span, :] = middle
        scale = lax.rsqrt(jnp.mean(middle * middle, axis=1, keepdims=True) + EPS)
        all_ref[me, span] = (middle * scale * gains[1:2]).astype(BF)
        gather.start_half(h)
    gather.relay()
    for j in range(1, n):
        line_u.close(j)
    line_u.gathered()
    keeps.append(pltpu.make_async_copy(r.gu_map, r.gu_map_hbm, r.stores.at[size + 3]))
    keeps[3].start()

    def out_copies(step):
        g, two = group.from_own(step), lax.rem(step, 2)
        return (
            pltpu.make_async_copy(
                r.hidden.at[two], r.hidden_hbm.at[g], r.hidden_store.at[two]
            ),
            pltpu.make_async_copy(
                r.gu_grad.at[two], r.gu_grad_hbm.at[g], r.gu_store.at[two]
            ),
        )

    def norm_copy(g):
        return pltpu.make_async_copy(all_ref.at[g], r.norm_hbm.at[g], r.stores.at[g])

    def feed(step, is_step):
        g, two = group.from_own(step), lax.rem(step, 2)
        for k in others:
            is_step(k)(functools.partial(gather.ready, k))
            is_step(k)(functools.partial(grads.ready, k))

        @pl.when(step >= 2)
        def _():
            for copy in out_copies(step - 2):
                copy.wait()

        norm_copy(g).start()
        weights = r.gu_map[...].reshape(-1, r.gu_map.shape[3])
        acts = dot(all_ref[g], weights)
        gate, up = acts[:, :inner], acts[:, inner:]
        sigma = jax.nn.sigmoid(gate)
        silu = gate * sigma
        r.hidden[two] = (silu * up).astype(BF)
        grad_hidden = dot_trans(r.grads[g], r.down_map[...])
        grad_gate = grad_hidden * up * sigma * (1.0 + gate * (1.0 - sigma))
        r.gu_grad[two] = jnp.concatenate([grad_gate, grad_hidden * silu], 1).astype(BF)
        for copy in out_copies(step):
            copy.start()

    each_step(size, feed)
    keeps.append(pltpu.make_async_copy(r.grads, r.grads_hbm, r.stores.at[size + 4]))
    keeps[4].start()
    for k in range(4):
        for step in others:
            swap(k, step).wait_send()
    scatter.finish()
    gather.finish()
    grads.finish()
    line_q.finish()
    line_u.finish()

    @pl.when(rank < parts - 1)
    def _():
        for step in range(size):
            halo(step).wait_send()

    for keep in keeps[1:]:
        keep.wait()
    for g in range(size):
        norm_copy(g).wait()
    for step in (size - 2, size - 1):
        for copy in out_copies(step):
            copy.wait()


def forward_part(ident, count, tokens, edge, grad, gains, table, qkv_piece, gu_piece, out_weight, down_weight):
    size, parts = lax.axis_size("fsdp"), lax.axis_size("seq")
    rows, width = tokens.shape
    local, inner = out_weight.shape[0], down_weight.shape[0]
    piece, cols = gu_piece.shape[1:]
    vmem = pl.BlockSpec(memory_space=pltpu.VMEM)
    hbm = pl.BlockSpec(memory_space=pl.ANY)
    shape = lambda w: (size, rows, w)
    low = lambda s: jax.ShapeDtypeStruct(s, BF)
    maps = [(size, parts, piece, 3 * local), (size, parts, piece, cols)]
    dma = lambda *s: pltpu.SemaphoreType.DMA(s)
    hop = transfers(size)
    scratch = scatter_shapes(size, rows, width)
    return pl.pallas_call(
        functools.partial(forward_kernel, size, parts, count),
        out_shape=[
            low(shape(width)),
            low(shape(3 * local)),
            low((size, WINDOW, 2 * local)),
            low(maps[0]),
            jax.ShapeDtypeStruct((rows, width), F32),
            low(shape(local)),
            low(shape(width)),
            low(shape(width)),
            low(shape(inner)),
            low(shape(cols)),
            low(maps[1]),
            low((size,) + gains.shape),
            jax.ShapeDtypeStruct((size,) + table.shape, jnp.int32),
        ],
        in_specs=[vmem] * 5 + [hbm, hbm, vmem, vmem],
        out_specs=[hbm, hbm, vmem, hbm, vmem, vmem, hbm, hbm, hbm, hbm, hbm, vmem, vmem],
        scratch_shapes=scratch[:-2]
        + [
            pltpu.VMEM(shape(width), BF),
            pltpu.VMEM(shape(width), BF),
            pltpu.VMEM(shape(3 * local), BF),
            pltpu.VMEM(maps[0], BF),
            pltpu.VMEM(maps[1], BF),
            pltpu.VMEM((size, WINDOW, 2 * local), BF),
            pltpu.VMEM((rows, width), F32),
            pltpu.VMEM((2, rows, inner), BF),
            pltpu.VMEM((2, rows, cols), BF),
        ]
        + [dma(hop)] * 8
        + [dma(4, size - 1)] * 2
        + [dma(size)] * 2
        + [dma(2), dma(size + 5), dma(2), dma(2)]
        + line_sems(parts)
        + line_sems(parts),
        compiler_params=pltpu.CompilerParams(
            collective_id=ident, has_side_effects=True, vmem_limit_bytes=67_000_000
        ),
        cost_estimate=pl.CostEstimate(
            flops=2 * size * rows * width * (4 * local + 3 * inner),
            bytes_accessed=500_000_000,
            transcendentals=0,
        ),
        name="forward_part",
    )(tokens, edge, grad, gains, table, qkv_piece, gu_piece, out_weight, down_weight)


def heads_back(group, slot, count, lens_ref, starts_ref, own, edge, grad):
    rows, local = own.shape[0], own.shape[1] // 3
    head_of = lane_head(local)
    queries = own[:, :local]
    keys = jnp.concatenate([edge[:, :local], own[:, local : 2 * local]], 0)
    values = jnp.concatenate([edge[:, local:], own[:, 2 * local :]], 0)
    dqs, dks, dvs = [], [], []
    for block in range(rows // BLOCK):
        mask = masks_of(
            slot, block, count, lambda j: lens_ref[group, j], lambda j: starts_ref[group, j]
        )
        low = block * BLOCK
        span = slice(low, low + BLOCK + WINDOW)
        query, grads = queries[low : low + BLOCK], grad[low : low + BLOCK]
        key, value = keys[span], values[span]
        dq = jnp.zeros((BLOCK, local), F32)
        dk = jnp.zeros((BLOCK + WINDOW, local), F32)
        dv = jnp.zeros((BLOCK + WINDOW, local), F32)
        for head in range(local // HEAD_DIM):
            mine = head_of == head
            own_q = jnp.where(mine, query, jnp.zeros_like(query))
            own_g = jnp.where(mine, grads, jnp.zeros_like(grads))
            soft = soft_of(own_q, key, mask)
            grad_soft = dot_trans(own_g, value)
            total = jnp.sum(grad_soft * soft, axis=1, keepdims=True)
            grad_scores = (soft * (grad_soft - total)).astype(BF)
            dq = jnp.where(mine, dot(grad_scores, key), dq)
            dk = dk + dot_rows(grad_scores, own_q)
            dv = dv + dot_rows(soft.astype(BF), own_g)
        dqs.append(dq * SCALE)
        dks.append(dk * SCALE)
        dvs.append(dv)

    def joined(pieces):
        out = [pieces[0][:BLOCK]]
        for left, right in zip(pieces, pieces[1:]):
            out.append(left[BLOCK:] + right[:WINDOW])
            out.append(right[WINDOW:BLOCK])
        out.append(pieces[-1][BLOCK:])
        return jnp.concatenate(out, 0)

    return jnp.concatenate(dqs, 0), joined(dks), joined(dvs)


class BackRefs(NamedTuple):
    lens: Any
    starts: Any
    grad_gu_hbm: Any
    gu_map_hbm: Any
    middle: Any
    grad: Any
    gain: Any
    out_map: Any
    edge: Any
    qkv: Any
    qkv_map_hbm: Any
    gu_x: Any
    down_x: Any
    grad_middle: Any
    norm: Any
    all: Any
    dqkv: Any
    own: Any
    gu_piece: Any
    down_every: Any
    gu_pre: Any
    gu_up: Any
    gu_down: Any
    down_pre: Any
    down_up: Any
    down_down: Any
    part: Any
    first: Any
    over: Any
    joined: Any
    last: Any
    s_send: Any
    s_recv: Any
    t_send: Any
    t_recv: Any
    g_send: Any
    g_recv: Any
    grad_gu: Any
    gu_map: Any
    qkv_map: Any
    dedge: Any
    back: Any
    tail: Any
    h_send: Any
    h_recv: Any
    loads: Any
    gu_acc: Any
    gu_stage: Any
    gu_load: Any
    down_acc: Any
    down_stage: Any
    down_load: Any


def back_kernel(size, parts, count, *refs):
    named = len(BackRefs._fields)
    r, sems = BackRefs(*refs[:named]), refs[named:]
    line = Line(parts, sems[:6])
    gu_sum = StagedSum(
        r.gu_stage, r.gu_load, line, r.gu_x, r.gu_pre, r.gu_acc, r.gu_up, r.gu_down, sems[6:12]
    )
    down_sum = StagedSum(
        r.down_stage,
        r.down_load,
        line,
        r.down_x,
        r.down_pre,
        r.down_acc,
        r.down_up,
        r.down_down,
        sems[12:],
    )
    rows = r.middle.shape[0]
    local = r.out_map.shape[0]
    rank = lax.axis_index("seq")
    slot = rank * rows
    group = Group(size)
    barrier = pltpu.get_barrier_semaphore()
    greet_group(barrier, size)

    def greet(peer):
        pl.semaphore_signal(barrier, inc=1, device_id={"seq": peer}, device_id_type=MESH_ID)

    known = line.greet(barrier)
    pl.when(line.has_above & (line.core == 1))(lambda: greet(rank + 1))
    pl.when(line.has_below & (line.core == 0))(lambda: greet(rank - 1))
    n, z = line.length, line.z
    known = known + (2 * n - 2 - z) // n * line.core + (z + n - 1) // n * (1 - line.core)
    fetches = [
        pltpu.make_async_copy(src, dst, r.loads.at[k])
        for k, (src, dst) in enumerate(
            ((r.grad_gu_hbm, r.grad_gu), (r.gu_map_hbm, r.gu_map), (r.qkv_map_hbm, r.qkv_map))
        )
    ]
    for fetch in fetches:
        fetch.start()
    pl.semaphore_wait(barrier, size - 1 + known)
    down_sum.trade()
    gu_sum.trade()
    scatter = Scatter(
        group, r.part, r.first, r.over, r.joined, r.last, r.s_send, r.s_recv
    )
    gather = Gather(group, r.all, r.g_send, r.g_recv)
    fetches[0].wait()
    fetches[1].wait()

    def step_two(step, is_step):
        partial = dot_trans(r.grad_gu[group.to_own(step)], r.gu_map[...])
        is_step(size - 1)(lambda: r.own.__setitem__(..., partial))
        pl.when(step < size - 1)(lambda: r.part.__setitem__(step, partial.astype(BF)))
        for k in range(size - 1):
            is_step(k)(functools.partial(scatter.made, k))

    each_step(size, step_two)
    for m in range(n):
        down_sum.begin(m)
    scatter.join()
    gu_sum.begin(0)
    down_sum.advance(1)
    half = rows // 2
    norm_sum = jnp.zeros((1, r.middle.shape[1]), F32)
    for h in range(2):
        span = slice(h * half, (h + 1) * half)
        grad = r.own[span, :] + scatter.total(h)
        middle = r.middle[span, :]
        scale = lax.rsqrt(jnp.mean(middle * middle, axis=1, keepdims=True) + EPS)
        unit = middle * scale
        scaled = grad * r.gain[...]
        norm_sum = norm_sum + jnp.sum(grad * unit, axis=0, keepdims=True)
        grad_out = r.grad[span, :].astype(F32)
        grad_middle = grad_out + scale * (
            scaled - unit * jnp.mean(scaled * unit, axis=1, keepdims=True)
        )
        r.grad_middle[span, :] = grad_middle
        r.all[group.me, span] = grad_middle.astype(BF)
        gather.start_half(h)
    r.norm[...] = norm_sum
    own_down = pltpu.make_async_copy(r.down_acc.at[z], r.down_every.at[rank], r.down_load.at[0])

    def halo(step):
        g = group.from_own(step)
        sems = r.h_send.at[step], r.h_recv.at[step]
        return remote(r.dedge.at[g], r.back.at[g], *sems, seq=rank - 1)

    def step_heads(step, is_step):
        g = group.from_own(step)

        @is_step(1)
        def _():
            gather.relay()
            for t in range(2, n - 1):
                down_sum.advance(t)

        @is_step(2)
        def _():
            down_sum.total()
            own_down.start()
            own_down.wait()
            line.gather(lambda owner: r.down_every.at[owner])
            for m in range(1, n):
                gu_sum.begin(m)

        for k in range(1, size):
            is_step(k)(functools.partial(gather.ready, k))
        grad = dot_trans(r.all[g], r.out_map[...]).astype(BF)
        dq, dk, dv = heads_back(
            g, slot, count, r.lens, r.starts, r.qkv[g], r.edge[g], grad
        )
        r.dedge[g] = jnp.concatenate([dk[:WINDOW], dv[:WINDOW]], 1).astype(BF)
        full = jnp.concatenate([dq, dk[WINDOW:], dv[WINDOW:]], 1)
        r.dqkv[g] = full.astype(BF)
        r.tail[g] = full[rows - WINDOW :]
        pl.when(rank > 0)(lambda: halo(step).start())

    each_step(size, step_heads)
    gu_sum.advance(1)
    scatter.finish()
    fetches[2].wait()

    @pl.when(rank == parts - 1)
    def _():
        r.back[...] = jnp.zeros_like(r.back)

    @pl.when(rank < parts - 1)
    def _():
        for step in range(size):
            halo(step).wait_recv()

    scatter = Scatter(
        group, r.part, r.first, r.over, r.joined, r.last, r.t_send, r.t_recv
    )

    def step_one(step, is_step):
        g = group.to_own(step)
        back = r.back[g].astype(F32)
        wide = jnp.concatenate([jnp.zeros((WINDOW, local), F32), back], 1)
        r.dqkv[g, pl.ds(rows - WINDOW, WINDOW)] = (r.tail[g] + wide).astype(BF)
        partial = dot_trans(r.dqkv[g], r.qkv_map[...])
        is_step(size - 1)(lambda: r.own.__setitem__(..., partial))
        pl.when(step < size - 1)(lambda: r.part.__setitem__(step, partial.astype(BF)))
        for k in range(size - 1):
            is_step(k)(functools.partial(scatter.made, k))

    each_step(size, step_one)
    line.relay(1)
    scatter.join()
    for t in range(2, n - 1):
        gu_sum.advance(t)
        line.relay(t)
    line.relay(n - 1)
    for h in range(2):
        span = slice(h * half, (h + 1) * half)
        r.own[span, :] = r.own[span, :] + scatter.total(h)
    gu_sum.total()
    out_piece = pltpu.make_async_copy(r.gu_acc.at[z], r.gu_piece, r.gu_load.at[0])
    out_piece.start()
    for j in range(1, n):
        line.close(j)
    line.gathered()
    scatter.finish()
    gather.finish()
    down_sum.finish()
    gu_sum.finish()
    line.finish()
    out_piece.wait()

    @pl.when(rank > 0)
    def _():
        for step in range(size):
            halo(step).wait_send()


def back_part(
    ident, lens, starts, grad_gu, gu_map, middle, grad, gain, out_weight, edge, qkv, qkv_map, gu_x, down_x
):
    size, parts = lax.axis_size("fsdp"), lax.axis_size("seq")
    rows, width = middle.shape
    local = out_weight.shape[0]
    n = parts // 2
    vmem = pl.BlockSpec(memory_space=pltpu.VMEM)
    smem = pl.BlockSpec(memory_space=pltpu.SMEM)
    hbm = pl.BlockSpec(memory_space=pl.ANY)
    dma = lambda *s: pltpu.SemaphoreType.DMA(s)
    low = lambda *s: jax.ShapeDtypeStruct(s, BF)
    sems = [dma(transfers(size))] * 2
    gu, down = gu_x.shape[1:], down_x.shape[1:]
    outs = pl.pallas_call(
        functools.partial(back_kernel, size, parts, lens.shape[1]),
        out_shape=[
            jax.ShapeDtypeStruct((rows, width), F32),
            jax.ShapeDtypeStruct((1, width), F32),
            low(size, rows, width),
            low(*qkv.shape),
            jax.ShapeDtypeStruct((rows, width), F32),
            low(*gu),
            low(parts, *down),
        ]
        + [low(n, *gu)] * 3
        + [low(n, *down)] * 3,
        in_specs=[smem, smem, hbm, hbm] + [vmem] * 6 + [hbm] * 3,
        out_specs=[vmem] * 5 + [hbm] * 8,
        scratch_shapes=scatter_shapes(size, rows, width)
        + sems
        + sems
        + [
            pltpu.VMEM(grad_gu.shape, BF),
            pltpu.VMEM(gu_map.shape, BF),
            pltpu.VMEM(qkv_map.shape, BF),
            pltpu.VMEM((size, WINDOW, 2 * local), BF),
            pltpu.VMEM((size, WINDOW, 2 * local), BF),
            pltpu.VMEM((size, WINDOW, 3 * local), F32),
            dma(size),
            dma(size),
            dma(3),
            pltpu.VMEM((n,) + gu, BF),
            pltpu.VMEM((2,) + gu, BF),
            dma(2),
            pltpu.VMEM((n,) + down, BF),
            pltpu.VMEM((2,) + down, BF),
            dma(2),
        ]
        + line_sems(parts) * 3,
        compiler_params=pltpu.CompilerParams(
            collective_id=ident, has_side_effects=True, vmem_limit_bytes=67_000_000
        ),
        cost_estimate=pl.CostEstimate(
            flops=2 * size * rows * (gu_map.size + qkv_map.size + width * local),
            bytes_accessed=400_000_000,
            transcendentals=0,
        ),
        name="back_part",
    )(lens, starts, grad_gu, gu_map, middle, grad, gain, out_weight, edge, qkv, qkv_map, gu_x, down_x)
    return outs[:7]


class CloseRefs(NamedTuple):
    x: Any
    gu_piece: Any
    terms: Any
    hidden: Any
    down_map: Any
    every_hbm: Any
    gu_every_hbm: Any
    feed: Any
    terms_out: Any
    part: Any
    first: Any
    over: Any
    joined: Any
    last: Any
    pre: Any
    acc: Any
    up_in: Any
    down_in: Any
    every: Any
    slots: Any
    gu_every: Any
    terms_in: Any
    terms_all: Any
    s_send: Any
    s_recv: Any
    m_send: Any
    m_recv: Any
    t_send: Any
    t_recv: Any
    loads: Any


def close_kernel(size, parts, *refs):
    named = len(CloseRefs._fields)
    r, sems = CloseRefs(*refs[:named]), refs[named:]
    rank = lax.axis_index("seq")
    group = Group(size)
    me = group.me
    line_u, line_q = Line(parts, sems[:6]), Line(parts, sems[6:12])
    n, z = line_q.length, line_q.z
    sums = LineSum(line_q, r.x, r.pre, r.acc, r.up_in, r.down_in, sems[12:])
    rows = r.feed.shape[0]
    half = rows // 2
    barrier = pltpu.get_barrier_semaphore()
    greet_group(barrier, size)
    for step in range(1, parts):
        peer = lax.rem(rank + step, parts)
        pl.semaphore_signal(barrier, inc=1, device_id={"seq": peer}, device_id_type=MESH_ID)
    own_piece = pltpu.make_async_copy(
        r.gu_piece.at[me], r.gu_every.at[rank, me], r.loads.at[0]
    )
    own_piece.start()
    r.terms_in[me] = r.terms[me]
    pl.semaphore_wait(barrier, size + parts - 2)
    sums.trade()

    def swap(k, step):
        peer = lax.rem(me + step, size)
        src, dst = (
            lambda: (r.gu_piece.at[peer], r.gu_every.at[rank, me]),
            lambda: (r.terms.at[peer], r.terms_in.at[me]),
            lambda: (r.acc.at[z, peer], r.slots.at[me]),
        )[k]()
        return remote(src, dst, r.m_send.at[k, step - 1], r.m_recv.at[k, step - 1], fsdp=peer)

    others = range(1, size)
    for k in range(2):
        for step in others:
            swap(k, step).start()

    scatter = Scatter(
        group, r.part, r.first, r.over, r.joined, r.last, r.s_send, r.s_recv
    )

    def down(step, is_step):
        partial = dot(r.hidden[group.to_own(step)], r.down_map[...])
        is_step(size - 1)(lambda: r.feed.__setitem__(..., partial))
        pl.when(step < size - 1)(lambda: r.part.__setitem__(step, partial.astype(BF)))
        for k in range(size - 1):
            is_step(k)(functools.partial(scatter.made, k))

    for m in range(n):
        sums.begin(m)
    each_step(size, down)
    own_piece.wait()
    for step in others:
        swap(0, step).wait_recv()
    line_u.gather(lambda owner: r.gu_every.at[owner])

    for step in others:
        swap(1, step).wait_recv()
    small = r.terms_in[0]
    for f in others:
        small = small + r.terms_in[f]
    r.terms_all[rank] = small

    def spread(step):
        peer = lax.rem(rank + step, parts)
        view = r.terms_all.at[rank]
        return remote(view, view, r.t_send.at[step - 1], r.t_recv.at[step - 1], seq=peer)

    for step in range(1, parts):
        spread(step).start()
    scatter.join()

    for t in range(1, n - 1):
        sums.advance(t)
        if t == 1:
            pl.when(z >= 2)(lambda: line_u.relay_up(1))
            pl.when(z <= n - 3)(lambda: line_u.relay_down(1))
    sums.total()
    for step in others:
        swap(2, step).start()
    for h in range(2):
        span = slice(h * half, (h + 1) * half)
        r.feed[span, :] = r.feed[span, :] + scatter.total(h)
    pl.when(z < 2)(lambda: line_u.relay_up(1))
    pl.when(z > n - 3)(lambda: line_u.relay_down(1))
    r.slots[me] = r.acc[z, me]
    for step in others:
        swap(2, step).wait_recv()
    local = r.x.shape[3] // 4
    lane = lax.broadcasted_iota(jnp.int32, (1, 1, 4 * local), 2)
    r.every[rank] = jnp.where(lane < 3 * local, r.slots[...], r.acc[z])
    line_q.gather(lambda owner: r.every.at[owner])
    for j in range(2, n):
        line_u.relay(j)
        line_q.relay(j - 1)
    for j in range(1, n):
        line_u.close(j)
    line_u.gathered()
    stores = [pltpu.make_async_copy(r.gu_every, r.gu_every_hbm, r.loads.at[0])]
    stores[0].start()
    line_q.relay(n - 1)
    for j in range(1, n):
        line_q.close(j)
    line_q.gathered()
    stores.append(pltpu.make_async_copy(r.every, r.every_hbm, r.loads.at[1]))
    stores[1].start()
    for step in range(1, parts):
        spread(step).wait_recv()
    small = r.terms_all[0]
    for k in range(1, parts):
        small = small + r.terms_all[k]
    r.terms_out[...] = small
    for k in range(3):
        for step in others:
            swap(k, step).wait_send()
    for step in range(1, parts):
        spread(step).wait_send()
    scatter.finish()
    sums.finish()
    line_u.finish()
    line_q.finish()
    for store in stores:
        store.wait()


def close_part(ident, packed, gu_piece, terms, hidden, down_weight):
    parts, size, piece, cols = packed.shape
    n = parts // 2
    rows, width = hidden.shape[1], down_weight.shape[1]
    vmem = pl.BlockSpec(memory_space=pltpu.VMEM)
    hbm = pl.BlockSpec(memory_space=pl.ANY)
    dma = lambda *s: pltpu.SemaphoreType.DMA(s)
    gu_shape = (parts,) + gu_piece.shape
    scratch = scatter_shapes(size, rows, width)
    chips = pltpu.VMEM((n, size, piece, cols), BF)
    return pl.pallas_call(
        functools.partial(close_kernel, size, parts),
        out_shape=[
            jax.ShapeDtypeStruct(packed.shape, BF),
            jax.ShapeDtypeStruct(gu_shape, BF),
            jax.ShapeDtypeStruct((rows, width), F32),
            jax.ShapeDtypeStruct(terms.shape[1:], F32),
        ],
        in_specs=[vmem, hbm, vmem, vmem, vmem],
        out_specs=[hbm, hbm, vmem, vmem],
        scratch_shapes=scratch[:-2]
        + [
            chips,
            chips,
            chips,
            chips,
            pltpu.VMEM(packed.shape, BF),
            pltpu.VMEM((size, piece, cols), BF),
            pltpu.VMEM(gu_shape, BF),
            pltpu.VMEM(terms.shape, F32),
            pltpu.VMEM((parts,) + terms.shape[1:], F32),
        ]
        + scratch[-2:]
        + [dma(3, size - 1)] * 2
        + [dma(parts - 1)] * 2
        + [dma(2)]
        + line_sems(parts) * 3,
        compiler_params=pltpu.CompilerParams(
            collective_id=ident, has_side_effects=True, vmem_limit_bytes=67_000_000
        ),
        cost_estimate=pl.CostEstimate(
            flops=2 * size * rows * down_weight.size, bytes_accessed=500_000_000, transcendentals=0
        ),
        name="close_part",
    )(packed, gu_piece, terms, hidden, down_weight)


def pack_kernel(size, parts, x_ref, g_ref, *refs):
    out_ref = refs[-1]
    full = dot_rows(x_ref[...], g_ref[...])
    pair = out_ref.shape[1]
    rows = full.shape[0] // pair
    piece = rows // parts
    for k in range(pair):
        own = full[k * rows : (k + 1) * rows]
        if len(refs) == 3:
            heads_ref, gb_ref = refs[0], refs[1]
            side = dot_rows(heads_ref[...], gb_ref[...])
            wide = side.shape[1] // pair
            own = jnp.concatenate([own, side[:, k * wide : (k + 1) * wide]], 1)
        out_ref[:, k] = own.astype(BF).reshape(parts, piece, own.shape[1])


def pack_grads(parts, size, x, g, heads=None, gb=None):
    width, cols = x.shape[1], g.shape[1]
    rows = width // size
    piece = rows // parts
    if piece % 8 or (2 * rows) % 128:
        full = dot_rows(x, g).reshape(size, parts, piece, cols)
        if heads is not None:
            side = dot_rows(heads, gb).reshape(parts, piece, size, -1).transpose(2, 0, 1, 3)
            full = jnp.concatenate([full, side], 3)
        return full.transpose(1, 0, 2, 3).astype(BF)
    total = x.shape[0]
    pair = pl.BlockSpec((total, 2 * rows), lambda i: (0, i))
    whole = lambda a: pl.BlockSpec(a.shape, lambda i: (0, 0), pipeline_mode=pl.Buffered(1))
    args, specs = [x, g], [pair, whole(g)]
    out_cols = cols
    if heads is not None:
        args += [heads, gb]
        specs += [whole(heads), pair]
        out_cols += rows
    return pl.pallas_call(
        functools.partial(pack_kernel, size, parts),
        grid=(size // 2,),
        out_shape=jax.ShapeDtypeStruct((parts, size, piece, out_cols), BF),
        in_specs=specs,
        out_specs=pl.BlockSpec((parts, 2, piece, out_cols), lambda i: (0, i, 0, 0)),
        cost_estimate=pl.CostEstimate(
            flops=2 * total * width * out_cols,
            bytes_accessed=2 * (x.size + g.size + width * out_cols),
            transcendentals=0,
        ),
        name="pack_grads",
    )(*args)


def unpack_kernel(widths, every_ref, *outs):
    size = every_ref.shape[1]
    blocks = [every_ref[0, i].astype(F32) for i in range(size)]
    low = 0
    for width, out in zip(widths, outs):
        out[...] = jnp.concatenate([b[:, low : low + width] for b in blocks], 1)
        low += width


def unpack_grads(every, widths):
    parts, size, piece, cols = every.shape
    if piece % 8:
        outs, low = [], 0
        for width in widths:
            block = every[:, :, :, low : low + width].transpose(0, 2, 1, 3)
            outs.append(block.reshape(parts * piece, size * width).astype(F32))
            low += width
        return outs
    return pl.pallas_call(
        functools.partial(unpack_kernel, widths),
        grid=(parts,),
        out_shape=[jax.ShapeDtypeStruct((parts * piece, size * w), F32) for w in widths],
        in_specs=[pl.BlockSpec((1, size, piece, cols), lambda i: (i, 0, 0, 0))],
        out_specs=[pl.BlockSpec((piece, size * w), lambda i: (i, 0)) for w in widths],
        cost_estimate=pl.CostEstimate(flops=0, bytes_accessed=every.size * 6, transcendentals=0),
        name="unpack_grads",
    )(every)


def columns_piece(weights, part, parts):
    size = lax.axis_size("fsdp")
    rows = weights[0].shape[0] // parts
    pieces = []
    for weight in weights:
        own = lax.dynamic_slice_in_dim(weight, part * rows, rows, 0)
        pieces.append(own.reshape(rows, size, -1))
    return jnp.concatenate(pieces, 2).transpose(1, 0, 2)


def shards(
    tokens,
    seq_lengths,
    seq_offsets,
    norm1_gain,
    conv_weight,
    query_weight,
    key_weight,
    value_weight,
    out_weight,
    norm2_gain,
    gate_weight,
    up_weight,
    down_weight,
    cotangent,
):
    size = lax.axis_size("fsdp")
    parts = lax.axis_size("seq")
    part = lax.axis_index("seq")
    me = lax.axis_index("fsdp")
    own_tokens = tokens[0]
    rows, width = own_tokens.shape
    slice_width = norm1_gain.shape[0]
    first_slot = part * rows
    count = seq_lengths.shape[1]

    slot_ext = first_slot - 2 + jnp.arange(rows + 2, dtype=jnp.int32)
    segment_ext = segment_of(
        slot_ext, count, lambda j: seq_lengths[0, j], lambda j: seq_offsets[0, j]
    )
    segment_own = segment_ext[2:]
    same_one = (segment_own == segment_ext[1:-1]).astype(F32)[:, None]
    same_two = (segment_own == segment_ext[:-2]).astype(F32)[:, None]
    live_mask = (segment_own >= 0).astype(F32)[:, None]

    gains = jnp.concatenate(
        [
            norm1_gain[None],
            norm2_gain[None],
            conv_weight.T,
            jnp.zeros((3, slice_width), BF),
        ],
        0,
    )
    table = jnp.zeros((8, 128), jnp.int32)
    table = table.at[0, :count].set(seq_lengths[0]).at[1, :count].set(seq_offsets[0])
    qkv_piece = columns_piece((query_weight, key_weight, value_weight), part, parts)
    gu_piece = columns_piece((gate_weight, up_weight), part, parts)
    edge_tokens = shifted(own_tokens[rows - 2 :], "seq", 1)
    grad_down = (cotangent[0].astype(F32) * live_mask).astype(BF)
    (
        gated_all,
        qkv,
        edge,
        qkv_map,
        middle,
        heads_out,
        grad_down_all,
        normed_all,
        hidden,
        grad_gu,
        gu_map,
        gains_all,
        table_all,
    ) = forward_part(
        0,
        count,
        own_tokens,
        jnp.pad(edge_tokens, ((0, 6), (0, 0))),
        grad_down,
        gains,
        table,
        qkv_piece,
        gu_piece,
        out_weight,
        down_weight,
    )
    local = out_weight.shape[0]
    flat = lambda a: a.reshape(-1, a.shape[-1])
    lens_all, starts_all = table_all[:, 0, :count], table_all[:, 1, :count]
    gains_all = gains_all.transpose(1, 0, 2).reshape(8, width)
    norm_one = gains_all[0].astype(F32)
    norm_two = gains_all[1].astype(F32)
    taps = gains_all[2:5].astype(F32)
    qkv_map, gu_map = qkv_map.reshape(width, -1), gu_map.reshape(width, -1)
    grad_down_all = flat(grad_down_all)

    extended = jnp.concatenate([edge_tokens, own_tokens], 0).astype(F32)
    scale_one = lax.rsqrt(jnp.mean(extended * extended, axis=1, keepdims=True) + EPS)
    normed = extended * scale_one * norm_one
    conv_mix = (
        normed[2:] * taps[0]
        + same_one * normed[1:-1] * taps[1]
        + same_two * normed[:-2] * taps[2]
    )

    gu_packed = pack_grads(parts, size, flat(normed_all), flat(grad_gu))
    down_packed = dot_rows(flat(hidden), grad_down_all).astype(BF)
    grad_middle, norm2_term, grad_branch_all, dqkv, grad_gated, gu_piece, down_every = back_part(
        4,
        lens_all,
        starts_all,
        grad_gu,
        gu_map,
        middle,
        grad_down,
        norm_two[None],
        out_weight,
        edge,
        qkv,
        qkv_map,
        gu_packed,
        down_packed.reshape(parts, -1, width),
    )
    norm2_term = norm2_term[0]
    down_total = down_every.reshape(-1, width).astype(F32)
    qkvo_packed = pack_grads(
        parts, size, flat(gated_all), flat(dqkv), flat(heads_out), flat(grad_branch_all)
    )

    normed_own = normed[2:]
    grad_mix = grad_gated * normed_own
    part_zero = jnp.pad(grad_gated * conv_mix + grad_mix * taps[0], ((2, 0), (0, 0)))
    part_one = jnp.pad(grad_mix * same_one * taps[1], ((1, 1), (0, 0)))
    part_two = jnp.pad(grad_mix * same_two * taps[2], ((0, 2), (0, 0)))
    grad_normed = part_zero + part_one + part_two
    unit_one = extended * scale_one
    grad_unit_one = grad_normed * norm_one
    grad_extended = scale_one * (
        grad_unit_one - unit_one * jnp.mean(grad_unit_one * unit_one, axis=1, keepdims=True)
    )
    edge_back = shifted(grad_extended[:2], "seq", -1)
    tokens_grad = grad_middle + grad_extended[2:] + jnp.pad(edge_back, ((rows - 2, 0), (0, 0)))

    terms = jnp.stack(
        [
            jnp.sum(grad_normed * unit_one, axis=0),
            norm2_term,
            jnp.sum(grad_mix * normed_own, axis=0),
            jnp.sum(grad_mix * same_one * normed[1:-1], axis=0),
            jnp.sum(grad_mix * same_two * normed[:-2], axis=0),
        ]
    )
    terms = jnp.pad(terms, ((0, 3), (0, 0))).reshape(8, size, slice_width).transpose(1, 0, 2)
    qkvo_packed, gu_piece, terms, down_total, tokens_grad = lax.optimization_barrier(
        (qkvo_packed, gu_piece, terms, down_total, tokens_grad)
    )
    qkvo_every, gu_every, feed, terms = close_part(
        5, qkvo_packed, gu_piece, terms, hidden, down_weight
    )
    gate_total, up_total = unpack_grads(gu_every, (gu_map.shape[1] // 2,) * 2)
    query_total, key_total, value_total, out_total = unpack_grads(qkvo_every, (local,) * 4)

    layer_out = (live_mask * (middle + feed)).astype(BF)[None]
    return (
        layer_out,
        tokens_grad[None],
        terms[0],
        terms[2:5].T,
        query_total,
        key_total,
        value_total,
        out_total,
        terms[1],
        gate_total,
        up_total,
        down_total,
    )


def solution(mesh):
    placed = (
        P("fsdp", "seq", None),
        P("fsdp", None),
        P("fsdp", None),
        P("fsdp"),
        P("fsdp", None),
        P("fsdp", None),
        P("fsdp", None),
        P("fsdp", None),
        P("fsdp", None),
        P("fsdp"),
        P("fsdp", None),
        P("fsdp", None),
        P("fsdp", None),
        P("fsdp", "seq", None),
    )
    return jax.shard_map(
        shards,
        mesh=mesh,
        in_specs=placed,
        out_specs=(
            P("fsdp", "seq", None),
            P("fsdp", "seq", None),
            P("fsdp"),
            P("fsdp", None),
            P("fsdp", None),
            P("fsdp", None),
            P("fsdp", None),
            P("fsdp", None),
            P("fsdp"),
            P("fsdp", None),
            P("fsdp", None),
            P("fsdp", None),
        ),
        check_vma=False,
    )
```

```python
import functools
from typing import Any, NamedTuple

import jax
import jax.numpy as jnp
from jax import lax
from jax.experimental import pallas as pl
from jax.experimental.pallas import tpu as pltpu
from jax.sharding import PartitionSpec as P

HEADS = 16
WINDOW = 64
HEAD_DIM = 112
BLOCK = 128

EPS = 1e-05
NEG = -1e30
SCALE = HEAD_DIM ** (-0.5)
MESH_ID = pl.DeviceIdType.MESH
BF = jnp.bfloat16
F32 = jnp.float32


def shifted(array, axis, by):
    length = lax.axis_size(axis)
    pairs = [(i, i + by) for i in range(length) if 0 <= i + by < length]
    return lax.ppermute(array, axis, pairs)


def segment_of(slot, count, lengths, starts):
    found = jnp.full(slot.shape, -1, jnp.int32)
    for j in range(count):
        inside = (slot >= starts(j)) & (slot < starts(j) + lengths(j))
        found = jnp.where(inside, j, found)
    return jnp.where(slot < 0, -2, found)


def dot_rows(left, right):
    return lax.dot_general(left, right, (((0,), (0,)), ((), ())), preferred_element_type=F32)


def dot_trans(left, right):
    return lax.dot_general(left, right, (((1,), (1,)), ((), ())), preferred_element_type=F32)


def dot(left, right):
    return jnp.dot(left, right, preferred_element_type=F32)


def masks_of(first, block, count, length, start):
    rows = first + block * BLOCK
    query = rows + lax.broadcasted_iota(jnp.int32, (BLOCK, 1), 0)
    keys = rows - WINDOW + lax.broadcasted_iota(jnp.int32, (1, BLOCK + WINDOW), 1)
    seg_q = segment_of(query, count, length, start)
    seg_k = segment_of(keys, count, length, start)
    far = query - keys
    return (far >= 0) & (far <= WINDOW) & (seg_q == seg_k)


def soft_of(query, keys, mask):
    scores = dot_trans(query, keys) * SCALE
    scores = jnp.where(mask, scores, NEG)
    peak = jnp.max(scores, axis=1, keepdims=True)
    exponent = jnp.exp(scores - peak)
    return exponent / jnp.sum(exponent, axis=1, keepdims=True)


def lane_head(width):
    return lax.broadcasted_iota(jnp.int32, (1, width), 1) // HEAD_DIM


def remote(src, dst, send, recv, **peer):
    return pltpu.make_async_remote_copy(
        src_ref=src,
        dst_ref=dst,
        send_sem=send,
        recv_sem=recv,
        device_id=peer,
        device_id_type=MESH_ID,
    )


def greet_group(barrier, size):
    me = lax.axis_index("fsdp")
    for step in range(1, size):
        peer = lax.rem(me + step, size)
        pl.semaphore_signal(barrier, inc=1, device_id={"fsdp": peer}, device_id_type=MESH_ID)


class Group:
    def __init__(self, size):
        self.size = size
        self.me = lax.axis_index("fsdp")
        self.square = size == 4
        if self.square:
            x, y = lax.rem(self.me, 2), self.me // 2
            self.at = lambda bx, by: lax.rem(y + by, 2) * 2 + lax.rem(x + bx, 2)
            self.x, self.y, self.far = self.at(1, 0), self.at(0, 1), self.at(1, 1)

    def from_own(self, step):
        if self.square:
            return self.at(lax.rem(step, 2), step // 2)
        return lax.rem(self.me - step + self.size, self.size)

    def to_own(self, step):
        if self.square:
            return self.at(1 - step // 2, 1 - lax.rem(step, 2))
        return lax.rem(self.me + 1 + step, self.size)


class Gather:
    def __init__(self, group, ref, send, recv):
        self.group, self.ref, self.send, self.recv = group, ref, send, recv
        self.half = ref.shape[1] // 2

    def part(self, k, slot, half, peer):
        view = self.ref.at[slot, pl.ds(half * self.half, self.half)]
        return remote(view, view, self.send.at[k], self.recv.at[k], fsdp=peer)

    def whole(self, k):
        g = self.group
        view = self.ref.at[g.me]
        sems = self.send.at[k - 1], self.recv.at[k - 1]
        return remote(view, view, *sems, fsdp=lax.rem(g.me + k, g.size))

    def copy(self, k):
        g = self.group
        if not g.square:
            return self.whole(k + 1)
        slot = (g.me, g.me, g.me, g.me, g.x, g.y)[k]
        half = (0, 1, 0, 1, 0, 1)[k]
        return self.part(k, slot, half, (g.x, g.x, g.y, g.y, g.y, g.x)[k])

    def start_half(self, half):
        if self.group.square:
            self.copy(half).start()
            self.copy(2 + half).start()
        elif half == 1:
            for k in range(self.group.size - 1):
                self.copy(k).start()

    def relay(self):
        if self.group.square:
            self.copy(0).wait_recv()
            self.copy(4).start()
            self.copy(3).wait_recv()
            self.copy(5).start()

    def ready(self, step):
        if not self.group.square:
            self.copy(step - 1).wait_recv()
        elif step == 3:
            self.copy(4).wait_recv()
            self.copy(5).wait_recv()
        else:
            self.copy(step).wait_recv()

    def finish(self):
        for k in range(transfers(self.group.size)):
            self.copy(k).wait_send()


class Scatter:
    def __init__(self, group, part, first, over, joined, last, send, recv):
        self.group, self.part = group, part
        self.first, self.over, self.joined, self.last = first, over, joined, last
        self.send, self.recv = send, recv
        self.half = part.shape[1] // 2

    def copy(self, k):
        g, half = self.group, self.half
        low, high = pl.ds(0, half), pl.ds(half, half)
        if not g.square:
            src, dst, peer = self.part.at[k], self.first.at[k], lax.rem(g.me + 1 + k, g.size)
        else:
            src, dst, peer = (
                lambda: (self.part.at[0, low], self.over.at[0], g.x),
                lambda: (self.part.at[0, high], self.over.at[1], g.y),
                lambda: (self.part.at[1, low], self.first.at[0], g.x),
                lambda: (self.part.at[2, high], self.first.at[1], g.y),
                lambda: (self.joined.at[0], self.last.at[0], g.y),
                lambda: (self.joined.at[1], self.last.at[1], g.x),
            )[k]()
        return remote(src, dst, self.send.at[k], self.recv.at[k], fsdp=peer)

    def made(self, step):
        if not self.group.square:
            self.copy(step).start()
        elif step == 0:
            self.copy(0).start()
            self.copy(1).start()
        elif step in (1, 2):
            self.copy(step + 1).start()

    def join(self):
        if not self.group.square:
            return
        half = self.half
        for k, (step, rows) in enumerate(((2, slice(0, half)), (1, slice(half, 2 * half)))):
            self.copy(k).wait_recv()
            own = self.part[step, rows].astype(F32)
            self.joined[k] = (own + self.over[k].astype(F32)).astype(BF)
            self.copy(4 + k).start()

    def total(self, half):
        count = self.half
        if self.group.square:
            self.copy(2 + half).wait_recv()
            self.copy(4 + half).wait_recv()
            return self.first[half].astype(F32) + self.last[half].astype(F32)
        if half == 0:
            for k in range(self.group.size - 1):
                self.copy(k).wait_recv()
        rows = slice(half * count, (half + 1) * count)
        out = self.first[0, rows].astype(F32)
        for k in range(1, self.group.size - 1):
            out = out + self.first[k, rows].astype(F32)
        return out

    def finish(self):
        for k in range(transfers(self.group.size)):
            self.copy(k).wait_send()


class Line:
    def __init__(self, parts, sems):
        self.rank = lax.axis_index("seq")
        self.parts, self.length = parts, parts // 2
        self.z, self.core = self.rank // 2, lax.rem(self.rank, 2)
        self.above, self.below = self.rank + 2, self.rank - 2
        self.beside = self.rank + 1 - 2 * self.core
        self.has_above, self.has_below = self.z < self.length - 1, self.z > 0
        self.sems = sems

    def greet(self, barrier):
        def one(peer):
            pl.semaphore_signal(barrier, inc=1, device_id={"seq": peer}, device_id_type=MESH_ID)

        one(self.beside)
        pl.when(self.has_above)(lambda: one(self.above))
        pl.when(self.has_below)(lambda: one(self.below))
        n, z = self.length, self.z
        return 1 + (2 * n - 2 - z) // n + (z + n - 1) // n

    def up(self, k, owner):
        view = self.view(owner)
        return remote(view, view, self.sems[0].at[k], self.sems[1].at[k], seq=self.above)

    def down(self, k, owner):
        view = self.view(owner)
        return remote(view, view, self.sems[2].at[k], self.sems[3].at[k], seq=self.below)

    def side(self, k, owner):
        view = self.view(owner)
        return remote(view, view, self.sems[4].at[k], self.sems[5].at[k], seq=self.beside)

    def gather(self, view):
        self.view = view
        pl.when(self.has_above)(lambda: self.up(0, self.rank).start())
        pl.when(self.has_below)(lambda: self.down(0, self.rank).start())
        self.side(self.z, self.rank).start()

    def own_up(self):
        pl.when(self.has_above)(lambda: self.up(0, self.rank).start())

    def own_down(self):
        pl.when(self.has_below)(lambda: self.down(0, self.rank).start())

    def relay_up(self, j):
        rank, z = self.rank, self.z

        @pl.when((z >= j) & self.has_above)
        def _():
            self.up(j - 1, rank).wait_recv()
            self.up(j, rank - 2 * j).start()
            self.side(z - j, rank - 2 * j).start()

    def relay_down(self, j):
        rank, z = self.rank, self.z

        @pl.when((z + j < self.length) & self.has_below)
        def _():
            self.down(j - 1, rank).wait_recv()
            self.down(j, rank + 2 * j).start()
            self.side(z + j, rank + 2 * j).start()

    def relay(self, j):
        self.relay_up(j)
        self.relay_down(j)

    def close(self, j):
        rank, z = self.rank, self.z

        @pl.when((z >= j) & (z == self.length - 1))
        def _():
            self.up(j - 1, rank).wait_recv()
            self.side(z - j, rank - 2 * j).start()

        @pl.when((z + j < self.length) & (z == 0))
        def _():
            self.down(j - 1, rank).wait_recv()
            self.side(z + j, rank + 2 * j).start()

    def gathered(self):
        for k in range(self.length):
            self.side(k, self.rank).wait_recv()

    def finish(self):
        rank, z = self.rank, self.z
        for k in range(self.length):
            self.side(k, rank).wait_send()
        pl.when(self.has_above)(lambda: self.up(0, rank).wait_send())
        pl.when(self.has_below)(lambda: self.down(0, rank).wait_send())
        for j in range(1, self.length):
            pl.when((z >= j) & self.has_above)(lambda: self.up(j, rank).wait_send())
            pl.when((z + j < self.length) & self.has_below)(lambda: self.down(j, rank).wait_send())


class LineSum:
    def __init__(self, line, x, pre, acc, up_in, down_in, sems):
        self.line, self.x, self.pre, self.acc = line, x, pre, acc
        self.up_in, self.down_in, self.sems = up_in, down_in, sems

    def share(self, k):
        line = self.line
        src = self.x.at[2 * k + 1 - line.core]
        return remote(src, self.pre.at[k], self.sems[0].at[k], self.sems[1].at[k], seq=line.beside)

    def up(self, k):
        sems = self.sems[2].at[k], self.sems[3].at[k]
        return remote(self.acc.at[k], self.up_in.at[k], *sems, seq=self.line.above)

    def down(self, k):
        sems = self.sems[4].at[k], self.sems[5].at[k]
        return remote(self.acc.at[k], self.down_in.at[k], *sems, seq=self.line.below)

    def pair(self, m):
        return self.line.length - 1 - m, m

    def trade(self):
        n = self.line.length
        for m in range((n + 1) // 2):
            for k in sorted(set(self.pair(m))):
                self.share(k).start()

    def merge(self, k):
        self.share(k).wait_recv()
        own = self.x[2 * k + self.line.core].astype(F32)
        self.acc[k] = (own + self.pre[k].astype(F32)).astype(BF)

    def begin(self, m):
        n, z = self.line.length, self.line.z
        far, near = self.pair(m)
        if m < (n + 1) // 2:
            for k in sorted({far, near}):
                self.merge(k)
        if m < n - 1:
            pl.when(z == 0)(lambda: self.up(far).start())
            pl.when(z == n - 1)(lambda: self.down(near).start())

    def add(self, k, more):
        self.acc[k] = (self.acc[k].astype(F32) + more[k].astype(F32)).astype(BF)

    def advance(self, t):
        z, n = self.line.z, self.line.length
        far, near = n - 1 + z - t, t - n + 1 + z

        @pl.when((z >= 1) & (z <= t))
        def _():
            self.up(far).wait_recv()
            self.add(far, self.up_in)
            self.up(far).start()

        @pl.when((z <= n - 2) & (z >= n - 1 - t))
        def _():
            self.down(near).wait_recv()
            self.add(near, self.down_in)
            self.down(near).start()

    def total(self):
        z = self.line.z

        @pl.when(z > 0)
        def _():
            self.up(z).wait_recv()
            self.add(z, self.up_in)

        @pl.when(z < self.line.length - 1)
        def _():
            self.down(z).wait_recv()
            self.add(z, self.down_in)

    def finish(self):
        for k in range(self.line.length):
            self.share(k).wait_send()
            pl.when(k > self.line.z)(lambda: self.up(k).wait_send())
            pl.when(k < self.line.z)(lambda: self.down(k).wait_send())


class StagedSum(LineSum):
    def __init__(self, stage, load, *args):
        super().__init__(*args)
        self.stage, self.load = stage, load

    def fetch(self, slot, src):
        return pltpu.make_async_copy(src, self.stage.at[slot], self.load.at[slot])

    def merge(self, k):
        self.share(k).wait_recv()
        own = self.fetch(0, self.x.at[2 * k + self.line.core])
        other = self.fetch(1, self.pre.at[k])
        own.start()
        other.start()
        own.wait()
        other.wait()
        self.acc[k] = (self.stage[0].astype(F32) + self.stage[1].astype(F32)).astype(BF)

    def add(self, k, more):
        came = self.fetch(0, more.at[k])
        came.start()
        came.wait()
        self.acc[k] = (self.acc[k].astype(F32) + self.stage[0].astype(F32)).astype(BF)


def line_sems(parts):
    return [pltpu.SemaphoreType.DMA((parts // 2,))] * 6


def transfers(size):
    return 6 if size == 4 else size - 1


def scatter_shapes(size, rows, width):
    half = rows // 2
    slots = (2, half, width) if size == 4 else (size - 1, rows, width)
    return [
        pltpu.VMEM((size - 1, rows, width), BF),
        pltpu.VMEM(slots, BF),
        pltpu.VMEM((2, half, width), BF),
        pltpu.VMEM((2, half, width), BF),
        pltpu.VMEM((2, half, width), BF),
        pltpu.SemaphoreType.DMA((transfers(size),)),
        pltpu.SemaphoreType.DMA((transfers(size),)),
    ]


def each_step(size, body):
    def one(step, carry):
        body(step, lambda k: pl.when(step == k))
        return carry

    lax.fori_loop(0, size, one, 0)


class ForwardRefs(NamedTuple):
    tokens: Any
    edge_tok: Any
    grad: Any
    gains: Any
    table: Any
    qkv_piece: Any
    gu_piece: Any
    out_map: Any
    down_map: Any
    gated_hbm: Any
    qkv_hbm: Any
    edge: Any
    qkv_map_hbm: Any
    middle: Any
    heads: Any
    grads_hbm: Any
    norm_hbm: Any
    hidden_hbm: Any
    gu_grad_hbm: Any
    gu_map_hbm: Any
    gains_all: Any
    table_all: Any
    part: Any
    first: Any
    over: Any
    joined: Any
    last: Any
    all: Any
    grads: Any
    qkv: Any
    qkv_map: Any
    gu_map: Any
    tail: Any
    own: Any
    hidden: Any
    gu_grad: Any
    s_send: Any
    s_recv: Any
    a_send: Any
    a_recv: Any
    g_send: Any
    g_recv: Any
    c_send: Any
    c_recv: Any
    m_send: Any
    m_recv: Any
    halo_send: Any
    halo_recv: Any
    loads: Any
    stores: Any
    hidden_store: Any
    gu_store: Any


def forward_kernel(size, parts, count, *refs):
    named = len(ForwardRefs._fields)
    r, sems = ForwardRefs(*refs[:named]), refs[named:]
    rank = lax.axis_index("seq")
    rows = r.tokens.shape[0]
    half = rows // 2
    local = r.out_map.shape[0]
    inner = r.down_map.shape[0]
    slot = rank * rows
    group = Group(size)
    me = group.me
    line_q, line_u = Line(parts, sems[:6]), Line(parts, sems[6:])

    barrier = pltpu.get_barrier_semaphore()
    greet_group(barrier, size)
    known = line_q.greet(barrier)

    def greet(peer):
        pl.semaphore_signal(barrier, inc=1, device_id={"seq": peer}, device_id_type=MESH_ID)

    pl.when(line_q.has_above & (line_q.core == 1))(lambda: greet(rank + 1))
    pl.when(line_q.has_below & (line_q.core == 0))(lambda: greet(rank - 1))
    n, z = line_q.length, line_q.z
    known = known + (2 * n - 2 - z) // n * line_q.core + (z + n - 1) // n * (1 - line_q.core)
    own_pieces = [
        pltpu.make_async_copy(src.at[me], dst.at[me, rank], r.loads.at[k])
        for k, (src, dst) in enumerate(
            ((r.qkv_piece, r.qkv_map), (r.gu_piece, r.gu_map))
        )
    ]
    for copy in own_pieces:
        copy.start()
    r.gains_all[me] = r.gains[...]
    r.table_all[me] = r.table[...]
    r.grads[me] = r.grad[...]
    pl.semaphore_wait(barrier, size - 1 + known)

    def swap(k, step):
        peer = lax.rem(me + step, size)
        src, dst = (
            lambda: (r.gains_all.at[me], r.gains_all.at[me]),
            lambda: (r.table_all.at[me], r.table_all.at[me]),
            lambda: (r.qkv_piece.at[peer], r.qkv_map.at[me, rank]),
            lambda: (r.gu_piece.at[peer], r.gu_map.at[me, rank]),
        )[k]()
        return remote(src, dst, r.m_send.at[k, step - 1], r.m_recv.at[k, step - 1], fsdp=peer)

    others = range(1, size)
    for k in range(4):
        for step in others:
            swap(k, step).start()
    for k in range(2):
        for step in others:
            swap(k, step).wait_recv()

    gains = jnp.concatenate([r.gains_all[f] for f in range(size)], 1).astype(F32)
    own_table = r.table_all[me]
    slots = slot + lax.broadcasted_iota(jnp.int32, (rows, 1), 0)
    length = lambda j: own_table[0:1, j : j + 1]
    start = lambda j: own_table[1:2, j : j + 1]
    segment = segment_of(slots, count, length, start)
    same_one = (segment == segment_of(slots - 1, count, length, start)).astype(F32)
    same_two = (segment == segment_of(slots - 2, count, length, start)).astype(F32)
    tokens = r.tokens[...].astype(F32)
    edge = r.edge_tok[...].astype(F32)

    def norm(a):
        return a * lax.rsqrt(jnp.mean(a * a, axis=1, keepdims=True) + EPS) * gains[0:1]

    normed, edge = norm(tokens), norm(edge)
    row = lax.broadcasted_iota(jnp.int32, (rows, 1), 0)
    back_one = jnp.where(row == 0, edge[1:2], pltpu.roll(normed, 1, 0))
    back_two = jnp.where(
        row == 0, edge[0:1], jnp.where(row == 1, edge[1:2], pltpu.roll(normed, 2, 0))
    )
    mixed = (
        normed * gains[2:3]
        + same_one * back_one * gains[3:4]
        + same_two * back_two * gains[4:5]
    )
    all_ref = r.all
    all_ref[me] = (mixed * normed).astype(BF)
    gather = Gather(group, all_ref, r.a_send, r.a_recv)
    gather.start_half(0)
    gather.start_half(1)

    own_pieces[0].wait()
    for step in others:
        swap(2, step).wait_recv()
    line_q.gather(lambda owner: r.qkv_map.at[:, owner])
    line_u.view = lambda owner: r.gu_map.at[:, owner]
    gather.relay()
    grads = Gather(group, r.grads, r.c_send, r.c_recv)
    grads.start_half(0)
    grads.start_half(1)
    own_pieces[1].wait()
    for step in others:
        swap(3, step).wait_recv()
    line_u.side(z, rank).start()
    pl.when(z == 0)(line_u.own_up)
    pl.when(z == n - 1)(line_u.own_down)
    for j in range(1, n):
        line_q.relay(j)
        line_q.close(j)
        pl.when(z == j)(line_u.own_up)
        pl.when(z == n - 1 - j)(line_u.own_down)
    for step in others:
        gather.ready(step)
    grads.relay()
    line_q.gathered()
    keeps = [
        pltpu.make_async_copy(all_ref, r.gated_hbm, r.stores.at[size]),
        pltpu.make_async_copy(r.qkv_map, r.qkv_map_hbm, r.stores.at[size + 1]),
    ]
    for keep in keeps:
        keep.start()

    weights = r.qkv_map[...].reshape(-1, r.qkv_map.shape[3])

    def halo(step):
        g = group.to_own(step)
        sem = r.halo_send.at[step], r.halo_recv.at[step]
        return remote(r.tail.at[g], r.edge.at[g], *sem, seq=rank + 1)

    def project(step, is_step):
        g = group.to_own(step)
        out = dot(all_ref[g], weights).astype(BF)
        r.qkv[g] = out
        r.tail[g] = out[rows - WINDOW :, local:]
        pl.when(rank < parts - 1)(lambda: halo(step).start())

    each_step(size, project)

    @pl.when(rank == 0)
    def _():
        r.edge[...] = jnp.zeros_like(r.edge)

    keeps.append(pltpu.make_async_copy(r.qkv, r.qkv_hbm, r.stores.at[size + 2]))
    keeps[2].start()
    line_u.relay(1)
    gather.finish()
    keeps[0].wait()

    scatter = Scatter(
        group, r.part, r.first, r.over, r.joined, r.last, r.s_send, r.s_recv
    )
    head_of = lane_head(local)

    def mix(step, is_step):
        g = group.to_own(step)
        pl.when(rank > 0)(lambda: halo(step).wait_recv())
        own, edge, table = r.qkv[g], r.edge[g], r.table_all[g]
        queries = own[:, :local]
        keys = jnp.concatenate([edge[:, :local], own[:, local : 2 * local]], 0)
        values = jnp.concatenate([edge[:, local:], own[:, 2 * local :]], 0)
        outs = []
        for block in range(rows // BLOCK):
            mask = masks_of(
                slot,
                block,
                count,
                lambda j: table[0:1, j : j + 1],
                lambda j: table[1:2, j : j + 1],
            )
            low = block * BLOCK
            query = queries[low : low + BLOCK]
            key = keys[low : low + BLOCK + WINDOW]
            value = values[low : low + BLOCK + WINDOW]
            out = jnp.zeros((BLOCK, local), F32)
            for head in range(local // HEAD_DIM):
                mine = head_of == head
                soft = soft_of(jnp.where(mine, query, jnp.zeros_like(query)), key, mask)
                out = jnp.where(mine, dot(soft.astype(BF), value), out)
            outs.append(out.astype(BF))
        heads = jnp.concatenate(outs, 0)
        r.heads[g] = heads
        branch = dot(heads, r.out_map[...])
        is_step(size - 1)(lambda: r.own.__setitem__(..., branch))
        pl.when(step < size - 1)(lambda: r.part.__setitem__(step, branch.astype(BF)))
        for k in range(size - 1):
            is_step(k)(functools.partial(scatter.made, k))

    each_step(size, mix)
    scatter.join()
    for j in range(2, n):
        line_u.relay(j)
    gather = Gather(group, all_ref, r.g_send, r.g_recv)
    for h in range(2):
        span = slice(h * half, (h + 1) * half)
        total = r.own[span, :] + scatter.total(h)
        middle = r.tokens[span, :].astype(F32) + total
        r.middle[span, :] = middle
        scale = lax.rsqrt(jnp.mean(middle * middle, axis=1, keepdims=True) + EPS)
        all_ref[me, span] = (middle * scale * gains[1:2]).astype(BF)
        gather.start_half(h)
    gather.relay()
    for j in range(1, n):
        line_u.close(j)
    line_u.gathered()
    keeps.append(pltpu.make_async_copy(r.gu_map, r.gu_map_hbm, r.stores.at[size + 3]))
    keeps[3].start()

    def out_copies(step):
        g, two = group.from_own(step), lax.rem(step, 2)
        return (
            pltpu.make_async_copy(
                r.hidden.at[two], r.hidden_hbm.at[g], r.hidden_store.at[two]
            ),
            pltpu.make_async_copy(
                r.gu_grad.at[two], r.gu_grad_hbm.at[g], r.gu_store.at[two]
            ),
        )

    def norm_copy(g):
        return pltpu.make_async_copy(all_ref.at[g], r.norm_hbm.at[g], r.stores.at[g])

    def feed(step, is_step):
        g, two = group.from_own(step), lax.rem(step, 2)
        for k in others:
            is_step(k)(functools.partial(gather.ready, k))
            is_step(k)(functools.partial(grads.ready, k))

        @pl.when(step >= 2)
        def _():
            for copy in out_copies(step - 2):
                copy.wait()

        norm_copy(g).start()
        weights = r.gu_map[...].reshape(-1, r.gu_map.shape[3])
        acts = dot(all_ref[g], weights)
        gate, up = acts[:, :inner], acts[:, inner:]
        sigma = jax.nn.sigmoid(gate)
        silu = gate * sigma
        r.hidden[two] = (silu * up).astype(BF)
        grad_hidden = dot_trans(r.grads[g], r.down_map[...])
        grad_gate = grad_hidden * up * sigma * (1.0 + gate * (1.0 - sigma))
        r.gu_grad[two] = jnp.concatenate([grad_gate, grad_hidden * silu], 1).astype(BF)
        for copy in out_copies(step):
            copy.start()

    each_step(size, feed)
    keeps.append(pltpu.make_async_copy(r.grads, r.grads_hbm, r.stores.at[size + 4]))
    keeps[4].start()
    for k in range(4):
        for step in others:
            swap(k, step).wait_send()
    scatter.finish()
    gather.finish()
    grads.finish()
    line_q.finish()
    line_u.finish()

    @pl.when(rank < parts - 1)
    def _():
        for step in range(size):
            halo(step).wait_send()

    for keep in keeps[1:]:
        keep.wait()
    for g in range(size):
        norm_copy(g).wait()
    for step in (size - 2, size - 1):
        for copy in out_copies(step):
            copy.wait()


def forward_part(ident, count, tokens, edge, grad, gains, table, qkv_piece, gu_piece, out_weight, down_weight):
    size, parts = lax.axis_size("fsdp"), lax.axis_size("seq")
    rows, width = tokens.shape
    local, inner = out_weight.shape[0], down_weight.shape[0]
    piece, cols = gu_piece.shape[1:]
    vmem = pl.BlockSpec(memory_space=pltpu.VMEM)
    hbm = pl.BlockSpec(memory_space=pl.ANY)
    shape = lambda w: (size, rows, w)
    low = lambda s: jax.ShapeDtypeStruct(s, BF)
    maps = [(size, parts, piece, 3 * local), (size, parts, piece, cols)]
    dma = lambda *s: pltpu.SemaphoreType.DMA(s)
    hop = transfers(size)
    scratch = scatter_shapes(size, rows, width)
    return pl.pallas_call(
        functools.partial(forward_kernel, size, parts, count),
        out_shape=[
            low(shape(width)),
            low(shape(3 * local)),
            low((size, WINDOW, 2 * local)),
            low(maps[0]),
            jax.ShapeDtypeStruct((rows, width), F32),
            low(shape(local)),
            low(shape(width)),
            low(shape(width)),
            low(shape(inner)),
            low(shape(cols)),
            low(maps[1]),
            low((size,) + gains.shape),
            jax.ShapeDtypeStruct((size,) + table.shape, jnp.int32),
        ],
        in_specs=[vmem] * 5 + [hbm, hbm, vmem, vmem],
        out_specs=[hbm, hbm, vmem, hbm, vmem, vmem, hbm, hbm, hbm, hbm, hbm, vmem, vmem],
        scratch_shapes=scratch[:-2]
        + [
            pltpu.VMEM(shape(width), BF),
            pltpu.VMEM(shape(width), BF),
            pltpu.VMEM(shape(3 * local), BF),
            pltpu.VMEM(maps[0], BF),
            pltpu.VMEM(maps[1], BF),
            pltpu.VMEM((size, WINDOW, 2 * local), BF),
            pltpu.VMEM((rows, width), F32),
            pltpu.VMEM((2, rows, inner), BF),
            pltpu.VMEM((2, rows, cols), BF),
        ]
        + [dma(hop)] * 8
        + [dma(4, size - 1)] * 2
        + [dma(size)] * 2
        + [dma(2), dma(size + 5), dma(2), dma(2)]
        + line_sems(parts)
        + line_sems(parts),
        compiler_params=pltpu.CompilerParams(
            collective_id=ident, has_side_effects=True, vmem_limit_bytes=67_000_000
        ),
        cost_estimate=pl.CostEstimate(
            flops=2 * size * rows * width * (4 * local + 3 * inner),
            bytes_accessed=500_000_000,
            transcendentals=0,
        ),
        name="forward_part",
    )(tokens, edge, grad, gains, table, qkv_piece, gu_piece, out_weight, down_weight)


def heads_back(group, slot, count, lens_ref, starts_ref, own, edge, grad):
    rows, local = own.shape[0], own.shape[1] // 3
    head_of = lane_head(local)
    queries = own[:, :local]
    keys = jnp.concatenate([edge[:, :local], own[:, local : 2 * local]], 0)
    values = jnp.concatenate([edge[:, local:], own[:, 2 * local :]], 0)
    dqs, dks, dvs = [], [], []
    for block in range(rows // BLOCK):
        mask = masks_of(
            slot, block, count, lambda j: lens_ref[group, j], lambda j: starts_ref[group, j]
        )
        low = block * BLOCK
        span = slice(low, low + BLOCK + WINDOW)
        query, grads = queries[low : low + BLOCK], grad[low : low + BLOCK]
        key, value = keys[span], values[span]
        dq = jnp.zeros((BLOCK, local), F32)
        dk = jnp.zeros((BLOCK + WINDOW, local), F32)
        dv = jnp.zeros((BLOCK + WINDOW, local), F32)
        for head in range(local // HEAD_DIM):
            mine = head_of == head
            own_q = jnp.where(mine, query, jnp.zeros_like(query))
            own_g = jnp.where(mine, grads, jnp.zeros_like(grads))
            soft = soft_of(own_q, key, mask)
            grad_soft = dot_trans(own_g, value)
            total = jnp.sum(grad_soft * soft, axis=1, keepdims=True)
            grad_scores = (soft * (grad_soft - total)).astype(BF)
            dq = jnp.where(mine, dot(grad_scores, key), dq)
            dk = dk + dot_rows(grad_scores, own_q)
            dv = dv + dot_rows(soft.astype(BF), own_g)
        dqs.append(dq * SCALE)
        dks.append(dk * SCALE)
        dvs.append(dv)

    def joined(pieces):
        out = [pieces[0][:BLOCK]]
        for left, right in zip(pieces, pieces[1:]):
            out.append(left[BLOCK:] + right[:WINDOW])
            out.append(right[WINDOW:BLOCK])
        out.append(pieces[-1][BLOCK:])
        return jnp.concatenate(out, 0)

    return jnp.concatenate(dqs, 0), joined(dks), joined(dvs)


class BackRefs(NamedTuple):
    lens: Any
    starts: Any
    grad_gu_hbm: Any
    gu_map_hbm: Any
    middle: Any
    grad: Any
    gain: Any
    out_map: Any
    edge: Any
    qkv: Any
    qkv_map_hbm: Any
    gu_x: Any
    down_x: Any
    grad_middle: Any
    norm: Any
    all: Any
    dqkv: Any
    own: Any
    gu_slots: Any
    down_every: Any
    gu_pre: Any
    gu_up: Any
    gu_down: Any
    down_pre: Any
    down_up: Any
    down_down: Any
    part: Any
    first: Any
    over: Any
    joined: Any
    last: Any
    s_send: Any
    s_recv: Any
    t_send: Any
    t_recv: Any
    g_send: Any
    g_recv: Any
    grad_gu: Any
    gu_map: Any
    qkv_map: Any
    dedge: Any
    back: Any
    tail: Any
    h_send: Any
    h_recv: Any
    loads: Any
    gu_acc: Any
    gu_stage: Any
    gu_load: Any
    down_acc: Any
    down_stage: Any
    down_load: Any
    m_send: Any
    m_recv: Any


def back_kernel(size, parts, count, *refs):
    named = len(BackRefs._fields)
    r, sems = BackRefs(*refs[:named]), refs[named:]
    line = Line(parts, sems[:6])
    gu_sum = StagedSum(
        r.gu_stage, r.gu_load, line, r.gu_x, r.gu_pre, r.gu_acc, r.gu_up, r.gu_down, sems[6:12]
    )
    down_sum = StagedSum(
        r.down_stage,
        r.down_load,
        line,
        r.down_x,
        r.down_pre,
        r.down_acc,
        r.down_up,
        r.down_down,
        sems[12:],
    )
    rows = r.middle.shape[0]
    local = r.out_map.shape[0]
    rank = lax.axis_index("seq")
    slot = rank * rows
    group = Group(size)
    barrier = pltpu.get_barrier_semaphore()
    greet_group(barrier, size)

    def greet(peer):
        pl.semaphore_signal(barrier, inc=1, device_id={"seq": peer}, device_id_type=MESH_ID)

    known = line.greet(barrier)
    pl.when(line.has_above & (line.core == 1))(lambda: greet(rank + 1))
    pl.when(line.has_below & (line.core == 0))(lambda: greet(rank - 1))
    n, z = line.length, line.z
    known = known + (2 * n - 2 - z) // n * line.core + (z + n - 1) // n * (1 - line.core)
    fetches = [
        pltpu.make_async_copy(src, dst, r.loads.at[k])
        for k, (src, dst) in enumerate(
            ((r.grad_gu_hbm, r.grad_gu), (r.gu_map_hbm, r.gu_map), (r.qkv_map_hbm, r.qkv_map))
        )
    ]
    for fetch in fetches:
        fetch.start()
    pl.semaphore_wait(barrier, size - 1 + known)
    down_sum.trade()
    gu_sum.trade()
    for m in range(n):
        down_sum.begin(m)
    scatter = Scatter(
        group, r.part, r.first, r.over, r.joined, r.last, r.s_send, r.s_recv
    )
    gather = Gather(group, r.all, r.g_send, r.g_recv)
    fetches[0].wait()
    fetches[1].wait()

    def step_two(step, is_step):
        partial = dot_trans(r.grad_gu[group.to_own(step)], r.gu_map[...])
        is_step(size - 1)(lambda: r.own.__setitem__(..., partial))
        pl.when(step < size - 1)(lambda: r.part.__setitem__(step, partial.astype(BF)))
        for k in range(size - 1):
            is_step(k)(functools.partial(scatter.made, k))

    each_step(size, step_two)
    scatter.join()
    gu_sum.begin(0)
    down_sum.advance(1)
    half = rows // 2
    norm_sum = jnp.zeros((1, r.middle.shape[1]), F32)
    for h in range(2):
        span = slice(h * half, (h + 1) * half)
        grad = r.own[span, :] + scatter.total(h)
        middle = r.middle[span, :]
        scale = lax.rsqrt(jnp.mean(middle * middle, axis=1, keepdims=True) + EPS)
        unit = middle * scale
        scaled = grad * r.gain[...]
        norm_sum = norm_sum + jnp.sum(grad * unit, axis=0, keepdims=True)
        grad_out = r.grad[span, :].astype(F32)
        grad_middle = grad_out + scale * (
            scaled - unit * jnp.mean(scaled * unit, axis=1, keepdims=True)
        )
        r.grad_middle[span, :] = grad_middle
        r.all[group.me, span] = grad_middle.astype(BF)
        gather.start_half(h)
    r.norm[...] = norm_sum
    own_down = pltpu.make_async_copy(r.down_acc.at[z], r.down_every.at[rank], r.down_load.at[0])

    def halo(step):
        g = group.from_own(step)
        sems = r.h_send.at[step], r.h_recv.at[step]
        return remote(r.dedge.at[g], r.back.at[g], *sems, seq=rank - 1)

    def step_heads(step, is_step):
        g = group.from_own(step)

        @is_step(1)
        def _():
            gather.relay()
            for t in range(2, n - 1):
                down_sum.advance(t)

        @is_step(2)
        def _():
            down_sum.total()
            own_down.start()
            own_down.wait()
            line.gather(lambda owner: r.down_every.at[owner])
            for m in range(1, n):
                gu_sum.begin(m)

        for k in range(1, size):
            is_step(k)(functools.partial(gather.ready, k))
        grad = dot_trans(r.all[g], r.out_map[...]).astype(BF)
        dq, dk, dv = heads_back(
            g, slot, count, r.lens, r.starts, r.qkv[g], r.edge[g], grad
        )
        r.dedge[g] = jnp.concatenate([dk[:WINDOW], dv[:WINDOW]], 1).astype(BF)
        full = jnp.concatenate([dq, dk[WINDOW:], dv[WINDOW:]], 1)
        r.dqkv[g] = full.astype(BF)
        r.tail[g] = full[rows - WINDOW :]
        pl.when(rank > 0)(lambda: halo(step).start())

    each_step(size, step_heads)
    gu_sum.advance(1)
    scatter.finish()
    fetches[2].wait()

    @pl.when(rank == parts - 1)
    def _():
        r.back[...] = jnp.zeros_like(r.back)

    @pl.when(rank < parts - 1)
    def _():
        for step in range(size):
            halo(step).wait_recv()

    scatter = Scatter(
        group, r.part, r.first, r.over, r.joined, r.last, r.t_send, r.t_recv
    )

    def step_one(step, is_step):
        g = group.to_own(step)
        back = r.back[g].astype(F32)
        wide = jnp.concatenate([jnp.zeros((WINDOW, local), F32), back], 1)
        r.dqkv[g, pl.ds(rows - WINDOW, WINDOW)] = (r.tail[g] + wide).astype(BF)
        partial = dot_trans(r.dqkv[g], r.qkv_map[...])
        is_step(size - 1)(lambda: r.own.__setitem__(..., partial))
        pl.when(step < size - 1)(lambda: r.part.__setitem__(step, partial.astype(BF)))
        for k in range(size - 1):
            is_step(k)(functools.partial(scatter.made, k))

    each_step(size, step_one)
    line.relay(1)
    scatter.join()
    for t in range(2, n - 1):
        gu_sum.advance(t)
        line.relay(t)
    line.relay(n - 1)
    for h in range(2):
        span = slice(h * half, (h + 1) * half)
        r.own[span, :] = r.own[span, :] + scatter.total(h)
    gu_sum.total()

    def swap(step):
        peer = lax.rem(group.me + step, size)
        sems = r.m_send.at[step - 1], r.m_recv.at[step - 1]
        return remote(r.gu_acc.at[z, peer], r.gu_slots.at[group.me], *sems, fsdp=peer)

    for step in range(1, size):
        swap(step).start()
    own_slot = pltpu.make_async_copy(
        r.gu_acc.at[z, group.me], r.gu_slots.at[group.me], r.gu_load.at[0]
    )
    own_slot.start()
    for j in range(1, n):
        line.close(j)
    line.gathered()
    for step in range(1, size):
        swap(step).wait()
    scatter.finish()
    gather.finish()
    down_sum.finish()
    gu_sum.finish()
    line.finish()
    own_slot.wait()

    @pl.when(rank > 0)
    def _():
        for step in range(size):
            halo(step).wait_send()


def back_part(
    ident, lens, starts, grad_gu, gu_map, middle, grad, gain, out_weight, edge, qkv, qkv_map, gu_x, down_x
):
    size, parts = lax.axis_size("fsdp"), lax.axis_size("seq")
    rows, width = middle.shape
    local = out_weight.shape[0]
    n = parts // 2
    vmem = pl.BlockSpec(memory_space=pltpu.VMEM)
    smem = pl.BlockSpec(memory_space=pltpu.SMEM)
    hbm = pl.BlockSpec(memory_space=pl.ANY)
    dma = lambda *s: pltpu.SemaphoreType.DMA(s)
    low = lambda *s: jax.ShapeDtypeStruct(s, BF)
    sems = [dma(transfers(size))] * 2
    gu, down = gu_x.shape[1:], down_x.shape[1:]
    outs = pl.pallas_call(
        functools.partial(back_kernel, size, parts, lens.shape[1]),
        out_shape=[
            jax.ShapeDtypeStruct((rows, width), F32),
            jax.ShapeDtypeStruct((1, width), F32),
            low(size, rows, width),
            low(*qkv.shape),
            jax.ShapeDtypeStruct((rows, width), F32),
            low(*gu),
            low(parts, *down),
        ]
        + [low(n, *gu)] * 3
        + [low(n, *down)] * 3,
        in_specs=[smem, smem, hbm, hbm] + [vmem] * 6 + [hbm] * 3,
        out_specs=[vmem] * 5 + [hbm] * 8,
        scratch_shapes=scatter_shapes(size, rows, width)
        + sems
        + sems
        + [
            pltpu.VMEM(grad_gu.shape, BF),
            pltpu.VMEM(gu_map.shape, BF),
            pltpu.VMEM(qkv_map.shape, BF),
            pltpu.VMEM((size, WINDOW, 2 * local), BF),
            pltpu.VMEM((size, WINDOW, 2 * local), BF),
            pltpu.VMEM((size, WINDOW, 3 * local), F32),
            dma(size),
            dma(size),
            dma(3),
            pltpu.VMEM((n,) + gu, BF),
            pltpu.VMEM((2,) + gu, BF),
            dma(2),
            pltpu.VMEM((n,) + down, BF),
            pltpu.VMEM((2,) + down, BF),
            dma(2),
            dma(size - 1),
            dma(size - 1),
        ]
        + line_sems(parts) * 3,
        compiler_params=pltpu.CompilerParams(
            collective_id=ident, has_side_effects=True, vmem_limit_bytes=67_000_000
        ),
        cost_estimate=pl.CostEstimate(
            flops=2 * size * rows * (gu_map.size + qkv_map.size + width * local),
            bytes_accessed=400_000_000,
            transcendentals=0,
        ),
        name="back_part",
    )(lens, starts, grad_gu, gu_map, middle, grad, gain, out_weight, edge, qkv, qkv_map, gu_x, down_x)
    return outs[:7]


class CloseRefs(NamedTuple):
    x: Any
    gu_slots: Any
    terms: Any
    hidden: Any
    down_map: Any
    every_hbm: Any
    gu_every_hbm: Any
    feed: Any
    terms_out: Any
    part: Any
    first: Any
    over: Any
    joined: Any
    last: Any
    pre: Any
    acc: Any
    up_in: Any
    down_in: Any
    every: Any
    slots: Any
    gu_every: Any
    terms_in: Any
    terms_all: Any
    s_send: Any
    s_recv: Any
    m_send: Any
    m_recv: Any
    t_send: Any
    t_recv: Any
    loads: Any


def close_kernel(size, parts, *refs):
    named = len(CloseRefs._fields)
    r, sems = CloseRefs(*refs[:named]), refs[named:]
    rank = lax.axis_index("seq")
    group = Group(size)
    me = group.me
    line_u, line_q = Line(parts, sems[:6]), Line(parts, sems[6:12])
    n, z = line_q.length, line_q.z
    sums = LineSum(line_q, r.x, r.pre, r.acc, r.up_in, r.down_in, sems[12:])
    rows = r.feed.shape[0]
    half = rows // 2
    barrier = pltpu.get_barrier_semaphore()
    greet_group(barrier, size)
    for step in range(1, parts):
        peer = lax.rem(rank + step, parts)
        pl.semaphore_signal(barrier, inc=1, device_id={"seq": peer}, device_id_type=MESH_ID)
    own_slots = pltpu.make_async_copy(r.gu_slots, r.gu_every.at[rank], r.loads.at[0])
    own_slots.start()
    r.terms_in[me] = r.terms[me]
    pl.semaphore_wait(barrier, size + parts - 2)
    sums.trade()
    own_slots.wait()
    line_u.gather(lambda owner: r.gu_every.at[owner])

    def swap(k, step):
        peer = lax.rem(me + step, size)
        src, dst = (
            lambda: (r.terms.at[peer], r.terms_in.at[me]),
            lambda: (r.acc.at[z, peer], r.slots.at[me]),
        )[k]()
        return remote(src, dst, r.m_send.at[k, step - 1], r.m_recv.at[k, step - 1], fsdp=peer)

    others = range(1, size)
    for step in others:
        swap(0, step).start()

    scatter = Scatter(
        group, r.part, r.first, r.over, r.joined, r.last, r.s_send, r.s_recv
    )

    def down(step, is_step):
        partial = dot(r.hidden[group.to_own(step)], r.down_map[...])
        is_step(size - 1)(lambda: r.feed.__setitem__(..., partial))
        pl.when(step < size - 1)(lambda: r.part.__setitem__(step, partial.astype(BF)))
        for k in range(size - 1):
            is_step(k)(functools.partial(scatter.made, k))

    for m in range(n):
        sums.begin(m)
    each_step(size, down)
    line_u.relay(1)

    for step in others:
        swap(0, step).wait_recv()
    small = r.terms_in[0]
    for f in others:
        small = small + r.terms_in[f]
    r.terms_all[rank] = small

    def spread(step):
        peer = lax.rem(rank + step, parts)
        view = r.terms_all.at[rank]
        return remote(view, view, r.t_send.at[step - 1], r.t_recv.at[step - 1], seq=peer)

    for step in range(1, parts):
        spread(step).start()
    scatter.join()

    for t in range(1, n - 1):
        sums.advance(t)
        line_u.relay(t + 1)
    for h in range(2):
        span = slice(h * half, (h + 1) * half)
        r.feed[span, :] = r.feed[span, :] + scatter.total(h)
    sums.total()
    for step in others:
        swap(1, step).start()
    for j in range(1, n):
        line_u.close(j)
    r.slots[me] = r.acc[z, me]
    for step in others:
        swap(1, step).wait_recv()
    local = r.x.shape[3] // 4
    lane = lax.broadcasted_iota(jnp.int32, (1, 1, 4 * local), 2)
    r.every[rank] = jnp.where(lane < 3 * local, r.slots[...], r.acc[z])
    line_q.gather(lambda owner: r.every.at[owner])
    line_u.gathered()
    stores = [pltpu.make_async_copy(r.gu_every, r.gu_every_hbm, r.loads.at[0])]
    stores[0].start()
    for j in range(1, n):
        line_q.relay(j)
    for j in range(1, n):
        line_q.close(j)
    line_q.gathered()
    stores.append(pltpu.make_async_copy(r.every, r.every_hbm, r.loads.at[1]))
    stores[1].start()
    for step in range(1, parts):
        spread(step).wait_recv()
    small = r.terms_all[0]
    for k in range(1, parts):
        small = small + r.terms_all[k]
    r.terms_out[...] = small
    for k in range(2):
        for step in others:
            swap(k, step).wait_send()
    for step in range(1, parts):
        spread(step).wait_send()
    scatter.finish()
    sums.finish()
    line_u.finish()
    line_q.finish()
    for store in stores:
        store.wait()


def close_part(ident, packed, gu_slots, terms, hidden, down_weight):
    parts, size, piece, cols = packed.shape
    n = parts // 2
    rows, width = hidden.shape[1], down_weight.shape[1]
    vmem = pl.BlockSpec(memory_space=pltpu.VMEM)
    hbm = pl.BlockSpec(memory_space=pl.ANY)
    dma = lambda *s: pltpu.SemaphoreType.DMA(s)
    gu_shape = (parts,) + gu_slots.shape
    scratch = scatter_shapes(size, rows, width)
    chips = pltpu.VMEM((n, size, piece, cols), BF)
    return pl.pallas_call(
        functools.partial(close_kernel, size, parts),
        out_shape=[
            jax.ShapeDtypeStruct(packed.shape, BF),
            jax.ShapeDtypeStruct(gu_shape, BF),
            jax.ShapeDtypeStruct((rows, width), F32),
            jax.ShapeDtypeStruct(terms.shape[1:], F32),
        ],
        in_specs=[vmem, hbm, vmem, vmem, vmem],
        out_specs=[hbm, hbm, vmem, vmem],
        scratch_shapes=scratch[:-2]
        + [
            chips,
            chips,
            chips,
            chips,
            pltpu.VMEM(packed.shape, BF),
            pltpu.VMEM((size, piece, cols), BF),
            pltpu.VMEM(gu_shape, BF),
            pltpu.VMEM(terms.shape, F32),
            pltpu.VMEM((parts,) + terms.shape[1:], F32),
        ]
        + scratch[-2:]
        + [dma(2, size - 1)] * 2
        + [dma(parts - 1)] * 2
        + [dma(2)]
        + line_sems(parts) * 3,
        compiler_params=pltpu.CompilerParams(
            collective_id=ident, has_side_effects=True, vmem_limit_bytes=67_000_000
        ),
        cost_estimate=pl.CostEstimate(
            flops=2 * size * rows * down_weight.size, bytes_accessed=500_000_000, transcendentals=0
        ),
        name="close_part",
    )(packed, gu_slots, terms, hidden, down_weight)


def pack_kernel(size, parts, x_ref, g_ref, *refs):
    out_ref = refs[-1]
    full = dot_rows(x_ref[...], g_ref[...])
    pair = out_ref.shape[1]
    rows = full.shape[0] // pair
    piece = rows // parts
    for k in range(pair):
        own = full[k * rows : (k + 1) * rows]
        if len(refs) == 3:
            heads_ref, gb_ref = refs[0], refs[1]
            side = dot_rows(heads_ref[...], gb_ref[...])
            wide = side.shape[1] // pair
            own = jnp.concatenate([own, side[:, k * wide : (k + 1) * wide]], 1)
        out_ref[:, k] = own.astype(BF).reshape(parts, piece, own.shape[1])


def pack_grads(parts, size, x, g, heads=None, gb=None):
    width, cols = x.shape[1], g.shape[1]
    rows = width // size
    piece = rows // parts
    if piece % 8 or (2 * rows) % 128:
        full = dot_rows(x, g).reshape(size, parts, piece, cols)
        if heads is not None:
            side = dot_rows(heads, gb).reshape(parts, piece, size, -1).transpose(2, 0, 1, 3)
            full = jnp.concatenate([full, side], 3)
        return full.transpose(1, 0, 2, 3).astype(BF)
    total = x.shape[0]
    pair = pl.BlockSpec((total, 2 * rows), lambda i: (0, i))
    whole = lambda a: pl.BlockSpec(a.shape, lambda i: (0, 0), pipeline_mode=pl.Buffered(1))
    args, specs = [x, g], [pair, whole(g)]
    out_cols = cols
    if heads is not None:
        args += [heads, gb]
        specs += [whole(heads), pair]
        out_cols += rows
    return pl.pallas_call(
        functools.partial(pack_kernel, size, parts),
        grid=(size // 2,),
        out_shape=jax.ShapeDtypeStruct((parts, size, piece, out_cols), BF),
        in_specs=specs,
        out_specs=pl.BlockSpec((parts, 2, piece, out_cols), lambda i: (0, i, 0, 0)),
        cost_estimate=pl.CostEstimate(
            flops=2 * total * width * out_cols,
            bytes_accessed=2 * (x.size + g.size + width * out_cols),
            transcendentals=0,
        ),
        name="pack_grads",
    )(*args)


def unpack_kernel(widths, every_ref, *outs):
    size = every_ref.shape[1]
    blocks = [every_ref[0, i].astype(F32) for i in range(size)]
    low = 0
    for width, out in zip(widths, outs):
        out[...] = jnp.concatenate([b[:, low : low + width] for b in blocks], 1)
        low += width


def unpack_grads(every, widths):
    parts, size, piece, cols = every.shape
    if piece % 8:
        outs, low = [], 0
        for width in widths:
            block = every[:, :, :, low : low + width].transpose(0, 2, 1, 3)
            outs.append(block.reshape(parts * piece, size * width).astype(F32))
            low += width
        return outs
    return pl.pallas_call(
        functools.partial(unpack_kernel, widths),
        grid=(parts,),
        out_shape=[jax.ShapeDtypeStruct((parts * piece, size * w), F32) for w in widths],
        in_specs=[pl.BlockSpec((1, size, piece, cols), lambda i: (i, 0, 0, 0))],
        out_specs=[pl.BlockSpec((piece, size * w), lambda i: (i, 0)) for w in widths],
        cost_estimate=pl.CostEstimate(flops=0, bytes_accessed=every.size * 6, transcendentals=0),
        name="unpack_grads",
    )(every)


def columns_piece(weights, part, parts):
    size = lax.axis_size("fsdp")
    rows = weights[0].shape[0] // parts
    pieces = []
    for weight in weights:
        own = lax.dynamic_slice_in_dim(weight, part * rows, rows, 0)
        pieces.append(own.reshape(rows, size, -1))
    return jnp.concatenate(pieces, 2).transpose(1, 0, 2)


def shards(
    tokens,
    seq_lengths,
    seq_offsets,
    norm1_gain,
    conv_weight,
    query_weight,
    key_weight,
    value_weight,
    out_weight,
    norm2_gain,
    gate_weight,
    up_weight,
    down_weight,
    cotangent,
):
    size = lax.axis_size("fsdp")
    parts = lax.axis_size("seq")
    part = lax.axis_index("seq")
    me = lax.axis_index("fsdp")
    own_tokens = tokens[0]
    rows, width = own_tokens.shape
    slice_width = norm1_gain.shape[0]
    first_slot = part * rows
    count = seq_lengths.shape[1]

    slot_ext = first_slot - 2 + jnp.arange(rows + 2, dtype=jnp.int32)
    segment_ext = segment_of(
        slot_ext, count, lambda j: seq_lengths[0, j], lambda j: seq_offsets[0, j]
    )
    segment_own = segment_ext[2:]
    same_one = (segment_own == segment_ext[1:-1]).astype(F32)[:, None]
    same_two = (segment_own == segment_ext[:-2]).astype(F32)[:, None]
    live_mask = (segment_own >= 0).astype(F32)[:, None]

    gains = jnp.concatenate(
        [
            norm1_gain[None],
            norm2_gain[None],
            conv_weight.T,
            jnp.zeros((3, slice_width), BF),
        ],
        0,
    )
    table = jnp.zeros((8, 128), jnp.int32)
    table = table.at[0, :count].set(seq_lengths[0]).at[1, :count].set(seq_offsets[0])
    qkv_piece = columns_piece((query_weight, key_weight, value_weight), part, parts)
    gu_piece = columns_piece((gate_weight, up_weight), part, parts)
    edge_tokens = shifted(own_tokens[rows - 2 :], "seq", 1)
    grad_down = (cotangent[0].astype(F32) * live_mask).astype(BF)
    (
        gated_all,
        qkv,
        edge,
        qkv_map,
        middle,
        heads_out,
        grad_down_all,
        normed_all,
        hidden,
        grad_gu,
        gu_map,
        gains_all,
        table_all,
    ) = forward_part(
        0,
        count,
        own_tokens,
        jnp.pad(edge_tokens, ((0, 6), (0, 0))),
        grad_down,
        gains,
        table,
        qkv_piece,
        gu_piece,
        out_weight,
        down_weight,
    )
    local = out_weight.shape[0]
    flat = lambda a: a.reshape(-1, a.shape[-1])
    lens_all, starts_all = table_all[:, 0, :count], table_all[:, 1, :count]
    gains_all = gains_all.transpose(1, 0, 2).reshape(8, width)
    norm_one = gains_all[0].astype(F32)
    norm_two = gains_all[1].astype(F32)
    taps = gains_all[2:5].astype(F32)
    qkv_map, gu_map = qkv_map.reshape(width, -1), gu_map.reshape(width, -1)
    grad_down_all = flat(grad_down_all)

    extended = jnp.concatenate([edge_tokens, own_tokens], 0).astype(F32)
    scale_one = lax.rsqrt(jnp.mean(extended * extended, axis=1, keepdims=True) + EPS)
    normed = extended * scale_one * norm_one
    conv_mix = (
        normed[2:] * taps[0]
        + same_one * normed[1:-1] * taps[1]
        + same_two * normed[:-2] * taps[2]
    )

    gu_packed = pack_grads(parts, size, flat(normed_all), flat(grad_gu))
    down_packed = dot_rows(flat(hidden), grad_down_all).astype(BF)
    grad_middle, norm2_term, grad_branch_all, dqkv, grad_gated, gu_slots, down_every = back_part(
        4,
        lens_all,
        starts_all,
        grad_gu,
        gu_map,
        middle,
        grad_down,
        norm_two[None],
        out_weight,
        edge,
        qkv,
        qkv_map,
        gu_packed,
        down_packed.reshape(parts, -1, width),
    )
    norm2_term = norm2_term[0]
    down_total = down_every.reshape(-1, width).astype(F32)
    qkvo_packed = pack_grads(
        parts, size, flat(gated_all), flat(dqkv), flat(heads_out), flat(grad_branch_all)
    )

    normed_own = normed[2:]
    grad_mix = grad_gated * normed_own
    part_zero = jnp.pad(grad_gated * conv_mix + grad_mix * taps[0], ((2, 0), (0, 0)))
    part_one = jnp.pad(grad_mix * same_one * taps[1], ((1, 1), (0, 0)))
    part_two = jnp.pad(grad_mix * same_two * taps[2], ((0, 2), (0, 0)))
    grad_normed = part_zero + part_one + part_two
    unit_one = extended * scale_one
    grad_unit_one = grad_normed * norm_one
    grad_extended = scale_one * (
        grad_unit_one - unit_one * jnp.mean(grad_unit_one * unit_one, axis=1, keepdims=True)
    )
    edge_back = shifted(grad_extended[:2], "seq", -1)
    tokens_grad = grad_middle + grad_extended[2:] + jnp.pad(edge_back, ((rows - 2, 0), (0, 0)))

    terms = jnp.stack(
        [
            jnp.sum(grad_normed * unit_one, axis=0),
            norm2_term,
            jnp.sum(grad_mix * normed_own, axis=0),
            jnp.sum(grad_mix * same_one * normed[1:-1], axis=0),
            jnp.sum(grad_mix * same_two * normed[:-2], axis=0),
        ]
    )
    terms = jnp.pad(terms, ((0, 3), (0, 0))).reshape(8, size, slice_width).transpose(1, 0, 2)
    qkvo_packed, gu_slots, terms, down_total, tokens_grad = lax.optimization_barrier(
        (qkvo_packed, gu_slots, terms, down_total, tokens_grad)
    )
    qkvo_every, gu_every, feed, terms = close_part(
        5, qkvo_packed, gu_slots, terms, hidden, down_weight
    )
    gate_total, up_total = unpack_grads(gu_every, (gu_map.shape[1] // 2,) * 2)
    query_total, key_total, value_total, out_total = unpack_grads(qkvo_every, (local,) * 4)

    layer_out = (live_mask * (middle + feed)).astype(BF)[None]
    return (
        layer_out,
        tokens_grad[None],
        terms[0],
        terms[2:5].T,
        query_total,
        key_total,
        value_total,
        out_total,
        terms[1],
        gate_total,
        up_total,
        down_total,
    )


def solution(mesh):
    placed = (
        P("fsdp", "seq", None),
        P("fsdp", None),
        P("fsdp", None),
        P("fsdp"),
        P("fsdp", None),
        P("fsdp", None),
        P("fsdp", None),
        P("fsdp", None),
        P("fsdp", None),
        P("fsdp"),
        P("fsdp", None),
        P("fsdp", None),
        P("fsdp", None),
        P("fsdp", "seq", None),
    )
    return jax.shard_map(
        shards,
        mesh=mesh,
        in_specs=placed,
        out_specs=(
            P("fsdp", "seq", None),
            P("fsdp", "seq", None),
            P("fsdp"),
            P("fsdp", None),
            P("fsdp", None),
            P("fsdp", None),
            P("fsdp", None),
            P("fsdp", None),
            P("fsdp"),
            P("fsdp", None),
            P("fsdp", None),
            P("fsdp", None),
        ),
        check_vma=False,
    )
```

```python
import functools
from typing import Any, NamedTuple

import jax
import jax.numpy as jnp
from jax import lax
from jax.experimental import pallas as pl
from jax.experimental.pallas import tpu as pltpu
from jax.sharding import PartitionSpec as P

HEADS = 16
WINDOW = 64
HEAD_DIM = 112
BLOCK = 128

EPS = 1e-05
NEG = -1e30
SCALE = HEAD_DIM ** (-0.5)
MESH_ID = pl.DeviceIdType.MESH
BF = jnp.bfloat16
F32 = jnp.float32


def shifted(array, axis, by):
    length = lax.axis_size(axis)
    pairs = [(i, i + by) for i in range(length) if 0 <= i + by < length]
    return lax.ppermute(array, axis, pairs)


def segment_of(slot, count, lengths, starts):
    found = jnp.full(slot.shape, -1, jnp.int32)
    for j in range(count):
        inside = (slot >= starts(j)) & (slot < starts(j) + lengths(j))
        found = jnp.where(inside, j, found)
    return jnp.where(slot < 0, -2, found)


def dot_rows(left, right):
    return lax.dot_general(left, right, (((0,), (0,)), ((), ())), preferred_element_type=F32)


def dot_trans(left, right):
    return lax.dot_general(left, right, (((1,), (1,)), ((), ())), preferred_element_type=F32)


def dot(left, right):
    return jnp.dot(left, right, preferred_element_type=F32)


def masks_of(first, block, count, length, start):
    rows = first + block * BLOCK
    query = rows + lax.broadcasted_iota(jnp.int32, (BLOCK, 1), 0)
    keys = rows - WINDOW + lax.broadcasted_iota(jnp.int32, (1, BLOCK + WINDOW), 1)
    seg_q = segment_of(query, count, length, start)
    seg_k = segment_of(keys, count, length, start)
    far = query - keys
    return (far >= 0) & (far <= WINDOW) & (seg_q == seg_k)


def soft_of(query, keys, mask):
    scores = dot_trans(query, keys) * SCALE
    scores = jnp.where(mask, scores, NEG)
    peak = jnp.max(scores, axis=1, keepdims=True)
    exponent = jnp.exp(scores - peak)
    return exponent / jnp.sum(exponent, axis=1, keepdims=True)


def lane_head(width):
    return lax.broadcasted_iota(jnp.int32, (1, width), 1) // HEAD_DIM


def remote(src, dst, send, recv, **peer):
    return pltpu.make_async_remote_copy(
        src_ref=src,
        dst_ref=dst,
        send_sem=send,
        recv_sem=recv,
        device_id=peer,
        device_id_type=MESH_ID,
    )


def greet_group(barrier, size):
    me = lax.axis_index("fsdp")
    for step in range(1, size):
        peer = lax.rem(me + step, size)
        pl.semaphore_signal(barrier, inc=1, device_id={"fsdp": peer}, device_id_type=MESH_ID)


class Group:
    def __init__(self, size):
        self.size = size
        self.me = lax.axis_index("fsdp")
        self.square = size == 4
        if self.square:
            x, y = lax.rem(self.me, 2), self.me // 2
            self.at = lambda bx, by: lax.rem(y + by, 2) * 2 + lax.rem(x + bx, 2)
            self.x, self.y, self.far = self.at(1, 0), self.at(0, 1), self.at(1, 1)

    def from_own(self, step):
        if self.square:
            return self.at(lax.rem(step, 2), step // 2)
        return lax.rem(self.me - step + self.size, self.size)

    def to_own(self, step):
        if self.square:
            return self.at(1 - step // 2, 1 - lax.rem(step, 2))
        return lax.rem(self.me + 1 + step, self.size)


class Gather:
    def __init__(self, group, ref, send, recv):
        self.group, self.ref, self.send, self.recv = group, ref, send, recv
        self.half = ref.shape[1] // 2

    def part(self, k, slot, half, peer):
        view = self.ref.at[slot, pl.ds(half * self.half, self.half)]
        return remote(view, view, self.send.at[k], self.recv.at[k], fsdp=peer)

    def whole(self, k):
        g = self.group
        view = self.ref.at[g.me]
        sems = self.send.at[k - 1], self.recv.at[k - 1]
        return remote(view, view, *sems, fsdp=lax.rem(g.me + k, g.size))

    def copy(self, k):
        g = self.group
        if not g.square:
            return self.whole(k + 1)
        slot = (g.me, g.me, g.me, g.me, g.x, g.y)[k]
        half = (0, 1, 0, 1, 0, 1)[k]
        return self.part(k, slot, half, (g.x, g.x, g.y, g.y, g.y, g.x)[k])

    def start_half(self, half):
        if self.group.square:
            self.copy(half).start()
            self.copy(2 + half).start()
        elif half == 1:
            for k in range(self.group.size - 1):
                self.copy(k).start()

    def relay(self):
        if self.group.square:
            self.copy(0).wait_recv()
            self.copy(4).start()
            self.copy(3).wait_recv()
            self.copy(5).start()

    def ready(self, step):
        if not self.group.square:
            self.copy(step - 1).wait_recv()
        elif step == 3:
            self.copy(4).wait_recv()
            self.copy(5).wait_recv()
        else:
            self.copy(step).wait_recv()

    def finish(self):
        for k in range(transfers(self.group.size)):
            self.copy(k).wait_send()


class Scatter:
    def __init__(self, group, part, first, over, joined, last, send, recv):
        self.group, self.part = group, part
        self.first, self.over, self.joined, self.last = first, over, joined, last
        self.send, self.recv = send, recv
        self.half = part.shape[1] // 2

    def copy(self, k):
        g, half = self.group, self.half
        low, high = pl.ds(0, half), pl.ds(half, half)
        if not g.square:
            src, dst, peer = self.part.at[k], self.first.at[k], lax.rem(g.me + 1 + k, g.size)
        else:
            src, dst, peer = (
                lambda: (self.part.at[0, low], self.over.at[0], g.x),
                lambda: (self.part.at[0, high], self.over.at[1], g.y),
                lambda: (self.part.at[1, low], self.first.at[0], g.x),
                lambda: (self.part.at[2, high], self.first.at[1], g.y),
                lambda: (self.joined.at[0], self.last.at[0], g.y),
                lambda: (self.joined.at[1], self.last.at[1], g.x),
            )[k]()
        return remote(src, dst, self.send.at[k], self.recv.at[k], fsdp=peer)

    def made(self, step):
        if not self.group.square:
            self.copy(step).start()
        elif step == 0:
            self.copy(0).start()
            self.copy(1).start()
        elif step in (1, 2):
            self.copy(step + 1).start()

    def join(self):
        if not self.group.square:
            return
        half = self.half
        for k, (step, rows) in enumerate(((2, slice(0, half)), (1, slice(half, 2 * half)))):
            self.copy(k).wait_recv()
            own = self.part[step, rows].astype(F32)
            self.joined[k] = (own + self.over[k].astype(F32)).astype(BF)
            self.copy(4 + k).start()

    def total(self, half):
        count = self.half
        if self.group.square:
            self.copy(2 + half).wait_recv()
            self.copy(4 + half).wait_recv()
            return self.first[half].astype(F32) + self.last[half].astype(F32)
        if half == 0:
            for k in range(self.group.size - 1):
                self.copy(k).wait_recv()
        rows = slice(half * count, (half + 1) * count)
        out = self.first[0, rows].astype(F32)
        for k in range(1, self.group.size - 1):
            out = out + self.first[k, rows].astype(F32)
        return out

    def finish(self):
        for k in range(transfers(self.group.size)):
            self.copy(k).wait_send()


class Line:
    def __init__(self, parts, sems):
        self.rank = lax.axis_index("seq")
        self.parts, self.length = parts, parts // 2
        self.z, self.core = self.rank // 2, lax.rem(self.rank, 2)
        self.above, self.below = self.rank + 2, self.rank - 2
        self.beside = self.rank + 1 - 2 * self.core
        self.has_above, self.has_below = self.z < self.length - 1, self.z > 0
        self.sems = sems

    def greet(self, barrier):
        def one(peer):
            pl.semaphore_signal(barrier, inc=1, device_id={"seq": peer}, device_id_type=MESH_ID)

        one(self.beside)
        pl.when(self.has_above)(lambda: one(self.above))
        pl.when(self.has_below)(lambda: one(self.below))
        n, z = self.length, self.z
        return 1 + (2 * n - 2 - z) // n + (z + n - 1) // n

    def up(self, k, owner):
        view = self.view(owner)
        return remote(view, view, self.sems[0].at[k], self.sems[1].at[k], seq=self.above)

    def down(self, k, owner):
        view = self.view(owner)
        return remote(view, view, self.sems[2].at[k], self.sems[3].at[k], seq=self.below)

    def side(self, k, owner):
        view = self.view(owner)
        return remote(view, view, self.sems[4].at[k], self.sems[5].at[k], seq=self.beside)

    def gather(self, view):
        self.view = view
        pl.when(self.has_above)(lambda: self.up(0, self.rank).start())
        pl.when(self.has_below)(lambda: self.down(0, self.rank).start())
        self.side(self.z, self.rank).start()

    def own_up(self):
        pl.when(self.has_above)(lambda: self.up(0, self.rank).start())

    def own_down(self):
        pl.when(self.has_below)(lambda: self.down(0, self.rank).start())

    def relay_up(self, j):
        rank, z = self.rank, self.z

        @pl.when((z >= j) & self.has_above)
        def _():
            self.up(j - 1, rank).wait_recv()
            self.up(j, rank - 2 * j).start()
            self.side(z - j, rank - 2 * j).start()

    def relay_down(self, j):
        rank, z = self.rank, self.z

        @pl.when((z + j < self.length) & self.has_below)
        def _():
            self.down(j - 1, rank).wait_recv()
            self.down(j, rank + 2 * j).start()
            self.side(z + j, rank + 2 * j).start()

    def relay(self, j):
        self.relay_up(j)
        self.relay_down(j)

    def close(self, j):
        rank, z = self.rank, self.z

        @pl.when((z >= j) & (z == self.length - 1))
        def _():
            self.up(j - 1, rank).wait_recv()
            self.side(z - j, rank - 2 * j).start()

        @pl.when((z + j < self.length) & (z == 0))
        def _():
            self.down(j - 1, rank).wait_recv()
            self.side(z + j, rank + 2 * j).start()

    def gathered(self):
        for k in range(self.length):
            self.side(k, self.rank).wait_recv()

    def finish(self):
        rank, z = self.rank, self.z
        for k in range(self.length):
            self.side(k, rank).wait_send()
        pl.when(self.has_above)(lambda: self.up(0, rank).wait_send())
        pl.when(self.has_below)(lambda: self.down(0, rank).wait_send())
        for j in range(1, self.length):
            pl.when((z >= j) & self.has_above)(lambda: self.up(j, rank).wait_send())
            pl.when((z + j < self.length) & self.has_below)(lambda: self.down(j, rank).wait_send())


class LineSum:
    def __init__(self, line, x, pre, acc, up_in, down_in, sems):
        self.line, self.x, self.pre, self.acc = line, x, pre, acc
        self.up_in, self.down_in, self.sems = up_in, down_in, sems

    def share(self, k):
        line = self.line
        src = self.x.at[2 * k + 1 - line.core]
        return remote(src, self.pre.at[k], self.sems[0].at[k], self.sems[1].at[k], seq=line.beside)

    def up(self, k):
        sems = self.sems[2].at[k], self.sems[3].at[k]
        return remote(self.acc.at[k], self.up_in.at[k], *sems, seq=self.line.above)

    def down(self, k):
        sems = self.sems[4].at[k], self.sems[5].at[k]
        return remote(self.acc.at[k], self.down_in.at[k], *sems, seq=self.line.below)

    def pair(self, m):
        return self.line.length - 1 - m, m

    def trade(self):
        n = self.line.length
        for m in range((n + 1) // 2):
            for k in sorted(set(self.pair(m))):
                self.share(k).start()

    def merge(self, k):
        self.share(k).wait_recv()
        own = self.x[2 * k + self.line.core].astype(F32)
        self.acc[k] = (own + self.pre[k].astype(F32)).astype(BF)

    def begin(self, m):
        n, z = self.line.length, self.line.z
        far, near = self.pair(m)
        if m < (n + 1) // 2:
            for k in sorted({far, near}):
                self.merge(k)
        if m < n - 1:
            pl.when(z == 0)(lambda: self.up(far).start())
            pl.when(z == n - 1)(lambda: self.down(near).start())

    def add(self, k, more):
        self.acc[k] = (self.acc[k].astype(F32) + more[k].astype(F32)).astype(BF)

    def advance(self, t):
        z, n = self.line.z, self.line.length
        far, near = n - 1 + z - t, t - n + 1 + z

        @pl.when((z >= 1) & (z <= t))
        def _():
            self.up(far).wait_recv()
            self.add(far, self.up_in)
            self.up(far).start()

        @pl.when((z <= n - 2) & (z >= n - 1 - t))
        def _():
            self.down(near).wait_recv()
            self.add(near, self.down_in)
            self.down(near).start()

    def total(self):
        z = self.line.z

        @pl.when(z > 0)
        def _():
            self.up(z).wait_recv()
            self.add(z, self.up_in)

        @pl.when(z < self.line.length - 1)
        def _():
            self.down(z).wait_recv()
            self.add(z, self.down_in)

    def finish(self):
        for k in range(self.line.length):
            self.share(k).wait_send()
            pl.when(k > self.line.z)(lambda: self.up(k).wait_send())
            pl.when(k < self.line.z)(lambda: self.down(k).wait_send())


class StagedSum(LineSum):
    def __init__(self, stage, load, *args):
        super().__init__(*args)
        self.stage, self.load = stage, load

    def fetch(self, slot, src):
        return pltpu.make_async_copy(src, self.stage.at[slot], self.load.at[slot])

    def merge(self, k):
        self.share(k).wait_recv()
        own = self.fetch(0, self.x.at[2 * k + self.line.core])
        other = self.fetch(1, self.pre.at[k])
        own.start()
        other.start()
        own.wait()
        other.wait()
        self.acc[k] = (self.stage[0].astype(F32) + self.stage[1].astype(F32)).astype(BF)

    def add(self, k, more):
        came = self.fetch(0, more.at[k])
        came.start()
        came.wait()
        self.acc[k] = (self.acc[k].astype(F32) + self.stage[0].astype(F32)).astype(BF)


class MixedSum(StagedSum):
    def merge(self, k):
        self.share(k).wait_recv()
        other = self.fetch(1, self.pre.at[k])
        other.start()
        other.wait()
        own = self.x[2 * k + self.line.core].astype(F32)
        self.acc[k] = (own + self.stage[1].astype(F32)).astype(BF)


def line_sems(parts):
    return [pltpu.SemaphoreType.DMA((parts // 2,))] * 6


def transfers(size):
    return 6 if size == 4 else size - 1


def scatter_shapes(size, rows, width):
    half = rows // 2
    slots = (2, half, width) if size == 4 else (size - 1, rows, width)
    return [
        pltpu.VMEM((size - 1, rows, width), BF),
        pltpu.VMEM(slots, BF),
        pltpu.VMEM((2, half, width), BF),
        pltpu.VMEM((2, half, width), BF),
        pltpu.VMEM((2, half, width), BF),
        pltpu.SemaphoreType.DMA((transfers(size),)),
        pltpu.SemaphoreType.DMA((transfers(size),)),
    ]


def each_step(size, body):
    def one(step, carry):
        body(step, lambda k: pl.when(step == k))
        return carry

    lax.fori_loop(0, size, one, 0)


class ForwardRefs(NamedTuple):
    tokens: Any
    edge_tok: Any
    grad: Any
    gains: Any
    table: Any
    qkv_piece: Any
    gu_piece: Any
    out_map: Any
    down_map: Any
    gated_hbm: Any
    qkv_hbm: Any
    edge: Any
    qkv_map_hbm: Any
    middle: Any
    heads: Any
    grads_hbm: Any
    norm_hbm: Any
    hidden_hbm: Any
    gu_grad_hbm: Any
    gu_map_hbm: Any
    gains_all: Any
    table_all: Any
    part: Any
    first: Any
    over: Any
    joined: Any
    last: Any
    all: Any
    grads: Any
    qkv: Any
    qkv_map: Any
    gu_map: Any
    tail: Any
    own: Any
    hidden: Any
    gu_grad: Any
    s_send: Any
    s_recv: Any
    a_send: Any
    a_recv: Any
    g_send: Any
    g_recv: Any
    c_send: Any
    c_recv: Any
    m_send: Any
    m_recv: Any
    halo_send: Any
    halo_recv: Any
    loads: Any
    stores: Any
    hidden_store: Any
    gu_store: Any


def forward_kernel(size, parts, count, *refs):
    named = len(ForwardRefs._fields)
    r, sems = ForwardRefs(*refs[:named]), refs[named:]
    rank = lax.axis_index("seq")
    rows = r.tokens.shape[0]
    half = rows // 2
    local = r.out_map.shape[0]
    inner = r.down_map.shape[0]
    slot = rank * rows
    group = Group(size)
    me = group.me
    line_q, line_u = Line(parts, sems[:6]), Line(parts, sems[6:])

    barrier = pltpu.get_barrier_semaphore()
    greet_group(barrier, size)
    known = line_q.greet(barrier)

    def greet(peer):
        pl.semaphore_signal(barrier, inc=1, device_id={"seq": peer}, device_id_type=MESH_ID)

    pl.when(line_q.has_above & (line_q.core == 1))(lambda: greet(rank + 1))
    pl.when(line_q.has_below & (line_q.core == 0))(lambda: greet(rank - 1))
    n, z = line_q.length, line_q.z
    known = known + (2 * n - 2 - z) // n * line_q.core + (z + n - 1) // n * (1 - line_q.core)
    own_pieces = [
        pltpu.make_async_copy(src.at[me], dst.at[me, rank], r.loads.at[k])
        for k, (src, dst) in enumerate(
            ((r.qkv_piece, r.qkv_map), (r.gu_piece, r.gu_map))
        )
    ]
    for copy in own_pieces:
        copy.start()
    r.gains_all[me] = r.gains[...]
    r.table_all[me] = r.table[...]
    r.grads[me] = r.grad[...]
    pl.semaphore_wait(barrier, size - 1 + known)

    def swap(k, step):
        peer = lax.rem(me + step, size)
        src, dst = (
            lambda: (r.gains_all.at[me], r.gains_all.at[me]),
            lambda: (r.table_all.at[me], r.table_all.at[me]),
            lambda: (r.qkv_piece.at[peer], r.qkv_map.at[me, rank]),
            lambda: (r.gu_piece.at[peer], r.gu_map.at[me, rank]),
        )[k]()
        return remote(src, dst, r.m_send.at[k, step - 1], r.m_recv.at[k, step - 1], fsdp=peer)

    others = range(1, size)
    for k in range(4):
        for step in others:
            swap(k, step).start()
    for k in range(2):
        for step in others:
            swap(k, step).wait_recv()

    gains = jnp.concatenate([r.gains_all[f] for f in range(size)], 1).astype(F32)
    own_table = r.table_all[me]
    slots = slot + lax.broadcasted_iota(jnp.int32, (rows, 1), 0)
    length = lambda j: own_table[0:1, j : j + 1]
    start = lambda j: own_table[1:2, j : j + 1]
    segment = segment_of(slots, count, length, start)
    same_one = (segment == segment_of(slots - 1, count, length, start)).astype(F32)
    same_two = (segment == segment_of(slots - 2, count, length, start)).astype(F32)
    tokens = r.tokens[...].astype(F32)
    edge = r.edge_tok[...].astype(F32)

    def norm(a):
        return a * lax.rsqrt(jnp.mean(a * a, axis=1, keepdims=True) + EPS) * gains[0:1]

    normed, edge = norm(tokens), norm(edge)
    row = lax.broadcasted_iota(jnp.int32, (rows, 1), 0)
    back_one = jnp.where(row == 0, edge[1:2], pltpu.roll(normed, 1, 0))
    back_two = jnp.where(
        row == 0, edge[0:1], jnp.where(row == 1, edge[1:2], pltpu.roll(normed, 2, 0))
    )
    mixed = (
        normed * gains[2:3]
        + same_one * back_one * gains[3:4]
        + same_two * back_two * gains[4:5]
    )
    all_ref = r.all
    all_ref[me] = (mixed * normed).astype(BF)
    gather = Gather(group, all_ref, r.a_send, r.a_recv)
    gather.start_half(0)
    gather.start_half(1)

    own_pieces[0].wait()
    for step in others:
        swap(2, step).wait_recv()
    line_q.gather(lambda owner: r.qkv_map.at[:, owner])
    line_u.view = lambda owner: r.gu_map.at[:, owner]
    gather.relay()
    grads = Gather(group, r.grads, r.c_send, r.c_recv)
    grads.start_half(0)
    grads.start_half(1)
    own_pieces[1].wait()
    for step in others:
        swap(3, step).wait_recv()
    line_u.side(z, rank).start()
    pl.when(z == 0)(line_u.own_up)
    pl.when(z == n - 1)(line_u.own_down)
    for j in range(1, n):
        line_q.relay(j)
        line_q.close(j)
        pl.when(z == j)(line_u.own_up)
        pl.when(z == n - 1 - j)(line_u.own_down)
    for step in others:
        gather.ready(step)
    grads.relay()
    line_q.gathered()
    keeps = [
        pltpu.make_async_copy(all_ref, r.gated_hbm, r.stores.at[size]),
        pltpu.make_async_copy(r.qkv_map, r.qkv_map_hbm, r.stores.at[size + 1]),
    ]
    for keep in keeps:
        keep.start()

    weights = r.qkv_map[...].reshape(-1, r.qkv_map.shape[3])

    def halo(step):
        g = group.to_own(step)
        sem = r.halo_send.at[step], r.halo_recv.at[step]
        return remote(r.tail.at[g], r.edge.at[g], *sem, seq=rank + 1)

    def project(step, is_step):
        g = group.to_own(step)
        out = dot(all_ref[g], weights).astype(BF)
        r.qkv[g] = out
        r.tail[g] = out[rows - WINDOW :, local:]
        pl.when(rank < parts - 1)(lambda: halo(step).start())

    each_step(size, project)

    @pl.when(rank == 0)
    def _():
        r.edge[...] = jnp.zeros_like(r.edge)

    keeps.append(pltpu.make_async_copy(r.qkv, r.qkv_hbm, r.stores.at[size + 2]))
    keeps[2].start()
    line_u.relay(1)
    gather.finish()
    keeps[0].wait()

    scatter = Scatter(
        group, r.part, r.first, r.over, r.joined, r.last, r.s_send, r.s_recv
    )
    head_of = lane_head(local)

    def mix(step, is_step):
        g = group.to_own(step)
        pl.when(rank > 0)(lambda: halo(step).wait_recv())
        own, edge, table = r.qkv[g], r.edge[g], r.table_all[g]
        queries = own[:, :local]
        keys = jnp.concatenate([edge[:, :local], own[:, local : 2 * local]], 0)
        values = jnp.concatenate([edge[:, local:], own[:, 2 * local :]], 0)
        outs = []
        for block in range(rows // BLOCK):
            mask = masks_of(
                slot,
                block,
                count,
                lambda j: table[0:1, j : j + 1],
                lambda j: table[1:2, j : j + 1],
            )
            low = block * BLOCK
            query = queries[low : low + BLOCK]
            key = keys[low : low + BLOCK + WINDOW]
            value = values[low : low + BLOCK + WINDOW]
            out = jnp.zeros((BLOCK, local), F32)
            for head in range(local // HEAD_DIM):
                mine = head_of == head
                soft = soft_of(jnp.where(mine, query, jnp.zeros_like(query)), key, mask)
                out = jnp.where(mine, dot(soft.astype(BF), value), out)
            outs.append(out.astype(BF))
        heads = jnp.concatenate(outs, 0)
        r.heads[g] = heads
        branch = dot(heads, r.out_map[...])
        is_step(size - 1)(lambda: r.own.__setitem__(..., branch))
        pl.when(step < size - 1)(lambda: r.part.__setitem__(step, branch.astype(BF)))
        for k in range(size - 1):
            is_step(k)(functools.partial(scatter.made, k))

    each_step(size, mix)
    scatter.join()
    for j in range(2, n):
        line_u.relay(j)
    gather = Gather(group, all_ref, r.g_send, r.g_recv)
    for h in range(2):
        span = slice(h * half, (h + 1) * half)
        total = r.own[span, :] + scatter.total(h)
        middle = r.tokens[span, :].astype(F32) + total
        r.middle[span, :] = middle
        scale = lax.rsqrt(jnp.mean(middle * middle, axis=1, keepdims=True) + EPS)
        all_ref[me, span] = (middle * scale * gains[1:2]).astype(BF)
        gather.start_half(h)
    gather.relay()
    for j in range(1, n):
        line_u.close(j)
    line_u.gathered()
    keeps.append(pltpu.make_async_copy(r.gu_map, r.gu_map_hbm, r.stores.at[size + 3]))
    keeps[3].start()

    def out_copies(step):
        g, two = group.from_own(step), lax.rem(step, 2)
        return (
            pltpu.make_async_copy(
                r.hidden.at[two], r.hidden_hbm.at[g], r.hidden_store.at[two]
            ),
            pltpu.make_async_copy(
                r.gu_grad.at[two], r.gu_grad_hbm.at[g], r.gu_store.at[two]
            ),
        )

    def norm_copy(g):
        return pltpu.make_async_copy(all_ref.at[g], r.norm_hbm.at[g], r.stores.at[g])

    def feed(step, is_step):
        g, two = group.from_own(step), lax.rem(step, 2)
        for k in others:
            is_step(k)(functools.partial(gather.ready, k))
            is_step(k)(functools.partial(grads.ready, k))

        @pl.when(step >= 2)
        def _():
            for copy in out_copies(step - 2):
                copy.wait()

        norm_copy(g).start()
        weights = r.gu_map[...].reshape(-1, r.gu_map.shape[3])
        acts = dot(all_ref[g], weights)
        gate, up = acts[:, :inner], acts[:, inner:]
        sigma = jax.nn.sigmoid(gate)
        silu = gate * sigma
        r.hidden[two] = (silu * up).astype(BF)
        grad_hidden = dot_trans(r.grads[g], r.down_map[...])
        grad_gate = grad_hidden * up * sigma * (1.0 + gate * (1.0 - sigma))
        r.gu_grad[two] = jnp.concatenate([grad_gate, grad_hidden * silu], 1).astype(BF)
        for copy in out_copies(step):
            copy.start()

    each_step(size, feed)
    keeps.append(pltpu.make_async_copy(r.grads, r.grads_hbm, r.stores.at[size + 4]))
    keeps[4].start()
    for k in range(4):
        for step in others:
            swap(k, step).wait_send()
    scatter.finish()
    gather.finish()
    grads.finish()
    line_q.finish()
    line_u.finish()

    @pl.when(rank < parts - 1)
    def _():
        for step in range(size):
            halo(step).wait_send()

    for keep in keeps[1:]:
        keep.wait()
    for g in range(size):
        norm_copy(g).wait()
    for step in (size - 2, size - 1):
        for copy in out_copies(step):
            copy.wait()


def forward_part(ident, count, tokens, edge, grad, gains, table, qkv_piece, gu_piece, out_weight, down_weight):
    size, parts = lax.axis_size("fsdp"), lax.axis_size("seq")
    rows, width = tokens.shape
    local, inner = out_weight.shape[0], down_weight.shape[0]
    piece, cols = gu_piece.shape[1:]
    vmem = pl.BlockSpec(memory_space=pltpu.VMEM)
    hbm = pl.BlockSpec(memory_space=pl.ANY)
    shape = lambda w: (size, rows, w)
    low = lambda s: jax.ShapeDtypeStruct(s, BF)
    maps = [(size, parts, piece, 3 * local), (size, parts, piece, cols)]
    dma = lambda *s: pltpu.SemaphoreType.DMA(s)
    hop = transfers(size)
    scratch = scatter_shapes(size, rows, width)
    return pl.pallas_call(
        functools.partial(forward_kernel, size, parts, count),
        out_shape=[
            low(shape(width)),
            low(shape(3 * local)),
            low((size, WINDOW, 2 * local)),
            low(maps[0]),
            jax.ShapeDtypeStruct((rows, width), F32),
            low(shape(local)),
            low(shape(width)),
            low(shape(width)),
            low(shape(inner)),
            low(shape(cols)),
            low(maps[1]),
            low((size,) + gains.shape),
            jax.ShapeDtypeStruct((size,) + table.shape, jnp.int32),
        ],
        in_specs=[vmem] * 5 + [hbm, hbm, vmem, vmem],
        out_specs=[hbm, hbm, vmem, hbm, vmem, vmem, hbm, hbm, hbm, hbm, hbm, vmem, vmem],
        scratch_shapes=scratch[:-2]
        + [
            pltpu.VMEM(shape(width), BF),
            pltpu.VMEM(shape(width), BF),
            pltpu.VMEM(shape(3 * local), BF),
            pltpu.VMEM(maps[0], BF),
            pltpu.VMEM(maps[1], BF),
            pltpu.VMEM((size, WINDOW, 2 * local), BF),
            pltpu.VMEM((rows, width), F32),
            pltpu.VMEM((2, rows, inner), BF),
            pltpu.VMEM((2, rows, cols), BF),
        ]
        + [dma(hop)] * 8
        + [dma(4, size - 1)] * 2
        + [dma(size)] * 2
        + [dma(2), dma(size + 5), dma(2), dma(2)]
        + line_sems(parts)
        + line_sems(parts),
        compiler_params=pltpu.CompilerParams(
            collective_id=ident, has_side_effects=True, vmem_limit_bytes=67_000_000
        ),
        cost_estimate=pl.CostEstimate(
            flops=2 * size * rows * width * (4 * local + 3 * inner),
            bytes_accessed=500_000_000,
            transcendentals=0,
        ),
        name="forward_part",
    )(tokens, edge, grad, gains, table, qkv_piece, gu_piece, out_weight, down_weight)


def heads_back(group, slot, count, lens_ref, starts_ref, own, edge, grad):
    rows, local = own.shape[0], own.shape[1] // 3
    head_of = lane_head(local)
    queries = own[:, :local]
    keys = jnp.concatenate([edge[:, :local], own[:, local : 2 * local]], 0)
    values = jnp.concatenate([edge[:, local:], own[:, 2 * local :]], 0)
    dqs, dks, dvs = [], [], []
    for block in range(rows // BLOCK):
        mask = masks_of(
            slot, block, count, lambda j: lens_ref[group, j], lambda j: starts_ref[group, j]
        )
        low = block * BLOCK
        span = slice(low, low + BLOCK + WINDOW)
        query, grads = queries[low : low + BLOCK], grad[low : low + BLOCK]
        key, value = keys[span], values[span]
        dq = jnp.zeros((BLOCK, local), F32)
        dk = jnp.zeros((BLOCK + WINDOW, local), F32)
        dv = jnp.zeros((BLOCK + WINDOW, local), F32)
        for head in range(local // HEAD_DIM):
            mine = head_of == head
            own_q = jnp.where(mine, query, jnp.zeros_like(query))
            own_g = jnp.where(mine, grads, jnp.zeros_like(grads))
            soft = soft_of(own_q, key, mask)
            grad_soft = dot_trans(own_g, value)
            total = jnp.sum(grad_soft * soft, axis=1, keepdims=True)
            grad_scores = (soft * (grad_soft - total)).astype(BF)
            dq = jnp.where(mine, dot(grad_scores, key), dq)
            dk = dk + dot_rows(grad_scores, own_q)
            dv = dv + dot_rows(soft.astype(BF), own_g)
        dqs.append(dq * SCALE)
        dks.append(dk * SCALE)
        dvs.append(dv)

    def joined(pieces):
        out = [pieces[0][:BLOCK]]
        for left, right in zip(pieces, pieces[1:]):
            out.append(left[BLOCK:] + right[:WINDOW])
            out.append(right[WINDOW:BLOCK])
        out.append(pieces[-1][BLOCK:])
        return jnp.concatenate(out, 0)

    return jnp.concatenate(dqs, 0), joined(dks), joined(dvs)


class BackRefs(NamedTuple):
    lens: Any
    starts: Any
    grad_gu_hbm: Any
    gu_map_hbm: Any
    middle: Any
    grad: Any
    gain: Any
    out_map: Any
    edge: Any
    qkv: Any
    qkv_map_hbm: Any
    gu_x: Any
    down_x: Any
    grad_middle: Any
    norm: Any
    all: Any
    dqkv: Any
    own: Any
    gu_slots: Any
    down_every: Any
    gu_pre: Any
    gu_up: Any
    gu_down: Any
    down_pre: Any
    down_up: Any
    down_down: Any
    part: Any
    first: Any
    over: Any
    joined: Any
    last: Any
    s_send: Any
    s_recv: Any
    t_send: Any
    t_recv: Any
    g_send: Any
    g_recv: Any
    grad_gu: Any
    gu_map: Any
    qkv_map: Any
    dedge: Any
    back: Any
    tail: Any
    h_send: Any
    h_recv: Any
    loads: Any
    gu_acc: Any
    gu_stage: Any
    gu_load: Any
    down_acc: Any
    down_stage: Any
    down_load: Any
    m_send: Any
    m_recv: Any


def back_kernel(size, parts, count, *refs):
    named = len(BackRefs._fields)
    r, sems = BackRefs(*refs[:named]), refs[named:]
    line = Line(parts, sems[:6])
    gu_sum = StagedSum(
        r.gu_stage, r.gu_load, line, r.gu_x, r.gu_pre, r.gu_acc, r.gu_up, r.gu_down, sems[6:12]
    )
    down_sum = StagedSum(
        r.down_stage,
        r.down_load,
        line,
        r.down_x,
        r.down_pre,
        r.down_acc,
        r.down_up,
        r.down_down,
        sems[12:],
    )
    rows = r.middle.shape[0]
    local = r.out_map.shape[0]
    rank = lax.axis_index("seq")
    slot = rank * rows
    group = Group(size)
    barrier = pltpu.get_barrier_semaphore()
    greet_group(barrier, size)

    def greet(peer):
        pl.semaphore_signal(barrier, inc=1, device_id={"seq": peer}, device_id_type=MESH_ID)

    known = line.greet(barrier)
    pl.when(line.has_above & (line.core == 1))(lambda: greet(rank + 1))
    pl.when(line.has_below & (line.core == 0))(lambda: greet(rank - 1))
    n, z = line.length, line.z
    known = known + (2 * n - 2 - z) // n * line.core + (z + n - 1) // n * (1 - line.core)
    fetches = [
        pltpu.make_async_copy(src, dst, r.loads.at[k])
        for k, (src, dst) in enumerate(
            ((r.grad_gu_hbm, r.grad_gu), (r.gu_map_hbm, r.gu_map), (r.qkv_map_hbm, r.qkv_map))
        )
    ]
    for fetch in fetches:
        fetch.start()
    pl.semaphore_wait(barrier, size - 1 + known)
    down_sum.trade()
    gu_sum.trade()
    for m in range(n):
        down_sum.begin(m)
    scatter = Scatter(
        group, r.part, r.first, r.over, r.joined, r.last, r.s_send, r.s_recv
    )
    gather = Gather(group, r.all, r.g_send, r.g_recv)
    fetches[0].wait()
    fetches[1].wait()

    def step_two(step, is_step):
        partial = dot_trans(r.grad_gu[group.to_own(step)], r.gu_map[...])
        is_step(size - 1)(lambda: r.own.__setitem__(..., partial))
        pl.when(step < size - 1)(lambda: r.part.__setitem__(step, partial.astype(BF)))
        for k in range(size - 1):
            is_step(k)(functools.partial(scatter.made, k))

    each_step(size, step_two)
    scatter.join()
    gu_sum.begin(0)
    down_sum.advance(1)
    half = rows // 2
    norm_sum = jnp.zeros((1, r.middle.shape[1]), F32)
    for h in range(2):
        span = slice(h * half, (h + 1) * half)
        grad = r.own[span, :] + scatter.total(h)
        middle = r.middle[span, :]
        scale = lax.rsqrt(jnp.mean(middle * middle, axis=1, keepdims=True) + EPS)
        unit = middle * scale
        scaled = grad * r.gain[...]
        norm_sum = norm_sum + jnp.sum(grad * unit, axis=0, keepdims=True)
        grad_out = r.grad[span, :].astype(F32)
        grad_middle = grad_out + scale * (
            scaled - unit * jnp.mean(scaled * unit, axis=1, keepdims=True)
        )
        r.grad_middle[span, :] = grad_middle
        r.all[group.me, span] = grad_middle.astype(BF)
        gather.start_half(h)
    r.norm[...] = norm_sum
    own_down = pltpu.make_async_copy(r.down_acc.at[z], r.down_every.at[rank], r.down_load.at[0])

    def halo(step):
        g = group.from_own(step)
        sems = r.h_send.at[step], r.h_recv.at[step]
        return remote(r.dedge.at[g], r.back.at[g], *sems, seq=rank - 1)

    def step_heads(step, is_step):
        g = group.from_own(step)

        @is_step(1)
        def _():
            gather.relay()
            for t in range(2, n - 1):
                down_sum.advance(t)

        @is_step(2)
        def _():
            down_sum.total()
            own_down.start()
            own_down.wait()
            line.gather(lambda owner: r.down_every.at[owner])
            for m in range(1, n):
                gu_sum.begin(m)

        is_step(size - 1)(lambda: gu_sum.advance(1))

        for k in range(1, size):
            is_step(k)(functools.partial(gather.ready, k))
        grad = dot_trans(r.all[g], r.out_map[...]).astype(BF)
        dq, dk, dv = heads_back(
            g, slot, count, r.lens, r.starts, r.qkv[g], r.edge[g], grad
        )
        r.dedge[g] = jnp.concatenate([dk[:WINDOW], dv[:WINDOW]], 1).astype(BF)
        full = jnp.concatenate([dq, dk[WINDOW:], dv[WINDOW:]], 1)
        r.dqkv[g] = full.astype(BF)
        r.tail[g] = full[rows - WINDOW :]
        pl.when(rank > 0)(lambda: halo(step).start())

    each_step(size, step_heads)
    scatter.finish()
    fetches[2].wait()

    @pl.when(rank == parts - 1)
    def _():
        r.back[...] = jnp.zeros_like(r.back)

    @pl.when(rank < parts - 1)
    def _():
        for step in range(size):
            halo(step).wait_recv()

    scatter = Scatter(
        group, r.part, r.first, r.over, r.joined, r.last, r.t_send, r.t_recv
    )

    def step_one(step, is_step):
        g = group.to_own(step)
        back = r.back[g].astype(F32)
        wide = jnp.concatenate([jnp.zeros((WINDOW, local), F32), back], 1)
        r.dqkv[g, pl.ds(rows - WINDOW, WINDOW)] = (r.tail[g] + wide).astype(BF)
        partial = dot_trans(r.dqkv[g], r.qkv_map[...])
        is_step(size - 1)(lambda: r.own.__setitem__(..., partial))
        pl.when(step < size - 1)(lambda: r.part.__setitem__(step, partial.astype(BF)))
        for k in range(size - 1):
            is_step(k)(functools.partial(scatter.made, k))

    each_step(size, step_one)
    line.relay(1)
    scatter.join()
    for t in range(2, n - 1):
        gu_sum.advance(t)
        line.relay(t)
    line.relay(n - 1)
    for h in range(2):
        span = slice(h * half, (h + 1) * half)
        r.own[span, :] = r.own[span, :] + scatter.total(h)
    gu_sum.total()

    def swap(step):
        peer = lax.rem(group.me + step, size)
        sems = r.m_send.at[step - 1], r.m_recv.at[step - 1]
        return remote(r.gu_acc.at[z, peer], r.gu_slots.at[group.me], *sems, fsdp=peer)

    for step in range(1, size):
        swap(step).start()
    own_slot = pltpu.make_async_copy(
        r.gu_acc.at[z, group.me], r.gu_slots.at[group.me], r.gu_load.at[0]
    )
    own_slot.start()
    for j in range(1, n):
        line.close(j)
    line.gathered()
    for step in range(1, size):
        swap(step).wait()
    scatter.finish()
    gather.finish()
    down_sum.finish()
    gu_sum.finish()
    line.finish()
    own_slot.wait()

    @pl.when(rank > 0)
    def _():
        for step in range(size):
            halo(step).wait_send()


def back_part(
    ident, lens, starts, grad_gu, gu_map, middle, grad, gain, out_weight, edge, qkv, qkv_map, gu_x, down_x
):
    size, parts = lax.axis_size("fsdp"), lax.axis_size("seq")
    rows, width = middle.shape
    local = out_weight.shape[0]
    n = parts // 2
    vmem = pl.BlockSpec(memory_space=pltpu.VMEM)
    smem = pl.BlockSpec(memory_space=pltpu.SMEM)
    hbm = pl.BlockSpec(memory_space=pl.ANY)
    dma = lambda *s: pltpu.SemaphoreType.DMA(s)
    low = lambda *s: jax.ShapeDtypeStruct(s, BF)
    sems = [dma(transfers(size))] * 2
    gu, down = gu_x.shape[1:], down_x.shape[1:]
    outs = pl.pallas_call(
        functools.partial(back_kernel, size, parts, lens.shape[1]),
        out_shape=[
            jax.ShapeDtypeStruct((rows, width), F32),
            jax.ShapeDtypeStruct((1, width), F32),
            low(size, rows, width),
            low(*qkv.shape),
            jax.ShapeDtypeStruct((rows, width), F32),
            low(*gu),
            low(parts, *down),
        ]
        + [low(n, *gu)] * 3
        + [low(n, *down)] * 3,
        in_specs=[smem, smem, hbm, hbm] + [vmem] * 6 + [hbm] * 3,
        out_specs=[vmem] * 5 + [hbm] * 8,
        scratch_shapes=scatter_shapes(size, rows, width)
        + sems
        + sems
        + [
            pltpu.VMEM(grad_gu.shape, BF),
            pltpu.VMEM(gu_map.shape, BF),
            pltpu.VMEM(qkv_map.shape, BF),
            pltpu.VMEM((size, WINDOW, 2 * local), BF),
            pltpu.VMEM((size, WINDOW, 2 * local), BF),
            pltpu.VMEM((size, WINDOW, 3 * local), F32),
            dma(size),
            dma(size),
            dma(3),
            pltpu.VMEM((n,) + gu, BF),
            pltpu.VMEM((2,) + gu, BF),
            dma(2),
            pltpu.VMEM((n,) + down, BF),
            pltpu.VMEM((2,) + down, BF),
            dma(2),
            dma(size - 1),
            dma(size - 1),
        ]
        + line_sems(parts) * 3,
        compiler_params=pltpu.CompilerParams(
            collective_id=ident, has_side_effects=True, vmem_limit_bytes=67_000_000
        ),
        cost_estimate=pl.CostEstimate(
            flops=2 * size * rows * (gu_map.size + qkv_map.size + width * local),
            bytes_accessed=400_000_000,
            transcendentals=0,
        ),
        name="back_part",
    )(lens, starts, grad_gu, gu_map, middle, grad, gain, out_weight, edge, qkv, qkv_map, gu_x, down_x)
    return outs[:7]


class CloseRefs(NamedTuple):
    gated_hbm: Any
    dqkv_hbm: Any
    heads_hbm: Any
    gb_hbm: Any
    gu_slots: Any
    terms: Any
    hidden_hbm: Any
    down_hbm: Any
    every_hbm: Any
    gu_every: Any
    feed: Any
    terms_out: Any
    pre: Any
    up_in: Any
    down_in: Any
    part: Any
    first: Any
    over: Any
    joined: Any
    last: Any
    x: Any
    acc: Any
    stage: Any
    stage_load: Any
    every: Any
    slots: Any
    gu_own: Any
    gated: Any
    dqkv: Any
    heads: Any
    gb: Any
    hidden: Any
    down_map: Any
    terms_in: Any
    terms_all: Any
    s_send: Any
    s_recv: Any
    m_send: Any
    m_recv: Any
    t_send: Any
    t_recv: Any
    loads: Any


def close_kernel(size, parts, made, *refs):
    named = len(CloseRefs._fields)
    r, sems = CloseRefs(*refs[:named]), refs[named:]
    rank = lax.axis_index("seq")
    group = Group(size)
    me = group.me
    line_u, line_q = Line(parts, sems[:6]), Line(parts, sems[6:12])
    n, z = line_q.length, line_q.z
    sums = MixedSum(
        r.stage, r.stage_load, line_q, r.x, r.pre, r.acc, r.up_in, r.down_in, sems[12:]
    )
    rows = r.feed.shape[0]
    half = rows // 2
    barrier = pltpu.get_barrier_semaphore()
    greet_group(barrier, size)
    for step in range(1, parts):
        peer = lax.rem(rank + step, parts)
        pl.semaphore_signal(barrier, inc=1, device_id={"seq": peer}, device_id_type=MESH_ID)
    moves = [
        (r.gu_slots, r.gu_own),
        (r.hidden_hbm, r.hidden),
        (r.down_hbm, r.down_map),
    ]
    if made:
        moves += [
            (r.gated_hbm, r.gated),
            (r.dqkv_hbm, r.dqkv),
            (r.heads_hbm, r.heads),
            (r.gb_hbm, r.gb),
        ]
    else:
        moves += [(r.gated_hbm, r.x)]
    fetches = [
        pltpu.make_async_copy(src, dst, r.loads.at[k]) for k, (src, dst) in enumerate(moves)
    ]
    for k in [0] + list(range(3, len(moves))) + [1, 2]:
        fetches[k].start()
    r.terms_in[me] = r.terms[me]
    own_slots = pltpu.make_async_copy(r.gu_own, r.gu_every.at[rank], r.loads.at[0])
    fetches[0].wait()
    own_slots.start()
    own_slots.wait()
    pl.semaphore_wait(barrier, size + parts - 2)
    line_u.gather(lambda owner: r.gu_every.at[owner])

    def swap(k, step):
        peer = lax.rem(me + step, size)
        src, dst = (
            lambda: (r.terms.at[peer], r.terms_in.at[me]),
            lambda: (r.acc.at[z, peer], r.slots.at[me]),
        )[k]()
        return remote(src, dst, r.m_send.at[k, step - 1], r.m_recv.at[k, step - 1], fsdp=peer)

    others = range(1, size)
    for step in others:
        swap(0, step).start()

    scatter = Scatter(
        group, r.part, r.first, r.over, r.joined, r.last, r.s_send, r.s_recv
    )

    def down(step, is_step):
        partial = dot(r.hidden[group.to_own(step)], r.down_map[...])
        is_step(size - 1)(lambda: r.feed.__setitem__(..., partial))
        pl.when(step < size - 1)(lambda: r.part.__setitem__(step, partial.astype(BF)))
        for k in range(size - 1):
            is_step(k)(functools.partial(scatter.made, k))

    for fetch in fetches[3:]:
        fetch.wait()
    if made:
        span = r.gated.shape[1] // (size // 2)
        for h in range(size // 2):
            lanes = slice(h * span, (h + 1) * span)
            pack_pair(
                r.x, h, r.gated[:, lanes], r.dqkv[...], r.heads[...], r.gb[:, lanes]
            )
    sums.trade()
    line_u.relay(1)
    fetches[1].wait()
    fetches[2].wait()
    for m in range(n):
        sums.begin(m)
    each_step(size, down)

    for step in others:
        swap(0, step).wait_recv()
    small = r.terms_in[0]
    for f in others:
        small = small + r.terms_in[f]
    r.terms_all[rank] = small

    def spread(step):
        peer = lax.rem(rank + step, parts)
        view = r.terms_all.at[rank]
        return remote(view, view, r.t_send.at[step - 1], r.t_recv.at[step - 1], seq=peer)

    for step in range(1, parts):
        spread(step).start()
    scatter.join()

    for t in range(1, n - 1):
        sums.advance(t)
        line_u.relay(t + 1)
    for h in range(2):
        span = slice(h * half, (h + 1) * half)
        r.feed[span, :] = r.feed[span, :] + scatter.total(h)
    sums.total()
    for step in others:
        swap(1, step).start()
    for j in range(1, n):
        line_u.close(j)
    r.slots[me] = r.acc[z, me]
    for step in others:
        swap(1, step).wait_recv()
    local = r.x.shape[3] // 4
    lane = lax.broadcasted_iota(jnp.int32, (1, 1, 4 * local), 2)
    r.every[rank] = jnp.where(lane < 3 * local, r.slots[...], r.acc[z])
    line_q.gather(lambda owner: r.every.at[owner])
    line_u.gathered()
    for j in range(1, n):
        line_q.relay(j)
    for j in range(1, n):
        line_q.close(j)
    line_q.gathered()
    store = pltpu.make_async_copy(r.every, r.every_hbm, r.loads.at[1])
    store.start()
    for step in range(1, parts):
        spread(step).wait_recv()
    small = r.terms_all[0]
    for k in range(1, parts):
        small = small + r.terms_all[k]
    r.terms_out[...] = small
    for k in range(2):
        for step in others:
            swap(k, step).wait_send()
    for step in range(1, parts):
        spread(step).wait_send()
    scatter.finish()
    sums.finish()
    line_u.finish()
    line_q.finish()
    store.wait()


def close_part(ident, gated, dqkv, heads, gb, gu_slots, terms, hidden, down_weight):
    size, parts = lax.axis_size("fsdp"), lax.axis_size("seq")
    width = gated.shape[1]
    made = packs(size, parts, width)
    piece, cols = width // (size * parts), dqkv.shape[1] + heads.shape[1]
    if not made:
        gated = pack_plain(parts, size, gated, dqkv, heads, gb)
    n = parts // 2
    rows = hidden.shape[1]
    vmem = pl.BlockSpec(memory_space=pltpu.VMEM)
    hbm = pl.BlockSpec(memory_space=pl.ANY)
    dma = lambda *s: pltpu.SemaphoreType.DMA(s)
    gu_shape = (parts,) + gu_slots.shape
    packed = (parts, size, piece, cols)
    scratch = scatter_shapes(size, rows, width)
    low = lambda *s: jax.ShapeDtypeStruct(s, BF)
    copy_of = lambda a: pltpu.VMEM(a.shape if made else (8, 128), BF)
    return pl.pallas_call(
        functools.partial(close_kernel, size, parts, made),
        out_shape=[
            low(*packed),
            low(*gu_shape),
            jax.ShapeDtypeStruct((rows, width), F32),
            jax.ShapeDtypeStruct(terms.shape[1:], F32),
        ]
        + [low(n, size, piece, cols)] * 3,
        in_specs=[hbm] * 5 + [vmem, hbm, hbm],
        out_specs=[hbm, hbm, vmem, vmem, hbm, hbm, hbm],
        scratch_shapes=scratch[:-2]
        + [
            pltpu.VMEM(packed, BF),
            pltpu.VMEM((n, size, piece, cols), BF),
            pltpu.VMEM((2, size, piece, cols), BF),
            dma(2),
            pltpu.VMEM(packed, BF),
            pltpu.VMEM((size, piece, cols), BF),
            pltpu.VMEM(gu_slots.shape, BF),
            copy_of(gated),
            copy_of(dqkv),
            copy_of(heads),
            copy_of(gb),
            pltpu.VMEM(hidden.shape, BF),
            pltpu.VMEM(down_weight.shape, BF),
            pltpu.VMEM(terms.shape, F32),
            pltpu.VMEM((parts,) + terms.shape[1:], F32),
        ]
        + scratch[-2:]
        + [dma(2, size - 1)] * 2
        + [dma(parts - 1)] * 2
        + [dma(7)]
        + line_sems(parts) * 3,
        compiler_params=pltpu.CompilerParams(
            collective_id=ident, has_side_effects=True, vmem_limit_bytes=67_000_000
        ),
        cost_estimate=pl.CostEstimate(
            flops=2 * size * rows * (down_weight.size + width * cols),
            bytes_accessed=500_000_000,
            transcendentals=0,
        ),
        name="close_part",
    )(gated, dqkv, heads, gb, gu_slots, terms, hidden, down_weight)[:4]


def pack_pair(out, pair, x, g, heads=None, gb=None):
    parts, _, piece, _ = out.shape
    rows = parts * piece
    full = dot_rows(x, g)
    side = None if heads is None else dot_rows(heads, gb)
    for k in range(2):
        own = full[k * rows : (k + 1) * rows]
        if side is not None:
            wide = side.shape[1] // 2
            own = jnp.concatenate([own, side[:, k * wide : (k + 1) * wide]], 1)
        out[:, pair * 2 + k] = own.astype(BF).reshape(parts, piece, own.shape[1])


def pack_kernel(x_ref, g_ref, out_ref):
    pack_pair(out_ref, 0, x_ref[...], g_ref[...])


def packs(size, parts, width):
    return width // (size * parts) % 8 == 0 and 2 * width // size % 128 == 0


def pack_plain(parts, size, x, g, heads=None, gb=None):
    width, cols = x.shape[1], g.shape[1]
    piece = width // (size * parts)
    full = dot_rows(x, g).reshape(size, parts, piece, cols)
    if heads is not None:
        side = dot_rows(heads, gb).reshape(parts, piece, size, -1).transpose(2, 0, 1, 3)
        full = jnp.concatenate([full, side], 3)
    return full.transpose(1, 0, 2, 3).astype(BF)


def pack_grads(parts, size, x, g):
    total, width = x.shape
    cols = g.shape[1]
    if not packs(size, parts, width):
        return pack_plain(parts, size, x, g)
    piece = width // (size * parts)
    pair = pl.BlockSpec((total, 2 * width // size), lambda i: (0, i))
    whole = pl.BlockSpec(g.shape, lambda i: (0, 0), pipeline_mode=pl.Buffered(1))
    return pl.pallas_call(
        pack_kernel,
        grid=(size // 2,),
        out_shape=jax.ShapeDtypeStruct((parts, size, piece, cols), BF),
        in_specs=[pair, whole],
        out_specs=pl.BlockSpec((parts, 2, piece, cols), lambda i: (0, i, 0, 0)),
        cost_estimate=pl.CostEstimate(
            flops=2 * total * width * cols,
            bytes_accessed=2 * (x.size + g.size + width * cols),
            transcendentals=0,
        ),
        name="pack_grads",
    )(x, g)


def unpack_kernel(widths, every_ref, *outs):
    size = every_ref.shape[1]
    blocks = [every_ref[0, i].astype(F32) for i in range(size)]
    low = 0
    for width, out in zip(widths, outs):
        out[...] = jnp.concatenate([b[:, low : low + width] for b in blocks], 1)
        low += width


def unpack_grads(every, widths):
    parts, size, piece, cols = every.shape
    if piece % 8:
        outs, low = [], 0
        for width in widths:
            block = every[:, :, :, low : low + width].transpose(0, 2, 1, 3)
            outs.append(block.reshape(parts * piece, size * width).astype(F32))
            low += width
        return outs
    return pl.pallas_call(
        functools.partial(unpack_kernel, widths),
        grid=(parts,),
        out_shape=[jax.ShapeDtypeStruct((parts * piece, size * w), F32) for w in widths],
        in_specs=[pl.BlockSpec((1, size, piece, cols), lambda i: (i, 0, 0, 0))],
        out_specs=[pl.BlockSpec((piece, size * w), lambda i: (i, 0)) for w in widths],
        cost_estimate=pl.CostEstimate(flops=0, bytes_accessed=every.size * 6, transcendentals=0),
        name="unpack_grads",
    )(every)


def columns_piece(weights, part, parts):
    size = lax.axis_size("fsdp")
    rows = weights[0].shape[0] // parts
    pieces = []
    for weight in weights:
        own = lax.dynamic_slice_in_dim(weight, part * rows, rows, 0)
        pieces.append(own.reshape(rows, size, -1))
    return jnp.concatenate(pieces, 2).transpose(1, 0, 2)


def shards(
    tokens,
    seq_lengths,
    seq_offsets,
    norm1_gain,
    conv_weight,
    query_weight,
    key_weight,
    value_weight,
    out_weight,
    norm2_gain,
    gate_weight,
    up_weight,
    down_weight,
    cotangent,
):
    size = lax.axis_size("fsdp")
    parts = lax.axis_size("seq")
    part = lax.axis_index("seq")
    me = lax.axis_index("fsdp")
    own_tokens = tokens[0]
    rows, width = own_tokens.shape
    slice_width = norm1_gain.shape[0]
    first_slot = part * rows
    count = seq_lengths.shape[1]

    slot_ext = first_slot - 2 + jnp.arange(rows + 2, dtype=jnp.int32)
    segment_ext = segment_of(
        slot_ext, count, lambda j: seq_lengths[0, j], lambda j: seq_offsets[0, j]
    )
    segment_own = segment_ext[2:]
    same_one = (segment_own == segment_ext[1:-1]).astype(F32)[:, None]
    same_two = (segment_own == segment_ext[:-2]).astype(F32)[:, None]
    live_mask = (segment_own >= 0).astype(F32)[:, None]

    gains = jnp.concatenate(
        [
            norm1_gain[None],
            norm2_gain[None],
            conv_weight.T,
            jnp.zeros((3, slice_width), BF),
        ],
        0,
    )
    table = jnp.zeros((8, 128), jnp.int32)
    table = table.at[0, :count].set(seq_lengths[0]).at[1, :count].set(seq_offsets[0])
    qkv_piece = columns_piece((query_weight, key_weight, value_weight), part, parts)
    gu_piece = columns_piece((gate_weight, up_weight), part, parts)
    edge_tokens = shifted(own_tokens[rows - 2 :], "seq", 1)
    grad_down = (cotangent[0].astype(F32) * live_mask).astype(BF)
    (
        gated_all,
        qkv,
        edge,
        qkv_map,
        middle,
        heads_out,
        grad_down_all,
        normed_all,
        hidden,
        grad_gu,
        gu_map,
        gains_all,
        table_all,
    ) = forward_part(
        0,
        count,
        own_tokens,
        jnp.pad(edge_tokens, ((0, 6), (0, 0))),
        grad_down,
        gains,
        table,
        qkv_piece,
        gu_piece,
        out_weight,
        down_weight,
    )
    local = out_weight.shape[0]
    flat = lambda a: a.reshape(-1, a.shape[-1])
    lens_all, starts_all = table_all[:, 0, :count], table_all[:, 1, :count]
    gains_all = gains_all.transpose(1, 0, 2).reshape(8, width)
    norm_one = gains_all[0].astype(F32)
    norm_two = gains_all[1].astype(F32)
    taps = gains_all[2:5].astype(F32)
    qkv_map, gu_map = qkv_map.reshape(width, -1), gu_map.reshape(width, -1)
    grad_down_all = flat(grad_down_all)

    extended = jnp.concatenate([edge_tokens, own_tokens], 0).astype(F32)
    scale_one = lax.rsqrt(jnp.mean(extended * extended, axis=1, keepdims=True) + EPS)
    normed = extended * scale_one * norm_one
    conv_mix = (
        normed[2:] * taps[0]
        + same_one * normed[1:-1] * taps[1]
        + same_two * normed[:-2] * taps[2]
    )

    gu_packed = pack_grads(parts, size, flat(normed_all), flat(grad_gu))
    down_packed = dot_rows(flat(hidden), grad_down_all).astype(BF)
    grad_middle, norm2_term, grad_branch_all, dqkv, grad_gated, gu_slots, down_every = back_part(
        4,
        lens_all,
        starts_all,
        grad_gu,
        gu_map,
        middle,
        grad_down,
        norm_two[None],
        out_weight,
        edge,
        qkv,
        qkv_map,
        gu_packed,
        down_packed.reshape(parts, -1, width),
    )
    norm2_term = norm2_term[0]
    down_total = down_every.reshape(-1, width).astype(F32)
    normed_own = normed[2:]
    grad_mix = grad_gated * normed_own
    part_zero = jnp.pad(grad_gated * conv_mix + grad_mix * taps[0], ((2, 0), (0, 0)))
    part_one = jnp.pad(grad_mix * same_one * taps[1], ((1, 1), (0, 0)))
    part_two = jnp.pad(grad_mix * same_two * taps[2], ((0, 2), (0, 0)))
    grad_normed = part_zero + part_one + part_two
    unit_one = extended * scale_one
    grad_unit_one = grad_normed * norm_one
    grad_extended = scale_one * (
        grad_unit_one - unit_one * jnp.mean(grad_unit_one * unit_one, axis=1, keepdims=True)
    )
    edge_back = shifted(grad_extended[:2], "seq", -1)
    tokens_grad = grad_middle + grad_extended[2:] + jnp.pad(edge_back, ((rows - 2, 0), (0, 0)))

    terms = jnp.stack(
        [
            jnp.sum(grad_normed * unit_one, axis=0),
            norm2_term,
            jnp.sum(grad_mix * normed_own, axis=0),
            jnp.sum(grad_mix * same_one * normed[1:-1], axis=0),
            jnp.sum(grad_mix * same_two * normed[:-2], axis=0),
        ]
    )
    terms = jnp.pad(terms, ((0, 3), (0, 0))).reshape(8, size, slice_width).transpose(1, 0, 2)
    gu_slots, terms, down_total, tokens_grad = lax.optimization_barrier(
        (gu_slots, terms, down_total, tokens_grad)
    )
    qkvo_every, gu_every, feed, terms = close_part(
        5,
        flat(gated_all),
        flat(dqkv),
        flat(heads_out),
        flat(grad_branch_all),
        gu_slots,
        terms,
        hidden,
        down_weight,
    )
    gate_total, up_total = unpack_grads(gu_every, (gu_map.shape[1] // 2,) * 2)
    query_total, key_total, value_total, out_total = unpack_grads(qkvo_every, (local,) * 4)

    layer_out = (live_mask * (middle + feed)).astype(BF)[None]
    return (
        layer_out,
        tokens_grad[None],
        terms[0],
        terms[2:5].T,
        query_total,
        key_total,
        value_total,
        out_total,
        terms[1],
        gate_total,
        up_total,
        down_total,
    )


def solution(mesh):
    placed = (
        P("fsdp", "seq", None),
        P("fsdp", None),
        P("fsdp", None),
        P("fsdp"),
        P("fsdp", None),
        P("fsdp", None),
        P("fsdp", None),
        P("fsdp", None),
        P("fsdp", None),
        P("fsdp"),
        P("fsdp", None),
        P("fsdp", None),
        P("fsdp", None),
        P("fsdp", "seq", None),
    )
    return jax.shard_map(
        shards,
        mesh=mesh,
        in_specs=placed,
        out_specs=(
            P("fsdp", "seq", None),
            P("fsdp", "seq", None),
            P("fsdp"),
            P("fsdp", None),
            P("fsdp", None),
            P("fsdp", None),
            P("fsdp", None),
            P("fsdp", None),
            P("fsdp"),
            P("fsdp", None),
            P("fsdp", None),
            P("fsdp", None),
        ),
        check_vma=False,
    )
```

```python
import functools
from typing import Any, NamedTuple

import jax
import jax.numpy as jnp
from jax import lax
from jax.experimental import pallas as pl
from jax.experimental.pallas import tpu as pltpu
from jax.sharding import PartitionSpec as P

HEADS = 16
WINDOW = 64
HEAD_DIM = 112
BLOCK = 128

EPS = 1e-05
NEG = -1e30
SCALE = HEAD_DIM ** (-0.5)
MESH_ID = pl.DeviceIdType.MESH
BF = jnp.bfloat16
F32 = jnp.float32


def shifted(array, axis, by):
    length = lax.axis_size(axis)
    pairs = [(i, i + by) for i in range(length) if 0 <= i + by < length]
    return lax.ppermute(array, axis, pairs)


def segment_of(slot, count, lengths, starts):
    found = jnp.full(slot.shape, -1, jnp.int32)
    for j in range(count):
        inside = (slot >= starts(j)) & (slot < starts(j) + lengths(j))
        found = jnp.where(inside, j, found)
    return jnp.where(slot < 0, -2, found)


def dot_rows(left, right):
    return lax.dot_general(left, right, (((0,), (0,)), ((), ())), preferred_element_type=F32)


def dot_trans(left, right):
    return lax.dot_general(left, right, (((1,), (1,)), ((), ())), preferred_element_type=F32)


def dot(left, right):
    return jnp.dot(left, right, preferred_element_type=F32)


def masks_of(first, block, count, length, start):
    rows = first + block * BLOCK
    query = rows + lax.broadcasted_iota(jnp.int32, (BLOCK, 1), 0)
    keys = rows - WINDOW + lax.broadcasted_iota(jnp.int32, (1, BLOCK + WINDOW), 1)
    seg_q = segment_of(query, count, length, start)
    seg_k = segment_of(keys, count, length, start)
    far = query - keys
    return (far >= 0) & (far <= WINDOW) & (seg_q == seg_k)


def soft_of(query, keys, mask):
    scores = dot_trans(query, keys) * SCALE
    scores = jnp.where(mask, scores, NEG)
    peak = jnp.max(scores, axis=1, keepdims=True)
    exponent = jnp.exp(scores - peak)
    return exponent / jnp.sum(exponent, axis=1, keepdims=True)


def lane_head(width):
    return lax.broadcasted_iota(jnp.int32, (1, width), 1) // HEAD_DIM


def remote(src, dst, send, recv, **peer):
    return pltpu.make_async_remote_copy(
        src_ref=src,
        dst_ref=dst,
        send_sem=send,
        recv_sem=recv,
        device_id=peer,
        device_id_type=MESH_ID,
    )


def greet_group(barrier, size):
    me = lax.axis_index("fsdp")
    for step in range(1, size):
        peer = lax.rem(me + step, size)
        pl.semaphore_signal(barrier, inc=1, device_id={"fsdp": peer}, device_id_type=MESH_ID)


class Group:
    def __init__(self, size):
        self.size = size
        self.me = lax.axis_index("fsdp")
        self.square = size == 4
        if self.square:
            x, y = lax.rem(self.me, 2), self.me // 2
            self.at = lambda bx, by: lax.rem(y + by, 2) * 2 + lax.rem(x + bx, 2)
            self.x, self.y, self.far = self.at(1, 0), self.at(0, 1), self.at(1, 1)

    def from_own(self, step):
        if self.square:
            return self.at(lax.rem(step, 2), step // 2)
        return lax.rem(self.me - step + self.size, self.size)

    def to_own(self, step):
        if self.square:
            return self.at(1 - step // 2, 1 - lax.rem(step, 2))
        return lax.rem(self.me + 1 + step, self.size)


class Gather:
    def __init__(self, group, ref, send, recv):
        self.group, self.ref, self.send, self.recv = group, ref, send, recv
        self.half = ref.shape[1] // 2

    def part(self, k, slot, half, peer):
        view = self.ref.at[slot, pl.ds(half * self.half, self.half)]
        return remote(view, view, self.send.at[k], self.recv.at[k], fsdp=peer)

    def whole(self, k):
        g = self.group
        view = self.ref.at[g.me]
        sems = self.send.at[k - 1], self.recv.at[k - 1]
        return remote(view, view, *sems, fsdp=lax.rem(g.me + k, g.size))

    def copy(self, k):
        g = self.group
        if not g.square:
            return self.whole(k + 1)
        slot = (g.me, g.me, g.me, g.me, g.x, g.y)[k]
        half = (0, 1, 0, 1, 0, 1)[k]
        return self.part(k, slot, half, (g.x, g.x, g.y, g.y, g.y, g.x)[k])

    def start_half(self, half):
        if self.group.square:
            self.copy(half).start()
            self.copy(2 + half).start()
        elif half == 1:
            for k in range(self.group.size - 1):
                self.copy(k).start()

    def relay(self):
        if self.group.square:
            self.copy(0).wait_recv()
            self.copy(4).start()
            self.copy(3).wait_recv()
            self.copy(5).start()

    def ready(self, step):
        if not self.group.square:
            self.copy(step - 1).wait_recv()
        elif step == 3:
            self.copy(4).wait_recv()
            self.copy(5).wait_recv()
        else:
            self.copy(step).wait_recv()

    def finish(self):
        for k in range(transfers(self.group.size)):
            self.copy(k).wait_send()


class Scatter:
    def __init__(self, group, part, first, over, joined, last, send, recv):
        self.group, self.part = group, part
        self.first, self.over, self.joined, self.last = first, over, joined, last
        self.send, self.recv = send, recv
        self.half = part.shape[1] // 2

    def copy(self, k):
        g, half = self.group, self.half
        low, high = pl.ds(0, half), pl.ds(half, half)
        if not g.square:
            src, dst, peer = self.part.at[k], self.first.at[k], lax.rem(g.me + 1 + k, g.size)
        else:
            src, dst, peer = (
                lambda: (self.part.at[0, low], self.over.at[0], g.x),
                lambda: (self.part.at[0, high], self.over.at[1], g.y),
                lambda: (self.part.at[1, low], self.first.at[0], g.x),
                lambda: (self.part.at[2, high], self.first.at[1], g.y),
                lambda: (self.joined.at[0], self.last.at[0], g.y),
                lambda: (self.joined.at[1], self.last.at[1], g.x),
            )[k]()
        return remote(src, dst, self.send.at[k], self.recv.at[k], fsdp=peer)

    def made(self, step):
        if not self.group.square:
            self.copy(step).start()
        elif step == 0:
            self.copy(0).start()
            self.copy(1).start()
        elif step in (1, 2):
            self.copy(step + 1).start()

    def join(self):
        if not self.group.square:
            return
        half = self.half
        for k, (step, rows) in enumerate(((2, slice(0, half)), (1, slice(half, 2 * half)))):
            self.copy(k).wait_recv()
            own = self.part[step, rows].astype(F32)
            self.joined[k] = (own + self.over[k].astype(F32)).astype(BF)
            self.copy(4 + k).start()

    def total(self, half):
        count = self.half
        if self.group.square:
            self.copy(2 + half).wait_recv()
            self.copy(4 + half).wait_recv()
            return self.first[half].astype(F32) + self.last[half].astype(F32)
        if half == 0:
            for k in range(self.group.size - 1):
                self.copy(k).wait_recv()
        rows = slice(half * count, (half + 1) * count)
        out = self.first[0, rows].astype(F32)
        for k in range(1, self.group.size - 1):
            out = out + self.first[k, rows].astype(F32)
        return out

    def finish(self):
        for k in range(transfers(self.group.size)):
            self.copy(k).wait_send()


class Line:
    def __init__(self, parts, sems):
        self.rank = lax.axis_index("seq")
        self.parts, self.length = parts, parts // 2
        self.z, self.core = self.rank // 2, lax.rem(self.rank, 2)
        self.above, self.below = self.rank + 2, self.rank - 2
        self.beside = self.rank + 1 - 2 * self.core
        self.has_above, self.has_below = self.z < self.length - 1, self.z > 0
        self.sems = sems

    def greet(self, barrier):
        def one(peer):
            pl.semaphore_signal(barrier, inc=1, device_id={"seq": peer}, device_id_type=MESH_ID)

        one(self.beside)
        pl.when(self.has_above)(lambda: one(self.above))
        pl.when(self.has_below)(lambda: one(self.below))
        n, z = self.length, self.z
        return 1 + (2 * n - 2 - z) // n + (z + n - 1) // n

    def up(self, k, owner):
        view = self.view(owner)
        return remote(view, view, self.sems[0].at[k], self.sems[1].at[k], seq=self.above)

    def down(self, k, owner):
        view = self.view(owner)
        return remote(view, view, self.sems[2].at[k], self.sems[3].at[k], seq=self.below)

    def side(self, k, owner):
        view = self.view(owner)
        return remote(view, view, self.sems[4].at[k], self.sems[5].at[k], seq=self.beside)

    def gather(self, view):
        self.view = view
        pl.when(self.has_above)(lambda: self.up(0, self.rank).start())
        pl.when(self.has_below)(lambda: self.down(0, self.rank).start())
        self.side(self.z, self.rank).start()

    def own_up(self):
        pl.when(self.has_above)(lambda: self.up(0, self.rank).start())

    def own_down(self):
        pl.when(self.has_below)(lambda: self.down(0, self.rank).start())

    def relay_up(self, j):
        rank, z = self.rank, self.z

        @pl.when((z >= j) & self.has_above)
        def _():
            self.up(j - 1, rank).wait_recv()
            self.up(j, rank - 2 * j).start()
            self.side(z - j, rank - 2 * j).start()

    def relay_down(self, j):
        rank, z = self.rank, self.z

        @pl.when((z + j < self.length) & self.has_below)
        def _():
            self.down(j - 1, rank).wait_recv()
            self.down(j, rank + 2 * j).start()
            self.side(z + j, rank + 2 * j).start()

    def relay(self, j):
        self.relay_up(j)
        self.relay_down(j)

    def close(self, j):
        rank, z = self.rank, self.z

        @pl.when((z >= j) & (z == self.length - 1))
        def _():
            self.up(j - 1, rank).wait_recv()
            self.side(z - j, rank - 2 * j).start()

        @pl.when((z + j < self.length) & (z == 0))
        def _():
            self.down(j - 1, rank).wait_recv()
            self.side(z + j, rank + 2 * j).start()

    def gathered(self):
        for k in range(self.length):
            self.side(k, self.rank).wait_recv()

    def finish(self):
        rank, z = self.rank, self.z
        for k in range(self.length):
            self.side(k, rank).wait_send()
        pl.when(self.has_above)(lambda: self.up(0, rank).wait_send())
        pl.when(self.has_below)(lambda: self.down(0, rank).wait_send())
        for j in range(1, self.length):
            pl.when((z >= j) & self.has_above)(lambda: self.up(j, rank).wait_send())
            pl.when((z + j < self.length) & self.has_below)(lambda: self.down(j, rank).wait_send())


class LineSum:
    def __init__(self, line, x, pre, acc, up_in, down_in, sems):
        self.line, self.x, self.pre, self.acc = line, x, pre, acc
        self.up_in, self.down_in, self.sems = up_in, down_in, sems

    def share(self, k):
        line = self.line
        src = self.x.at[2 * k + 1 - line.core]
        return remote(src, self.pre.at[k], self.sems[0].at[k], self.sems[1].at[k], seq=line.beside)

    def up(self, k):
        sems = self.sems[2].at[k], self.sems[3].at[k]
        return remote(self.acc.at[k], self.up_in.at[k], *sems, seq=self.line.above)

    def down(self, k):
        sems = self.sems[4].at[k], self.sems[5].at[k]
        return remote(self.acc.at[k], self.down_in.at[k], *sems, seq=self.line.below)

    def pair(self, m):
        return self.line.length - 1 - m, m

    def trade(self):
        n = self.line.length
        for m in range((n + 1) // 2):
            for k in sorted(set(self.pair(m))):
                self.share(k).start()

    def merge(self, k):
        self.share(k).wait_recv()
        own = self.x[2 * k + self.line.core].astype(F32)
        self.acc[k] = (own + self.pre[k].astype(F32)).astype(BF)

    def begin(self, m):
        n, z = self.line.length, self.line.z
        far, near = self.pair(m)
        if m < (n + 1) // 2:
            for k in sorted({far, near}):
                self.merge(k)
        if m < n - 1:
            pl.when(z == 0)(lambda: self.up(far).start())
            pl.when(z == n - 1)(lambda: self.down(near).start())

    def add(self, k, more):
        self.acc[k] = (self.acc[k].astype(F32) + more[k].astype(F32)).astype(BF)

    def advance(self, t):
        z, n = self.line.z, self.line.length
        far, near = n - 1 + z - t, t - n + 1 + z

        @pl.when((z >= 1) & (z <= t))
        def _():
            self.up(far).wait_recv()
            self.add(far, self.up_in)
            self.up(far).start()

        @pl.when((z <= n - 2) & (z >= n - 1 - t))
        def _():
            self.down(near).wait_recv()
            self.add(near, self.down_in)
            self.down(near).start()

    def total(self):
        z = self.line.z

        @pl.when(z > 0)
        def _():
            self.up(z).wait_recv()
            self.add(z, self.up_in)

        @pl.when(z < self.line.length - 1)
        def _():
            self.down(z).wait_recv()
            self.add(z, self.down_in)

    def finish(self):
        for k in range(self.line.length):
            self.share(k).wait_send()
            pl.when(k > self.line.z)(lambda: self.up(k).wait_send())
            pl.when(k < self.line.z)(lambda: self.down(k).wait_send())


class StagedSum(LineSum):
    def __init__(self, stage, load, *args):
        super().__init__(*args)
        self.stage, self.load = stage, load

    def fetch(self, slot, src):
        return pltpu.make_async_copy(src, self.stage.at[slot], self.load.at[slot])

    def merge(self, k):
        self.share(k).wait_recv()
        own = self.fetch(0, self.x.at[2 * k + self.line.core])
        other = self.fetch(1, self.pre.at[k])
        own.start()
        other.start()
        own.wait()
        other.wait()
        self.acc[k] = (self.stage[0].astype(F32) + self.stage[1].astype(F32)).astype(BF)

    def add(self, k, more):
        came = self.fetch(0, more.at[k])
        came.start()
        came.wait()
        self.acc[k] = (self.acc[k].astype(F32) + self.stage[0].astype(F32)).astype(BF)


class MixedSum(StagedSum):
    def merge(self, k):
        self.share(k).wait_recv()
        other = self.fetch(1, self.pre.at[k])
        other.start()
        other.wait()
        own = self.x[2 * k + self.line.core].astype(F32)
        self.acc[k] = (own + self.stage[1].astype(F32)).astype(BF)


def line_sems(parts):
    return [pltpu.SemaphoreType.DMA((parts // 2,))] * 6


def transfers(size):
    return 6 if size == 4 else size - 1


def scatter_shapes(size, rows, width):
    half = rows // 2
    slots = (2, half, width) if size == 4 else (size - 1, rows, width)
    return [
        pltpu.VMEM((size - 1, rows, width), BF),
        pltpu.VMEM(slots, BF),
        pltpu.VMEM((2, half, width), BF),
        pltpu.VMEM((2, half, width), BF),
        pltpu.VMEM((2, half, width), BF),
        pltpu.SemaphoreType.DMA((transfers(size),)),
        pltpu.SemaphoreType.DMA((transfers(size),)),
    ]


def each_step(size, body):
    def one(step, carry):
        body(step, lambda k: pl.when(step == k))
        return carry

    lax.fori_loop(0, size, one, 0)


class ForwardRefs(NamedTuple):
    tokens: Any
    edge_tok: Any
    grad: Any
    gains: Any
    table: Any
    qkv_piece: Any
    gu_piece: Any
    out_map: Any
    down_map: Any
    gated_hbm: Any
    qkv_hbm: Any
    edge: Any
    qkv_map_hbm: Any
    middle: Any
    heads: Any
    grads_hbm: Any
    norm_hbm: Any
    hidden_hbm: Any
    gu_grad_hbm: Any
    gu_map_hbm: Any
    gains_all: Any
    table_all: Any
    part: Any
    first: Any
    over: Any
    joined: Any
    last: Any
    all: Any
    grads: Any
    qkv: Any
    qkv_map: Any
    gu_map: Any
    tail: Any
    own: Any
    grad_hidden: Any
    hidden: Any
    gu_grad: Any
    s_send: Any
    s_recv: Any
    a_send: Any
    a_recv: Any
    g_send: Any
    g_recv: Any
    c_send: Any
    c_recv: Any
    m_send: Any
    m_recv: Any
    halo_send: Any
    halo_recv: Any
    loads: Any
    stores: Any
    hidden_store: Any
    gu_store: Any


def forward_kernel(size, parts, count, *refs):
    named = len(ForwardRefs._fields)
    r, sems = ForwardRefs(*refs[:named]), refs[named:]
    rank = lax.axis_index("seq")
    rows = r.tokens.shape[0]
    half = rows // 2
    local = r.out_map.shape[0]
    inner = r.down_map.shape[0]
    slot = rank * rows
    group = Group(size)
    me = group.me
    line_q, line_u = Line(parts, sems[:6]), Line(parts, sems[6:])

    barrier = pltpu.get_barrier_semaphore()
    greet_group(barrier, size)
    known = line_q.greet(barrier)

    def greet(peer):
        pl.semaphore_signal(barrier, inc=1, device_id={"seq": peer}, device_id_type=MESH_ID)

    pl.when(line_q.has_above & (line_q.core == 1))(lambda: greet(rank + 1))
    pl.when(line_q.has_below & (line_q.core == 0))(lambda: greet(rank - 1))
    n, z = line_q.length, line_q.z
    known = known + (2 * n - 2 - z) // n * line_q.core + (z + n - 1) // n * (1 - line_q.core)
    own_pieces = [
        pltpu.make_async_copy(src.at[me], dst.at[me, rank], r.loads.at[k])
        for k, (src, dst) in enumerate(
            ((r.qkv_piece, r.qkv_map), (r.gu_piece, r.gu_map))
        )
    ]
    for copy in own_pieces:
        copy.start()
    r.gains_all[me] = r.gains[...]
    r.table_all[me] = r.table[...]
    r.grads[me] = r.grad[...]
    pl.semaphore_wait(barrier, size - 1 + known)

    def swap(k, step):
        peer = lax.rem(me + step, size)
        src, dst = (
            lambda: (r.gains_all.at[me], r.gains_all.at[me]),
            lambda: (r.table_all.at[me], r.table_all.at[me]),
            lambda: (r.qkv_piece.at[peer], r.qkv_map.at[me, rank]),
            lambda: (r.gu_piece.at[peer], r.gu_map.at[me, rank]),
        )[k]()
        return remote(src, dst, r.m_send.at[k, step - 1], r.m_recv.at[k, step - 1], fsdp=peer)

    others = range(1, size)
    for k in range(4):
        for step in others:
            swap(k, step).start()
    for k in range(2):
        for step in others:
            swap(k, step).wait_recv()

    gains = jnp.concatenate([r.gains_all[f] for f in range(size)], 1).astype(F32)
    own_table = r.table_all[me]
    slots = slot + lax.broadcasted_iota(jnp.int32, (rows, 1), 0)
    length = lambda j: own_table[0:1, j : j + 1]
    start = lambda j: own_table[1:2, j : j + 1]
    segment = segment_of(slots, count, length, start)
    same_one = (segment == segment_of(slots - 1, count, length, start)).astype(F32)
    same_two = (segment == segment_of(slots - 2, count, length, start)).astype(F32)
    tokens = r.tokens[...].astype(F32)
    edge = r.edge_tok[...].astype(F32)

    def norm(a):
        return a * lax.rsqrt(jnp.mean(a * a, axis=1, keepdims=True) + EPS) * gains[0:1]

    normed, edge = norm(tokens), norm(edge)
    row = lax.broadcasted_iota(jnp.int32, (rows, 1), 0)
    back_one = jnp.where(row == 0, edge[1:2], pltpu.roll(normed, 1, 0))
    back_two = jnp.where(
        row == 0, edge[0:1], jnp.where(row == 1, edge[1:2], pltpu.roll(normed, 2, 0))
    )
    mixed = (
        normed * gains[2:3]
        + same_one * back_one * gains[3:4]
        + same_two * back_two * gains[4:5]
    )
    all_ref = r.all
    all_ref[me] = (mixed * normed).astype(BF)
    gather = Gather(group, all_ref, r.a_send, r.a_recv)
    gather.start_half(0)
    gather.start_half(1)

    own_pieces[0].wait()
    for step in others:
        swap(2, step).wait_recv()
    line_q.gather(lambda owner: r.qkv_map.at[:, owner])
    line_u.view = lambda owner: r.gu_map.at[:, owner]
    gather.relay()
    grads = Gather(group, r.grads, r.c_send, r.c_recv)
    grads.start_half(0)
    grads.start_half(1)
    own_pieces[1].wait()
    for step in others:
        swap(3, step).wait_recv()
    line_u.side(z, rank).start()
    pl.when(z == 0)(line_u.own_up)
    pl.when(z == n - 1)(line_u.own_down)
    for j in range(1, n):
        line_q.relay(j)
        line_q.close(j)
        pl.when(z == j)(line_u.own_up)
        pl.when(z == n - 1 - j)(line_u.own_down)
    for step in others:
        gather.ready(step)
    grads.relay()
    line_q.gathered()
    keeps = [
        pltpu.make_async_copy(all_ref, r.gated_hbm, r.stores.at[size]),
        pltpu.make_async_copy(r.qkv_map, r.qkv_map_hbm, r.stores.at[size + 1]),
    ]
    for keep in keeps:
        keep.start()

    weights = r.qkv_map[...].reshape(-1, r.qkv_map.shape[3])

    def halo(step):
        g = group.to_own(step)
        sem = r.halo_send.at[step], r.halo_recv.at[step]
        return remote(r.tail.at[g], r.edge.at[g], *sem, seq=rank + 1)

    def project(step, is_step):
        g = group.to_own(step)
        out = dot(all_ref[g], weights).astype(BF)
        r.qkv[g] = out
        r.tail[g] = out[rows - WINDOW :, local:]
        pl.when(rank < parts - 1)(lambda: halo(step).start())

    each_step(size, project)

    @pl.when(rank == 0)
    def _():
        r.edge[...] = jnp.zeros_like(r.edge)

    keeps.append(pltpu.make_async_copy(r.qkv, r.qkv_hbm, r.stores.at[size + 2]))
    keeps[2].start()
    line_u.relay(1)
    gather.finish()
    keeps[0].wait()

    scatter = Scatter(
        group, r.part, r.first, r.over, r.joined, r.last, r.s_send, r.s_recv
    )
    head_of = lane_head(local)

    def mix(step, is_step):
        g = group.to_own(step)
        pl.when(rank > 0)(lambda: halo(step).wait_recv())
        own, edge, table = r.qkv[g], r.edge[g], r.table_all[g]
        queries = own[:, :local]
        keys = jnp.concatenate([edge[:, :local], own[:, local : 2 * local]], 0)
        values = jnp.concatenate([edge[:, local:], own[:, 2 * local :]], 0)
        outs = []
        for block in range(rows // BLOCK):
            mask = masks_of(
                slot,
                block,
                count,
                lambda j: table[0:1, j : j + 1],
                lambda j: table[1:2, j : j + 1],
            )
            low = block * BLOCK
            query = queries[low : low + BLOCK]
            key = keys[low : low + BLOCK + WINDOW]
            value = values[low : low + BLOCK + WINDOW]
            out = jnp.zeros((BLOCK, local), F32)
            for head in range(local // HEAD_DIM):
                mine = head_of == head
                soft = soft_of(jnp.where(mine, query, jnp.zeros_like(query)), key, mask)
                out = jnp.where(mine, dot(soft.astype(BF), value), out)
            outs.append(out.astype(BF))
        heads = jnp.concatenate(outs, 0)
        r.heads[g] = heads
        branch = dot(heads, r.out_map[...])
        is_step(size - 1)(lambda: r.own.__setitem__(..., branch))
        pl.when(step < size - 1)(lambda: r.part.__setitem__(step, branch.astype(BF)))
        for k in range(size - 1):
            is_step(k)(functools.partial(scatter.made, k))

    each_step(size, mix)
    scatter.join()
    for j in range(2, n):
        line_u.relay(j)
    gather = Gather(group, all_ref, r.g_send, r.g_recv)
    for h in range(2):
        span = slice(h * half, (h + 1) * half)
        total = r.own[span, :] + scatter.total(h)
        middle = r.tokens[span, :].astype(F32) + total
        r.middle[span, :] = middle
        scale = lax.rsqrt(jnp.mean(middle * middle, axis=1, keepdims=True) + EPS)
        all_ref[me, span] = (middle * scale * gains[1:2]).astype(BF)
        gather.start_half(h)
    gather.relay()

    def grad_of(step, is_step):
        g = group.from_own(step)
        for k in others:
            is_step(k)(functools.partial(grads.ready, k))
        r.grad_hidden[g] = dot_trans(r.grads[g], r.down_map[...])

    each_step(size, grad_of)
    for j in range(1, n):
        line_u.close(j)
    line_u.gathered()
    keeps.append(pltpu.make_async_copy(r.gu_map, r.gu_map_hbm, r.stores.at[size + 3]))
    keeps[3].start()

    def out_copies(step):
        g, two = group.from_own(step), lax.rem(step, 2)
        return (
            pltpu.make_async_copy(
                r.hidden.at[two], r.hidden_hbm.at[g], r.hidden_store.at[two]
            ),
            pltpu.make_async_copy(
                r.gu_grad.at[two], r.gu_grad_hbm.at[g], r.gu_store.at[two]
            ),
        )

    def norm_copy(g):
        return pltpu.make_async_copy(all_ref.at[g], r.norm_hbm.at[g], r.stores.at[g])

    def feed(step, is_step):
        g, two = group.from_own(step), lax.rem(step, 2)
        for k in others:
            is_step(k)(functools.partial(gather.ready, k))

        @pl.when(step >= 2)
        def _():
            for copy in out_copies(step - 2):
                copy.wait()

        norm_copy(g).start()
        weights = r.gu_map[...].reshape(-1, r.gu_map.shape[3])
        acts = dot(all_ref[g], weights)
        gate, up = acts[:, :inner], acts[:, inner:]
        sigma = jax.nn.sigmoid(gate)
        silu = gate * sigma
        r.hidden[two] = (silu * up).astype(BF)
        grad_hidden = r.grad_hidden[g]
        grad_gate = grad_hidden * up * sigma * (1.0 + gate * (1.0 - sigma))
        r.gu_grad[two] = jnp.concatenate([grad_gate, grad_hidden * silu], 1).astype(BF)
        for copy in out_copies(step):
            copy.start()

    each_step(size, feed)
    keeps.append(pltpu.make_async_copy(r.grads, r.grads_hbm, r.stores.at[size + 4]))
    keeps[4].start()
    for k in range(4):
        for step in others:
            swap(k, step).wait_send()
    scatter.finish()
    gather.finish()
    grads.finish()
    line_q.finish()
    line_u.finish()

    @pl.when(rank < parts - 1)
    def _():
        for step in range(size):
            halo(step).wait_send()

    for keep in keeps[1:]:
        keep.wait()
    for g in range(size):
        norm_copy(g).wait()
    for step in (size - 2, size - 1):
        for copy in out_copies(step):
            copy.wait()


def forward_part(ident, count, tokens, edge, grad, gains, table, qkv_piece, gu_piece, out_weight, down_weight):
    size, parts = lax.axis_size("fsdp"), lax.axis_size("seq")
    rows, width = tokens.shape
    local, inner = out_weight.shape[0], down_weight.shape[0]
    piece, cols = gu_piece.shape[1:]
    vmem = pl.BlockSpec(memory_space=pltpu.VMEM)
    hbm = pl.BlockSpec(memory_space=pl.ANY)
    shape = lambda w: (size, rows, w)
    low = lambda s: jax.ShapeDtypeStruct(s, BF)
    maps = [(size, parts, piece, 3 * local), (size, parts, piece, cols)]
    dma = lambda *s: pltpu.SemaphoreType.DMA(s)
    hop = transfers(size)
    scratch = scatter_shapes(size, rows, width)
    return pl.pallas_call(
        functools.partial(forward_kernel, size, parts, count),
        out_shape=[
            low(shape(width)),
            low(shape(3 * local)),
            low((size, WINDOW, 2 * local)),
            low(maps[0]),
            jax.ShapeDtypeStruct((rows, width), F32),
            low(shape(local)),
            low(shape(width)),
            low(shape(width)),
            low(shape(inner)),
            low(shape(cols)),
            low(maps[1]),
            low((size,) + gains.shape),
            jax.ShapeDtypeStruct((size,) + table.shape, jnp.int32),
        ],
        in_specs=[vmem] * 5 + [hbm, hbm, vmem, vmem],
        out_specs=[hbm, hbm, vmem, hbm, vmem, vmem, hbm, hbm, hbm, hbm, hbm, vmem, vmem],
        scratch_shapes=scratch[:-2]
        + [
            pltpu.VMEM(shape(width), BF),
            pltpu.VMEM(shape(width), BF),
            pltpu.VMEM(shape(3 * local), BF),
            pltpu.VMEM(maps[0], BF),
            pltpu.VMEM(maps[1], BF),
            pltpu.VMEM((size, WINDOW, 2 * local), BF),
            pltpu.VMEM((rows, width), F32),
            pltpu.VMEM(shape(inner), F32),
            pltpu.VMEM((2, rows, inner), BF),
            pltpu.VMEM((2, rows, cols), BF),
        ]
        + [dma(hop)] * 8
        + [dma(4, size - 1)] * 2
        + [dma(size)] * 2
        + [dma(2), dma(size + 5), dma(2), dma(2)]
        + line_sems(parts)
        + line_sems(parts),
        compiler_params=pltpu.CompilerParams(
            collective_id=ident, has_side_effects=True, vmem_limit_bytes=67_000_000
        ),
        cost_estimate=pl.CostEstimate(
            flops=2 * size * rows * width * (4 * local + 3 * inner),
            bytes_accessed=500_000_000,
            transcendentals=0,
        ),
        name="forward_part",
    )(tokens, edge, grad, gains, table, qkv_piece, gu_piece, out_weight, down_weight)


def heads_back(group, slot, count, lens_ref, starts_ref, own, edge, grad):
    rows, local = own.shape[0], own.shape[1] // 3
    head_of = lane_head(local)
    queries = own[:, :local]
    keys = jnp.concatenate([edge[:, :local], own[:, local : 2 * local]], 0)
    values = jnp.concatenate([edge[:, local:], own[:, 2 * local :]], 0)
    dqs, dks, dvs = [], [], []
    for block in range(rows // BLOCK):
        mask = masks_of(
            slot, block, count, lambda j: lens_ref[group, j], lambda j: starts_ref[group, j]
        )
        low = block * BLOCK
        span = slice(low, low + BLOCK + WINDOW)
        query, grads = queries[low : low + BLOCK], grad[low : low + BLOCK]
        key, value = keys[span], values[span]
        dq = jnp.zeros((BLOCK, local), F32)
        dk = jnp.zeros((BLOCK + WINDOW, local), F32)
        dv = jnp.zeros((BLOCK + WINDOW, local), F32)
        for head in range(local // HEAD_DIM):
            mine = head_of == head
            own_q = jnp.where(mine, query, jnp.zeros_like(query))
            own_g = jnp.where(mine, grads, jnp.zeros_like(grads))
            soft = soft_of(own_q, key, mask)
            grad_soft = dot_trans(own_g, value)
            total = jnp.sum(grad_soft * soft, axis=1, keepdims=True)
            grad_scores = (soft * (grad_soft - total)).astype(BF)
            dq = jnp.where(mine, dot(grad_scores, key), dq)
            dk = dk + dot_rows(grad_scores, own_q)
            dv = dv + dot_rows(soft.astype(BF), own_g)
        dqs.append(dq * SCALE)
        dks.append(dk * SCALE)
        dvs.append(dv)

    def joined(pieces):
        out = [pieces[0][:BLOCK]]
        for left, right in zip(pieces, pieces[1:]):
            out.append(left[BLOCK:] + right[:WINDOW])
            out.append(right[WINDOW:BLOCK])
        out.append(pieces[-1][BLOCK:])
        return jnp.concatenate(out, 0)

    return jnp.concatenate(dqs, 0), joined(dks), joined(dvs)


class BackRefs(NamedTuple):
    lens: Any
    starts: Any
    grad_gu_hbm: Any
    gu_map_hbm: Any
    middle: Any
    grad: Any
    gain: Any
    out_map: Any
    edge: Any
    qkv: Any
    qkv_map_hbm: Any
    gu_x: Any
    down_x: Any
    grad_middle: Any
    norm: Any
    all: Any
    dqkv: Any
    own: Any
    gu_slots: Any
    down_every: Any
    gu_pre: Any
    gu_up: Any
    gu_down: Any
    down_pre: Any
    down_up: Any
    down_down: Any
    part: Any
    first: Any
    over: Any
    joined: Any
    last: Any
    s_send: Any
    s_recv: Any
    t_send: Any
    t_recv: Any
    g_send: Any
    g_recv: Any
    grad_gu: Any
    gu_map: Any
    qkv_map: Any
    dedge: Any
    back: Any
    tail: Any
    h_send: Any
    h_recv: Any
    loads: Any
    gu_acc: Any
    gu_stage: Any
    gu_load: Any
    down_acc: Any
    down_stage: Any
    down_load: Any
    m_send: Any
    m_recv: Any


def back_kernel(size, parts, count, *refs):
    named = len(BackRefs._fields)
    r, sems = BackRefs(*refs[:named]), refs[named:]
    line = Line(parts, sems[:6])
    gu_sum = StagedSum(
        r.gu_stage, r.gu_load, line, r.gu_x, r.gu_pre, r.gu_acc, r.gu_up, r.gu_down, sems[6:12]
    )
    down_sum = StagedSum(
        r.down_stage,
        r.down_load,
        line,
        r.down_x,
        r.down_pre,
        r.down_acc,
        r.down_up,
        r.down_down,
        sems[12:],
    )
    rows = r.middle.shape[0]
    local = r.out_map.shape[0]
    rank = lax.axis_index("seq")
    slot = rank * rows
    group = Group(size)
    barrier = pltpu.get_barrier_semaphore()
    greet_group(barrier, size)

    def greet(peer):
        pl.semaphore_signal(barrier, inc=1, device_id={"seq": peer}, device_id_type=MESH_ID)

    known = line.greet(barrier)
    pl.when(line.has_above & (line.core == 1))(lambda: greet(rank + 1))
    pl.when(line.has_below & (line.core == 0))(lambda: greet(rank - 1))
    n, z = line.length, line.z
    known = known + (2 * n - 2 - z) // n * line.core + (z + n - 1) // n * (1 - line.core)
    fetches = [
        pltpu.make_async_copy(src, dst, r.loads.at[k])
        for k, (src, dst) in enumerate(
            ((r.grad_gu_hbm, r.grad_gu), (r.gu_map_hbm, r.gu_map), (r.qkv_map_hbm, r.qkv_map))
        )
    ]
    for fetch in fetches:
        fetch.start()
    pl.semaphore_wait(barrier, size - 1 + known)
    down_sum.trade()
    gu_sum.trade()
    for m in range(n):
        down_sum.begin(m)
    scatter = Scatter(
        group, r.part, r.first, r.over, r.joined, r.last, r.s_send, r.s_recv
    )
    gather = Gather(group, r.all, r.g_send, r.g_recv)
    fetches[0].wait()
    fetches[1].wait()

    def step_two(step, is_step):
        partial = dot_trans(r.grad_gu[group.to_own(step)], r.gu_map[...])
        is_step(size - 1)(lambda: r.own.__setitem__(..., partial))
        pl.when(step < size - 1)(lambda: r.part.__setitem__(step, partial.astype(BF)))
        for k in range(size - 1):
            is_step(k)(functools.partial(scatter.made, k))

    each_step(size, step_two)
    scatter.join()
    gu_sum.begin(0)
    down_sum.advance(1)
    half = rows // 2
    norm_sum = jnp.zeros((1, r.middle.shape[1]), F32)
    for h in range(2):
        span = slice(h * half, (h + 1) * half)
        grad = r.own[span, :] + scatter.total(h)
        middle = r.middle[span, :]
        scale = lax.rsqrt(jnp.mean(middle * middle, axis=1, keepdims=True) + EPS)
        unit = middle * scale
        scaled = grad * r.gain[...]
        norm_sum = norm_sum + jnp.sum(grad * unit, axis=0, keepdims=True)
        grad_out = r.grad[span, :].astype(F32)
        grad_middle = grad_out + scale * (
            scaled - unit * jnp.mean(scaled * unit, axis=1, keepdims=True)
        )
        r.grad_middle[span, :] = grad_middle
        r.all[group.me, span] = grad_middle.astype(BF)
        gather.start_half(h)
    r.norm[...] = norm_sum
    own_down = pltpu.make_async_copy(r.down_acc.at[z], r.down_every.at[rank], r.down_load.at[0])

    def halo(step):
        g = group.from_own(step)
        sems = r.h_send.at[step], r.h_recv.at[step]
        return remote(r.dedge.at[g], r.back.at[g], *sems, seq=rank - 1)

    def step_heads(step, is_step):
        g = group.from_own(step)

        @is_step(1)
        def _():
            gather.relay()
            for t in range(2, n - 1):
                down_sum.advance(t)

        @is_step(2)
        def _():
            down_sum.total()
            own_down.start()
            own_down.wait()
            for m in range(1, n):
                gu_sum.begin(m)
            line.gather(lambda owner: r.down_every.at[owner])

        is_step(size - 1)(lambda: gu_sum.advance(1))

        for k in range(1, size):
            is_step(k)(functools.partial(gather.ready, k))
        grad = dot_trans(r.all[g], r.out_map[...]).astype(BF)
        dq, dk, dv = heads_back(
            g, slot, count, r.lens, r.starts, r.qkv[g], r.edge[g], grad
        )
        r.dedge[g] = jnp.concatenate([dk[:WINDOW], dv[:WINDOW]], 1).astype(BF)
        full = jnp.concatenate([dq, dk[WINDOW:], dv[WINDOW:]], 1)
        r.dqkv[g] = full.astype(BF)
        r.tail[g] = full[rows - WINDOW :]
        pl.when(rank > 0)(lambda: halo(step).start())

    each_step(size, step_heads)
    scatter.finish()
    fetches[2].wait()

    @pl.when(rank == parts - 1)
    def _():
        r.back[...] = jnp.zeros_like(r.back)

    @pl.when(rank < parts - 1)
    def _():
        for step in range(size):
            halo(step).wait_recv()

    scatter = Scatter(
        group, r.part, r.first, r.over, r.joined, r.last, r.t_send, r.t_recv
    )

    def step_one(step, is_step):
        g = group.to_own(step)
        back = r.back[g].astype(F32)
        wide = jnp.concatenate([jnp.zeros((WINDOW, local), F32), back], 1)
        r.dqkv[g, pl.ds(rows - WINDOW, WINDOW)] = (r.tail[g] + wide).astype(BF)
        partial = dot_trans(r.dqkv[g], r.qkv_map[...])
        is_step(size - 1)(lambda: r.own.__setitem__(..., partial))
        pl.when(step < size - 1)(lambda: r.part.__setitem__(step, partial.astype(BF)))
        for k in range(size - 1):
            is_step(k)(functools.partial(scatter.made, k))

    each_step(size, step_one)
    line.relay(1)
    scatter.join()
    for t in range(2, n - 1):
        gu_sum.advance(t)
        line.relay(t)
    line.relay(n - 1)
    for h in range(2):
        span = slice(h * half, (h + 1) * half)
        r.own[span, :] = r.own[span, :] + scatter.total(h)
    gu_sum.total()

    def swap(step):
        peer = lax.rem(group.me + step, size)
        sems = r.m_send.at[step - 1], r.m_recv.at[step - 1]
        return remote(r.gu_acc.at[z, peer], r.gu_slots.at[group.me], *sems, fsdp=peer)

    for step in range(1, size):
        swap(step).start()
    own_slot = pltpu.make_async_copy(
        r.gu_acc.at[z, group.me], r.gu_slots.at[group.me], r.gu_load.at[0]
    )
    own_slot.start()
    for j in range(1, n):
        line.close(j)
    line.gathered()
    for step in range(1, size):
        swap(step).wait()
    scatter.finish()
    gather.finish()
    down_sum.finish()
    gu_sum.finish()
    line.finish()
    own_slot.wait()

    @pl.when(rank > 0)
    def _():
        for step in range(size):
            halo(step).wait_send()


def back_part(
    ident, lens, starts, grad_gu, gu_map, middle, grad, gain, out_weight, edge, qkv, qkv_map, gu_x, down_x
):
    size, parts = lax.axis_size("fsdp"), lax.axis_size("seq")
    rows, width = middle.shape
    local = out_weight.shape[0]
    n = parts // 2
    vmem = pl.BlockSpec(memory_space=pltpu.VMEM)
    smem = pl.BlockSpec(memory_space=pltpu.SMEM)
    hbm = pl.BlockSpec(memory_space=pl.ANY)
    dma = lambda *s: pltpu.SemaphoreType.DMA(s)
    low = lambda *s: jax.ShapeDtypeStruct(s, BF)
    sems = [dma(transfers(size))] * 2
    gu, down = gu_x.shape[1:], down_x.shape[1:]
    outs = pl.pallas_call(
        functools.partial(back_kernel, size, parts, lens.shape[1]),
        out_shape=[
            jax.ShapeDtypeStruct((rows, width), F32),
            jax.ShapeDtypeStruct((1, width), F32),
            low(size, rows, width),
            low(*qkv.shape),
            jax.ShapeDtypeStruct((rows, width), F32),
            low(*gu),
            low(parts, *down),
        ]
        + [low(n, *gu)] * 3
        + [low(n, *down)] * 3,
        in_specs=[smem, smem, hbm, hbm] + [vmem] * 6 + [hbm] * 3,
        out_specs=[vmem] * 5 + [hbm] * 8,
        scratch_shapes=scatter_shapes(size, rows, width)
        + sems
        + sems
        + [
            pltpu.VMEM(grad_gu.shape, BF),
            pltpu.VMEM(gu_map.shape, BF),
            pltpu.VMEM(qkv_map.shape, BF),
            pltpu.VMEM((size, WINDOW, 2 * local), BF),
            pltpu.VMEM((size, WINDOW, 2 * local), BF),
            pltpu.VMEM((size, WINDOW, 3 * local), F32),
            dma(size),
            dma(size),
            dma(3),
            pltpu.VMEM((n,) + gu, BF),
            pltpu.VMEM((2,) + gu, BF),
            dma(2),
            pltpu.VMEM((n,) + down, BF),
            pltpu.VMEM((2,) + down, BF),
            dma(2),
            dma(size - 1),
            dma(size - 1),
        ]
        + line_sems(parts) * 3,
        compiler_params=pltpu.CompilerParams(
            collective_id=ident, has_side_effects=True, vmem_limit_bytes=67_000_000
        ),
        cost_estimate=pl.CostEstimate(
            flops=2 * size * rows * (gu_map.size + qkv_map.size + width * local),
            bytes_accessed=400_000_000,
            transcendentals=0,
        ),
        name="back_part",
    )(lens, starts, grad_gu, gu_map, middle, grad, gain, out_weight, edge, qkv, qkv_map, gu_x, down_x)
    return outs[:7]


class CloseRefs(NamedTuple):
    gated_hbm: Any
    dqkv_hbm: Any
    heads_hbm: Any
    gb_hbm: Any
    gu_slots: Any
    terms: Any
    hidden_hbm: Any
    down_hbm: Any
    every_hbm: Any
    gu_every: Any
    feed: Any
    terms_out: Any
    pre: Any
    up_in: Any
    down_in: Any
    part: Any
    first: Any
    over: Any
    joined: Any
    last: Any
    x: Any
    acc: Any
    stage: Any
    stage_load: Any
    every: Any
    slots: Any
    gu_own: Any
    gated: Any
    dqkv: Any
    heads: Any
    gb: Any
    hidden: Any
    down_map: Any
    terms_in: Any
    terms_all: Any
    s_send: Any
    s_recv: Any
    m_send: Any
    m_recv: Any
    t_send: Any
    t_recv: Any
    loads: Any


def close_kernel(size, parts, made, *refs):
    named = len(CloseRefs._fields)
    r, sems = CloseRefs(*refs[:named]), refs[named:]
    rank = lax.axis_index("seq")
    group = Group(size)
    me = group.me
    line_u, line_q = Line(parts, sems[:6]), Line(parts, sems[6:12])
    n, z = line_q.length, line_q.z
    sums = MixedSum(
        r.stage, r.stage_load, line_q, r.x, r.pre, r.acc, r.up_in, r.down_in, sems[12:]
    )
    rows = r.feed.shape[0]
    half = rows // 2
    barrier = pltpu.get_barrier_semaphore()
    greet_group(barrier, size)
    for step in range(1, parts):
        peer = lax.rem(rank + step, parts)
        pl.semaphore_signal(barrier, inc=1, device_id={"seq": peer}, device_id_type=MESH_ID)
    moves = [
        (r.gu_slots, r.gu_own),
        (r.hidden_hbm, r.hidden),
        (r.down_hbm, r.down_map),
    ]
    if made:
        moves += [
            (r.gated_hbm, r.gated),
            (r.dqkv_hbm, r.dqkv),
            (r.heads_hbm, r.heads),
            (r.gb_hbm, r.gb),
        ]
    else:
        moves += [(r.gated_hbm, r.x)]
    fetches = [
        pltpu.make_async_copy(src, dst, r.loads.at[k]) for k, (src, dst) in enumerate(moves)
    ]
    for k in [0] + list(range(3, len(moves))) + [1, 2]:
        fetches[k].start()
    r.terms_in[me] = r.terms[me]
    own_slots = pltpu.make_async_copy(r.gu_own, r.gu_every.at[rank], r.loads.at[0])
    fetches[0].wait()
    own_slots.start()
    own_slots.wait()
    pl.semaphore_wait(barrier, size + parts - 2)
    line_u.gather(lambda owner: r.gu_every.at[owner])

    def swap(k, step):
        peer = lax.rem(me + step, size)
        src, dst = (
            lambda: (r.terms.at[peer], r.terms_in.at[me]),
            lambda: (r.acc.at[z, peer], r.slots.at[me]),
        )[k]()
        return remote(src, dst, r.m_send.at[k, step - 1], r.m_recv.at[k, step - 1], fsdp=peer)

    others = range(1, size)
    for step in others:
        swap(0, step).start()

    scatter = Scatter(
        group, r.part, r.first, r.over, r.joined, r.last, r.s_send, r.s_recv
    )

    def down(step, is_step):
        partial = dot(r.hidden[group.to_own(step)], r.down_map[...])
        is_step(size - 1)(lambda: r.feed.__setitem__(..., partial))
        pl.when(step < size - 1)(lambda: r.part.__setitem__(step, partial.astype(BF)))
        for k in range(size - 1):
            is_step(k)(functools.partial(scatter.made, k))

    for fetch in fetches[3:]:
        fetch.wait()
    if made:
        span = r.gated.shape[1] // (size // 2)
        for h in range(size // 2):
            lanes = slice(h * span, (h + 1) * span)
            pack_pair(
                r.x, h, r.gated[:, lanes], r.dqkv[...], r.heads[...], r.gb[:, lanes]
            )
    sums.trade()
    line_u.relay(1)
    fetches[1].wait()
    fetches[2].wait()
    for m in range(n):
        sums.begin(m)
    each_step(size, down)

    for step in others:
        swap(0, step).wait_recv()
    small = r.terms_in[0]
    for f in others:
        small = small + r.terms_in[f]
    r.terms_all[rank] = small

    def spread(step):
        peer = lax.rem(rank + step, parts)
        view = r.terms_all.at[rank]
        return remote(view, view, r.t_send.at[step - 1], r.t_recv.at[step - 1], seq=peer)

    for step in range(1, parts):
        spread(step).start()
    scatter.join()

    for t in range(1, n - 1):
        sums.advance(t)
        line_u.relay(t + 1)
    for h in range(2):
        span = slice(h * half, (h + 1) * half)
        r.feed[span, :] = r.feed[span, :] + scatter.total(h)
    sums.total()
    for step in others:
        swap(1, step).start()
    for j in range(1, n):
        line_u.close(j)
    r.slots[me] = r.acc[z, me]
    for step in others:
        swap(1, step).wait_recv()
    local = r.x.shape[3] // 4
    lane = lax.broadcasted_iota(jnp.int32, (1, 1, 4 * local), 2)
    r.every[rank] = jnp.where(lane < 3 * local, r.slots[...], r.acc[z])
    line_q.gather(lambda owner: r.every.at[owner])
    line_u.gathered()
    for j in range(1, n):
        line_q.relay(j)
    for j in range(1, n):
        line_q.close(j)
    line_q.gathered()
    store = pltpu.make_async_copy(r.every, r.every_hbm, r.loads.at[1])
    store.start()
    for step in range(1, parts):
        spread(step).wait_recv()
    small = r.terms_all[0]
    for k in range(1, parts):
        small = small + r.terms_all[k]
    r.terms_out[...] = small
    for k in range(2):
        for step in others:
            swap(k, step).wait_send()
    for step in range(1, parts):
        spread(step).wait_send()
    scatter.finish()
    sums.finish()
    line_u.finish()
    line_q.finish()
    store.wait()


def close_part(ident, gated, dqkv, heads, gb, gu_slots, terms, hidden, down_weight):
    size, parts = lax.axis_size("fsdp"), lax.axis_size("seq")
    width = gated.shape[1]
    made = packs(size, parts, width)
    piece, cols = width // (size * parts), dqkv.shape[1] + heads.shape[1]
    if not made:
        gated = pack_plain(parts, size, gated, dqkv, heads, gb)
    n = parts // 2
    rows = hidden.shape[1]
    vmem = pl.BlockSpec(memory_space=pltpu.VMEM)
    hbm = pl.BlockSpec(memory_space=pl.ANY)
    dma = lambda *s: pltpu.SemaphoreType.DMA(s)
    gu_shape = (parts,) + gu_slots.shape
    packed = (parts, size, piece, cols)
    scratch = scatter_shapes(size, rows, width)
    low = lambda *s: jax.ShapeDtypeStruct(s, BF)
    copy_of = lambda a: pltpu.VMEM(a.shape if made else (8, 128), BF)
    return pl.pallas_call(
        functools.partial(close_kernel, size, parts, made),
        out_shape=[
            low(*packed),
            low(*gu_shape),
            jax.ShapeDtypeStruct((rows, width), F32),
            jax.ShapeDtypeStruct(terms.shape[1:], F32),
        ]
        + [low(n, size, piece, cols)] * 3,
        in_specs=[hbm] * 5 + [vmem, hbm, hbm],
        out_specs=[hbm, hbm, vmem, vmem, hbm, hbm, hbm],
        scratch_shapes=scratch[:-2]
        + [
            pltpu.VMEM(packed, BF),
            pltpu.VMEM((n, size, piece, cols), BF),
            pltpu.VMEM((2, size, piece, cols), BF),
            dma(2),
            pltpu.VMEM(packed, BF),
            pltpu.VMEM((size, piece, cols), BF),
            pltpu.VMEM(gu_slots.shape, BF),
            copy_of(gated),
            copy_of(dqkv),
            copy_of(heads),
            copy_of(gb),
            pltpu.VMEM(hidden.shape, BF),
            pltpu.VMEM(down_weight.shape, BF),
            pltpu.VMEM(terms.shape, F32),
            pltpu.VMEM((parts,) + terms.shape[1:], F32),
        ]
        + scratch[-2:]
        + [dma(2, size - 1)] * 2
        + [dma(parts - 1)] * 2
        + [dma(7)]
        + line_sems(parts) * 3,
        compiler_params=pltpu.CompilerParams(
            collective_id=ident, has_side_effects=True, vmem_limit_bytes=67_000_000
        ),
        cost_estimate=pl.CostEstimate(
            flops=2 * size * rows * (down_weight.size + width * cols),
            bytes_accessed=500_000_000,
            transcendentals=0,
        ),
        name="close_part",
    )(gated, dqkv, heads, gb, gu_slots, terms, hidden, down_weight)[:4]


def pack_pair(out, pair, x, g, heads=None, gb=None):
    parts, _, piece, _ = out.shape
    rows = parts * piece
    full = dot_rows(x, g)
    side = None if heads is None else dot_rows(heads, gb)
    for k in range(2):
        own = full[k * rows : (k + 1) * rows]
        if side is not None:
            wide = side.shape[1] // 2
            own = jnp.concatenate([own, side[:, k * wide : (k + 1) * wide]], 1)
        out[:, pair * 2 + k] = own.astype(BF).reshape(parts, piece, own.shape[1])


def pack_kernel(x_ref, g_ref, out_ref):
    pack_pair(out_ref, 0, x_ref[...], g_ref[...])


def down_kernel(x_ref, g_ref, out_ref):
    out_ref[...] = dot_rows(x_ref[...], g_ref[...]).astype(BF)


def down_grad(x, g):
    total, inner = x.shape
    half = g.shape[1] // 2
    return pl.pallas_call(
        down_kernel,
        grid=(2,),
        out_shape=jax.ShapeDtypeStruct((inner, 2 * half), BF),
        in_specs=[
            pl.BlockSpec(x.shape, lambda i: (0, 0), pipeline_mode=pl.Buffered(1)),
            pl.BlockSpec((total, half), lambda i: (0, i)),
        ],
        out_specs=pl.BlockSpec((inner, half), lambda i: (0, i)),
        cost_estimate=pl.CostEstimate(
            flops=4 * total * inner * half,
            bytes_accessed=2 * (x.size + g.size) + 4 * inner * half,
            transcendentals=0,
        ),
        name="down_grad",
    )(x, g)


def packs(size, parts, width):
    return width // (size * parts) % 8 == 0 and 2 * width // size % 128 == 0


def pack_plain(parts, size, x, g, heads=None, gb=None):
    width, cols = x.shape[1], g.shape[1]
    piece = width // (size * parts)
    full = dot_rows(x, g).reshape(size, parts, piece, cols)
    if heads is not None:
        side = dot_rows(heads, gb).reshape(parts, piece, size, -1).transpose(2, 0, 1, 3)
        full = jnp.concatenate([full, side], 3)
    return full.transpose(1, 0, 2, 3).astype(BF)


def pack_grads(parts, size, x, g):
    total, width = x.shape
    cols = g.shape[1]
    if not packs(size, parts, width):
        return pack_plain(parts, size, x, g)
    piece = width // (size * parts)
    pair = pl.BlockSpec((total, 2 * width // size), lambda i: (0, i))
    whole = pl.BlockSpec(g.shape, lambda i: (0, 0), pipeline_mode=pl.Buffered(1))
    return pl.pallas_call(
        pack_kernel,
        grid=(size // 2,),
        out_shape=jax.ShapeDtypeStruct((parts, size, piece, cols), BF),
        in_specs=[pair, whole],
        out_specs=pl.BlockSpec((parts, 2, piece, cols), lambda i: (0, i, 0, 0)),
        cost_estimate=pl.CostEstimate(
            flops=2 * total * width * cols,
            bytes_accessed=2 * (x.size + g.size + width * cols),
            transcendentals=0,
        ),
        name="pack_grads",
    )(x, g)


def unpack_kernel(widths, *refs):
    outs = list(refs[len(widths) :])
    for every_ref, wide in zip(refs, widths):
        blocks = [every_ref[0, i].astype(F32) for i in range(every_ref.shape[1])]
        low = 0
        for width in wide:
            outs.pop(0)[...] = jnp.concatenate([b[:, low : low + width] for b in blocks], 1)
            low += width


def unpack_grads(arrays, widths):
    parts, size, piece, _ = arrays[0].shape
    every = [w for wide in widths for w in wide]
    if piece % 8:
        outs = []
        for array, wide in zip(arrays, widths):
            low = 0
            for width in wide:
                block = array[:, :, :, low : low + width].transpose(0, 2, 1, 3)
                outs.append(block.reshape(parts * piece, size * width).astype(F32))
                low += width
        return outs
    return pl.pallas_call(
        functools.partial(unpack_kernel, widths),
        grid=(parts,),
        out_shape=[jax.ShapeDtypeStruct((parts * piece, size * w), F32) for w in every],
        in_specs=[
            pl.BlockSpec((1, size, piece, a.shape[3]), lambda i: (i, 0, 0, 0)) for a in arrays
        ],
        out_specs=[pl.BlockSpec((piece, size * w), lambda i: (i, 0)) for w in every],
        cost_estimate=pl.CostEstimate(
            flops=0, bytes_accessed=6 * sum(a.size for a in arrays), transcendentals=0
        ),
        name="unpack_grads",
    )(*arrays)


def columns_piece(weights, part, parts):
    size = lax.axis_size("fsdp")
    rows = weights[0].shape[0] // parts
    pieces = []
    for weight in weights:
        own = lax.dynamic_slice_in_dim(weight, part * rows, rows, 0)
        pieces.append(own.reshape(rows, size, -1))
    return jnp.concatenate(pieces, 2).transpose(1, 0, 2)


def shards(
    tokens,
    seq_lengths,
    seq_offsets,
    norm1_gain,
    conv_weight,
    query_weight,
    key_weight,
    value_weight,
    out_weight,
    norm2_gain,
    gate_weight,
    up_weight,
    down_weight,
    cotangent,
):
    size = lax.axis_size("fsdp")
    parts = lax.axis_size("seq")
    part = lax.axis_index("seq")
    me = lax.axis_index("fsdp")
    own_tokens = tokens[0]
    rows, width = own_tokens.shape
    slice_width = norm1_gain.shape[0]
    first_slot = part * rows
    count = seq_lengths.shape[1]

    slot_ext = first_slot - 2 + jnp.arange(rows + 2, dtype=jnp.int32)
    segment_ext = segment_of(
        slot_ext, count, lambda j: seq_lengths[0, j], lambda j: seq_offsets[0, j]
    )
    segment_own = segment_ext[2:]
    same_one = (segment_own == segment_ext[1:-1]).astype(F32)[:, None]
    same_two = (segment_own == segment_ext[:-2]).astype(F32)[:, None]
    live_mask = (segment_own >= 0).astype(F32)[:, None]

    gains = jnp.concatenate(
        [
            norm1_gain[None],
            norm2_gain[None],
            conv_weight.T,
            jnp.zeros((3, slice_width), BF),
        ],
        0,
    )
    table = jnp.zeros((8, 128), jnp.int32)
    table = table.at[0, :count].set(seq_lengths[0]).at[1, :count].set(seq_offsets[0])
    qkv_piece = columns_piece((query_weight, key_weight, value_weight), part, parts)
    gu_piece = columns_piece((gate_weight, up_weight), part, parts)
    edge_tokens = shifted(own_tokens[rows - 2 :], "seq", 1)
    grad_down = (cotangent[0].astype(F32) * live_mask).astype(BF)
    (
        gated_all,
        qkv,
        edge,
        qkv_map,
        middle,
        heads_out,
        grad_down_all,
        normed_all,
        hidden,
        grad_gu,
        gu_map,
        gains_all,
        table_all,
    ) = forward_part(
        0,
        count,
        own_tokens,
        jnp.pad(edge_tokens, ((0, 6), (0, 0))),
        grad_down,
        gains,
        table,
        qkv_piece,
        gu_piece,
        out_weight,
        down_weight,
    )
    local = out_weight.shape[0]
    flat = lambda a: a.reshape(-1, a.shape[-1])
    lens_all, starts_all = table_all[:, 0, :count], table_all[:, 1, :count]
    gains_all = gains_all.transpose(1, 0, 2).reshape(8, width)
    norm_one = gains_all[0].astype(F32)
    norm_two = gains_all[1].astype(F32)
    taps = gains_all[2:5].astype(F32)
    qkv_map, gu_map = qkv_map.reshape(width, -1), gu_map.reshape(width, -1)
    grad_down_all = flat(grad_down_all)

    extended = jnp.concatenate([edge_tokens, own_tokens], 0).astype(F32)
    scale_one = lax.rsqrt(jnp.mean(extended * extended, axis=1, keepdims=True) + EPS)
    normed = extended * scale_one * norm_one
    conv_mix = (
        normed[2:] * taps[0]
        + same_one * normed[1:-1] * taps[1]
        + same_two * normed[:-2] * taps[2]
    )

    gu_packed = pack_grads(parts, size, flat(normed_all), flat(grad_gu))
    down_packed = down_grad(flat(hidden), grad_down_all)
    grad_middle, norm2_term, grad_branch_all, dqkv, grad_gated, gu_slots, down_every = back_part(
        4,
        lens_all,
        starts_all,
        grad_gu,
        gu_map,
        middle,
        grad_down,
        norm_two[None],
        out_weight,
        edge,
        qkv,
        qkv_map,
        gu_packed,
        down_packed.reshape(parts, -1, width),
    )
    norm2_term = norm2_term[0]
    down_total = down_every.reshape(-1, width).astype(F32)
    normed_own = normed[2:]
    grad_mix = grad_gated * normed_own
    part_zero = jnp.pad(grad_gated * conv_mix + grad_mix * taps[0], ((2, 0), (0, 0)))
    part_one = jnp.pad(grad_mix * same_one * taps[1], ((1, 1), (0, 0)))
    part_two = jnp.pad(grad_mix * same_two * taps[2], ((0, 2), (0, 0)))
    grad_normed = part_zero + part_one + part_two
    unit_one = extended * scale_one
    grad_unit_one = grad_normed * norm_one
    grad_extended = scale_one * (
        grad_unit_one - unit_one * jnp.mean(grad_unit_one * unit_one, axis=1, keepdims=True)
    )
    edge_back = shifted(grad_extended[:2], "seq", -1)
    tokens_grad = grad_middle + grad_extended[2:] + jnp.pad(edge_back, ((rows - 2, 0), (0, 0)))

    terms = jnp.stack(
        [
            jnp.sum(grad_normed * unit_one, axis=0),
            norm2_term,
            jnp.sum(grad_mix * normed_own, axis=0),
            jnp.sum(grad_mix * same_one * normed[1:-1], axis=0),
            jnp.sum(grad_mix * same_two * normed[:-2], axis=0),
        ]
    )
    terms = jnp.pad(terms, ((0, 3), (0, 0))).reshape(8, size, slice_width).transpose(1, 0, 2)
    gu_slots, terms, down_total, tokens_grad = lax.optimization_barrier(
        (gu_slots, terms, down_total, tokens_grad)
    )
    qkvo_every, gu_every, feed, terms = close_part(
        5,
        flat(gated_all),
        flat(dqkv),
        flat(heads_out),
        flat(grad_branch_all),
        gu_slots,
        terms,
        hidden,
        down_weight,
    )
    gate_total, up_total, query_total, key_total, value_total, out_total = unpack_grads(
        (gu_every, qkvo_every), ((gu_map.shape[1] // 2,) * 2, (local,) * 4)
    )

    layer_out = (live_mask * (middle + feed)).astype(BF)[None]
    return (
        layer_out,
        tokens_grad[None],
        terms[0],
        terms[2:5].T,
        query_total,
        key_total,
        value_total,
        out_total,
        terms[1],
        gate_total,
        up_total,
        down_total,
    )


def solution(mesh):
    placed = (
        P("fsdp", "seq", None),
        P("fsdp", None),
        P("fsdp", None),
        P("fsdp"),
        P("fsdp", None),
        P("fsdp", None),
        P("fsdp", None),
        P("fsdp", None),
        P("fsdp", None),
        P("fsdp"),
        P("fsdp", None),
        P("fsdp", None),
        P("fsdp", None),
        P("fsdp", "seq", None),
    )
    return jax.shard_map(
        shards,
        mesh=mesh,
        in_specs=placed,
        out_specs=(
            P("fsdp", "seq", None),
            P("fsdp", "seq", None),
            P("fsdp"),
            P("fsdp", None),
            P("fsdp", None),
            P("fsdp", None),
            P("fsdp", None),
            P("fsdp", None),
            P("fsdp"),
            P("fsdp", None),
            P("fsdp", None),
            P("fsdp", None),
        ),
        check_vma=False,
    )
```

```python
import functools
from typing import Any, NamedTuple

import jax
import jax.numpy as jnp
from jax import lax
from jax.experimental import pallas as pl
from jax.experimental.pallas import tpu as pltpu
from jax.sharding import PartitionSpec as P

HEADS = 16
WINDOW = 64
HEAD_DIM = 112
BLOCK = 128

EPS = 1e-05
NEG = -1e30
SCALE = HEAD_DIM ** (-0.5)
MESH_ID = pl.DeviceIdType.MESH
BF = jnp.bfloat16
F32 = jnp.float32


def shifted(array, axis, by):
    length = lax.axis_size(axis)
    pairs = [(i, i + by) for i in range(length) if 0 <= i + by < length]
    return lax.ppermute(array, axis, pairs)


def segment_of(slot, count, lengths, starts):
    found = jnp.full(slot.shape, -1, jnp.int32)
    for j in range(count):
        inside = (slot >= starts(j)) & (slot < starts(j) + lengths(j))
        found = jnp.where(inside, j, found)
    return jnp.where(slot < 0, -2, found)


def dot_rows(left, right):
    return lax.dot_general(left, right, (((0,), (0,)), ((), ())), preferred_element_type=F32)


def dot_trans(left, right):
    return lax.dot_general(left, right, (((1,), (1,)), ((), ())), preferred_element_type=F32)


def dot(left, right):
    return jnp.dot(left, right, preferred_element_type=F32)


def masks_of(first, block, count, length, start):
    rows = first + block * BLOCK
    query = rows + lax.broadcasted_iota(jnp.int32, (BLOCK, 1), 0)
    keys = rows - WINDOW + lax.broadcasted_iota(jnp.int32, (1, BLOCK + WINDOW), 1)
    seg_q = segment_of(query, count, length, start)
    seg_k = segment_of(keys, count, length, start)
    far = query - keys
    return (far >= 0) & (far <= WINDOW) & (seg_q == seg_k)


def soft_of(query, keys, mask):
    scores = dot_trans(query, keys) * SCALE
    scores = jnp.where(mask, scores, NEG)
    peak = jnp.max(scores, axis=1, keepdims=True)
    exponent = jnp.exp(scores - peak)
    return exponent / jnp.sum(exponent, axis=1, keepdims=True)


def lane_head(width):
    return lax.broadcasted_iota(jnp.int32, (1, width), 1) // HEAD_DIM


def remote(src, dst, send, recv, **peer):
    return pltpu.make_async_remote_copy(
        src_ref=src,
        dst_ref=dst,
        send_sem=send,
        recv_sem=recv,
        device_id=peer,
        device_id_type=MESH_ID,
    )


def greet_group(barrier, size):
    me = lax.axis_index("fsdp")
    for step in range(1, size):
        peer = lax.rem(me + step, size)
        pl.semaphore_signal(barrier, inc=1, device_id={"fsdp": peer}, device_id_type=MESH_ID)


class Group:
    def __init__(self, size):
        self.size = size
        self.me = lax.axis_index("fsdp")
        self.square = size == 4
        if self.square:
            x, y = lax.rem(self.me, 2), self.me // 2
            self.at = lambda bx, by: lax.rem(y + by, 2) * 2 + lax.rem(x + bx, 2)
            self.x, self.y, self.far = self.at(1, 0), self.at(0, 1), self.at(1, 1)

    def from_own(self, step):
        if self.square:
            return self.at(lax.rem(step, 2), step // 2)
        return lax.rem(self.me - step + self.size, self.size)

    def to_own(self, step):
        if self.square:
            return self.at(1 - step // 2, 1 - lax.rem(step, 2))
        return lax.rem(self.me + 1 + step, self.size)


class Gather:
    def __init__(self, group, ref, send, recv):
        self.group, self.ref, self.send, self.recv = group, ref, send, recv
        self.half = ref.shape[1] // 2

    def part(self, k, slot, half, peer):
        view = self.ref.at[slot, pl.ds(half * self.half, self.half)]
        return remote(view, view, self.send.at[k], self.recv.at[k], fsdp=peer)

    def whole(self, k):
        g = self.group
        view = self.ref.at[g.me]
        sems = self.send.at[k - 1], self.recv.at[k - 1]
        return remote(view, view, *sems, fsdp=lax.rem(g.me + k, g.size))

    def copy(self, k):
        g = self.group
        if not g.square:
            return self.whole(k + 1)
        slot = (g.me, g.me, g.me, g.me, g.x, g.y)[k]
        half = (0, 1, 0, 1, 0, 1)[k]
        return self.part(k, slot, half, (g.x, g.x, g.y, g.y, g.y, g.x)[k])

    def start_half(self, half):
        if self.group.square:
            self.copy(half).start()
            self.copy(2 + half).start()
        elif half == 1:
            for k in range(self.group.size - 1):
                self.copy(k).start()

    def relay(self):
        if self.group.square:
            self.copy(0).wait_recv()
            self.copy(4).start()
            self.copy(3).wait_recv()
            self.copy(5).start()

    def ready(self, step):
        if not self.group.square:
            self.copy(step - 1).wait_recv()
        elif step == 3:
            self.copy(4).wait_recv()
            self.copy(5).wait_recv()
        else:
            self.copy(step).wait_recv()

    def finish(self):
        for k in range(transfers(self.group.size)):
            self.copy(k).wait_send()


class Scatter:
    def __init__(self, group, part, first, over, joined, last, send, recv):
        self.group, self.part = group, part
        self.first, self.over, self.joined, self.last = first, over, joined, last
        self.send, self.recv = send, recv
        self.half = part.shape[1] // 2

    def copy(self, k):
        g, half = self.group, self.half
        low, high = pl.ds(0, half), pl.ds(half, half)
        if not g.square:
            src, dst, peer = self.part.at[k], self.first.at[k], lax.rem(g.me + 1 + k, g.size)
        else:
            src, dst, peer = (
                lambda: (self.part.at[0, low], self.over.at[0], g.x),
                lambda: (self.part.at[0, high], self.over.at[1], g.y),
                lambda: (self.part.at[1, low], self.first.at[0], g.x),
                lambda: (self.part.at[2, high], self.first.at[1], g.y),
                lambda: (self.joined.at[0], self.last.at[0], g.y),
                lambda: (self.joined.at[1], self.last.at[1], g.x),
            )[k]()
        return remote(src, dst, self.send.at[k], self.recv.at[k], fsdp=peer)

    def made(self, step):
        if not self.group.square:
            self.copy(step).start()
        elif step == 0:
            self.copy(0).start()
            self.copy(1).start()
        elif step in (1, 2):
            self.copy(step + 1).start()

    def join(self):
        if not self.group.square:
            return
        half = self.half
        for k, (step, rows) in enumerate(((2, slice(0, half)), (1, slice(half, 2 * half)))):
            self.copy(k).wait_recv()
            own = self.part[step, rows].astype(F32)
            self.joined[k] = (own + self.over[k].astype(F32)).astype(BF)
            self.copy(4 + k).start()

    def total(self, half):
        count = self.half
        if self.group.square:
            self.copy(2 + half).wait_recv()
            self.copy(4 + half).wait_recv()
            return self.first[half].astype(F32) + self.last[half].astype(F32)
        if half == 0:
            for k in range(self.group.size - 1):
                self.copy(k).wait_recv()
        rows = slice(half * count, (half + 1) * count)
        out = self.first[0, rows].astype(F32)
        for k in range(1, self.group.size - 1):
            out = out + self.first[k, rows].astype(F32)
        return out

    def finish(self):
        for k in range(transfers(self.group.size)):
            self.copy(k).wait_send()


class Line:
    def __init__(self, parts, sems):
        self.rank = lax.axis_index("seq")
        self.parts, self.length = parts, parts // 2
        self.z, self.core = self.rank // 2, lax.rem(self.rank, 2)
        self.above, self.below = self.rank + 2, self.rank - 2
        self.beside = self.rank + 1 - 2 * self.core
        self.has_above, self.has_below = self.z < self.length - 1, self.z > 0
        self.sems = sems

    def greet(self, barrier):
        def one(peer):
            pl.semaphore_signal(barrier, inc=1, device_id={"seq": peer}, device_id_type=MESH_ID)

        one(self.beside)
        pl.when(self.has_above)(lambda: one(self.above))
        pl.when(self.has_below)(lambda: one(self.below))
        n, z = self.length, self.z
        return 1 + (2 * n - 2 - z) // n + (z + n - 1) // n

    def up(self, k, owner):
        view = self.view(owner)
        return remote(view, view, self.sems[0].at[k], self.sems[1].at[k], seq=self.above)

    def down(self, k, owner):
        view = self.view(owner)
        return remote(view, view, self.sems[2].at[k], self.sems[3].at[k], seq=self.below)

    def side(self, k, owner):
        view = self.view(owner)
        return remote(view, view, self.sems[4].at[k], self.sems[5].at[k], seq=self.beside)

    def gather(self, view):
        self.view = view
        pl.when(self.has_above)(lambda: self.up(0, self.rank).start())
        pl.when(self.has_below)(lambda: self.down(0, self.rank).start())
        self.side(self.z, self.rank).start()

    def own_up(self):
        pl.when(self.has_above)(lambda: self.up(0, self.rank).start())

    def own_down(self):
        pl.when(self.has_below)(lambda: self.down(0, self.rank).start())

    def relay_up(self, j):
        rank, z = self.rank, self.z

        @pl.when((z >= j) & self.has_above)
        def _():
            self.up(j - 1, rank).wait_recv()
            self.up(j, rank - 2 * j).start()
            self.side(z - j, rank - 2 * j).start()

    def relay_down(self, j):
        rank, z = self.rank, self.z

        @pl.when((z + j < self.length) & self.has_below)
        def _():
            self.down(j - 1, rank).wait_recv()
            self.down(j, rank + 2 * j).start()
            self.side(z + j, rank + 2 * j).start()

    def relay(self, j):
        self.relay_up(j)
        self.relay_down(j)

    def close(self, j):
        rank, z = self.rank, self.z

        @pl.when((z >= j) & (z == self.length - 1))
        def _():
            self.up(j - 1, rank).wait_recv()
            self.side(z - j, rank - 2 * j).start()

        @pl.when((z + j < self.length) & (z == 0))
        def _():
            self.down(j - 1, rank).wait_recv()
            self.side(z + j, rank + 2 * j).start()

    def gathered(self):
        for k in range(self.length):
            self.side(k, self.rank).wait_recv()

    def finish(self):
        rank, z = self.rank, self.z
        for k in range(self.length):
            self.side(k, rank).wait_send()
        pl.when(self.has_above)(lambda: self.up(0, rank).wait_send())
        pl.when(self.has_below)(lambda: self.down(0, rank).wait_send())
        for j in range(1, self.length):
            pl.when((z >= j) & self.has_above)(lambda: self.up(j, rank).wait_send())
            pl.when((z + j < self.length) & self.has_below)(lambda: self.down(j, rank).wait_send())


class LineSum:
    def __init__(self, line, x, pre, acc, up_in, down_in, sems):
        self.line, self.x, self.pre, self.acc = line, x, pre, acc
        self.up_in, self.down_in, self.sems = up_in, down_in, sems

    def share(self, k):
        line = self.line
        src = self.x.at[2 * k + 1 - line.core]
        return remote(src, self.pre.at[k], self.sems[0].at[k], self.sems[1].at[k], seq=line.beside)

    def up(self, k):
        sems = self.sems[2].at[k], self.sems[3].at[k]
        return remote(self.acc.at[k], self.up_in.at[k], *sems, seq=self.line.above)

    def down(self, k):
        sems = self.sems[4].at[k], self.sems[5].at[k]
        return remote(self.acc.at[k], self.down_in.at[k], *sems, seq=self.line.below)

    def pair(self, m):
        return self.line.length - 1 - m, m

    def trade(self):
        n = self.line.length
        for m in range((n + 1) // 2):
            for k in sorted(set(self.pair(m))):
                self.share(k).start()

    def merge(self, k):
        self.share(k).wait_recv()
        own = self.x[2 * k + self.line.core].astype(F32)
        self.acc[k] = (own + self.pre[k].astype(F32)).astype(BF)

    def begin(self, m):
        n, z = self.line.length, self.line.z
        far, near = self.pair(m)
        if m < (n + 1) // 2:
            for k in sorted({far, near}):
                self.merge(k)
        if m < n - 1:
            pl.when(z == 0)(lambda: self.up(far).start())
            pl.when(z == n - 1)(lambda: self.down(near).start())

    def add(self, k, more):
        self.acc[k] = (self.acc[k].astype(F32) + more[k].astype(F32)).astype(BF)

    def advance(self, t):
        z, n = self.line.z, self.line.length
        far, near = n - 1 + z - t, t - n + 1 + z

        @pl.when((z >= 1) & (z <= t))
        def _():
            self.up(far).wait_recv()
            self.add(far, self.up_in)
            self.up(far).start()

        @pl.when((z <= n - 2) & (z >= n - 1 - t))
        def _():
            self.down(near).wait_recv()
            self.add(near, self.down_in)
            self.down(near).start()

    def total(self):
        z = self.line.z

        @pl.when(z > 0)
        def _():
            self.up(z).wait_recv()
            self.add(z, self.up_in)

        @pl.when(z < self.line.length - 1)
        def _():
            self.down(z).wait_recv()
            self.add(z, self.down_in)

    def finish(self):
        for k in range(self.line.length):
            self.share(k).wait_send()
            pl.when(k > self.line.z)(lambda: self.up(k).wait_send())
            pl.when(k < self.line.z)(lambda: self.down(k).wait_send())


class StagedSum(LineSum):
    def __init__(self, stage, load, *args):
        super().__init__(*args)
        self.stage, self.load = stage, load

    def fetch(self, slot, src):
        return pltpu.make_async_copy(src, self.stage.at[slot], self.load.at[slot])

    def merge(self, k):
        self.share(k).wait_recv()
        own = self.fetch(0, self.x.at[2 * k + self.line.core])
        other = self.fetch(1, self.pre.at[k])
        own.start()
        other.start()
        own.wait()
        other.wait()
        self.acc[k] = (self.stage[0].astype(F32) + self.stage[1].astype(F32)).astype(BF)

    def add(self, k, more):
        came = self.fetch(0, more.at[k])
        came.start()
        came.wait()
        self.acc[k] = (self.acc[k].astype(F32) + self.stage[0].astype(F32)).astype(BF)


class MixedSum(StagedSum):
    def merge(self, k):
        self.share(k).wait_recv()
        other = self.fetch(1, self.pre.at[k])
        other.start()
        other.wait()
        own = self.x[2 * k + self.line.core].astype(F32)
        self.acc[k] = (own + self.stage[1].astype(F32)).astype(BF)


def line_sems(parts):
    return [pltpu.SemaphoreType.DMA((parts // 2,))] * 6


def transfers(size):
    return 6 if size == 4 else size - 1


def scatter_shapes(size, rows, width):
    half = rows // 2
    slots = (2, half, width) if size == 4 else (size - 1, rows, width)
    return [
        pltpu.VMEM((size - 1, rows, width), BF),
        pltpu.VMEM(slots, BF),
        pltpu.VMEM((2, half, width), BF),
        pltpu.VMEM((2, half, width), BF),
        pltpu.VMEM((2, half, width), BF),
        pltpu.SemaphoreType.DMA((transfers(size),)),
        pltpu.SemaphoreType.DMA((transfers(size),)),
    ]


def each_step(size, body):
    def one(step, carry):
        body(step, lambda k: pl.when(step == k))
        return carry

    lax.fori_loop(0, size, one, 0)


class ForwardRefs(NamedTuple):
    tokens: Any
    cot: Any
    gains: Any
    table: Any
    qkv_piece: Any
    gu_piece: Any
    out_map: Any
    down_map: Any
    gated_hbm: Any
    qkv_hbm: Any
    edge: Any
    qkv_map_hbm: Any
    middle: Any
    heads: Any
    grads_hbm: Any
    norm_hbm: Any
    hidden_hbm: Any
    gu_grad_hbm: Any
    gu_map_hbm: Any
    gains_all: Any
    table_all: Any
    edge_tok: Any
    part: Any
    first: Any
    over: Any
    joined: Any
    last: Any
    all: Any
    grads: Any
    qkv: Any
    qkv_map: Any
    gu_map: Any
    tail: Any
    own: Any
    grad_hidden: Any
    hidden: Any
    gu_grad: Any
    s_send: Any
    s_recv: Any
    a_send: Any
    a_recv: Any
    g_send: Any
    g_recv: Any
    c_send: Any
    c_recv: Any
    m_send: Any
    m_recv: Any
    halo_send: Any
    halo_recv: Any
    edge_send: Any
    edge_recv: Any
    loads: Any
    stores: Any
    hidden_store: Any
    gu_store: Any


def forward_kernel(size, parts, count, *refs):
    named = len(ForwardRefs._fields)
    r, sems = ForwardRefs(*refs[:named]), refs[named:]
    rank = lax.axis_index("seq")
    rows = r.tokens.shape[0]
    half = rows // 2
    local = r.out_map.shape[0]
    inner = r.down_map.shape[0]
    slot = rank * rows
    group = Group(size)
    me = group.me
    line_q, line_u = Line(parts, sems[:6]), Line(parts, sems[6:])

    barrier = pltpu.get_barrier_semaphore()
    greet_group(barrier, size)
    known = line_q.greet(barrier)

    def greet(peer):
        pl.semaphore_signal(barrier, inc=1, device_id={"seq": peer}, device_id_type=MESH_ID)

    pl.when(line_q.has_above & (line_q.core == 1))(lambda: greet(rank + 1))
    pl.when(line_q.has_below & (line_q.core == 0))(lambda: greet(rank - 1))
    n, z = line_q.length, line_q.z
    known = known + (2 * n - 2 - z) // n * line_q.core + (z + n - 1) // n * (1 - line_q.core)
    own_pieces = [
        pltpu.make_async_copy(src.at[me], dst.at[me, rank], r.loads.at[k])
        for k, (src, dst) in enumerate(
            ((r.qkv_piece, r.qkv_map), (r.gu_piece, r.gu_map))
        )
    ]
    for copy in own_pieces:
        copy.start()
    r.gains_all[me] = r.gains[...]
    r.table_all[me] = r.table[...]
    own_table = r.table[...]
    slots = slot + lax.broadcasted_iota(jnp.int32, (rows, 1), 0)
    length = lambda j: own_table[0:1, j : j + 1]
    start = lambda j: own_table[1:2, j : j + 1]
    segment = segment_of(slots, count, length, start)
    r.grads[me] = jnp.where(segment >= 0, r.cot[...].astype(F32), 0.0).astype(BF)

    @pl.when(rank == 0)
    def _():
        r.edge_tok[...] = jnp.zeros_like(r.edge_tok)

    def edge_rows():
        last = r.tokens.at[pl.ds(rows - 8, 8)]
        return remote(last, r.edge_tok, r.edge_send, r.edge_recv, seq=rank + 1)

    pl.semaphore_wait(barrier, size - 1 + known)
    pl.when(rank < parts - 1)(lambda: edge_rows().start())

    def swap(k, step):
        peer = lax.rem(me + step, size)
        src, dst = (
            lambda: (r.gains_all.at[me], r.gains_all.at[me]),
            lambda: (r.table_all.at[me], r.table_all.at[me]),
            lambda: (r.qkv_piece.at[peer], r.qkv_map.at[me, rank]),
            lambda: (r.gu_piece.at[peer], r.gu_map.at[me, rank]),
        )[k]()
        return remote(src, dst, r.m_send.at[k, step - 1], r.m_recv.at[k, step - 1], fsdp=peer)

    others = range(1, size)
    for k in range(4):
        for step in others:
            swap(k, step).start()
    for k in range(2):
        for step in others:
            swap(k, step).wait_recv()

    gains = jnp.concatenate([r.gains_all[f] for f in range(size)], 1).astype(F32)
    same_one = (segment == segment_of(slots - 1, count, length, start)).astype(F32)
    same_two = (segment == segment_of(slots - 2, count, length, start)).astype(F32)
    tokens = r.tokens[...].astype(F32)
    pl.when(rank > 0)(lambda: edge_rows().wait_recv())
    edge = r.edge_tok[...].astype(F32)

    def norm(a):
        return a * lax.rsqrt(jnp.mean(a * a, axis=1, keepdims=True) + EPS) * gains[0:1]

    normed, edge = norm(tokens), norm(edge)
    row = lax.broadcasted_iota(jnp.int32, (rows, 1), 0)
    back_one = jnp.where(row == 0, edge[7:8], pltpu.roll(normed, 1, 0))
    back_two = jnp.where(
        row == 0, edge[6:7], jnp.where(row == 1, edge[7:8], pltpu.roll(normed, 2, 0))
    )
    mixed = (
        normed * gains[2:3]
        + same_one * back_one * gains[3:4]
        + same_two * back_two * gains[4:5]
    )
    all_ref = r.all
    all_ref[me] = (mixed * normed).astype(BF)
    gather = Gather(group, all_ref, r.a_send, r.a_recv)
    gather.start_half(0)
    gather.start_half(1)

    own_pieces[0].wait()
    for step in others:
        swap(2, step).wait_recv()
    line_q.gather(lambda owner: r.qkv_map.at[:, owner])
    line_u.view = lambda owner: r.gu_map.at[:, owner]
    gather.relay()
    grads = Gather(group, r.grads, r.c_send, r.c_recv)
    grads.start_half(0)
    grads.start_half(1)
    own_pieces[1].wait()
    for step in others:
        swap(3, step).wait_recv()
    line_u.side(z, rank).start()
    pl.when(z == 0)(line_u.own_up)
    pl.when(z == n - 1)(line_u.own_down)
    for j in range(1, n):
        line_q.relay(j)
        line_q.close(j)
        pl.when(z == j)(line_u.own_up)
        pl.when(z == n - 1 - j)(line_u.own_down)
    for step in others:
        gather.ready(step)
    grads.relay()
    line_q.gathered()
    keeps = [
        pltpu.make_async_copy(all_ref, r.gated_hbm, r.stores.at[size]),
        pltpu.make_async_copy(r.qkv_map, r.qkv_map_hbm, r.stores.at[size + 1]),
    ]
    for keep in keeps:
        keep.start()

    weights = r.qkv_map[...].reshape(-1, r.qkv_map.shape[3])

    def halo(step):
        g = group.to_own(step)
        sem = r.halo_send.at[step], r.halo_recv.at[step]
        return remote(r.tail.at[g], r.edge.at[g], *sem, seq=rank + 1)

    def project(step, is_step):
        g = group.to_own(step)
        out = dot(all_ref[g], weights).astype(BF)
        r.qkv[g] = out
        r.tail[g] = out[rows - WINDOW :, local:]
        pl.when(rank < parts - 1)(lambda: halo(step).start())

    each_step(size, project)

    @pl.when(rank == 0)
    def _():
        r.edge[...] = jnp.zeros_like(r.edge)

    keeps.append(pltpu.make_async_copy(r.qkv, r.qkv_hbm, r.stores.at[size + 2]))
    keeps[2].start()
    line_u.relay(1)
    gather.finish()
    keeps[0].wait()

    scatter = Scatter(
        group, r.part, r.first, r.over, r.joined, r.last, r.s_send, r.s_recv
    )
    head_of = lane_head(local)

    def mix(step, is_step):
        g = group.to_own(step)
        pl.when(rank > 0)(lambda: halo(step).wait_recv())
        own, edge, table = r.qkv[g], r.edge[g], r.table_all[g]
        queries = own[:, :local]
        keys = jnp.concatenate([edge[:, :local], own[:, local : 2 * local]], 0)
        values = jnp.concatenate([edge[:, local:], own[:, 2 * local :]], 0)
        outs = []
        for block in range(rows // BLOCK):
            mask = masks_of(
                slot,
                block,
                count,
                lambda j: table[0:1, j : j + 1],
                lambda j: table[1:2, j : j + 1],
            )
            low = block * BLOCK
            query = queries[low : low + BLOCK]
            key = keys[low : low + BLOCK + WINDOW]
            value = values[low : low + BLOCK + WINDOW]
            out = jnp.zeros((BLOCK, local), F32)
            for head in range(local // HEAD_DIM):
                mine = head_of == head
                soft = soft_of(jnp.where(mine, query, jnp.zeros_like(query)), key, mask)
                out = jnp.where(mine, dot(soft.astype(BF), value), out)
            outs.append(out.astype(BF))
        heads = jnp.concatenate(outs, 0)
        r.heads[g] = heads
        branch = dot(heads, r.out_map[...])
        is_step(size - 1)(lambda: r.own.__setitem__(..., branch))
        pl.when(step < size - 1)(lambda: r.part.__setitem__(step, branch.astype(BF)))
        for k in range(size - 1):
            is_step(k)(functools.partial(scatter.made, k))

    each_step(size, mix)
    scatter.join()
    for j in range(2, n):
        line_u.relay(j)
    gather = Gather(group, all_ref, r.g_send, r.g_recv)
    for h in range(2):
        span = slice(h * half, (h + 1) * half)
        total = r.own[span, :] + scatter.total(h)
        middle = r.tokens[span, :].astype(F32) + total
        r.middle[span, :] = middle
        scale = lax.rsqrt(jnp.mean(middle * middle, axis=1, keepdims=True) + EPS)
        all_ref[me, span] = (middle * scale * gains[1:2]).astype(BF)
        gather.start_half(h)
    gather.relay()

    def grad_of(step, is_step):
        g = group.from_own(step)
        for k in others:
            is_step(k)(functools.partial(grads.ready, k))
        r.grad_hidden[g] = dot_trans(r.grads[g], r.down_map[...])

    each_step(size, grad_of)
    for j in range(1, n):
        line_u.close(j)
    line_u.gathered()
    keeps.append(pltpu.make_async_copy(r.gu_map, r.gu_map_hbm, r.stores.at[size + 3]))
    keeps[3].start()

    def out_copies(step):
        g, two = group.from_own(step), lax.rem(step, 2)
        return (
            pltpu.make_async_copy(
                r.hidden.at[two], r.hidden_hbm.at[g], r.hidden_store.at[two]
            ),
            pltpu.make_async_copy(
                r.gu_grad.at[two], r.gu_grad_hbm.at[g], r.gu_store.at[two]
            ),
        )

    def norm_copy(g):
        return pltpu.make_async_copy(all_ref.at[g], r.norm_hbm.at[g], r.stores.at[g])

    def feed(step, is_step):
        g, two = group.from_own(step), lax.rem(step, 2)
        for k in others:
            is_step(k)(functools.partial(gather.ready, k))

        @pl.when(step >= 2)
        def _():
            for copy in out_copies(step - 2):
                copy.wait()

        norm_copy(g).start()
        weights = r.gu_map[...].reshape(-1, r.gu_map.shape[3])
        acts = dot(all_ref[g], weights)
        gate, up = acts[:, :inner], acts[:, inner:]
        sigma = jax.nn.sigmoid(gate)
        silu = gate * sigma
        r.hidden[two] = (silu * up).astype(BF)
        grad_hidden = r.grad_hidden[g]
        grad_gate = grad_hidden * up * sigma * (1.0 + gate * (1.0 - sigma))
        r.gu_grad[two] = jnp.concatenate([grad_gate, grad_hidden * silu], 1).astype(BF)
        for copy in out_copies(step):
            copy.start()

    each_step(size, feed)
    keeps.append(pltpu.make_async_copy(r.grads, r.grads_hbm, r.stores.at[size + 4]))
    keeps[4].start()
    for k in range(4):
        for step in others:
            swap(k, step).wait_send()
    scatter.finish()
    gather.finish()
    grads.finish()
    line_q.finish()
    line_u.finish()

    @pl.when(rank < parts - 1)
    def _():
        edge_rows().wait_send()
        for step in range(size):
            halo(step).wait_send()

    for keep in keeps[1:]:
        keep.wait()
    for g in range(size):
        norm_copy(g).wait()
    for step in (size - 2, size - 1):
        for copy in out_copies(step):
            copy.wait()


def forward_part(ident, count, tokens, cot, gains, table, qkv_piece, gu_piece, out_weight, down_weight):
    size, parts = lax.axis_size("fsdp"), lax.axis_size("seq")
    rows, width = tokens.shape
    local, inner = out_weight.shape[0], down_weight.shape[0]
    piece, cols = gu_piece.shape[1:]
    vmem = pl.BlockSpec(memory_space=pltpu.VMEM)
    hbm = pl.BlockSpec(memory_space=pl.ANY)
    shape = lambda w: (size, rows, w)
    low = lambda s: jax.ShapeDtypeStruct(s, BF)
    maps = [(size, parts, piece, 3 * local), (size, parts, piece, cols)]
    dma = lambda *s: pltpu.SemaphoreType.DMA(s)
    hop = transfers(size)
    scratch = scatter_shapes(size, rows, width)
    return pl.pallas_call(
        functools.partial(forward_kernel, size, parts, count),
        out_shape=[
            low(shape(width)),
            low(shape(3 * local)),
            low((size, WINDOW, 2 * local)),
            low(maps[0]),
            jax.ShapeDtypeStruct((rows, width), F32),
            low(shape(local)),
            low(shape(width)),
            low(shape(width)),
            low(shape(inner)),
            low(shape(cols)),
            low(maps[1]),
            low((size,) + gains.shape),
            jax.ShapeDtypeStruct((size,) + table.shape, jnp.int32),
            low((8, width)),
        ],
        in_specs=[vmem] * 4 + [hbm, hbm, vmem, vmem],
        out_specs=[hbm, hbm, vmem, hbm, vmem, vmem, hbm, hbm, hbm, hbm, hbm, vmem, vmem, vmem],
        scratch_shapes=scratch[:-2]
        + [
            pltpu.VMEM(shape(width), BF),
            pltpu.VMEM(shape(width), BF),
            pltpu.VMEM(shape(3 * local), BF),
            pltpu.VMEM(maps[0], BF),
            pltpu.VMEM(maps[1], BF),
            pltpu.VMEM((size, WINDOW, 2 * local), BF),
            pltpu.VMEM((rows, width), F32),
            pltpu.VMEM(shape(inner), F32),
            pltpu.VMEM((2, rows, inner), BF),
            pltpu.VMEM((2, rows, cols), BF),
        ]
        + [dma(hop)] * 8
        + [dma(4, size - 1)] * 2
        + [dma(size)] * 2
        + [pltpu.SemaphoreType.DMA] * 2
        + [dma(2), dma(size + 5), dma(2), dma(2)]
        + line_sems(parts)
        + line_sems(parts),
        compiler_params=pltpu.CompilerParams(
            collective_id=ident, has_side_effects=True, vmem_limit_bytes=67_000_000
        ),
        cost_estimate=pl.CostEstimate(
            flops=2 * size * rows * width * (4 * local + 3 * inner),
            bytes_accessed=500_000_000,
            transcendentals=0,
        ),
        name="forward_part",
    )(tokens, cot, gains, table, qkv_piece, gu_piece, out_weight, down_weight)


def heads_back(group, slot, count, lens_ref, starts_ref, own, edge, grad):
    rows, local = own.shape[0], own.shape[1] // 3
    head_of = lane_head(local)
    queries = own[:, :local]
    keys = jnp.concatenate([edge[:, :local], own[:, local : 2 * local]], 0)
    values = jnp.concatenate([edge[:, local:], own[:, 2 * local :]], 0)
    dqs, dks, dvs = [], [], []
    for block in range(rows // BLOCK):
        mask = masks_of(
            slot, block, count, lambda j: lens_ref[group, j], lambda j: starts_ref[group, j]
        )
        low = block * BLOCK
        span = slice(low, low + BLOCK + WINDOW)
        query, grads = queries[low : low + BLOCK], grad[low : low + BLOCK]
        key, value = keys[span], values[span]
        dq = jnp.zeros((BLOCK, local), F32)
        dk = jnp.zeros((BLOCK + WINDOW, local), F32)
        dv = jnp.zeros((BLOCK + WINDOW, local), F32)
        for head in range(local // HEAD_DIM):
            mine = head_of == head
            own_q = jnp.where(mine, query, jnp.zeros_like(query))
            own_g = jnp.where(mine, grads, jnp.zeros_like(grads))
            soft = soft_of(own_q, key, mask)
            grad_soft = dot_trans(own_g, value)
            total = jnp.sum(grad_soft * soft, axis=1, keepdims=True)
            grad_scores = (soft * (grad_soft - total)).astype(BF)
            dq = jnp.where(mine, dot(grad_scores, key), dq)
            dk = dk + dot_rows(grad_scores, own_q)
            dv = dv + dot_rows(soft.astype(BF), own_g)
        dqs.append(dq * SCALE)
        dks.append(dk * SCALE)
        dvs.append(dv)

    def joined(pieces):
        out = [pieces[0][:BLOCK]]
        for left, right in zip(pieces, pieces[1:]):
            out.append(left[BLOCK:] + right[:WINDOW])
            out.append(right[WINDOW:BLOCK])
        out.append(pieces[-1][BLOCK:])
        return jnp.concatenate(out, 0)

    return jnp.concatenate(dqs, 0), joined(dks), joined(dvs)


class BackRefs(NamedTuple):
    lens: Any
    starts: Any
    grad_gu_hbm: Any
    gu_map_hbm: Any
    middle: Any
    grads_hbm: Any
    gain: Any
    out_map: Any
    edge: Any
    qkv: Any
    qkv_map_hbm: Any
    gu_x: Any
    down_x: Any
    grad_middle: Any
    norm: Any
    all: Any
    dqkv: Any
    own: Any
    gu_slots: Any
    down_every: Any
    gu_pre: Any
    gu_up: Any
    gu_down: Any
    down_pre: Any
    down_up: Any
    down_down: Any
    part: Any
    first: Any
    over: Any
    joined: Any
    last: Any
    s_send: Any
    s_recv: Any
    t_send: Any
    t_recv: Any
    g_send: Any
    g_recv: Any
    grad_gu: Any
    gu_map: Any
    qkv_map: Any
    dedge: Any
    back: Any
    tail: Any
    h_send: Any
    h_recv: Any
    loads: Any
    gu_acc: Any
    gu_stage: Any
    gu_load: Any
    down_acc: Any
    down_stage: Any
    down_load: Any
    m_send: Any
    m_recv: Any
    grad: Any


def back_kernel(size, parts, count, *refs):
    named = len(BackRefs._fields)
    r, sems = BackRefs(*refs[:named]), refs[named:]
    line = Line(parts, sems[:6])
    gu_sum = StagedSum(
        r.gu_stage, r.gu_load, line, r.gu_x, r.gu_pre, r.gu_acc, r.gu_up, r.gu_down, sems[6:12]
    )
    down_sum = StagedSum(
        r.down_stage,
        r.down_load,
        line,
        r.down_x,
        r.down_pre,
        r.down_acc,
        r.down_up,
        r.down_down,
        sems[12:],
    )
    rows = r.middle.shape[0]
    local = r.out_map.shape[0]
    rank = lax.axis_index("seq")
    slot = rank * rows
    group = Group(size)
    barrier = pltpu.get_barrier_semaphore()
    greet_group(barrier, size)

    def greet(peer):
        pl.semaphore_signal(barrier, inc=1, device_id={"seq": peer}, device_id_type=MESH_ID)

    known = line.greet(barrier)
    pl.when(line.has_above & (line.core == 1))(lambda: greet(rank + 1))
    pl.when(line.has_below & (line.core == 0))(lambda: greet(rank - 1))
    n, z = line.length, line.z
    known = known + (2 * n - 2 - z) // n * line.core + (z + n - 1) // n * (1 - line.core)
    fetches = [
        pltpu.make_async_copy(src, dst, r.loads.at[k])
        for k, (src, dst) in enumerate(
            (
                (r.grad_gu_hbm, r.grad_gu),
                (r.gu_map_hbm, r.gu_map),
                (r.qkv_map_hbm, r.qkv_map),
                (r.grads_hbm.at[group.me], r.grad),
            )
        )
    ]
    for fetch in fetches:
        fetch.start()
    pl.semaphore_wait(barrier, size - 1 + known)
    down_sum.trade()
    gu_sum.trade()
    for m in range(n):
        down_sum.begin(m)
    scatter = Scatter(
        group, r.part, r.first, r.over, r.joined, r.last, r.s_send, r.s_recv
    )
    gather = Gather(group, r.all, r.g_send, r.g_recv)
    fetches[0].wait()
    fetches[1].wait()
    fetches[3].wait()

    def step_two(step, is_step):
        partial = dot_trans(r.grad_gu[group.to_own(step)], r.gu_map[...])
        is_step(size - 1)(lambda: r.own.__setitem__(..., partial))
        pl.when(step < size - 1)(lambda: r.part.__setitem__(step, partial.astype(BF)))
        for k in range(size - 1):
            is_step(k)(functools.partial(scatter.made, k))

    each_step(size, step_two)
    scatter.join()
    gu_sum.begin(0)
    down_sum.advance(1)
    half = rows // 2
    norm_sum = jnp.zeros((1, r.middle.shape[1]), F32)
    for h in range(2):
        span = slice(h * half, (h + 1) * half)
        grad = r.own[span, :] + scatter.total(h)
        middle = r.middle[span, :]
        scale = lax.rsqrt(jnp.mean(middle * middle, axis=1, keepdims=True) + EPS)
        unit = middle * scale
        scaled = grad * r.gain[...]
        norm_sum = norm_sum + jnp.sum(grad * unit, axis=0, keepdims=True)
        grad_out = r.grad[span, :].astype(F32)
        grad_middle = grad_out + scale * (
            scaled - unit * jnp.mean(scaled * unit, axis=1, keepdims=True)
        )
        r.grad_middle[span, :] = grad_middle
        r.all[group.me, span] = grad_middle.astype(BF)
        gather.start_half(h)
    r.norm[...] = norm_sum
    own_down = pltpu.make_async_copy(r.down_acc.at[z], r.down_every.at[rank], r.down_load.at[0])

    def halo(step):
        g = group.from_own(step)
        sems = r.h_send.at[step], r.h_recv.at[step]
        return remote(r.dedge.at[g], r.back.at[g], *sems, seq=rank - 1)

    def step_heads(step, is_step):
        g = group.from_own(step)

        @is_step(1)
        def _():
            gather.relay()
            for t in range(2, n - 1):
                down_sum.advance(t)

        @is_step(2)
        def _():
            down_sum.total()
            own_down.start()
            own_down.wait()
            line.gather(lambda owner: r.down_every.at[owner])
            for m in range(1, n):
                gu_sum.begin(m)

        is_step(size - 1)(lambda: gu_sum.advance(1))

        for k in range(1, size):
            is_step(k)(functools.partial(gather.ready, k))
        grad = dot_trans(r.all[g], r.out_map[...]).astype(BF)
        dq, dk, dv = heads_back(
            g, slot, count, r.lens, r.starts, r.qkv[g], r.edge[g], grad
        )
        r.dedge[g] = jnp.concatenate([dk[:WINDOW], dv[:WINDOW]], 1).astype(BF)
        full = jnp.concatenate([dq, dk[WINDOW:], dv[WINDOW:]], 1)
        r.dqkv[g] = full.astype(BF)
        r.tail[g] = full[rows - WINDOW :]
        pl.when(rank > 0)(lambda: halo(step).start())

    each_step(size, step_heads)
    line.relay(1)
    scatter.finish()
    fetches[2].wait()

    @pl.when(rank == parts - 1)
    def _():
        r.back[...] = jnp.zeros_like(r.back)

    @pl.when(rank < parts - 1)
    def _():
        for step in range(size):
            halo(step).wait_recv()

    scatter = Scatter(
        group, r.part, r.first, r.over, r.joined, r.last, r.t_send, r.t_recv
    )

    def step_one(step, is_step):
        g = group.to_own(step)
        back = r.back[g].astype(F32)
        wide = jnp.concatenate([jnp.zeros((WINDOW, local), F32), back], 1)
        r.dqkv[g, pl.ds(rows - WINDOW, WINDOW)] = (r.tail[g] + wide).astype(BF)
        partial = dot_trans(r.dqkv[g], r.qkv_map[...])
        is_step(size - 1)(lambda: r.own.__setitem__(..., partial))
        pl.when(step < size - 1)(lambda: r.part.__setitem__(step, partial.astype(BF)))
        for k in range(size - 1):
            is_step(k)(functools.partial(scatter.made, k))

    each_step(size, step_one)
    scatter.join()
    for t in range(2, n - 1):
        gu_sum.advance(t)
        line.relay(t)
    line.relay(n - 1)
    for h in range(2):
        span = slice(h * half, (h + 1) * half)
        r.own[span, :] = r.own[span, :] + scatter.total(h)
    gu_sum.total()

    def swap(step):
        peer = lax.rem(group.me + step, size)
        sems = r.m_send.at[step - 1], r.m_recv.at[step - 1]
        return remote(r.gu_acc.at[z, peer], r.gu_slots.at[group.me], *sems, fsdp=peer)

    for step in range(1, size):
        swap(step).start()
    own_slot = pltpu.make_async_copy(
        r.gu_acc.at[z, group.me], r.gu_slots.at[group.me], r.gu_load.at[0]
    )
    own_slot.start()
    for j in range(1, n):
        line.close(j)
    line.gathered()
    for step in range(1, size):
        swap(step).wait()
    scatter.finish()
    gather.finish()
    down_sum.finish()
    gu_sum.finish()
    line.finish()
    own_slot.wait()

    @pl.when(rank > 0)
    def _():
        for step in range(size):
            halo(step).wait_send()


def back_part(
    ident, lens, starts, grad_gu, gu_map, middle, grads, gain, out_weight, edge, qkv, qkv_map, gu_x, down_x
):
    size, parts = lax.axis_size("fsdp"), lax.axis_size("seq")
    rows, width = middle.shape
    local = out_weight.shape[0]
    n = parts // 2
    vmem = pl.BlockSpec(memory_space=pltpu.VMEM)
    smem = pl.BlockSpec(memory_space=pltpu.SMEM)
    hbm = pl.BlockSpec(memory_space=pl.ANY)
    dma = lambda *s: pltpu.SemaphoreType.DMA(s)
    low = lambda *s: jax.ShapeDtypeStruct(s, BF)
    sems = [dma(transfers(size))] * 2
    gu, down = gu_x.shape[1:], down_x.shape[1:]
    outs = pl.pallas_call(
        functools.partial(back_kernel, size, parts, lens.shape[1]),
        out_shape=[
            jax.ShapeDtypeStruct((rows, width), F32),
            jax.ShapeDtypeStruct((1, width), F32),
            low(size, rows, width),
            low(*qkv.shape),
            jax.ShapeDtypeStruct((rows, width), F32),
            low(*gu),
            low(parts, *down),
        ]
        + [low(n, *gu)] * 3
        + [low(n, *down)] * 3,
        in_specs=[smem, smem, hbm, hbm, vmem, hbm] + [vmem] * 4 + [hbm] * 3,
        out_specs=[vmem] * 5 + [hbm] * 8,
        scratch_shapes=scatter_shapes(size, rows, width)
        + sems
        + sems
        + [
            pltpu.VMEM(grad_gu.shape, BF),
            pltpu.VMEM(gu_map.shape, BF),
            pltpu.VMEM(qkv_map.shape, BF),
            pltpu.VMEM((size, WINDOW, 2 * local), BF),
            pltpu.VMEM((size, WINDOW, 2 * local), BF),
            pltpu.VMEM((size, WINDOW, 3 * local), F32),
            dma(size),
            dma(size),
            dma(4),
            pltpu.VMEM((n,) + gu, BF),
            pltpu.VMEM((2,) + gu, BF),
            dma(2),
            pltpu.VMEM((n,) + down, BF),
            pltpu.VMEM((2,) + down, BF),
            dma(2),
            dma(size - 1),
            dma(size - 1),
            pltpu.VMEM((rows, width), BF),
        ]
        + line_sems(parts) * 3,
        compiler_params=pltpu.CompilerParams(
            collective_id=ident, has_side_effects=True, vmem_limit_bytes=67_000_000
        ),
        cost_estimate=pl.CostEstimate(
            flops=2 * size * rows * (gu_map.size + qkv_map.size + width * local),
            bytes_accessed=400_000_000,
            transcendentals=0,
        ),
        name="back_part",
    )(lens, starts, grad_gu, gu_map, middle, grads, gain, out_weight, edge, qkv, qkv_map, gu_x, down_x)
    return outs[:7]


class CloseRefs(NamedTuple):
    gated_hbm: Any
    dqkv_hbm: Any
    heads_hbm: Any
    gb_hbm: Any
    gu_slots: Any
    terms: Any
    hidden_hbm: Any
    down_hbm: Any
    every_hbm: Any
    gu_every: Any
    feed: Any
    terms_out: Any
    pre: Any
    up_in: Any
    down_in: Any
    part: Any
    first: Any
    over: Any
    joined: Any
    last: Any
    x: Any
    acc: Any
    stage: Any
    stage_load: Any
    every: Any
    slots: Any
    gu_own: Any
    gated: Any
    dqkv: Any
    heads: Any
    gb: Any
    hidden: Any
    down_map: Any
    terms_in: Any
    terms_all: Any
    s_send: Any
    s_recv: Any
    m_send: Any
    m_recv: Any
    t_send: Any
    t_recv: Any
    loads: Any


def close_kernel(size, parts, made, *refs):
    named = len(CloseRefs._fields)
    r, sems = CloseRefs(*refs[:named]), refs[named:]
    rank = lax.axis_index("seq")
    group = Group(size)
    me = group.me
    line_u, line_q = Line(parts, sems[:6]), Line(parts, sems[6:12])
    n, z = line_q.length, line_q.z
    sums = MixedSum(
        r.stage, r.stage_load, line_q, r.x, r.pre, r.acc, r.up_in, r.down_in, sems[12:]
    )
    rows = r.feed.shape[0]
    half = rows // 2
    barrier = pltpu.get_barrier_semaphore()
    greet_group(barrier, size)
    for step in range(1, parts):
        peer = lax.rem(rank + step, parts)
        pl.semaphore_signal(barrier, inc=1, device_id={"seq": peer}, device_id_type=MESH_ID)
    moves = [
        (r.gu_slots, r.gu_own),
        (r.hidden_hbm, r.hidden),
        (r.down_hbm, r.down_map),
    ]
    if made:
        moves += [
            (r.gated_hbm, r.gated),
            (r.dqkv_hbm, r.dqkv),
            (r.heads_hbm, r.heads),
            (r.gb_hbm, r.gb),
        ]
    else:
        moves += [(r.gated_hbm, r.x)]
    fetches = [
        pltpu.make_async_copy(src, dst, r.loads.at[k]) for k, (src, dst) in enumerate(moves)
    ]
    for k in [0] + list(range(3, len(moves))) + [1, 2]:
        fetches[k].start()
    r.terms_in[me] = r.terms[me]
    own_slots = pltpu.make_async_copy(r.gu_own, r.gu_every.at[rank], r.loads.at[0])
    fetches[0].wait()
    own_slots.start()
    own_slots.wait()
    pl.semaphore_wait(barrier, size + parts - 2)
    line_u.gather(lambda owner: r.gu_every.at[owner])

    def swap(k, step):
        peer = lax.rem(me + step, size)
        src, dst = (
            lambda: (r.terms.at[peer], r.terms_in.at[me]),
            lambda: (r.acc.at[z, peer], r.slots.at[me]),
        )[k]()
        return remote(src, dst, r.m_send.at[k, step - 1], r.m_recv.at[k, step - 1], fsdp=peer)

    others = range(1, size)
    for step in others:
        swap(0, step).start()

    scatter = Scatter(
        group, r.part, r.first, r.over, r.joined, r.last, r.s_send, r.s_recv
    )

    def down(step, is_step):
        partial = dot(r.hidden[group.to_own(step)], r.down_map[...])
        is_step(size - 1)(lambda: r.feed.__setitem__(..., partial))
        pl.when(step < size - 1)(lambda: r.part.__setitem__(step, partial.astype(BF)))
        for k in range(size - 1):
            is_step(k)(functools.partial(scatter.made, k))

    for fetch in fetches[3:]:
        fetch.wait()
    if made:
        span = r.gated.shape[1] // (size // 2)
        for h in range(size // 2):
            lanes = slice(h * span, (h + 1) * span)
            pack_pair(
                r.x, h, r.gated[:, lanes], r.dqkv[...], r.heads[...], r.gb[:, lanes]
            )
    sums.trade()
    line_u.relay(1)
    fetches[1].wait()
    fetches[2].wait()
    for m in range(n):
        sums.begin(m)
    each_step(size, down)

    for step in others:
        swap(0, step).wait_recv()
    small = r.terms_in[0]
    for f in others:
        small = small + r.terms_in[f]
    r.terms_all[rank] = small

    def spread(step):
        peer = lax.rem(rank + step, parts)
        view = r.terms_all.at[rank]
        return remote(view, view, r.t_send.at[step - 1], r.t_recv.at[step - 1], seq=peer)

    for step in range(1, parts):
        spread(step).start()
    scatter.join()

    for t in range(1, n - 1):
        sums.advance(t)
        line_u.relay(t + 1)
    for h in range(2):
        span = slice(h * half, (h + 1) * half)
        r.feed[span, :] = r.feed[span, :] + scatter.total(h)
    sums.total()
    for step in others:
        swap(1, step).start()
    for j in range(1, n):
        line_u.close(j)
    r.slots[me] = r.acc[z, me]
    for step in others:
        swap(1, step).wait_recv()
    local = r.x.shape[3] // 4
    lane = lax.broadcasted_iota(jnp.int32, (1, 1, 4 * local), 2)
    r.every[rank] = jnp.where(lane < 3 * local, r.slots[...], r.acc[z])
    line_q.gather(lambda owner: r.every.at[owner])
    line_u.gathered()
    for j in range(1, n):
        line_q.relay(j)
    for j in range(1, n):
        line_q.close(j)
    line_q.gathered()
    store = pltpu.make_async_copy(r.every, r.every_hbm, r.loads.at[1])
    store.start()
    for step in range(1, parts):
        spread(step).wait_recv()
    small = r.terms_all[0]
    for k in range(1, parts):
        small = small + r.terms_all[k]
    r.terms_out[...] = small
    for k in range(2):
        for step in others:
            swap(k, step).wait_send()
    for step in range(1, parts):
        spread(step).wait_send()
    scatter.finish()
    sums.finish()
    line_u.finish()
    line_q.finish()
    store.wait()


def close_part(ident, gated, dqkv, heads, gb, gu_slots, terms, hidden, down_weight):
    size, parts = lax.axis_size("fsdp"), lax.axis_size("seq")
    width = gated.shape[1]
    made = packs(size, parts, width)
    piece, cols = width // (size * parts), dqkv.shape[1] + heads.shape[1]
    if not made:
        gated = pack_plain(parts, size, gated, dqkv, heads, gb)
    n = parts // 2
    rows = hidden.shape[1]
    vmem = pl.BlockSpec(memory_space=pltpu.VMEM)
    hbm = pl.BlockSpec(memory_space=pl.ANY)
    dma = lambda *s: pltpu.SemaphoreType.DMA(s)
    gu_shape = (parts,) + gu_slots.shape
    packed = (parts, size, piece, cols)
    scratch = scatter_shapes(size, rows, width)
    low = lambda *s: jax.ShapeDtypeStruct(s, BF)
    copy_of = lambda a: pltpu.VMEM(a.shape if made else (8, 128), BF)
    return pl.pallas_call(
        functools.partial(close_kernel, size, parts, made),
        out_shape=[
            low(*packed),
            low(*gu_shape),
            jax.ShapeDtypeStruct((rows, width), F32),
            jax.ShapeDtypeStruct(terms.shape[1:], F32),
        ]
        + [low(n, size, piece, cols)] * 3,
        in_specs=[hbm] * 5 + [vmem, hbm, hbm],
        out_specs=[hbm, hbm, vmem, vmem, hbm, hbm, hbm],
        scratch_shapes=scratch[:-2]
        + [
            pltpu.VMEM(packed, BF),
            pltpu.VMEM((n, size, piece, cols), BF),
            pltpu.VMEM((2, size, piece, cols), BF),
            dma(2),
            pltpu.VMEM(packed, BF),
            pltpu.VMEM((size, piece, cols), BF),
            pltpu.VMEM(gu_slots.shape, BF),
            copy_of(gated),
            copy_of(dqkv),
            copy_of(heads),
            copy_of(gb),
            pltpu.VMEM(hidden.shape, BF),
            pltpu.VMEM(down_weight.shape, BF),
            pltpu.VMEM(terms.shape, F32),
            pltpu.VMEM((parts,) + terms.shape[1:], F32),
        ]
        + scratch[-2:]
        + [dma(2, size - 1)] * 2
        + [dma(parts - 1)] * 2
        + [dma(7)]
        + line_sems(parts) * 3,
        compiler_params=pltpu.CompilerParams(
            collective_id=ident, has_side_effects=True, vmem_limit_bytes=67_000_000
        ),
        cost_estimate=pl.CostEstimate(
            flops=2 * size * rows * (down_weight.size + width * cols),
            bytes_accessed=500_000_000,
            transcendentals=0,
        ),
        name="close_part",
    )(gated, dqkv, heads, gb, gu_slots, terms, hidden, down_weight)[:4]


def pack_pair(out, pair, x, g, heads=None, gb=None):
    parts, _, piece, _ = out.shape
    rows = parts * piece
    full = dot_rows(x, g)
    side = None if heads is None else dot_rows(heads, gb)
    for k in range(2):
        own = full[k * rows : (k + 1) * rows]
        if side is not None:
            wide = side.shape[1] // 2
            own = jnp.concatenate([own, side[:, k * wide : (k + 1) * wide]], 1)
        out[:, pair * 2 + k] = own.astype(BF).reshape(parts, piece, own.shape[1])


def pack_kernel(x_ref, g_ref, out_ref):
    pack_pair(out_ref, 0, x_ref[...], g_ref[...])


def down_kernel(x_ref, g_ref, out_ref):
    out_ref[...] = dot_rows(x_ref[...], g_ref[...]).astype(BF)


def down_grad(x, g):
    total, inner = x.shape
    half = g.shape[1] // 2
    return pl.pallas_call(
        down_kernel,
        grid=(2,),
        out_shape=jax.ShapeDtypeStruct((inner, 2 * half), BF),
        in_specs=[
            pl.BlockSpec(x.shape, lambda i: (0, 0), pipeline_mode=pl.Buffered(1)),
            pl.BlockSpec((total, half), lambda i: (0, i)),
        ],
        out_specs=pl.BlockSpec((inner, half), lambda i: (0, i)),
        cost_estimate=pl.CostEstimate(
            flops=4 * total * inner * half,
            bytes_accessed=2 * (x.size + g.size) + 4 * inner * half,
            transcendentals=0,
        ),
        name="down_grad",
    )(x, g)


def packs(size, parts, width):
    return width // (size * parts) % 8 == 0 and 2 * width // size % 128 == 0


def pack_plain(parts, size, x, g, heads=None, gb=None):
    width, cols = x.shape[1], g.shape[1]
    piece = width // (size * parts)
    full = dot_rows(x, g).reshape(size, parts, piece, cols)
    if heads is not None:
        side = dot_rows(heads, gb).reshape(parts, piece, size, -1).transpose(2, 0, 1, 3)
        full = jnp.concatenate([full, side], 3)
    return full.transpose(1, 0, 2, 3).astype(BF)


def pack_grads(parts, size, x, g):
    total, width = x.shape
    cols = g.shape[1]
    if not packs(size, parts, width):
        return pack_plain(parts, size, x, g)
    piece = width // (size * parts)
    pair = pl.BlockSpec((total, 2 * width // size), lambda i: (0, i))
    whole = pl.BlockSpec(g.shape, lambda i: (0, 0), pipeline_mode=pl.Buffered(1))
    return pl.pallas_call(
        pack_kernel,
        grid=(size // 2,),
        out_shape=jax.ShapeDtypeStruct((parts, size, piece, cols), BF),
        in_specs=[pair, whole],
        out_specs=pl.BlockSpec((parts, 2, piece, cols), lambda i: (0, i, 0, 0)),
        cost_estimate=pl.CostEstimate(
            flops=2 * total * width * cols,
            bytes_accessed=2 * (x.size + g.size + width * cols),
            transcendentals=0,
        ),
        name="pack_grads",
    )(x, g)


def unpack_kernel(widths, *refs):
    outs = list(refs[len(widths) :])
    for every_ref, wide in zip(refs, widths):
        blocks = [every_ref[0, i].astype(F32) for i in range(every_ref.shape[1])]
        low = 0
        for width in wide:
            outs.pop(0)[...] = jnp.concatenate([b[:, low : low + width] for b in blocks], 1)
            low += width


def unpack_grads(arrays, widths):
    parts, size, piece, _ = arrays[0].shape
    every = [w for wide in widths for w in wide]
    if piece % 8:
        outs = []
        for array, wide in zip(arrays, widths):
            low = 0
            for width in wide:
                block = array[:, :, :, low : low + width].transpose(0, 2, 1, 3)
                outs.append(block.reshape(parts * piece, size * width).astype(F32))
                low += width
        return outs
    return pl.pallas_call(
        functools.partial(unpack_kernel, widths),
        grid=(parts,),
        out_shape=[jax.ShapeDtypeStruct((parts * piece, size * w), F32) for w in every],
        in_specs=[
            pl.BlockSpec((1, size, piece, a.shape[3]), lambda i: (i, 0, 0, 0)) for a in arrays
        ],
        out_specs=[pl.BlockSpec((piece, size * w), lambda i: (i, 0)) for w in every],
        cost_estimate=pl.CostEstimate(
            flops=0, bytes_accessed=6 * sum(a.size for a in arrays), transcendentals=0
        ),
        name="unpack_grads",
    )(*arrays)


def columns_piece(weights, part, parts):
    size = lax.axis_size("fsdp")
    rows = weights[0].shape[0] // parts
    pieces = []
    for weight in weights:
        own = lax.dynamic_slice_in_dim(weight, part * rows, rows, 0)
        pieces.append(own.reshape(rows, size, -1))
    return jnp.concatenate(pieces, 2).transpose(1, 0, 2)


def shards(
    tokens,
    seq_lengths,
    seq_offsets,
    norm1_gain,
    conv_weight,
    query_weight,
    key_weight,
    value_weight,
    out_weight,
    norm2_gain,
    gate_weight,
    up_weight,
    down_weight,
    cotangent,
):
    size = lax.axis_size("fsdp")
    parts = lax.axis_size("seq")
    part = lax.axis_index("seq")
    me = lax.axis_index("fsdp")
    own_tokens = tokens[0]
    rows, width = own_tokens.shape
    slice_width = norm1_gain.shape[0]
    first_slot = part * rows
    count = seq_lengths.shape[1]

    slot_ext = first_slot - 2 + jnp.arange(rows + 2, dtype=jnp.int32)
    segment_ext = segment_of(
        slot_ext, count, lambda j: seq_lengths[0, j], lambda j: seq_offsets[0, j]
    )
    segment_own = segment_ext[2:]
    same_one = (segment_own == segment_ext[1:-1]).astype(F32)[:, None]
    same_two = (segment_own == segment_ext[:-2]).astype(F32)[:, None]
    live_mask = (segment_own >= 0).astype(F32)[:, None]

    gains = jnp.concatenate(
        [
            norm1_gain[None],
            norm2_gain[None],
            conv_weight.T,
            jnp.zeros((3, slice_width), BF),
        ],
        0,
    )
    table = jnp.zeros((8, 128), jnp.int32)
    table = table.at[0, :count].set(seq_lengths[0]).at[1, :count].set(seq_offsets[0])
    qkv_piece = columns_piece((query_weight, key_weight, value_weight), part, parts)
    gu_piece = columns_piece((gate_weight, up_weight), part, parts)
    (
        gated_all,
        qkv,
        edge,
        qkv_map,
        middle,
        heads_out,
        grad_down_all,
        normed_all,
        hidden,
        grad_gu,
        gu_map,
        gains_all,
        table_all,
        edge_tokens,
    ) = forward_part(
        0,
        count,
        own_tokens,
        cotangent[0],
        gains,
        table,
        qkv_piece,
        gu_piece,
        out_weight,
        down_weight,
    )
    local = out_weight.shape[0]
    flat = lambda a: a.reshape(-1, a.shape[-1])
    lens_all, starts_all = table_all[:, 0, :count], table_all[:, 1, :count]
    gains_all = gains_all.transpose(1, 0, 2).reshape(8, width)
    norm_one = gains_all[0].astype(F32)
    norm_two = gains_all[1].astype(F32)
    taps = gains_all[2:5].astype(F32)
    qkv_map, gu_map = qkv_map.reshape(width, -1), gu_map.reshape(width, -1)

    extended = jnp.concatenate([edge_tokens[6:], own_tokens], 0).astype(F32)
    scale_one = lax.rsqrt(jnp.mean(extended * extended, axis=1, keepdims=True) + EPS)
    normed = extended * scale_one * norm_one
    conv_mix = (
        normed[2:] * taps[0]
        + same_one * normed[1:-1] * taps[1]
        + same_two * normed[:-2] * taps[2]
    )

    gu_packed = pack_grads(parts, size, flat(normed_all), flat(grad_gu))
    down_packed = down_grad(flat(hidden), flat(grad_down_all))
    grad_middle, norm2_term, grad_branch_all, dqkv, grad_gated, gu_slots, down_every = back_part(
        4,
        lens_all,
        starts_all,
        grad_gu,
        gu_map,
        middle,
        grad_down_all,
        norm_two[None],
        out_weight,
        edge,
        qkv,
        qkv_map,
        gu_packed,
        down_packed.reshape(parts, -1, width),
    )
    norm2_term = norm2_term[0]
    down_total = down_every.reshape(-1, width).astype(F32)
    normed_own = normed[2:]
    grad_mix = grad_gated * normed_own
    part_zero = jnp.pad(grad_gated * conv_mix + grad_mix * taps[0], ((2, 0), (0, 0)))
    part_one = jnp.pad(grad_mix * same_one * taps[1], ((1, 1), (0, 0)))
    part_two = jnp.pad(grad_mix * same_two * taps[2], ((0, 2), (0, 0)))
    grad_normed = part_zero + part_one + part_two
    unit_one = extended * scale_one
    grad_unit_one = grad_normed * norm_one
    grad_extended = scale_one * (
        grad_unit_one - unit_one * jnp.mean(grad_unit_one * unit_one, axis=1, keepdims=True)
    )
    edge_back = shifted(grad_extended[:2], "seq", -1)
    tokens_grad = grad_middle + grad_extended[2:] + jnp.pad(edge_back, ((rows - 2, 0), (0, 0)))

    terms = jnp.stack(
        [
            jnp.sum(grad_normed * unit_one, axis=0),
            norm2_term,
            jnp.sum(grad_mix * normed_own, axis=0),
            jnp.sum(grad_mix * same_one * normed[1:-1], axis=0),
            jnp.sum(grad_mix * same_two * normed[:-2], axis=0),
        ]
    )
    terms = jnp.pad(terms, ((0, 3), (0, 0))).reshape(8, size, slice_width).transpose(1, 0, 2)
    gu_slots, terms, down_total, tokens_grad = lax.optimization_barrier(
        (gu_slots, terms, down_total, tokens_grad)
    )
    qkvo_every, gu_every, feed, terms = close_part(
        5,
        flat(gated_all),
        flat(dqkv),
        flat(heads_out),
        flat(grad_branch_all),
        gu_slots,
        terms,
        hidden,
        down_weight,
    )
    gate_total, up_total, query_total, key_total, value_total, out_total = unpack_grads(
        (gu_every, qkvo_every), ((gu_map.shape[1] // 2,) * 2, (local,) * 4)
    )

    layer_out = (live_mask * (middle + feed)).astype(BF)[None]
    return (
        layer_out,
        tokens_grad[None],
        terms[0],
        terms[2:5].T,
        query_total,
        key_total,
        value_total,
        out_total,
        terms[1],
        gate_total,
        up_total,
        down_total,
    )


def solution(mesh):
    placed = (
        P("fsdp", "seq", None),
        P("fsdp", None),
        P("fsdp", None),
        P("fsdp"),
        P("fsdp", None),
        P("fsdp", None),
        P("fsdp", None),
        P("fsdp", None),
        P("fsdp", None),
        P("fsdp"),
        P("fsdp", None),
        P("fsdp", None),
        P("fsdp", None),
        P("fsdp", "seq", None),
    )
    return jax.shard_map(
        shards,
        mesh=mesh,
        in_specs=placed,
        out_specs=(
            P("fsdp", "seq", None),
            P("fsdp", "seq", None),
            P("fsdp"),
            P("fsdp", None),
            P("fsdp", None),
            P("fsdp", None),
            P("fsdp", None),
            P("fsdp", None),
            P("fsdp"),
            P("fsdp", None),
            P("fsdp", None),
            P("fsdp", None),
        ),
        check_vma=False,
    )
```

```python
import functools
from typing import Any, NamedTuple

import jax
import jax.numpy as jnp
from jax import lax
from jax.experimental import pallas as pl
from jax.experimental.pallas import tpu as pltpu
from jax.sharding import PartitionSpec as P

HEADS = 16
WINDOW = 64
HEAD_DIM = 112
BLOCK = 128

EPS = 1e-05
NEG = -1e30
SCALE = HEAD_DIM ** (-0.5)
MESH_ID = pl.DeviceIdType.MESH
BF = jnp.bfloat16
F32 = jnp.float32


def shifted(array, axis, by):
    length = lax.axis_size(axis)
    pairs = [(i, i + by) for i in range(length) if 0 <= i + by < length]
    return lax.ppermute(array, axis, pairs)


def segment_of(slot, count, lengths, starts):
    found = jnp.full(slot.shape, -1, jnp.int32)
    for j in range(count):
        inside = (slot >= starts(j)) & (slot < starts(j) + lengths(j))
        found = jnp.where(inside, j, found)
    return jnp.where(slot < 0, -2, found)


def dot_rows(left, right):
    return lax.dot_general(left, right, (((0,), (0,)), ((), ())), preferred_element_type=F32)


def dot_trans(left, right):
    return lax.dot_general(left, right, (((1,), (1,)), ((), ())), preferred_element_type=F32)


def dot(left, right):
    return jnp.dot(left, right, preferred_element_type=F32)


def masks_of(first, block, count, length, start):
    rows = first + block * BLOCK
    query = rows + lax.broadcasted_iota(jnp.int32, (BLOCK, 1), 0)
    keys = rows - WINDOW + lax.broadcasted_iota(jnp.int32, (1, BLOCK + WINDOW), 1)
    seg_q = segment_of(query, count, length, start)
    seg_k = segment_of(keys, count, length, start)
    far = query - keys
    return (far >= 0) & (far <= WINDOW) & (seg_q == seg_k)


def soft_of(query, keys, mask):
    scores = dot_trans(query, keys) * SCALE
    scores = jnp.where(mask, scores, NEG)
    peak = jnp.max(scores, axis=1, keepdims=True)
    exponent = jnp.exp(scores - peak)
    return exponent / jnp.sum(exponent, axis=1, keepdims=True)


def lane_head(width):
    return lax.broadcasted_iota(jnp.int32, (1, width), 1) // HEAD_DIM


def remote(src, dst, send, recv, **peer):
    return pltpu.make_async_remote_copy(
        src_ref=src,
        dst_ref=dst,
        send_sem=send,
        recv_sem=recv,
        device_id=peer,
        device_id_type=MESH_ID,
    )


def greet_group(barrier, size):
    me = lax.axis_index("fsdp")
    for step in range(1, size):
        peer = lax.rem(me + step, size)
        pl.semaphore_signal(barrier, inc=1, device_id={"fsdp": peer}, device_id_type=MESH_ID)


class Group:
    def __init__(self, size):
        self.size = size
        self.me = lax.axis_index("fsdp")
        self.square = size == 4
        if self.square:
            x, y = lax.rem(self.me, 2), self.me // 2
            self.at = lambda bx, by: lax.rem(y + by, 2) * 2 + lax.rem(x + bx, 2)
            self.x, self.y, self.far = self.at(1, 0), self.at(0, 1), self.at(1, 1)

    def from_own(self, step):
        if self.square:
            return self.at(lax.rem(step, 2), step // 2)
        return lax.rem(self.me - step + self.size, self.size)

    def to_own(self, step):
        if self.square:
            return self.at(1 - step // 2, 1 - lax.rem(step, 2))
        return lax.rem(self.me + 1 + step, self.size)


class Gather:
    def __init__(self, group, ref, send, recv):
        self.group, self.ref, self.send, self.recv = group, ref, send, recv
        self.half = ref.shape[1] // 2

    def part(self, k, slot, half, peer):
        view = self.ref.at[slot, pl.ds(half * self.half, self.half)]
        return remote(view, view, self.send.at[k], self.recv.at[k], fsdp=peer)

    def whole(self, k):
        g = self.group
        view = self.ref.at[g.me]
        sems = self.send.at[k - 1], self.recv.at[k - 1]
        return remote(view, view, *sems, fsdp=lax.rem(g.me + k, g.size))

    def copy(self, k):
        g = self.group
        if not g.square:
            return self.whole(k + 1)
        slot = (g.me, g.me, g.me, g.me, g.x, g.y)[k]
        half = (0, 1, 0, 1, 0, 1)[k]
        return self.part(k, slot, half, (g.x, g.x, g.y, g.y, g.y, g.x)[k])

    def start_half(self, half):
        if self.group.square:
            self.copy(half).start()
            self.copy(2 + half).start()
        elif half == 1:
            for k in range(self.group.size - 1):
                self.copy(k).start()

    def relay(self):
        if self.group.square:
            self.copy(0).wait_recv()
            self.copy(4).start()
            self.copy(3).wait_recv()
            self.copy(5).start()

    def ready(self, step):
        if not self.group.square:
            self.copy(step - 1).wait_recv()
        elif step == 3:
            self.copy(4).wait_recv()
            self.copy(5).wait_recv()
        else:
            self.copy(step).wait_recv()

    def finish(self):
        for k in range(transfers(self.group.size)):
            self.copy(k).wait_send()


class Scatter:
    def __init__(self, group, part, first, over, joined, last, send, recv):
        self.group, self.part = group, part
        self.first, self.over, self.joined, self.last = first, over, joined, last
        self.send, self.recv = send, recv
        self.half = part.shape[1] // 2

    def copy(self, k):
        g, half = self.group, self.half
        low, high = pl.ds(0, half), pl.ds(half, half)
        if not g.square:
            src, dst, peer = self.part.at[k], self.first.at[k], lax.rem(g.me + 1 + k, g.size)
        else:
            src, dst, peer = (
                lambda: (self.part.at[0, low], self.over.at[0], g.x),
                lambda: (self.part.at[0, high], self.over.at[1], g.y),
                lambda: (self.part.at[1, low], self.first.at[0], g.x),
                lambda: (self.part.at[2, high], self.first.at[1], g.y),
                lambda: (self.joined.at[0], self.last.at[0], g.y),
                lambda: (self.joined.at[1], self.last.at[1], g.x),
            )[k]()
        return remote(src, dst, self.send.at[k], self.recv.at[k], fsdp=peer)

    def made(self, step):
        if not self.group.square:
            self.copy(step).start()
        elif step == 0:
            self.copy(0).start()
            self.copy(1).start()
        elif step in (1, 2):
            self.copy(step + 1).start()

    def join(self):
        if not self.group.square:
            return
        half = self.half
        for k, (step, rows) in enumerate(((2, slice(0, half)), (1, slice(half, 2 * half)))):
            self.copy(k).wait_recv()
            own = self.part[step, rows].astype(F32)
            self.joined[k] = (own + self.over[k].astype(F32)).astype(BF)
            self.copy(4 + k).start()

    def total(self, half):
        count = self.half
        if self.group.square:
            self.copy(2 + half).wait_recv()
            self.copy(4 + half).wait_recv()
            return self.first[half].astype(F32) + self.last[half].astype(F32)
        if half == 0:
            for k in range(self.group.size - 1):
                self.copy(k).wait_recv()
        rows = slice(half * count, (half + 1) * count)
        out = self.first[0, rows].astype(F32)
        for k in range(1, self.group.size - 1):
            out = out + self.first[k, rows].astype(F32)
        return out

    def finish(self):
        for k in range(transfers(self.group.size)):
            self.copy(k).wait_send()


class Line:
    def __init__(self, parts, sems):
        self.rank = lax.axis_index("seq")
        self.parts, self.length = parts, parts // 2
        self.z, self.core = self.rank // 2, lax.rem(self.rank, 2)
        self.above, self.below = self.rank + 2, self.rank - 2
        self.beside = self.rank + 1 - 2 * self.core
        self.has_above, self.has_below = self.z < self.length - 1, self.z > 0
        self.sems = sems

    def greet(self, barrier):
        def one(peer):
            pl.semaphore_signal(barrier, inc=1, device_id={"seq": peer}, device_id_type=MESH_ID)

        one(self.beside)
        pl.when(self.has_above)(lambda: one(self.above))
        pl.when(self.has_below)(lambda: one(self.below))
        n, z = self.length, self.z
        return 1 + (2 * n - 2 - z) // n + (z + n - 1) // n

    def up(self, k, owner):
        view = self.view(owner)
        return remote(view, view, self.sems[0].at[k], self.sems[1].at[k], seq=self.above)

    def down(self, k, owner):
        view = self.view(owner)
        return remote(view, view, self.sems[2].at[k], self.sems[3].at[k], seq=self.below)

    def side(self, k, owner):
        view = self.view(owner)
        return remote(view, view, self.sems[4].at[k], self.sems[5].at[k], seq=self.beside)

    def gather(self, view):
        self.view = view
        pl.when(self.has_above)(lambda: self.up(0, self.rank).start())
        pl.when(self.has_below)(lambda: self.down(0, self.rank).start())
        self.side(self.z, self.rank).start()

    def own_up(self):
        pl.when(self.has_above)(lambda: self.up(0, self.rank).start())

    def own_down(self):
        pl.when(self.has_below)(lambda: self.down(0, self.rank).start())

    def relay_up(self, j):
        rank, z = self.rank, self.z

        @pl.when((z >= j) & self.has_above)
        def _():
            self.up(j - 1, rank).wait_recv()
            self.up(j, rank - 2 * j).start()
            self.side(z - j, rank - 2 * j).start()

    def relay_down(self, j):
        rank, z = self.rank, self.z

        @pl.when((z + j < self.length) & self.has_below)
        def _():
            self.down(j - 1, rank).wait_recv()
            self.down(j, rank + 2 * j).start()
            self.side(z + j, rank + 2 * j).start()

    def relay(self, j):
        self.relay_up(j)
        self.relay_down(j)

    def close(self, j):
        rank, z = self.rank, self.z

        @pl.when((z >= j) & (z == self.length - 1))
        def _():
            self.up(j - 1, rank).wait_recv()
            self.side(z - j, rank - 2 * j).start()

        @pl.when((z + j < self.length) & (z == 0))
        def _():
            self.down(j - 1, rank).wait_recv()
            self.side(z + j, rank + 2 * j).start()

    def gathered(self):
        for k in range(self.length):
            self.side(k, self.rank).wait_recv()

    def finish(self):
        rank, z = self.rank, self.z
        for k in range(self.length):
            self.side(k, rank).wait_send()
        pl.when(self.has_above)(lambda: self.up(0, rank).wait_send())
        pl.when(self.has_below)(lambda: self.down(0, rank).wait_send())
        for j in range(1, self.length):
            pl.when((z >= j) & self.has_above)(lambda: self.up(j, rank).wait_send())
            pl.when((z + j < self.length) & self.has_below)(lambda: self.down(j, rank).wait_send())


class LineSum:
    def __init__(self, line, x, pre, acc, up_in, down_in, sems):
        self.line, self.x, self.pre, self.acc = line, x, pre, acc
        self.up_in, self.down_in, self.sems = up_in, down_in, sems

    def share(self, k):
        line = self.line
        src = self.x.at[2 * k + 1 - line.core]
        return remote(src, self.pre.at[k], self.sems[0].at[k], self.sems[1].at[k], seq=line.beside)

    def up(self, k):
        sems = self.sems[2].at[k], self.sems[3].at[k]
        return remote(self.acc.at[k], self.up_in.at[k], *sems, seq=self.line.above)

    def down(self, k):
        sems = self.sems[4].at[k], self.sems[5].at[k]
        return remote(self.acc.at[k], self.down_in.at[k], *sems, seq=self.line.below)

    def pair(self, m):
        return self.line.length - 1 - m, m

    def trade(self):
        n = self.line.length
        for m in range((n + 1) // 2):
            for k in sorted(set(self.pair(m))):
                self.share(k).start()

    def merge(self, k):
        self.share(k).wait_recv()
        own = self.x[2 * k + self.line.core].astype(F32)
        self.acc[k] = (own + self.pre[k].astype(F32)).astype(BF)

    def begin(self, m):
        n, z = self.line.length, self.line.z
        far, near = self.pair(m)
        if m < (n + 1) // 2:
            for k in sorted({far, near}):
                self.merge(k)
        if m < n - 1:
            pl.when(z == 0)(lambda: self.up(far).start())
            pl.when(z == n - 1)(lambda: self.down(near).start())

    def add(self, k, more):
        self.acc[k] = (self.acc[k].astype(F32) + more[k].astype(F32)).astype(BF)

    def advance(self, t):
        z, n = self.line.z, self.line.length
        far, near = n - 1 + z - t, t - n + 1 + z

        @pl.when((z >= 1) & (z <= t))
        def _():
            self.up(far).wait_recv()
            self.add(far, self.up_in)
            self.up(far).start()

        @pl.when((z <= n - 2) & (z >= n - 1 - t))
        def _():
            self.down(near).wait_recv()
            self.add(near, self.down_in)
            self.down(near).start()

    def total(self):
        z = self.line.z

        @pl.when(z > 0)
        def _():
            self.up(z).wait_recv()
            self.add(z, self.up_in)

        @pl.when(z < self.line.length - 1)
        def _():
            self.down(z).wait_recv()
            self.add(z, self.down_in)

    def finish(self):
        for k in range(self.line.length):
            self.share(k).wait_send()
            pl.when(k > self.line.z)(lambda: self.up(k).wait_send())
            pl.when(k < self.line.z)(lambda: self.down(k).wait_send())


class StagedSum(LineSum):
    def __init__(self, stage, load, *args):
        super().__init__(*args)
        self.stage, self.load = stage, load

    def fetch(self, slot, src):
        return pltpu.make_async_copy(src, self.stage.at[slot], self.load.at[slot])

    def merge(self, k):
        self.share(k).wait_recv()
        own = self.fetch(0, self.x.at[2 * k + self.line.core])
        other = self.fetch(1, self.pre.at[k])
        own.start()
        other.start()
        own.wait()
        other.wait()
        self.acc[k] = (self.stage[0].astype(F32) + self.stage[1].astype(F32)).astype(BF)

    def add(self, k, more):
        came = self.fetch(0, more.at[k])
        came.start()
        came.wait()
        self.acc[k] = (self.acc[k].astype(F32) + self.stage[0].astype(F32)).astype(BF)


class MixedSum(StagedSum):
    def merge(self, k):
        self.share(k).wait_recv()
        other = self.fetch(1, self.pre.at[k])
        other.start()
        other.wait()
        own = self.x[2 * k + self.line.core].astype(F32)
        self.acc[k] = (own + self.stage[1].astype(F32)).astype(BF)


def line_sems(parts):
    return [pltpu.SemaphoreType.DMA((parts // 2,))] * 6


def transfers(size):
    return 6 if size == 4 else size - 1


def scatter_shapes(size, rows, width):
    half = rows // 2
    slots = (2, half, width) if size == 4 else (size - 1, rows, width)
    return [
        pltpu.VMEM((size - 1, rows, width), BF),
        pltpu.VMEM(slots, BF),
        pltpu.VMEM((2, half, width), BF),
        pltpu.VMEM((2, half, width), BF),
        pltpu.VMEM((2, half, width), BF),
        pltpu.SemaphoreType.DMA((transfers(size),)),
        pltpu.SemaphoreType.DMA((transfers(size),)),
    ]


def each_step(size, body):
    def one(step, carry):
        body(step, lambda k: pl.when(step == k))
        return carry

    lax.fori_loop(0, size, one, 0)


class ForwardRefs(NamedTuple):
    tokens: Any
    cot: Any
    gains: Any
    table: Any
    qkv_piece: Any
    gu_piece: Any
    out_map: Any
    down_map: Any
    gated_hbm: Any
    qkv_hbm: Any
    edge: Any
    qkv_map_hbm: Any
    middle: Any
    heads: Any
    grads_hbm: Any
    norm_hbm: Any
    hidden_hbm: Any
    gu_grad_hbm: Any
    gu_map_hbm: Any
    gains_all: Any
    table_all: Any
    edge_tok: Any
    part: Any
    first: Any
    over: Any
    joined: Any
    last: Any
    all: Any
    grads: Any
    qkv: Any
    qkv_map: Any
    gu_map: Any
    tail: Any
    own: Any
    grad_hidden: Any
    hidden: Any
    gu_grad: Any
    s_send: Any
    s_recv: Any
    a_send: Any
    a_recv: Any
    g_send: Any
    g_recv: Any
    c_send: Any
    c_recv: Any
    m_send: Any
    m_recv: Any
    halo_send: Any
    halo_recv: Any
    edge_send: Any
    edge_recv: Any
    loads: Any
    stores: Any
    hidden_store: Any
    gu_store: Any


def forward_kernel(size, parts, count, *refs):
    named = len(ForwardRefs._fields)
    r, sems = ForwardRefs(*refs[:named]), refs[named:]
    rank = lax.axis_index("seq")
    rows = r.tokens.shape[0]
    half = rows // 2
    local = r.out_map.shape[0]
    inner = r.down_map.shape[0]
    slot = rank * rows
    group = Group(size)
    me = group.me
    line_q, line_u = Line(parts, sems[:6]), Line(parts, sems[6:])

    barrier = pltpu.get_barrier_semaphore()
    greet_group(barrier, size)
    known = line_q.greet(barrier)

    def greet(peer):
        pl.semaphore_signal(barrier, inc=1, device_id={"seq": peer}, device_id_type=MESH_ID)

    pl.when(line_q.has_above & (line_q.core == 1))(lambda: greet(rank + 1))
    pl.when(line_q.has_below & (line_q.core == 0))(lambda: greet(rank - 1))
    n, z = line_q.length, line_q.z
    known = known + (2 * n - 2 - z) // n * line_q.core + (z + n - 1) // n * (1 - line_q.core)
    own_pieces = [
        pltpu.make_async_copy(src.at[me], dst.at[me, rank], r.loads.at[k])
        for k, (src, dst) in enumerate(
            ((r.qkv_piece, r.qkv_map), (r.gu_piece, r.gu_map))
        )
    ]
    for copy in own_pieces:
        copy.start()
    r.gains_all[me] = r.gains[...]
    r.table_all[me] = r.table[...]
    own_table = r.table[...]
    slots = slot + lax.broadcasted_iota(jnp.int32, (rows, 1), 0)
    length = lambda j: own_table[0:1, j : j + 1]
    start = lambda j: own_table[1:2, j : j + 1]
    segment = segment_of(slots, count, length, start)
    r.grads[me] = jnp.where(segment >= 0, r.cot[...].astype(F32), 0.0).astype(BF)

    @pl.when(rank == 0)
    def _():
        r.edge_tok[...] = jnp.zeros_like(r.edge_tok)

    def edge_rows():
        last = r.tokens.at[pl.ds(rows - 8, 8)]
        return remote(last, r.edge_tok, r.edge_send, r.edge_recv, seq=rank + 1)

    pl.semaphore_wait(barrier, size - 1 + known)
    pl.when(rank < parts - 1)(lambda: edge_rows().start())

    def swap(k, step):
        peer = lax.rem(me + step, size)
        src, dst = (
            lambda: (r.gains_all.at[me], r.gains_all.at[me]),
            lambda: (r.table_all.at[me], r.table_all.at[me]),
            lambda: (r.qkv_piece.at[peer], r.qkv_map.at[me, rank]),
            lambda: (r.gu_piece.at[peer], r.gu_map.at[me, rank]),
        )[k]()
        return remote(src, dst, r.m_send.at[k, step - 1], r.m_recv.at[k, step - 1], fsdp=peer)

    others = range(1, size)
    for k in range(4):
        for step in others:
            swap(k, step).start()
    for k in range(2):
        for step in others:
            swap(k, step).wait_recv()

    gains = jnp.concatenate([r.gains_all[f] for f in range(size)], 1).astype(F32)
    same_one = (segment == segment_of(slots - 1, count, length, start)).astype(F32)
    same_two = (segment == segment_of(slots - 2, count, length, start)).astype(F32)
    tokens = r.tokens[...].astype(F32)
    pl.when(rank > 0)(lambda: edge_rows().wait_recv())
    edge = r.edge_tok[...].astype(F32)

    def norm(a):
        return a * lax.rsqrt(jnp.mean(a * a, axis=1, keepdims=True) + EPS) * gains[0:1]

    normed, edge = norm(tokens), norm(edge)
    row = lax.broadcasted_iota(jnp.int32, (rows, 1), 0)
    back_one = jnp.where(row == 0, edge[7:8], pltpu.roll(normed, 1, 0))
    back_two = jnp.where(
        row == 0, edge[6:7], jnp.where(row == 1, edge[7:8], pltpu.roll(normed, 2, 0))
    )
    mixed = (
        normed * gains[2:3]
        + same_one * back_one * gains[3:4]
        + same_two * back_two * gains[4:5]
    )
    all_ref = r.all
    all_ref[me] = (mixed * normed).astype(BF)
    gather = Gather(group, all_ref, r.a_send, r.a_recv)
    gather.start_half(0)
    gather.start_half(1)

    own_pieces[0].wait()
    for step in others:
        swap(2, step).wait_recv()
    line_q.gather(lambda owner: r.qkv_map.at[:, owner])
    line_u.view = lambda owner: r.gu_map.at[:, owner]
    gather.relay()
    grads = Gather(group, r.grads, r.c_send, r.c_recv)
    grads.start_half(0)
    grads.start_half(1)
    own_pieces[1].wait()
    for step in others:
        swap(3, step).wait_recv()
    line_u.side(z, rank).start()
    pl.when(z == 0)(line_u.own_up)
    pl.when(z == n - 1)(line_u.own_down)
    for j in range(1, n):
        line_q.relay(j)
        line_q.close(j)
        pl.when(z == j)(line_u.own_up)
        pl.when(z == n - 1 - j)(line_u.own_down)
    for step in others:
        gather.ready(step)
    grads.relay()
    line_q.gathered()
    keeps = [
        pltpu.make_async_copy(all_ref, r.gated_hbm, r.stores.at[size]),
        pltpu.make_async_copy(r.qkv_map, r.qkv_map_hbm, r.stores.at[size + 1]),
    ]
    for keep in keeps:
        keep.start()

    weights = r.qkv_map[...].reshape(-1, r.qkv_map.shape[3])

    def halo(step):
        g = group.to_own(step)
        sem = r.halo_send.at[step], r.halo_recv.at[step]
        return remote(r.tail.at[g], r.edge.at[g], *sem, seq=rank + 1)

    def project(step, is_step):
        g = group.to_own(step)
        out = dot(all_ref[g], weights).astype(BF)
        r.qkv[g] = out
        r.tail[g] = out[rows - WINDOW :, local:]
        pl.when(rank < parts - 1)(lambda: halo(step).start())

    each_step(size, project)

    @pl.when(rank == 0)
    def _():
        r.edge[...] = jnp.zeros_like(r.edge)

    keeps.append(pltpu.make_async_copy(r.qkv, r.qkv_hbm, r.stores.at[size + 2]))
    keeps[2].start()
    line_u.relay(1)
    gather.finish()
    keeps[0].wait()

    scatter = Scatter(
        group, r.part, r.first, r.over, r.joined, r.last, r.s_send, r.s_recv
    )
    head_of = lane_head(local)

    def mix(step, is_step):
        g = group.to_own(step)
        pl.when(rank > 0)(lambda: halo(step).wait_recv())
        own, edge, table = r.qkv[g], r.edge[g], r.table_all[g]
        queries = own[:, :local]
        keys = jnp.concatenate([edge[:, :local], own[:, local : 2 * local]], 0)
        values = jnp.concatenate([edge[:, local:], own[:, 2 * local :]], 0)
        outs = []
        for block in range(rows // BLOCK):
            mask = masks_of(
                slot,
                block,
                count,
                lambda j: table[0:1, j : j + 1],
                lambda j: table[1:2, j : j + 1],
            )
            low = block * BLOCK
            query = queries[low : low + BLOCK]
            key = keys[low : low + BLOCK + WINDOW]
            value = values[low : low + BLOCK + WINDOW]
            out = jnp.zeros((BLOCK, local), F32)
            for head in range(local // HEAD_DIM):
                mine = head_of == head
                soft = soft_of(jnp.where(mine, query, jnp.zeros_like(query)), key, mask)
                out = jnp.where(mine, dot(soft.astype(BF), value), out)
            outs.append(out.astype(BF))
        heads = jnp.concatenate(outs, 0)
        r.heads[g] = heads
        branch = dot(heads, r.out_map[...])
        is_step(size - 1)(lambda: r.own.__setitem__(..., branch))
        pl.when(step < size - 1)(lambda: r.part.__setitem__(step, branch.astype(BF)))
        for k in range(size - 1):
            is_step(k)(functools.partial(scatter.made, k))

    each_step(size, mix)
    scatter.join()
    for j in range(2, n):
        line_u.relay(j)
    gather = Gather(group, all_ref, r.g_send, r.g_recv)
    for h in range(2):
        span = slice(h * half, (h + 1) * half)
        total = r.own[span, :] + scatter.total(h)
        middle = r.tokens[span, :].astype(F32) + total
        r.middle[span, :] = middle
        scale = lax.rsqrt(jnp.mean(middle * middle, axis=1, keepdims=True) + EPS)
        all_ref[me, span] = (middle * scale * gains[1:2]).astype(BF)
        gather.start_half(h)
    gather.relay()

    def grad_of(step, is_step):
        g = group.from_own(step)
        for k in others:
            is_step(k)(functools.partial(grads.ready, k))
        r.grad_hidden[g] = dot_trans(r.grads[g], r.down_map[...])

    each_step(size, grad_of)
    for j in range(1, n):
        line_u.close(j)
    line_u.gathered()
    keeps.append(pltpu.make_async_copy(r.gu_map, r.gu_map_hbm, r.stores.at[size + 3]))
    keeps[3].start()

    def out_copies(step):
        g, two = group.from_own(step), lax.rem(step, 2)
        return (
            pltpu.make_async_copy(
                r.hidden.at[two], r.hidden_hbm.at[g], r.hidden_store.at[two]
            ),
            pltpu.make_async_copy(
                r.gu_grad.at[two], r.gu_grad_hbm.at[g], r.gu_store.at[two]
            ),
        )

    def norm_copy(g):
        return pltpu.make_async_copy(all_ref.at[g], r.norm_hbm.at[g], r.stores.at[g])

    def feed(step, is_step):
        g, two = group.from_own(step), lax.rem(step, 2)
        for k in others:
            is_step(k)(functools.partial(gather.ready, k))

        @pl.when(step >= 2)
        def _():
            for copy in out_copies(step - 2):
                copy.wait()

        norm_copy(g).start()
        weights = r.gu_map[...].reshape(-1, r.gu_map.shape[3])
        acts = dot(all_ref[g], weights)
        gate, up = acts[:, :inner], acts[:, inner:]
        sigma = jax.nn.sigmoid(gate)
        silu = gate * sigma
        r.hidden[two] = (silu * up).astype(BF)
        grad_hidden = r.grad_hidden[g]
        grad_gate = grad_hidden * up * sigma * (1.0 + gate * (1.0 - sigma))
        r.gu_grad[two] = jnp.concatenate([grad_gate, grad_hidden * silu], 1).astype(BF)
        for copy in out_copies(step):
            copy.start()

    each_step(size, feed)
    keeps.append(pltpu.make_async_copy(r.grads, r.grads_hbm, r.stores.at[size + 4]))
    keeps[4].start()
    for k in range(4):
        for step in others:
            swap(k, step).wait_send()
    scatter.finish()
    gather.finish()
    grads.finish()
    line_q.finish()
    line_u.finish()

    @pl.when(rank < parts - 1)
    def _():
        edge_rows().wait_send()
        for step in range(size):
            halo(step).wait_send()

    for keep in keeps[1:]:
        keep.wait()
    for g in range(size):
        norm_copy(g).wait()
    for step in (size - 2, size - 1):
        for copy in out_copies(step):
            copy.wait()


def forward_part(ident, count, tokens, cot, gains, table, qkv_piece, gu_piece, out_weight, down_weight):
    size, parts = lax.axis_size("fsdp"), lax.axis_size("seq")
    rows, width = tokens.shape
    local, inner = out_weight.shape[0], down_weight.shape[0]
    piece, cols = gu_piece.shape[1:]
    vmem = pl.BlockSpec(memory_space=pltpu.VMEM)
    hbm = pl.BlockSpec(memory_space=pl.ANY)
    shape = lambda w: (size, rows, w)
    low = lambda s: jax.ShapeDtypeStruct(s, BF)
    maps = [(size, parts, piece, 3 * local), (size, parts, piece, cols)]
    dma = lambda *s: pltpu.SemaphoreType.DMA(s)
    hop = transfers(size)
    scratch = scatter_shapes(size, rows, width)
    return pl.pallas_call(
        functools.partial(forward_kernel, size, parts, count),
        out_shape=[
            low(shape(width)),
            low(shape(3 * local)),
            low((size, WINDOW, 2 * local)),
            low(maps[0]),
            jax.ShapeDtypeStruct((rows, width), F32),
            low(shape(local)),
            low(shape(width)),
            low(shape(width)),
            low(shape(inner)),
            low(shape(cols)),
            low(maps[1]),
            low((size,) + gains.shape),
            jax.ShapeDtypeStruct((size,) + table.shape, jnp.int32),
            low((8, width)),
        ],
        in_specs=[vmem] * 4 + [hbm, hbm, vmem, vmem],
        out_specs=[hbm, hbm, vmem, hbm, vmem, vmem, hbm, hbm, hbm, hbm, hbm, vmem, vmem, vmem],
        scratch_shapes=scratch[:-2]
        + [
            pltpu.VMEM(shape(width), BF),
            pltpu.VMEM(shape(width), BF),
            pltpu.VMEM(shape(3 * local), BF),
            pltpu.VMEM(maps[0], BF),
            pltpu.VMEM(maps[1], BF),
            pltpu.VMEM((size, WINDOW, 2 * local), BF),
            pltpu.VMEM((rows, width), F32),
            pltpu.VMEM(shape(inner), F32),
            pltpu.VMEM((2, rows, inner), BF),
            pltpu.VMEM((2, rows, cols), BF),
        ]
        + [dma(hop)] * 8
        + [dma(4, size - 1)] * 2
        + [dma(size)] * 2
        + [pltpu.SemaphoreType.DMA] * 2
        + [dma(2), dma(size + 5), dma(2), dma(2)]
        + line_sems(parts)
        + line_sems(parts),
        compiler_params=pltpu.CompilerParams(
            collective_id=ident, has_side_effects=True, vmem_limit_bytes=67_000_000
        ),
        cost_estimate=pl.CostEstimate(
            flops=2 * size * rows * width * (4 * local + 3 * inner),
            bytes_accessed=500_000_000,
            transcendentals=0,
        ),
        name="forward_part",
    )(tokens, cot, gains, table, qkv_piece, gu_piece, out_weight, down_weight)


def heads_back(group, slot, count, lens_ref, starts_ref, own, edge, grad):
    rows, local = own.shape[0], own.shape[1] // 3
    head_of = lane_head(local)
    queries = own[:, :local]
    keys = jnp.concatenate([edge[:, :local], own[:, local : 2 * local]], 0)
    values = jnp.concatenate([edge[:, local:], own[:, 2 * local :]], 0)
    dqs, dks, dvs = [], [], []
    for block in range(rows // BLOCK):
        mask = masks_of(
            slot, block, count, lambda j: lens_ref[group, j], lambda j: starts_ref[group, j]
        )
        low = block * BLOCK
        span = slice(low, low + BLOCK + WINDOW)
        query, grads = queries[low : low + BLOCK], grad[low : low + BLOCK]
        key, value = keys[span], values[span]
        dq = jnp.zeros((BLOCK, local), F32)
        dk = jnp.zeros((BLOCK + WINDOW, local), F32)
        dv = jnp.zeros((BLOCK + WINDOW, local), F32)
        for head in range(local // HEAD_DIM):
            mine = head_of == head
            own_q = jnp.where(mine, query, jnp.zeros_like(query))
            own_g = jnp.where(mine, grads, jnp.zeros_like(grads))
            soft = soft_of(own_q, key, mask)
            grad_soft = dot_trans(own_g, value)
            total = jnp.sum(grad_soft * soft, axis=1, keepdims=True)
            grad_scores = (soft * (grad_soft - total)).astype(BF)
            dq = jnp.where(mine, dot(grad_scores, key), dq)
            dk = dk + dot_rows(grad_scores, own_q)
            dv = dv + dot_rows(soft.astype(BF), own_g)
        dqs.append(dq * SCALE)
        dks.append(dk * SCALE)
        dvs.append(dv)

    def joined(pieces):
        out = [pieces[0][:BLOCK]]
        for left, right in zip(pieces, pieces[1:]):
            out.append(left[BLOCK:] + right[:WINDOW])
            out.append(right[WINDOW:BLOCK])
        out.append(pieces[-1][BLOCK:])
        return jnp.concatenate(out, 0)

    return jnp.concatenate(dqs, 0), joined(dks), joined(dvs)


class BackRefs(NamedTuple):
    lens: Any
    starts: Any
    grad_gu_hbm: Any
    gu_map_hbm: Any
    middle: Any
    grads_hbm: Any
    gain: Any
    out_map: Any
    edge: Any
    qkv: Any
    qkv_map_hbm: Any
    gu_x: Any
    down_x: Any
    grad_middle: Any
    norm: Any
    all: Any
    dqkv: Any
    own: Any
    gu_slots: Any
    down_every: Any
    gu_pre: Any
    gu_up: Any
    gu_down: Any
    down_pre: Any
    down_up: Any
    down_down: Any
    part: Any
    first: Any
    over: Any
    joined: Any
    last: Any
    s_send: Any
    s_recv: Any
    t_send: Any
    t_recv: Any
    g_send: Any
    g_recv: Any
    grad_gu: Any
    gu_map: Any
    qkv_map: Any
    dedge: Any
    back: Any
    tail: Any
    h_send: Any
    h_recv: Any
    loads: Any
    gu_acc: Any
    gu_stage: Any
    gu_load: Any
    down_acc: Any
    down_stage: Any
    down_load: Any
    m_send: Any
    m_recv: Any
    grad: Any


def back_kernel(size, parts, count, *refs):
    named = len(BackRefs._fields)
    r, sems = BackRefs(*refs[:named]), refs[named:]
    line = Line(parts, sems[:6])
    gu_sum = StagedSum(
        r.gu_stage, r.gu_load, line, r.gu_x, r.gu_pre, r.gu_acc, r.gu_up, r.gu_down, sems[6:12]
    )
    down_sum = StagedSum(
        r.down_stage,
        r.down_load,
        line,
        r.down_x,
        r.down_pre,
        r.down_acc,
        r.down_up,
        r.down_down,
        sems[12:],
    )
    rows = r.middle.shape[0]
    local = r.out_map.shape[0]
    rank = lax.axis_index("seq")
    slot = rank * rows
    group = Group(size)
    barrier = pltpu.get_barrier_semaphore()
    greet_group(barrier, size)

    def greet(peer):
        pl.semaphore_signal(barrier, inc=1, device_id={"seq": peer}, device_id_type=MESH_ID)

    known = line.greet(barrier)
    pl.when(line.has_above & (line.core == 1))(lambda: greet(rank + 1))
    pl.when(line.has_below & (line.core == 0))(lambda: greet(rank - 1))
    n, z = line.length, line.z
    known = known + (2 * n - 2 - z) // n * line.core + (z + n - 1) // n * (1 - line.core)
    fetches = [
        pltpu.make_async_copy(src, dst, r.loads.at[k])
        for k, (src, dst) in enumerate(
            (
                (r.grad_gu_hbm, r.grad_gu),
                (r.gu_map_hbm, r.gu_map),
                (r.qkv_map_hbm, r.qkv_map),
                (r.grads_hbm.at[group.me], r.grad),
            )
        )
    ]
    for fetch in fetches:
        fetch.start()
    pl.semaphore_wait(barrier, size - 1 + known)
    down_sum.trade()
    gu_sum.trade()
    for m in range(n):
        down_sum.begin(m)
    scatter = Scatter(
        group, r.part, r.first, r.over, r.joined, r.last, r.s_send, r.s_recv
    )
    gather = Gather(group, r.all, r.g_send, r.g_recv)
    fetches[0].wait()
    fetches[1].wait()
    fetches[3].wait()

    def step_two(step, is_step):
        partial = dot_trans(r.grad_gu[group.to_own(step)], r.gu_map[...])
        is_step(size - 1)(lambda: r.own.__setitem__(..., partial))
        pl.when(step < size - 1)(lambda: r.part.__setitem__(step, partial.astype(BF)))
        for k in range(size - 1):
            is_step(k)(functools.partial(scatter.made, k))

    each_step(size, step_two)
    scatter.join()
    gu_sum.begin(0)
    down_sum.advance(1)
    half = rows // 2
    norm_sum = jnp.zeros((1, r.middle.shape[1]), F32)
    for h in range(2):
        span = slice(h * half, (h + 1) * half)
        grad = r.own[span, :] + scatter.total(h)
        middle = r.middle[span, :]
        scale = lax.rsqrt(jnp.mean(middle * middle, axis=1, keepdims=True) + EPS)
        unit = middle * scale
        scaled = grad * r.gain[...]
        norm_sum = norm_sum + jnp.sum(grad * unit, axis=0, keepdims=True)
        grad_out = r.grad[span, :].astype(F32)
        grad_middle = grad_out + scale * (
            scaled - unit * jnp.mean(scaled * unit, axis=1, keepdims=True)
        )
        r.grad_middle[span, :] = grad_middle
        r.all[group.me, span] = grad_middle.astype(BF)
        gather.start_half(h)
    r.norm[...] = norm_sum
    own_down = pltpu.make_async_copy(r.down_acc.at[z], r.down_every.at[rank], r.down_load.at[0])

    def halo(step):
        g = group.from_own(step)
        sems = r.h_send.at[step], r.h_recv.at[step]
        return remote(r.dedge.at[g], r.back.at[g], *sems, seq=rank - 1)

    def step_heads(step, is_step):
        g = group.from_own(step)

        @is_step(1)
        def _():
            gather.relay()
            for t in range(2, n - 1):
                down_sum.advance(t)

        @is_step(2)
        def _():
            down_sum.total()
            own_down.start()
            own_down.wait()
            line.gather(lambda owner: r.down_every.at[owner])

        for k in range(1, size):
            is_step(k)(functools.partial(gather.ready, k))
        grad = dot_trans(r.all[g], r.out_map[...]).astype(BF)
        dq, dk, dv = heads_back(
            g, slot, count, r.lens, r.starts, r.qkv[g], r.edge[g], grad
        )
        r.dedge[g] = jnp.concatenate([dk[:WINDOW], dv[:WINDOW]], 1).astype(BF)
        full = jnp.concatenate([dq, dk[WINDOW:], dv[WINDOW:]], 1)
        r.dqkv[g] = full.astype(BF)
        r.tail[g] = full[rows - WINDOW :]
        pl.when(rank > 0)(lambda: halo(step).start())

    each_step(size, step_heads)
    for m in range(1, n):
        gu_sum.begin(m)
    gu_sum.advance(1)
    line.relay(1)
    scatter.finish()
    fetches[2].wait()

    @pl.when(rank == parts - 1)
    def _():
        r.back[...] = jnp.zeros_like(r.back)

    @pl.when(rank < parts - 1)
    def _():
        for step in range(size):
            halo(step).wait_recv()

    scatter = Scatter(
        group, r.part, r.first, r.over, r.joined, r.last, r.t_send, r.t_recv
    )

    def step_one(step, is_step):
        g = group.to_own(step)
        back = r.back[g].astype(F32)
        wide = jnp.concatenate([jnp.zeros((WINDOW, local), F32), back], 1)
        r.dqkv[g, pl.ds(rows - WINDOW, WINDOW)] = (r.tail[g] + wide).astype(BF)
        partial = dot_trans(r.dqkv[g], r.qkv_map[...])
        is_step(size - 1)(lambda: r.own.__setitem__(..., partial))
        pl.when(step < size - 1)(lambda: r.part.__setitem__(step, partial.astype(BF)))
        for k in range(size - 1):
            is_step(k)(functools.partial(scatter.made, k))

    each_step(size, step_one)
    scatter.join()
    for t in range(2, n - 1):
        gu_sum.advance(t)
        line.relay(t)
    line.relay(n - 1)
    for h in range(2):
        span = slice(h * half, (h + 1) * half)
        r.own[span, :] = r.own[span, :] + scatter.total(h)
    gu_sum.total()

    def swap(step):
        peer = lax.rem(group.me + step, size)
        sems = r.m_send.at[step - 1], r.m_recv.at[step - 1]
        return remote(r.gu_acc.at[z, peer], r.gu_slots.at[group.me], *sems, fsdp=peer)

    for step in range(1, size):
        swap(step).start()
    own_slot = pltpu.make_async_copy(
        r.gu_acc.at[z, group.me], r.gu_slots.at[group.me], r.gu_load.at[0]
    )
    own_slot.start()
    for j in range(1, n):
        line.close(j)
    line.gathered()
    for step in range(1, size):
        swap(step).wait()
    scatter.finish()
    gather.finish()
    down_sum.finish()
    gu_sum.finish()
    line.finish()
    own_slot.wait()

    @pl.when(rank > 0)
    def _():
        for step in range(size):
            halo(step).wait_send()


def back_part(
    ident, lens, starts, grad_gu, gu_map, middle, grads, gain, out_weight, edge, qkv, qkv_map, gu_x, down_x
):
    size, parts = lax.axis_size("fsdp"), lax.axis_size("seq")
    rows, width = middle.shape
    local = out_weight.shape[0]
    n = parts // 2
    vmem = pl.BlockSpec(memory_space=pltpu.VMEM)
    smem = pl.BlockSpec(memory_space=pltpu.SMEM)
    hbm = pl.BlockSpec(memory_space=pl.ANY)
    dma = lambda *s: pltpu.SemaphoreType.DMA(s)
    low = lambda *s: jax.ShapeDtypeStruct(s, BF)
    sems = [dma(transfers(size))] * 2
    gu, down = gu_x.shape[1:], down_x.shape[1:]
    outs = pl.pallas_call(
        functools.partial(back_kernel, size, parts, lens.shape[1]),
        out_shape=[
            jax.ShapeDtypeStruct((rows, width), F32),
            jax.ShapeDtypeStruct((1, width), F32),
            low(size, rows, width),
            low(*qkv.shape),
            jax.ShapeDtypeStruct((rows, width), F32),
            low(*gu),
            low(parts, *down),
        ]
        + [low(n, *gu)] * 3
        + [low(n, *down)] * 3,
        in_specs=[smem, smem, hbm, hbm, vmem, hbm] + [vmem] * 4 + [hbm] * 3,
        out_specs=[vmem] * 5 + [hbm] * 8,
        scratch_shapes=scatter_shapes(size, rows, width)
        + sems
        + sems
        + [
            pltpu.VMEM(grad_gu.shape, BF),
            pltpu.VMEM(gu_map.shape, BF),
            pltpu.VMEM(qkv_map.shape, BF),
            pltpu.VMEM((size, WINDOW, 2 * local), BF),
            pltpu.VMEM((size, WINDOW, 2 * local), BF),
            pltpu.VMEM((size, WINDOW, 3 * local), F32),
            dma(size),
            dma(size),
            dma(4),
            pltpu.VMEM((n,) + gu, BF),
            pltpu.VMEM((2,) + gu, BF),
            dma(2),
            pltpu.VMEM((n,) + down, BF),
            pltpu.VMEM((2,) + down, BF),
            dma(2),
            dma(size - 1),
            dma(size - 1),
            pltpu.VMEM((rows, width), BF),
        ]
        + line_sems(parts) * 3,
        compiler_params=pltpu.CompilerParams(
            collective_id=ident, has_side_effects=True, vmem_limit_bytes=67_000_000
        ),
        cost_estimate=pl.CostEstimate(
            flops=2 * size * rows * (gu_map.size + qkv_map.size + width * local),
            bytes_accessed=400_000_000,
            transcendentals=0,
        ),
        name="back_part",
    )(lens, starts, grad_gu, gu_map, middle, grads, gain, out_weight, edge, qkv, qkv_map, gu_x, down_x)
    return outs[:7]


class CloseRefs(NamedTuple):
    gated_hbm: Any
    dqkv_hbm: Any
    heads_hbm: Any
    gb_hbm: Any
    gu_slots: Any
    terms: Any
    hidden_hbm: Any
    down_hbm: Any
    every_hbm: Any
    gu_every: Any
    feed: Any
    terms_out: Any
    pre: Any
    up_in: Any
    down_in: Any
    part: Any
    first: Any
    over: Any
    joined: Any
    last: Any
    x: Any
    acc: Any
    stage: Any
    stage_load: Any
    every: Any
    slots: Any
    gu_own: Any
    gated: Any
    dqkv: Any
    heads: Any
    gb: Any
    hidden: Any
    down_map: Any
    terms_in: Any
    terms_all: Any
    s_send: Any
    s_recv: Any
    m_send: Any
    m_recv: Any
    t_send: Any
    t_recv: Any
    loads: Any


def close_kernel(size, parts, made, *refs):
    named = len(CloseRefs._fields)
    r, sems = CloseRefs(*refs[:named]), refs[named:]
    rank = lax.axis_index("seq")
    group = Group(size)
    me = group.me
    line_u, line_q = Line(parts, sems[:6]), Line(parts, sems[6:12])
    n, z = line_q.length, line_q.z
    sums = MixedSum(
        r.stage, r.stage_load, line_q, r.x, r.pre, r.acc, r.up_in, r.down_in, sems[12:]
    )
    rows = r.feed.shape[0]
    half = rows // 2
    barrier = pltpu.get_barrier_semaphore()
    greet_group(barrier, size)
    for step in range(1, parts):
        peer = lax.rem(rank + step, parts)
        pl.semaphore_signal(barrier, inc=1, device_id={"seq": peer}, device_id_type=MESH_ID)
    moves = [
        (r.gu_slots, r.gu_own),
        (r.hidden_hbm, r.hidden),
        (r.down_hbm, r.down_map),
    ]
    if made:
        moves += [
            (r.gated_hbm, r.gated),
            (r.dqkv_hbm, r.dqkv),
            (r.heads_hbm, r.heads),
            (r.gb_hbm, r.gb),
        ]
    else:
        moves += [(r.gated_hbm, r.x)]
    fetches = [
        pltpu.make_async_copy(src, dst, r.loads.at[k]) for k, (src, dst) in enumerate(moves)
    ]
    for k in [0] + list(range(3, len(moves))) + [1, 2]:
        fetches[k].start()
    r.terms_in[me] = r.terms[me]
    own_slots = pltpu.make_async_copy(r.gu_own, r.gu_every.at[rank], r.loads.at[0])
    fetches[0].wait()
    own_slots.start()
    own_slots.wait()
    pl.semaphore_wait(barrier, size + parts - 2)
    line_u.gather(lambda owner: r.gu_every.at[owner])

    def swap(k, step):
        peer = lax.rem(me + step, size)
        src, dst = (
            lambda: (r.terms.at[peer], r.terms_in.at[me]),
            lambda: (r.acc.at[z, peer], r.slots.at[me]),
        )[k]()
        return remote(src, dst, r.m_send.at[k, step - 1], r.m_recv.at[k, step - 1], fsdp=peer)

    others = range(1, size)
    for step in others:
        swap(0, step).start()

    scatter = Scatter(
        group, r.part, r.first, r.over, r.joined, r.last, r.s_send, r.s_recv
    )

    def down(step, is_step):
        partial = dot(r.hidden[group.to_own(step)], r.down_map[...])
        is_step(size - 1)(lambda: r.feed.__setitem__(..., partial))
        pl.when(step < size - 1)(lambda: r.part.__setitem__(step, partial.astype(BF)))
        for k in range(size - 1):
            is_step(k)(functools.partial(scatter.made, k))

    for fetch in fetches[3:]:
        fetch.wait()
    if made:
        span = r.gated.shape[1] // (size // 2)
        for h in range(size // 2):
            lanes = slice(h * span, (h + 1) * span)
            pack_pair(
                r.x, h, r.gated[:, lanes], r.dqkv[...], r.heads[...], r.gb[:, lanes]
            )
    sums.trade()
    line_u.relay(1)
    fetches[1].wait()
    fetches[2].wait()
    for m in range(n):
        sums.begin(m)
    each_step(size, down)

    for step in others:
        swap(0, step).wait_recv()
    small = r.terms_in[0]
    for f in others:
        small = small + r.terms_in[f]
    r.terms_all[rank] = small

    def spread(step):
        peer = lax.rem(rank + step, parts)
        view = r.terms_all.at[rank]
        return remote(view, view, r.t_send.at[step - 1], r.t_recv.at[step - 1], seq=peer)

    for step in range(1, parts):
        spread(step).start()
    scatter.join()

    for t in range(1, n - 1):
        sums.advance(t)
        line_u.relay(t + 1)
    for h in range(2):
        span = slice(h * half, (h + 1) * half)
        r.feed[span, :] = r.feed[span, :] + scatter.total(h)
    sums.total()
    for step in others:
        swap(1, step).start()
    for j in range(1, n):
        line_u.close(j)
    r.slots[me] = r.acc[z, me]
    for step in others:
        swap(1, step).wait_recv()
    local = r.x.shape[3] // 4
    lane = lax.broadcasted_iota(jnp.int32, (1, 1, 4 * local), 2)
    r.every[rank] = jnp.where(lane < 3 * local, r.slots[...], r.acc[z])
    line_q.gather(lambda owner: r.every.at[owner])
    line_u.gathered()
    for j in range(1, n):
        line_q.relay(j)
    for j in range(1, n):
        line_q.close(j)
    line_q.gathered()
    store = pltpu.make_async_copy(r.every, r.every_hbm, r.loads.at[1])
    store.start()
    for step in range(1, parts):
        spread(step).wait_recv()
    small = r.terms_all[0]
    for k in range(1, parts):
        small = small + r.terms_all[k]
    r.terms_out[...] = small
    for k in range(2):
        for step in others:
            swap(k, step).wait_send()
    for step in range(1, parts):
        spread(step).wait_send()
    scatter.finish()
    sums.finish()
    line_u.finish()
    line_q.finish()
    store.wait()


def close_part(ident, gated, dqkv, heads, gb, gu_slots, terms, hidden, down_weight):
    size, parts = lax.axis_size("fsdp"), lax.axis_size("seq")
    width = gated.shape[1]
    made = packs(size, parts, width)
    piece, cols = width // (size * parts), dqkv.shape[1] + heads.shape[1]
    if not made:
        gated = pack_plain(parts, size, gated, dqkv, heads, gb)
    n = parts // 2
    rows = hidden.shape[1]
    vmem = pl.BlockSpec(memory_space=pltpu.VMEM)
    hbm = pl.BlockSpec(memory_space=pl.ANY)
    dma = lambda *s: pltpu.SemaphoreType.DMA(s)
    gu_shape = (parts,) + gu_slots.shape
    packed = (parts, size, piece, cols)
    scratch = scatter_shapes(size, rows, width)
    low = lambda *s: jax.ShapeDtypeStruct(s, BF)
    copy_of = lambda a: pltpu.VMEM(a.shape if made else (8, 128), BF)
    return pl.pallas_call(
        functools.partial(close_kernel, size, parts, made),
        out_shape=[
            low(*packed),
            low(*gu_shape),
            jax.ShapeDtypeStruct((rows, width), F32),
            jax.ShapeDtypeStruct(terms.shape[1:], F32),
        ]
        + [low(n, size, piece, cols)] * 3,
        in_specs=[hbm] * 5 + [vmem, hbm, hbm],
        out_specs=[hbm, hbm, vmem, vmem, hbm, hbm, hbm],
        scratch_shapes=scratch[:-2]
        + [
            pltpu.VMEM(packed, BF),
            pltpu.VMEM((n, size, piece, cols), BF),
            pltpu.VMEM((2, size, piece, cols), BF),
            dma(2),
            pltpu.VMEM(packed, BF),
            pltpu.VMEM((size, piece, cols), BF),
            pltpu.VMEM(gu_slots.shape, BF),
            copy_of(gated),
            copy_of(dqkv),
            copy_of(heads),
            copy_of(gb),
            pltpu.VMEM(hidden.shape, BF),
            pltpu.VMEM(down_weight.shape, BF),
            pltpu.VMEM(terms.shape, F32),
            pltpu.VMEM((parts,) + terms.shape[1:], F32),
        ]
        + scratch[-2:]
        + [dma(2, size - 1)] * 2
        + [dma(parts - 1)] * 2
        + [dma(7)]
        + line_sems(parts) * 3,
        compiler_params=pltpu.CompilerParams(
            collective_id=ident, has_side_effects=True, vmem_limit_bytes=67_000_000
        ),
        cost_estimate=pl.CostEstimate(
            flops=2 * size * rows * (down_weight.size + width * cols),
            bytes_accessed=500_000_000,
            transcendentals=0,
        ),
        name="close_part",
    )(gated, dqkv, heads, gb, gu_slots, terms, hidden, down_weight)[:4]


def pack_pair(out, pair, x, g, heads=None, gb=None):
    parts, _, piece, _ = out.shape
    rows = parts * piece
    full = dot_rows(x, g)
    side = None if heads is None else dot_rows(heads, gb)
    for k in range(2):
        own = full[k * rows : (k + 1) * rows]
        if side is not None:
            wide = side.shape[1] // 2
            own = jnp.concatenate([own, side[:, k * wide : (k + 1) * wide]], 1)
        out[:, pair * 2 + k] = own.astype(BF).reshape(parts, piece, own.shape[1])


def pack_kernel(x_ref, g_ref, out_ref):
    pack_pair(out_ref, 0, x_ref[...], g_ref[...])


def down_kernel(x_ref, g_ref, out_ref):
    out_ref[...] = dot_rows(x_ref[...], g_ref[...]).astype(BF)


def down_grad(x, g):
    total, inner = x.shape
    half = g.shape[1] // 2
    return pl.pallas_call(
        down_kernel,
        grid=(2,),
        out_shape=jax.ShapeDtypeStruct((inner, 2 * half), BF),
        in_specs=[
            pl.BlockSpec(x.shape, lambda i: (0, 0), pipeline_mode=pl.Buffered(1)),
            pl.BlockSpec((total, half), lambda i: (0, i)),
        ],
        out_specs=pl.BlockSpec((inner, half), lambda i: (0, i)),
        cost_estimate=pl.CostEstimate(
            flops=4 * total * inner * half,
            bytes_accessed=2 * (x.size + g.size) + 4 * inner * half,
            transcendentals=0,
        ),
        name="down_grad",
    )(x, g)


def packs(size, parts, width):
    return width // (size * parts) % 8 == 0 and 2 * width // size % 128 == 0


def pack_plain(parts, size, x, g, heads=None, gb=None):
    width, cols = x.shape[1], g.shape[1]
    piece = width // (size * parts)
    full = dot_rows(x, g).reshape(size, parts, piece, cols)
    if heads is not None:
        side = dot_rows(heads, gb).reshape(parts, piece, size, -1).transpose(2, 0, 1, 3)
        full = jnp.concatenate([full, side], 3)
    return full.transpose(1, 0, 2, 3).astype(BF)


def pack_grads(parts, size, x, g):
    total, width = x.shape
    cols = g.shape[1]
    if not packs(size, parts, width):
        return pack_plain(parts, size, x, g)
    piece = width // (size * parts)
    pair = pl.BlockSpec((total, 2 * width // size), lambda i: (0, i))
    whole = pl.BlockSpec(g.shape, lambda i: (0, 0), pipeline_mode=pl.Buffered(1))
    return pl.pallas_call(
        pack_kernel,
        grid=(size // 2,),
        out_shape=jax.ShapeDtypeStruct((parts, size, piece, cols), BF),
        in_specs=[pair, whole],
        out_specs=pl.BlockSpec((parts, 2, piece, cols), lambda i: (0, i, 0, 0)),
        cost_estimate=pl.CostEstimate(
            flops=2 * total * width * cols,
            bytes_accessed=2 * (x.size + g.size + width * cols),
            transcendentals=0,
        ),
        name="pack_grads",
    )(x, g)


def unpack_kernel(widths, *refs):
    outs = list(refs[len(widths) :])
    for every_ref, wide in zip(refs, widths):
        blocks = [every_ref[0, i].astype(F32) for i in range(every_ref.shape[1])]
        low = 0
        for width in wide:
            outs.pop(0)[...] = jnp.concatenate([b[:, low : low + width] for b in blocks], 1)
            low += width


def unpack_grads(arrays, widths):
    parts, size, piece, _ = arrays[0].shape
    every = [w for wide in widths for w in wide]
    if piece % 8:
        outs = []
        for array, wide in zip(arrays, widths):
            low = 0
            for width in wide:
                block = array[:, :, :, low : low + width].transpose(0, 2, 1, 3)
                outs.append(block.reshape(parts * piece, size * width).astype(F32))
                low += width
        return outs
    return pl.pallas_call(
        functools.partial(unpack_kernel, widths),
        grid=(parts,),
        out_shape=[jax.ShapeDtypeStruct((parts * piece, size * w), F32) for w in every],
        in_specs=[
            pl.BlockSpec((1, size, piece, a.shape[3]), lambda i: (i, 0, 0, 0)) for a in arrays
        ],
        out_specs=[pl.BlockSpec((piece, size * w), lambda i: (i, 0)) for w in every],
        cost_estimate=pl.CostEstimate(
            flops=0, bytes_accessed=6 * sum(a.size for a in arrays), transcendentals=0
        ),
        name="unpack_grads",
    )(*arrays)


def columns_piece(weights, part, parts):
    size = lax.axis_size("fsdp")
    rows = weights[0].shape[0] // parts
    pieces = []
    for weight in weights:
        own = lax.dynamic_slice_in_dim(weight, part * rows, rows, 0)
        pieces.append(own.reshape(rows, size, -1))
    return jnp.concatenate(pieces, 2).transpose(1, 0, 2)


def shards(
    tokens,
    seq_lengths,
    seq_offsets,
    norm1_gain,
    conv_weight,
    query_weight,
    key_weight,
    value_weight,
    out_weight,
    norm2_gain,
    gate_weight,
    up_weight,
    down_weight,
    cotangent,
):
    size = lax.axis_size("fsdp")
    parts = lax.axis_size("seq")
    part = lax.axis_index("seq")
    me = lax.axis_index("fsdp")
    own_tokens = tokens[0]
    rows, width = own_tokens.shape
    slice_width = norm1_gain.shape[0]
    first_slot = part * rows
    count = seq_lengths.shape[1]

    slot_ext = first_slot - 2 + jnp.arange(rows + 2, dtype=jnp.int32)
    segment_ext = segment_of(
        slot_ext, count, lambda j: seq_lengths[0, j], lambda j: seq_offsets[0, j]
    )
    segment_own = segment_ext[2:]
    same_one = (segment_own == segment_ext[1:-1]).astype(F32)[:, None]
    same_two = (segment_own == segment_ext[:-2]).astype(F32)[:, None]
    live_mask = (segment_own >= 0).astype(F32)[:, None]

    gains = jnp.concatenate(
        [
            norm1_gain[None],
            norm2_gain[None],
            conv_weight.T,
            jnp.zeros((3, slice_width), BF),
        ],
        0,
    )
    table = jnp.zeros((8, 128), jnp.int32)
    table = table.at[0, :count].set(seq_lengths[0]).at[1, :count].set(seq_offsets[0])
    qkv_piece = columns_piece((query_weight, key_weight, value_weight), part, parts)
    gu_piece = columns_piece((gate_weight, up_weight), part, parts)
    (
        gated_all,
        qkv,
        edge,
        qkv_map,
        middle,
        heads_out,
        grad_down_all,
        normed_all,
        hidden,
        grad_gu,
        gu_map,
        gains_all,
        table_all,
        edge_tokens,
    ) = forward_part(
        0,
        count,
        own_tokens,
        cotangent[0],
        gains,
        table,
        qkv_piece,
        gu_piece,
        out_weight,
        down_weight,
    )
    local = out_weight.shape[0]
    flat = lambda a: a.reshape(-1, a.shape[-1])
    lens_all, starts_all = table_all[:, 0, :count], table_all[:, 1, :count]
    gains_all = gains_all.transpose(1, 0, 2).reshape(8, width)
    norm_one = gains_all[0].astype(F32)
    norm_two = gains_all[1].astype(F32)
    taps = gains_all[2:5].astype(F32)
    qkv_map, gu_map = qkv_map.reshape(width, -1), gu_map.reshape(width, -1)

    extended = jnp.concatenate([edge_tokens[6:], own_tokens], 0).astype(F32)
    scale_one = lax.rsqrt(jnp.mean(extended * extended, axis=1, keepdims=True) + EPS)
    normed = extended * scale_one * norm_one
    conv_mix = (
        normed[2:] * taps[0]
        + same_one * normed[1:-1] * taps[1]
        + same_two * normed[:-2] * taps[2]
    )

    gu_packed = pack_grads(parts, size, flat(normed_all), flat(grad_gu))
    down_packed = down_grad(flat(hidden), flat(grad_down_all))
    grad_middle, norm2_term, grad_branch_all, dqkv, grad_gated, gu_slots, down_every = back_part(
        4,
        lens_all,
        starts_all,
        grad_gu,
        gu_map,
        middle,
        grad_down_all,
        norm_two[None],
        out_weight,
        edge,
        qkv,
        qkv_map,
        gu_packed,
        down_packed.reshape(parts, -1, width),
    )
    norm2_term = norm2_term[0]
    down_total = down_every.reshape(-1, width).astype(F32)
    normed_own = normed[2:]
    grad_mix = grad_gated * normed_own
    part_zero = jnp.pad(grad_gated * conv_mix + grad_mix * taps[0], ((2, 0), (0, 0)))
    part_one = jnp.pad(grad_mix * same_one * taps[1], ((1, 1), (0, 0)))
    part_two = jnp.pad(grad_mix * same_two * taps[2], ((0, 2), (0, 0)))
    grad_normed = part_zero + part_one + part_two
    unit_one = extended * scale_one
    grad_unit_one = grad_normed * norm_one
    grad_extended = scale_one * (
        grad_unit_one - unit_one * jnp.mean(grad_unit_one * unit_one, axis=1, keepdims=True)
    )
    edge_back = shifted(grad_extended[:2], "seq", -1)
    tokens_grad = grad_middle + grad_extended[2:] + jnp.pad(edge_back, ((rows - 2, 0), (0, 0)))

    terms = jnp.stack(
        [
            jnp.sum(grad_normed * unit_one, axis=0),
            norm2_term,
            jnp.sum(grad_mix * normed_own, axis=0),
            jnp.sum(grad_mix * same_one * normed[1:-1], axis=0),
            jnp.sum(grad_mix * same_two * normed[:-2], axis=0),
        ]
    )
    terms = jnp.pad(terms, ((0, 3), (0, 0))).reshape(8, size, slice_width).transpose(1, 0, 2)
    gu_slots, terms, down_total, tokens_grad = lax.optimization_barrier(
        (gu_slots, terms, down_total, tokens_grad)
    )
    qkvo_every, gu_every, feed, terms = close_part(
        5,
        flat(gated_all),
        flat(dqkv),
        flat(heads_out),
        flat(grad_branch_all),
        gu_slots,
        terms,
        hidden,
        down_weight,
    )
    gate_total, up_total, query_total, key_total, value_total, out_total = unpack_grads(
        (gu_every, qkvo_every), ((gu_map.shape[1] // 2,) * 2, (local,) * 4)
    )

    layer_out = (live_mask * (middle + feed)).astype(BF)[None]
    return (
        layer_out,
        tokens_grad[None],
        terms[0],
        terms[2:5].T,
        query_total,
        key_total,
        value_total,
        out_total,
        terms[1],
        gate_total,
        up_total,
        down_total,
    )


def solution(mesh):
    placed = (
        P("fsdp", "seq", None),
        P("fsdp", None),
        P("fsdp", None),
        P("fsdp"),
        P("fsdp", None),
        P("fsdp", None),
        P("fsdp", None),
        P("fsdp", None),
        P("fsdp", None),
        P("fsdp"),
        P("fsdp", None),
        P("fsdp", None),
        P("fsdp", None),
        P("fsdp", "seq", None),
    )
    return jax.shard_map(
        shards,
        mesh=mesh,
        in_specs=placed,
        out_specs=(
            P("fsdp", "seq", None),
            P("fsdp", "seq", None),
            P("fsdp"),
            P("fsdp", None),
            P("fsdp", None),
            P("fsdp", None),
            P("fsdp", None),
            P("fsdp", None),
            P("fsdp"),
            P("fsdp", None),
            P("fsdp", None),
            P("fsdp", None),
        ),
        check_vma=False,
    )
```

```python
import functools
from typing import Any, NamedTuple

import jax
import jax.numpy as jnp
from jax import lax
from jax.experimental import pallas as pl
from jax.experimental.pallas import tpu as pltpu
from jax.sharding import PartitionSpec as P

HEADS = 16
WINDOW = 64
HEAD_DIM = 112
BLOCK = 128

EPS = 1e-05
NEG = -1e30
SCALE = HEAD_DIM ** (-0.5)
MESH_ID = pl.DeviceIdType.MESH
BF = jnp.bfloat16
F32 = jnp.float32


def shifted(array, axis, by):
    length = lax.axis_size(axis)
    pairs = [(i, i + by) for i in range(length) if 0 <= i + by < length]
    return lax.ppermute(array, axis, pairs)


def segment_of(slot, count, lengths, starts):
    found = jnp.full(slot.shape, -1, jnp.int32)
    for j in range(count):
        inside = (slot >= starts(j)) & (slot < starts(j) + lengths(j))
        found = jnp.where(inside, j, found)
    return jnp.where(slot < 0, -2, found)


def dot_rows(left, right):
    return lax.dot_general(left, right, (((0,), (0,)), ((), ())), preferred_element_type=F32)


def dot_trans(left, right):
    return lax.dot_general(left, right, (((1,), (1,)), ((), ())), preferred_element_type=F32)


def dot(left, right):
    return jnp.dot(left, right, preferred_element_type=F32)


def masks_of(first, block, count, length, start):
    rows = first + block * BLOCK
    query = rows + lax.broadcasted_iota(jnp.int32, (BLOCK, 1), 0)
    keys = rows - WINDOW + lax.broadcasted_iota(jnp.int32, (1, BLOCK + WINDOW), 1)
    seg_q = segment_of(query, count, length, start)
    seg_k = segment_of(keys, count, length, start)
    far = query - keys
    return (far >= 0) & (far <= WINDOW) & (seg_q == seg_k)


def soft_of(query, keys, mask):
    scores = dot_trans(query, keys) * SCALE
    scores = jnp.where(mask, scores, NEG)
    peak = jnp.max(scores, axis=1, keepdims=True)
    exponent = jnp.exp(scores - peak)
    return exponent / jnp.sum(exponent, axis=1, keepdims=True)


def lane_head(width):
    return lax.broadcasted_iota(jnp.int32, (1, width), 1) // HEAD_DIM


def remote(src, dst, send, recv, **peer):
    return pltpu.make_async_remote_copy(
        src_ref=src,
        dst_ref=dst,
        send_sem=send,
        recv_sem=recv,
        device_id=peer,
        device_id_type=MESH_ID,
    )


def greet_group(barrier, size):
    me = lax.axis_index("fsdp")
    for step in range(1, size):
        peer = lax.rem(me + step, size)
        pl.semaphore_signal(barrier, inc=1, device_id={"fsdp": peer}, device_id_type=MESH_ID)


class Group:
    def __init__(self, size):
        self.size = size
        self.me = lax.axis_index("fsdp")
        self.square = size == 4
        if self.square:
            x, y = lax.rem(self.me, 2), self.me // 2
            self.at = lambda bx, by: lax.rem(y + by, 2) * 2 + lax.rem(x + bx, 2)
            self.x, self.y, self.far = self.at(1, 0), self.at(0, 1), self.at(1, 1)

    def from_own(self, step):
        if self.square:
            return self.at(lax.rem(step, 2), step // 2)
        return lax.rem(self.me - step + self.size, self.size)

    def to_own(self, step):
        if self.square:
            return self.at(1 - step // 2, 1 - lax.rem(step, 2))
        return lax.rem(self.me + 1 + step, self.size)


class Gather:
    def __init__(self, group, ref, send, recv):
        self.group, self.ref, self.send, self.recv = group, ref, send, recv
        self.half = ref.shape[1] // 2

    def part(self, k, slot, half, peer):
        view = self.ref.at[slot, pl.ds(half * self.half, self.half)]
        return remote(view, view, self.send.at[k], self.recv.at[k], fsdp=peer)

    def whole(self, k):
        g = self.group
        view = self.ref.at[g.me]
        sems = self.send.at[k - 1], self.recv.at[k - 1]
        return remote(view, view, *sems, fsdp=lax.rem(g.me + k, g.size))

    def copy(self, k):
        g = self.group
        if not g.square:
            return self.whole(k + 1)
        slot = (g.me, g.me, g.me, g.me, g.x, g.y)[k]
        half = (0, 1, 0, 1, 0, 1)[k]
        return self.part(k, slot, half, (g.x, g.x, g.y, g.y, g.y, g.x)[k])

    def start_half(self, half):
        if self.group.square:
            self.copy(half).start()
            self.copy(2 + half).start()
        elif half == 1:
            for k in range(self.group.size - 1):
                self.copy(k).start()

    def relay(self):
        if self.group.square:
            self.copy(0).wait_recv()
            self.copy(4).start()
            self.copy(3).wait_recv()
            self.copy(5).start()

    def ready(self, step):
        if not self.group.square:
            self.copy(step - 1).wait_recv()
        elif step == 3:
            self.copy(4).wait_recv()
            self.copy(5).wait_recv()
        else:
            self.copy(step).wait_recv()

    def finish(self):
        for k in range(transfers(self.group.size)):
            self.copy(k).wait_send()


class Scatter:
    def __init__(self, group, part, first, over, joined, last, send, recv):
        self.group, self.part = group, part
        self.first, self.over, self.joined, self.last = first, over, joined, last
        self.send, self.recv = send, recv
        self.half = part.shape[1] // 2

    def copy(self, k):
        g, half = self.group, self.half
        low, high = pl.ds(0, half), pl.ds(half, half)
        if not g.square:
            src, dst, peer = self.part.at[k], self.first.at[k], lax.rem(g.me + 1 + k, g.size)
        else:
            src, dst, peer = (
                lambda: (self.part.at[0, low], self.over.at[0], g.x),
                lambda: (self.part.at[0, high], self.over.at[1], g.y),
                lambda: (self.part.at[1, low], self.first.at[0], g.x),
                lambda: (self.part.at[2, high], self.first.at[1], g.y),
                lambda: (self.joined.at[0], self.last.at[0], g.y),
                lambda: (self.joined.at[1], self.last.at[1], g.x),
            )[k]()
        return remote(src, dst, self.send.at[k], self.recv.at[k], fsdp=peer)

    def made(self, step):
        if not self.group.square:
            self.copy(step).start()
        elif step == 0:
            self.copy(0).start()
            self.copy(1).start()
        elif step in (1, 2):
            self.copy(step + 1).start()

    def join(self):
        if not self.group.square:
            return
        half = self.half
        for k, (step, rows) in enumerate(((2, slice(0, half)), (1, slice(half, 2 * half)))):
            self.copy(k).wait_recv()
            own = self.part[step, rows].astype(F32)
            self.joined[k] = (own + self.over[k].astype(F32)).astype(BF)
            self.copy(4 + k).start()

    def total(self, half):
        count = self.half
        if self.group.square:
            self.copy(2 + half).wait_recv()
            self.copy(4 + half).wait_recv()
            return self.first[half].astype(F32) + self.last[half].astype(F32)
        if half == 0:
            for k in range(self.group.size - 1):
                self.copy(k).wait_recv()
        rows = slice(half * count, (half + 1) * count)
        out = self.first[0, rows].astype(F32)
        for k in range(1, self.group.size - 1):
            out = out + self.first[k, rows].astype(F32)
        return out

    def finish(self):
        for k in range(transfers(self.group.size)):
            self.copy(k).wait_send()


class Line:
    def __init__(self, parts, sems):
        self.rank = lax.axis_index("seq")
        self.parts, self.length = parts, parts // 2
        self.z, self.core = self.rank // 2, lax.rem(self.rank, 2)
        self.above, self.below = self.rank + 2, self.rank - 2
        self.beside = self.rank + 1 - 2 * self.core
        self.has_above, self.has_below = self.z < self.length - 1, self.z > 0
        self.sems = sems

    def greet(self, barrier):
        def one(peer):
            pl.semaphore_signal(barrier, inc=1, device_id={"seq": peer}, device_id_type=MESH_ID)

        one(self.beside)
        pl.when(self.has_above)(lambda: one(self.above))
        pl.when(self.has_below)(lambda: one(self.below))
        n, z = self.length, self.z
        return 1 + (2 * n - 2 - z) // n + (z + n - 1) // n

    def up(self, k, owner):
        view = self.view(owner)
        return remote(view, view, self.sems[0].at[k], self.sems[1].at[k], seq=self.above)

    def down(self, k, owner):
        view = self.view(owner)
        return remote(view, view, self.sems[2].at[k], self.sems[3].at[k], seq=self.below)

    def side(self, k, owner):
        view = self.view(owner)
        return remote(view, view, self.sems[4].at[k], self.sems[5].at[k], seq=self.beside)

    def gather(self, view):
        self.view = view
        pl.when(self.has_above)(lambda: self.up(0, self.rank).start())
        pl.when(self.has_below)(lambda: self.down(0, self.rank).start())
        self.side(self.z, self.rank).start()

    def own_up(self):
        pl.when(self.has_above)(lambda: self.up(0, self.rank).start())

    def own_down(self):
        pl.when(self.has_below)(lambda: self.down(0, self.rank).start())

    def relay_up(self, j):
        rank, z = self.rank, self.z

        @pl.when((z >= j) & self.has_above)
        def _():
            self.up(j - 1, rank).wait_recv()
            self.up(j, rank - 2 * j).start()
            self.side(z - j, rank - 2 * j).start()

    def relay_down(self, j):
        rank, z = self.rank, self.z

        @pl.when((z + j < self.length) & self.has_below)
        def _():
            self.down(j - 1, rank).wait_recv()
            self.down(j, rank + 2 * j).start()
            self.side(z + j, rank + 2 * j).start()

    def relay(self, j):
        self.relay_up(j)
        self.relay_down(j)

    def close(self, j):
        rank, z = self.rank, self.z

        @pl.when((z >= j) & (z == self.length - 1))
        def _():
            self.up(j - 1, rank).wait_recv()
            self.side(z - j, rank - 2 * j).start()

        @pl.when((z + j < self.length) & (z == 0))
        def _():
            self.down(j - 1, rank).wait_recv()
            self.side(z + j, rank + 2 * j).start()

    def gathered(self):
        for k in range(self.length):
            self.side(k, self.rank).wait_recv()

    def finish(self):
        rank, z = self.rank, self.z
        for k in range(self.length):
            self.side(k, rank).wait_send()
        pl.when(self.has_above)(lambda: self.up(0, rank).wait_send())
        pl.when(self.has_below)(lambda: self.down(0, rank).wait_send())
        for j in range(1, self.length):
            pl.when((z >= j) & self.has_above)(lambda: self.up(j, rank).wait_send())
            pl.when((z + j < self.length) & self.has_below)(lambda: self.down(j, rank).wait_send())


class LineSum:
    def __init__(self, line, x, pre, acc, up_in, down_in, sems):
        self.line, self.x, self.pre, self.acc = line, x, pre, acc
        self.up_in, self.down_in, self.sems = up_in, down_in, sems

    def share(self, k):
        line = self.line
        src = self.x.at[2 * k + 1 - line.core]
        return remote(src, self.pre.at[k], self.sems[0].at[k], self.sems[1].at[k], seq=line.beside)

    def up(self, k):
        sems = self.sems[2].at[k], self.sems[3].at[k]
        return remote(self.acc.at[k], self.up_in.at[k], *sems, seq=self.line.above)

    def down(self, k):
        sems = self.sems[4].at[k], self.sems[5].at[k]
        return remote(self.acc.at[k], self.down_in.at[k], *sems, seq=self.line.below)

    def pair(self, m):
        return self.line.length - 1 - m, m

    def trade(self):
        n = self.line.length
        for m in range((n + 1) // 2):
            for k in sorted(set(self.pair(m))):
                self.share(k).start()

    def merge(self, k):
        self.share(k).wait_recv()
        own = self.x[2 * k + self.line.core].astype(F32)
        self.acc[k] = (own + self.pre[k].astype(F32)).astype(BF)

    def begin(self, m):
        n, z = self.line.length, self.line.z
        far, near = self.pair(m)
        if m < (n + 1) // 2:
            for k in sorted({far, near}):
                self.merge(k)
        if m < n - 1:
            pl.when(z == 0)(lambda: self.up(far).start())
            pl.when(z == n - 1)(lambda: self.down(near).start())

    def add(self, k, more):
        self.acc[k] = (self.acc[k].astype(F32) + more[k].astype(F32)).astype(BF)

    def advance(self, t):
        z, n = self.line.z, self.line.length
        far, near = n - 1 + z - t, t - n + 1 + z

        @pl.when((z >= 1) & (z <= t))
        def _():
            self.up(far).wait_recv()
            self.add(far, self.up_in)
            self.up(far).start()

        @pl.when((z <= n - 2) & (z >= n - 1 - t))
        def _():
            self.down(near).wait_recv()
            self.add(near, self.down_in)
            self.down(near).start()

    def total(self):
        z = self.line.z

        @pl.when(z > 0)
        def _():
            self.up(z).wait_recv()
            self.add(z, self.up_in)

        @pl.when(z < self.line.length - 1)
        def _():
            self.down(z).wait_recv()
            self.add(z, self.down_in)

    def finish(self):
        for k in range(self.line.length):
            self.share(k).wait_send()
            pl.when(k > self.line.z)(lambda: self.up(k).wait_send())
            pl.when(k < self.line.z)(lambda: self.down(k).wait_send())


class StagedSum(LineSum):
    def __init__(self, stage, load, *args):
        super().__init__(*args)
        self.stage, self.load = stage, load

    def fetch(self, slot, src):
        return pltpu.make_async_copy(src, self.stage.at[slot], self.load.at[slot])

    def merge(self, k):
        self.share(k).wait_recv()
        own = self.fetch(0, self.x.at[2 * k + self.line.core])
        other = self.fetch(1, self.pre.at[k])
        own.start()
        other.start()
        own.wait()
        other.wait()
        self.acc[k] = (self.stage[0].astype(F32) + self.stage[1].astype(F32)).astype(BF)

    def add(self, k, more):
        came = self.fetch(0, more.at[k])
        came.start()
        came.wait()
        self.acc[k] = (self.acc[k].astype(F32) + self.stage[0].astype(F32)).astype(BF)


class MixedSum(StagedSum):
    def merge(self, k):
        self.share(k).wait_recv()
        other = self.fetch(1, self.pre.at[k])
        other.start()
        other.wait()
        own = self.x[2 * k + self.line.core].astype(F32)
        self.acc[k] = (own + self.stage[1].astype(F32)).astype(BF)


def line_sems(parts):
    return [pltpu.SemaphoreType.DMA((parts // 2,))] * 6


def transfers(size):
    return 6 if size == 4 else size - 1


def scatter_shapes(size, rows, width):
    half = rows // 2
    slots = (2, half, width) if size == 4 else (size - 1, rows, width)
    return [
        pltpu.VMEM((size - 1, rows, width), BF),
        pltpu.VMEM(slots, BF),
        pltpu.VMEM((2, half, width), BF),
        pltpu.VMEM((2, half, width), BF),
        pltpu.VMEM((2, half, width), BF),
        pltpu.SemaphoreType.DMA((transfers(size),)),
        pltpu.SemaphoreType.DMA((transfers(size),)),
    ]


def each_step(size, body):
    def one(step, carry):
        body(step, lambda k: pl.when(step == k))
        return carry

    lax.fori_loop(0, size, one, 0)


class ForwardRefs(NamedTuple):
    tokens: Any
    cot: Any
    gains: Any
    table: Any
    qkv_piece: Any
    gu_piece: Any
    out_map: Any
    down_map: Any
    gated_hbm: Any
    qkv_hbm: Any
    edge: Any
    qkv_map_hbm: Any
    middle: Any
    heads: Any
    grads_hbm: Any
    norm_hbm: Any
    hidden_hbm: Any
    gu_grad_hbm: Any
    gu_map_hbm: Any
    gains_all: Any
    table_all: Any
    edge_tok: Any
    part: Any
    first: Any
    over: Any
    joined: Any
    last: Any
    all: Any
    grads: Any
    qkv: Any
    qkv_map: Any
    gu_map: Any
    tail: Any
    own: Any
    grad_hidden: Any
    hidden: Any
    gu_grad: Any
    s_send: Any
    s_recv: Any
    a_send: Any
    a_recv: Any
    g_send: Any
    g_recv: Any
    c_send: Any
    c_recv: Any
    m_send: Any
    m_recv: Any
    halo_send: Any
    halo_recv: Any
    edge_send: Any
    edge_recv: Any
    loads: Any
    stores: Any
    hidden_store: Any
    gu_store: Any


def forward_kernel(size, parts, count, *refs):
    named = len(ForwardRefs._fields)
    r, sems = ForwardRefs(*refs[:named]), refs[named:]
    rank = lax.axis_index("seq")
    rows = r.tokens.shape[0]
    half = rows // 2
    local = r.out_map.shape[0]
    inner = r.down_map.shape[0]
    slot = rank * rows
    group = Group(size)
    me = group.me
    line_q, line_u = Line(parts, sems[:6]), Line(parts, sems[6:])

    barrier = pltpu.get_barrier_semaphore()
    greet_group(barrier, size)
    known = line_q.greet(barrier)

    def greet(peer):
        pl.semaphore_signal(barrier, inc=1, device_id={"seq": peer}, device_id_type=MESH_ID)

    pl.when(line_q.has_above & (line_q.core == 1))(lambda: greet(rank + 1))
    pl.when(line_q.has_below & (line_q.core == 0))(lambda: greet(rank - 1))
    n, z = line_q.length, line_q.z
    known = known + (2 * n - 2 - z) // n * line_q.core + (z + n - 1) // n * (1 - line_q.core)
    own_pieces = [
        pltpu.make_async_copy(src.at[me], dst.at[me, rank], r.loads.at[k])
        for k, (src, dst) in enumerate(
            ((r.qkv_piece, r.qkv_map), (r.gu_piece, r.gu_map))
        )
    ]
    for copy in own_pieces:
        copy.start()
    r.gains_all[me] = r.gains[...]
    r.table_all[me] = r.table[...]
    own_table = r.table[...]
    slots = slot + lax.broadcasted_iota(jnp.int32, (rows, 1), 0)
    length = lambda j: own_table[0:1, j : j + 1]
    start = lambda j: own_table[1:2, j : j + 1]
    segment = segment_of(slots, count, length, start)
    r.grads[me] = jnp.where(segment >= 0, r.cot[...].astype(F32), 0.0).astype(BF)

    @pl.when(rank == 0)
    def _():
        r.edge_tok[...] = jnp.zeros_like(r.edge_tok)

    def edge_rows():
        last = r.tokens.at[pl.ds(rows - 8, 8)]
        return remote(last, r.edge_tok, r.edge_send, r.edge_recv, seq=rank + 1)

    pl.semaphore_wait(barrier, size - 1 + known)
    pl.when(rank < parts - 1)(lambda: edge_rows().start())

    def swap(k, step):
        peer = lax.rem(me + step, size)
        src, dst = (
            lambda: (r.gains_all.at[me], r.gains_all.at[me]),
            lambda: (r.table_all.at[me], r.table_all.at[me]),
            lambda: (r.qkv_piece.at[peer], r.qkv_map.at[me, rank]),
            lambda: (r.gu_piece.at[peer], r.gu_map.at[me, rank]),
        )[k]()
        return remote(src, dst, r.m_send.at[k, step - 1], r.m_recv.at[k, step - 1], fsdp=peer)

    others = range(1, size)
    for k in range(4):
        for step in others:
            swap(k, step).start()
    for k in range(2):
        for step in others:
            swap(k, step).wait_recv()

    gains = jnp.concatenate([r.gains_all[f] for f in range(size)], 1).astype(F32)
    same_one = (segment == segment_of(slots - 1, count, length, start)).astype(F32)
    same_two = (segment == segment_of(slots - 2, count, length, start)).astype(F32)
    tokens = r.tokens[...].astype(F32)
    pl.when(rank > 0)(lambda: edge_rows().wait_recv())
    edge = r.edge_tok[...].astype(F32)

    def norm(a):
        return a * lax.rsqrt(jnp.mean(a * a, axis=1, keepdims=True) + EPS) * gains[0:1]

    normed, edge = norm(tokens), norm(edge)
    row = lax.broadcasted_iota(jnp.int32, (rows, 1), 0)
    back_one = jnp.where(row == 0, edge[7:8], pltpu.roll(normed, 1, 0))
    back_two = jnp.where(
        row == 0, edge[6:7], jnp.where(row == 1, edge[7:8], pltpu.roll(normed, 2, 0))
    )
    mixed = (
        normed * gains[2:3]
        + same_one * back_one * gains[3:4]
        + same_two * back_two * gains[4:5]
    )
    all_ref = r.all
    all_ref[me] = (mixed * normed).astype(BF)
    gather = Gather(group, all_ref, r.a_send, r.a_recv)
    gather.start_half(0)
    gather.start_half(1)

    own_pieces[0].wait()
    for step in others:
        swap(2, step).wait_recv()
    line_q.gather(lambda owner: r.qkv_map.at[:, owner])
    line_u.view = lambda owner: r.gu_map.at[:, owner]
    gather.relay()
    grads = Gather(group, r.grads, r.c_send, r.c_recv)
    grads.start_half(0)
    grads.start_half(1)
    own_pieces[1].wait()
    for step in others:
        swap(3, step).wait_recv()
    line_u.side(z, rank).start()
    pl.when(z == 0)(line_u.own_up)
    pl.when(z == n - 1)(line_u.own_down)
    for j in range(1, n):
        line_q.relay(j)
        line_q.close(j)
        pl.when(z == j)(line_u.own_up)
        pl.when(z == n - 1 - j)(line_u.own_down)
    for step in others:
        gather.ready(step)
    grads.relay()
    line_q.gathered()
    keeps = [
        pltpu.make_async_copy(all_ref, r.gated_hbm, r.stores.at[size]),
        pltpu.make_async_copy(r.qkv_map, r.qkv_map_hbm, r.stores.at[size + 1]),
    ]
    for keep in keeps:
        keep.start()

    weights = r.qkv_map[...].reshape(-1, r.qkv_map.shape[3])

    def halo(step):
        g = group.to_own(step)
        sem = r.halo_send.at[step], r.halo_recv.at[step]
        return remote(r.tail.at[g], r.edge.at[g], *sem, seq=rank + 1)

    def project(step, is_step):
        g = group.to_own(step)
        out = dot(all_ref[g], weights).astype(BF)
        r.qkv[g] = out
        r.tail[g] = out[rows - WINDOW :, local:]
        pl.when(rank < parts - 1)(lambda: halo(step).start())

    each_step(size, project)

    @pl.when(rank == 0)
    def _():
        r.edge[...] = jnp.zeros_like(r.edge)

    keeps.append(pltpu.make_async_copy(r.qkv, r.qkv_hbm, r.stores.at[size + 2]))
    keeps[2].start()
    line_u.relay(1)
    gather.finish()
    keeps[0].wait()

    scatter = Scatter(
        group, r.part, r.first, r.over, r.joined, r.last, r.s_send, r.s_recv
    )
    head_of = lane_head(local)

    def mix(step, is_step):
        g = group.to_own(step)
        pl.when(rank > 0)(lambda: halo(step).wait_recv())
        own, edge, table = r.qkv[g], r.edge[g], r.table_all[g]
        queries = own[:, :local]
        keys = jnp.concatenate([edge[:, :local], own[:, local : 2 * local]], 0)
        values = jnp.concatenate([edge[:, local:], own[:, 2 * local :]], 0)
        outs = []
        for block in range(rows // BLOCK):
            mask = masks_of(
                slot,
                block,
                count,
                lambda j: table[0:1, j : j + 1],
                lambda j: table[1:2, j : j + 1],
            )
            low = block * BLOCK
            query = queries[low : low + BLOCK]
            key = keys[low : low + BLOCK + WINDOW]
            value = values[low : low + BLOCK + WINDOW]
            out = jnp.zeros((BLOCK, local), F32)
            for head in range(local // HEAD_DIM):
                mine = head_of == head
                soft = soft_of(jnp.where(mine, query, jnp.zeros_like(query)), key, mask)
                out = jnp.where(mine, dot(soft.astype(BF), value), out)
            outs.append(out.astype(BF))
        heads = jnp.concatenate(outs, 0)
        r.heads[g] = heads
        branch = dot(heads, r.out_map[...])
        is_step(size - 1)(lambda: r.own.__setitem__(..., branch))
        pl.when(step < size - 1)(lambda: r.part.__setitem__(step, branch.astype(BF)))
        for k in range(size - 1):
            is_step(k)(functools.partial(scatter.made, k))

    each_step(size, mix)
    scatter.join()
    for j in range(2, n):
        line_u.relay(j)
    gather = Gather(group, all_ref, r.g_send, r.g_recv)
    for h in range(2):
        span = slice(h * half, (h + 1) * half)
        total = r.own[span, :] + scatter.total(h)
        middle = r.tokens[span, :].astype(F32) + total
        r.middle[span, :] = middle
        scale = lax.rsqrt(jnp.mean(middle * middle, axis=1, keepdims=True) + EPS)
        all_ref[me, span] = (middle * scale * gains[1:2]).astype(BF)
        gather.start_half(h)
    gather.relay()

    def grad_of(step, is_step):
        g = group.from_own(step)
        for k in others:
            is_step(k)(functools.partial(grads.ready, k))
        r.grad_hidden[g] = dot_trans(r.grads[g], r.down_map[...])

    each_step(size, grad_of)
    for j in range(1, n):
        line_u.close(j)
    line_u.gathered()
    keeps.append(pltpu.make_async_copy(r.gu_map, r.gu_map_hbm, r.stores.at[size + 3]))
    keeps[3].start()

    def out_copies(step):
        g, two = group.from_own(step), lax.rem(step, 2)
        return (
            pltpu.make_async_copy(
                r.hidden.at[two], r.hidden_hbm.at[g], r.hidden_store.at[two]
            ),
            pltpu.make_async_copy(
                r.gu_grad.at[two], r.gu_grad_hbm.at[g], r.gu_store.at[two]
            ),
        )

    def norm_copy(g):
        return pltpu.make_async_copy(all_ref.at[g], r.norm_hbm.at[g], r.stores.at[g])

    def feed(step, is_step):
        g, two = group.from_own(step), lax.rem(step, 2)
        for k in others:
            is_step(k)(functools.partial(gather.ready, k))

        @pl.when(step >= 2)
        def _():
            for copy in out_copies(step - 2):
                copy.wait()

        norm_copy(g).start()
        weights = r.gu_map[...].reshape(-1, r.gu_map.shape[3])
        acts = dot(all_ref[g], weights)
        gate, up = acts[:, :inner], acts[:, inner:]
        sigma = jax.nn.sigmoid(gate)
        silu = gate * sigma
        r.hidden[two] = (silu * up).astype(BF)
        grad_hidden = r.grad_hidden[g]
        grad_gate = grad_hidden * up * sigma * (1.0 + gate * (1.0 - sigma))
        r.gu_grad[two] = jnp.concatenate([grad_gate, grad_hidden * silu], 1).astype(BF)
        for copy in out_copies(step):
            copy.start()

    each_step(size, feed)
    keeps.append(pltpu.make_async_copy(r.grads, r.grads_hbm, r.stores.at[size + 4]))
    keeps[4].start()
    for k in range(4):
        for step in others:
            swap(k, step).wait_send()
    scatter.finish()
    gather.finish()
    grads.finish()
    line_q.finish()
    line_u.finish()

    @pl.when(rank < parts - 1)
    def _():
        edge_rows().wait_send()
        for step in range(size):
            halo(step).wait_send()

    for keep in keeps[1:]:
        keep.wait()
    for g in range(size):
        norm_copy(g).wait()
    for step in (size - 2, size - 1):
        for copy in out_copies(step):
            copy.wait()


def forward_part(ident, count, tokens, cot, gains, table, qkv_piece, gu_piece, out_weight, down_weight):
    size, parts = lax.axis_size("fsdp"), lax.axis_size("seq")
    rows, width = tokens.shape
    local, inner = out_weight.shape[0], down_weight.shape[0]
    piece, cols = gu_piece.shape[1:]
    vmem = pl.BlockSpec(memory_space=pltpu.VMEM)
    hbm = pl.BlockSpec(memory_space=pl.ANY)
    shape = lambda w: (size, rows, w)
    low = lambda s: jax.ShapeDtypeStruct(s, BF)
    maps = [(size, parts, piece, 3 * local), (size, parts, piece, cols)]
    dma = lambda *s: pltpu.SemaphoreType.DMA(s)
    hop = transfers(size)
    scratch = scatter_shapes(size, rows, width)
    return pl.pallas_call(
        functools.partial(forward_kernel, size, parts, count),
        out_shape=[
            low(shape(width)),
            low(shape(3 * local)),
            low((size, WINDOW, 2 * local)),
            low(maps[0]),
            jax.ShapeDtypeStruct((rows, width), F32),
            low(shape(local)),
            low(shape(width)),
            low(shape(width)),
            low(shape(inner)),
            low(shape(cols)),
            low(maps[1]),
            low((size,) + gains.shape),
            jax.ShapeDtypeStruct((size,) + table.shape, jnp.int32),
            low((8, width)),
        ],
        in_specs=[vmem] * 4 + [hbm, hbm, vmem, vmem],
        out_specs=[hbm, hbm, vmem, hbm, vmem, vmem, hbm, hbm, hbm, hbm, hbm, vmem, vmem, vmem],
        scratch_shapes=scratch[:-2]
        + [
            pltpu.VMEM(shape(width), BF),
            pltpu.VMEM(shape(width), BF),
            pltpu.VMEM(shape(3 * local), BF),
            pltpu.VMEM(maps[0], BF),
            pltpu.VMEM(maps[1], BF),
            pltpu.VMEM((size, WINDOW, 2 * local), BF),
            pltpu.VMEM((rows, width), F32),
            pltpu.VMEM(shape(inner), F32),
            pltpu.VMEM((2, rows, inner), BF),
            pltpu.VMEM((2, rows, cols), BF),
        ]
        + [dma(hop)] * 8
        + [dma(4, size - 1)] * 2
        + [dma(size)] * 2
        + [pltpu.SemaphoreType.DMA] * 2
        + [dma(2), dma(size + 5), dma(2), dma(2)]
        + line_sems(parts)
        + line_sems(parts),
        compiler_params=pltpu.CompilerParams(
            collective_id=ident, has_side_effects=True, vmem_limit_bytes=67_000_000
        ),
        cost_estimate=pl.CostEstimate(
            flops=2 * size * rows * width * (4 * local + 3 * inner),
            bytes_accessed=500_000_000,
            transcendentals=0,
        ),
        name="forward_part",
    )(tokens, cot, gains, table, qkv_piece, gu_piece, out_weight, down_weight)


def heads_back(group, slot, count, lens_ref, starts_ref, own, edge, grad):
    rows, local = own.shape[0], own.shape[1] // 3
    head_of = lane_head(local)
    queries = own[:, :local]
    keys = jnp.concatenate([edge[:, :local], own[:, local : 2 * local]], 0)
    values = jnp.concatenate([edge[:, local:], own[:, 2 * local :]], 0)
    dqs, dks, dvs = [], [], []
    for block in range(rows // BLOCK):
        mask = masks_of(
            slot, block, count, lambda j: lens_ref[group, j], lambda j: starts_ref[group, j]
        )
        low = block * BLOCK
        span = slice(low, low + BLOCK + WINDOW)
        query, grads = queries[low : low + BLOCK], grad[low : low + BLOCK]
        key, value = keys[span], values[span]
        dq = jnp.zeros((BLOCK, local), F32)
        dk = jnp.zeros((BLOCK + WINDOW, local), F32)
        dv = jnp.zeros((BLOCK + WINDOW, local), F32)
        for head in range(local // HEAD_DIM):
            mine = head_of == head
            own_q = jnp.where(mine, query, jnp.zeros_like(query))
            own_g = jnp.where(mine, grads, jnp.zeros_like(grads))
            soft = soft_of(own_q, key, mask)
            grad_soft = dot_trans(own_g, value)
            total = jnp.sum(grad_soft * soft, axis=1, keepdims=True)
            grad_scores = (soft * (grad_soft - total)).astype(BF)
            dq = jnp.where(mine, dot(grad_scores, key), dq)
            dk = dk + dot_rows(grad_scores, own_q)
            dv = dv + dot_rows(soft.astype(BF), own_g)
        dqs.append(dq * SCALE)
        dks.append(dk * SCALE)
        dvs.append(dv)

    def joined(pieces):
        out = [pieces[0][:BLOCK]]
        for left, right in zip(pieces, pieces[1:]):
            out.append(left[BLOCK:] + right[:WINDOW])
            out.append(right[WINDOW:BLOCK])
        out.append(pieces[-1][BLOCK:])
        return jnp.concatenate(out, 0)

    return jnp.concatenate(dqs, 0), joined(dks), joined(dvs)


class BackRefs(NamedTuple):
    lens: Any
    starts: Any
    grad_gu_hbm: Any
    gu_map_hbm: Any
    middle: Any
    grads_hbm: Any
    gain: Any
    out_map: Any
    edge: Any
    qkv: Any
    qkv_map_hbm: Any
    gu_x: Any
    down_x: Any
    grad_middle: Any
    norm: Any
    all: Any
    dqkv: Any
    own: Any
    gu_slots: Any
    down_every: Any
    gu_pre: Any
    gu_up: Any
    gu_down: Any
    down_pre: Any
    down_up: Any
    down_down: Any
    part: Any
    first: Any
    over: Any
    joined: Any
    last: Any
    s_send: Any
    s_recv: Any
    t_send: Any
    t_recv: Any
    g_send: Any
    g_recv: Any
    grad_gu: Any
    gu_map: Any
    qkv_map: Any
    dedge: Any
    back: Any
    tail: Any
    h_send: Any
    h_recv: Any
    loads: Any
    gu_acc: Any
    gu_stage: Any
    gu_load: Any
    down_acc: Any
    down_stage: Any
    down_load: Any
    m_send: Any
    m_recv: Any
    grad: Any


def back_kernel(size, parts, count, *refs):
    named = len(BackRefs._fields)
    r, sems = BackRefs(*refs[:named]), refs[named:]
    line = Line(parts, sems[:6])
    gu_sum = StagedSum(
        r.gu_stage, r.gu_load, line, r.gu_x, r.gu_pre, r.gu_acc, r.gu_up, r.gu_down, sems[6:12]
    )
    down_sum = StagedSum(
        r.down_stage,
        r.down_load,
        line,
        r.down_x,
        r.down_pre,
        r.down_acc,
        r.down_up,
        r.down_down,
        sems[12:],
    )
    rows = r.middle.shape[0]
    local = r.out_map.shape[0]
    rank = lax.axis_index("seq")
    slot = rank * rows
    group = Group(size)
    barrier = pltpu.get_barrier_semaphore()
    greet_group(barrier, size)

    def greet(peer):
        pl.semaphore_signal(barrier, inc=1, device_id={"seq": peer}, device_id_type=MESH_ID)

    known = line.greet(barrier)
    pl.when(line.has_above & (line.core == 1))(lambda: greet(rank + 1))
    pl.when(line.has_below & (line.core == 0))(lambda: greet(rank - 1))
    n, z = line.length, line.z
    known = known + (2 * n - 2 - z) // n * line.core + (z + n - 1) // n * (1 - line.core)
    fetches = [
        pltpu.make_async_copy(src, dst, r.loads.at[k])
        for k, (src, dst) in enumerate(
            (
                (r.grad_gu_hbm, r.grad_gu),
                (r.gu_map_hbm, r.gu_map),
                (r.qkv_map_hbm, r.qkv_map),
                (r.grads_hbm.at[group.me], r.grad),
            )
        )
    ]
    for fetch in fetches:
        fetch.start()
    pl.semaphore_wait(barrier, size - 1 + known)
    down_sum.trade()
    gu_sum.trade()
    for m in range(n):
        down_sum.begin(m)
    scatter = Scatter(
        group, r.part, r.first, r.over, r.joined, r.last, r.s_send, r.s_recv
    )
    gather = Gather(group, r.all, r.g_send, r.g_recv)
    fetches[0].wait()
    fetches[1].wait()
    fetches[3].wait()

    def step_two(step, is_step):
        partial = dot_trans(r.grad_gu[group.to_own(step)], r.gu_map[...])
        is_step(size - 1)(lambda: r.own.__setitem__(..., partial))
        pl.when(step < size - 1)(lambda: r.part.__setitem__(step, partial.astype(BF)))
        for k in range(size - 1):
            is_step(k)(functools.partial(scatter.made, k))

    each_step(size, step_two)
    scatter.join()
    gu_sum.begin(0)
    down_sum.advance(1)
    half = rows // 2
    norm_sum = jnp.zeros((1, r.middle.shape[1]), F32)
    for h in range(2):
        span = slice(h * half, (h + 1) * half)
        grad = r.own[span, :] + scatter.total(h)
        middle = r.middle[span, :]
        scale = lax.rsqrt(jnp.mean(middle * middle, axis=1, keepdims=True) + EPS)
        unit = middle * scale
        scaled = grad * r.gain[...]
        norm_sum = norm_sum + jnp.sum(grad * unit, axis=0, keepdims=True)
        grad_out = r.grad[span, :].astype(F32)
        grad_middle = grad_out + scale * (
            scaled - unit * jnp.mean(scaled * unit, axis=1, keepdims=True)
        )
        r.grad_middle[span, :] = grad_middle
        r.all[group.me, span] = grad_middle.astype(BF)
        gather.start_half(h)
    r.norm[...] = norm_sum
    own_down = pltpu.make_async_copy(r.down_acc.at[z], r.down_every.at[rank], r.down_load.at[0])

    def halo(step):
        g = group.from_own(step)
        sems = r.h_send.at[step], r.h_recv.at[step]
        return remote(r.dedge.at[g], r.back.at[g], *sems, seq=rank - 1)

    def step_heads(step, is_step):
        g = group.from_own(step)

        @is_step(1)
        def _():
            gather.relay()
            for t in range(2, n - 1):
                down_sum.advance(t)

        @is_step(2)
        def _():
            down_sum.total()
            own_down.start()
            own_down.wait()
            line.gather(lambda owner: r.down_every.at[owner])

        for k in range(1, size):
            is_step(k)(functools.partial(gather.ready, k))
        grad = dot_trans(r.all[g], r.out_map[...]).astype(BF)
        dq, dk, dv = heads_back(
            g, slot, count, r.lens, r.starts, r.qkv[g], r.edge[g], grad
        )
        r.dedge[g] = jnp.concatenate([dk[:WINDOW], dv[:WINDOW]], 1).astype(BF)
        full = jnp.concatenate([dq, dk[WINDOW:], dv[WINDOW:]], 1)
        r.dqkv[g] = full.astype(BF)
        r.tail[g] = full[rows - WINDOW :]
        pl.when(rank > 0)(lambda: halo(step).start())

    each_step(size, step_heads)
    gu_sum.advance(1)
    for m in range(1, n):
        gu_sum.begin(m)
    line.relay(1)
    scatter.finish()
    fetches[2].wait()

    @pl.when(rank == parts - 1)
    def _():
        r.back[...] = jnp.zeros_like(r.back)

    @pl.when(rank < parts - 1)
    def _():
        for step in range(size):
            halo(step).wait_recv()

    scatter = Scatter(
        group, r.part, r.first, r.over, r.joined, r.last, r.t_send, r.t_recv
    )

    def step_one(step, is_step):
        g = group.to_own(step)
        back = r.back[g].astype(F32)
        wide = jnp.concatenate([jnp.zeros((WINDOW, local), F32), back], 1)
        r.dqkv[g, pl.ds(rows - WINDOW, WINDOW)] = (r.tail[g] + wide).astype(BF)
        partial = dot_trans(r.dqkv[g], r.qkv_map[...])
        is_step(size - 1)(lambda: r.own.__setitem__(..., partial))
        pl.when(step < size - 1)(lambda: r.part.__setitem__(step, partial.astype(BF)))
        for k in range(size - 1):
            is_step(k)(functools.partial(scatter.made, k))

    each_step(size, step_one)
    scatter.join()
    for t in range(2, n - 1):
        gu_sum.advance(t)
        line.relay(t)
    line.relay(n - 1)
    for h in range(2):
        span = slice(h * half, (h + 1) * half)
        r.own[span, :] = r.own[span, :] + scatter.total(h)
    gu_sum.total()

    def swap(step):
        peer = lax.rem(group.me + step, size)
        sems = r.m_send.at[step - 1], r.m_recv.at[step - 1]
        return remote(r.gu_acc.at[z, peer], r.gu_slots.at[group.me], *sems, fsdp=peer)

    for step in range(1, size):
        swap(step).start()
    own_slot = pltpu.make_async_copy(
        r.gu_acc.at[z, group.me], r.gu_slots.at[group.me], r.gu_load.at[0]
    )
    own_slot.start()
    for j in range(1, n):
        line.close(j)
    line.gathered()
    for step in range(1, size):
        swap(step).wait()
    scatter.finish()
    gather.finish()
    down_sum.finish()
    gu_sum.finish()
    line.finish()
    own_slot.wait()

    @pl.when(rank > 0)
    def _():
        for step in range(size):
            halo(step).wait_send()


def back_part(
    ident, lens, starts, grad_gu, gu_map, middle, grads, gain, out_weight, edge, qkv, qkv_map, gu_x, down_x
):
    size, parts = lax.axis_size("fsdp"), lax.axis_size("seq")
    rows, width = middle.shape
    local = out_weight.shape[0]
    n = parts // 2
    vmem = pl.BlockSpec(memory_space=pltpu.VMEM)
    smem = pl.BlockSpec(memory_space=pltpu.SMEM)
    hbm = pl.BlockSpec(memory_space=pl.ANY)
    dma = lambda *s: pltpu.SemaphoreType.DMA(s)
    low = lambda *s: jax.ShapeDtypeStruct(s, BF)
    sems = [dma(transfers(size))] * 2
    gu, down = gu_x.shape[1:], down_x.shape[1:]
    outs = pl.pallas_call(
        functools.partial(back_kernel, size, parts, lens.shape[1]),
        out_shape=[
            jax.ShapeDtypeStruct((rows, width), F32),
            jax.ShapeDtypeStruct((1, width), F32),
            low(size, rows, width),
            low(*qkv.shape),
            jax.ShapeDtypeStruct((rows, width), F32),
            low(*gu),
            low(parts, *down),
        ]
        + [low(n, *gu)] * 3
        + [low(n, *down)] * 3,
        in_specs=[smem, smem, hbm, hbm, vmem, hbm] + [vmem] * 4 + [hbm] * 3,
        out_specs=[vmem] * 5 + [hbm] * 8,
        scratch_shapes=scatter_shapes(size, rows, width)
        + sems
        + sems
        + [
            pltpu.VMEM(grad_gu.shape, BF),
            pltpu.VMEM(gu_map.shape, BF),
            pltpu.VMEM(qkv_map.shape, BF),
            pltpu.VMEM((size, WINDOW, 2 * local), BF),
            pltpu.VMEM((size, WINDOW, 2 * local), BF),
            pltpu.VMEM((size, WINDOW, 3 * local), F32),
            dma(size),
            dma(size),
            dma(4),
            pltpu.VMEM((n,) + gu, BF),
            pltpu.VMEM((2,) + gu, BF),
            dma(2),
            pltpu.VMEM((n,) + down, BF),
            pltpu.VMEM((2,) + down, BF),
            dma(2),
            dma(size - 1),
            dma(size - 1),
            pltpu.VMEM((rows, width), BF),
        ]
        + line_sems(parts) * 3,
        compiler_params=pltpu.CompilerParams(
            collective_id=ident, has_side_effects=True, vmem_limit_bytes=67_000_000
        ),
        cost_estimate=pl.CostEstimate(
            flops=2 * size * rows * (gu_map.size + qkv_map.size + width * local),
            bytes_accessed=400_000_000,
            transcendentals=0,
        ),
        name="back_part",
    )(lens, starts, grad_gu, gu_map, middle, grads, gain, out_weight, edge, qkv, qkv_map, gu_x, down_x)
    return outs[:7]


class CloseRefs(NamedTuple):
    gated_hbm: Any
    dqkv_hbm: Any
    heads_hbm: Any
    gb_hbm: Any
    gu_slots: Any
    terms: Any
    hidden_hbm: Any
    down_hbm: Any
    every_hbm: Any
    gu_every: Any
    feed: Any
    terms_out: Any
    pre: Any
    up_in: Any
    down_in: Any
    part: Any
    first: Any
    over: Any
    joined: Any
    last: Any
    x: Any
    acc: Any
    stage: Any
    stage_load: Any
    every: Any
    slots: Any
    gu_own: Any
    gated: Any
    dqkv: Any
    heads: Any
    gb: Any
    hidden: Any
    down_map: Any
    terms_in: Any
    terms_all: Any
    s_send: Any
    s_recv: Any
    m_send: Any
    m_recv: Any
    t_send: Any
    t_recv: Any
    loads: Any


def close_kernel(size, parts, made, *refs):
    named = len(CloseRefs._fields)
    r, sems = CloseRefs(*refs[:named]), refs[named:]
    rank = lax.axis_index("seq")
    group = Group(size)
    me = group.me
    line_u, line_q = Line(parts, sems[:6]), Line(parts, sems[6:12])
    n, z = line_q.length, line_q.z
    sums = MixedSum(
        r.stage, r.stage_load, line_q, r.x, r.pre, r.acc, r.up_in, r.down_in, sems[12:]
    )
    rows = r.feed.shape[0]
    half = rows // 2
    barrier = pltpu.get_barrier_semaphore()
    greet_group(barrier, size)
    for step in range(1, parts):
        peer = lax.rem(rank + step, parts)
        pl.semaphore_signal(barrier, inc=1, device_id={"seq": peer}, device_id_type=MESH_ID)
    moves = [
        (r.gu_slots, r.gu_own),
        (r.hidden_hbm, r.hidden),
        (r.down_hbm, r.down_map),
    ]
    if made:
        moves += [
            (r.gated_hbm, r.gated),
            (r.dqkv_hbm, r.dqkv),
            (r.heads_hbm, r.heads),
            (r.gb_hbm, r.gb),
        ]
    else:
        moves += [(r.gated_hbm, r.x)]
    fetches = [
        pltpu.make_async_copy(src, dst, r.loads.at[k]) for k, (src, dst) in enumerate(moves)
    ]
    for k in [0] + list(range(3, len(moves))) + [1, 2]:
        fetches[k].start()
    r.terms_in[me] = r.terms[me]
    own_slots = pltpu.make_async_copy(r.gu_own, r.gu_every.at[rank], r.loads.at[0])
    fetches[0].wait()
    own_slots.start()
    own_slots.wait()
    pl.semaphore_wait(barrier, size + parts - 2)
    line_u.gather(lambda owner: r.gu_every.at[owner])

    def swap(k, step):
        peer = lax.rem(me + step, size)
        src, dst = (
            lambda: (r.terms.at[peer], r.terms_in.at[me]),
            lambda: (r.acc.at[z, peer], r.slots.at[me]),
        )[k]()
        return remote(src, dst, r.m_send.at[k, step - 1], r.m_recv.at[k, step - 1], fsdp=peer)

    others = range(1, size)
    for step in others:
        swap(0, step).start()

    scatter = Scatter(
        group, r.part, r.first, r.over, r.joined, r.last, r.s_send, r.s_recv
    )

    def down(step, is_step):
        partial = dot(r.hidden[group.to_own(step)], r.down_map[...])
        is_step(size - 1)(lambda: r.feed.__setitem__(..., partial))
        pl.when(step < size - 1)(lambda: r.part.__setitem__(step, partial.astype(BF)))
        for k in range(size - 1):
            is_step(k)(functools.partial(scatter.made, k))

    for fetch in fetches[3:]:
        fetch.wait()
    if made:
        span = r.gated.shape[1] // (size // 2)
        for h in range(size // 2):
            lanes = slice(h * span, (h + 1) * span)
            pack_pair(
                r.x, h, r.gated[:, lanes], r.dqkv[...], r.heads[...], r.gb[:, lanes]
            )
    sums.trade()
    line_u.relay(1)
    fetches[1].wait()
    fetches[2].wait()
    for m in range(n):
        sums.begin(m)
    each_step(size, down)

    for step in others:
        swap(0, step).wait_recv()
    small = r.terms_in[0]
    for f in others:
        small = small + r.terms_in[f]
    r.terms_all[rank] = small

    def spread(step):
        peer = lax.rem(rank + step, parts)
        view = r.terms_all.at[rank]
        return remote(view, view, r.t_send.at[step - 1], r.t_recv.at[step - 1], seq=peer)

    for step in range(1, parts):
        spread(step).start()
    scatter.join()

    for t in range(1, n - 1):
        sums.advance(t)
        line_u.relay(t + 1)
    for h in range(2):
        span = slice(h * half, (h + 1) * half)
        r.feed[span, :] = r.feed[span, :] + scatter.total(h)
    sums.total()
    for step in others:
        swap(1, step).start()
    for j in range(1, n):
        line_u.close(j)
    r.slots[me] = r.acc[z, me]
    for step in others:
        swap(1, step).wait_recv()
    local = r.x.shape[3] // 4
    lane = lax.broadcasted_iota(jnp.int32, (1, 1, 4 * local), 2)
    r.every[rank] = jnp.where(lane < 3 * local, r.slots[...], r.acc[z])
    line_q.gather(lambda owner: r.every.at[owner])
    line_u.gathered()
    for j in range(1, n):
        line_q.relay(j)
    for j in range(1, n):
        line_q.close(j)
    line_q.gathered()
    store = pltpu.make_async_copy(r.every, r.every_hbm, r.loads.at[1])
    store.start()
    for step in range(1, parts):
        spread(step).wait_recv()
    small = r.terms_all[0]
    for k in range(1, parts):
        small = small + r.terms_all[k]
    r.terms_out[...] = small
    for k in range(2):
        for step in others:
            swap(k, step).wait_send()
    for step in range(1, parts):
        spread(step).wait_send()
    scatter.finish()
    sums.finish()
    line_u.finish()
    line_q.finish()
    store.wait()


def close_part(ident, gated, dqkv, heads, gb, gu_slots, terms, hidden, down_weight):
    size, parts = lax.axis_size("fsdp"), lax.axis_size("seq")
    width = gated.shape[1]
    made = packs(size, parts, width)
    piece, cols = width // (size * parts), dqkv.shape[1] + heads.shape[1]
    if not made:
        gated = pack_plain(parts, size, gated, dqkv, heads, gb)
    n = parts // 2
    rows = hidden.shape[1]
    vmem = pl.BlockSpec(memory_space=pltpu.VMEM)
    hbm = pl.BlockSpec(memory_space=pl.ANY)
    dma = lambda *s: pltpu.SemaphoreType.DMA(s)
    gu_shape = (parts,) + gu_slots.shape
    packed = (parts, size, piece, cols)
    scratch = scatter_shapes(size, rows, width)
    low = lambda *s: jax.ShapeDtypeStruct(s, BF)
    copy_of = lambda a: pltpu.VMEM(a.shape if made else (8, 128), BF)
    return pl.pallas_call(
        functools.partial(close_kernel, size, parts, made),
        out_shape=[
            low(*packed),
            low(*gu_shape),
            jax.ShapeDtypeStruct((rows, width), F32),
            jax.ShapeDtypeStruct(terms.shape[1:], F32),
        ]
        + [low(n, size, piece, cols)] * 3,
        in_specs=[hbm] * 5 + [vmem, hbm, hbm],
        out_specs=[hbm, hbm, vmem, vmem, hbm, hbm, hbm],
        scratch_shapes=scratch[:-2]
        + [
            pltpu.VMEM(packed, BF),
            pltpu.VMEM((n, size, piece, cols), BF),
            pltpu.VMEM((2, size, piece, cols), BF),
            dma(2),
            pltpu.VMEM(packed, BF),
            pltpu.VMEM((size, piece, cols), BF),
            pltpu.VMEM(gu_slots.shape, BF),
            copy_of(gated),
            copy_of(dqkv),
            copy_of(heads),
            copy_of(gb),
            pltpu.VMEM(hidden.shape, BF),
            pltpu.VMEM(down_weight.shape, BF),
            pltpu.VMEM(terms.shape, F32),
            pltpu.VMEM((parts,) + terms.shape[1:], F32),
        ]
        + scratch[-2:]
        + [dma(2, size - 1)] * 2
        + [dma(parts - 1)] * 2
        + [dma(7)]
        + line_sems(parts) * 3,
        compiler_params=pltpu.CompilerParams(
            collective_id=ident, has_side_effects=True, vmem_limit_bytes=67_000_000
        ),
        cost_estimate=pl.CostEstimate(
            flops=2 * size * rows * (down_weight.size + width * cols),
            bytes_accessed=500_000_000,
            transcendentals=0,
        ),
        name="close_part",
    )(gated, dqkv, heads, gb, gu_slots, terms, hidden, down_weight)[:4]


def pack_pair(out, pair, x, g, heads=None, gb=None):
    parts, _, piece, _ = out.shape
    rows = parts * piece
    full = dot_rows(x, g)
    side = None if heads is None else dot_rows(heads, gb)
    for k in range(2):
        own = full[k * rows : (k + 1) * rows]
        if side is not None:
            wide = side.shape[1] // 2
            own = jnp.concatenate([own, side[:, k * wide : (k + 1) * wide]], 1)
        out[:, pair * 2 + k] = own.astype(BF).reshape(parts, piece, own.shape[1])


def pack_kernel(x_ref, g_ref, out_ref):
    pack_pair(out_ref, 0, x_ref[...], g_ref[...])


def down_kernel(x_ref, g_ref, out_ref):
    out_ref[...] = dot_rows(x_ref[...], g_ref[...]).astype(BF)


def down_grad(x, g):
    total, inner = x.shape
    half = g.shape[1] // 2
    return pl.pallas_call(
        down_kernel,
        grid=(2,),
        out_shape=jax.ShapeDtypeStruct((inner, 2 * half), BF),
        in_specs=[
            pl.BlockSpec(x.shape, lambda i: (0, 0), pipeline_mode=pl.Buffered(1)),
            pl.BlockSpec((total, half), lambda i: (0, i)),
        ],
        out_specs=pl.BlockSpec((inner, half), lambda i: (0, i)),
        cost_estimate=pl.CostEstimate(
            flops=4 * total * inner * half,
            bytes_accessed=2 * (x.size + g.size) + 4 * inner * half,
            transcendentals=0,
        ),
        name="down_grad",
    )(x, g)


def packs(size, parts, width):
    return width // (size * parts) % 8 == 0 and 2 * width // size % 128 == 0


def pack_plain(parts, size, x, g, heads=None, gb=None):
    width, cols = x.shape[1], g.shape[1]
    piece = width // (size * parts)
    full = dot_rows(x, g).reshape(size, parts, piece, cols)
    if heads is not None:
        side = dot_rows(heads, gb).reshape(parts, piece, size, -1).transpose(2, 0, 1, 3)
        full = jnp.concatenate([full, side], 3)
    return full.transpose(1, 0, 2, 3).astype(BF)


def pack_grads(parts, size, x, g):
    total, width = x.shape
    cols = g.shape[1]
    if not packs(size, parts, width):
        return pack_plain(parts, size, x, g)
    piece = width // (size * parts)
    pair = pl.BlockSpec((total, 2 * width // size), lambda i: (0, i))
    whole = pl.BlockSpec(g.shape, lambda i: (0, 0), pipeline_mode=pl.Buffered(1))
    return pl.pallas_call(
        pack_kernel,
        grid=(size // 2,),
        out_shape=jax.ShapeDtypeStruct((parts, size, piece, cols), BF),
        in_specs=[pair, whole],
        out_specs=pl.BlockSpec((parts, 2, piece, cols), lambda i: (0, i, 0, 0)),
        cost_estimate=pl.CostEstimate(
            flops=2 * total * width * cols,
            bytes_accessed=2 * (x.size + g.size + width * cols),
            transcendentals=0,
        ),
        name="pack_grads",
    )(x, g)


def unpack_kernel(widths, *refs):
    outs = list(refs[len(widths) :])
    for every_ref, wide in zip(refs, widths):
        blocks = [every_ref[0, i].astype(F32) for i in range(every_ref.shape[1])]
        low = 0
        for width in wide:
            outs.pop(0)[...] = jnp.concatenate([b[:, low : low + width] for b in blocks], 1)
            low += width


def unpack_grads(arrays, widths):
    parts, size, piece, _ = arrays[0].shape
    every = [w for wide in widths for w in wide]
    if piece % 8:
        outs = []
        for array, wide in zip(arrays, widths):
            low = 0
            for width in wide:
                block = array[:, :, :, low : low + width].transpose(0, 2, 1, 3)
                outs.append(block.reshape(parts * piece, size * width).astype(F32))
                low += width
        return outs
    return pl.pallas_call(
        functools.partial(unpack_kernel, widths),
        grid=(parts,),
        out_shape=[jax.ShapeDtypeStruct((parts * piece, size * w), F32) for w in every],
        in_specs=[
            pl.BlockSpec((1, size, piece, a.shape[3]), lambda i: (i, 0, 0, 0)) for a in arrays
        ],
        out_specs=[pl.BlockSpec((piece, size * w), lambda i: (i, 0)) for w in every],
        cost_estimate=pl.CostEstimate(
            flops=0, bytes_accessed=6 * sum(a.size for a in arrays), transcendentals=0
        ),
        name="unpack_grads",
    )(*arrays)


def columns_piece(weights, part, parts):
    size = lax.axis_size("fsdp")
    rows = weights[0].shape[0] // parts
    pieces = []
    for weight in weights:
        own = lax.dynamic_slice_in_dim(weight, part * rows, rows, 0)
        pieces.append(own.reshape(rows, size, -1))
    return jnp.concatenate(pieces, 2).transpose(1, 0, 2)


def shards(
    tokens,
    seq_lengths,
    seq_offsets,
    norm1_gain,
    conv_weight,
    query_weight,
    key_weight,
    value_weight,
    out_weight,
    norm2_gain,
    gate_weight,
    up_weight,
    down_weight,
    cotangent,
):
    size = lax.axis_size("fsdp")
    parts = lax.axis_size("seq")
    part = lax.axis_index("seq")
    me = lax.axis_index("fsdp")
    own_tokens = tokens[0]
    rows, width = own_tokens.shape
    slice_width = norm1_gain.shape[0]
    first_slot = part * rows
    count = seq_lengths.shape[1]

    slot_ext = first_slot - 2 + jnp.arange(rows + 2, dtype=jnp.int32)
    segment_ext = segment_of(
        slot_ext, count, lambda j: seq_lengths[0, j], lambda j: seq_offsets[0, j]
    )
    segment_own = segment_ext[2:]
    same_one = (segment_own == segment_ext[1:-1]).astype(F32)[:, None]
    same_two = (segment_own == segment_ext[:-2]).astype(F32)[:, None]
    live_mask = (segment_own >= 0).astype(F32)[:, None]

    gains = jnp.concatenate(
        [
            norm1_gain[None],
            norm2_gain[None],
            conv_weight.T,
            jnp.zeros((3, slice_width), BF),
        ],
        0,
    )
    table = jnp.zeros((8, 128), jnp.int32)
    table = table.at[0, :count].set(seq_lengths[0]).at[1, :count].set(seq_offsets[0])
    qkv_piece = columns_piece((query_weight, key_weight, value_weight), part, parts)
    gu_piece = columns_piece((gate_weight, up_weight), part, parts)
    (
        gated_all,
        qkv,
        edge,
        qkv_map,
        middle,
        heads_out,
        grad_down_all,
        normed_all,
        hidden,
        grad_gu,
        gu_map,
        gains_all,
        table_all,
        edge_tokens,
    ) = forward_part(
        0,
        count,
        own_tokens,
        cotangent[0],
        gains,
        table,
        qkv_piece,
        gu_piece,
        out_weight,
        down_weight,
    )
    local = out_weight.shape[0]
    flat = lambda a: a.reshape(-1, a.shape[-1])
    lens_all, starts_all = table_all[:, 0, :count], table_all[:, 1, :count]
    gains_all = gains_all.transpose(1, 0, 2).reshape(8, width)
    norm_one = gains_all[0].astype(F32)
    norm_two = gains_all[1].astype(F32)
    taps = gains_all[2:5].astype(F32)
    qkv_map, gu_map = qkv_map.reshape(width, -1), gu_map.reshape(width, -1)

    extended = jnp.concatenate([edge_tokens[6:], own_tokens], 0).astype(F32)
    scale_one = lax.rsqrt(jnp.mean(extended * extended, axis=1, keepdims=True) + EPS)
    normed = extended * scale_one * norm_one
    conv_mix = (
        normed[2:] * taps[0]
        + same_one * normed[1:-1] * taps[1]
        + same_two * normed[:-2] * taps[2]
    )

    gu_packed = pack_grads(parts, size, flat(normed_all), flat(grad_gu))
    down_packed = down_grad(flat(hidden), flat(grad_down_all))
    grad_middle, norm2_term, grad_branch_all, dqkv, grad_gated, gu_slots, down_every = back_part(
        4,
        lens_all,
        starts_all,
        grad_gu,
        gu_map,
        middle,
        grad_down_all,
        norm_two[None],
        out_weight,
        edge,
        qkv,
        qkv_map,
        gu_packed,
        down_packed.reshape(parts, -1, width),
    )
    norm2_term = norm2_term[0]
    down_total = down_every.reshape(-1, width).astype(F32)
    normed_own = normed[2:]
    grad_mix = grad_gated * normed_own
    part_zero = jnp.pad(grad_gated * conv_mix + grad_mix * taps[0], ((2, 0), (0, 0)))
    part_one = jnp.pad(grad_mix * same_one * taps[1], ((1, 1), (0, 0)))
    part_two = jnp.pad(grad_mix * same_two * taps[2], ((0, 2), (0, 0)))
    grad_normed = part_zero + part_one + part_two
    unit_one = extended * scale_one
    grad_unit_one = grad_normed * norm_one
    grad_extended = scale_one * (
        grad_unit_one - unit_one * jnp.mean(grad_unit_one * unit_one, axis=1, keepdims=True)
    )
    edge_back = shifted(grad_extended[:2], "seq", -1)
    tokens_grad = grad_middle + grad_extended[2:] + jnp.pad(edge_back, ((rows - 2, 0), (0, 0)))

    terms = jnp.stack(
        [
            jnp.sum(grad_normed * unit_one, axis=0),
            norm2_term,
            jnp.sum(grad_mix * normed_own, axis=0),
            jnp.sum(grad_mix * same_one * normed[1:-1], axis=0),
            jnp.sum(grad_mix * same_two * normed[:-2], axis=0),
        ]
    )
    terms = jnp.pad(terms, ((0, 3), (0, 0))).reshape(8, size, slice_width).transpose(1, 0, 2)
    qkvo_every, gu_every, feed, terms = close_part(
        5,
        flat(gated_all),
        flat(dqkv),
        flat(heads_out),
        flat(grad_branch_all),
        gu_slots,
        terms,
        hidden,
        down_weight,
    )
    gate_total, up_total, query_total, key_total, value_total, out_total = unpack_grads(
        (gu_every, qkvo_every), ((gu_map.shape[1] // 2,) * 2, (local,) * 4)
    )

    layer_out = (live_mask * (middle + feed)).astype(BF)[None]
    return (
        layer_out,
        tokens_grad[None],
        terms[0],
        terms[2:5].T,
        query_total,
        key_total,
        value_total,
        out_total,
        terms[1],
        gate_total,
        up_total,
        down_total,
    )


def solution(mesh):
    placed = (
        P("fsdp", "seq", None),
        P("fsdp", None),
        P("fsdp", None),
        P("fsdp"),
        P("fsdp", None),
        P("fsdp", None),
        P("fsdp", None),
        P("fsdp", None),
        P("fsdp", None),
        P("fsdp"),
        P("fsdp", None),
        P("fsdp", None),
        P("fsdp", None),
        P("fsdp", "seq", None),
    )
    return jax.shard_map(
        shards,
        mesh=mesh,
        in_specs=placed,
        out_specs=(
            P("fsdp", "seq", None),
            P("fsdp", "seq", None),
            P("fsdp"),
            P("fsdp", None),
            P("fsdp", None),
            P("fsdp", None),
            P("fsdp", None),
            P("fsdp", None),
            P("fsdp"),
            P("fsdp", None),
            P("fsdp", None),
            P("fsdp", None),
        ),
        check_vma=False,
    )
```

```python
import functools
from typing import Any, NamedTuple

import jax
import jax.numpy as jnp
from jax import lax
from jax.experimental import pallas as pl
from jax.experimental.pallas import tpu as pltpu
from jax.sharding import PartitionSpec as P

HEADS = 16
WINDOW = 64
HEAD_DIM = 112
BLOCK = 128

EPS = 1e-05
NEG = -1e30
SCALE = HEAD_DIM ** (-0.5)
MESH_ID = pl.DeviceIdType.MESH
BF = jnp.bfloat16
F32 = jnp.float32


def shifted(array, axis, by):
    length = lax.axis_size(axis)
    pairs = [(i, i + by) for i in range(length) if 0 <= i + by < length]
    return lax.ppermute(array, axis, pairs)


def segment_of(slot, count, lengths, starts):
    found = jnp.full(slot.shape, -1, jnp.int32)
    for j in range(count):
        inside = (slot >= starts(j)) & (slot < starts(j) + lengths(j))
        found = jnp.where(inside, j, found)
    return jnp.where(slot < 0, -2, found)


def dot_rows(left, right):
    return lax.dot_general(left, right, (((0,), (0,)), ((), ())), preferred_element_type=F32)


def dot_trans(left, right):
    return lax.dot_general(left, right, (((1,), (1,)), ((), ())), preferred_element_type=F32)


def dot(left, right):
    return jnp.dot(left, right, preferred_element_type=F32)


def masks_of(first, block, count, length, start):
    rows = first + block * BLOCK
    query = rows + lax.broadcasted_iota(jnp.int32, (BLOCK, 1), 0)
    keys = rows - WINDOW + lax.broadcasted_iota(jnp.int32, (1, BLOCK + WINDOW), 1)
    seg_q = segment_of(query, count, length, start)
    seg_k = segment_of(keys, count, length, start)
    far = query - keys
    return (far >= 0) & (far <= WINDOW) & (seg_q == seg_k)


def soft_of(query, keys, mask):
    scores = dot_trans(query, keys) * SCALE
    scores = jnp.where(mask, scores, NEG)
    peak = jnp.max(scores, axis=1, keepdims=True)
    exponent = jnp.exp(scores - peak)
    return exponent / jnp.sum(exponent, axis=1, keepdims=True)


def lane_head(width):
    return lax.broadcasted_iota(jnp.int32, (1, width), 1) // HEAD_DIM


def remote(src, dst, send, recv, **peer):
    return pltpu.make_async_remote_copy(
        src_ref=src,
        dst_ref=dst,
        send_sem=send,
        recv_sem=recv,
        device_id=peer,
        device_id_type=MESH_ID,
    )


def greet_group(barrier, size):
    me = lax.axis_index("fsdp")
    for step in range(1, size):
        peer = lax.rem(me + step, size)
        pl.semaphore_signal(barrier, inc=1, device_id={"fsdp": peer}, device_id_type=MESH_ID)


class Group:
    def __init__(self, size):
        self.size = size
        self.me = lax.axis_index("fsdp")
        self.square = size == 4
        if self.square:
            x, y = lax.rem(self.me, 2), self.me // 2
            self.at = lambda bx, by: lax.rem(y + by, 2) * 2 + lax.rem(x + bx, 2)
            self.x, self.y, self.far = self.at(1, 0), self.at(0, 1), self.at(1, 1)

    def from_own(self, step):
        if self.square:
            return self.at(lax.rem(step, 2), step // 2)
        return lax.rem(self.me - step + self.size, self.size)

    def to_own(self, step):
        if self.square:
            return self.at(1 - step // 2, 1 - lax.rem(step, 2))
        return lax.rem(self.me + 1 + step, self.size)


class Gather:
    def __init__(self, group, ref, send, recv):
        self.group, self.ref, self.send, self.recv = group, ref, send, recv
        self.half = ref.shape[1] // 2

    def part(self, k, slot, half, peer):
        view = self.ref.at[slot, pl.ds(half * self.half, self.half)]
        return remote(view, view, self.send.at[k], self.recv.at[k], fsdp=peer)

    def whole(self, k):
        g = self.group
        view = self.ref.at[g.me]
        sems = self.send.at[k - 1], self.recv.at[k - 1]
        return remote(view, view, *sems, fsdp=lax.rem(g.me + k, g.size))

    def copy(self, k):
        g = self.group
        if not g.square:
            return self.whole(k + 1)
        slot = (g.me, g.me, g.me, g.me, g.x, g.y)[k]
        half = (0, 1, 0, 1, 0, 1)[k]
        return self.part(k, slot, half, (g.x, g.x, g.y, g.y, g.y, g.x)[k])

    def start_half(self, half):
        if self.group.square:
            self.copy(half).start()
            self.copy(2 + half).start()
        elif half == 1:
            for k in range(self.group.size - 1):
                self.copy(k).start()

    def relay(self):
        if self.group.square:
            self.copy(0).wait_recv()
            self.copy(4).start()
            self.copy(3).wait_recv()
            self.copy(5).start()

    def ready(self, step):
        if not self.group.square:
            self.copy(step - 1).wait_recv()
        elif step == 3:
            self.copy(4).wait_recv()
            self.copy(5).wait_recv()
        else:
            self.copy(step).wait_recv()

    def finish(self):
        for k in range(transfers(self.group.size)):
            self.copy(k).wait_send()


class Scatter:
    def __init__(self, group, part, first, over, joined, last, send, recv):
        self.group, self.part = group, part
        self.first, self.over, self.joined, self.last = first, over, joined, last
        self.send, self.recv = send, recv
        self.half = part.shape[1] // 2

    def copy(self, k):
        g, half = self.group, self.half
        low, high = pl.ds(0, half), pl.ds(half, half)
        if not g.square:
            src, dst, peer = self.part.at[k], self.first.at[k], lax.rem(g.me + 1 + k, g.size)
        else:
            src, dst, peer = (
                lambda: (self.part.at[0, low], self.over.at[0], g.x),
                lambda: (self.part.at[0, high], self.over.at[1], g.y),
                lambda: (self.part.at[1, low], self.first.at[0], g.x),
                lambda: (self.part.at[2, high], self.first.at[1], g.y),
                lambda: (self.joined.at[0], self.last.at[0], g.y),
                lambda: (self.joined.at[1], self.last.at[1], g.x),
            )[k]()
        return remote(src, dst, self.send.at[k], self.recv.at[k], fsdp=peer)

    def made(self, step):
        if not self.group.square:
            self.copy(step).start()
        elif step == 0:
            self.copy(0).start()
            self.copy(1).start()
        elif step in (1, 2):
            self.copy(step + 1).start()

    def join(self):
        if not self.group.square:
            return
        half = self.half
        for k, (step, rows) in enumerate(((2, slice(0, half)), (1, slice(half, 2 * half)))):
            self.copy(k).wait_recv()
            own = self.part[step, rows].astype(F32)
            self.joined[k] = (own + self.over[k].astype(F32)).astype(BF)
            self.copy(4 + k).start()

    def total(self, half):
        count = self.half
        if self.group.square:
            self.copy(2 + half).wait_recv()
            self.copy(4 + half).wait_recv()
            return self.first[half].astype(F32) + self.last[half].astype(F32)
        if half == 0:
            for k in range(self.group.size - 1):
                self.copy(k).wait_recv()
        rows = slice(half * count, (half + 1) * count)
        out = self.first[0, rows].astype(F32)
        for k in range(1, self.group.size - 1):
            out = out + self.first[k, rows].astype(F32)
        return out

    def finish(self):
        for k in range(transfers(self.group.size)):
            self.copy(k).wait_send()


class Line:
    def __init__(self, parts, sems):
        self.rank = lax.axis_index("seq")
        self.parts, self.length = parts, parts // 2
        self.z, self.core = self.rank // 2, lax.rem(self.rank, 2)
        self.above, self.below = self.rank + 2, self.rank - 2
        self.beside = self.rank + 1 - 2 * self.core
        self.has_above, self.has_below = self.z < self.length - 1, self.z > 0
        self.sems = sems

    def greet(self, barrier):
        def one(peer):
            pl.semaphore_signal(barrier, inc=1, device_id={"seq": peer}, device_id_type=MESH_ID)

        one(self.beside)
        pl.when(self.has_above)(lambda: one(self.above))
        pl.when(self.has_below)(lambda: one(self.below))
        n, z = self.length, self.z
        return 1 + (2 * n - 2 - z) // n + (z + n - 1) // n

    def up(self, k, owner):
        view = self.view(owner)
        return remote(view, view, self.sems[0].at[k], self.sems[1].at[k], seq=self.above)

    def down(self, k, owner):
        view = self.view(owner)
        return remote(view, view, self.sems[2].at[k], self.sems[3].at[k], seq=self.below)

    def side(self, k, owner):
        view = self.view(owner)
        return remote(view, view, self.sems[4].at[k], self.sems[5].at[k], seq=self.beside)

    def gather(self, view):
        self.view = view
        pl.when(self.has_above)(lambda: self.up(0, self.rank).start())
        pl.when(self.has_below)(lambda: self.down(0, self.rank).start())
        self.side(self.z, self.rank).start()

    def own_up(self):
        pl.when(self.has_above)(lambda: self.up(0, self.rank).start())

    def own_down(self):
        pl.when(self.has_below)(lambda: self.down(0, self.rank).start())

    def relay_up(self, j):
        rank, z = self.rank, self.z

        @pl.when((z >= j) & self.has_above)
        def _():
            self.up(j - 1, rank).wait_recv()
            self.up(j, rank - 2 * j).start()
            self.side(z - j, rank - 2 * j).start()

    def relay_down(self, j):
        rank, z = self.rank, self.z

        @pl.when((z + j < self.length) & self.has_below)
        def _():
            self.down(j - 1, rank).wait_recv()
            self.down(j, rank + 2 * j).start()
            self.side(z + j, rank + 2 * j).start()

    def relay(self, j):
        self.relay_up(j)
        self.relay_down(j)

    def close(self, j):
        rank, z = self.rank, self.z

        @pl.when((z >= j) & (z == self.length - 1))
        def _():
            self.up(j - 1, rank).wait_recv()
            self.side(z - j, rank - 2 * j).start()

        @pl.when((z + j < self.length) & (z == 0))
        def _():
            self.down(j - 1, rank).wait_recv()
            self.side(z + j, rank + 2 * j).start()

    def gathered(self):
        for k in range(self.length):
            self.side(k, self.rank).wait_recv()

    def finish(self):
        rank, z = self.rank, self.z
        for k in range(self.length):
            self.side(k, rank).wait_send()
        pl.when(self.has_above)(lambda: self.up(0, rank).wait_send())
        pl.when(self.has_below)(lambda: self.down(0, rank).wait_send())
        for j in range(1, self.length):
            pl.when((z >= j) & self.has_above)(lambda: self.up(j, rank).wait_send())
            pl.when((z + j < self.length) & self.has_below)(lambda: self.down(j, rank).wait_send())


class LineSum:
    def __init__(self, line, x, pre, acc, up_in, down_in, sems):
        self.line, self.x, self.pre, self.acc = line, x, pre, acc
        self.up_in, self.down_in, self.sems = up_in, down_in, sems

    def share(self, k):
        line = self.line
        src = self.x.at[2 * k + 1 - line.core]
        return remote(src, self.pre.at[k], self.sems[0].at[k], self.sems[1].at[k], seq=line.beside)

    def up(self, k):
        sems = self.sems[2].at[k], self.sems[3].at[k]
        return remote(self.acc.at[k], self.up_in.at[k], *sems, seq=self.line.above)

    def down(self, k):
        sems = self.sems[4].at[k], self.sems[5].at[k]
        return remote(self.acc.at[k], self.down_in.at[k], *sems, seq=self.line.below)

    def pair(self, m):
        return self.line.length - 1 - m, m

    def trade(self):
        n = self.line.length
        for m in range((n + 1) // 2):
            for k in sorted(set(self.pair(m))):
                self.share(k).start()

    def merge(self, k):
        self.share(k).wait_recv()
        own = self.x[2 * k + self.line.core].astype(F32)
        self.acc[k] = (own + self.pre[k].astype(F32)).astype(BF)

    def begin(self, m):
        n, z = self.line.length, self.line.z
        far, near = self.pair(m)
        if m < (n + 1) // 2:
            for k in sorted({far, near}):
                self.merge(k)
        if m < n - 1:
            pl.when(z == 0)(lambda: self.up(far).start())
            pl.when(z == n - 1)(lambda: self.down(near).start())

    def add(self, k, more):
        self.acc[k] = (self.acc[k].astype(F32) + more[k].astype(F32)).astype(BF)

    def advance(self, t):
        z, n = self.line.z, self.line.length
        far, near = n - 1 + z - t, t - n + 1 + z

        @pl.when((z >= 1) & (z <= t))
        def _():
            self.up(far).wait_recv()
            self.add(far, self.up_in)
            self.up(far).start()

        @pl.when((z <= n - 2) & (z >= n - 1 - t))
        def _():
            self.down(near).wait_recv()
            self.add(near, self.down_in)
            self.down(near).start()

    def total(self):
        z = self.line.z

        @pl.when(z > 0)
        def _():
            self.up(z).wait_recv()
            self.add(z, self.up_in)

        @pl.when(z < self.line.length - 1)
        def _():
            self.down(z).wait_recv()
            self.add(z, self.down_in)

    def finish(self):
        for k in range(self.line.length):
            self.share(k).wait_send()
            pl.when(k > self.line.z)(lambda: self.up(k).wait_send())
            pl.when(k < self.line.z)(lambda: self.down(k).wait_send())


class StagedSum(LineSum):
    def __init__(self, stage, load, *args):
        super().__init__(*args)
        self.stage, self.load = stage, load

    def fetch(self, slot, src):
        return pltpu.make_async_copy(src, self.stage.at[slot], self.load.at[slot])

    def merge(self, k):
        self.share(k).wait_recv()
        own = self.fetch(0, self.x.at[2 * k + self.line.core])
        other = self.fetch(1, self.pre.at[k])
        own.start()
        other.start()
        own.wait()
        other.wait()
        self.acc[k] = (self.stage[0].astype(F32) + self.stage[1].astype(F32)).astype(BF)

    def add(self, k, more):
        came = self.fetch(0, more.at[k])
        came.start()
        came.wait()
        self.acc[k] = (self.acc[k].astype(F32) + self.stage[0].astype(F32)).astype(BF)


class MixedSum(StagedSum):
    def merge(self, k):
        self.share(k).wait_recv()
        other = self.fetch(1, self.pre.at[k])
        other.start()
        other.wait()
        own = self.x[2 * k + self.line.core].astype(F32)
        self.acc[k] = (own + self.stage[1].astype(F32)).astype(BF)


def line_sems(parts):
    return [pltpu.SemaphoreType.DMA((parts // 2,))] * 6


def transfers(size):
    return 6 if size == 4 else size - 1


def scatter_shapes(size, rows, width):
    half = rows // 2
    slots = (2, half, width) if size == 4 else (size - 1, rows, width)
    return [
        pltpu.VMEM((size - 1, rows, width), BF),
        pltpu.VMEM(slots, BF),
        pltpu.VMEM((2, half, width), BF),
        pltpu.VMEM((2, half, width), BF),
        pltpu.VMEM((2, half, width), BF),
        pltpu.SemaphoreType.DMA((transfers(size),)),
        pltpu.SemaphoreType.DMA((transfers(size),)),
    ]


def each_step(size, body):
    def one(step, carry):
        body(step, lambda k: pl.when(step == k))
        return carry

    lax.fori_loop(0, size, one, 0)


class ForwardRefs(NamedTuple):
    tokens: Any
    cot: Any
    gains: Any
    table: Any
    qkv_piece: Any
    gu_piece: Any
    out_map: Any
    down_map: Any
    gated_hbm: Any
    qkv_hbm: Any
    edge: Any
    qkv_map_hbm: Any
    middle: Any
    heads: Any
    grads_hbm: Any
    norm_hbm: Any
    hidden_hbm: Any
    gu_grad_hbm: Any
    gu_map_hbm: Any
    gains_all: Any
    table_all: Any
    edge_tok: Any
    part: Any
    first: Any
    over: Any
    joined: Any
    last: Any
    all: Any
    grads: Any
    qkv: Any
    qkv_map: Any
    gu_map: Any
    tail: Any
    own: Any
    grad_hidden: Any
    hidden: Any
    gu_grad: Any
    s_send: Any
    s_recv: Any
    a_send: Any
    a_recv: Any
    g_send: Any
    g_recv: Any
    c_send: Any
    c_recv: Any
    m_send: Any
    m_recv: Any
    halo_send: Any
    halo_recv: Any
    edge_send: Any
    edge_recv: Any
    loads: Any
    stores: Any
    hidden_store: Any
    gu_store: Any


def forward_kernel(size, parts, count, *refs):
    named = len(ForwardRefs._fields)
    r, sems = ForwardRefs(*refs[:named]), refs[named:]
    rank = lax.axis_index("seq")
    rows = r.tokens.shape[0]
    half = rows // 2
    local = r.out_map.shape[0]
    inner = r.down_map.shape[0]
    slot = rank * rows
    group = Group(size)
    me = group.me
    line_q, line_u = Line(parts, sems[:6]), Line(parts, sems[6:])

    barrier = pltpu.get_barrier_semaphore()
    greet_group(barrier, size)
    known = line_q.greet(barrier)

    def greet(peer):
        pl.semaphore_signal(barrier, inc=1, device_id={"seq": peer}, device_id_type=MESH_ID)

    pl.when(line_q.has_above & (line_q.core == 1))(lambda: greet(rank + 1))
    pl.when(line_q.has_below & (line_q.core == 0))(lambda: greet(rank - 1))
    n, z = line_q.length, line_q.z
    known = known + (2 * n - 2 - z) // n * line_q.core + (z + n - 1) // n * (1 - line_q.core)
    own_pieces = [
        pltpu.make_async_copy(src.at[me], dst.at[me, rank], r.loads.at[k])
        for k, (src, dst) in enumerate(
            ((r.qkv_piece, r.qkv_map), (r.gu_piece, r.gu_map))
        )
    ]
    for copy in own_pieces:
        copy.start()
    r.gains_all[me] = r.gains[...]
    r.table_all[me] = r.table[...]
    own_table = r.table[...]
    slots = slot + lax.broadcasted_iota(jnp.int32, (rows, 1), 0)
    length = lambda j: own_table[0:1, j : j + 1]
    start = lambda j: own_table[1:2, j : j + 1]
    segment = segment_of(slots, count, length, start)
    r.grads[me] = jnp.where(segment >= 0, r.cot[...].astype(F32), 0.0).astype(BF)

    @pl.when(rank == 0)
    def _():
        r.edge_tok[...] = jnp.zeros_like(r.edge_tok)

    def edge_rows():
        last = r.tokens.at[pl.ds(rows - 8, 8)]
        return remote(last, r.edge_tok, r.edge_send, r.edge_recv, seq=rank + 1)

    pl.semaphore_wait(barrier, size - 1 + known)
    pl.when(rank < parts - 1)(lambda: edge_rows().start())

    def swap(k, step):
        peer = lax.rem(me + step, size)
        src, dst = (
            lambda: (r.gains_all.at[me], r.gains_all.at[me]),
            lambda: (r.table_all.at[me], r.table_all.at[me]),
            lambda: (r.qkv_piece.at[peer], r.qkv_map.at[me, rank]),
            lambda: (r.gu_piece.at[peer], r.gu_map.at[me, rank]),
        )[k]()
        return remote(src, dst, r.m_send.at[k, step - 1], r.m_recv.at[k, step - 1], fsdp=peer)

    others = range(1, size)
    for k in range(4):
        for step in others:
            swap(k, step).start()
    for k in range(2):
        for step in others:
            swap(k, step).wait_recv()

    gains = jnp.concatenate([r.gains_all[f] for f in range(size)], 1).astype(F32)
    same_one = (segment == segment_of(slots - 1, count, length, start)).astype(F32)
    same_two = (segment == segment_of(slots - 2, count, length, start)).astype(F32)
    tokens = r.tokens[...].astype(F32)
    pl.when(rank > 0)(lambda: edge_rows().wait_recv())
    edge = r.edge_tok[...].astype(F32)

    def norm(a):
        return a * lax.rsqrt(jnp.mean(a * a, axis=1, keepdims=True) + EPS) * gains[0:1]

    normed, edge = norm(tokens), norm(edge)
    row = lax.broadcasted_iota(jnp.int32, (rows, 1), 0)
    back_one = jnp.where(row == 0, edge[7:8], pltpu.roll(normed, 1, 0))
    back_two = jnp.where(
        row == 0, edge[6:7], jnp.where(row == 1, edge[7:8], pltpu.roll(normed, 2, 0))
    )
    mixed = (
        normed * gains[2:3]
        + same_one * back_one * gains[3:4]
        + same_two * back_two * gains[4:5]
    )
    all_ref = r.all
    all_ref[me] = (mixed * normed).astype(BF)
    gather = Gather(group, all_ref, r.a_send, r.a_recv)
    gather.start_half(0)
    gather.start_half(1)

    own_pieces[0].wait()
    for step in others:
        swap(2, step).wait_recv()
    line_q.gather(lambda owner: r.qkv_map.at[:, owner])
    line_u.view = lambda owner: r.gu_map.at[:, owner]
    gather.relay()
    grads = Gather(group, r.grads, r.c_send, r.c_recv)
    grads.start_half(0)
    grads.start_half(1)
    own_pieces[1].wait()
    for step in others:
        swap(3, step).wait_recv()
    line_u.side(z, rank).start()
    pl.when(z == 0)(line_u.own_up)
    pl.when(z == n - 1)(line_u.own_down)
    for j in range(1, n):
        line_q.relay(j)
        line_q.close(j)
        pl.when(z == j)(line_u.own_up)
        pl.when(z == n - 1 - j)(line_u.own_down)
    for step in others:
        gather.ready(step)
    line_q.gathered()
    keeps = [
        pltpu.make_async_copy(all_ref, r.gated_hbm, r.stores.at[size]),
        pltpu.make_async_copy(r.qkv_map, r.qkv_map_hbm, r.stores.at[size + 1]),
    ]
    for keep in keeps:
        keep.start()

    weights = r.qkv_map[...].reshape(-1, r.qkv_map.shape[3])

    def halo(step):
        g = group.to_own(step)
        sem = r.halo_send.at[step], r.halo_recv.at[step]
        return remote(r.tail.at[g], r.edge.at[g], *sem, seq=rank + 1)

    def project(step, is_step):
        g = group.to_own(step)
        out = dot(all_ref[g], weights).astype(BF)
        r.qkv[g] = out
        r.tail[g] = out[rows - WINDOW :, local:]
        pl.when(rank < parts - 1)(lambda: halo(step).start())

    each_step(size, project)

    @pl.when(rank == 0)
    def _():
        r.edge[...] = jnp.zeros_like(r.edge)

    keeps.append(pltpu.make_async_copy(r.qkv, r.qkv_hbm, r.stores.at[size + 2]))
    keeps[2].start()
    line_u.relay(1)
    gather.finish()
    keeps[0].wait()

    scatter = Scatter(
        group, r.part, r.first, r.over, r.joined, r.last, r.s_send, r.s_recv
    )
    head_of = lane_head(local)

    def mix(step, is_step):
        g = group.to_own(step)
        pl.when(rank > 0)(lambda: halo(step).wait_recv())
        own, edge, table = r.qkv[g], r.edge[g], r.table_all[g]
        queries = own[:, :local]
        keys = jnp.concatenate([edge[:, :local], own[:, local : 2 * local]], 0)
        values = jnp.concatenate([edge[:, local:], own[:, 2 * local :]], 0)
        outs = []
        for block in range(rows // BLOCK):
            mask = masks_of(
                slot,
                block,
                count,
                lambda j: table[0:1, j : j + 1],
                lambda j: table[1:2, j : j + 1],
            )
            low = block * BLOCK
            query = queries[low : low + BLOCK]
            key = keys[low : low + BLOCK + WINDOW]
            value = values[low : low + BLOCK + WINDOW]
            out = jnp.zeros((BLOCK, local), F32)
            for head in range(local // HEAD_DIM):
                mine = head_of == head
                soft = soft_of(jnp.where(mine, query, jnp.zeros_like(query)), key, mask)
                out = jnp.where(mine, dot(soft.astype(BF), value), out)
            outs.append(out.astype(BF))
        heads = jnp.concatenate(outs, 0)
        r.heads[g] = heads
        branch = dot(heads, r.out_map[...])
        is_step(size - 1)(lambda: r.own.__setitem__(..., branch))
        pl.when(step < size - 1)(lambda: r.part.__setitem__(step, branch.astype(BF)))
        for k in range(size - 1):
            is_step(k)(functools.partial(scatter.made, k))

    each_step(size, mix)
    scatter.join()
    grads.relay()
    for j in range(2, n):
        line_u.relay(j)
    gather = Gather(group, all_ref, r.g_send, r.g_recv)
    for h in range(2):
        span = slice(h * half, (h + 1) * half)
        total = r.own[span, :] + scatter.total(h)
        middle = r.tokens[span, :].astype(F32) + total
        r.middle[span, :] = middle
        scale = lax.rsqrt(jnp.mean(middle * middle, axis=1, keepdims=True) + EPS)
        all_ref[me, span] = (middle * scale * gains[1:2]).astype(BF)
        gather.start_half(h)
    gather.relay()

    def grad_of(step, is_step):
        g = group.from_own(step)
        for k in others:
            is_step(k)(functools.partial(grads.ready, k))
        r.grad_hidden[g] = dot_trans(r.grads[g], r.down_map[...])

    each_step(size, grad_of)
    for j in range(1, n):
        line_u.close(j)
    line_u.gathered()
    keeps.append(pltpu.make_async_copy(r.gu_map, r.gu_map_hbm, r.stores.at[size + 3]))
    keeps[3].start()

    def out_copies(step):
        g, two = group.from_own(step), lax.rem(step, 2)
        return (
            pltpu.make_async_copy(
                r.hidden.at[two], r.hidden_hbm.at[g], r.hidden_store.at[two]
            ),
            pltpu.make_async_copy(
                r.gu_grad.at[two], r.gu_grad_hbm.at[g], r.gu_store.at[two]
            ),
        )

    def norm_copy(g):
        return pltpu.make_async_copy(all_ref.at[g], r.norm_hbm.at[g], r.stores.at[g])

    def feed(step, is_step):
        g, two = group.from_own(step), lax.rem(step, 2)
        for k in others:
            is_step(k)(functools.partial(gather.ready, k))

        @pl.when(step >= 2)
        def _():
            for copy in out_copies(step - 2):
                copy.wait()

        norm_copy(g).start()
        weights = r.gu_map[...].reshape(-1, r.gu_map.shape[3])
        acts = dot(all_ref[g], weights)
        gate, up = acts[:, :inner], acts[:, inner:]
        sigma = jax.nn.sigmoid(gate)
        silu = gate * sigma
        r.hidden[two] = (silu * up).astype(BF)
        grad_hidden = r.grad_hidden[g]
        grad_gate = grad_hidden * up * sigma * (1.0 + gate * (1.0 - sigma))
        r.gu_grad[two] = jnp.concatenate([grad_gate, grad_hidden * silu], 1).astype(BF)
        for copy in out_copies(step):
            copy.start()

    each_step(size, feed)
    keeps.append(pltpu.make_async_copy(r.grads, r.grads_hbm, r.stores.at[size + 4]))
    keeps[4].start()
    for k in range(4):
        for step in others:
            swap(k, step).wait_send()
    scatter.finish()
    gather.finish()
    grads.finish()
    line_q.finish()
    line_u.finish()

    @pl.when(rank < parts - 1)
    def _():
        edge_rows().wait_send()
        for step in range(size):
            halo(step).wait_send()

    for keep in keeps[1:]:
        keep.wait()
    for g in range(size):
        norm_copy(g).wait()
    for step in (size - 2, size - 1):
        for copy in out_copies(step):
            copy.wait()


def forward_part(ident, count, tokens, cot, gains, table, qkv_piece, gu_piece, out_weight, down_weight):
    size, parts = lax.axis_size("fsdp"), lax.axis_size("seq")
    rows, width = tokens.shape
    local, inner = out_weight.shape[0], down_weight.shape[0]
    piece, cols = gu_piece.shape[1:]
    vmem = pl.BlockSpec(memory_space=pltpu.VMEM)
    hbm = pl.BlockSpec(memory_space=pl.ANY)
    shape = lambda w: (size, rows, w)
    low = lambda s: jax.ShapeDtypeStruct(s, BF)
    maps = [(size, parts, piece, 3 * local), (size, parts, piece, cols)]
    dma = lambda *s: pltpu.SemaphoreType.DMA(s)
    hop = transfers(size)
    scratch = scatter_shapes(size, rows, width)
    return pl.pallas_call(
        functools.partial(forward_kernel, size, parts, count),
        out_shape=[
            low(shape(width)),
            low(shape(3 * local)),
            low((size, WINDOW, 2 * local)),
            low(maps[0]),
            jax.ShapeDtypeStruct((rows, width), F32),
            low(shape(local)),
            low(shape(width)),
            low(shape(width)),
            low(shape(inner)),
            low(shape(cols)),
            low(maps[1]),
            low((size,) + gains.shape),
            jax.ShapeDtypeStruct((size,) + table.shape, jnp.int32),
            low((8, width)),
        ],
        in_specs=[vmem] * 4 + [hbm, hbm, vmem, vmem],
        out_specs=[hbm, hbm, vmem, hbm, vmem, vmem, hbm, hbm, hbm, hbm, hbm, vmem, vmem, vmem],
        scratch_shapes=scratch[:-2]
        + [
            pltpu.VMEM(shape(width), BF),
            pltpu.VMEM(shape(width), BF),
            pltpu.VMEM(shape(3 * local), BF),
            pltpu.VMEM(maps[0], BF),
            pltpu.VMEM(maps[1], BF),
            pltpu.VMEM((size, WINDOW, 2 * local), BF),
            pltpu.VMEM((rows, width), F32),
            pltpu.VMEM(shape(inner), F32),
            pltpu.VMEM((2, rows, inner), BF),
            pltpu.VMEM((2, rows, cols), BF),
        ]
        + [dma(hop)] * 8
        + [dma(4, size - 1)] * 2
        + [dma(size)] * 2
        + [pltpu.SemaphoreType.DMA] * 2
        + [dma(2), dma(size + 5), dma(2), dma(2)]
        + line_sems(parts)
        + line_sems(parts),
        compiler_params=pltpu.CompilerParams(
            collective_id=ident, has_side_effects=True, vmem_limit_bytes=67_000_000
        ),
        cost_estimate=pl.CostEstimate(
            flops=2 * size * rows * width * (4 * local + 3 * inner),
            bytes_accessed=500_000_000,
            transcendentals=0,
        ),
        name="forward_part",
    )(tokens, cot, gains, table, qkv_piece, gu_piece, out_weight, down_weight)


def heads_back(group, slot, count, lens_ref, starts_ref, own, edge, grad):
    rows, local = own.shape[0], own.shape[1] // 3
    head_of = lane_head(local)
    queries = own[:, :local]
    keys = jnp.concatenate([edge[:, :local], own[:, local : 2 * local]], 0)
    values = jnp.concatenate([edge[:, local:], own[:, 2 * local :]], 0)
    dqs, dks, dvs = [], [], []
    for block in range(rows // BLOCK):
        mask = masks_of(
            slot, block, count, lambda j: lens_ref[group, j], lambda j: starts_ref[group, j]
        )
        low = block * BLOCK
        span = slice(low, low + BLOCK + WINDOW)
        query, grads = queries[low : low + BLOCK], grad[low : low + BLOCK]
        key, value = keys[span], values[span]
        dq = jnp.zeros((BLOCK, local), F32)
        dk = jnp.zeros((BLOCK + WINDOW, local), F32)
        dv = jnp.zeros((BLOCK + WINDOW, local), F32)
        for head in range(local // HEAD_DIM):
            mine = head_of == head
            own_q = jnp.where(mine, query, jnp.zeros_like(query))
            own_g = jnp.where(mine, grads, jnp.zeros_like(grads))
            soft = soft_of(own_q, key, mask)
            grad_soft = dot_trans(own_g, value)
            total = jnp.sum(grad_soft * soft, axis=1, keepdims=True)
            grad_scores = (soft * (grad_soft - total)).astype(BF)
            dq = jnp.where(mine, dot(grad_scores, key), dq)
            dk = dk + dot_rows(grad_scores, own_q)
            dv = dv + dot_rows(soft.astype(BF), own_g)
        dqs.append(dq * SCALE)
        dks.append(dk * SCALE)
        dvs.append(dv)

    def joined(pieces):
        out = [pieces[0][:BLOCK]]
        for left, right in zip(pieces, pieces[1:]):
            out.append(left[BLOCK:] + right[:WINDOW])
            out.append(right[WINDOW:BLOCK])
        out.append(pieces[-1][BLOCK:])
        return jnp.concatenate(out, 0)

    return jnp.concatenate(dqs, 0), joined(dks), joined(dvs)


class BackRefs(NamedTuple):
    lens: Any
    starts: Any
    grad_gu_hbm: Any
    gu_map_hbm: Any
    middle: Any
    grads_hbm: Any
    gain: Any
    out_map: Any
    edge: Any
    qkv: Any
    qkv_map_hbm: Any
    gu_x: Any
    down_x: Any
    grad_middle: Any
    norm: Any
    all: Any
    dqkv: Any
    own: Any
    gu_slots: Any
    down_every: Any
    gu_pre: Any
    gu_up: Any
    gu_down: Any
    down_pre: Any
    down_up: Any
    down_down: Any
    part: Any
    first: Any
    over: Any
    joined: Any
    last: Any
    s_send: Any
    s_recv: Any
    t_send: Any
    t_recv: Any
    g_send: Any
    g_recv: Any
    grad_gu: Any
    gu_map: Any
    qkv_map: Any
    dedge: Any
    back: Any
    tail: Any
    h_send: Any
    h_recv: Any
    loads: Any
    gu_acc: Any
    gu_stage: Any
    gu_load: Any
    down_acc: Any
    down_stage: Any
    down_load: Any
    m_send: Any
    m_recv: Any
    grad: Any


def back_kernel(size, parts, count, *refs):
    named = len(BackRefs._fields)
    r, sems = BackRefs(*refs[:named]), refs[named:]
    line = Line(parts, sems[:6])
    gu_sum = StagedSum(
        r.gu_stage, r.gu_load, line, r.gu_x, r.gu_pre, r.gu_acc, r.gu_up, r.gu_down, sems[6:12]
    )
    down_sum = StagedSum(
        r.down_stage,
        r.down_load,
        line,
        r.down_x,
        r.down_pre,
        r.down_acc,
        r.down_up,
        r.down_down,
        sems[12:],
    )
    rows = r.middle.shape[0]
    local = r.out_map.shape[0]
    rank = lax.axis_index("seq")
    slot = rank * rows
    group = Group(size)
    barrier = pltpu.get_barrier_semaphore()
    greet_group(barrier, size)

    def greet(peer):
        pl.semaphore_signal(barrier, inc=1, device_id={"seq": peer}, device_id_type=MESH_ID)

    known = line.greet(barrier)
    pl.when(line.has_above & (line.core == 1))(lambda: greet(rank + 1))
    pl.when(line.has_below & (line.core == 0))(lambda: greet(rank - 1))
    n, z = line.length, line.z
    known = known + (2 * n - 2 - z) // n * line.core + (z + n - 1) // n * (1 - line.core)
    fetches = [
        pltpu.make_async_copy(src, dst, r.loads.at[k])
        for k, (src, dst) in enumerate(
            (
                (r.grad_gu_hbm, r.grad_gu),
                (r.gu_map_hbm, r.gu_map),
                (r.qkv_map_hbm, r.qkv_map),
                (r.grads_hbm.at[group.me], r.grad),
            )
        )
    ]
    for fetch in fetches:
        fetch.start()
    pl.semaphore_wait(barrier, size - 1 + known)
    down_sum.trade()
    gu_sum.trade()
    for m in range(n):
        down_sum.begin(m)
    scatter = Scatter(
        group, r.part, r.first, r.over, r.joined, r.last, r.s_send, r.s_recv
    )
    gather = Gather(group, r.all, r.g_send, r.g_recv)
    fetches[0].wait()
    fetches[1].wait()
    fetches[3].wait()

    def step_two(step, is_step):
        partial = dot_trans(r.grad_gu[group.to_own(step)], r.gu_map[...])
        is_step(size - 1)(lambda: r.own.__setitem__(..., partial))
        pl.when(step < size - 1)(lambda: r.part.__setitem__(step, partial.astype(BF)))
        for k in range(size - 1):
            is_step(k)(functools.partial(scatter.made, k))

    each_step(size, step_two)
    scatter.join()
    gu_sum.begin(0)
    down_sum.advance(1)
    half = rows // 2
    norm_sum = jnp.zeros((1, r.middle.shape[1]), F32)
    for h in range(2):
        span = slice(h * half, (h + 1) * half)
        grad = r.own[span, :] + scatter.total(h)
        middle = r.middle[span, :]
        scale = lax.rsqrt(jnp.mean(middle * middle, axis=1, keepdims=True) + EPS)
        unit = middle * scale
        scaled = grad * r.gain[...]
        norm_sum = norm_sum + jnp.sum(grad * unit, axis=0, keepdims=True)
        grad_out = r.grad[span, :].astype(F32)
        grad_middle = grad_out + scale * (
            scaled - unit * jnp.mean(scaled * unit, axis=1, keepdims=True)
        )
        r.grad_middle[span, :] = grad_middle
        r.all[group.me, span] = grad_middle.astype(BF)
        gather.start_half(h)
    r.norm[...] = norm_sum
    own_down = pltpu.make_async_copy(r.down_acc.at[z], r.down_every.at[rank], r.down_load.at[0])

    def halo(step):
        g = group.from_own(step)
        sems = r.h_send.at[step], r.h_recv.at[step]
        return remote(r.dedge.at[g], r.back.at[g], *sems, seq=rank - 1)

    def step_heads(step, is_step):
        g = group.from_own(step)

        @is_step(1)
        def _():
            gather.relay()
            for t in range(2, n - 1):
                down_sum.advance(t)

        @is_step(2)
        def _():
            down_sum.total()
            own_down.start()
            own_down.wait()
            line.gather(lambda owner: r.down_every.at[owner])

        for k in range(1, size):
            is_step(k)(functools.partial(gather.ready, k))
        grad = dot_trans(r.all[g], r.out_map[...]).astype(BF)
        dq, dk, dv = heads_back(
            g, slot, count, r.lens, r.starts, r.qkv[g], r.edge[g], grad
        )
        r.dedge[g] = jnp.concatenate([dk[:WINDOW], dv[:WINDOW]], 1).astype(BF)
        full = jnp.concatenate([dq, dk[WINDOW:], dv[WINDOW:]], 1)
        r.dqkv[g] = full.astype(BF)
        r.tail[g] = full[rows - WINDOW :]
        pl.when(rank > 0)(lambda: halo(step).start())

    each_step(size, step_heads)
    gu_sum.advance(1)
    for m in range(1, n):
        gu_sum.begin(m)
    line.relay(1)
    scatter.finish()
    fetches[2].wait()

    @pl.when(rank == parts - 1)
    def _():
        r.back[...] = jnp.zeros_like(r.back)

    @pl.when(rank < parts - 1)
    def _():
        for step in range(size):
            halo(step).wait_recv()

    scatter = Scatter(
        group, r.part, r.first, r.over, r.joined, r.last, r.t_send, r.t_recv
    )

    def step_one(step, is_step):
        g = group.to_own(step)
        back = r.back[g].astype(F32)
        wide = jnp.concatenate([jnp.zeros((WINDOW, local), F32), back], 1)
        r.dqkv[g, pl.ds(rows - WINDOW, WINDOW)] = (r.tail[g] + wide).astype(BF)
        partial = dot_trans(r.dqkv[g], r.qkv_map[...])
        is_step(size - 1)(lambda: r.own.__setitem__(..., partial))
        pl.when(step < size - 1)(lambda: r.part.__setitem__(step, partial.astype(BF)))
        for k in range(size - 1):
            is_step(k)(functools.partial(scatter.made, k))

    each_step(size, step_one)
    scatter.join()
    for t in range(2, n - 1):
        gu_sum.advance(t)
        line.relay(t)
    line.relay(n - 1)
    for h in range(2):
        span = slice(h * half, (h + 1) * half)
        r.own[span, :] = r.own[span, :] + scatter.total(h)
    gu_sum.total()

    def swap(step):
        peer = lax.rem(group.me + step, size)
        sems = r.m_send.at[step - 1], r.m_recv.at[step - 1]
        return remote(r.gu_acc.at[z, peer], r.gu_slots.at[group.me], *sems, fsdp=peer)

    for step in range(1, size):
        swap(step).start()
    own_slot = pltpu.make_async_copy(
        r.gu_acc.at[z, group.me], r.gu_slots.at[group.me], r.gu_load.at[0]
    )
    own_slot.start()
    for j in range(1, n):
        line.close(j)
    line.gathered()
    for step in range(1, size):
        swap(step).wait()
    scatter.finish()
    gather.finish()
    down_sum.finish()
    gu_sum.finish()
    line.finish()
    own_slot.wait()

    @pl.when(rank > 0)
    def _():
        for step in range(size):
            halo(step).wait_send()


def back_part(
    ident, lens, starts, grad_gu, gu_map, middle, grads, gain, out_weight, edge, qkv, qkv_map, gu_x, down_x
):
    size, parts = lax.axis_size("fsdp"), lax.axis_size("seq")
    rows, width = middle.shape
    local = out_weight.shape[0]
    n = parts // 2
    vmem = pl.BlockSpec(memory_space=pltpu.VMEM)
    smem = pl.BlockSpec(memory_space=pltpu.SMEM)
    hbm = pl.BlockSpec(memory_space=pl.ANY)
    dma = lambda *s: pltpu.SemaphoreType.DMA(s)
    low = lambda *s: jax.ShapeDtypeStruct(s, BF)
    sems = [dma(transfers(size))] * 2
    gu, down = gu_x.shape[1:], down_x.shape[1:]
    outs = pl.pallas_call(
        functools.partial(back_kernel, size, parts, lens.shape[1]),
        out_shape=[
            jax.ShapeDtypeStruct((rows, width), F32),
            jax.ShapeDtypeStruct((1, width), F32),
            low(size, rows, width),
            low(*qkv.shape),
            jax.ShapeDtypeStruct((rows, width), F32),
            low(*gu),
            low(parts, *down),
        ]
        + [low(n, *gu)] * 3
        + [low(n, *down)] * 3,
        in_specs=[smem, smem, hbm, hbm, vmem, hbm] + [vmem] * 4 + [hbm] * 3,
        out_specs=[vmem] * 5 + [hbm] * 8,
        scratch_shapes=scatter_shapes(size, rows, width)
        + sems
        + sems
        + [
            pltpu.VMEM(grad_gu.shape, BF),
            pltpu.VMEM(gu_map.shape, BF),
            pltpu.VMEM(qkv_map.shape, BF),
            pltpu.VMEM((size, WINDOW, 2 * local), BF),
            pltpu.VMEM((size, WINDOW, 2 * local), BF),
            pltpu.VMEM((size, WINDOW, 3 * local), F32),
            dma(size),
            dma(size),
            dma(4),
            pltpu.VMEM((n,) + gu, BF),
            pltpu.VMEM((2,) + gu, BF),
            dma(2),
            pltpu.VMEM((n,) + down, BF),
            pltpu.VMEM((2,) + down, BF),
            dma(2),
            dma(size - 1),
            dma(size - 1),
            pltpu.VMEM((rows, width), BF),
        ]
        + line_sems(parts) * 3,
        compiler_params=pltpu.CompilerParams(
            collective_id=ident, has_side_effects=True, vmem_limit_bytes=67_000_000
        ),
        cost_estimate=pl.CostEstimate(
            flops=2 * size * rows * (gu_map.size + qkv_map.size + width * local),
            bytes_accessed=400_000_000,
            transcendentals=0,
        ),
        name="back_part",
    )(lens, starts, grad_gu, gu_map, middle, grads, gain, out_weight, edge, qkv, qkv_map, gu_x, down_x)
    return outs[:7]


class CloseRefs(NamedTuple):
    gated_hbm: Any
    dqkv_hbm: Any
    heads_hbm: Any
    gb_hbm: Any
    gu_slots: Any
    terms: Any
    hidden_hbm: Any
    down_hbm: Any
    every_hbm: Any
    gu_every: Any
    feed: Any
    terms_out: Any
    pre: Any
    up_in: Any
    down_in: Any
    part: Any
    first: Any
    over: Any
    joined: Any
    last: Any
    x: Any
    acc: Any
    stage: Any
    stage_load: Any
    every: Any
    slots: Any
    gu_own: Any
    gated: Any
    dqkv: Any
    heads: Any
    gb: Any
    hidden: Any
    down_map: Any
    terms_in: Any
    terms_all: Any
    s_send: Any
    s_recv: Any
    m_send: Any
    m_recv: Any
    t_send: Any
    t_recv: Any
    loads: Any


def close_kernel(size, parts, made, *refs):
    named = len(CloseRefs._fields)
    r, sems = CloseRefs(*refs[:named]), refs[named:]
    rank = lax.axis_index("seq")
    group = Group(size)
    me = group.me
    line_u, line_q = Line(parts, sems[:6]), Line(parts, sems[6:12])
    n, z = line_q.length, line_q.z
    sums = MixedSum(
        r.stage, r.stage_load, line_q, r.x, r.pre, r.acc, r.up_in, r.down_in, sems[12:]
    )
    rows = r.feed.shape[0]
    half = rows // 2
    barrier = pltpu.get_barrier_semaphore()
    greet_group(barrier, size)
    for step in range(1, parts):
        peer = lax.rem(rank + step, parts)
        pl.semaphore_signal(barrier, inc=1, device_id={"seq": peer}, device_id_type=MESH_ID)
    moves = [
        (r.gu_slots, r.gu_own),
        (r.hidden_hbm, r.hidden),
        (r.down_hbm, r.down_map),
    ]
    if made:
        moves += [
            (r.gated_hbm, r.gated),
            (r.dqkv_hbm, r.dqkv),
            (r.heads_hbm, r.heads),
            (r.gb_hbm, r.gb),
        ]
    else:
        moves += [(r.gated_hbm, r.x)]
    fetches = [
        pltpu.make_async_copy(src, dst, r.loads.at[k]) for k, (src, dst) in enumerate(moves)
    ]
    for k in [0] + list(range(3, len(moves))) + [1, 2]:
        fetches[k].start()
    r.terms_in[me] = r.terms[me]
    own_slots = pltpu.make_async_copy(r.gu_own, r.gu_every.at[rank], r.loads.at[0])
    fetches[0].wait()
    own_slots.start()
    own_slots.wait()
    pl.semaphore_wait(barrier, size + parts - 2)
    line_u.gather(lambda owner: r.gu_every.at[owner])

    def swap(k, step):
        peer = lax.rem(me + step, size)
        src, dst = (
            lambda: (r.terms.at[peer], r.terms_in.at[me]),
            lambda: (r.acc.at[z, peer], r.slots.at[me]),
        )[k]()
        return remote(src, dst, r.m_send.at[k, step - 1], r.m_recv.at[k, step - 1], fsdp=peer)

    others = range(1, size)
    for step in others:
        swap(0, step).start()

    scatter = Scatter(
        group, r.part, r.first, r.over, r.joined, r.last, r.s_send, r.s_recv
    )

    def down(step, is_step):
        partial = dot(r.hidden[group.to_own(step)], r.down_map[...])
        is_step(size - 1)(lambda: r.feed.__setitem__(..., partial))
        pl.when(step < size - 1)(lambda: r.part.__setitem__(step, partial.astype(BF)))
        for k in range(size - 1):
            is_step(k)(functools.partial(scatter.made, k))

    for fetch in fetches[3:]:
        fetch.wait()
    if made:
        span = r.gated.shape[1] // (size // 2)
        for h in range(size // 2):
            lanes = slice(h * span, (h + 1) * span)
            pack_pair(
                r.x, h, r.gated[:, lanes], r.dqkv[...], r.heads[...], r.gb[:, lanes]
            )
    sums.trade()
    line_u.relay(1)
    fetches[1].wait()
    fetches[2].wait()
    for m in range(n):
        sums.begin(m)
    each_step(size, down)

    for step in others:
        swap(0, step).wait_recv()
    small = r.terms_in[0]
    for f in others:
        small = small + r.terms_in[f]
    r.terms_all[rank] = small

    def spread(step):
        peer = lax.rem(rank + step, parts)
        view = r.terms_all.at[rank]
        return remote(view, view, r.t_send.at[step - 1], r.t_recv.at[step - 1], seq=peer)

    for step in range(1, parts):
        spread(step).start()
    scatter.join()

    for t in range(1, n - 1):
        sums.advance(t)
        line_u.relay(t + 1)
    for h in range(2):
        span = slice(h * half, (h + 1) * half)
        r.feed[span, :] = r.feed[span, :] + scatter.total(h)
    sums.total()
    for step in others:
        swap(1, step).start()
    for j in range(1, n):
        line_u.close(j)
    r.slots[me] = r.acc[z, me]
    for step in others:
        swap(1, step).wait_recv()
    local = r.x.shape[3] // 4
    lane = lax.broadcasted_iota(jnp.int32, (1, 1, 4 * local), 2)
    r.every[rank] = jnp.where(lane < 3 * local, r.slots[...], r.acc[z])
    line_q.gather(lambda owner: r.every.at[owner])
    line_u.gathered()
    for j in range(1, n):
        line_q.relay(j)
    for j in range(1, n):
        line_q.close(j)
    line_q.gathered()
    store = pltpu.make_async_copy(r.every, r.every_hbm, r.loads.at[1])
    store.start()
    for step in range(1, parts):
        spread(step).wait_recv()
    small = r.terms_all[0]
    for k in range(1, parts):
        small = small + r.terms_all[k]
    r.terms_out[...] = small
    for k in range(2):
        for step in others:
            swap(k, step).wait_send()
    for step in range(1, parts):
        spread(step).wait_send()
    scatter.finish()
    sums.finish()
    line_u.finish()
    line_q.finish()
    store.wait()


def close_part(ident, gated, dqkv, heads, gb, gu_slots, terms, hidden, down_weight):
    size, parts = lax.axis_size("fsdp"), lax.axis_size("seq")
    width = gated.shape[1]
    made = packs(size, parts, width)
    piece, cols = width // (size * parts), dqkv.shape[1] + heads.shape[1]
    if not made:
        gated = pack_plain(parts, size, gated, dqkv, heads, gb)
    n = parts // 2
    rows = hidden.shape[1]
    vmem = pl.BlockSpec(memory_space=pltpu.VMEM)
    hbm = pl.BlockSpec(memory_space=pl.ANY)
    dma = lambda *s: pltpu.SemaphoreType.DMA(s)
    gu_shape = (parts,) + gu_slots.shape
    packed = (parts, size, piece, cols)
    scratch = scatter_shapes(size, rows, width)
    low = lambda *s: jax.ShapeDtypeStruct(s, BF)
    copy_of = lambda a: pltpu.VMEM(a.shape if made else (8, 128), BF)
    return pl.pallas_call(
        functools.partial(close_kernel, size, parts, made),
        out_shape=[
            low(*packed),
            low(*gu_shape),
            jax.ShapeDtypeStruct((rows, width), F32),
            jax.ShapeDtypeStruct(terms.shape[1:], F32),
        ]
        + [low(n, size, piece, cols)] * 3,
        in_specs=[hbm] * 5 + [vmem, hbm, hbm],
        out_specs=[hbm, hbm, vmem, vmem, hbm, hbm, hbm],
        scratch_shapes=scratch[:-2]
        + [
            pltpu.VMEM(packed, BF),
            pltpu.VMEM((n, size, piece, cols), BF),
            pltpu.VMEM((2, size, piece, cols), BF),
            dma(2),
            pltpu.VMEM(packed, BF),
            pltpu.VMEM((size, piece, cols), BF),
            pltpu.VMEM(gu_slots.shape, BF),
            copy_of(gated),
            copy_of(dqkv),
            copy_of(heads),
            copy_of(gb),
            pltpu.VMEM(hidden.shape, BF),
            pltpu.VMEM(down_weight.shape, BF),
            pltpu.VMEM(terms.shape, F32),
            pltpu.VMEM((parts,) + terms.shape[1:], F32),
        ]
        + scratch[-2:]
        + [dma(2, size - 1)] * 2
        + [dma(parts - 1)] * 2
        + [dma(7)]
        + line_sems(parts) * 3,
        compiler_params=pltpu.CompilerParams(
            collective_id=ident, has_side_effects=True, vmem_limit_bytes=67_000_000
        ),
        cost_estimate=pl.CostEstimate(
            flops=2 * size * rows * (down_weight.size + width * cols),
            bytes_accessed=500_000_000,
            transcendentals=0,
        ),
        name="close_part",
    )(gated, dqkv, heads, gb, gu_slots, terms, hidden, down_weight)[:4]


def pack_pair(out, pair, x, g, heads=None, gb=None):
    parts, _, piece, _ = out.shape
    rows = parts * piece
    full = dot_rows(x, g)
    side = None if heads is None else dot_rows(heads, gb)
    for k in range(2):
        own = full[k * rows : (k + 1) * rows]
        if side is not None:
            wide = side.shape[1] // 2
            own = jnp.concatenate([own, side[:, k * wide : (k + 1) * wide]], 1)
        out[:, pair * 2 + k] = own.astype(BF).reshape(parts, piece, own.shape[1])


def pack_kernel(x_ref, g_ref, out_ref):
    pack_pair(out_ref, 0, x_ref[...], g_ref[...])


def down_kernel(x_ref, g_ref, out_ref):
    out_ref[...] = dot_rows(x_ref[...], g_ref[...]).astype(BF)


def down_grad(x, g):
    total, inner = x.shape
    half = g.shape[1] // 2
    return pl.pallas_call(
        down_kernel,
        grid=(2,),
        out_shape=jax.ShapeDtypeStruct((inner, 2 * half), BF),
        in_specs=[
            pl.BlockSpec(x.shape, lambda i: (0, 0), pipeline_mode=pl.Buffered(1)),
            pl.BlockSpec((total, half), lambda i: (0, i)),
        ],
        out_specs=pl.BlockSpec((inner, half), lambda i: (0, i)),
        cost_estimate=pl.CostEstimate(
            flops=4 * total * inner * half,
            bytes_accessed=2 * (x.size + g.size) + 4 * inner * half,
            transcendentals=0,
        ),
        name="down_grad",
    )(x, g)


def packs(size, parts, width):
    return width // (size * parts) % 8 == 0 and 2 * width // size % 128 == 0


def pack_plain(parts, size, x, g, heads=None, gb=None):
    width, cols = x.shape[1], g.shape[1]
    piece = width // (size * parts)
    full = dot_rows(x, g).reshape(size, parts, piece, cols)
    if heads is not None:
        side = dot_rows(heads, gb).reshape(parts, piece, size, -1).transpose(2, 0, 1, 3)
        full = jnp.concatenate([full, side], 3)
    return full.transpose(1, 0, 2, 3).astype(BF)


def pack_grads(parts, size, x, g):
    total, width = x.shape
    cols = g.shape[1]
    if not packs(size, parts, width):
        return pack_plain(parts, size, x, g)
    piece = width // (size * parts)
    pair = pl.BlockSpec((total, 2 * width // size), lambda i: (0, i))
    whole = pl.BlockSpec(g.shape, lambda i: (0, 0), pipeline_mode=pl.Buffered(1))
    return pl.pallas_call(
        pack_kernel,
        grid=(size // 2,),
        out_shape=jax.ShapeDtypeStruct((parts, size, piece, cols), BF),
        in_specs=[pair, whole],
        out_specs=pl.BlockSpec((parts, 2, piece, cols), lambda i: (0, i, 0, 0)),
        cost_estimate=pl.CostEstimate(
            flops=2 * total * width * cols,
            bytes_accessed=2 * (x.size + g.size + width * cols),
            transcendentals=0,
        ),
        name="pack_grads",
    )(x, g)


def unpack_kernel(widths, *refs):
    outs = list(refs[len(widths) :])
    for every_ref, wide in zip(refs, widths):
        blocks = [every_ref[0, i].astype(F32) for i in range(every_ref.shape[1])]
        low = 0
        for width in wide:
            outs.pop(0)[...] = jnp.concatenate([b[:, low : low + width] for b in blocks], 1)
            low += width


def unpack_grads(arrays, widths):
    parts, size, piece, _ = arrays[0].shape
    every = [w for wide in widths for w in wide]
    if piece % 8:
        outs = []
        for array, wide in zip(arrays, widths):
            low = 0
            for width in wide:
                block = array[:, :, :, low : low + width].transpose(0, 2, 1, 3)
                outs.append(block.reshape(parts * piece, size * width).astype(F32))
                low += width
        return outs
    return pl.pallas_call(
        functools.partial(unpack_kernel, widths),
        grid=(parts,),
        out_shape=[jax.ShapeDtypeStruct((parts * piece, size * w), F32) for w in every],
        in_specs=[
            pl.BlockSpec((1, size, piece, a.shape[3]), lambda i: (i, 0, 0, 0)) for a in arrays
        ],
        out_specs=[pl.BlockSpec((piece, size * w), lambda i: (i, 0)) for w in every],
        cost_estimate=pl.CostEstimate(
            flops=0, bytes_accessed=6 * sum(a.size for a in arrays), transcendentals=0
        ),
        name="unpack_grads",
    )(*arrays)


def columns_piece(weights, part, parts):
    size = lax.axis_size("fsdp")
    rows = weights[0].shape[0] // parts
    pieces = []
    for weight in weights:
        own = lax.dynamic_slice_in_dim(weight, part * rows, rows, 0)
        pieces.append(own.reshape(rows, size, -1))
    return jnp.concatenate(pieces, 2).transpose(1, 0, 2)


def shards(
    tokens,
    seq_lengths,
    seq_offsets,
    norm1_gain,
    conv_weight,
    query_weight,
    key_weight,
    value_weight,
    out_weight,
    norm2_gain,
    gate_weight,
    up_weight,
    down_weight,
    cotangent,
):
    size = lax.axis_size("fsdp")
    parts = lax.axis_size("seq")
    part = lax.axis_index("seq")
    me = lax.axis_index("fsdp")
    own_tokens = tokens[0]
    rows, width = own_tokens.shape
    slice_width = norm1_gain.shape[0]
    first_slot = part * rows
    count = seq_lengths.shape[1]

    slot_ext = first_slot - 2 + jnp.arange(rows + 2, dtype=jnp.int32)
    segment_ext = segment_of(
        slot_ext, count, lambda j: seq_lengths[0, j], lambda j: seq_offsets[0, j]
    )
    segment_own = segment_ext[2:]
    same_one = (segment_own == segment_ext[1:-1]).astype(F32)[:, None]
    same_two = (segment_own == segment_ext[:-2]).astype(F32)[:, None]
    live_mask = (segment_own >= 0).astype(F32)[:, None]

    gains = jnp.concatenate(
        [
            norm1_gain[None],
            norm2_gain[None],
            conv_weight.T,
            jnp.zeros((3, slice_width), BF),
        ],
        0,
    )
    table = jnp.zeros((8, 128), jnp.int32)
    table = table.at[0, :count].set(seq_lengths[0]).at[1, :count].set(seq_offsets[0])
    qkv_piece = columns_piece((query_weight, key_weight, value_weight), part, parts)
    gu_piece = columns_piece((gate_weight, up_weight), part, parts)
    (
        gated_all,
        qkv,
        edge,
        qkv_map,
        middle,
        heads_out,
        grad_down_all,
        normed_all,
        hidden,
        grad_gu,
        gu_map,
        gains_all,
        table_all,
        edge_tokens,
    ) = forward_part(
        0,
        count,
        own_tokens,
        cotangent[0],
        gains,
        table,
        qkv_piece,
        gu_piece,
        out_weight,
        down_weight,
    )
    local = out_weight.shape[0]
    flat = lambda a: a.reshape(-1, a.shape[-1])
    lens_all, starts_all = table_all[:, 0, :count], table_all[:, 1, :count]
    gains_all = gains_all.transpose(1, 0, 2).reshape(8, width)
    norm_one = gains_all[0].astype(F32)
    norm_two = gains_all[1].astype(F32)
    taps = gains_all[2:5].astype(F32)
    qkv_map, gu_map = qkv_map.reshape(width, -1), gu_map.reshape(width, -1)

    extended = jnp.concatenate([edge_tokens[6:], own_tokens], 0).astype(F32)
    scale_one = lax.rsqrt(jnp.mean(extended * extended, axis=1, keepdims=True) + EPS)
    normed = extended * scale_one * norm_one
    conv_mix = (
        normed[2:] * taps[0]
        + same_one * normed[1:-1] * taps[1]
        + same_two * normed[:-2] * taps[2]
    )

    gu_packed = pack_grads(parts, size, flat(normed_all), flat(grad_gu))
    down_packed = down_grad(flat(hidden), flat(grad_down_all))
    grad_middle, norm2_term, grad_branch_all, dqkv, grad_gated, gu_slots, down_every = back_part(
        4,
        lens_all,
        starts_all,
        grad_gu,
        gu_map,
        middle,
        grad_down_all,
        norm_two[None],
        out_weight,
        edge,
        qkv,
        qkv_map,
        gu_packed,
        down_packed.reshape(parts, -1, width),
    )
    norm2_term = norm2_term[0]
    down_total = down_every.reshape(-1, width).astype(F32)
    normed_own = normed[2:]
    grad_mix = grad_gated * normed_own
    part_zero = jnp.pad(grad_gated * conv_mix + grad_mix * taps[0], ((2, 0), (0, 0)))
    part_one = jnp.pad(grad_mix * same_one * taps[1], ((1, 1), (0, 0)))
    part_two = jnp.pad(grad_mix * same_two * taps[2], ((0, 2), (0, 0)))
    grad_normed = part_zero + part_one + part_two
    unit_one = extended * scale_one
    grad_unit_one = grad_normed * norm_one
    grad_extended = scale_one * (
        grad_unit_one - unit_one * jnp.mean(grad_unit_one * unit_one, axis=1, keepdims=True)
    )
    edge_back = shifted(grad_extended[:2], "seq", -1)
    tokens_grad = grad_middle + grad_extended[2:] + jnp.pad(edge_back, ((rows - 2, 0), (0, 0)))

    terms = jnp.stack(
        [
            jnp.sum(grad_normed * unit_one, axis=0),
            norm2_term,
            jnp.sum(grad_mix * normed_own, axis=0),
            jnp.sum(grad_mix * same_one * normed[1:-1], axis=0),
            jnp.sum(grad_mix * same_two * normed[:-2], axis=0),
        ]
    )
    terms = jnp.pad(terms, ((0, 3), (0, 0))).reshape(8, size, slice_width).transpose(1, 0, 2)
    qkvo_every, gu_every, feed, terms = close_part(
        5,
        flat(gated_all),
        flat(dqkv),
        flat(heads_out),
        flat(grad_branch_all),
        gu_slots,
        terms,
        hidden,
        down_weight,
    )
    gate_total, up_total, query_total, key_total, value_total, out_total = unpack_grads(
        (gu_every, qkvo_every), ((gu_map.shape[1] // 2,) * 2, (local,) * 4)
    )

    layer_out = (live_mask * (middle + feed)).astype(BF)[None]
    return (
        layer_out,
        tokens_grad[None],
        terms[0],
        terms[2:5].T,
        query_total,
        key_total,
        value_total,
        out_total,
        terms[1],
        gate_total,
        up_total,
        down_total,
    )


def solution(mesh):
    placed = (
        P("fsdp", "seq", None),
        P("fsdp", None),
        P("fsdp", None),
        P("fsdp"),
        P("fsdp", None),
        P("fsdp", None),
        P("fsdp", None),
        P("fsdp", None),
        P("fsdp", None),
        P("fsdp"),
        P("fsdp", None),
        P("fsdp", None),
        P("fsdp", None),
        P("fsdp", "seq", None),
    )
    return jax.shard_map(
        shards,
        mesh=mesh,
        in_specs=placed,
        out_specs=(
            P("fsdp", "seq", None),
            P("fsdp", "seq", None),
            P("fsdp"),
            P("fsdp", None),
            P("fsdp", None),
            P("fsdp", None),
            P("fsdp", None),
            P("fsdp", None),
            P("fsdp"),
            P("fsdp", None),
            P("fsdp", None),
            P("fsdp", None),
        ),
        check_vma=False,
    )
```
